32 devices in a mesh: fs: 4 (over z), sp: 8 (over y, x, core).
Axes of the slice: x: 2, y: 2, z: 4, core: 2. Of those that a mesh axis runs over, the one named last changes fastest.
Arguments:
- layer_input: bfloat16 [8, 2048, 1024], P(None, ('fs', 'sp')), may hold values from -6 to 6
- first_gain: bfloat16 [1024], P('fs'), may hold values from 0.099609375 to 1.8984375
- first_shift: bfloat16 [1024], P('fs'), may hold values from -1.1953125 to 1.1953125
- joined_weight: bfloat16 [1024, 3072], P('fs'), may hold values from -0.1875 to 0.1875
- query_bias: bfloat16 [1024], P('fs'), may hold values from -1.1953125 to 1.1953125
- value_bias: bfloat16 [1024], P('fs'), may hold values from -1.1953125 to 1.1953125
- output_weight: bfloat16 [1024, 1024], P('fs'), may hold values from -0.5 to 0.5
- output_bias: bfloat16 [1024], P('fs'), may hold values from -1.1953125 to 1.1953125
- second_gain: bfloat16 [1024], P('fs'), may hold values from 0.099609375 to 1.8984375
- second_shift: bfloat16 [1024], P('fs'), may hold values from -1.1953125 to 1.1953125
- expand_weight: bfloat16 [1024, 4096], P('fs'), may hold values from -0.1875 to 0.1875
- expand_bias: bfloat16 [4096], P('fs'), may hold values from -1.1953125 to 1.1953125
- contract_weight: bfloat16 [4096, 1024], P('fs'), may hold values from -0.09375 to 0.09375
- contract_bias: bfloat16 [1024], P('fs'), may hold values from -1.1953125 to 1.1953125
- alibi_slopes: float32 [16], replicated, may hold values from 2.4414063e-05 to 0.04
- upstream: bfloat16 [8, 2048, 1024], P(None, ('fs', 'sp')), may hold values from -6 to 6
Outputs:
- layer_output: bfloat16 [8, 2048, 1024], P(None, ('fs', 'sp'))
- input_grad: bfloat16 [8, 2048, 1024], P(None, ('fs', 'sp'))
- first_gain_grad: float32 [1024], P(('fs', 'sp'))
- first_shift_grad: float32 [1024], P(('fs', 'sp'))
- joined_grad: float32 [1024, 3072], P(('fs', 'sp'))
- query_bias_grad: float32 [1024], P(('fs', 'sp'))
- value_bias_grad: float32 [1024], P(('fs', 'sp'))
- output_weight_grad: float32 [1024, 1024], P(('fs', 'sp'))
- output_bias_grad: float32 [1024], P(('fs', 'sp'))
- second_gain_grad: float32 [1024], P(('fs', 'sp'))
- second_shift_grad: float32 [1024], P(('fs', 'sp'))
- expand_grad: float32 [1024, 4096], P(('fs', 'sp'))
- expand_bias_grad: float32 [4096], P(('fs', 'sp'))
- contract_grad: float32 [4096, 1024], P(('fs', 'sp'))
- contract_bias_grad: float32 [1024], P(('fs', 'sp'))
The draws below stay inside these ranges and needn't reach their ends.
All inputs are finite; a program needn't handle non-finite values.
Results may differ from the reference program's by a relative error of at most 0.014.
Values may be sent and summed in bfloat16 or wider, within the bound.
A program may use at most 256 MiB of HBM per device.

```python
import math
from functools import partial
import jax
import jax.numpy as jnp
from jax import lax

D = 1024
H = 16
FF = 4096
SEQS = 8
SEQ_LEN = 2048


def with_spikes(values, rng, source, target, parts, factor):
    owner, partner = [(jnp.arange(values.shape[dim]) // (values.shape[dim] // parts)).reshape([-1 if axis == dim else 1 for axis in range(values.ndim)]) for dim in (source, target)]
    chosen = jax.random.permutation(rng, parts)[partner]
    strong = (owner == chosen) | (owner == (partner + parts // 2) % parts)
    return jnp.where(strong, factor * values, values)


def shard_levels(key, dims, split, least, largest):
    loudness, own = 1.0, jax.random.fold_in(key, 6)
    for axis_at, shards_of in split:
        steps = jnp.exp(jax.random.uniform(jax.random.fold_in(own, axis_at), (shards_of,), jnp.float32, least / len(split), largest / len(split)))
        loudness = loudness * jnp.repeat(steps, dims[axis_at] // shards_of).reshape([-1 if axis == axis_at else 1 for axis in range(len(dims))])
    return loudness


def scatter_about(own_key, extent, width, reach, split=(), held_as=jnp.bfloat16):
    array = width * jax.random.normal(own_key, extent, jnp.float32)
    if split:
        array = array * shard_levels(own_key, extent, split, -0.22, 0.18)
    return jnp.clip(array, -reach, reach).astype(held_as)


def gaussian_with(rng, shape, scale, most, cuts, heavy, kind=jnp.bfloat16):
    drawn = scale * jax.random.normal(rng, shape, jnp.float32)
    if cuts:
        drawn = drawn * shard_levels(rng, shape, cuts, -0.22, 0.18)
    return jnp.clip(with_spikes(drawn, jax.random.fold_in(rng, 3), *heavy), -most, most).astype(kind)


def setup_inputs(seed: int = 0) -> dict:
    seeds = jax.random.split(jax.random.key(seed), 17)
    layer_input = scatter_about(seeds[0], (SEQS, SEQ_LEN, D), 1.0, 6.0, ((1, 32),))
    first_gain = jnp.clip(1.0 + 0.18 * jax.random.normal(seeds[1], (D,), jnp.float32), 0.099609375, 1.8984375).astype(jnp.bfloat16)
    first_shift = scatter_about(seeds[2], (D,), 0.3, 1.1953125, ((0, 4),))
    joined_weight = scatter_about(seeds[3], (D, 3 * D), D ** -0.5, 0.1875, ((0, 4),))
    query_bias = scatter_about(seeds[4], (D,), 0.3, 1.1953125, ((0, 4),))
    value_bias = scatter_about(seeds[5], (D,), 0.3, 1.1953125, ((0, 4),))
    output_weight = scatter_about(seeds[6], (D, D), (D // 8) ** -0.5, 0.5, ((0, 4),))
    output_bias = scatter_about(seeds[7], (D,), 0.3, 1.1953125, ((0, 4),))
    second_gain = jnp.clip(1.0 + 0.18 * jax.random.normal(seeds[8], (D,), jnp.float32), 0.099609375, 1.8984375).astype(jnp.bfloat16)
    second_shift = scatter_about(seeds[9], (D,), 0.3, 1.1953125, ((0, 4),))
    expand_weight = scatter_about(seeds[10], (D, FF), D ** -0.5, 0.1875, ((0, 4),))
    expand_bias = scatter_about(seeds[11], (FF,), 0.3, 1.1953125, ((0, 4),))
    contract_weight = scatter_about(seeds[12], (FF, D), FF ** -0.5, 0.09375, ((0, 4),))
    contract_bias = scatter_about(seeds[13], (D,), 0.3, 1.1953125, ((0, 4),))
    alibi_slopes = jnp.clip(jnp.exp(jax.random.uniform(seeds[14], (H,), jnp.float32, math.log(2.441406286379788e-05), math.log(0.04))), 2.441406286379788e-05, 0.04)
    upstream = gaussian_with(seeds[15], (SEQS, SEQ_LEN, D), 1.0, 6.0, ((1, 32),), (1, 2, 32, 2.75))
    return dict(layer_input=layer_input, first_gain=first_gain, first_shift=first_shift, joined_weight=joined_weight, query_bias=query_bias, value_bias=value_bias, output_weight=output_weight, output_bias=output_bias, second_gain=second_gain, second_shift=second_shift, expand_weight=expand_weight, expand_bias=expand_bias, contract_weight=contract_weight, contract_bias=contract_bias, alibi_slopes=alibi_slopes, upstream=upstream)


norm_eps = 1e-05
gelu_coef = 0.7978845608028654
masked_value = -1e+30
highest = lax.Precision.HIGHEST

@jax.custom_vjp
def low(v):
    return lax.optimization_barrier(v.astype(jnp.bfloat16)).astype(jnp.float32)

@jax.custom_vjp
def low_back(v):
    return v

def low_keep(v):
    return (low(v), None)

def low_pass(kept, grad):
    return (grad,)

def back_keep(v):
    return (v, None)

def back_low(kept, grad):
    return (low(grad),)
low.defvjp(low_keep, low_pass)
low_back.defvjp(back_keep, back_low)

def matmul(left_side, right_side):
    return jnp.dot(left_side, right_side, precision=highest, preferred_element_type=jnp.float32)

def normalize(values, norm_gain, norm_shift):
    center = values - lax.optimization_barrier(jnp.mean(values, axis=-1, keepdims=True))
    variance = lax.optimization_barrier(jnp.mean(center * center, axis=-1, keepdims=True))
    return center * lax.rsqrt(variance + norm_eps) * norm_gain + norm_shift

def gelu_tanh(values):
    return 0.5 * values * (1.0 + jnp.tanh(gelu_coef * (values + 0.044715 * values * values * values)))

def attend(operands):
    queries, key_rows, value_rows, head_slope = operands
    length, head_dim = queries.shape
    scores = matmul(queries, key_rows.T) * (1.0 / math.sqrt(head_dim))
    position = jnp.arange(length, dtype=jnp.int32)
    distance = (position[None, :] - position[:, None]).astype(jnp.float32)
    scores = low_back(scores + head_slope * distance)
    scores = jnp.where(position[None, :] <= position[:, None], scores, masked_value)
    row_top = lax.optimization_barrier(jnp.max(scores, axis=-1, keepdims=True))
    exp_scores = jnp.exp(scores - row_top)
    probs_low = low(exp_scores / lax.optimization_barrier(jnp.sum(exp_scores, axis=-1, keepdims=True)))
    return low(low_back(matmul(probs_low, value_rows)))

def forward(alibi_slopes, layer_input, first_gain, first_shift, joined_weight, query_bias, value_bias, output_weight, output_bias, second_gain, second_shift, expand_weight, expand_bias, contract_weight, contract_bias):
    seq_count, length, features = layer_input.shape
    head_count = alibi_slopes.shape[0]
    head_dim = features // head_count
    tokens = layer_input.reshape(seq_count * length, features)
    normed = low(normalize(tokens, first_gain, first_shift))
    query_part = query_bias.reshape(head_count, head_dim)
    value_part = value_bias.reshape(head_count, head_dim)
    joined_bias = jnp.stack([query_part, jnp.zeros_like(query_part), value_part], axis=1).reshape(3 * features)
    joined_all = low(low_back(matmul(normed, joined_weight) + joined_bias))
    joined_all = joined_all.reshape(seq_count, length, head_count, 3, head_dim).transpose(0, 2, 3, 1, 4)
    joined_all = joined_all.reshape(seq_count * head_count, 3, length, head_dim)
    slope_list = jnp.tile(alibi_slopes, seq_count)
    attended = lax.map(jax.checkpoint(attend), (joined_all[:, 0], joined_all[:, 1], joined_all[:, 2], slope_list))
    attended = attended.reshape(seq_count, head_count, length, head_dim).transpose(0, 2, 1, 3)
    attended = attended.reshape(seq_count * length, features)
    branch = low_back(matmul(attended, output_weight) + output_bias)
    residual = tokens + branch
    second = low(normalize(residual, second_gain, second_shift))
    expanded = low_back(matmul(second, expand_weight) + expand_bias)
    activated = low(gelu_tanh(expanded))
    shrunk = low_back(matmul(activated, contract_weight) + contract_bias)
    return (residual + shrunk).reshape(seq_count, length, features)

def reference(layer_input, first_gain, first_shift, joined_weight, query_bias, value_bias, output_weight, output_bias, second_gain, second_shift, expand_weight, expand_bias, contract_weight, contract_bias, alibi_slopes, upstream):
    parameters = tuple((item.astype(jnp.float32) for item in (layer_input, first_gain, first_shift, joined_weight, query_bias, value_bias, output_weight, output_bias, second_gain, second_shift, expand_weight, expand_bias, contract_weight, contract_bias)))
    result, pullback = jax.vjp(partial(forward, alibi_slopes), *parameters)
    gradients = pullback(upstream.astype(jnp.float32))
    return (result.astype(jnp.bfloat16), gradients[0].astype(jnp.bfloat16), gradients[1], gradients[2], gradients[3], gradients[4], gradients[5], gradients[6], gradients[7], gradients[8], gradients[9], gradients[10], gradients[11], gradients[12], gradients[13])
```

```python
import functools
import math

import jax
import jax.numpy as jnp
from jax import lax
from jax.experimental import pallas as pl
from jax.experimental.pallas import tpu as pltpu
from jax.sharding import PartitionSpec as P

norm_eps = 1e-05
gelu_coef = 0.7978845608028654
masked_value = -1e30
f32 = jnp.float32
bf16 = jnp.bfloat16
MESH = pl.DeviceIdType.MESH
HBM = pl.BlockSpec(memory_space=pl.ANY)
VMEM = pl.BlockSpec(memory_space=pltpu.VMEM)
vmem_bytes = 60 * 1024 * 1024


def normalize(values, norm_gain, norm_shift):
    center = values - jnp.mean(values, axis=-1, keepdims=True)
    variance = jnp.mean(center * center, axis=-1, keepdims=True)
    return center * lax.rsqrt(variance + norm_eps) * norm_gain + norm_shift


def gelu_tanh(values):
    return (
        0.5 * values * (1.0 + jnp.tanh(gelu_coef * (values + 0.044715 * values * values * values)))
    )


def matmul(left_side, right_side):
    return jnp.dot(left_side, right_side, preferred_element_type=f32)


def matmul_lt(left_side, right_side):
    return lax.dot_general(
        left_side, right_side, (((0,), (0,)), ((), ())), preferred_element_type=f32
    )


def matmul_rt(left_side, right_side):
    return lax.dot_general(
        left_side, right_side, (((1,), (1,)), ((), ())), preferred_element_type=f32
    )


def joined_bias_of(query_bias, value_bias, head_count):
    query_part = query_bias.astype(f32).reshape(head_count, -1)
    value_part = value_bias.astype(f32).reshape(head_count, -1)
    return jnp.stack([query_part, jnp.zeros_like(query_part), value_part], axis=1).reshape(-1)


def split_three(values):
    high = values.astype(bf16).astype(f32)
    rest = values - high
    middle = rest.astype(bf16).astype(f32)
    return high, middle, rest - middle


def key_columns(key_rows, slope, start):
    rows, width = key_rows.shape
    position = (start + lax.broadcasted_iota(jnp.int32, (rows, width), 0)).astype(f32)
    lane = lax.broadcasted_iota(jnp.int32, (rows, width), 1)
    high, middle, low = split_three(slope * position)
    extra = jnp.where(lane == 0, high, jnp.where(lane == 1, middle, jnp.where(lane == 2, low, 0.0)))
    return jnp.concatenate([key_rows.astype(f32), extra], axis=1).astype(bf16)


def query_columns(queries, scale):
    rows, width = queries.shape
    lane = lax.broadcasted_iota(jnp.int32, (rows, width), 1)
    ones = jnp.where(lane < 3, 1.0, 0.0)
    return jnp.concatenate([queries.astype(f32) * scale, ones], axis=1).astype(bf16)


def forward_kernel(heads, width, block, slopes, qkv, out, out_t, lse, keys, queries, values_t):
    seqs, length, _ = qkv.shape
    blocks = length // block
    scale = 1.0 / math.sqrt(width)

    def one_seq(b, _):
        def prepare(i, _):
            start = pl.multiple_of(i * block, block)
            rows = pl.ds(start, block)
            for h in range(heads):
                base = h * 3 * width
                keys[h, rows, :] = key_columns(
                    qkv[b, rows, base + width : base + 2 * width], slopes[h], start
                )
                queries[h, rows, :] = query_columns(qkv[b, rows, base : base + width], scale)
                value = qkv[b, rows, base + 2 * width : base + 3 * width]
                values_t[h, :, rows] = value.astype(f32).T.astype(bf16)
            return 0

        lax.fori_loop(0, blocks, prepare, 0)

        def one_block(i, _):
            rows = pl.ds(pl.multiple_of(i * block, block), block)
            query = [queries[h, rows, :] for h in range(heads)]

            def step(j, state, diagonal):
                columns = pl.ds(pl.multiple_of(j * block, block), block)
                result = []
                for h in range(heads):
                    top, total, acc = state[h]
                    scores = matmul_rt(keys[h, columns, :], query[h])
                    if diagonal:
                        key_at = lax.broadcasted_iota(jnp.int32, (block, block), 0)
                        query_at = lax.broadcasted_iota(jnp.int32, (block, block), 1)
                        scores = jnp.where(key_at <= query_at, scores, masked_value)
                    newest = jnp.maximum(top, jnp.max(scores, axis=0, keepdims=True))
                    shrink = jnp.exp(top - newest)
                    probs = jnp.exp(scores - newest)
                    total = total * shrink + jnp.sum(probs, axis=0, keepdims=True)
                    acc = acc * shrink + matmul(values_t[h, :, columns], probs.astype(bf16))
                    result.append((newest, total, acc))
                return tuple(result)

            state = tuple(
                (
                    jnp.full((1, block), masked_value, f32),
                    jnp.zeros((1, block), f32),
                    jnp.zeros((width, block), f32),
                )
                for h in range(heads)
            )
            state = lax.fori_loop(0, i, lambda j, s: step(j, s, False), state)
            state = step(i, state, True)
            finished = []
            for h in range(heads):
                top, total, acc = state[h]
                result = acc / total
                out_t[b, h, :, rows] = result
                lse[b, h, :, rows] = top + jnp.log(total)
                finished.append(result)
            joined = finished[0] if heads == 1 else jnp.concatenate(finished, axis=0)
            out[b, rows, :] = joined.T.astype(bf16)
            return 0

        lax.fori_loop(0, blocks, one_block, 0)
        return 0

    lax.fori_loop(0, seqs, one_seq, 0)


def attention_forward(qkv, slopes, heads, width):
    seqs, length, _ = qkv.shape
    block = min(512, length)
    return pl.pallas_call(
        functools.partial(forward_kernel, heads, width, block),
        name="attention_forward",
        out_shape=(
            jax.ShapeDtypeStruct((seqs, length, heads * width), bf16),
            jax.ShapeDtypeStruct((seqs, heads, width, length), f32),
            jax.ShapeDtypeStruct((seqs, heads, 1, length), f32),
        ),
        in_specs=[pl.BlockSpec(memory_space=pltpu.SMEM), VMEM],
        out_specs=(VMEM, VMEM, VMEM),
        scratch_shapes=[
            pltpu.VMEM((heads, length, 2 * width), bf16),
            pltpu.VMEM((heads, length, 2 * width), bf16),
            pltpu.VMEM((heads, width, length), bf16),
        ],
        compiler_params=pltpu.CompilerParams(vmem_limit_bytes=vmem_bytes),
    )(slopes, qkv)


def backward_kernel(
    heads, width, block, slopes, qkv, diff, out_t, lse, joined,
    keys, queries, keys_t, values, diffs, delta, query_acc,
):
    seqs, length, _ = qkv.shape
    blocks = length // block
    scale = 1.0 / math.sqrt(width)

    def one_seq(b, _):
        def prepare(i, _):
            start = pl.multiple_of(i * block, block)
            rows = pl.ds(start, block)
            for h in range(heads):
                base = h * 3 * width
                key = qkv[b, rows, base + width : base + 2 * width]
                keys[h, rows, :] = key_columns(key, slopes[h], start)
                keys_t[h, :, rows] = key.astype(f32).T.astype(bf16)
                queries[h, rows, :] = query_columns(qkv[b, rows, base : base + width], scale)
                values[h, rows, :] = qkv[b, rows, base + 2 * width : base + 3 * width]
                part = diff[b, rows, h * width : (h + 1) * width]
                diffs[h, rows, :] = part
                delta[h, :, rows] = jnp.sum(
                    part.astype(f32).T * out_t[b, h, :, rows], axis=0, keepdims=True
                )
                query_acc[h, :, rows] = jnp.zeros((width, block), f32)
            return 0

        lax.fori_loop(0, blocks, prepare, 0)

        def one_block(j, _):
            columns = pl.ds(pl.multiple_of(j * block, block), block)

            def step(i, state, diagonal):
                rows = pl.ds(pl.multiple_of(i * block, block), block)
                result = []
                for h in range(heads):
                    key_acc, value_acc = state[h]
                    query = queries[h, rows, :]
                    part = diffs[h, rows, :]
                    scores = matmul_rt(keys[h, columns, :], query)
                    probs = jnp.exp(scores - lse[b, h, :, rows])
                    if diagonal:
                        key_at = lax.broadcasted_iota(jnp.int32, (block, block), 0)
                        query_at = lax.broadcasted_iota(jnp.int32, (block, block), 1)
                        probs = jnp.where(key_at <= query_at, probs, 0.0)
                    prob_diff = matmul_rt(values[h, columns, :], part)
                    score_diff = (probs * (prob_diff - delta[h, :, rows])).astype(bf16)
                    value_acc = value_acc + matmul(probs.astype(bf16), part)
                    key_acc = key_acc + matmul(score_diff, query)
                    query_acc[h, :, rows] += matmul(keys_t[h, :, columns], score_diff)
                    result.append((key_acc, value_acc))
                return tuple(result)

            state = tuple(
                (jnp.zeros((block, 2 * width), f32), jnp.zeros((block, width), f32))
                for h in range(heads)
            )
            state = step(j, state, True)
            state = lax.fori_loop(j + 1, blocks, lambda i, s: step(i, s, False), state)
            for h in range(heads):
                base = h * 3 * width
                key_acc, value_acc = state[h]
                joined[b, columns, base + width : base + 2 * width] = key_acc[:, :width].astype(bf16)
                joined[b, columns, base + 2 * width : base + 3 * width] = value_acc.astype(bf16)
            return 0

        lax.fori_loop(0, blocks, one_block, 0)

        def finish(i, _):
            rows = pl.ds(pl.multiple_of(i * block, block), block)
            for h in range(heads):
                base = h * 3 * width
                joined[b, rows, base : base + width] = (
                    (query_acc[h, :, rows] * scale).T.astype(bf16)
                )
            return 0

        lax.fori_loop(0, blocks, finish, 0)
        return 0

    lax.fori_loop(0, seqs, one_seq, 0)


def attention_backward(qkv, diff, out_t, lse, slopes, heads, width):
    seqs, length, _ = qkv.shape
    block = min(512, length)
    return pl.pallas_call(
        functools.partial(backward_kernel, heads, width, block),
        name="attention_backward",
        out_shape=jax.ShapeDtypeStruct((seqs, length, heads * 3 * width), bf16),
        in_specs=[pl.BlockSpec(memory_space=pltpu.SMEM), VMEM, VMEM, VMEM, VMEM],
        out_specs=VMEM,
        scratch_shapes=[
            pltpu.VMEM((heads, length, 2 * width), bf16),
            pltpu.VMEM((heads, length, 2 * width), bf16),
            pltpu.VMEM((heads, width, length), bf16),
            pltpu.VMEM((heads, length, width), bf16),
            pltpu.VMEM((heads, length, width), bf16),
            pltpu.VMEM((heads, 1, length), f32),
            pltpu.VMEM((heads, width, length), f32),
        ],
        compiler_params=pltpu.CompilerParams(vmem_limit_bytes=vmem_bytes),
    )(slopes, qkv, diff, out_t, lse)


def to_own_seqs(values):
    seqs, piece, features = values.shape
    parts = lax.axis_size("fs")
    values = values.reshape(parts, seqs // parts, piece, features)
    return lax.all_to_all(values, "fs", split_axis=0, concat_axis=0).transpose(1, 0, 2, 3)


def from_own_seqs(values):
    own, parts, piece, features = values.shape
    values = lax.all_to_all(values.transpose(1, 0, 2, 3), "fs", split_axis=0, concat_axis=0)
    return values.reshape(parts * own, piece, features)


def to_heads(values):
    own, parts, piece, features = values.shape
    ranks = lax.axis_size("sp")
    values = values.reshape(own, parts, piece, ranks, features // ranks)
    values = lax.all_to_all(values, "sp", split_axis=3, concat_axis=2)
    return values.reshape(own, parts * ranks * piece, features // ranks)


def from_heads(values, parts, piece):
    own, _, features = values.shape
    ranks = lax.axis_size("sp")
    values = values.reshape(own, parts, ranks, piece, features)
    values = lax.all_to_all(values, "sp", split_axis=2, concat_axis=3)
    return values.reshape(own, parts, piece, ranks * features)


def per_device(
    layer_input,
    first_gain,
    first_shift,
    joined_weight,
    query_bias,
    value_bias,
    output_weight,
    output_bias,
    second_gain,
    second_shift,
    expand_weight,
    expand_bias,
    contract_weight,
    contract_bias,
    alibi_slopes,
    upstream,
):
    seqs, piece, features = layer_input.shape
    fs_count = lax.axis_size("fs")
    sp_count = lax.axis_size("sp")
    head_count = alibi_slopes.shape[0]
    width = features // head_count
    heads = head_count // sp_count
    rows = seqs * piece
    own = seqs // fs_count
    shape = (own, fs_count, piece)
    slopes = lax.dynamic_slice_in_dim(alibi_slopes, lax.axis_index("sp") * heads, heads)

    vectors = (
        first_gain, first_shift, query_bias, value_bias, output_bias,
        second_gain, second_shift, contract_bias, expand_bias,
    )
    packed = lax.all_gather(jnp.concatenate(vectors), "fs", axis=0)
    whole, at = [], 0
    for item in vectors:
        whole.append(packed[:, at : at + item.shape[0]].reshape(-1))
        at += item.shape[0]
    gain_one, shift_one, qbias, vbias, obias, gain_two, shift_two, cbias, ebias = [
        item.astype(f32) for item in whole
    ]
    gather = lambda item: lax.all_gather(item, "fs", axis=0, tiled=True)
    joined_full, out_full = gather(joined_weight), gather(output_weight)
    expand_full, contract_full = gather(expand_weight), gather(contract_weight)

    tokens = to_own_seqs(layer_input).reshape(rows, features).astype(f32)
    upstream_low = to_own_seqs(upstream).reshape(rows, features)

    normed_f, norm_back_one = jax.vjp(normalize, tokens, gain_one, shift_one)
    normed = normed_f.astype(bf16)
    joined_all = (matmul(normed, joined_full) + joined_bias_of(qbias, vbias, head_count)).astype(
        bf16
    )
    qkv = to_heads(joined_all.reshape(*shape, 3 * features))
    attended_heads, out_t, lse = attention_forward(qkv, slopes, heads, width)
    attended = from_heads(attended_heads, fs_count, piece).reshape(rows, features)

    residual = tokens + (matmul(attended, out_full) + obias)
    second_f, norm_back_two = jax.vjp(normalize, residual, gain_two, shift_two)
    second = second_f.astype(bf16)
    expanded = matmul(second, expand_full) + ebias
    activated_f, gelu_back = jax.vjp(gelu_tanh, expanded)
    activated = activated_f.astype(bf16)
    result = residual + (matmul(activated, contract_full) + cbias)
    layer_output = from_own_seqs(result.astype(bf16).reshape(*shape, features))

    upstream_f = upstream_low.astype(f32)
    contract_grad = matmul_lt(activated, upstream_low)
    contract_bias_grad = jnp.sum(upstream_f, axis=0)
    act_grad = matmul_rt(upstream_low, contract_full)
    expand_diff = gelu_back(act_grad)[0].astype(bf16)
    expand_grad = matmul_lt(second, expand_diff)
    expand_bias_grad = jnp.sum(expand_diff.astype(f32), axis=0)
    second_back = matmul_rt(expand_diff, expand_full)
    resid_part, second_gain_grad, second_shift_grad = norm_back_two(second_back)
    residual_grad = upstream_f + resid_part

    branch_diff = residual_grad.astype(bf16)
    output_weight_grad = matmul_lt(attended, branch_diff)
    output_bias_grad = jnp.sum(branch_diff.astype(f32), axis=0)
    attended_diff = matmul_rt(branch_diff, out_full).astype(bf16)
    diff_heads = to_heads(attended_diff.reshape(*shape, features))
    joined_heads = attention_backward(qkv, diff_heads, out_t, lse, slopes, heads, width)
    joined_diff = from_heads(joined_heads, fs_count, piece).reshape(rows, 3 * features)

    joined_grad = matmul_lt(normed, joined_diff)
    column_sums = jnp.sum(joined_diff.astype(f32), axis=0).reshape(head_count, 3, width)
    query_bias_grad = column_sums[:, 0].reshape(features)
    value_bias_grad = column_sums[:, 2].reshape(features)
    normed_back = matmul_rt(joined_diff, joined_full)
    input_part, first_gain_grad, first_shift_grad = norm_back_one(normed_back)
    input_grad = (residual_grad + input_part).astype(bf16)
    input_grad = from_own_seqs(input_grad.reshape(*shape, features))

    scatter = lambda item: lax.psum_scatter(
        item, ("fs", "sp"), scatter_dimension=0, tiled=True
    )
    vector_grads = (
        first_gain_grad, first_shift_grad, query_bias_grad, value_bias_grad, output_bias_grad,
        second_gain_grad, second_shift_grad, contract_bias_grad, expand_bias_grad,
    )
    devices = fs_count * sp_count
    packed = jnp.concatenate([item.reshape(devices, -1) for item in vector_grads], axis=1)
    packed = scatter(packed.reshape(-1))
    own_grads, at = [], 0
    for item in vector_grads:
        size = item.shape[0] // devices
        own_grads.append(packed[at : at + size])
        at += size
    g1, s1, qb, vb, ob, g2, s2, cb, eb = own_grads
    return (
        layer_output,
        input_grad,
        g1,
        s1,
        scatter(joined_grad),
        qb,
        vb,
        scatter(output_weight_grad),
        ob,
        g2,
        s2,
        scatter(expand_grad),
        eb,
        scatter(contract_grad),
        cb,
    )


def solution(mesh):
    tokens = P(None, ("fs", "sp"), None)
    both, both_rows = P(("fs", "sp")), P(("fs", "sp"), None)
    one, one_rows = P("fs"), P("fs", None)
    return jax.shard_map(
        per_device,
        mesh=mesh,
        in_specs=(
            tokens, one, one, one_rows, one, one, one_rows, one, one, one, one_rows, one,
            one_rows, one, P(), tokens,
        ),
        out_specs=(
            tokens, tokens, both, both, both_rows, both, both, both_rows, both, both, both,
            both_rows, both, both_rows, both,
        ),
        check_vma=False,
    )
```

```python
import functools
import math

import jax
import jax.numpy as jnp
from jax import lax
from jax.experimental import pallas as pl
from jax.experimental.pallas import tpu as pltpu
from jax.sharding import PartitionSpec as P

norm_eps = 1e-05
gelu_coef = 0.7978845608028654
masked_value = -1e30
f32 = jnp.float32
bf16 = jnp.bfloat16
MESH = pl.DeviceIdType.MESH
HBM = pl.BlockSpec(memory_space=pl.ANY)
VMEM = pl.BlockSpec(memory_space=pltpu.VMEM)
vmem_bytes = 60 * 1024 * 1024


def normalize(values, norm_gain, norm_shift):
    center = values - jnp.mean(values, axis=-1, keepdims=True)
    variance = jnp.mean(center * center, axis=-1, keepdims=True)
    return center * lax.rsqrt(variance + norm_eps) * norm_gain + norm_shift


def gelu_tanh(values):
    return (
        0.5 * values * (1.0 + jnp.tanh(gelu_coef * (values + 0.044715 * values * values * values)))
    )


def matmul(left_side, right_side):
    return jnp.dot(left_side, right_side, preferred_element_type=f32)


def matmul_lt(left_side, right_side):
    return lax.dot_general(
        left_side, right_side, (((0,), (0,)), ((), ())), preferred_element_type=f32
    )


def matmul_rt(left_side, right_side):
    return lax.dot_general(
        left_side, right_side, (((1,), (1,)), ((), ())), preferred_element_type=f32
    )


def joined_bias_of(query_bias, value_bias, head_count):
    query_part = query_bias.astype(f32).reshape(head_count, -1)
    value_part = value_bias.astype(f32).reshape(head_count, -1)
    return jnp.stack([query_part, jnp.zeros_like(query_part), value_part], axis=1).reshape(-1)


def split_three(values):
    high = values.astype(bf16).astype(f32)
    rest = values - high
    middle = rest.astype(bf16).astype(f32)
    return high, middle, rest - middle


def key_columns(key_rows, slope, start):
    rows, width = key_rows.shape
    position = (start + lax.broadcasted_iota(jnp.int32, (rows, width), 0)).astype(f32)
    lane = lax.broadcasted_iota(jnp.int32, (rows, width), 1)
    high, middle, low = split_three(slope * position)
    extra = jnp.where(lane == 0, high, jnp.where(lane == 1, middle, jnp.where(lane == 2, low, 0.0)))
    return jnp.concatenate([key_rows.astype(f32), extra], axis=1).astype(bf16)


def query_columns(queries, scale):
    rows, width = queries.shape
    lane = lax.broadcasted_iota(jnp.int32, (rows, width), 1)
    ones = jnp.where(lane < 3, 1.0, 0.0)
    return jnp.concatenate([queries.astype(f32) * scale, ones], axis=1).astype(bf16)


def forward_kernel(heads, width, block, slopes, qkv, out, out_t, lse, keys, queries, values_t):
    seqs, length, _ = qkv.shape
    blocks = length // block
    scale = 1.0 / math.sqrt(width)

    def one_seq(b, _):
        def prepare(i, _):
            start = pl.multiple_of(i * block, block)
            rows = pl.ds(start, block)
            for h in range(heads):
                base = h * 3 * width
                keys[h, rows, :] = key_columns(
                    qkv[b, rows, base + width : base + 2 * width], slopes[h], start
                )
                queries[h, rows, :] = query_columns(qkv[b, rows, base : base + width], scale)
                value = qkv[b, rows, base + 2 * width : base + 3 * width]
                values_t[h, :, rows] = value.astype(f32).T.astype(bf16)
            return 0

        lax.fori_loop(0, blocks, prepare, 0)

        def one_block(i, _):
            rows = pl.ds(pl.multiple_of(i * block, block), block)
            query = [queries[h, rows, :] for h in range(heads)]

            def step(j, state, diagonal):
                columns = pl.ds(pl.multiple_of(j * block, block), block)
                result = []
                for h in range(heads):
                    top, total, acc = state[h]
                    scores = matmul_rt(keys[h, columns, :], query[h])
                    if diagonal:
                        key_at = lax.broadcasted_iota(jnp.int32, (block, block), 0)
                        query_at = lax.broadcasted_iota(jnp.int32, (block, block), 1)
                        scores = jnp.where(key_at <= query_at, scores, masked_value)
                    newest = jnp.maximum(top, jnp.max(scores, axis=0, keepdims=True))
                    shrink = jnp.exp(top - newest)
                    probs = jnp.exp(scores - newest)
                    total = total * shrink + jnp.sum(probs, axis=0, keepdims=True)
                    acc = acc * shrink + matmul(values_t[h, :, columns], probs.astype(bf16))
                    result.append((newest, total, acc))
                return tuple(result)

            state = tuple(
                (
                    jnp.full((1, block), masked_value, f32),
                    jnp.zeros((1, block), f32),
                    jnp.zeros((width, block), f32),
                )
                for h in range(heads)
            )
            state = lax.fori_loop(0, i, lambda j, s: step(j, s, False), state)
            state = step(i, state, True)
            finished = []
            for h in range(heads):
                top, total, acc = state[h]
                result = acc / total
                out_t[b, h, :, rows] = result
                lse[b, h, :, rows] = top + jnp.log(total)
                finished.append(result)
            joined = finished[0] if heads == 1 else jnp.concatenate(finished, axis=0)
            out[b, rows, :] = joined.T.astype(bf16)
            return 0

        lax.fori_loop(0, blocks, one_block, 0)
        return 0

    lax.fori_loop(0, seqs, one_seq, 0)


def attention_forward(qkv, slopes, heads, width):
    seqs, length, _ = qkv.shape
    block = min(512, length)
    return pl.pallas_call(
        functools.partial(forward_kernel, heads, width, block),
        name="attention_forward",
        out_shape=(
            jax.ShapeDtypeStruct((seqs, length, heads * width), bf16),
            jax.ShapeDtypeStruct((seqs, heads, width, length), f32),
            jax.ShapeDtypeStruct((seqs, heads, 1, length), f32),
        ),
        in_specs=[pl.BlockSpec(memory_space=pltpu.SMEM), VMEM],
        out_specs=(VMEM, VMEM, VMEM),
        scratch_shapes=[
            pltpu.VMEM((heads, length, 2 * width), bf16),
            pltpu.VMEM((heads, length, 2 * width), bf16),
            pltpu.VMEM((heads, width, length), bf16),
        ],
        compiler_params=pltpu.CompilerParams(vmem_limit_bytes=vmem_bytes),
    )(slopes, qkv)


def backward_kernel(
    heads, width, block, slopes, qkv, diff, out_t, lse, joined,
    keys, queries, keys_t, values, diffs, delta, query_acc,
):
    seqs, length, _ = qkv.shape
    blocks = length // block
    scale = 1.0 / math.sqrt(width)

    def one_seq(b, _):
        def prepare(i, _):
            start = pl.multiple_of(i * block, block)
            rows = pl.ds(start, block)
            for h in range(heads):
                base = h * 3 * width
                key = qkv[b, rows, base + width : base + 2 * width]
                keys[h, rows, :] = key_columns(key, slopes[h], start)
                keys_t[h, :, rows] = key.astype(f32).T.astype(bf16)
                queries[h, rows, :] = query_columns(qkv[b, rows, base : base + width], scale)
                values[h, rows, :] = qkv[b, rows, base + 2 * width : base + 3 * width]
                part = diff[b, rows, h * width : (h + 1) * width]
                diffs[h, rows, :] = part
                delta[h, :, rows] = jnp.sum(
                    part.astype(f32).T * out_t[b, h, :, rows], axis=0, keepdims=True
                )
                query_acc[h, :, rows] = jnp.zeros((width, block), f32)
            return 0

        lax.fori_loop(0, blocks, prepare, 0)

        def one_block(j, _):
            columns = pl.ds(pl.multiple_of(j * block, block), block)

            def step(i, state, diagonal):
                rows = pl.ds(pl.multiple_of(i * block, block), block)
                result = []
                for h in range(heads):
                    key_acc, value_acc = state[h]
                    query = queries[h, rows, :]
                    part = diffs[h, rows, :]
                    scores = matmul_rt(keys[h, columns, :], query)
                    probs = jnp.exp(scores - lse[b, h, :, rows])
                    if diagonal:
                        key_at = lax.broadcasted_iota(jnp.int32, (block, block), 0)
                        query_at = lax.broadcasted_iota(jnp.int32, (block, block), 1)
                        probs = jnp.where(key_at <= query_at, probs, 0.0)
                    prob_diff = matmul_rt(values[h, columns, :], part)
                    score_diff = (probs * (prob_diff - delta[h, :, rows])).astype(bf16)
                    value_acc = value_acc + matmul(probs.astype(bf16), part)
                    key_acc = key_acc + matmul(score_diff, query)
                    query_acc[h, :, rows] += matmul(keys_t[h, :, columns], score_diff)
                    result.append((key_acc, value_acc))
                return tuple(result)

            state = tuple(
                (jnp.zeros((block, 2 * width), f32), jnp.zeros((block, width), f32))
                for h in range(heads)
            )
            state = step(j, state, True)
            state = lax.fori_loop(j + 1, blocks, lambda i, s: step(i, s, False), state)
            for h in range(heads):
                base = h * 3 * width
                key_acc, value_acc = state[h]
                joined[b, columns, base + width : base + 2 * width] = key_acc[:, :width].astype(bf16)
                joined[b, columns, base + 2 * width : base + 3 * width] = value_acc.astype(bf16)
            return 0

        lax.fori_loop(0, blocks, one_block, 0)

        def finish(i, _):
            rows = pl.ds(pl.multiple_of(i * block, block), block)
            for h in range(heads):
                base = h * 3 * width
                joined[b, rows, base : base + width] = (
                    (query_acc[h, :, rows] * scale).T.astype(bf16)
                )
            return 0

        lax.fori_loop(0, blocks, finish, 0)
        return 0

    lax.fori_loop(0, seqs, one_seq, 0)


def attention_backward(qkv, diff, out_t, lse, slopes, heads, width):
    seqs, length, _ = qkv.shape
    block = min(512, length)
    return pl.pallas_call(
        functools.partial(backward_kernel, heads, width, block),
        name="attention_backward",
        out_shape=jax.ShapeDtypeStruct((seqs, length, heads * 3 * width), bf16),
        in_specs=[pl.BlockSpec(memory_space=pltpu.SMEM), VMEM, VMEM, VMEM, VMEM],
        out_specs=VMEM,
        scratch_shapes=[
            pltpu.VMEM((heads, length, 2 * width), bf16),
            pltpu.VMEM((heads, length, 2 * width), bf16),
            pltpu.VMEM((heads, width, length), bf16),
            pltpu.VMEM((heads, length, width), bf16),
            pltpu.VMEM((heads, length, width), bf16),
            pltpu.VMEM((heads, 1, length), f32),
            pltpu.VMEM((heads, width, length), f32),
        ],
        compiler_params=pltpu.CompilerParams(vmem_limit_bytes=vmem_bytes),
    )(slopes, qkv, diff, out_t, lse)


def to_own_seqs(values):
    seqs, piece, features = values.shape
    parts = lax.axis_size("fs")
    values = values.reshape(parts, seqs // parts, piece, features)
    return lax.all_to_all(values, "fs", split_axis=0, concat_axis=0).transpose(1, 0, 2, 3)


def from_own_seqs(values):
    own, parts, piece, features = values.shape
    values = lax.all_to_all(values.transpose(1, 0, 2, 3), "fs", split_axis=0, concat_axis=0)
    return values.reshape(parts * own, piece, features)


def to_heads(values):
    own, parts, piece, features = values.shape
    ranks = lax.axis_size("sp")
    values = values.reshape(own, parts, piece, ranks, features // ranks)
    values = lax.all_to_all(values, "sp", split_axis=3, concat_axis=2)
    return values.reshape(own, parts * ranks * piece, features // ranks)


def from_heads(values, parts, piece):
    own, _, features = values.shape
    ranks = lax.axis_size("sp")
    values = values.reshape(own, parts, ranks, piece, features)
    values = lax.all_to_all(values, "sp", split_axis=2, concat_axis=3)
    return values.reshape(own, parts, piece, ranks * features)


class Copies:
    def __init__(self, send, recv):
        self.send, self.recv, self.used, self.made = send, recv, 0, []

    def start(self, source, target, device):
        copy = pltpu.make_async_remote_copy(
            src_ref=source,
            dst_ref=target,
            send_sem=self.send.at[self.used],
            recv_sem=self.recv.at[self.used],
            device_id=device,
            device_id_type=MESH,
        )
        self.used += 1
        self.made.append(copy)
        copy.start()
        return copy

    def finish(self):
        assert self.used == self.send.shape[0]
        for copy in self.made:
            copy.wait_send()


class Locals:
    def __init__(self, sems):
        self.sems, self.used = sems, 0

    def start(self, source, target):
        copy = pltpu.make_async_copy(source, target, self.sems.at[self.used])
        self.used += 1
        copy.start()
        return copy


def arrive(copies):
    for copy in copies:
        copy.wait_recv()


def greet(devices):
    barrier = pltpu.get_barrier_semaphore()
    for device in devices:
        pl.semaphore_signal(barrier, inc=1, device_id=device, device_id_type=MESH)
    pl.semaphore_wait(barrier, len(devices))


def place():
    z, s = lax.axis_index("fs"), lax.axis_index("sp")
    along_x = s + 2 - 4 * ((s // 2) % 2)
    along_y = s + 4 - 8 * (s // 4)
    partner = s + 1 - 2 * (s % 2)
    return z, s, along_x, along_y, partner


def gather_kernel(count, *refs):
    seq_in, vector_in, weights = refs[:2], refs[2], refs[3 : 3 + count]
    refs = refs[3 + count :]
    seq_out, vector_out, wholes = refs[:2], refs[2], refs[3 : 3 + count]
    refs = refs[3 + count :]
    seq_own, vector_own, weight_own = refs[:2], refs[2], refs[3 : 3 + count]
    send, recv, local = refs[3 + count :]
    z, s, along_x, along_y, partner = place()
    diagonal = along_x + along_y - s
    lines = [(lax.rem(z + k, 4), s) for k in range(1, 4)]
    to_x, to_y, to_core = (z, along_x), (z, along_y), (z, partner)
    copies, locals_ = Copies(send, recv), Locals(local)
    greet(lines + [to_x, to_y, to_core])

    own_in = [locals_.start(item.at[z], kept) for item, kept in zip(seq_in, seq_own)]
    own_in.append(locals_.start(vector_in, vector_own))
    own_in += [locals_.start(item, kept) for item, kept in zip(weights, weight_own)]
    waiting = []
    for to in lines:
        waiting.append(copies.start(seq_in[0].at[to[0]], seq_out[0].at[:, z], to))
        waiting.append(copies.start(vector_in, vector_out.at[z], to))
    first = []
    for item, whole in zip(weights, wholes):
        first.append([copies.start(item.at[s], whole.at[z, s], to) for to in lines])
    for to in lines:
        waiting.append(copies.start(seq_in[1].at[to[0]], seq_out[1].at[:, z], to))
    for copy in own_in:
        copy.wait()
    own_out = [locals_.start(kept, item.at[:, z]) for item, kept in zip(seq_out, seq_own)]
    own_out.append(locals_.start(vector_own, vector_out.at[z]))
    own_out += [locals_.start(kept, item.at[z]) for item, kept in zip(wholes, weight_own)]

    def same(whole, where, to):
        return copies.start(whole.at[where], whole.at[where], to)

    second, third = [], []
    for t in range(count + 2):
        if t < count:
            whole = wholes[t]
            half = whole.shape[2] // 2
            low, high, every = pl.ds(0, half), pl.ds(half, half), pl.ds(0, 2 * half)
            arrive(first[t])
            step = []
            for k, _ in lines:
                step.append(same(whole, (k, s, low), to_x))
                step.append(same(whole, (k, s, high), to_y))
                waiting.append(same(whole, (k, s, every), to_core))
            second.append(step)
        if 0 <= t - 1 < count:
            whole = wholes[t - 1]
            half = whole.shape[2] // 2
            low, high = pl.ds(0, half), pl.ds(half, half)
            arrive(second[t - 1])
            step = []
            for k, _ in lines:
                step.append(same(whole, (k, s, low), to_y))
                step.append(same(whole, (k, along_x, low), to_y))
                step.append(same(whole, (k, s, high), to_x))
                step.append(same(whole, (k, along_y, high), to_x))
                waiting.append(same(whole, (k, along_x, low), to_core))
                waiting.append(same(whole, (k, along_y, high), to_core))
            third.append(step)
        if 0 <= t - 2 < count:
            whole = wholes[t - 2]
            half = whole.shape[2] // 2
            low, high = pl.ds(0, half), pl.ds(half, half)
            arrive(third[t - 2])
            for k, _ in lines:
                waiting.append(same(whole, (k, along_y, low), to_core))
                waiting.append(same(whole, (k, diagonal, low), to_core))
                waiting.append(same(whole, (k, along_x, high), to_core))
                waiting.append(same(whole, (k, diagonal, high), to_core))
    arrive(waiting)
    copies.finish()
    for copy in own_out:
        copy.wait()


def gather_all(tokens, upstream, vector, weights):
    seqs, piece, features = tokens.shape
    own = seqs // 4
    count = len(weights)
    vector = vector.reshape(-1, 128)
    cut = [item.reshape(8, item.shape[0] // 8, item.shape[1]) for item in weights]
    seq_shape = (own, 4, piece, features)
    copies = 9 + count * 42
    out = pl.pallas_call(
        functools.partial(gather_kernel, count),
        name="gather_all",
        out_shape=(
            jax.ShapeDtypeStruct(seq_shape, bf16),
            jax.ShapeDtypeStruct(seq_shape, bf16),
            jax.ShapeDtypeStruct((4, *vector.shape), bf16),
            *[jax.ShapeDtypeStruct((4, *item.shape), bf16) for item in cut],
        ),
        in_specs=[HBM] * (3 + count),
        out_specs=(HBM,) * (3 + count),
        scratch_shapes=[
            pltpu.VMEM((own, piece, features), bf16),
            pltpu.VMEM((own, piece, features), bf16),
            pltpu.VMEM(vector.shape, bf16),
            *[pltpu.VMEM(item.shape, bf16) for item in cut],
            pltpu.SemaphoreType.DMA((copies,)),
            pltpu.SemaphoreType.DMA((copies,)),
            pltpu.SemaphoreType.DMA((2 * (3 + count),)),
        ],
        compiler_params=pltpu.CompilerParams(
            collective_id=0, has_side_effects=True, vmem_limit_bytes=vmem_bytes
        ),
    )(
        tokens.reshape(4, own, piece, features),
        upstream.reshape(4, own, piece, features),
        vector,
        *cut,
    )
    wholes = [
        whole.reshape(4 * item.shape[0], item.shape[1]) for whole, item in zip(out[3:], weights)
    ]
    return out[0], out[1], out[2].reshape(4, -1), wholes


def heads_kernel(features, into, source, target, kept, send, recv, local):
    z, s, _, _, _ = place()
    copies, locals_ = Copies(send, recv), Locals(local)
    peers = [(z, lax.rem(s + d, 8)) for d in range(1, 8)]

    def columns(rank):
        return pl.ds(pl.multiple_of(rank * features, 128), features)

    def piece_for(rank):
        return source.at[:, :, :, columns(rank)] if into else source.at[:, :, rank]

    mine = target.at[:, :, s] if into else target.at[:, :, :, columns(s)]
    own = locals_.start(piece_for(s), kept)
    greet(peers)
    waiting = [copies.start(piece_for(to[1]), mine, to) for to in peers]
    own.wait()
    own = locals_.start(kept, mine)
    arrive(waiting)
    copies.finish()
    own.wait()


def heads_call(values, collective, into, features):
    own, parts, piece = values.shape[0], values.shape[1], values.shape[-2]
    wide, tall = (own, parts, piece, 8 * features), (own, parts, 8, piece, features)
    return pl.pallas_call(
        functools.partial(heads_kernel, features, into),
        name="to_heads" if into else "from_heads",
        out_shape=jax.ShapeDtypeStruct(tall if into else wide, bf16),
        in_specs=[HBM],
        out_specs=HBM,
        scratch_shapes=[
            pltpu.VMEM((own, parts, piece, features), bf16),
            pltpu.SemaphoreType.DMA((7,)),
            pltpu.SemaphoreType.DMA((7,)),
            pltpu.SemaphoreType.DMA((2,)),
        ],
        compiler_params=pltpu.CompilerParams(
            collective_id=collective, has_side_effects=True, vmem_limit_bytes=vmem_bytes
        ),
    )(values)


def add_blocks(steps, block_of):
    def body(i, _):
        target, others = block_of(i)
        total = target[...].astype(f32)
        for other in others:
            total = total + other[...].astype(f32)
        target[...] = total.astype(target.dtype)
        return 0

    lax.fori_loop(0, steps, body, 0)


def reduce_kernel(count, *refs):
    seq_in, vector_in, grads = refs[:2], refs[2], refs[3 : 3 + count]
    refs = refs[3 + count :]
    seq_out, vector_out, outs = refs[:2], refs[2], refs[3 : 3 + count]
    refs = refs[3 + count :]
    seq_own, vector_ranks, vector_sum, vector_lines = refs[:2], refs[2], refs[3], refs[4]
    bufs = [refs[5 + 7 * t : 12 + 7 * t] for t in range(count)]
    send, recv, local = refs[5 + 7 * count :]
    z, s, along_x, along_y, partner = place()
    core, chip = s % 2, s // 2
    x, y = chip % 2, chip // 2
    chip_x, chip_y = along_x // 2, along_y // 2
    lines = [(lax.rem(z + k, 4), s) for k in range(1, 4)]
    plane = [(z, lax.rem(s + d, 8)) for d in range(1, 8)]
    to_x, to_y, to_core = (z, along_x), (z, along_y), (z, partner)
    copies, locals_ = Copies(send, recv), Locals(local)
    loads = [locals_.start(g.at[:, :, core], b[0]) for g, b in zip(grads, bufs)]
    own_seq = [locals_.start(item.at[:, z], kept) for item, kept in zip(seq_in, seq_own)]
    own_vector = locals_.start(vector_in.at[:, s], vector_ranks.at[0])
    greet(lines + plane)

    cores = [copies.start(g.at[:, :, 1 - core], b[1], to_core) for g, b in zip(grads, bufs)]
    waiting = []
    for to in lines:
        for item, out in zip(seq_in, seq_out):
            waiting.append(copies.start(item.at[:, to[0]], out.at[z], to))
    vectors = [
        copies.start(vector_in.at[:, to[1]], vector_ranks.at[d + 1], to)
        for d, to in enumerate(plane)
    ]
    for copy in own_seq:
        copy.wait()
    own_out = [locals_.start(kept, out.at[z]) for kept, out in zip(seq_own, seq_out)]
    second, third, fourth = [], [], []
    for t in range(count + 3):
        if t < count:
            own, from_core, from_x, from_y = bufs[t][:4]
            rows = own.shape[2]
            half = rows // 2
            low, high = pl.ds(0, half), pl.ds(half, half)
            loads[t].wait()
            arrive([cores[t]])
            add_blocks(16, lambda i: (own.at[i // 4, i % 4], [from_core.at[i // 4, i % 4]]))
            step = []
            for k in range(2):
                step.append(copies.start(own.at[:, 2 * k + 1 - x, low], from_x.at[:, k], to_x))
                step.append(
                    copies.start(own.at[:, 2 * (1 - y) + k, high], from_y.at[:, k], to_y)
                )
            second.append(step)
        if 0 <= t - 1 < count:
            own, _, from_x, from_y, late_y, late_x = bufs[t - 1][:6]
            half = own.shape[2] // 2
            low, high = pl.ds(0, half), pl.ds(half, half)
            arrive(second[t - 1])
            add_blocks(
                8, lambda i: (own.at[i // 2, 2 * (i % 2) + x, low], [from_x.at[i // 2, i % 2]])
            )
            add_blocks(
                8, lambda i: (own.at[i // 2, 2 * y + i % 2, high], [from_y.at[i // 2, i % 2]])
            )
            third.append(
                [
                    copies.start(own.at[:, chip_y, low], late_y, to_y),
                    copies.start(own.at[:, chip_x, high], late_x, to_x),
                ]
            )
        if 0 <= t - 2 < count:
            own, _, _, _, late_y, late_x, from_z = bufs[t - 2]
            half = own.shape[2] // 2
            low, high = pl.ds(0, half), pl.ds(half, half)
            arrive(third[t - 2])
            add_blocks(4, lambda i: (own.at[i, chip, low], [late_y.at[i]]))
            add_blocks(4, lambda i: (own.at[i, chip, high], [late_x.at[i]]))
            fourth.append(
                [copies.start(own.at[to[0], chip], from_z.at[k], to) for k, to in enumerate(lines)]
            )
        if t == 0:
            own_vector.wait()
            arrive(vectors)
            total = vector_ranks[0]
            for d in range(1, 8):
                total = total + vector_ranks[d]
            vector_sum[...] = total
            vectors = [
                copies.start(vector_sum.at[to[0]], vector_lines.at[k], to)
                for k, to in enumerate(lines)
            ]
        if 0 <= t - 3 < count:
            own, from_z = bufs[t - 3][0], bufs[t - 3][6]
            arrive(fourth[t - 3])
            total = own[z, chip].astype(f32)
            for k in range(3):
                total = total + from_z[k].astype(f32)
            outs[t - 3][...] = total
    arrive(vectors)
    total = vector_sum[z]
    for k in range(3):
        total = total + vector_lines[k]
    vector_out[...] = total
    arrive(waiting)
    copies.finish()
    for copy in own_out:
        copy.wait()


def reduce_all(layer_output, input_grad, vector, grads):
    own, parts, piece, features = layer_output.shape
    count = len(grads)
    lanes = vector.shape[-1]
    padded = -(-lanes // 1024) * 1024
    vector = jnp.pad(vector, ((0, 0), (0, padded - lanes))).reshape(4, 8, padded // 128, 128)
    cut = [item.reshape(4, 4, 2, item.shape[0] // 32, item.shape[1]) for item in grads]
    scratch = []
    for item in cut:
        rows, columns = item.shape[3:]
        half = rows // 2
        scratch += [
            pltpu.VMEM((4, 4, rows, columns), bf16),
            pltpu.VMEM((4, 4, rows, columns), bf16),
            pltpu.VMEM((4, 2, half, columns), bf16),
            pltpu.VMEM((4, 2, half, columns), bf16),
            pltpu.VMEM((4, half, columns), bf16),
            pltpu.VMEM((4, half, columns), bf16),
            pltpu.VMEM((3, rows, columns), bf16),
        ]
    copies = 6 + 7 + 3 + count * 10
    seq_shape = (4, own, piece, features)
    out = pl.pallas_call(
        functools.partial(reduce_kernel, count),
        name="reduce_all",
        out_shape=(
            jax.ShapeDtypeStruct(seq_shape, bf16),
            jax.ShapeDtypeStruct(seq_shape, bf16),
            jax.ShapeDtypeStruct(vector.shape[2:], f32),
            *[jax.ShapeDtypeStruct(item.shape[3:], f32) for item in cut],
        ),
        in_specs=[HBM] * (3 + count),
        out_specs=(HBM, HBM) + (VMEM,) * (1 + count),
        scratch_shapes=[
            pltpu.VMEM((own, piece, features), bf16),
            pltpu.VMEM((own, piece, features), bf16),
            pltpu.VMEM((8, 4, padded // 128, 128), f32),
            pltpu.VMEM((4, padded // 128, 128), f32),
            pltpu.VMEM((3, padded // 128, 128), f32),
            *scratch,
            pltpu.SemaphoreType.DMA((copies,)),
            pltpu.SemaphoreType.DMA((copies,)),
            pltpu.SemaphoreType.DMA((count + 5,)),
        ],
        compiler_params=pltpu.CompilerParams(
            collective_id=1, has_side_effects=True, vmem_limit_bytes=vmem_bytes
        ),
    )(layer_output, input_grad, vector, *cut)
    return (
        out[0].reshape(4 * own, piece, features),
        out[1].reshape(4 * own, piece, features),
        out[2].reshape(-1)[:lanes],
        out[3:],
    )


def per_device(
    layer_input,
    first_gain,
    first_shift,
    joined_weight,
    query_bias,
    value_bias,
    output_weight,
    output_bias,
    second_gain,
    second_shift,
    expand_weight,
    expand_bias,
    contract_weight,
    contract_bias,
    alibi_slopes,
    upstream,
):
    seqs, piece, features = layer_input.shape
    fs_count = lax.axis_size("fs")
    sp_count = lax.axis_size("sp")
    head_count = alibi_slopes.shape[0]
    width = features // head_count
    heads = head_count // sp_count
    rows = seqs * piece
    own = seqs // fs_count
    shape = (own, fs_count, piece)
    slopes = lax.dynamic_slice_in_dim(alibi_slopes, lax.axis_index("sp") * heads, heads)

    vectors = (
        first_gain, first_shift, query_bias, value_bias, output_bias,
        second_gain, second_shift, contract_bias, expand_bias,
    )
    fast = (fs_count, sp_count) == (4, 8) and own >= 1
    weights = (joined_weight, output_weight, expand_weight, contract_weight)
    if fast:
        tokens, upstream_low, packed, weights = gather_all(
            layer_input, upstream, jnp.concatenate(vectors), weights
        )
    else:
        tokens, upstream_low = to_own_seqs(layer_input), to_own_seqs(upstream)
        packed = lax.all_gather(jnp.concatenate(vectors), "fs", axis=0)
        weights = [lax.all_gather(item, "fs", axis=0, tiled=True) for item in weights]
    joined_full, out_full, expand_full, contract_full = weights
    tokens = tokens.reshape(rows, features).astype(f32)
    upstream_low = upstream_low.reshape(rows, features)
    whole, at = [], 0
    for item in vectors:
        whole.append(packed[:, at : at + item.shape[0]].reshape(-1))
        at += item.shape[0]
    gain_one, shift_one, qbias, vbias, obias, gain_two, shift_two, cbias, ebias = [
        item.astype(f32) for item in whole
    ]

    def into_heads(values, collective):
        if fast:
            columns = values.shape[1] // 8
            found = heads_call(values.reshape(*shape, -1), collective, True, columns)
            return found.reshape(own, -1, columns)
        return to_heads(values.reshape(*shape, -1))

    def out_of_heads(values, collective):
        if fast:
            columns = values.shape[-1]
            found = values.reshape(own, 4, 8, piece, columns)
            found = heads_call(found, collective, False, columns)
            return found.reshape(rows, -1)
        return from_heads(values, fs_count, piece).reshape(rows, -1)

    normed_f, norm_back_one = jax.vjp(normalize, tokens, gain_one, shift_one)
    normed = normed_f.astype(bf16)
    joined_all = (matmul(normed, joined_full) + joined_bias_of(qbias, vbias, head_count)).astype(
        bf16
    )
    qkv = into_heads(joined_all, 2)
    attended_heads, out_t, lse = attention_forward(qkv, slopes, heads, width)
    attended = out_of_heads(attended_heads, 3)

    residual = tokens + (matmul(attended, out_full) + obias)
    second_f, norm_back_two = jax.vjp(normalize, residual, gain_two, shift_two)
    second = second_f.astype(bf16)
    expanded = matmul(second, expand_full) + ebias
    activated_f, gelu_back = jax.vjp(gelu_tanh, expanded)
    activated = activated_f.astype(bf16)
    result = residual + (matmul(activated, contract_full) + cbias)
    layer_output = result.astype(bf16).reshape(*shape, features)

    upstream_f = upstream_low.astype(f32)
    contract_grad = matmul_lt(activated, upstream_low)
    contract_bias_grad = jnp.sum(upstream_f, axis=0)
    act_grad = matmul_rt(upstream_low, contract_full)
    expand_diff = gelu_back(act_grad)[0].astype(bf16)
    expand_grad = matmul_lt(second, expand_diff)
    expand_bias_grad = jnp.sum(expand_diff.astype(f32), axis=0)
    second_back = matmul_rt(expand_diff, expand_full)
    resid_part, second_gain_grad, second_shift_grad = norm_back_two(second_back)
    residual_grad = upstream_f + resid_part

    branch_diff = residual_grad.astype(bf16)
    output_weight_grad = matmul_lt(attended, branch_diff)
    output_bias_grad = jnp.sum(branch_diff.astype(f32), axis=0)
    attended_diff = matmul_rt(branch_diff, out_full).astype(bf16)
    diff_heads = into_heads(attended_diff, 4)
    joined_heads = attention_backward(qkv, diff_heads, out_t, lse, slopes, heads, width)
    joined_diff = out_of_heads(joined_heads, 5)

    joined_grad = matmul_lt(normed, joined_diff)
    column_sums = jnp.sum(joined_diff.astype(f32), axis=0).reshape(head_count, 3, width)
    query_bias_grad = column_sums[:, 0].reshape(features)
    value_bias_grad = column_sums[:, 2].reshape(features)
    normed_back = matmul_rt(joined_diff, joined_full)
    input_part, first_gain_grad, first_shift_grad = norm_back_one(normed_back)
    input_grad = (residual_grad + input_part).astype(bf16).reshape(*shape, features)

    vector_grads = (
        first_gain_grad, first_shift_grad, query_bias_grad, value_bias_grad, output_bias_grad,
        second_gain_grad, second_shift_grad, contract_bias_grad, expand_bias_grad,
    )
    devices = fs_count * sp_count
    packed = jnp.concatenate([item.reshape(devices, -1) for item in vector_grads], axis=1)
    grads = (contract_grad, expand_grad, joined_grad, output_weight_grad)
    if fast:
        layer_output, input_grad, packed, grads = reduce_all(
            layer_output, input_grad, packed, [item.astype(bf16) for item in grads]
        )
    else:
        layer_output, input_grad = from_own_seqs(layer_output), from_own_seqs(input_grad)
        scatter = functools.partial(
            lax.psum_scatter, axis_name=("fs", "sp"), scatter_dimension=0, tiled=True
        )
        packed = scatter(packed.reshape(-1))
        grads = [scatter(item) for item in grads]
    contract_grad, expand_grad, joined_grad, output_weight_grad = grads
    own_grads, at = [], 0
    for item in vector_grads:
        size = item.shape[0] // devices
        own_grads.append(packed[at : at + size])
        at += size
    g1, s1, qb, vb, ob, g2, s2, cb, eb = own_grads
    return (
        layer_output,
        input_grad,
        g1,
        s1,
        joined_grad,
        qb,
        vb,
        output_weight_grad,
        ob,
        g2,
        s2,
        expand_grad,
        eb,
        contract_grad,
        cb,
    )


def solution(mesh):
    tokens = P(None, ("fs", "sp"), None)
    both, both_rows = P(("fs", "sp")), P(("fs", "sp"), None)
    one, one_rows = P("fs"), P("fs", None)
    return jax.shard_map(
        per_device,
        mesh=mesh,
        in_specs=(
            tokens, one, one, one_rows, one, one, one_rows, one, one, one, one_rows, one,
            one_rows, one, P(), tokens,
        ),
        out_specs=(
            tokens, tokens, both, both, both_rows, both, both, both_rows, both, both, both,
            both_rows, both, both_rows, both,
        ),
        check_vma=False,
    )
```

```python
import functools
import math

import jax
import jax.numpy as jnp
from jax import lax
from jax.experimental import pallas as pl
from jax.experimental.pallas import tpu as pltpu
from jax.sharding import PartitionSpec as P

norm_eps = 1e-05
gelu_coef = 0.7978845608028654
masked_value = -1e30
f32 = jnp.float32
bf16 = jnp.bfloat16
MESH = pl.DeviceIdType.MESH
HBM = pl.BlockSpec(memory_space=pl.ANY)
VMEM = pl.BlockSpec(memory_space=pltpu.VMEM)
SMEM = pl.BlockSpec(memory_space=pltpu.SMEM)
vmem_bytes = 60 * 1024 * 1024


def normalize(values, norm_gain, norm_shift):
    center = values - jnp.mean(values, axis=-1, keepdims=True)
    variance = jnp.mean(center * center, axis=-1, keepdims=True)
    return center * lax.rsqrt(variance + norm_eps) * norm_gain + norm_shift


def gelu_tanh(values):
    return (
        0.5 * values * (1.0 + jnp.tanh(gelu_coef * (values + 0.044715 * values * values * values)))
    )


def matmul(left_side, right_side):
    return jnp.dot(left_side, right_side, preferred_element_type=f32)


def matmul_lt(left_side, right_side):
    return lax.dot_general(
        left_side, right_side, (((0,), (0,)), ((), ())), preferred_element_type=f32
    )


def matmul_rt(left_side, right_side):
    return lax.dot_general(
        left_side, right_side, (((1,), (1,)), ((), ())), preferred_element_type=f32
    )


def joined_bias_of(query_bias, value_bias, head_count):
    query_part = query_bias.astype(f32).reshape(head_count, -1)
    value_part = value_bias.astype(f32).reshape(head_count, -1)
    return jnp.stack([query_part, jnp.zeros_like(query_part), value_part], axis=1).reshape(-1)


def split_three(values):
    high = values.astype(bf16).astype(f32)
    rest = values - high
    middle = rest.astype(bf16).astype(f32)
    return high, middle, rest - middle


def key_columns(key_rows, slope, start):
    rows, width = key_rows.shape
    position = (start + lax.broadcasted_iota(jnp.int32, (rows, width), 0)).astype(f32)
    lane = lax.broadcasted_iota(jnp.int32, (rows, width), 1)
    high, middle, low = split_three(slope * position)
    extra = jnp.where(lane == 0, high, jnp.where(lane == 1, middle, jnp.where(lane == 2, low, 0.0)))
    return jnp.concatenate([key_rows.astype(f32), extra], axis=1).astype(bf16)


def query_columns(queries, scale):
    rows, width = queries.shape
    lane = lax.broadcasted_iota(jnp.int32, (rows, width), 1)
    ones = jnp.where(lane < 3, 1.0, 0.0)
    return jnp.concatenate([queries.astype(f32) * scale, ones], axis=1).astype(bf16)


class Forward:
    def __init__(self, heads, width, slopes, qkv, out, out_t, lse, keys, queries, values_t):
        self.heads, self.width, self.slopes, self.qkv, self.out = heads, width, slopes, qkv, out
        self.out_t, self.lse = out_t, lse
        self.keys, self.queries, self.values_t = keys, queries, values_t
        self.blocks = qkv.shape[1]
        self.block = qkv.shape[2] * qkv.shape[3]

    def rows(self, i):
        return pl.ds(pl.multiple_of(i * self.block, self.block), self.block)

    def prepare(self, b):
        width, block, qkv = self.width, self.block, self.qkv
        scale = 1.0 / math.sqrt(width)

        def body(i, _):
            rows = self.rows(i)
            for h in range(self.heads):
                base = h * 3 * width
                query, key, value = [
                    qkv[b, i, :, :, base + n * width : base + (n + 1) * width].reshape(block, width)
                    for n in range(3)
                ]
                self.keys[h, rows, :] = key_columns(key, self.slopes[h], i * block)
                self.queries[h, rows, :] = query_columns(query, scale)
                self.values_t[h, :, rows] = value.astype(f32).T.astype(bf16)
            return 0

        lax.fori_loop(0, self.blocks, body, 0)

    def run(self, b, low, high):
        heads, width, block = self.heads, self.width, self.block

        def one_block(i, _):
            rows = self.rows(i)
            query = [self.queries[h, rows, :] for h in range(heads)]

            def step(j, state, diagonal):
                columns = self.rows(j)
                result = []
                for h in range(heads):
                    top, total, acc = state[h]
                    scores = matmul_rt(self.keys[h, columns, :], query[h])
                    if diagonal:
                        key_at = lax.broadcasted_iota(jnp.int32, (block, block), 0)
                        query_at = lax.broadcasted_iota(jnp.int32, (block, block), 1)
                        scores = jnp.where(key_at <= query_at, scores, masked_value)
                    newest = jnp.maximum(top, jnp.max(scores, axis=0, keepdims=True))
                    shrink = jnp.exp(top - newest)
                    probs = jnp.exp(scores - newest)
                    total = total * shrink + jnp.sum(probs, axis=0, keepdims=True)
                    acc = acc * shrink + matmul(self.values_t[h, :, columns], probs.astype(bf16))
                    result.append((newest, total, acc))
                return tuple(result)

            state = tuple(
                (
                    jnp.full((1, block), masked_value, f32),
                    jnp.zeros((1, block), f32),
                    jnp.zeros((width, block), f32),
                )
                for h in range(heads)
            )
            state = lax.fori_loop(0, i, lambda j, s: step(j, s, False), state)
            state = step(i, state, True)
            finished = []
            for h in range(heads):
                top, total, acc = state[h]
                result = acc / total
                self.out_t[b, h, :, rows] = result
                self.lse[b, h, :, rows] = top + jnp.log(total)
                finished.append(result)
            joined = finished[0] if heads == 1 else jnp.concatenate(finished, axis=0)
            self.out[b, i] = joined.T.astype(bf16).reshape(self.out.shape[2:])
            return 0

        lax.fori_loop(low, high, one_block, 0)


def forward_kernel(heads, width, *refs):
    attention = Forward(heads, width, *refs)

    def one_seq(b, _):
        attention.prepare(b)
        attention.run(b, 0, attention.blocks)
        return 0

    lax.fori_loop(0, attention.qkv.shape[0], one_seq, 0)


def saved_shapes(seqs, length, heads, width):
    return (
        jax.ShapeDtypeStruct((seqs, heads, width, length), f32),
        jax.ShapeDtypeStruct((seqs, heads, 1, length), f32),
    )


def forward_scratch(length, heads, width):
    return [
        pltpu.VMEM((heads, length, 2 * width), bf16),
        pltpu.VMEM((heads, length, 2 * width), bf16),
        pltpu.VMEM((heads, width, length), bf16),
    ]


def attention_forward(qkv, slopes, heads, width):
    seqs, blocks, ranks, piece, _ = qkv.shape
    length = blocks * ranks * piece
    return pl.pallas_call(
        functools.partial(forward_kernel, heads, width),
        name="attention_forward",
        out_shape=(
            jax.ShapeDtypeStruct((seqs, blocks, ranks, piece, heads * width), bf16),
            *saved_shapes(seqs, length, heads, width),
        ),
        in_specs=[SMEM, VMEM],
        out_specs=(VMEM, VMEM, VMEM),
        scratch_shapes=forward_scratch(length, heads, width),
        compiler_params=pltpu.CompilerParams(vmem_limit_bytes=vmem_bytes),
    )(slopes, qkv)


class Backward:
    def __init__(
        self, heads, width, slopes, qkv, diff, out_t, lse, joined,
        keys, queries, keys_t, values, diffs, delta, query_acc,
    ):
        self.heads, self.width, self.slopes, self.qkv, self.diff = heads, width, slopes, qkv, diff
        self.out_t, self.lse, self.joined = out_t, lse, joined
        self.keys, self.queries, self.keys_t, self.values = keys, queries, keys_t, values
        self.diffs, self.delta, self.query_acc = diffs, delta, query_acc
        self.blocks = qkv.shape[1]
        self.block = qkv.shape[2] * qkv.shape[3]

    def rows(self, i):
        return pl.ds(pl.multiple_of(i * self.block, self.block), self.block)

    def prepare(self, b):
        width, block, qkv = self.width, self.block, self.qkv
        scale = 1.0 / math.sqrt(width)

        def body(i, _):
            rows = self.rows(i)
            for h in range(self.heads):
                base = h * 3 * width
                query, key, value = [
                    qkv[b, i, :, :, base + n * width : base + (n + 1) * width].reshape(block, width)
                    for n in range(3)
                ]
                self.keys[h, rows, :] = key_columns(key, self.slopes[h], i * block)
                self.keys_t[h, :, rows] = key.astype(f32).T.astype(bf16)
                self.queries[h, rows, :] = query_columns(query, scale)
                self.values[h, rows, :] = value
                part = self.diff[b, i, :, :, h * width : (h + 1) * width].reshape(block, width)
                self.diffs[h, rows, :] = part
                self.delta[h, :, rows] = jnp.sum(
                    part.astype(f32).T * self.out_t[b, h, :, rows], axis=0, keepdims=True
                )
                self.query_acc[h, :, rows] = jnp.zeros((width, block), f32)
            return 0

        lax.fori_loop(0, self.blocks, body, 0)

    def run(self, b, low, high):
        heads, width, block = self.heads, self.width, self.block
        tail = self.joined.shape[2:4] + (width,)

        def one_block(j, _):
            columns = self.rows(j)

            def step(i, state, diagonal):
                rows = self.rows(i)
                result = []
                for h in range(heads):
                    key_acc, value_acc = state[h]
                    query = self.queries[h, rows, :]
                    part = self.diffs[h, rows, :]
                    scores = matmul_rt(self.keys[h, columns, :], query)
                    probs = jnp.exp(scores - self.lse[b, h, :, rows])
                    if diagonal:
                        key_at = lax.broadcasted_iota(jnp.int32, (block, block), 0)
                        query_at = lax.broadcasted_iota(jnp.int32, (block, block), 1)
                        probs = jnp.where(key_at <= query_at, probs, 0.0)
                    prob_diff = matmul_rt(self.values[h, columns, :], part)
                    score_diff = (probs * (prob_diff - self.delta[h, :, rows])).astype(bf16)
                    value_acc = value_acc + matmul(probs.astype(bf16), part)
                    key_acc = key_acc + matmul(score_diff, query)
                    self.query_acc[h, :, rows] += matmul(self.keys_t[h, :, columns], score_diff)
                    result.append((key_acc, value_acc))
                return tuple(result)

            state = tuple(
                (jnp.zeros((block, 2 * width), f32), jnp.zeros((block, width), f32))
                for h in range(heads)
            )
            state = step(j, state, True)
            state = lax.fori_loop(j + 1, self.blocks, lambda i, s: step(i, s, False), state)
            for h in range(heads):
                base = (h * 3 + 1) * width
                key_acc, value_acc = state[h]
                self.joined[b, j, :, :, base : base + width] = (
                    key_acc[:, :width].astype(bf16).reshape(tail)
                )
                self.joined[b, j, :, :, base + width : base + 2 * width] = value_acc.astype(
                    bf16
                ).reshape(tail)
            return 0

        lax.fori_loop(low, high, one_block, 0)

    def finish(self, b):
        width = self.width
        scale = 1.0 / math.sqrt(width)
        tail = self.joined.shape[2:4] + (width,)

        def body(i, _):
            for h in range(self.heads):
                base = h * 3 * width
                result = (self.query_acc[h, :, self.rows(i)] * scale).T.astype(bf16)
                self.joined[b, i, :, :, base : base + width] = result.reshape(tail)
            return 0

        lax.fori_loop(0, self.blocks, body, 0)


def backward_kernel(heads, width, *refs):
    attention = Backward(heads, width, *refs)

    def one_seq(b, _):
        attention.prepare(b)
        attention.run(b, 0, attention.blocks)
        attention.finish(b)
        return 0

    lax.fori_loop(0, attention.qkv.shape[0], one_seq, 0)


def backward_scratch(length, heads, width):
    return [
        pltpu.VMEM((heads, length, 2 * width), bf16),
        pltpu.VMEM((heads, length, 2 * width), bf16),
        pltpu.VMEM((heads, width, length), bf16),
        pltpu.VMEM((heads, length, width), bf16),
        pltpu.VMEM((heads, length, width), bf16),
        pltpu.VMEM((heads, 1, length), f32),
        pltpu.VMEM((heads, width, length), f32),
    ]


def attention_backward(qkv, diff, out_t, lse, slopes, heads, width):
    length = qkv.shape[1] * qkv.shape[2] * qkv.shape[3]
    return pl.pallas_call(
        functools.partial(backward_kernel, heads, width),
        name="attention_backward",
        out_shape=jax.ShapeDtypeStruct(qkv.shape, bf16),
        in_specs=[SMEM, VMEM, VMEM, VMEM, VMEM],
        out_specs=VMEM,
        scratch_shapes=backward_scratch(length, heads, width),
        compiler_params=pltpu.CompilerParams(vmem_limit_bytes=vmem_bytes),
    )(slopes, qkv, diff, out_t, lse)


def to_own_seqs(values):
    seqs, piece, features = values.shape
    parts = lax.axis_size("fs")
    values = values.reshape(parts, seqs // parts, piece, features)
    return lax.all_to_all(values, "fs", split_axis=0, concat_axis=0).transpose(1, 0, 2, 3)


def from_own_seqs(values):
    own, parts, piece, features = values.shape
    values = lax.all_to_all(values.transpose(1, 0, 2, 3), "fs", split_axis=0, concat_axis=0)
    return values.reshape(parts * own, piece, features)


def to_heads(values):
    own, parts, piece, features = values.shape
    ranks = lax.axis_size("sp")
    values = values.reshape(own, parts, piece, ranks, features // ranks)
    return lax.all_to_all(values, "sp", split_axis=3, concat_axis=2)


def from_heads(values):
    own, parts, ranks, piece, features = values.shape
    values = lax.all_to_all(values, "sp", split_axis=2, concat_axis=3)
    return values.reshape(own, parts, piece, ranks * features)


class Copies:
    def __init__(self, send, recv):
        self.send, self.recv, self.used, self.made = send, recv, 0, []

    def start(self, source, target, device):
        copy = pltpu.make_async_remote_copy(
            src_ref=source,
            dst_ref=target,
            send_sem=self.send.at[self.used],
            recv_sem=self.recv.at[self.used],
            device_id=device,
            device_id_type=MESH,
        )
        self.used += 1
        self.made.append(copy)
        copy.start()
        return copy

    def finish(self):
        assert self.used == self.send.shape[0]
        for copy in self.made:
            copy.wait_send()


class Locals:
    def __init__(self, sems):
        self.sems, self.used = sems, 0

    def start(self, source, target):
        copy = pltpu.make_async_copy(source, target, self.sems.at[self.used])
        self.used += 1
        copy.start()
        return copy


def arrive(copies):
    for copy in copies:
        copy.wait_recv()


def greet(devices):
    barrier = pltpu.get_barrier_semaphore()
    for device in devices:
        pl.semaphore_signal(barrier, inc=1, device_id=device, device_id_type=MESH)
    pl.semaphore_wait(barrier, len(devices))


def place():
    z, s = lax.axis_index("fs"), lax.axis_index("sp")
    along_x = s + 2 - 4 * ((s // 2) % 2)
    along_y = s + 4 - 8 * (s // 4)
    partner = s + 1 - 2 * (s % 2)
    return z, s, along_x, along_y, partner


def line_of(z, s):
    return [(lax.rem(z + k, 4), s) for k in range(1, 4)]


def plane_of(z, s):
    return [(z, lax.rem(s + d, 8)) for d in range(1, 8)]


class Gather:
    copies_each = 45

    def __init__(self, weights, wholes, kept, copies, locals_):
        self.weights, self.wholes, self.kept = weights, wholes, kept
        self.copies, self.locals_ = copies, locals_
        self.z, self.s, self.along_x, self.along_y, self.partner = place()
        self.lines = line_of(self.z, self.s)
        self.first, self.second, self.third = {}, {}, {}
        self.waiting = []

    def load(self):
        self.loads = [self.locals_.start(w, k) for w, k in zip(self.weights, self.kept)]

    def keep(self):
        for copy in self.loads:
            copy.wait()
        self.own = [
            self.locals_.start(k, whole.at[self.z]) for k, whole in zip(self.kept, self.wholes)
        ]

    def start(self, t):
        self.first[t] = [
            self.copies.start(self.weights[t].at[self.s], self.wholes[t].at[self.z, self.s], to)
            for to in self.lines
        ]

    def refs(self, t):
        whole = self.wholes[t]
        half = whole.shape[2] // 2

        def same(k, rank, part, to):
            rows = pl.ds(part * half, half)
            where = (k, rank, rows)
            return self.copies.start(whole.at[where], whole.at[where], (self.z, to))

        return same

    def exchange(self, t):
        same = self.refs(t)
        arrive(self.first[t])
        step = []
        for k, _ in self.lines:
            step.append(same(k, self.s, 0, self.along_x))
            step.append(same(k, self.s, 1, self.along_y))
        for k, _ in self.lines:
            self.waiting.append(same(k, self.s, 0, self.partner))
            self.waiting.append(same(k, self.s, 1, self.partner))
        self.second[t] = step

    def spread(self, t):
        same = self.refs(t)
        arrive(self.second[t])
        step = []
        for k, _ in self.lines:
            step.append(same(k, self.s, 0, self.along_y))
            step.append(same(k, self.s, 1, self.along_x))
            step.append(same(k, self.along_x, 0, self.along_y))
            step.append(same(k, self.along_y, 1, self.along_x))
        for k, _ in self.lines:
            self.waiting.append(same(k, self.along_x, 0, self.partner))
            self.waiting.append(same(k, self.along_y, 1, self.partner))
        self.third[t] = step

    def share(self, t):
        same = self.refs(t)
        arrive(self.third[t])
        diagonal = self.along_x + self.along_y - self.s
        for k, _ in self.lines:
            self.waiting.append(same(k, self.along_y, 0, self.partner))
            self.waiting.append(same(k, self.along_x, 1, self.partner))
            self.waiting.append(same(k, diagonal, 0, self.partner))
            self.waiting.append(same(k, diagonal, 1, self.partner))

    def finish(self):
        arrive(self.waiting)
        for copy in self.own:
            copy.wait()


def add_blocks(steps, block_of):
    def body(i, _):
        target, other = block_of(i)
        target[...] = (target[...].astype(f32) + other[...].astype(f32)).astype(target.dtype)
        return 0

    lax.fori_loop(0, steps, body, 0)


class Reduce:
    copies_each = 10

    def __init__(self, grads, outs, bufs, copies, locals_):
        self.grads, self.outs, self.copies, self.locals_ = grads, outs, copies, locals_
        self.bufs = [bufs[7 * t : 7 * t + 7] for t in range(len(grads))]
        self.z, self.s, along_x, along_y, partner = place()
        self.core, self.chip = self.s % 2, self.s // 2
        self.x, self.y = self.chip % 2, self.chip // 2
        self.chip_x, self.chip_y = along_x // 2, along_y // 2
        self.lines = line_of(self.z, self.s)
        self.to_x, self.to_y, self.to_core = [(self.z, to) for to in (along_x, along_y, partner)]
        self.first, self.second, self.third, self.fourth = {}, {}, {}, {}

    def load(self):
        self.loads = [
            self.locals_.start(g.at[:, :, self.core], b[0]) for g, b in zip(self.grads, self.bufs)
        ]

    def start(self, t):
        self.first[t] = self.copies.start(
            self.grads[t].at[:, :, 1 - self.core], self.bufs[t][1], self.to_core
        )

    def halves(self, t):
        half = self.bufs[t][0].shape[2] // 2
        return pl.ds(0, half), pl.ds(half, half)

    def exchange(self, t):
        own, from_core, from_x, from_y = self.bufs[t][:4]
        low, high = self.halves(t)
        self.loads[t].wait()
        arrive([self.first[t]])
        add_blocks(16, lambda i: (own.at[i // 4, i % 4], from_core.at[i // 4, i % 4]))
        step = []
        for k in range(2):
            step.append(
                self.copies.start(own.at[:, 2 * k + 1 - self.x, low], from_x.at[:, k], self.to_x)
            )
            step.append(
                self.copies.start(
                    own.at[:, 2 * (1 - self.y) + k, high], from_y.at[:, k], self.to_y
                )
            )
        self.second[t] = step

    def spread(self, t):
        own, _, from_x, from_y, late_y, late_x, _ = self.bufs[t]
        low, high = self.halves(t)
        arrive(self.second[t])
        add_blocks(
            8, lambda i: (own.at[i // 2, 2 * (i % 2) + self.x, low], from_x.at[i // 2, i % 2])
        )
        add_blocks(
            8, lambda i: (own.at[i // 2, 2 * self.y + i % 2, high], from_y.at[i // 2, i % 2])
        )
        self.third[t] = [
            self.copies.start(own.at[:, self.chip_y, low], late_y, self.to_y),
            self.copies.start(own.at[:, self.chip_x, high], late_x, self.to_x),
        ]

    def send(self, t):
        own, _, _, _, late_y, late_x, from_z = self.bufs[t]
        low, high = self.halves(t)
        arrive(self.third[t])
        add_blocks(4, lambda i: (own.at[i, self.chip, low], late_y.at[i]))
        add_blocks(4, lambda i: (own.at[i, self.chip, high], late_x.at[i]))
        self.fourth[t] = [
            self.copies.start(own.at[to[0], self.chip], from_z.at[k], to)
            for k, to in enumerate(self.lines)
        ]

    def finish(self, t):
        own, from_z = self.bufs[t][0], self.bufs[t][6]
        arrive(self.fourth[t])
        total = own[self.z, self.chip].astype(f32)
        for k in range(3):
            total = total + from_z[k].astype(f32)
        self.outs[t][...] = total


def reduce_scratch(cut):
    scratch = []
    for item in cut:
        rows, columns = item.shape[3:]
        half = rows // 2
        scratch += [
            pltpu.VMEM((4, 4, rows, columns), bf16),
            pltpu.VMEM((4, 4, rows, columns), bf16),
            pltpu.VMEM((4, 2, half, columns), bf16),
            pltpu.VMEM((4, 2, half, columns), bf16),
            pltpu.VMEM((4, half, columns), bf16),
            pltpu.VMEM((4, half, columns), bf16),
            pltpu.VMEM((3, rows, columns), bf16),
        ]
    return scratch


def split_grad(item):
    return item.reshape(4, 4, 2, item.shape[0] // 32, item.shape[1])


def semaphores(remote, local):
    return [pltpu.SemaphoreType.DMA((n,)) for n in (remote, remote, local)]


def remote_call(kernel, name, collective, **options):
    return pl.pallas_call(
        kernel,
        name=name,
        compiler_params=pltpu.CompilerParams(
            collective_id=collective, has_side_effects=True, vmem_limit_bytes=vmem_bytes
        ),
        **options,
    )


def begin_kernel(
    tokens, vector, weight, tokens_out, vector_out, whole,
    tokens_own, vector_own, kept, send, recv, local,
):
    z, s, along_x, along_y, partner = place()
    lines = line_of(z, s)
    copies, locals_ = Copies(send, recv), Locals(local)
    gather = Gather([weight], [whole], [kept], copies, locals_)
    gather.load()
    own = [locals_.start(tokens.at[z], tokens_own), locals_.start(vector, vector_own)]
    greet(lines + [(z, to) for to in (along_x, along_y, partner)])
    waiting = []
    gather.start(0)
    for to in lines:
        waiting.append(copies.start(tokens.at[to[0]], tokens_out.at[:, z], to))
        waiting.append(copies.start(vector, vector_out.at[z], to))
    for copy in own:
        copy.wait()
    own = [
        locals_.start(tokens_own, tokens_out.at[:, z]),
        locals_.start(vector_own, vector_out.at[z]),
    ]
    gather.keep()
    gather.exchange(0)
    gather.spread(0)
    gather.share(0)
    gather.finish()
    arrive(waiting)
    copies.finish()
    for copy in own:
        copy.wait()


def begin(tokens, vector, weight):
    seqs, piece, features = tokens.shape
    own = seqs // 4
    vector = vector.reshape(-1, 128)
    cut = weight.reshape(8, weight.shape[0] // 8, weight.shape[1])
    out = remote_call(
        begin_kernel,
        "begin",
        0,
        out_shape=(
            jax.ShapeDtypeStruct((own, 4, piece, features), bf16),
            jax.ShapeDtypeStruct((4, *vector.shape), bf16),
            jax.ShapeDtypeStruct((4, *cut.shape), bf16),
        ),
        in_specs=[HBM] * 3,
        out_specs=(HBM,) * 3,
        scratch_shapes=[
            pltpu.VMEM((own, piece, features), bf16),
            pltpu.VMEM(vector.shape, bf16),
            pltpu.VMEM(cut.shape, bf16),
            *semaphores(6 + Gather.copies_each, 6),
        ],
    )(tokens.reshape(4, own, piece, features), vector, cut)
    return out[0], out[1].reshape(4, -1), out[2].reshape(4 * weight.shape[0], -1)


def columns_of(rank, features):
    return pl.ds(pl.multiple_of(rank * features, 128), features)


def forward_fused_kernel(
    heads, width, count, slopes, source, upstream, *refs
):
    weights, refs = refs[:count], refs[count:]
    qkv_out, attended, out_t, lse, upstream_out = refs[:5]
    wholes, refs = refs[5 : 5 + count], refs[5 + count :]
    qkv, result, upstream_own = refs[:3]
    attention = Forward(heads, width, slopes, qkv, result, out_t, lse, *refs[3:6])
    kept, (send, recv, local) = refs[6 : 6 + count], refs[6 + count :]
    z, s, along_x, along_y, partner = place()
    lines, plane = line_of(z, s), plane_of(z, s)
    copies, locals_ = Copies(send, recv), Locals(local)
    gather = Gather(weights, wholes, kept, copies, locals_)
    features = heads * width

    gather.load()
    own = [
        locals_.start(source.at[:, :, :, columns_of(s, 3 * features)], qkv.at[:, :, s]),
        locals_.start(upstream.at[z], upstream_own),
    ]
    greet(lines + plane)
    arriving = [
        copies.start(source.at[:, :, :, columns_of(to[1], 3 * features)], qkv.at[:, :, s], to)
        for to in plane
    ]
    for t in range(count):
        gather.start(t)
    waiting = [copies.start(upstream.at[to[0]], upstream_out.at[:, z], to) for to in lines]
    for copy in own:
        copy.wait()
    finishing = [locals_.start(upstream_own, upstream_out.at[:, z])]
    gather.keep()
    arrive(arriving)
    finishing.append(locals_.start(qkv, qkv_out))

    def hand_back(b):
        for to in plane:
            waiting.append(
                copies.start(
                    result.at[b, :, to[1]], attended.at[b, :, :, columns_of(s, features)], to
                )
            )
        finishing.append(
            locals_.start(result.at[b, :, s], attended.at[b, :, :, columns_of(s, features)])
        )

    gather.exchange(0)
    gather.exchange(1)
    attention.prepare(0)
    attention.run(0, 0, 3)
    gather.spread(0)
    gather.exchange(2)
    attention.run(0, 3, 4)
    hand_back(0)
    gather.spread(1)
    attention.prepare(1)
    attention.run(1, 0, 3)
    gather.share(0)
    gather.spread(2)
    attention.run(1, 3, 4)
    hand_back(1)
    gather.share(1)
    gather.share(2)
    gather.finish()
    arrive(waiting)
    copies.finish()
    for copy in finishing:
        copy.wait()


def forward_fused(joined_all, upstream, weights, slopes, heads, width):
    own, parts, piece, columns = joined_all.shape
    features = heads * width
    length = parts * 8 * piece
    count = len(weights)
    cut = [item.reshape(8, item.shape[0] // 8, item.shape[1]) for item in weights]
    seq_shape = (own, parts, piece, 8 * features)
    qkv_shape = (own, parts, 8, piece, 3 * features)
    out = remote_call(
        functools.partial(forward_fused_kernel, heads, width, count),
        "forward_fused",
        1,
        out_shape=(
            jax.ShapeDtypeStruct(qkv_shape, bf16),
            jax.ShapeDtypeStruct(seq_shape, bf16),
            *saved_shapes(own, length, heads, width),
            jax.ShapeDtypeStruct(seq_shape, bf16),
            *[jax.ShapeDtypeStruct((4, *item.shape), bf16) for item in cut],
        ),
        in_specs=[SMEM] + [HBM] * (2 + count),
        out_specs=(HBM, HBM, VMEM, VMEM, HBM) + (HBM,) * count,
        scratch_shapes=[
            pltpu.VMEM(qkv_shape, bf16),
            pltpu.VMEM((own, parts, 8, piece, features), bf16),
            pltpu.VMEM((own, piece, 8 * features), bf16),
            *forward_scratch(length, heads, width),
            *[pltpu.VMEM(item.shape, bf16) for item in cut],
            *semaphores(7 + 3 + 14 + count * Gather.copies_each, 2 * count + 6),
        ],
    )(slopes, joined_all, upstream.reshape(parts, own, piece, 8 * features), *cut)
    wholes = [
        whole.reshape(4 * item.shape[0], item.shape[1]) for whole, item in zip(out[5:], weights)
    ]
    return out[0], out[1], (out[2], out[3]), out[4], wholes


def backward_fused_kernel(heads, width, count, *refs):
    slopes, diff_in, qkv_in, out_t_in, lse_in, layer_output = refs[:6]
    grads, refs = refs[6 : 6 + count], refs[6 + count :]
    joined_out, layer_out = refs[:2]
    outs, refs = refs[2 : 2 + count], refs[2 + count :]
    diff, qkv, out_t, lse, joined, layer_own = refs[:6]
    attention = Backward(heads, width, slopes, qkv, diff, out_t, lse, joined, *refs[6:13])
    bufs, (send, recv, local) = refs[13 : 13 + 7 * count], refs[13 + 7 * count :]
    z, s, along_x, along_y, partner = place()
    lines, plane = line_of(z, s), plane_of(z, s)
    copies, locals_ = Copies(send, recv), Locals(local)
    features = heads * width
    reduce = Reduce(grads, outs, bufs, copies, locals_)

    own = [locals_.start(diff_in.at[:, :, :, columns_of(s, features)], diff.at[:, :, s])]
    own += [locals_.start(a, b) for a, b in ((qkv_in, qkv), (out_t_in, out_t), (lse_in, lse))]
    reduce.load()
    layer_load = locals_.start(layer_output.at[:, z], layer_own)
    greet(lines + plane)
    arriving = [
        copies.start(diff_in.at[:, :, :, columns_of(to[1], features)], diff.at[:, :, s], to)
        for to in plane
    ]
    for t in range(count):
        reduce.start(t)
    waiting = [copies.start(layer_output.at[:, to[0]], layer_out.at[z], to) for to in lines]
    finishing = []

    def hand_back(b):
        for to in plane:
            waiting.append(
                copies.start(
                    joined.at[b, :, to[1]], joined_out.at[b, :, :, columns_of(s, 3 * features)], to
                )
            )
        finishing.append(
            locals_.start(joined.at[b, :, s], joined_out.at[b, :, :, columns_of(s, 3 * features)])
        )

    reduce.exchange(0)
    layer_load.wait()
    finishing.append(locals_.start(layer_own, layer_out.at[z]))
    for copy in own:
        copy.wait()
    arrive(arriving)
    attention.prepare(0)
    attention.run(0, 0, 1)
    reduce.exchange(1)
    attention.run(0, 1, 4)
    reduce.spread(0)
    attention.finish(0)
    hand_back(0)
    attention.prepare(1)
    attention.run(1, 0, 1)
    reduce.exchange(2)
    reduce.spread(1)
    attention.run(1, 1, 4)
    attention.finish(1)
    reduce.spread(2)
    reduce.send(0)
    hand_back(1)
    reduce.send(1)
    reduce.send(2)
    for t in range(count):
        reduce.finish(t)
    arrive(waiting)
    copies.finish()
    for copy in finishing:
        copy.wait()


def backward_fused(attended_diff, qkv, saved, layer_output, grads, slopes, heads, width):
    own, parts, piece, columns = attended_diff.shape
    features = heads * width
    length = parts * 8 * piece
    cut = [split_grad(item) for item in grads]
    count = len(cut)
    out = remote_call(
        functools.partial(backward_fused_kernel, heads, width, count),
        "backward_fused",
        2,
        out_shape=(
            jax.ShapeDtypeStruct((own, parts, piece, 24 * features), bf16),
            jax.ShapeDtypeStruct((parts, own, piece, columns), bf16),
            *[jax.ShapeDtypeStruct(item.shape[3:], f32) for item in cut],
        ),
        in_specs=[SMEM] + [HBM] * (5 + count),
        out_specs=(HBM, HBM) + (VMEM,) * count,
        scratch_shapes=[
            pltpu.VMEM((own, parts, 8, piece, features), bf16),
            pltpu.VMEM(qkv.shape, bf16),
            *[pltpu.VMEM(item.shape, f32) for item in saved],
            pltpu.VMEM(qkv.shape, bf16),
            pltpu.VMEM((own, piece, columns), bf16),
            *backward_scratch(length, heads, width),
            *reduce_scratch(cut),
            *semaphores(7 + 3 + 14 + count * Reduce.copies_each, count + 8),
        ],
    )(slopes, attended_diff, qkv, *saved, layer_output, *cut)
    return out[0], out[1].reshape(parts * own, piece, columns), out[2:]


def end_kernel(input_grad, vector, grad, input_out, vector_out, out, *refs):
    input_own, ranks, plane_sum, others = refs[:4]
    bufs, (send, recv, local) = refs[4:11], refs[11:]
    z, s, _, _, _ = place()
    lines, plane = line_of(z, s), plane_of(z, s)
    copies, locals_ = Copies(send, recv), Locals(local)
    reduce = Reduce([grad], [out], bufs, copies, locals_)
    reduce.load()
    load = locals_.start(input_grad.at[:, z], input_own)
    load_vector = locals_.start(vector.at[:, s], ranks.at[0])
    greet(lines + plane)
    reduce.start(0)
    waiting = [copies.start(input_grad.at[:, to[0]], input_out.at[z], to) for to in lines]
    vectors = [
        copies.start(vector.at[:, to[1]], ranks.at[d + 1], to) for d, to in enumerate(plane)
    ]
    load.wait()
    keep = locals_.start(input_own, input_out.at[z])
    reduce.exchange(0)
    load_vector.wait()
    arrive(vectors)
    total = ranks[0]
    for d in range(1, 8):
        total = total + ranks[d]
    plane_sum[...] = total
    vectors = [
        copies.start(plane_sum.at[to[0]], others.at[k], to) for k, to in enumerate(lines)
    ]
    reduce.spread(0)
    reduce.send(0)
    arrive(vectors)
    total = plane_sum[z]
    for k in range(3):
        total = total + others[k]
    vector_out[...] = total
    reduce.finish(0)
    arrive(waiting)
    copies.finish()
    keep.wait()


def end(input_grad, vector, grad):
    own, parts, piece, features = input_grad.shape
    lanes = vector.shape[-1]
    padded = -(-lanes // 1024) * 1024
    vector = jnp.pad(vector, ((0, 0), (0, padded - lanes))).reshape(4, 8, padded // 128, 128)
    cut = split_grad(grad)
    out = remote_call(
        end_kernel,
        "end",
        3,
        out_shape=(
            jax.ShapeDtypeStruct((parts, own, piece, features), bf16),
            jax.ShapeDtypeStruct(vector.shape[2:], f32),
            jax.ShapeDtypeStruct(cut.shape[3:], f32),
        ),
        in_specs=[HBM] * 3,
        out_specs=(HBM, VMEM, VMEM),
        scratch_shapes=[
            pltpu.VMEM((own, piece, features), bf16),
            pltpu.VMEM((8, 4, padded // 128, 128), f32),
            pltpu.VMEM((4, padded // 128, 128), f32),
            pltpu.VMEM((3, padded // 128, 128), f32),
            *reduce_scratch([cut]),
            *semaphores(3 + 7 + 3 + Reduce.copies_each, 4),
        ],
    )(input_grad, vector, cut)
    return out[0].reshape(parts * own, piece, features), out[1].reshape(-1)[:lanes], out[2]


def per_device(
    layer_input,
    first_gain,
    first_shift,
    joined_weight,
    query_bias,
    value_bias,
    output_weight,
    output_bias,
    second_gain,
    second_shift,
    expand_weight,
    expand_bias,
    contract_weight,
    contract_bias,
    alibi_slopes,
    upstream,
):
    seqs, piece, features = layer_input.shape
    fs_count = lax.axis_size("fs")
    sp_count = lax.axis_size("sp")
    head_count = alibi_slopes.shape[0]
    width = features // head_count
    heads = head_count // sp_count
    rows = seqs * piece
    own = seqs // fs_count
    shape = (own, fs_count, piece)
    slopes = lax.dynamic_slice_in_dim(alibi_slopes, lax.axis_index("sp") * heads, heads)

    vectors = (
        first_gain, first_shift, query_bias, value_bias, output_bias,
        second_gain, second_shift, contract_bias, expand_bias,
    )
    fast = (fs_count, sp_count) == (4, 8) and own >= 1
    weights = (output_weight, expand_weight, contract_weight)
    gather = lambda item: lax.all_gather(item, "fs", axis=0, tiled=True)
    if fast:
        tokens, packed, joined_full = begin(layer_input, jnp.concatenate(vectors), joined_weight)
    else:
        tokens, joined_full = to_own_seqs(layer_input), gather(joined_weight)
        packed = lax.all_gather(jnp.concatenate(vectors), "fs", axis=0)
    tokens = tokens.reshape(rows, features).astype(f32)
    whole, at = [], 0
    for item in vectors:
        whole.append(packed[:, at : at + item.shape[0]].reshape(-1))
        at += item.shape[0]
    gain_one, shift_one, qbias, vbias, obias, gain_two, shift_two, cbias, ebias = [
        item.astype(f32) for item in whole
    ]

    normed_f, norm_back_one = jax.vjp(normalize, tokens, gain_one, shift_one)
    normed = normed_f.astype(bf16)
    joined_all = (matmul(normed, joined_full) + joined_bias_of(qbias, vbias, head_count)).astype(
        bf16
    )
    joined_all = joined_all.reshape(*shape, 3 * features)
    if fast:
        qkv, attended, saved, upstream_low, weights = forward_fused(
            joined_all, upstream, weights, slopes, heads, width
        )
    else:
        qkv = to_heads(joined_all)
        attended, *saved = attention_forward(qkv, slopes, heads, width)
        attended, upstream_low = from_heads(attended), to_own_seqs(upstream)
        weights = [gather(item) for item in weights]
    out_full, expand_full, contract_full = weights
    attended = attended.reshape(rows, features)
    upstream_low = upstream_low.reshape(rows, features)

    residual = tokens + (matmul(attended, out_full) + obias)
    second_f, norm_back_two = jax.vjp(normalize, residual, gain_two, shift_two)
    second = second_f.astype(bf16)
    expanded = matmul(second, expand_full) + ebias
    activated_f, gelu_back = jax.vjp(gelu_tanh, expanded)
    activated = activated_f.astype(bf16)
    result = residual + (matmul(activated, contract_full) + cbias)
    layer_output = result.astype(bf16).reshape(*shape, features)

    upstream_f = upstream_low.astype(f32)
    contract_grad = matmul_lt(activated, upstream_low)
    contract_bias_grad = jnp.sum(upstream_f, axis=0)
    act_grad = matmul_rt(upstream_low, contract_full)
    expand_diff = gelu_back(act_grad)[0].astype(bf16)
    expand_grad = matmul_lt(second, expand_diff)
    expand_bias_grad = jnp.sum(expand_diff.astype(f32), axis=0)
    second_back = matmul_rt(expand_diff, expand_full)
    resid_part, second_gain_grad, second_shift_grad = norm_back_two(second_back)
    residual_grad = upstream_f + resid_part

    branch_diff = residual_grad.astype(bf16)
    output_weight_grad = matmul_lt(attended, branch_diff)
    output_bias_grad = jnp.sum(branch_diff.astype(f32), axis=0)
    attended_diff = matmul_rt(branch_diff, out_full).astype(bf16)
    attended_diff = attended_diff.reshape(*shape, features)
    grads = (contract_grad, expand_grad, output_weight_grad)
    scatter = functools.partial(
        lax.psum_scatter, axis_name=("fs", "sp"), scatter_dimension=0, tiled=True
    )
    if fast:
        joined_diff, layer_output, grads = backward_fused(
            attended_diff, qkv, saved, layer_output, [item.astype(bf16) for item in grads],
            slopes, heads, width,
        )
    else:
        joined_diff = attention_backward(
            qkv, to_heads(attended_diff), *saved, slopes, heads, width
        )
        joined_diff, layer_output = from_heads(joined_diff), from_own_seqs(layer_output)
        grads = [scatter(item) for item in grads]
    contract_grad, expand_grad, output_weight_grad = grads
    joined_diff = joined_diff.reshape(rows, 3 * features)

    joined_grad = matmul_lt(normed, joined_diff)
    column_sums = jnp.sum(joined_diff.astype(f32), axis=0).reshape(head_count, 3, width)
    query_bias_grad = column_sums[:, 0].reshape(features)
    value_bias_grad = column_sums[:, 2].reshape(features)
    normed_back = matmul_rt(joined_diff, joined_full)
    input_part, first_gain_grad, first_shift_grad = norm_back_one(normed_back)
    input_grad = (residual_grad + input_part).astype(bf16).reshape(*shape, features)

    vector_grads = (
        first_gain_grad, first_shift_grad, query_bias_grad, value_bias_grad, output_bias_grad,
        second_gain_grad, second_shift_grad, contract_bias_grad, expand_bias_grad,
    )
    devices = fs_count * sp_count
    packed = jnp.concatenate([item.reshape(devices, -1) for item in vector_grads], axis=1)
    if fast:
        input_grad, packed, joined_grad = end(input_grad, packed, joined_grad.astype(bf16))
    else:
        input_grad, joined_grad = from_own_seqs(input_grad), scatter(joined_grad)
        packed = scatter(packed.reshape(-1))
    own_grads, at = [], 0
    for item in vector_grads:
        size = item.shape[0] // devices
        own_grads.append(packed[at : at + size])
        at += size
    g1, s1, qb, vb, ob, g2, s2, cb, eb = own_grads
    return (
        layer_output,
        input_grad,
        g1,
        s1,
        joined_grad,
        qb,
        vb,
        output_weight_grad,
        ob,
        g2,
        s2,
        expand_grad,
        eb,
        contract_grad,
        cb,
    )


def solution(mesh):
    tokens = P(None, ("fs", "sp"), None)
    both, both_rows = P(("fs", "sp")), P(("fs", "sp"), None)
    one, one_rows = P("fs"), P("fs", None)
    return jax.shard_map(
        per_device,
        mesh=mesh,
        in_specs=(
            tokens, one, one, one_rows, one, one, one_rows, one, one, one, one_rows, one,
            one_rows, one, P(), tokens,
        ),
        out_specs=(
            tokens, tokens, both, both, both_rows, both, both, both_rows, both, both, both,
            both_rows, both, both_rows, both,
        ),
        check_vma=False,
    )
```

```python
import functools
import math

import jax
import jax.numpy as jnp
from jax import lax
from jax.experimental import pallas as pl
from jax.experimental.pallas import tpu as pltpu
from jax.sharding import PartitionSpec as P

norm_eps = 1e-05
gelu_coef = 0.7978845608028654
masked_value = -1e30
f32 = jnp.float32
bf16 = jnp.bfloat16
MESH = pl.DeviceIdType.MESH
HBM = pl.BlockSpec(memory_space=pl.ANY)
VMEM = pl.BlockSpec(memory_space=pltpu.VMEM)
SMEM = pl.BlockSpec(memory_space=pltpu.SMEM)
vmem_bytes = 60 * 1024 * 1024


def normalize(values, norm_gain, norm_shift):
    center = values - jnp.mean(values, axis=-1, keepdims=True)
    variance = jnp.mean(center * center, axis=-1, keepdims=True)
    return center * lax.rsqrt(variance + norm_eps) * norm_gain + norm_shift


def gelu_tanh(values):
    return (
        0.5 * values * (1.0 + jnp.tanh(gelu_coef * (values + 0.044715 * values * values * values)))
    )


def matmul(left_side, right_side):
    return jnp.dot(left_side, right_side, preferred_element_type=f32)


def matmul_lt(left_side, right_side):
    return lax.dot_general(
        left_side, right_side, (((0,), (0,)), ((), ())), preferred_element_type=f32
    )


def matmul_rt(left_side, right_side):
    return lax.dot_general(
        left_side, right_side, (((1,), (1,)), ((), ())), preferred_element_type=f32
    )


def joined_bias_of(query_bias, value_bias, head_count):
    query_part = query_bias.astype(f32).reshape(head_count, -1)
    value_part = value_bias.astype(f32).reshape(head_count, -1)
    return jnp.stack([query_part, jnp.zeros_like(query_part), value_part], axis=1).reshape(-1)


def split_three(values):
    high = values.astype(bf16).astype(f32)
    rest = values - high
    middle = rest.astype(bf16).astype(f32)
    return high, middle, rest - middle


def key_columns(key_rows, slope, start):
    rows, width = key_rows.shape
    position = (start + lax.broadcasted_iota(jnp.int32, (rows, width), 0)).astype(f32)
    lane = lax.broadcasted_iota(jnp.int32, (rows, width), 1)
    high, middle, low = split_three(slope * position)
    extra = jnp.where(lane == 0, high, jnp.where(lane == 1, middle, jnp.where(lane == 2, low, 0.0)))
    return jnp.concatenate([key_rows.astype(f32), extra], axis=1).astype(bf16)


def query_columns(queries, scale):
    rows, width = queries.shape
    lane = lax.broadcasted_iota(jnp.int32, (rows, width), 1)
    ones = jnp.where(lane < 3, 1.0, 0.0)
    return jnp.concatenate([queries.astype(f32) * scale, ones], axis=1).astype(bf16)


def follow(n, after):
    for at, steps in after.items():

        def act(steps=steps):
            for step, *given in steps:
                step(*given)

        pl.when(n == at)(act)


class Forward:
    def __init__(self, heads, width, slopes, qkv, out, out_t, lse, keys, queries, values_t):
        self.heads, self.width, self.slopes, self.qkv, self.out = heads, width, slopes, qkv, out
        self.out_t, self.lse = out_t, lse
        self.keys, self.queries, self.values_t = keys, queries, values_t
        self.blocks = qkv.shape[1]
        self.block = qkv.shape[2] * qkv.shape[3]

    def rows(self, i):
        return pl.ds(pl.multiple_of(i * self.block, self.block), self.block)

    def prepare(self, b):
        width, block, qkv = self.width, self.block, self.qkv
        scale = 1.0 / math.sqrt(width)

        def body(i, _):
            rows = self.rows(i)
            for h in range(self.heads):
                base = h * 3 * width
                query, key, value = [
                    qkv[b, i, :, :, base + n * width : base + (n + 1) * width].reshape(block, width)
                    for n in range(3)
                ]
                self.keys[h, rows, :] = key_columns(key, self.slopes[h], i * block)
                self.queries[h, rows, :] = query_columns(query, scale)
                self.values_t[h, :, rows] = value.astype(f32).T.astype(bf16)
            return 0

        lax.fori_loop(0, self.blocks, body, 0)

    def one(self, b, i):
        heads, width, block = self.heads, self.width, self.block
        rows = self.rows(i)
        query = [self.queries[h, rows, :] for h in range(heads)]

        def step(j, state, diagonal):
            columns = self.rows(j)
            result = []
            for h in range(heads):
                top, total, acc = state[h]
                scores = matmul_rt(self.keys[h, columns, :], query[h])
                if diagonal:
                    key_at = lax.broadcasted_iota(jnp.int32, (block, block), 0)
                    query_at = lax.broadcasted_iota(jnp.int32, (block, block), 1)
                    scores = jnp.where(key_at <= query_at, scores, masked_value)
                newest = jnp.maximum(top, jnp.max(scores, axis=0, keepdims=True))
                shrink = jnp.exp(top - newest)
                probs = jnp.exp(scores - newest)
                total = total * shrink + jnp.sum(probs, axis=0, keepdims=True)
                acc = acc * shrink + matmul(self.values_t[h, :, columns], probs.astype(bf16))
                result.append((newest, total, acc))
            return tuple(result)

        state = tuple(
            (
                jnp.full((1, block), masked_value, f32),
                jnp.zeros((1, block), f32),
                jnp.zeros((width, block), f32),
            )
            for h in range(heads)
        )
        state = lax.fori_loop(0, i, lambda j, s: step(j, s, False), state)
        state = step(i, state, True)
        finished = []
        for h in range(heads):
            top, total, acc = state[h]
            result = acc / total
            self.out_t[b, h, :, rows] = result
            self.lse[b, h, :, rows] = top + jnp.log(total)
            finished.append(result)
        joined = finished[0] if heads == 1 else jnp.concatenate(finished, axis=0)
        self.out[b, i] = joined.T.astype(bf16).reshape(self.out.shape[2:])

    def run(self, after):
        blocks = self.blocks

        def body(n, _):
            b, i = n // blocks, n % blocks
            pl.when(i == 0)(lambda: self.prepare(b))
            self.one(b, i)
            follow(n, after)
            return 0

        lax.fori_loop(0, self.qkv.shape[0] * blocks, body, 0)


def forward_kernel(heads, width, *refs):
    Forward(heads, width, *refs).run({})


def saved_shapes(seqs, length, heads, width):
    return (
        jax.ShapeDtypeStruct((seqs, heads, width, length), f32),
        jax.ShapeDtypeStruct((seqs, heads, 1, length), f32),
    )


def forward_scratch(length, heads, width):
    return [
        pltpu.VMEM((heads, length, 2 * width), bf16),
        pltpu.VMEM((heads, length, 2 * width), bf16),
        pltpu.VMEM((heads, width, length), bf16),
    ]


def attention_forward(qkv, slopes, heads, width):
    seqs, blocks, ranks, piece, _ = qkv.shape
    length = blocks * ranks * piece
    return pl.pallas_call(
        functools.partial(forward_kernel, heads, width),
        name="attention_forward",
        out_shape=(
            jax.ShapeDtypeStruct((seqs, blocks, ranks, piece, heads * width), bf16),
            *saved_shapes(seqs, length, heads, width),
        ),
        in_specs=[SMEM, VMEM],
        out_specs=(VMEM, VMEM, VMEM),
        scratch_shapes=forward_scratch(length, heads, width),
        compiler_params=pltpu.CompilerParams(vmem_limit_bytes=vmem_bytes),
    )(slopes, qkv)


class Backward:
    def __init__(
        self, heads, width, slopes, qkv, diff, out_t, lse, joined,
        keys, queries, keys_t, values, diffs, delta, query_acc,
    ):
        self.heads, self.width, self.slopes, self.qkv, self.diff = heads, width, slopes, qkv, diff
        self.out_t, self.lse, self.joined = out_t, lse, joined
        self.keys, self.queries, self.keys_t, self.values = keys, queries, keys_t, values
        self.diffs, self.delta, self.query_acc = diffs, delta, query_acc
        self.blocks = qkv.shape[1]
        self.block = qkv.shape[2] * qkv.shape[3]

    def rows(self, i):
        return pl.ds(pl.multiple_of(i * self.block, self.block), self.block)

    def prepare(self, b):
        width, block, qkv = self.width, self.block, self.qkv
        scale = 1.0 / math.sqrt(width)

        def body(i, _):
            rows = self.rows(i)
            for h in range(self.heads):
                base = h * 3 * width
                query, key, value = [
                    qkv[b, i, :, :, base + n * width : base + (n + 1) * width].reshape(block, width)
                    for n in range(3)
                ]
                self.keys[h, rows, :] = key_columns(key, self.slopes[h], i * block)
                self.keys_t[h, :, rows] = key.astype(f32).T.astype(bf16)
                self.queries[h, rows, :] = query_columns(query, scale)
                self.values[h, rows, :] = value
                part = self.diff[b, i, :, :, h * width : (h + 1) * width].reshape(block, width)
                self.diffs[h, rows, :] = part
                self.delta[h, :, rows] = jnp.sum(
                    part.astype(f32).T * self.out_t[b, h, :, rows], axis=0, keepdims=True
                )
                self.query_acc[h, :, rows] = jnp.zeros((width, block), f32)
            return 0

        lax.fori_loop(0, self.blocks, body, 0)

    def one(self, b, j):
        heads, width, block = self.heads, self.width, self.block
        tail = self.joined.shape[2:4] + (width,)
        columns = self.rows(j)

        def step(i, state, diagonal):
            rows = self.rows(i)
            result = []
            for h in range(heads):
                key_acc, value_acc = state[h]
                query = self.queries[h, rows, :]
                part = self.diffs[h, rows, :]
                scores = matmul_rt(self.keys[h, columns, :], query)
                probs = jnp.exp(scores - self.lse[b, h, :, rows])
                if diagonal:
                    key_at = lax.broadcasted_iota(jnp.int32, (block, block), 0)
                    query_at = lax.broadcasted_iota(jnp.int32, (block, block), 1)
                    probs = jnp.where(key_at <= query_at, probs, 0.0)
                prob_diff = matmul_rt(self.values[h, columns, :], part)
                score_diff = (probs * (prob_diff - self.delta[h, :, rows])).astype(bf16)
                value_acc = value_acc + matmul(probs.astype(bf16), part)
                key_acc = key_acc + matmul(score_diff, query)
                self.query_acc[h, :, rows] += matmul(self.keys_t[h, :, columns], score_diff)
                result.append((key_acc, value_acc))
            return tuple(result)

        state = tuple(
            (jnp.zeros((block, 2 * width), f32), jnp.zeros((block, width), f32))
            for h in range(heads)
        )
        state = step(j, state, True)
        state = lax.fori_loop(j + 1, self.blocks, lambda i, s: step(i, s, False), state)
        for h in range(heads):
            base = (h * 3 + 1) * width
            key_acc, value_acc = state[h]
            self.joined[b, j, :, :, base : base + width] = (
                key_acc[:, :width].astype(bf16).reshape(tail)
            )
            self.joined[b, j, :, :, base + width : base + 2 * width] = value_acc.astype(
                bf16
            ).reshape(tail)

    def run(self, after):
        blocks = self.blocks

        def body(n, _):
            b, j = n // blocks, n % blocks
            pl.when(j == 0)(lambda: self.prepare(b))
            self.one(b, j)
            pl.when(j == blocks - 1)(lambda: self.finish(b))
            follow(n, after)
            return 0

        lax.fori_loop(0, self.qkv.shape[0] * blocks, body, 0)

    def finish(self, b):
        width = self.width
        scale = 1.0 / math.sqrt(width)
        tail = self.joined.shape[2:4] + (width,)

        def body(i, _):
            for h in range(self.heads):
                base = h * 3 * width
                result = (self.query_acc[h, :, self.rows(i)] * scale).T.astype(bf16)
                self.joined[b, i, :, :, base : base + width] = result.reshape(tail)
            return 0

        lax.fori_loop(0, self.blocks, body, 0)


def backward_kernel(heads, width, *refs):
    Backward(heads, width, *refs).run({})


def backward_scratch(length, heads, width):
    return [
        pltpu.VMEM((heads, length, 2 * width), bf16),
        pltpu.VMEM((heads, length, 2 * width), bf16),
        pltpu.VMEM((heads, width, length), bf16),
        pltpu.VMEM((heads, length, width), bf16),
        pltpu.VMEM((heads, length, width), bf16),
        pltpu.VMEM((heads, 1, length), f32),
        pltpu.VMEM((heads, width, length), f32),
    ]


def attention_backward(qkv, diff, out_t, lse, slopes, heads, width):
    length = qkv.shape[1] * qkv.shape[2] * qkv.shape[3]
    return pl.pallas_call(
        functools.partial(backward_kernel, heads, width),
        name="attention_backward",
        out_shape=jax.ShapeDtypeStruct(qkv.shape, bf16),
        in_specs=[SMEM, VMEM, VMEM, VMEM, VMEM],
        out_specs=VMEM,
        scratch_shapes=backward_scratch(length, heads, width),
        compiler_params=pltpu.CompilerParams(vmem_limit_bytes=vmem_bytes),
    )(slopes, qkv, diff, out_t, lse)


def to_own_seqs(values):
    seqs, piece, features = values.shape
    parts = lax.axis_size("fs")
    values = values.reshape(parts, seqs // parts, piece, features)
    return lax.all_to_all(values, "fs", split_axis=0, concat_axis=0).transpose(1, 0, 2, 3)


def from_own_seqs(values):
    own, parts, piece, features = values.shape
    values = lax.all_to_all(values.transpose(1, 0, 2, 3), "fs", split_axis=0, concat_axis=0)
    return values.reshape(parts * own, piece, features)


def to_heads(values):
    own, parts, piece, features = values.shape
    ranks = lax.axis_size("sp")
    values = values.reshape(own, parts, piece, ranks, features // ranks)
    return lax.all_to_all(values, "sp", split_axis=3, concat_axis=2)


def from_heads(values):
    own, parts, ranks, piece, features = values.shape
    values = lax.all_to_all(values, "sp", split_axis=2, concat_axis=3)
    return values.reshape(own, parts, piece, ranks * features)


class Copies:
    def __init__(self, send, recv, local):
        self.send, self.recv, self.local = send, recv, local
        self.used, self.used_local, self.made = 0, 0, []

    def plan(self, source, target, device):
        copy = pltpu.make_async_remote_copy(
            src_ref=source,
            dst_ref=target,
            send_sem=self.send.at[self.used],
            recv_sem=self.recv.at[self.used],
            device_id=device,
            device_id_type=MESH,
        )
        self.used += 1
        self.made.append(copy)
        return copy

    def inside(self, source, target):
        copy = pltpu.make_async_copy(source, target, self.local.at[self.used_local])
        self.used_local += 1
        return copy

    def finish(self):
        assert (self.used, self.used_local) == (self.send.shape[0], self.local.shape[0])
        for copy in self.made:
            copy.wait_send()


def go(copies):
    for copy in copies:
        copy.start()


def arrive(copies):
    for copy in copies:
        copy.wait_recv()


def done(copies):
    for copy in copies:
        copy.wait()


def greet(devices):
    barrier = pltpu.get_barrier_semaphore()
    for device in devices:
        pl.semaphore_signal(barrier, inc=1, device_id=device, device_id_type=MESH)
    pl.semaphore_wait(barrier, len(devices))


class Place:
    def __init__(self):
        z, s = lax.axis_index("fs"), lax.axis_index("sp")
        self.z, self.s = z, s
        self.core, self.chip = s % 2, s // 2
        self.x, self.y = self.chip % 2, self.chip // 2
        self.along_x = s + 2 - 4 * self.x
        self.along_y = s + 4 - 8 * self.y
        self.partner = s + 1 - 2 * self.core
        self.diagonal = self.along_x + self.along_y - s
        self.chip_x, self.chip_y = self.along_x // 2, self.along_y // 2
        self.lines = [(lax.rem(z + k, 4), s) for k in range(1, 4)]
        self.plane = [(z, lax.rem(s + d, 8)) for d in range(1, 8)]
        self.to_x, self.to_y, self.to_core = [
            (z, to) for to in (self.along_x, self.along_y, self.partner)
        ]
        self.near = self.lines + [self.to_x, self.to_y, self.to_core]


class Gather:
    copies_each = 33

    def __init__(self, place, weights, wholes, kept, chunks, copies):
        z, s, lines = place.z, place.s, place.lines
        self.loads = [copies.inside(w, k) for w, k in zip(weights, kept)]
        self.own = [copies.inside(k, whole.at[z]) for k, whole in zip(kept, wholes)]
        self.first, self.second, self.third, self.cores, self.last = [], [], [], [], []
        for t, row, rows, column, columns in chunks:
            whole = wholes[t]
            wide = pl.ds(column, columns)
            every = pl.ds(row, rows)
            low, high = pl.ds(row, rows // 2), pl.ds(row + rows // 2, rows // 2)

            def same(k, rank, part, to):
                where = (k, rank, part, wide)
                return copies.plan(whole.at[where], whole.at[where], to)

            self.first.append(
                [
                    copies.plan(weights[t].at[s, every, wide], whole.at[z, s, every, wide], to)
                    for to in lines
                ]
            )
            second, third, cores, last = [], [], [], []
            for k, _ in lines:
                second.append(same(k, s, low, place.to_x))
                second.append(same(k, s, high, place.to_y))
                cores.append(same(k, s, every, place.to_core))
                third.append(same(k, s, low, place.to_y))
                third.append(same(k, s, high, place.to_x))
                third.append(same(k, place.along_x, low, place.to_y))
                third.append(same(k, place.along_y, high, place.to_x))
                for rank in (place.along_x, place.along_y, place.diagonal):
                    last.append(same(k, rank, every, place.to_core))
            self.second.append(second)
            self.third.append(third)
            self.cores.append(cores)
            self.last.append(last)

    def keep(self):
        done(self.loads)
        go(self.own)

    def start(self, t):
        go(self.first[t])

    def exchange(self, t):
        arrive(self.first[t])
        go(self.second[t])
        go(self.cores[t])

    def spread(self, t):
        arrive(self.second[t])
        go(self.third[t])

    def share(self, t):
        arrive(self.third[t])
        go(self.last[t])

    def finish(self):
        for copies in self.cores + self.last:
            arrive(copies)
        done(self.own)


def add_into(target, other):
    target[...] = (target[...].astype(f32) + other[...].astype(f32)).astype(target.dtype)


def add_blocks(steps, block_of):
    def body(i, _):
        add_into(*block_of(i))
        return 0

    lax.fori_loop(0, steps, body, 0)


class Reduce:
    copies_each = 10

    def __init__(self, place, grads, outs, bufs, chunks, copies):
        self.place, self.outs, self.chunks = place, outs, chunks
        self.bufs = [bufs[7 * t : 7 * t + 7] for t in range(len(chunks))]
        self.loads, self.first, self.second, self.third, self.fourth = [], [], [], [], []
        for (t, row, rows, column, columns), buf in zip(chunks, self.bufs):
            own, from_core, from_x, from_y, late_y, late_x, from_z = buf
            every, wide = pl.ds(row, rows), pl.ds(column, columns)
            low, high = pl.ds(0, rows // 2), pl.ds(rows // 2, rows // 2)
            self.loads.append(
                copies.inside(grads[t].at[:, :, place.core, every, wide], own)
            )
            self.first.append(
                copies.plan(
                    grads[t].at[:, :, 1 - place.core, every, wide], from_core, place.to_core
                )
            )
            step = []
            for k in range(2):
                step.append(
                    copies.plan(own.at[:, 2 * k + 1 - place.x, low], from_x.at[:, k], place.to_x)
                )
                step.append(
                    copies.plan(
                        own.at[:, 2 * (1 - place.y) + k, high], from_y.at[:, k], place.to_y
                    )
                )
            self.second.append(step)
            self.third.append(
                [
                    copies.plan(own.at[:, place.chip_y, low], late_y, place.to_y),
                    copies.plan(own.at[:, place.chip_x, high], late_x, place.to_x),
                ]
            )
            self.fourth.append(
                [
                    copies.plan(own.at[to[0], place.chip], from_z.at[k], to)
                    for k, to in enumerate(place.lines)
                ]
            )

    def start(self):
        go(self.first)

    def halves(self, t):
        half = self.chunks[t][2] // 2
        return pl.ds(0, half), pl.ds(half, half)

    def exchange(self, t):
        own, from_core = self.bufs[t][:2]
        self.loads[t].wait()
        arrive([self.first[t]])
        add_blocks(16, lambda i: (own.at[i // 4, i % 4], from_core.at[i // 4, i % 4]))
        go(self.second[t])

    def spread(self, t):
        own, _, from_x, from_y = self.bufs[t][:4]
        low, high = self.halves(t)
        x, y = self.place.x, self.place.y
        arrive(self.second[t])
        add_blocks(8, lambda i: (own.at[i // 2, 2 * (i % 2) + x, low], from_x.at[i // 2, i % 2]))
        add_blocks(8, lambda i: (own.at[i // 2, 2 * y + i % 2, high], from_y.at[i // 2, i % 2]))
        go(self.third[t])

    def send(self, t):
        own, _, _, _, late_y, late_x, _ = self.bufs[t]
        low, high = self.halves(t)
        chip = self.place.chip
        arrive(self.third[t])
        add_blocks(4, lambda i: (own.at[i, chip, low], late_y.at[i]))
        add_blocks(4, lambda i: (own.at[i, chip, high], late_x.at[i]))
        go(self.fourth[t])

    def finish(self, t):
        own, from_z = self.bufs[t][0], self.bufs[t][6]
        index, row, rows, column, columns = self.chunks[t]
        arrive(self.fourth[t])
        total = own[self.place.z, self.place.chip].astype(f32)
        for k in range(3):
            total = total + from_z[k].astype(f32)
        self.outs[index][row : row + rows, column : column + columns] = total


def reduce_scratch(chunks):
    scratch = []
    for _, _, rows, _, columns in chunks:
        half = rows // 2
        scratch += [
            pltpu.VMEM((4, 4, rows, columns), bf16),
            pltpu.VMEM((4, 4, rows, columns), bf16),
            pltpu.VMEM((4, 2, half, columns), bf16),
            pltpu.VMEM((4, 2, half, columns), bf16),
            pltpu.VMEM((4, half, columns), bf16),
            pltpu.VMEM((4, half, columns), bf16),
            pltpu.VMEM((3, rows, columns), bf16),
        ]
    return scratch


class ReduceLines:
    copies = 4 * 7 + 3

    def __init__(self, place, grad, out, bufs, copies):
        self.place, self.grad, self.out, self.bufs = place, grad, out, bufs
        from_core, from_x, from_y, late_y, late_x, from_z = bufs
        core, x, y = place.core, place.x, place.y
        self.order = [to[0] for to in place.lines] + [place.z]
        rows = grad.shape[3]
        self.low, self.high = pl.ds(0, rows // 2), pl.ds(rows // 2, rows // 2)
        self.first, self.second, self.third, self.fourth = [], [], [], []
        for k, at in enumerate(self.order):
            self.first.append(
                copies.plan(grad.at[at, :, 1 - core], from_core.at[k], place.to_core)
            )
            step = []
            for j in range(2):
                step.append(
                    copies.plan(
                        grad.at[at, 2 * j + 1 - x, core, self.low], from_x.at[k, j], place.to_x
                    )
                )
                step.append(
                    copies.plan(
                        grad.at[at, 2 * (1 - y) + j, core, self.high], from_y.at[k, j], place.to_y
                    )
                )
            self.second.append(step)
            self.third.append(
                [
                    copies.plan(grad.at[at, place.chip_y, core, self.low], late_y.at[k], place.to_y),
                    copies.plan(
                        grad.at[at, place.chip_x, core, self.high], late_x.at[k], place.to_x
                    ),
                ]
            )
            if k < 3:
                self.fourth.append(
                    copies.plan(grad.at[at, place.chip, core], from_z.at[k], place.lines[k])
                )

    def start(self, k):
        go([self.first[k]])

    def exchange(self, k):
        arrive([self.first[k]])
        at, core = self.order[k], self.place.core
        add_blocks(4, lambda i: (self.grad.at[at, i, core], self.bufs[0].at[k, i]))
        go(self.second[k])

    def spread(self, k):
        arrive(self.second[k])
        at, core, x, y = self.order[k], self.place.core, self.place.x, self.place.y
        add_blocks(
            2, lambda j: (self.grad.at[at, 2 * j + x, core, self.low], self.bufs[1].at[k, j])
        )
        add_blocks(
            2, lambda j: (self.grad.at[at, 2 * y + j, core, self.high], self.bufs[2].at[k, j])
        )
        go(self.third[k])

    def send(self, k):
        arrive(self.third[k])
        at, core, chip = self.order[k], self.place.core, self.place.chip
        add_into(self.grad.at[at, chip, core, self.low], self.bufs[3].at[k])
        add_into(self.grad.at[at, chip, core, self.high], self.bufs[4].at[k])
        go(self.fourth[k : k + 1])

    def finish(self):
        arrive(self.fourth)
        place = self.place
        total = self.grad[place.z, place.chip, place.core].astype(f32)
        for k in range(3):
            total = total + self.bufs[5][k].astype(f32)
        self.out[...] = total


def reduce_lines_scratch(rows, columns):
    half = rows // 2
    return [
        pltpu.VMEM((4, 4, rows, columns), bf16),
        pltpu.VMEM((4, 2, half, columns), bf16),
        pltpu.VMEM((4, 2, half, columns), bf16),
        pltpu.VMEM((4, half, columns), bf16),
        pltpu.VMEM((4, half, columns), bf16),
        pltpu.VMEM((3, rows, columns), bf16),
    ]


def split_grad(item):
    return item.reshape(4, 4, 2, item.shape[0] // 32, item.shape[1])


def split_weight(item):
    return item.reshape(8, item.shape[0] // 8, item.shape[1])


def chunks_of(index, rows, columns, count):
    if rows >= 64:
        return [(index, rows // count * n, rows // count, 0, columns) for n in range(count)]
    return [(index, 0, rows, columns // count * n, columns // count) for n in range(count)]


def semaphores(remote, local):
    return [pltpu.SemaphoreType.DMA((n,)) for n in (remote, remote, local)]


def remote_call(kernel, name, collective, **options):
    return pl.pallas_call(
        kernel,
        name=name,
        compiler_params=pltpu.CompilerParams(
            collective_id=collective, has_side_effects=True, vmem_limit_bytes=vmem_bytes
        ),
        **options,
    )


def begin_kernel(count, chunks, tokens, weight, *refs):
    vectors, refs = refs[:count], refs[count:]
    tokens_out, whole = refs[:2]
    vectors_out, refs = refs[2 : 2 + count], refs[2 + count :]
    tokens_own, kept = refs[:2]
    copies = Copies(*refs[2:])
    place = Place()
    z, lines = place.z, place.lines
    gather = Gather(place, [weight], [whole], [kept], chunks, copies)
    load = copies.inside(tokens.at[z], tokens_own)
    own = [copies.inside(tokens_own, tokens_out.at[:, z])]
    small = [copies.inside(item, out.at[z]) for item, out in zip(vectors, vectors_out)]
    waiting = []
    for to in lines:
        waiting.append(copies.plan(tokens.at[to[0]], tokens_out.at[:, z], to))
        waiting += [
            copies.plan(item, out.at[z], to) for item, out in zip(vectors, vectors_out)
        ]
    go(gather.loads)
    go([load])
    go(small)
    greet(place.near)
    gather.start(0)
    go(waiting)
    for t in range(1, len(chunks)):
        gather.start(t)
    load.wait()
    go(own)
    gather.keep()
    for t in range(len(chunks) + 2):
        if t < len(chunks):
            gather.exchange(t)
        if 0 <= t - 1 < len(chunks):
            gather.spread(t - 1)
        if 0 <= t - 2:
            gather.share(t - 2)
    gather.finish()
    arrive(waiting)
    copies.finish()
    done(own + small)


def begin(tokens, vectors, weight):
    seqs, piece, features = tokens.shape
    own = seqs // 4
    vectors = [item.reshape(-1, 128) for item in vectors]
    count = len(vectors)
    cut = split_weight(weight)
    chunks = chunks_of(0, cut.shape[1], cut.shape[2], 3)
    out = remote_call(
        functools.partial(begin_kernel, count, chunks),
        "begin",
        0,
        out_shape=(
            jax.ShapeDtypeStruct((own, 4, piece, features), bf16),
            jax.ShapeDtypeStruct((4, *cut.shape), bf16),
            *[jax.ShapeDtypeStruct((4, *item.shape), bf16) for item in vectors],
        ),
        in_specs=[HBM] * (2 + count),
        out_specs=(HBM,) * (2 + count),
        scratch_shapes=[
            pltpu.VMEM((own, piece, features), bf16),
            pltpu.VMEM(cut.shape, bf16),
            *semaphores(3 + 3 * count + len(chunks) * Gather.copies_each, 4 + count),
        ],
    )(tokens.reshape(4, own, piece, features), cut, *vectors)
    return out[0], out[1].reshape(4 * weight.shape[0], -1), [item.reshape(-1) for item in out[2:]]


def columns_of(rank, features):
    return pl.ds(pl.multiple_of(rank * features, 128), features)


def forward_fused_kernel(heads, width, count, chunks, slopes, source, upstream, *refs):
    weights, refs = refs[:count], refs[count:]
    qkv_out, attended, out_t, lse, upstream_out = refs[:5]
    wholes, refs = refs[5 : 5 + count], refs[5 + count :]
    qkv, result, upstream_own = refs[:3]
    attention = Forward(heads, width, slopes, qkv, result, out_t, lse, *refs[3:6])
    kept, refs = refs[6 : 6 + count], refs[6 + count :]
    copies = Copies(*refs)
    place = Place()
    z, s, lines, plane = place.z, place.s, place.lines, place.plane
    gather = Gather(place, weights, wholes, kept, chunks, copies)
    features = heads * width
    mine = columns_of(s, features)

    own = [
        copies.inside(source.at[:, :, :, columns_of(s, 3 * features)], qkv.at[:, :, s]),
        copies.inside(upstream.at[z], upstream_own),
    ]
    arriving = [
        copies.plan(source.at[:, :, :, columns_of(to[1], 3 * features)], qkv.at[:, :, s], to)
        for to in plane
    ]
    later = [copies.plan(upstream.at[to[0]], upstream_out.at[:, z], to) for to in lines]
    keeping = [copies.inside(upstream_own, upstream_out.at[:, z]), copies.inside(qkv, qkv_out)]
    back = [
        [copies.plan(result.at[b, :, to[1]], attended.at[b, :, :, mine], to) for to in plane]
        for b in range(2)
    ]
    stay = [copies.inside(result.at[b, :, s], attended.at[b, :, :, mine]) for b in range(2)]

    def hand_back(b):
        go(back[b] + stay[b : b + 1])

    go(gather.loads + own)
    greet(lines + plane)
    go(arriving)
    for t in range(len(chunks)):
        gather.start(t)
    go(later)
    done(own)
    gather.keep()
    arrive(arriving)
    go(keeping)
    for t in range(3):
        gather.exchange(t)
    attention.run(
        {
            2: [(gather.spread, 0), (gather.spread, 1), (gather.exchange, 3)],
            3: [(hand_back, 0)],
            5: [(gather.spread, 2), (gather.exchange, 4)],
            6: [(gather.spread, 3), (gather.share, 0), (gather.share, 1)],
            7: [(hand_back, 1)],
        }
    )
    gather.share(2)
    gather.spread(4)
    gather.share(3)
    gather.share(4)
    gather.finish()
    arrive(later + back[0] + back[1])
    copies.finish()
    done(keeping + stay)


def forward_fused(joined_all, upstream, weights, slopes, heads, width):
    own, parts, piece, columns = joined_all.shape
    features = heads * width
    length = parts * 8 * piece
    count = len(weights)
    cut = [split_weight(item) for item in weights]
    chunks = []
    for t, pieces in enumerate((1, 2, 2)):
        chunks += chunks_of(t, *cut[t].shape[1:], pieces)
    seq_shape = (own, parts, piece, 8 * features)
    qkv_shape = (own, parts, 8, piece, 3 * features)
    out = remote_call(
        functools.partial(forward_fused_kernel, heads, width, count, chunks),
        "forward_fused",
        1,
        out_shape=(
            jax.ShapeDtypeStruct(qkv_shape, bf16),
            jax.ShapeDtypeStruct(seq_shape, bf16),
            *saved_shapes(own, length, heads, width),
            jax.ShapeDtypeStruct(seq_shape, bf16),
            *[jax.ShapeDtypeStruct((4, *item.shape), bf16) for item in cut],
        ),
        in_specs=[SMEM] + [HBM] * (2 + count),
        out_specs=(HBM, HBM, VMEM, VMEM, HBM) + (HBM,) * count,
        scratch_shapes=[
            pltpu.VMEM(qkv_shape, bf16),
            pltpu.VMEM((own, parts, 8, piece, features), bf16),
            pltpu.VMEM((own, piece, 8 * features), bf16),
            *forward_scratch(length, heads, width),
            *[pltpu.VMEM(item.shape, bf16) for item in cut],
            *semaphores(7 + 3 + 14 + len(chunks) * Gather.copies_each, 2 * count + 6),
        ],
    )(slopes, joined_all, upstream.reshape(parts, own, piece, 8 * features), *cut)
    wholes = [
        whole.reshape(4 * item.shape[0], item.shape[1]) for whole, item in zip(out[5:], weights)
    ]
    return out[0], out[1], (out[2], out[3]), out[4], wholes


def feed_forward_kernel(
    expand, contract, expand_bias, second, upstream, residual,
    layer_out, second_back, expand_grad, bias_grad, contract_grad,
    expand_in, contract_in, second_t, expanded, grad, layer, staged, *refs,
):
    bufs, refs = refs[:6], refs[6:]
    loaded, stored, refs = refs[0], refs[1], refs[2:]
    copies = Copies(*refs)
    place = Place()
    z, lines = place.z, place.lines
    reduce = ReduceLines(place, grad, contract_grad, bufs, copies)
    rows, features = second.shape
    steps = 8
    wide = expand.shape[1] // steps
    own, parts, piece, _ = layer.shape

    def at(n):
        part = (z + 1 + n // 2) % 4
        return part, n % 2, pl.ds(pl.multiple_of((2 * part + n % 2) * wide, wide), wide)

    def load(n):
        _, _, where = at(n)
        return (
            pltpu.make_async_copy(expand.at[:, where], expand_in.at[:, where], loaded.at[0, n]),
            pltpu.make_async_copy(contract.at[where], contract_in.at[where], loaded.at[1, n]),
        )

    def store(n):
        _, _, where = at(n)
        slot = n % 2
        return pltpu.make_async_copy(
            staged.at[slot], expand_grad.at[:, where], stored.at[slot]
        )

    returned = [copies.plan(layer.at[:, to[0]], layer_out.at[z], to) for to in lines]
    stay = copies.inside(layer.at[:, z], layer_out.at[z])
    for n in range(steps):
        go(load(n))
    greet(place.near)
    second_t[...] = second[...].T
    second_back[...] = residual[...]

    def forward(n, after):
        part, side, where = at(n)
        done(load(n))
        values = matmul(second[...], expand_in[:, where]) + expand_bias[:, where]
        expanded[:, where] = values
        activated = gelu_tanh(values).astype(bf16)
        made = matmul(activated.T, upstream[...]).astype(bf16)
        grad[part, pl.ds(2 * side, 2)] = made.reshape(2, 2, wide // 4, features)
        second_back[...] += matmul(activated, contract_in[where, :])
        follow(n, after)
        return 0

    def backward(n, after):
        _, _, where = at(n)
        values = expanded[:, where]
        act_grad = matmul_rt(upstream[...], contract_in[where, :])
        bent = jnp.tanh(gelu_coef * (values + 0.044715 * values * values * values))
        slope = 0.5 * (1.0 + bent) + 0.5 * values * (1.0 - bent * bent) * (
            gelu_coef * (1.0 + 3.0 * 0.044715 * values * values)
        )
        diff = (act_grad * slope).astype(bf16)
        bias_grad[:, where] = jnp.sum(diff.astype(f32), axis=0, keepdims=True)
        pl.when(n >= 2)(lambda: store(n - 2).wait())
        staged[n % 2] = matmul(second_t[...], diff).astype(bf16)
        store(n).start()
        second_back[...] += matmul_rt(diff, expand_in[:, where])
        follow(n, after)
        return 0

    first = {
        1: [(reduce.start, 0)],
        2: [(reduce.exchange, 0)],
        3: [(reduce.start, 1)],
        4: [(reduce.spread, 0), (reduce.exchange, 1)],
        5: [(reduce.start, 2)],
        6: [(reduce.send, 0), (reduce.spread, 1), (reduce.exchange, 2)],
        7: [(reduce.start, 3)],
    }
    second_steps = {
        0: [(reduce.send, 1), (reduce.spread, 2), (reduce.exchange, 3)],
        2: [(reduce.send, 2), (reduce.spread, 3)],
        4: [(reduce.send, 3)],
    }
    lax.fori_loop(0, steps, lambda n, _: forward(n, first), 0)
    layer[...] = second_back[...].astype(bf16).reshape(layer.shape)
    second_back[...] = jnp.zeros_like(second_back)
    go(returned + [stay])
    lax.fori_loop(0, steps, lambda n, _: backward(n, second_steps), 0)
    reduce.finish()
    store(steps - 2).wait()
    store(steps - 1).wait()
    arrive(returned)
    copies.finish()
    done([stay])


def feed_forward(shape, expand, contract, expand_bias, second, upstream, residual):
    own, parts, piece = shape
    rows, features = second.shape
    hidden = expand.shape[1]
    wide = hidden // 8
    each = hidden // 32
    out = remote_call(
        feed_forward_kernel,
        "feed_forward",
        4,
        out_shape=(
            jax.ShapeDtypeStruct((parts, own, piece, features), bf16),
            jax.ShapeDtypeStruct((rows, features), f32),
            jax.ShapeDtypeStruct((features, hidden), bf16),
            jax.ShapeDtypeStruct((1, hidden), f32),
            jax.ShapeDtypeStruct((each, features), f32),
        ),
        in_specs=[HBM, HBM, VMEM, VMEM, VMEM, VMEM],
        out_specs=(HBM, VMEM, HBM, VMEM, VMEM),
        scratch_shapes=[
            pltpu.VMEM((features, hidden), bf16),
            pltpu.VMEM((hidden, features), bf16),
            pltpu.VMEM((features, rows), bf16),
            pltpu.VMEM((rows, hidden), f32),
            pltpu.VMEM((4, 4, 2, each, features), bf16),
            pltpu.VMEM((own, parts, piece, features), bf16),
            pltpu.VMEM((2, features, wide), bf16),
            *reduce_lines_scratch(each, features),
            pltpu.SemaphoreType.DMA((2, 8)),
            pltpu.SemaphoreType.DMA((2,)),
            *semaphores(ReduceLines.copies + 3, 1),
        ],
    )(expand, contract, expand_bias, second, upstream, residual)
    return out[0].reshape(parts * own, piece, features), *out[1:]


def backward_fused_kernel(heads, width, count, chunks, *refs):
    slopes, diff_in, qkv_in, out_t_in, lse_in = refs[:5]
    grads, refs = refs[5 : 5 + count], refs[5 + count :]
    joined_out, outs, refs = refs[0], refs[1 : 1 + count], refs[1 + count :]
    diff, qkv, out_t, lse, joined = refs[:5]
    attention = Backward(heads, width, slopes, qkv, diff, out_t, lse, joined, *refs[5:12])
    bufs, refs = refs[12 : 12 + 7 * len(chunks)], refs[12 + 7 * len(chunks) :]
    copies = Copies(*refs)
    place = Place()
    s, plane = place.s, place.plane
    features = heads * width
    mine = columns_of(s, 3 * features)
    reduce = Reduce(place, grads, outs, bufs, chunks, copies)

    own = [copies.inside(diff_in.at[:, :, :, columns_of(s, features)], diff.at[:, :, s])]
    own += [copies.inside(a, b) for a, b in ((qkv_in, qkv), (out_t_in, out_t), (lse_in, lse))]
    arriving = [
        copies.plan(diff_in.at[:, :, :, columns_of(to[1], features)], diff.at[:, :, s], to)
        for to in plane
    ]
    back = [
        [copies.plan(joined.at[b, :, to[1]], joined_out.at[b, :, :, mine], to) for to in plane]
        for b in range(2)
    ]
    stay = [copies.inside(joined.at[b, :, s], joined_out.at[b, :, :, mine]) for b in range(2)]

    def hand_back(b):
        go(back[b] + stay[b : b + 1])

    go(own + reduce.loads)
    greet(place.lines + plane)
    go(arriving)
    reduce.start()
    for t in range(3):
        reduce.exchange(t)
    done(own)
    arrive(arriving)
    attention.run(
        {
            1: [(reduce.spread, 0)],
            3: [(hand_back, 0)],
            4: [(reduce.spread, 1), (reduce.spread, 2), (reduce.send, 0)],
            7: [(hand_back, 1)],
        }
    )
    reduce.send(1)
    reduce.send(2)
    for t in range(3):
        reduce.finish(t)
    arrive(back[0] + back[1])
    copies.finish()
    done(stay)


def backward_fused(attended_diff, qkv, saved, grads, slopes, heads, width):
    own, parts, piece, columns = attended_diff.shape
    features = heads * width
    length = parts * 8 * piece
    cut = [split_grad(item) for item in grads]
    count = len(cut)
    chunks = []
    for t, pieces in enumerate((2, 1)):
        chunks += chunks_of(t, *cut[t].shape[3:], pieces)
    out = remote_call(
        functools.partial(backward_fused_kernel, heads, width, count, chunks),
        "backward_fused",
        2,
        out_shape=(
            jax.ShapeDtypeStruct((own, parts, piece, 24 * features), bf16),
            *[jax.ShapeDtypeStruct(item.shape[3:], f32) for item in cut],
        ),
        in_specs=[SMEM] + [HBM] * (4 + count),
        out_specs=(HBM,) + (VMEM,) * count,
        scratch_shapes=[
            pltpu.VMEM((own, parts, 8, piece, features), bf16),
            pltpu.VMEM(qkv.shape, bf16),
            *[pltpu.VMEM(item.shape, f32) for item in saved],
            pltpu.VMEM(qkv.shape, bf16),
            *backward_scratch(length, heads, width),
            *reduce_scratch(chunks),
            *semaphores(7 + 14 + len(chunks) * Reduce.copies_each, len(chunks) + 6),
        ],
    )(slopes, attended_diff, qkv, *saved, *cut)
    return out[0], out[1:]


def end_kernel(chunks, input_grad, vector, grad, input_out, vector_out, out, *refs):
    input_own, ranks, plane_sum, others = refs[:4]
    bufs, refs = refs[4 : 4 + 7 * len(chunks)], refs[4 + 7 * len(chunks) :]
    copies = Copies(*refs)
    place = Place()
    z, s, lines, plane = place.z, place.s, place.lines, place.plane
    count = len(chunks)
    reduce = Reduce(place, [grad], [out], bufs, chunks, copies)
    load = copies.inside(input_grad.at[:, z], input_own)
    load_vector = copies.inside(vector.at[:, s], ranks.at[0])
    keep = copies.inside(input_own, input_out.at[z])
    waiting = [copies.plan(input_grad.at[:, to[0]], input_out.at[z], to) for to in lines]
    vectors = [
        copies.plan(vector.at[:, to[1]], ranks.at[d + 1], to) for d, to in enumerate(plane)
    ]
    sums = [copies.plan(plane_sum.at[to[0]], others.at[k], to) for k, to in enumerate(lines)]
    go(reduce.loads + [load, load_vector])
    greet(lines + plane)
    reduce.start()
    go(waiting + vectors)
    load.wait()
    go([keep])
    for t in range(count + 2):
        if t < count:
            reduce.exchange(t)
        if t == 0:
            load_vector.wait()
            arrive(vectors)
            total = ranks[0]
            for d in range(1, 8):
                total = total + ranks[d]
            plane_sum[...] = total
            go(sums)
        if 0 <= t - 1 < count:
            reduce.spread(t - 1)
        if 0 <= t - 2:
            reduce.send(t - 2)
    arrive(sums)
    total = plane_sum[z]
    for k in range(3):
        total = total + others[k]
    vector_out[...] = total
    for t in range(count):
        reduce.finish(t)
    arrive(waiting)
    copies.finish()
    keep.wait()


def end(input_grad, vector, grad):
    own, parts, piece, features = input_grad.shape
    lanes = vector.shape[-1]
    padded = -(-lanes // 1024) * 1024
    vector = jnp.pad(vector, ((0, 0), (0, padded - lanes))).reshape(4, 8, padded // 128, 128)
    cut = split_grad(grad)
    chunks = chunks_of(0, *cut.shape[3:], 3)
    out = remote_call(
        functools.partial(end_kernel, chunks),
        "end",
        3,
        out_shape=(
            jax.ShapeDtypeStruct((parts, own, piece, features), bf16),
            jax.ShapeDtypeStruct(vector.shape[2:], f32),
            jax.ShapeDtypeStruct(cut.shape[3:], f32),
        ),
        in_specs=[HBM] * 3,
        out_specs=(HBM, VMEM, VMEM),
        scratch_shapes=[
            pltpu.VMEM((own, piece, features), bf16),
            pltpu.VMEM((8, 4, padded // 128, 128), f32),
            pltpu.VMEM((4, padded // 128, 128), f32),
            pltpu.VMEM((3, padded // 128, 128), f32),
            *reduce_scratch(chunks),
            *semaphores(3 + 7 + 3 + len(chunks) * Reduce.copies_each, 3 + len(chunks)),
        ],
    )(input_grad, vector, cut)
    return out[0].reshape(parts * own, piece, features), out[1].reshape(-1)[:lanes], out[2]


def per_device(
    layer_input,
    first_gain,
    first_shift,
    joined_weight,
    query_bias,
    value_bias,
    output_weight,
    output_bias,
    second_gain,
    second_shift,
    expand_weight,
    expand_bias,
    contract_weight,
    contract_bias,
    alibi_slopes,
    upstream,
):
    seqs, piece, features = layer_input.shape
    fs_count = lax.axis_size("fs")
    sp_count = lax.axis_size("sp")
    head_count = alibi_slopes.shape[0]
    width = features // head_count
    heads = head_count // sp_count
    rows = seqs * piece
    own = seqs // fs_count
    shape = (own, fs_count, piece)
    slopes = lax.dynamic_slice_in_dim(alibi_slopes, lax.axis_index("sp") * heads, heads)

    vectors = (
        first_gain, first_shift, query_bias, value_bias, output_bias,
        second_gain, second_shift, contract_bias, expand_bias,
    )
    fast = (fs_count, sp_count) == (4, 8) and (own, heads) == (2, 2)
    weights = (output_weight, expand_weight, contract_weight)
    gather = lambda item: lax.all_gather(item, "fs", axis=0, tiled=True)
    if fast:
        tokens, joined_full, whole = begin(layer_input, vectors, joined_weight)
    else:
        tokens, joined_full = to_own_seqs(layer_input), gather(joined_weight)
        whole = [gather(item) for item in vectors]
    tokens = tokens.reshape(rows, features).astype(f32)
    gain_one, shift_one, qbias, vbias, obias, gain_two, shift_two, cbias, ebias = [
        item.astype(f32) for item in whole
    ]

    normed_f, norm_back_one = jax.vjp(normalize, tokens, gain_one, shift_one)
    normed = normed_f.astype(bf16)
    joined_all = (matmul(normed, joined_full) + joined_bias_of(qbias, vbias, head_count)).astype(
        bf16
    )
    joined_all = joined_all.reshape(*shape, 3 * features)
    if fast:
        qkv, attended, saved, upstream_low, weights = forward_fused(
            joined_all, upstream, weights, slopes, heads, width
        )
    else:
        qkv = to_heads(joined_all)
        attended, *saved = attention_forward(qkv, slopes, heads, width)
        attended, upstream_low = from_heads(attended), to_own_seqs(upstream)
        weights = [gather(item) for item in weights]
    out_full, expand_full, contract_full = weights
    attended = attended.reshape(rows, features)
    upstream_low = upstream_low.reshape(rows, features)

    residual = tokens + (matmul(attended, out_full) + obias)
    second_f, norm_back_two = jax.vjp(normalize, residual, gain_two, shift_two)
    second = second_f.astype(bf16)
    upstream_f = upstream_low.astype(f32)
    contract_bias_grad = jnp.sum(upstream_f, axis=0)
    if fast:
        layer_output, second_back, expand_grad, expand_bias_grad, contract_grad = feed_forward(
            shape, expand_full, contract_full, ebias.reshape(1, -1), second, upstream_low,
            residual + cbias,
        )
        expand_bias_grad = expand_bias_grad.reshape(-1)
    else:
        expanded = matmul(second, expand_full) + ebias
        activated_f, gelu_back = jax.vjp(gelu_tanh, expanded)
        activated = activated_f.astype(bf16)
        result = residual + (matmul(activated, contract_full) + cbias)
        layer_output = result.astype(bf16).reshape(*shape, features)

        contract_grad = matmul_lt(activated, upstream_low)
        act_grad = matmul_rt(upstream_low, contract_full)
        expand_diff = gelu_back(act_grad)[0].astype(bf16)
        expand_grad = matmul_lt(second, expand_diff)
        expand_bias_grad = jnp.sum(expand_diff.astype(f32), axis=0)
        second_back = matmul_rt(expand_diff, expand_full)
    resid_part, second_gain_grad, second_shift_grad = norm_back_two(second_back)
    residual_grad = upstream_f + resid_part

    branch_diff = residual_grad.astype(bf16)
    output_weight_grad = matmul_lt(attended, branch_diff)
    output_bias_grad = jnp.sum(branch_diff.astype(f32), axis=0)
    attended_diff = matmul_rt(branch_diff, out_full).astype(bf16)
    attended_diff = attended_diff.reshape(*shape, features)
    grads = (expand_grad, output_weight_grad)
    scatter = functools.partial(
        lax.psum_scatter, axis_name=("fs", "sp"), scatter_dimension=0, tiled=True
    )
    if fast:
        joined_diff, grads = backward_fused(
            attended_diff, qkv, saved, [item.astype(bf16) for item in grads], slopes, heads, width
        )
    else:
        joined_diff = attention_backward(
            qkv, to_heads(attended_diff), *saved, slopes, heads, width
        )
        joined_diff, layer_output = from_heads(joined_diff), from_own_seqs(layer_output)
        grads = [scatter(item) for item in grads]
        contract_grad = scatter(contract_grad)
    expand_grad, output_weight_grad = grads
    joined_diff = joined_diff.reshape(rows, 3 * features)

    joined_grad = matmul_lt(normed, joined_diff)
    column_sums = jnp.sum(joined_diff.astype(f32), axis=0).reshape(head_count, 3, width)
    query_bias_grad = column_sums[:, 0].reshape(features)
    value_bias_grad = column_sums[:, 2].reshape(features)
    normed_back = matmul_rt(joined_diff, joined_full)
    input_part, first_gain_grad, first_shift_grad = norm_back_one(normed_back)
    input_grad = (residual_grad + input_part).astype(bf16).reshape(*shape, features)

    vector_grads = (
        first_gain_grad, first_shift_grad, query_bias_grad, value_bias_grad, output_bias_grad,
        second_gain_grad, second_shift_grad, contract_bias_grad, expand_bias_grad,
    )
    devices = fs_count * sp_count
    packed = jnp.concatenate([item.reshape(devices, -1) for item in vector_grads], axis=1)
    if fast:
        input_grad, packed, joined_grad = end(input_grad, packed, joined_grad.astype(bf16))
    else:
        input_grad, joined_grad = from_own_seqs(input_grad), scatter(joined_grad)
        packed = scatter(packed.reshape(-1))
    own_grads, at = [], 0
    for item in vector_grads:
        size = item.shape[0] // devices
        own_grads.append(packed[at : at + size])
        at += size
    g1, s1, qb, vb, ob, g2, s2, cb, eb = own_grads
    return (
        layer_output,
        input_grad,
        g1,
        s1,
        joined_grad,
        qb,
        vb,
        output_weight_grad,
        ob,
        g2,
        s2,
        expand_grad,
        eb,
        contract_grad,
        cb,
    )


def solution(mesh):
    tokens = P(None, ("fs", "sp"), None)
    both, both_rows = P(("fs", "sp")), P(("fs", "sp"), None)
    one, one_rows = P("fs"), P("fs", None)
    return jax.shard_map(
        per_device,
        mesh=mesh,
        in_specs=(
            tokens, one, one, one_rows, one, one, one_rows, one, one, one, one_rows, one,
            one_rows, one, P(), tokens,
        ),
        out_specs=(
            tokens, tokens, both, both, both_rows, both, both, both_rows, both, both, both,
            both_rows, both, both_rows, both,
        ),
        check_vma=False,
    )
```

```python
import functools
import math

import jax
import jax.numpy as jnp
from jax import lax
from jax.experimental import pallas as pl
from jax.experimental.pallas import tpu as pltpu
from jax.sharding import PartitionSpec as P

norm_eps = 1e-05
gelu_coef = 0.7978845608028654
masked_value = -1e30
f32 = jnp.float32
bf16 = jnp.bfloat16
MESH = pl.DeviceIdType.MESH
HBM = pl.BlockSpec(memory_space=pl.ANY)
VMEM = pl.BlockSpec(memory_space=pltpu.VMEM)
SMEM = pl.BlockSpec(memory_space=pltpu.SMEM)
vmem_bytes = 60 * 1024 * 1024


def normalize(values, norm_gain, norm_shift):
    center = values - jnp.mean(values, axis=-1, keepdims=True)
    variance = jnp.mean(center * center, axis=-1, keepdims=True)
    return center * lax.rsqrt(variance + norm_eps) * norm_gain + norm_shift


def gelu_tanh(values):
    return (
        0.5 * values * (1.0 + jnp.tanh(gelu_coef * (values + 0.044715 * values * values * values)))
    )


def matmul(left_side, right_side):
    return jnp.dot(left_side, right_side, preferred_element_type=f32)


def matmul_lt(left_side, right_side):
    return lax.dot_general(
        left_side, right_side, (((0,), (0,)), ((), ())), preferred_element_type=f32
    )


def matmul_rt(left_side, right_side):
    return lax.dot_general(
        left_side, right_side, (((1,), (1,)), ((), ())), preferred_element_type=f32
    )


def joined_bias_of(query_bias, value_bias, head_count):
    query_part = query_bias.astype(f32).reshape(head_count, -1)
    value_part = value_bias.astype(f32).reshape(head_count, -1)
    return jnp.stack([query_part, jnp.zeros_like(query_part), value_part], axis=1).reshape(-1)


def split_three(values):
    high = values.astype(bf16).astype(f32)
    rest = values - high
    middle = rest.astype(bf16).astype(f32)
    return high, middle, rest - middle


def key_columns(key_rows, slope, start):
    rows, width = key_rows.shape
    position = (start + lax.broadcasted_iota(jnp.int32, (rows, width), 0)).astype(f32)
    lane = lax.broadcasted_iota(jnp.int32, (rows, width), 1)
    high, middle, low = split_three(slope * position)
    extra = jnp.where(lane == 0, high, jnp.where(lane == 1, middle, jnp.where(lane == 2, low, 0.0)))
    return jnp.concatenate([key_rows.astype(f32), extra], axis=1).astype(bf16)


def query_columns(queries, scale):
    rows, width = queries.shape
    lane = lax.broadcasted_iota(jnp.int32, (rows, width), 1)
    ones = jnp.where(lane < 3, 1.0, 0.0)
    return jnp.concatenate([queries.astype(f32) * scale, ones], axis=1).astype(bf16)


def follow(n, after):
    for at, steps in after.items():

        def act(steps=steps):
            for step, *given in steps:
                step(*given)

        pl.when(n == at)(act)


class Forward:
    def __init__(self, heads, width, slopes, qkv, out, out_t, lse, keys, queries, values_t):
        self.heads, self.width, self.slopes, self.qkv, self.out = heads, width, slopes, qkv, out
        self.out_t, self.lse = out_t, lse
        self.keys, self.queries, self.values_t = keys, queries, values_t
        self.blocks = qkv.shape[1]
        self.block = qkv.shape[2] * qkv.shape[3]

    def rows(self, i):
        return pl.ds(pl.multiple_of(i * self.block, self.block), self.block)

    def prepare(self, b):
        width, block, qkv = self.width, self.block, self.qkv
        scale = 1.0 / math.sqrt(width)

        def body(i, _):
            rows = self.rows(i)
            for h in range(self.heads):
                base = h * 3 * width
                query, key, value = [
                    qkv[b, i, :, :, base + n * width : base + (n + 1) * width].reshape(block, width)
                    for n in range(3)
                ]
                self.keys[h, rows, :] = key_columns(key, self.slopes[h], i * block)
                self.queries[h, rows, :] = query_columns(query, scale)
                self.values_t[h, :, rows] = value.astype(f32).T.astype(bf16)
            return 0

        lax.fori_loop(0, self.blocks, body, 0)

    def one(self, b, i):
        heads, width, block = self.heads, self.width, self.block
        rows = self.rows(i)
        query = [self.queries[h, rows, :] for h in range(heads)]

        def step(j, state, diagonal):
            columns = self.rows(j)
            result = []
            for h in range(heads):
                top, total, acc = state[h]
                scores = matmul_rt(self.keys[h, columns, :], query[h])
                if diagonal:
                    key_at = lax.broadcasted_iota(jnp.int32, (block, block), 0)
                    query_at = lax.broadcasted_iota(jnp.int32, (block, block), 1)
                    scores = jnp.where(key_at <= query_at, scores, masked_value)
                newest = jnp.maximum(top, jnp.max(scores, axis=0, keepdims=True))
                shrink = jnp.exp(top - newest)
                probs = jnp.exp(scores - newest)
                total = total * shrink + jnp.sum(probs, axis=0, keepdims=True)
                acc = acc * shrink + matmul(self.values_t[h, :, columns], probs.astype(bf16))
                result.append((newest, total, acc))
            return tuple(result)

        state = tuple(
            (
                jnp.full((1, block), masked_value, f32),
                jnp.zeros((1, block), f32),
                jnp.zeros((width, block), f32),
            )
            for h in range(heads)
        )
        state = lax.fori_loop(0, i, lambda j, s: step(j, s, False), state)
        state = step(i, state, True)
        finished = []
        for h in range(heads):
            top, total, acc = state[h]
            result = acc / total
            self.out_t[b, h, :, rows] = result
            self.lse[b, h, :, rows] = top + jnp.log(total)
            finished.append(result)
        joined = finished[0] if heads == 1 else jnp.concatenate(finished, axis=0)
        self.out[b, i] = joined.T.astype(bf16).reshape(self.out.shape[2:])

    def run(self, after):
        blocks = self.blocks

        def body(n, _):
            b, i = n // blocks, n % blocks
            pl.when(i == 0)(lambda: self.prepare(b))
            self.one(b, i)
            follow(n, after)
            return 0

        lax.fori_loop(0, self.qkv.shape[0] * blocks, body, 0)


def forward_kernel(heads, width, *refs):
    Forward(heads, width, *refs).run({})


def saved_shapes(seqs, length, heads, width):
    return (
        jax.ShapeDtypeStruct((seqs, heads, width, length), f32),
        jax.ShapeDtypeStruct((seqs, heads, 1, length), f32),
    )


def forward_scratch(length, heads, width):
    return [
        pltpu.VMEM((heads, length, 2 * width), bf16),
        pltpu.VMEM((heads, length, 2 * width), bf16),
        pltpu.VMEM((heads, width, length), bf16),
    ]


def attention_forward(qkv, slopes, heads, width):
    seqs, blocks, ranks, piece, _ = qkv.shape
    length = blocks * ranks * piece
    return pl.pallas_call(
        functools.partial(forward_kernel, heads, width),
        name="attention_forward",
        out_shape=(
            jax.ShapeDtypeStruct((seqs, blocks, ranks, piece, heads * width), bf16),
            *saved_shapes(seqs, length, heads, width),
        ),
        in_specs=[SMEM, VMEM],
        out_specs=(VMEM, VMEM, VMEM),
        scratch_shapes=forward_scratch(length, heads, width),
        compiler_params=pltpu.CompilerParams(vmem_limit_bytes=vmem_bytes),
    )(slopes, qkv)


class Backward:
    def __init__(
        self, heads, width, slopes, qkv, diff, out_t, lse, joined,
        keys, queries, keys_t, values, diffs, delta, query_acc,
    ):
        self.heads, self.width, self.slopes, self.qkv, self.diff = heads, width, slopes, qkv, diff
        self.out_t, self.lse, self.joined = out_t, lse, joined
        self.keys, self.queries, self.keys_t, self.values = keys, queries, keys_t, values
        self.diffs, self.delta, self.query_acc = diffs, delta, query_acc
        self.blocks = qkv.shape[1]
        self.block = qkv.shape[2] * qkv.shape[3]

    def rows(self, i):
        return pl.ds(pl.multiple_of(i * self.block, self.block), self.block)

    def prepare(self, b):
        width, block, qkv = self.width, self.block, self.qkv
        scale = 1.0 / math.sqrt(width)

        def body(i, _):
            rows = self.rows(i)
            for h in range(self.heads):
                base = h * 3 * width
                query, key, value = [
                    qkv[b, i, :, :, base + n * width : base + (n + 1) * width].reshape(block, width)
                    for n in range(3)
                ]
                self.keys[h, rows, :] = key_columns(key, self.slopes[h], i * block)
                self.keys_t[h, :, rows] = key.astype(f32).T.astype(bf16)
                self.queries[h, rows, :] = query_columns(query, scale)
                self.values[h, rows, :] = value
                part = self.diff[b, i, :, :, h * width : (h + 1) * width].reshape(block, width)
                self.diffs[h, rows, :] = part
                self.delta[h, :, rows] = jnp.sum(
                    part.astype(f32).T * self.out_t[b, h, :, rows], axis=0, keepdims=True
                )
                self.query_acc[h, :, rows] = jnp.zeros((width, block), f32)
            return 0

        lax.fori_loop(0, self.blocks, body, 0)

    def one(self, b, j):
        heads, width, block = self.heads, self.width, self.block
        tail = self.joined.shape[2:4] + (width,)
        columns = self.rows(j)

        def step(i, state, diagonal):
            rows = self.rows(i)
            result = []
            for h in range(heads):
                key_acc, value_acc = state[h]
                query = self.queries[h, rows, :]
                part = self.diffs[h, rows, :]
                scores = matmul_rt(self.keys[h, columns, :], query)
                probs = jnp.exp(scores - self.lse[b, h, :, rows])
                if diagonal:
                    key_at = lax.broadcasted_iota(jnp.int32, (block, block), 0)
                    query_at = lax.broadcasted_iota(jnp.int32, (block, block), 1)
                    probs = jnp.where(key_at <= query_at, probs, 0.0)
                prob_diff = matmul_rt(self.values[h, columns, :], part)
                score_diff = (probs * (prob_diff - self.delta[h, :, rows])).astype(bf16)
                value_acc = value_acc + matmul(probs.astype(bf16), part)
                key_acc = key_acc + matmul(score_diff, query)
                self.query_acc[h, :, rows] += matmul(self.keys_t[h, :, columns], score_diff)
                result.append((key_acc, value_acc))
            return tuple(result)

        state = tuple(
            (jnp.zeros((block, 2 * width), f32), jnp.zeros((block, width), f32))
            for h in range(heads)
        )
        state = step(j, state, True)
        state = lax.fori_loop(j + 1, self.blocks, lambda i, s: step(i, s, False), state)
        for h in range(heads):
            base = (h * 3 + 1) * width
            key_acc, value_acc = state[h]
            self.joined[b, j, :, :, base : base + width] = (
                key_acc[:, :width].astype(bf16).reshape(tail)
            )
            self.joined[b, j, :, :, base + width : base + 2 * width] = value_acc.astype(
                bf16
            ).reshape(tail)

    def run(self, after):
        blocks = self.blocks

        def body(n, _):
            b, j = n // blocks, n % blocks
            pl.when(j == 0)(lambda: self.prepare(b))
            self.one(b, j)
            pl.when(j == blocks - 1)(lambda: self.finish(b))
            follow(n, after)
            return 0

        lax.fori_loop(0, self.qkv.shape[0] * blocks, body, 0)

    def finish(self, b):
        width = self.width
        scale = 1.0 / math.sqrt(width)
        tail = self.joined.shape[2:4] + (width,)

        def body(i, _):
            for h in range(self.heads):
                base = h * 3 * width
                result = (self.query_acc[h, :, self.rows(i)] * scale).T.astype(bf16)
                self.joined[b, i, :, :, base : base + width] = result.reshape(tail)
            return 0

        lax.fori_loop(0, self.blocks, body, 0)


def backward_kernel(heads, width, *refs):
    Backward(heads, width, *refs).run({})


def backward_scratch(length, heads, width):
    return [
        pltpu.VMEM((heads, length, 2 * width), bf16),
        pltpu.VMEM((heads, length, 2 * width), bf16),
        pltpu.VMEM((heads, width, length), bf16),
        pltpu.VMEM((heads, length, width), bf16),
        pltpu.VMEM((heads, length, width), bf16),
        pltpu.VMEM((heads, 1, length), f32),
        pltpu.VMEM((heads, width, length), f32),
    ]


def attention_backward(qkv, diff, out_t, lse, slopes, heads, width):
    length = qkv.shape[1] * qkv.shape[2] * qkv.shape[3]
    return pl.pallas_call(
        functools.partial(backward_kernel, heads, width),
        name="attention_backward",
        out_shape=jax.ShapeDtypeStruct(qkv.shape, bf16),
        in_specs=[SMEM, VMEM, VMEM, VMEM, VMEM],
        out_specs=VMEM,
        scratch_shapes=backward_scratch(length, heads, width),
        compiler_params=pltpu.CompilerParams(vmem_limit_bytes=vmem_bytes),
    )(slopes, qkv, diff, out_t, lse)


def to_own_seqs(values):
    seqs, piece, features = values.shape
    parts = lax.axis_size("fs")
    values = values.reshape(parts, seqs // parts, piece, features)
    return lax.all_to_all(values, "fs", split_axis=0, concat_axis=0).transpose(1, 0, 2, 3)


def from_own_seqs(values):
    own, parts, piece, features = values.shape
    values = lax.all_to_all(values.transpose(1, 0, 2, 3), "fs", split_axis=0, concat_axis=0)
    return values.reshape(parts * own, piece, features)


def to_heads(values):
    own, parts, piece, features = values.shape
    ranks = lax.axis_size("sp")
    values = values.reshape(own, parts, piece, ranks, features // ranks)
    return lax.all_to_all(values, "sp", split_axis=3, concat_axis=2)


def from_heads(values):
    own, parts, ranks, piece, features = values.shape
    values = lax.all_to_all(values, "sp", split_axis=2, concat_axis=3)
    return values.reshape(own, parts, piece, ranks * features)


class Copies:
    def __init__(self, send, recv, local):
        self.send, self.recv, self.local = send, recv, local
        self.used, self.used_local, self.made = 0, 0, []

    def plan(self, source, target, device):
        copy = pltpu.make_async_remote_copy(
            src_ref=source,
            dst_ref=target,
            send_sem=self.send.at[self.used],
            recv_sem=self.recv.at[self.used],
            device_id=device,
            device_id_type=MESH,
        )
        self.used += 1
        self.made.append(copy)
        return copy

    def inside(self, source, target):
        copy = pltpu.make_async_copy(source, target, self.local.at[self.used_local])
        self.used_local += 1
        return copy

    def finish(self):
        assert (self.used, self.used_local) == (self.send.shape[0], self.local.shape[0])
        for copy in self.made:
            copy.wait_send()


def go(copies):
    for copy in copies:
        copy.start()


def arrive(copies):
    for copy in copies:
        copy.wait_recv()


def done(copies):
    for copy in copies:
        copy.wait()


def greet(devices):
    barrier = pltpu.get_barrier_semaphore()
    for device in devices:
        pl.semaphore_signal(barrier, inc=1, device_id=device, device_id_type=MESH)
    pl.semaphore_wait(barrier, len(devices))


class Place:
    def __init__(self):
        z, s = lax.axis_index("fs"), lax.axis_index("sp")
        self.z, self.s = z, s
        self.core, self.chip = s % 2, s // 2
        self.x, self.y = self.chip % 2, self.chip // 2
        self.along_x = s + 2 - 4 * self.x
        self.along_y = s + 4 - 8 * self.y
        self.partner = s + 1 - 2 * self.core
        self.diagonal = self.along_x + self.along_y - s
        self.chip_x, self.chip_y = self.along_x // 2, self.along_y // 2
        self.lines = [(lax.rem(z + k, 4), s) for k in range(1, 4)]
        self.plane = [(z, lax.rem(s + d, 8)) for d in range(1, 8)]
        self.to_x, self.to_y, self.to_core = [
            (z, to) for to in (self.along_x, self.along_y, self.partner)
        ]
        self.near = self.lines + [self.to_x, self.to_y, self.to_core]


class Gather:
    copies_each = 33

    def __init__(self, place, weights, wholes, kept, chunks, copies):
        z, s, lines = place.z, place.s, place.lines
        self.loads, self.own = [], []
        for weight, whole, keep in zip(weights, wholes, kept):
            if keep is None:
                self.loads.append(copies.inside(weight, whole.at[z]))
            else:
                self.loads.append(copies.inside(weight, keep))
                self.own.append(copies.inside(keep, whole.at[z]))
        self.first, self.second, self.third, self.cores, self.last = [], [], [], [], []
        for t, row, rows, column, columns in chunks:
            whole = wholes[t]
            wide = pl.ds(column, columns)
            every = pl.ds(row, rows)
            low, high = pl.ds(row, rows // 2), pl.ds(row + rows // 2, rows // 2)

            def same(k, rank, part, to):
                where = (k, rank, part, wide)
                return copies.plan(whole.at[where], whole.at[where], to)

            self.first.append(
                [
                    copies.plan(weights[t].at[s, every, wide], whole.at[z, s, every, wide], to)
                    for to in lines
                ]
            )
            second, third, cores, last = [], [], [], []
            for k, _ in lines:
                second.append(same(k, s, low, place.to_x))
                second.append(same(k, s, high, place.to_y))
                cores.append(same(k, s, every, place.to_core))
                third.append(same(k, s, low, place.to_y))
                third.append(same(k, s, high, place.to_x))
                third.append(same(k, place.along_x, low, place.to_y))
                third.append(same(k, place.along_y, high, place.to_x))
                for rank in (place.along_x, place.along_y, place.diagonal):
                    last.append(same(k, rank, every, place.to_core))
            self.second.append(second)
            self.third.append(third)
            self.cores.append(cores)
            self.last.append(last)

    def keep(self):
        done(self.loads)
        go(self.own)

    def start(self, t):
        go(self.first[t])

    def exchange(self, t):
        arrive(self.first[t])
        go(self.second[t])
        go(self.cores[t])

    def spread(self, t):
        arrive(self.second[t])
        go(self.third[t])

    def share(self, t):
        arrive(self.third[t])
        go(self.last[t])

    def complete(self, t):
        arrive(self.cores[t] + self.last[t])


def add_into(target, other):
    target[...] = (target[...].astype(f32) + other[...].astype(f32)).astype(target.dtype)


def add_blocks(steps, block_of):
    def body(i, _):
        add_into(*block_of(i))
        return 0

    lax.fori_loop(0, steps, body, 0)


class Reduce:
    copies_each = 10

    def __init__(self, place, grads, outs, bufs, chunks, copies):
        self.place, self.outs, self.chunks = place, outs, chunks
        self.bufs = [bufs[7 * t : 7 * t + 7] for t in range(len(chunks))]
        self.loads, self.first, self.second, self.third, self.fourth = [], [], [], [], []
        for (t, row, rows, column, columns), buf in zip(chunks, self.bufs):
            own, from_core, from_x, from_y, late_y, late_x, from_z = buf
            every, wide = pl.ds(row, rows), pl.ds(column, columns)
            low, high = pl.ds(0, rows // 2), pl.ds(rows // 2, rows // 2)
            self.loads.append(
                copies.inside(grads[t].at[:, :, place.core, every, wide], own)
            )
            self.first.append(
                copies.plan(
                    grads[t].at[:, :, 1 - place.core, every, wide], from_core, place.to_core
                )
            )
            step = []
            for k in range(2):
                step.append(
                    copies.plan(own.at[:, 2 * k + 1 - place.x, low], from_x.at[:, k], place.to_x)
                )
                step.append(
                    copies.plan(
                        own.at[:, 2 * (1 - place.y) + k, high], from_y.at[:, k], place.to_y
                    )
                )
            self.second.append(step)
            self.third.append(
                [
                    copies.plan(own.at[:, place.chip_y, low], late_y, place.to_y),
                    copies.plan(own.at[:, place.chip_x, high], late_x, place.to_x),
                ]
            )
            self.fourth.append(
                [
                    copies.plan(own.at[to[0], place.chip], from_z.at[k], to)
                    for k, to in enumerate(place.lines)
                ]
            )

    def start(self):
        go(self.first)

    def halves(self, t):
        half = self.chunks[t][2] // 2
        return pl.ds(0, half), pl.ds(half, half)

    def exchange(self, t):
        own, from_core = self.bufs[t][:2]
        self.loads[t].wait()
        arrive([self.first[t]])
        add_blocks(16, lambda i: (own.at[i // 4, i % 4], from_core.at[i // 4, i % 4]))
        go(self.second[t])

    def spread(self, t):
        own, _, from_x, from_y = self.bufs[t][:4]
        low, high = self.halves(t)
        x, y = self.place.x, self.place.y
        arrive(self.second[t])
        add_blocks(8, lambda i: (own.at[i // 2, 2 * (i % 2) + x, low], from_x.at[i // 2, i % 2]))
        add_blocks(8, lambda i: (own.at[i // 2, 2 * y + i % 2, high], from_y.at[i // 2, i % 2]))
        go(self.third[t])

    def send(self, t):
        own, _, _, _, late_y, late_x, _ = self.bufs[t]
        low, high = self.halves(t)
        chip = self.place.chip
        arrive(self.third[t])
        add_blocks(4, lambda i: (own.at[i, chip, low], late_y.at[i]))
        add_blocks(4, lambda i: (own.at[i, chip, high], late_x.at[i]))
        go(self.fourth[t])

    def finish(self, t):
        own, from_z = self.bufs[t][0], self.bufs[t][6]
        index, row, rows, column, columns = self.chunks[t]
        arrive(self.fourth[t])
        total = own[self.place.z, self.place.chip].astype(f32)
        for k in range(3):
            total = total + from_z[k].astype(f32)
        self.outs[index][row : row + rows, column : column + columns] = total


def reduce_scratch(chunks):
    scratch = []
    for _, _, rows, _, columns in chunks:
        half = rows // 2
        scratch += [
            pltpu.VMEM((4, 4, rows, columns), bf16),
            pltpu.VMEM((4, 4, rows, columns), bf16),
            pltpu.VMEM((4, 2, half, columns), bf16),
            pltpu.VMEM((4, 2, half, columns), bf16),
            pltpu.VMEM((4, half, columns), bf16),
            pltpu.VMEM((4, half, columns), bf16),
            pltpu.VMEM((3, rows, columns), bf16),
        ]
    return scratch


class ReduceLines:
    copies = 4 * 7 + 3

    def __init__(self, place, grad, out, bufs, copies):
        self.place, self.grad, self.out, self.bufs = place, grad, out, bufs
        from_core, from_x, from_y, late_y, late_x, from_z = bufs
        core, x, y = place.core, place.x, place.y
        self.order = [to[0] for to in place.lines] + [place.z]
        rows = grad.shape[3]
        self.low, self.high = pl.ds(0, rows // 2), pl.ds(rows // 2, rows // 2)
        self.first, self.second, self.third, self.fourth = [], [], [], []
        for k, at in enumerate(self.order):
            self.first.append(
                copies.plan(grad.at[at, :, 1 - core], from_core.at[k], place.to_core)
            )
            step = []
            for j in range(2):
                step.append(
                    copies.plan(
                        grad.at[at, 2 * j + 1 - x, core, self.low], from_x.at[k, j], place.to_x
                    )
                )
                step.append(
                    copies.plan(
                        grad.at[at, 2 * (1 - y) + j, core, self.high], from_y.at[k, j], place.to_y
                    )
                )
            self.second.append(step)
            self.third.append(
                [
                    copies.plan(grad.at[at, place.chip_y, core, self.low], late_y.at[k], place.to_y),
                    copies.plan(
                        grad.at[at, place.chip_x, core, self.high], late_x.at[k], place.to_x
                    ),
                ]
            )
            if k < 3:
                self.fourth.append(
                    copies.plan(grad.at[at, place.chip, core], from_z.at[k], place.lines[k])
                )

    def start(self, k):
        go([self.first[k]])

    def exchange(self, k):
        arrive([self.first[k]])
        at, core = self.order[k], self.place.core
        add_blocks(4, lambda i: (self.grad.at[at, i, core], self.bufs[0].at[k, i]))
        go(self.second[k])

    def spread(self, k):
        arrive(self.second[k])
        at, core, x, y = self.order[k], self.place.core, self.place.x, self.place.y
        add_blocks(
            2, lambda j: (self.grad.at[at, 2 * j + x, core, self.low], self.bufs[1].at[k, j])
        )
        add_blocks(
            2, lambda j: (self.grad.at[at, 2 * y + j, core, self.high], self.bufs[2].at[k, j])
        )
        go(self.third[k])

    def send(self, k):
        arrive(self.third[k])
        at, core, chip = self.order[k], self.place.core, self.place.chip
        add_into(self.grad.at[at, chip, core, self.low], self.bufs[3].at[k])
        add_into(self.grad.at[at, chip, core, self.high], self.bufs[4].at[k])
        go(self.fourth[k : k + 1])

    def finish(self):
        arrive(self.fourth)
        place = self.place
        total = self.grad[place.z, place.chip, place.core].astype(f32)
        for k in range(3):
            total = total + self.bufs[5][k].astype(f32)
        self.out[...] = total


def reduce_lines_scratch(rows, columns):
    half = rows // 2
    return [
        pltpu.VMEM((4, 4, rows, columns), bf16),
        pltpu.VMEM((4, 2, half, columns), bf16),
        pltpu.VMEM((4, 2, half, columns), bf16),
        pltpu.VMEM((4, half, columns), bf16),
        pltpu.VMEM((4, half, columns), bf16),
        pltpu.VMEM((3, rows, columns), bf16),
    ]


def split_grad(item):
    return item.reshape(4, 4, 2, item.shape[0] // 32, item.shape[1])


def split_weight(item):
    return item.reshape(8, item.shape[0] // 8, item.shape[1])


def chunks_of(index, rows, columns, count):
    if rows >= 64:
        return [(index, rows // count * n, rows // count, 0, columns) for n in range(count)]
    return [(index, 0, rows, columns // count * n, columns // count) for n in range(count)]


def semaphores(remote, local):
    return [pltpu.SemaphoreType.DMA((n,)) for n in (remote, remote, local)]


def remote_call(kernel, name, collective, **options):
    return pl.pallas_call(
        kernel,
        name=name,
        compiler_params=pltpu.CompilerParams(
            collective_id=collective, has_side_effects=True, vmem_limit_bytes=vmem_bytes
        ),
        **options,
    )


def columns_of(rank, features):
    return pl.ds(pl.multiple_of(rank * features, 128), features)


def forward_fused_kernel(heads, width, count, vector_count, chunks, slopes, tokens, upstream, *refs):
    vectors, refs = refs[:vector_count], refs[vector_count:]
    weights, refs = refs[:count], refs[count:]
    tokens_out, vectors_out, joined_out, qkv_out, attended, out_t, lse, upstream_out = refs[:8]
    wholes, refs = refs[8 : 7 + count], refs[7 + count :]
    held, small, values_of, joined, normed, outgoing, qkv, result, upstream_own = refs[:9]
    attention = Forward(heads, width, slopes, qkv, result, out_t, lse, *refs[9:12])
    kept, refs = refs[12 : 11 + count], refs[11 + count :]
    head_send, head_recv = refs[:2]
    copies = Copies(*refs[2:])
    place = Place()
    z, s, lines, plane = place.z, place.s, place.lines, place.plane
    gather = Gather(place, weights, [joined, *wholes], [None, *kept], chunks, copies)
    first = [t for t, chunk in enumerate(chunks) if chunk[0] == 0]
    later = [t for t, chunk in enumerate(chunks) if chunk[0] > 0]
    features = heads * width
    mine = columns_of(s, features)
    own_seqs, parts, piece, wide = held.shape

    load = copies.inside(tokens.at[z], held.at[:, z])
    load_upstream = copies.inside(upstream.at[z], upstream_own)
    seqs = [copies.plan(tokens.at[to[0]], held.at[:, z], to) for to in lines]
    vector_copies = [copies.plan(small.at[z], small.at[z], to) for to in lines]
    upstreams = [copies.plan(upstream.at[to[0]], upstream_out.at[:, z], to) for to in lines]
    keep_upstream = copies.inside(upstream_own, upstream_out.at[:, z])
    keeping = [
        copies.inside(held, tokens_out),
        copies.inside(small, vectors_out),
        copies.inside(joined, joined_out),
    ]
    keep_qkv = copies.inside(qkv, qkv_out)
    back = [
        [copies.plan(result.at[b, :, to[1]], attended.at[b, :, :, mine], to) for to in plane]
        for b in range(2)
    ]
    stay = [copies.inside(result.at[b, :, s], attended.at[b, :, :, mine]) for b in range(2)]

    def to_head(d):
        return pltpu.make_async_remote_copy(
            src_ref=outgoing.at[d],
            dst_ref=qkv.at[:, :, s],
            send_sem=head_send.at[d],
            recv_sem=head_recv.at[d],
            device_id=(z, lax.rem(s + 1 + d, 8)),
            device_id_type=MESH,
        )

    def hand_back(b):
        go(back[b] + stay[b : b + 1])

    go(gather.loads + [load, load_upstream])
    small[z] = jnp.zeros(small.shape[1:], bf16)
    for n, item in enumerate(vectors):
        small[z, n, : item.shape[0], :] = item[...]
    greet(lines + plane)
    for t in first:
        gather.start(t)
    go(seqs + vector_copies)
    for t in later:
        gather.start(t)
    go(upstreams)
    gather.keep()
    load.wait()
    for t in range(len(first) + 2):
        if t < len(first):
            gather.exchange(t)
        if 0 <= t - 1 < len(first):
            gather.spread(t - 1)
        if 0 <= t - 2:
            gather.share(t - 2)
    load_upstream.wait()
    keep_upstream.start()
    arrive(seqs + vector_copies)
    values_of[...] = small[...].astype(f32)

    def row_of(n):
        found = [values_of[k, n, r : r + 1, :] for k in range(4) for r in range(wide // 512)]
        return jnp.concatenate(found, axis=1)

    gain, shift = row_of(0), row_of(1)

    def norm(i, _):
        values = held[i // parts, i % parts].astype(f32)
        rows = pl.ds(pl.multiple_of(i * piece, piece), piece)
        normed[rows, :] = normalize(values, gain, shift).astype(bf16)
        return 0

    lax.fori_loop(0, own_seqs * parts, norm, 0)
    for t in first:
        gather.complete(t)
    go(keeping)

    def project(d, _):
        rank = lax.rem(s + 1 + d, 8)
        per = 8 // 4
        query_bias = values_of[rank // per, 2, pl.ds(rank % per, 1), :]
        value_bias = values_of[rank // per, 3, pl.ds(rank % per, 1), :]
        low = lax.broadcasted_iota(jnp.int32, query_bias.shape, 1) < width
        bias = jnp.concatenate(
            [
                jnp.where(low, query_bias, 0.0),
                jnp.where(low, value_bias, query_bias),
                jnp.where(low, 0.0, value_bias),
            ],
            axis=1,
        )
        weight = joined[:, :, :, columns_of(rank, 3 * features)].reshape(wide, 3 * features)
        made = (matmul(normed[...], weight) + bias).astype(bf16)
        outgoing[d] = made.reshape(outgoing.shape[1:])
        pl.when(d < 7)(lambda: to_head(d).start())
        return 0

    lax.fori_loop(0, 8, project, 0)
    own_copy = copies.inside(outgoing.at[7], qkv.at[:, :, s])
    own_copy.start()
    base = later[0]
    gather.exchange(base)
    gather.exchange(base + 1)
    own_copy.wait()
    for d in range(7):
        to_head(d).wait_recv()
    keep_qkv.start()
    gather.exchange(base + 2)
    attention.run(
        {
            2: [(gather.spread, base), (gather.spread, base + 1), (gather.exchange, base + 3)],
            3: [(hand_back, 0)],
            5: [(gather.spread, base + 2), (gather.exchange, base + 4)],
            6: [(gather.spread, base + 3), (gather.share, base), (gather.share, base + 1)],
            7: [(hand_back, 1)],
        }
    )
    gather.share(base + 2)
    gather.spread(base + 4)
    gather.share(base + 3)
    gather.share(base + 4)
    for t in later:
        gather.complete(t)
    arrive(upstreams + back[0] + back[1])
    for d in range(7):
        to_head(d).wait_send()
    copies.finish()
    done(gather.own + [keep_upstream, keep_qkv] + keeping + stay)


def forward_fused(tokens, upstream, vectors, weights, slopes, heads, width):
    seqs, piece, features = tokens.shape
    parts = 4
    own = seqs // parts
    columns = heads * width
    length = parts * 8 * piece
    vectors = [item.reshape(-1, 128) for item in vectors]
    cut = [split_weight(item) for item in weights]
    count, tall = len(cut), 8 * -(-max(item.shape[0] for item in vectors) // 8)
    chunks = []
    for t, pieces in enumerate((3, 1, 2, 2)):
        chunks += chunks_of(t, *cut[t].shape[1:], pieces)
    seq_shape = (own, parts, piece, features)
    qkv_shape = (own, parts, 8, piece, 3 * columns)
    small = (parts, len(vectors), tall, 128)
    out = remote_call(
        functools.partial(forward_fused_kernel, heads, width, count, len(vectors), chunks),
        "forward_fused",
        1,
        out_shape=(
            jax.ShapeDtypeStruct(seq_shape, bf16),
            jax.ShapeDtypeStruct(small, bf16),
            jax.ShapeDtypeStruct((parts, *cut[0].shape), bf16),
            jax.ShapeDtypeStruct(qkv_shape, bf16),
            jax.ShapeDtypeStruct(seq_shape, bf16),
            *saved_shapes(own, length, heads, width),
            jax.ShapeDtypeStruct(seq_shape, bf16),
            *[jax.ShapeDtypeStruct((parts, *item.shape), bf16) for item in cut[1:]],
        ),
        in_specs=[SMEM, HBM, HBM] + [VMEM] * len(vectors) + [HBM] * count,
        out_specs=(HBM,) * 5 + (VMEM, VMEM) + (HBM,) * count,
        scratch_shapes=[
            pltpu.VMEM(seq_shape, bf16),
            pltpu.VMEM(small, bf16),
            pltpu.VMEM(small, f32),
            pltpu.VMEM((parts, *cut[0].shape), bf16),
            pltpu.VMEM((own * parts * piece, features), bf16),
            pltpu.VMEM((8, own, parts, piece, 3 * columns), bf16),
            pltpu.VMEM(qkv_shape, bf16),
            pltpu.VMEM((own, parts, 8, piece, columns), bf16),
            pltpu.VMEM((own, piece, features), bf16),
            *forward_scratch(length, heads, width),
            *[pltpu.VMEM(item.shape, bf16) for item in cut[1:]],
            pltpu.SemaphoreType.DMA((7,)),
            pltpu.SemaphoreType.DMA((7,)),
            *semaphores(9 + 14 + len(chunks) * Gather.copies_each, 2 * count - 1 + 10),
        ],
    )(
        slopes,
        tokens.reshape(parts, own, piece, features),
        upstream.reshape(parts, own, piece, features),
        *vectors,
        *cut,
    )
    wholes = [
        whole.reshape(4 * item.shape[0], item.shape[1])
        for whole, item in zip((out[2], *out[8:]), weights)
    ]
    found = [out[1][:, n, : item.shape[0]].reshape(-1) for n, item in enumerate(vectors)]
    return out[0], found, wholes, out[3], out[4], (out[5], out[6]), out[7]


def feed_forward_kernel(
    expand, contract, expand_bias, second, upstream, residual,
    layer_out, second_back, expand_grad, bias_grad, contract_grad,
    expand_in, contract_in, second_t, expanded, grad, layer, staged, *refs,
):
    bufs, refs = refs[:6], refs[6:]
    loaded, stored, refs = refs[0], refs[1], refs[2:]
    copies = Copies(*refs)
    place = Place()
    z, lines = place.z, place.lines
    reduce = ReduceLines(place, grad, contract_grad, bufs, copies)
    rows, features = second.shape
    steps = 8
    wide = expand.shape[1] // steps
    own, parts, piece, _ = layer.shape

    def at(n):
        part = (z + 1 + n // 2) % 4
        return part, n % 2, pl.ds(pl.multiple_of((2 * part + n % 2) * wide, wide), wide)

    def load(n):
        _, _, where = at(n)
        return (
            pltpu.make_async_copy(expand.at[:, where], expand_in.at[:, where], loaded.at[0, n]),
            pltpu.make_async_copy(contract.at[where], contract_in.at[where], loaded.at[1, n]),
        )

    def store(n):
        _, _, where = at(n)
        slot = n % 2
        return pltpu.make_async_copy(
            staged.at[slot], expand_grad.at[:, where], stored.at[slot]
        )

    returned = [copies.plan(layer.at[:, to[0]], layer_out.at[z], to) for to in lines]
    stay = copies.inside(layer.at[:, z], layer_out.at[z])
    for n in range(steps):
        go(load(n))
    greet(place.near)
    second_t[...] = second[...].T
    second_back[...] = residual[...]

    def forward(n, after):
        part, side, where = at(n)
        done(load(n))
        values = matmul(second[...], expand_in[:, where]) + expand_bias[:, where]
        expanded[:, where] = values
        activated = gelu_tanh(values).astype(bf16)
        made = matmul(activated.T, upstream[...]).astype(bf16)
        grad[part, pl.ds(2 * side, 2)] = made.reshape(2, 2, wide // 4, features)
        second_back[...] += matmul(activated, contract_in[where, :])
        follow(n, after)
        return 0

    def backward(n, after):
        _, _, where = at(n)
        values = expanded[:, where]
        act_grad = matmul_rt(upstream[...], contract_in[where, :])
        bent = jnp.tanh(gelu_coef * (values + 0.044715 * values * values * values))
        slope = 0.5 * (1.0 + bent) + 0.5 * values * (1.0 - bent * bent) * (
            gelu_coef * (1.0 + 3.0 * 0.044715 * values * values)
        )
        diff = (act_grad * slope).astype(bf16)
        bias_grad[:, where] = jnp.sum(diff.astype(f32), axis=0, keepdims=True)
        pl.when(n >= 2)(lambda: store(n - 2).wait())
        staged[n % 2] = matmul(second_t[...], diff).astype(bf16)
        store(n).start()
        second_back[...] += matmul_rt(diff, expand_in[:, where])
        follow(n, after)
        return 0

    first = {
        1: [(reduce.start, 0)],
        2: [(reduce.exchange, 0)],
        3: [(reduce.start, 1)],
        4: [(reduce.spread, 0), (reduce.exchange, 1)],
        5: [(reduce.start, 2)],
        6: [(reduce.send, 0), (reduce.spread, 1), (reduce.exchange, 2)],
        7: [(reduce.start, 3)],
    }
    second_steps = {
        0: [(reduce.send, 1), (reduce.spread, 2), (reduce.exchange, 3)],
        2: [(reduce.send, 2), (reduce.spread, 3)],
        4: [(reduce.send, 3)],
    }
    lax.fori_loop(0, steps, lambda n, _: forward(n, first), 0)
    layer[...] = second_back[...].astype(bf16).reshape(layer.shape)
    second_back[...] = jnp.zeros_like(second_back)
    go(returned + [stay])
    lax.fori_loop(0, steps, lambda n, _: backward(n, second_steps), 0)
    reduce.finish()
    store(steps - 2).wait()
    store(steps - 1).wait()
    arrive(returned)
    copies.finish()
    done([stay])


def feed_forward(shape, expand, contract, expand_bias, second, upstream, residual):
    own, parts, piece = shape
    rows, features = second.shape
    hidden = expand.shape[1]
    wide = hidden // 8
    each = hidden // 32
    out = remote_call(
        feed_forward_kernel,
        "feed_forward",
        4,
        out_shape=(
            jax.ShapeDtypeStruct((parts, own, piece, features), bf16),
            jax.ShapeDtypeStruct((rows, features), f32),
            jax.ShapeDtypeStruct((features, hidden), bf16),
            jax.ShapeDtypeStruct((1, hidden), f32),
            jax.ShapeDtypeStruct((each, features), f32),
        ),
        in_specs=[HBM, HBM, VMEM, VMEM, VMEM, VMEM],
        out_specs=(HBM, VMEM, HBM, VMEM, VMEM),
        scratch_shapes=[
            pltpu.VMEM((features, hidden), bf16),
            pltpu.VMEM((hidden, features), bf16),
            pltpu.VMEM((features, rows), bf16),
            pltpu.VMEM((rows, hidden), f32),
            pltpu.VMEM((4, 4, 2, each, features), bf16),
            pltpu.VMEM((own, parts, piece, features), bf16),
            pltpu.VMEM((2, features, wide), bf16),
            *reduce_lines_scratch(each, features),
            pltpu.SemaphoreType.DMA((2, 8)),
            pltpu.SemaphoreType.DMA((2,)),
            *semaphores(ReduceLines.copies + 3, 1),
        ],
    )(expand, contract, expand_bias, second, upstream, residual)
    return out[0].reshape(parts * own, piece, features), *out[1:]


def backward_fused_kernel(heads, width, count, chunks, *refs):
    slopes, diff_in, qkv_in, out_t_in, lse_in = refs[:5]
    grads, refs = refs[5 : 5 + count], refs[5 + count :]
    joined_out, outs, refs = refs[0], refs[1 : 1 + count], refs[1 + count :]
    diff, qkv, out_t, lse, joined = refs[:5]
    attention = Backward(heads, width, slopes, qkv, diff, out_t, lse, joined, *refs[5:12])
    bufs, refs = refs[12 : 12 + 7 * len(chunks)], refs[12 + 7 * len(chunks) :]
    copies = Copies(*refs)
    place = Place()
    s, plane = place.s, place.plane
    features = heads * width
    mine = columns_of(s, 3 * features)
    reduce = Reduce(place, grads, outs, bufs, chunks, copies)

    own = [copies.inside(diff_in.at[:, :, :, columns_of(s, features)], diff.at[:, :, s])]
    own += [copies.inside(a, b) for a, b in ((qkv_in, qkv), (out_t_in, out_t), (lse_in, lse))]
    arriving = [
        copies.plan(diff_in.at[:, :, :, columns_of(to[1], features)], diff.at[:, :, s], to)
        for to in plane
    ]
    back = [
        [copies.plan(joined.at[b, :, to[1]], joined_out.at[b, :, :, mine], to) for to in plane]
        for b in range(2)
    ]
    stay = [copies.inside(joined.at[b, :, s], joined_out.at[b, :, :, mine]) for b in range(2)]

    def hand_back(b):
        go(back[b] + stay[b : b + 1])

    go(own + reduce.loads)
    greet(place.lines + plane)
    go(arriving)
    reduce.start()
    for t in range(3):
        reduce.exchange(t)
    done(own)
    arrive(arriving)
    attention.run(
        {
            1: [(reduce.spread, 0)],
            3: [(hand_back, 0)],
            4: [(reduce.spread, 1), (reduce.spread, 2), (reduce.send, 0)],
            7: [(hand_back, 1)],
        }
    )
    reduce.send(1)
    reduce.send(2)
    for t in range(3):
        reduce.finish(t)
    arrive(back[0] + back[1])
    copies.finish()
    done(stay)


def backward_fused(attended_diff, qkv, saved, grads, slopes, heads, width):
    own, parts, piece, columns = attended_diff.shape
    features = heads * width
    length = parts * 8 * piece
    cut = [split_grad(item) for item in grads]
    count = len(cut)
    chunks = []
    for t, pieces in enumerate((2, 1)):
        chunks += chunks_of(t, *cut[t].shape[3:], pieces)
    out = remote_call(
        functools.partial(backward_fused_kernel, heads, width, count, chunks),
        "backward_fused",
        2,
        out_shape=(
            jax.ShapeDtypeStruct((own, parts, piece, 24 * features), bf16),
            *[jax.ShapeDtypeStruct(item.shape[3:], f32) for item in cut],
        ),
        in_specs=[SMEM] + [HBM] * (4 + count),
        out_specs=(HBM,) + (VMEM,) * count,
        scratch_shapes=[
            pltpu.VMEM((own, parts, 8, piece, features), bf16),
            pltpu.VMEM(qkv.shape, bf16),
            *[pltpu.VMEM(item.shape, f32) for item in saved],
            pltpu.VMEM(qkv.shape, bf16),
            *backward_scratch(length, heads, width),
            *reduce_scratch(chunks),
            *semaphores(7 + 14 + len(chunks) * Reduce.copies_each, len(chunks) + 6),
        ],
    )(slopes, attended_diff, qkv, *saved, *cut)
    return out[0], out[1:]


def end_kernel(chunks, input_grad, vector, grad, input_out, vector_out, out, *refs):
    input_own, ranks, plane_sum, others = refs[:4]
    bufs, refs = refs[4 : 4 + 7 * len(chunks)], refs[4 + 7 * len(chunks) :]
    copies = Copies(*refs)
    place = Place()
    z, s, lines, plane = place.z, place.s, place.lines, place.plane
    count = len(chunks)
    reduce = Reduce(place, [grad], [out], bufs, chunks, copies)
    load = copies.inside(input_grad.at[:, z], input_own)
    load_vector = copies.inside(vector.at[:, s], ranks.at[0])
    keep = copies.inside(input_own, input_out.at[z])
    waiting = [copies.plan(input_grad.at[:, to[0]], input_out.at[z], to) for to in lines]
    vectors = [
        copies.plan(vector.at[:, to[1]], ranks.at[d + 1], to) for d, to in enumerate(plane)
    ]
    sums = [copies.plan(plane_sum.at[to[0]], others.at[k], to) for k, to in enumerate(lines)]
    go(reduce.loads + [load, load_vector])
    greet(lines + plane)
    reduce.start()
    go(waiting + vectors)
    load.wait()
    go([keep])
    for t in range(count + 2):
        if t < count:
            reduce.exchange(t)
        if t == 0:
            load_vector.wait()
            arrive(vectors)
            total = ranks[0]
            for d in range(1, 8):
                total = total + ranks[d]
            plane_sum[...] = total
            go(sums)
        if 0 <= t - 1 < count:
            reduce.spread(t - 1)
        if 0 <= t - 2:
            reduce.send(t - 2)
    arrive(sums)
    total = plane_sum[z]
    for k in range(3):
        total = total + others[k]
    vector_out[...] = total
    for t in range(count):
        reduce.finish(t)
    arrive(waiting)
    copies.finish()
    keep.wait()


def end(input_grad, vector, grad):
    own, parts, piece, features = input_grad.shape
    lanes = vector.shape[-1]
    padded = -(-lanes // 1024) * 1024
    vector = jnp.pad(vector, ((0, 0), (0, padded - lanes))).reshape(4, 8, padded // 128, 128)
    cut = split_grad(grad)
    chunks = chunks_of(0, *cut.shape[3:], 3)
    out = remote_call(
        functools.partial(end_kernel, chunks),
        "end",
        3,
        out_shape=(
            jax.ShapeDtypeStruct((parts, own, piece, features), bf16),
            jax.ShapeDtypeStruct(vector.shape[2:], f32),
            jax.ShapeDtypeStruct(cut.shape[3:], f32),
        ),
        in_specs=[HBM] * 3,
        out_specs=(HBM, VMEM, VMEM),
        scratch_shapes=[
            pltpu.VMEM((own, piece, features), bf16),
            pltpu.VMEM((8, 4, padded // 128, 128), f32),
            pltpu.VMEM((4, padded // 128, 128), f32),
            pltpu.VMEM((3, padded // 128, 128), f32),
            *reduce_scratch(chunks),
            *semaphores(3 + 7 + 3 + len(chunks) * Reduce.copies_each, 3 + len(chunks)),
        ],
    )(input_grad, vector, cut)
    return out[0].reshape(parts * own, piece, features), out[1].reshape(-1)[:lanes], out[2]


def per_device(
    layer_input,
    first_gain,
    first_shift,
    joined_weight,
    query_bias,
    value_bias,
    output_weight,
    output_bias,
    second_gain,
    second_shift,
    expand_weight,
    expand_bias,
    contract_weight,
    contract_bias,
    alibi_slopes,
    upstream,
):
    seqs, piece, features = layer_input.shape
    fs_count = lax.axis_size("fs")
    sp_count = lax.axis_size("sp")
    head_count = alibi_slopes.shape[0]
    width = features // head_count
    heads = head_count // sp_count
    rows = seqs * piece
    own = seqs // fs_count
    shape = (own, fs_count, piece)
    slopes = lax.dynamic_slice_in_dim(alibi_slopes, lax.axis_index("sp") * heads, heads)

    vectors = (
        first_gain, first_shift, query_bias, value_bias, output_bias,
        second_gain, second_shift, contract_bias, expand_bias,
    )
    fast = (fs_count, sp_count) == (4, 8) and (own, heads, width) == (2, 2, 64)
    weights = (joined_weight, output_weight, expand_weight, contract_weight)
    gather = lambda item: lax.all_gather(item, "fs", axis=0, tiled=True)
    if fast:
        tokens, whole, weights, qkv, attended, saved, upstream_low = forward_fused(
            layer_input, upstream, vectors, weights, slopes, heads, width
        )
    else:
        tokens, upstream_low = to_own_seqs(layer_input), to_own_seqs(upstream)
        whole, weights = [gather(item) for item in vectors], [gather(item) for item in weights]
    joined_full, out_full, expand_full, contract_full = weights
    tokens = tokens.reshape(rows, features).astype(f32)
    gain_one, shift_one, qbias, vbias, obias, gain_two, shift_two, cbias, ebias = [
        item.astype(f32) for item in whole
    ]

    normed_f, norm_back_one = jax.vjp(normalize, tokens, gain_one, shift_one)
    normed = normed_f.astype(bf16)
    if not fast:
        joined_bias = joined_bias_of(qbias, vbias, head_count)
        joined_all = (matmul(normed, joined_full) + joined_bias).astype(bf16)
        qkv = to_heads(joined_all.reshape(*shape, 3 * features))
        attended, *saved = attention_forward(qkv, slopes, heads, width)
        attended = from_heads(attended)
    attended = attended.reshape(rows, features)
    upstream_low = upstream_low.reshape(rows, features)

    residual = tokens + (matmul(attended, out_full) + obias)
    second_f, norm_back_two = jax.vjp(normalize, residual, gain_two, shift_two)
    second = second_f.astype(bf16)
    upstream_f = upstream_low.astype(f32)
    contract_bias_grad = jnp.sum(upstream_f, axis=0)
    if fast:
        layer_output, second_back, expand_grad, expand_bias_grad, contract_grad = feed_forward(
            shape, expand_full, contract_full, ebias.reshape(1, -1), second, upstream_low,
            residual + cbias,
        )
        expand_bias_grad = expand_bias_grad.reshape(-1)
    else:
        expanded = matmul(second, expand_full) + ebias
        activated_f, gelu_back = jax.vjp(gelu_tanh, expanded)
        activated = activated_f.astype(bf16)
        result = residual + (matmul(activated, contract_full) + cbias)
        layer_output = result.astype(bf16).reshape(*shape, features)

        contract_grad = matmul_lt(activated, upstream_low)
        act_grad = matmul_rt(upstream_low, contract_full)
        expand_diff = gelu_back(act_grad)[0].astype(bf16)
        expand_grad = matmul_lt(second, expand_diff)
        expand_bias_grad = jnp.sum(expand_diff.astype(f32), axis=0)
        second_back = matmul_rt(expand_diff, expand_full)
    resid_part, second_gain_grad, second_shift_grad = norm_back_two(second_back)
    residual_grad = upstream_f + resid_part

    branch_diff = residual_grad.astype(bf16)
    output_weight_grad = matmul_lt(attended, branch_diff)
    output_bias_grad = jnp.sum(branch_diff.astype(f32), axis=0)
    attended_diff = matmul_rt(branch_diff, out_full).astype(bf16)
    attended_diff = attended_diff.reshape(*shape, features)
    grads = (expand_grad, output_weight_grad)
    scatter = functools.partial(
        lax.psum_scatter, axis_name=("fs", "sp"), scatter_dimension=0, tiled=True
    )
    if fast:
        joined_diff, grads = backward_fused(
            attended_diff, qkv, saved, [item.astype(bf16) for item in grads], slopes, heads, width
        )
    else:
        joined_diff = attention_backward(
            qkv, to_heads(attended_diff), *saved, slopes, heads, width
        )
        joined_diff, layer_output = from_heads(joined_diff), from_own_seqs(layer_output)
        grads = [scatter(item) for item in grads]
        contract_grad = scatter(contract_grad)
    expand_grad, output_weight_grad = grads
    joined_diff = joined_diff.reshape(rows, 3 * features)

    joined_grad = matmul_lt(normed, joined_diff)
    column_sums = jnp.sum(joined_diff.astype(f32), axis=0).reshape(head_count, 3, width)
    query_bias_grad = column_sums[:, 0].reshape(features)
    value_bias_grad = column_sums[:, 2].reshape(features)
    normed_back = matmul_rt(joined_diff, joined_full)
    input_part, first_gain_grad, first_shift_grad = norm_back_one(normed_back)
    input_grad = (residual_grad + input_part).astype(bf16).reshape(*shape, features)

    vector_grads = (
        first_gain_grad, first_shift_grad, query_bias_grad, value_bias_grad, output_bias_grad,
        second_gain_grad, second_shift_grad, contract_bias_grad, expand_bias_grad,
    )
    devices = fs_count * sp_count
    packed = jnp.concatenate([item.reshape(devices, -1) for item in vector_grads], axis=1)
    if fast:
        input_grad, packed, joined_grad = end(input_grad, packed, joined_grad.astype(bf16))
    else:
        input_grad, joined_grad = from_own_seqs(input_grad), scatter(joined_grad)
        packed = scatter(packed.reshape(-1))
    own_grads, at = [], 0
    for item in vector_grads:
        size = item.shape[0] // devices
        own_grads.append(packed[at : at + size])
        at += size
    g1, s1, qb, vb, ob, g2, s2, cb, eb = own_grads
    return (
        layer_output,
        input_grad,
        g1,
        s1,
        joined_grad,
        qb,
        vb,
        output_weight_grad,
        ob,
        g2,
        s2,
        expand_grad,
        eb,
        contract_grad,
        cb,
    )


def solution(mesh):
    tokens = P(None, ("fs", "sp"), None)
    both, both_rows = P(("fs", "sp")), P(("fs", "sp"), None)
    one, one_rows = P("fs"), P("fs", None)
    return jax.shard_map(
        per_device,
        mesh=mesh,
        in_specs=(
            tokens, one, one, one_rows, one, one, one_rows, one, one, one, one_rows, one,
            one_rows, one, P(), tokens,
        ),
        out_specs=(
            tokens, tokens, both, both, both_rows, both, both, both_rows, both, both, both,
            both_rows, both, both_rows, both,
        ),
        check_vma=False,
    )
```

```python
import functools
import math

import jax
import jax.numpy as jnp
from jax import lax
from jax.experimental import pallas as pl
from jax.experimental.pallas import tpu as pltpu
from jax.sharding import PartitionSpec as P

norm_eps = 1e-05
gelu_coef = 0.7978845608028654
masked_value = -1e30
f32 = jnp.float32
bf16 = jnp.bfloat16
MESH = pl.DeviceIdType.MESH
HBM = pl.BlockSpec(memory_space=pl.ANY)
VMEM = pl.BlockSpec(memory_space=pltpu.VMEM)
SMEM = pl.BlockSpec(memory_space=pltpu.SMEM)
vmem_bytes = 60 * 1024 * 1024


def normalize(values, norm_gain, norm_shift):
    center = values - jnp.mean(values, axis=-1, keepdims=True)
    variance = jnp.mean(center * center, axis=-1, keepdims=True)
    return center * lax.rsqrt(variance + norm_eps) * norm_gain + norm_shift


def gelu_tanh(values):
    return (
        0.5 * values * (1.0 + jnp.tanh(gelu_coef * (values + 0.044715 * values * values * values)))
    )


def matmul(left_side, right_side):
    return jnp.dot(left_side, right_side, preferred_element_type=f32)


def matmul_lt(left_side, right_side):
    return lax.dot_general(
        left_side, right_side, (((0,), (0,)), ((), ())), preferred_element_type=f32
    )


def matmul_rt(left_side, right_side):
    return lax.dot_general(
        left_side, right_side, (((1,), (1,)), ((), ())), preferred_element_type=f32
    )


def joined_bias_of(query_bias, value_bias, head_count):
    query_part = query_bias.astype(f32).reshape(head_count, -1)
    value_part = value_bias.astype(f32).reshape(head_count, -1)
    return jnp.stack([query_part, jnp.zeros_like(query_part), value_part], axis=1).reshape(-1)


def split_three(values):
    high = values.astype(bf16).astype(f32)
    rest = values - high
    middle = rest.astype(bf16).astype(f32)
    return high, middle, rest - middle


def key_columns(key_rows, slope, start):
    rows, width = key_rows.shape
    position = (start + lax.broadcasted_iota(jnp.int32, (rows, width), 0)).astype(f32)
    lane = lax.broadcasted_iota(jnp.int32, (rows, width), 1)
    high, middle, low = split_three(slope * position)
    extra = jnp.where(lane == 0, high, jnp.where(lane == 1, middle, jnp.where(lane == 2, low, 0.0)))
    return jnp.concatenate([key_rows.astype(f32), extra], axis=1).astype(bf16)


def query_columns(queries, scale):
    rows, width = queries.shape
    lane = lax.broadcasted_iota(jnp.int32, (rows, width), 1)
    ones = jnp.where(lane < 3, 1.0, 0.0)
    return jnp.concatenate([queries.astype(f32) * scale, ones], axis=1).astype(bf16)


def follow(n, after):
    for at, steps in after.items():

        def act(steps=steps):
            for step, *given in steps:
                step(*given)

        pl.when(n == at)(act)


class Forward:
    def __init__(self, heads, width, slopes, qkv, out, out_t, lse, keys, queries, values_t):
        self.heads, self.width, self.slopes, self.qkv, self.out = heads, width, slopes, qkv, out
        self.out_t, self.lse = out_t, lse
        self.keys, self.queries, self.values_t = keys, queries, values_t
        self.blocks = qkv.shape[1]
        self.block = qkv.shape[2] * qkv.shape[3]

    def rows(self, i):
        return pl.ds(pl.multiple_of(i * self.block, self.block), self.block)

    def prepare(self, b):
        width, block, qkv = self.width, self.block, self.qkv
        scale = 1.0 / math.sqrt(width)

        def body(i, _):
            rows = self.rows(i)
            for h in range(self.heads):
                base = h * 3 * width
                query, key, value = [
                    qkv[b, i, :, :, base + n * width : base + (n + 1) * width].reshape(block, width)
                    for n in range(3)
                ]
                self.keys[h, rows, :] = key_columns(key, self.slopes[h], i * block)
                self.queries[h, rows, :] = query_columns(query, scale)
                self.values_t[h, :, rows] = value.astype(f32).T.astype(bf16)
            return 0

        lax.fori_loop(0, self.blocks, body, 0)

    def one(self, b, i):
        heads, width, block = self.heads, self.width, self.block
        rows = self.rows(i)
        query = [self.queries[h, rows, :] for h in range(heads)]

        def step(j, state, diagonal):
            columns = self.rows(j)
            result = []
            for h in range(heads):
                top, total, acc = state[h]
                scores = matmul_rt(self.keys[h, columns, :], query[h])
                if diagonal:
                    key_at = lax.broadcasted_iota(jnp.int32, (block, block), 0)
                    query_at = lax.broadcasted_iota(jnp.int32, (block, block), 1)
                    scores = jnp.where(key_at <= query_at, scores, masked_value)
                newest = jnp.maximum(top, jnp.max(scores, axis=0, keepdims=True))
                shrink = jnp.exp(top - newest)
                probs = jnp.exp(scores - newest)
                total = total * shrink + jnp.sum(probs, axis=0, keepdims=True)
                acc = acc * shrink + matmul(self.values_t[h, :, columns], probs.astype(bf16))
                result.append((newest, total, acc))
            return tuple(result)

        state = tuple(
            (
                jnp.full((1, block), masked_value, f32),
                jnp.zeros((1, block), f32),
                jnp.zeros((width, block), f32),
            )
            for h in range(heads)
        )
        state = lax.fori_loop(0, i, lambda j, s: step(j, s, False), state)
        state = step(i, state, True)
        finished = []
        for h in range(heads):
            top, total, acc = state[h]
            result = acc / total
            self.out_t[b, h, :, rows] = result
            self.lse[b, h, :, rows] = top + jnp.log(total)
            finished.append(result)
        joined = finished[0] if heads == 1 else jnp.concatenate(finished, axis=0)
        self.out[b, i] = joined.T.astype(bf16).reshape(self.out.shape[2:])

    def run(self, after, each=None):
        blocks = self.blocks

        def body(n, _):
            b, i = n // blocks, n % blocks
            pl.when(i == 0)(lambda: self.prepare(b))
            self.one(b, i)
            if each is not None:
                each(b, i)
            follow(n, after)
            return 0

        lax.fori_loop(0, self.qkv.shape[0] * blocks, body, 0)


def forward_kernel(heads, width, *refs):
    Forward(heads, width, *refs).run({})


def saved_shapes(seqs, length, heads, width):
    return (
        jax.ShapeDtypeStruct((seqs, heads, width, length), f32),
        jax.ShapeDtypeStruct((seqs, heads, 1, length), f32),
    )


def forward_scratch(length, heads, width):
    return [
        pltpu.VMEM((heads, length, 2 * width), bf16),
        pltpu.VMEM((heads, length, 2 * width), bf16),
        pltpu.VMEM((heads, width, length), bf16),
    ]


def attention_forward(qkv, slopes, heads, width):
    seqs, blocks, ranks, piece, _ = qkv.shape
    length = blocks * ranks * piece
    return pl.pallas_call(
        functools.partial(forward_kernel, heads, width),
        name="attention_forward",
        out_shape=(
            jax.ShapeDtypeStruct((seqs, blocks, ranks, piece, heads * width), bf16),
            *saved_shapes(seqs, length, heads, width),
        ),
        in_specs=[SMEM, VMEM],
        out_specs=(VMEM, VMEM, VMEM),
        scratch_shapes=forward_scratch(length, heads, width),
        compiler_params=pltpu.CompilerParams(vmem_limit_bytes=vmem_bytes),
    )(slopes, qkv)


class Backward:
    def __init__(
        self, heads, width, slopes, qkv, diff, out_t, lse, joined,
        keys, queries, keys_t, values, diffs, delta, query_acc,
    ):
        self.heads, self.width, self.slopes, self.qkv, self.diff = heads, width, slopes, qkv, diff
        self.out_t, self.lse, self.joined = out_t, lse, joined
        self.keys, self.queries, self.keys_t, self.values = keys, queries, keys_t, values
        self.diffs, self.delta, self.query_acc = diffs, delta, query_acc
        self.blocks = qkv.shape[1]
        self.block = qkv.shape[2] * qkv.shape[3]

    def rows(self, i):
        return pl.ds(pl.multiple_of(i * self.block, self.block), self.block)

    def prepare(self, b):
        width, block, qkv = self.width, self.block, self.qkv
        scale = 1.0 / math.sqrt(width)

        def body(i, _):
            rows = self.rows(i)
            for h in range(self.heads):
                base = h * 3 * width
                query, key, value = [
                    qkv[b, i, :, :, base + n * width : base + (n + 1) * width].reshape(block, width)
                    for n in range(3)
                ]
                self.keys[h, rows, :] = key_columns(key, self.slopes[h], i * block)
                self.keys_t[h, :, rows] = key.astype(f32).T.astype(bf16)
                self.queries[h, rows, :] = query_columns(query, scale)
                self.values[h, rows, :] = value
                part = self.diff[b, i, :, :, h * width : (h + 1) * width].reshape(block, width)
                self.diffs[h, rows, :] = part
                self.delta[h, :, rows] = jnp.sum(
                    part.astype(f32).T * self.out_t[b, h, :, rows], axis=0, keepdims=True
                )
                self.query_acc[h, :, rows] = jnp.zeros((width, block), f32)
            return 0

        lax.fori_loop(0, self.blocks, body, 0)

    def one(self, b, j):
        heads, width, block = self.heads, self.width, self.block
        tail = self.joined.shape[2:4] + (width,)
        columns = self.rows(j)

        def step(i, state, diagonal):
            rows = self.rows(i)
            result = []
            for h in range(heads):
                key_acc, value_acc = state[h]
                query = self.queries[h, rows, :]
                part = self.diffs[h, rows, :]
                scores = matmul_rt(self.keys[h, columns, :], query)
                probs = jnp.exp(scores - self.lse[b, h, :, rows])
                if diagonal:
                    key_at = lax.broadcasted_iota(jnp.int32, (block, block), 0)
                    query_at = lax.broadcasted_iota(jnp.int32, (block, block), 1)
                    probs = jnp.where(key_at <= query_at, probs, 0.0)
                prob_diff = matmul_rt(self.values[h, columns, :], part)
                score_diff = (probs * (prob_diff - self.delta[h, :, rows])).astype(bf16)
                value_acc = value_acc + matmul(probs.astype(bf16), part)
                key_acc = key_acc + matmul(score_diff, query)
                self.query_acc[h, :, rows] += matmul(self.keys_t[h, :, columns], score_diff)
                result.append((key_acc, value_acc))
            return tuple(result)

        state = tuple(
            (jnp.zeros((block, 2 * width), f32), jnp.zeros((block, width), f32))
            for h in range(heads)
        )
        state = step(j, state, True)
        state = lax.fori_loop(j + 1, self.blocks, lambda i, s: step(i, s, False), state)
        for h in range(heads):
            base = (h * 3 + 1) * width
            key_acc, value_acc = state[h]
            self.joined[b, j, :, :, base : base + width] = (
                key_acc[:, :width].astype(bf16).reshape(tail)
            )
            self.joined[b, j, :, :, base + width : base + 2 * width] = value_acc.astype(
                bf16
            ).reshape(tail)

    def run(self, after, each=None):
        blocks = self.blocks

        def body(n, _):
            b, j = n // blocks, n % blocks
            pl.when(j == 0)(lambda: self.prepare(b))
            self.one(b, j)
            self.finish(b, j)
            if each is not None:
                each(b, j)
            follow(n, after)
            return 0

        lax.fori_loop(0, self.qkv.shape[0] * blocks, body, 0)

    def finish(self, b, j):
        width = self.width
        scale = 1.0 / math.sqrt(width)
        for h in range(self.heads):
            base = h * 3 * width
            result = (self.query_acc[h, :, self.rows(j)] * scale).T.astype(bf16)
            self.joined[b, j, :, :, base : base + width] = result.reshape(
                self.joined.shape[2:4] + (width,)
            )


def backward_kernel(heads, width, *refs):
    Backward(heads, width, *refs).run({})


def backward_scratch(length, heads, width):
    return [
        pltpu.VMEM((heads, length, 2 * width), bf16),
        pltpu.VMEM((heads, length, 2 * width), bf16),
        pltpu.VMEM((heads, width, length), bf16),
        pltpu.VMEM((heads, length, width), bf16),
        pltpu.VMEM((heads, length, width), bf16),
        pltpu.VMEM((heads, 1, length), f32),
        pltpu.VMEM((heads, width, length), f32),
    ]


def attention_backward(qkv, diff, out_t, lse, slopes, heads, width):
    length = qkv.shape[1] * qkv.shape[2] * qkv.shape[3]
    return pl.pallas_call(
        functools.partial(backward_kernel, heads, width),
        name="attention_backward",
        out_shape=jax.ShapeDtypeStruct(qkv.shape, bf16),
        in_specs=[SMEM, VMEM, VMEM, VMEM, VMEM],
        out_specs=VMEM,
        scratch_shapes=backward_scratch(length, heads, width),
        compiler_params=pltpu.CompilerParams(vmem_limit_bytes=vmem_bytes),
    )(slopes, qkv, diff, out_t, lse)


def to_own_seqs(values):
    seqs, piece, features = values.shape
    parts = lax.axis_size("fs")
    values = values.reshape(parts, seqs // parts, piece, features)
    return lax.all_to_all(values, "fs", split_axis=0, concat_axis=0).transpose(1, 0, 2, 3)


def from_own_seqs(values):
    own, parts, piece, features = values.shape
    values = lax.all_to_all(values.transpose(1, 0, 2, 3), "fs", split_axis=0, concat_axis=0)
    return values.reshape(parts * own, piece, features)


def to_heads(values):
    own, parts, piece, features = values.shape
    ranks = lax.axis_size("sp")
    values = values.reshape(own, parts, piece, ranks, features // ranks)
    return lax.all_to_all(values, "sp", split_axis=3, concat_axis=2)


def from_heads(values):
    own, parts, ranks, piece, features = values.shape
    values = lax.all_to_all(values, "sp", split_axis=2, concat_axis=3)
    return values.reshape(own, parts, piece, ranks * features)


class Copies:
    def __init__(self, send, recv, local):
        self.send, self.recv, self.local = send, recv, local
        self.used, self.used_local, self.made = 0, 0, []

    def plan(self, source, target, device):
        copy = pltpu.make_async_remote_copy(
            src_ref=source,
            dst_ref=target,
            send_sem=self.send.at[self.used],
            recv_sem=self.recv.at[self.used],
            device_id=device,
            device_id_type=MESH,
        )
        self.used += 1
        self.made.append(copy)
        return copy

    def inside(self, source, target):
        copy = pltpu.make_async_copy(source, target, self.local.at[self.used_local])
        self.used_local += 1
        return copy

    def finish(self):
        assert (self.used, self.used_local) == (self.send.shape[0], self.local.shape[0])
        for copy in self.made:
            copy.wait_send()


def go(copies):
    for copy in copies:
        copy.start()


def arrive(copies):
    for copy in copies:
        copy.wait_recv()


def done(copies):
    for copy in copies:
        copy.wait()


def greet(devices):
    barrier = pltpu.get_barrier_semaphore()
    for device in devices:
        pl.semaphore_signal(barrier, inc=1, device_id=device, device_id_type=MESH)
    pl.semaphore_wait(barrier, len(devices))


class Place:
    def __init__(self):
        z, s = lax.axis_index("fs"), lax.axis_index("sp")
        self.z, self.s = z, s
        self.core, self.chip = s % 2, s // 2
        self.x, self.y = self.chip % 2, self.chip // 2
        self.along_x = s + 2 - 4 * self.x
        self.along_y = s + 4 - 8 * self.y
        self.partner = s + 1 - 2 * self.core
        self.diagonal = self.along_x + self.along_y - s
        self.chip_x, self.chip_y = self.along_x // 2, self.along_y // 2
        self.lines = [(lax.rem(z + k, 4), s) for k in range(1, 4)]
        self.plane = [(z, lax.rem(s + d, 8)) for d in range(1, 8)]
        self.to_x, self.to_y, self.to_core = [
            (z, to) for to in (self.along_x, self.along_y, self.partner)
        ]
        self.near = self.lines + [self.to_x, self.to_y, self.to_core]


class Gather:
    copies_each = 33

    def __init__(self, place, weights, wholes, kept, chunks, copies, given=None):
        z, s, lines = place.z, place.s, place.lines
        self.ready = arrive if given is None else done
        self.loads, self.own = [], []
        for weight, whole, keep in zip(weights, wholes, kept):
            if keep is None:
                self.loads.append(copies.inside(weight, whole.at[z]))
            else:
                self.loads.append(copies.inside(weight, keep))
                self.own.append(copies.inside(keep, whole.at[z]))
        self.first, self.second, self.third, self.cores, self.last = [], [], [], [], []
        for t, row, rows, column, columns in chunks:
            whole = wholes[t]
            wide = pl.ds(column, columns)
            every = pl.ds(row, rows)
            low, high = pl.ds(row, rows // 2), pl.ds(row + rows // 2, rows // 2)

            def same(k, rank, part, to):
                where = (k, rank, part, wide)
                return copies.plan(whole.at[where], whole.at[where], to)

            if given is None:
                first = [
                    copies.plan(weights[t].at[s, every, wide], whole.at[z, s, every, wide], to)
                    for to in lines
                ]
            else:
                first = [
                    copies.inside(given.at[k, every, wide], whole.at[k, s, every, wide])
                    for k, _ in lines
                ]
            self.first.append(first)
            second, third, cores, last = [], [], [], []
            for k, _ in lines:
                second.append(same(k, s, low, place.to_x))
                second.append(same(k, s, high, place.to_y))
                cores.append(same(k, s, every, place.to_core))
                third.append(same(k, s, low, place.to_y))
                third.append(same(k, s, high, place.to_x))
                third.append(same(k, place.along_x, low, place.to_y))
                third.append(same(k, place.along_y, high, place.to_x))
                for rank in (place.along_x, place.along_y, place.diagonal):
                    last.append(same(k, rank, every, place.to_core))
            self.second.append(second)
            self.third.append(third)
            self.cores.append(cores)
            self.last.append(last)

    def keep(self):
        done(self.loads)
        go(self.own)

    def start(self, t):
        go(self.first[t])

    def exchange(self, t):
        self.ready(self.first[t])
        go(self.second[t])
        go(self.cores[t])

    def spread(self, t):
        arrive(self.second[t])
        go(self.third[t])

    def share(self, t):
        arrive(self.third[t])
        go(self.last[t])

    def complete(self, t):
        arrive(self.cores[t] + self.last[t])


def add_into(target, other):
    target[...] = (target[...].astype(f32) + other[...].astype(f32)).astype(target.dtype)


def add_blocks(steps, block_of):
    def body(i, _):
        add_into(*block_of(i))
        return 0

    lax.fori_loop(0, steps, body, 0)


class Reduce:
    copies_each = 10

    def __init__(self, place, grads, outs, bufs, chunks, copies):
        self.place, self.outs, self.chunks = place, outs, chunks
        self.bufs = [bufs[7 * t : 7 * t + 7] for t in range(len(chunks))]
        self.loads, self.first, self.second, self.third, self.fourth = [], [], [], [], []
        for (t, row, rows, column, columns), buf in zip(chunks, self.bufs):
            own, from_core, from_x, from_y, late_y, late_x, from_z = buf
            every, wide = pl.ds(row, rows), pl.ds(column, columns)
            low, high = pl.ds(0, rows // 2), pl.ds(rows // 2, rows // 2)
            self.loads.append(
                copies.inside(grads[t].at[:, :, place.core, every, wide], own)
            )
            self.first.append(
                copies.plan(
                    grads[t].at[:, :, 1 - place.core, every, wide], from_core, place.to_core
                )
            )
            step = []
            for k in range(2):
                step.append(
                    copies.plan(own.at[:, 2 * k + 1 - place.x, low], from_x.at[:, k], place.to_x)
                )
                step.append(
                    copies.plan(
                        own.at[:, 2 * (1 - place.y) + k, high], from_y.at[:, k], place.to_y
                    )
                )
            self.second.append(step)
            self.third.append(
                [
                    copies.plan(own.at[:, place.chip_y, low], late_y, place.to_y),
                    copies.plan(own.at[:, place.chip_x, high], late_x, place.to_x),
                ]
            )
            self.fourth.append(
                [
                    copies.plan(own.at[to[0], place.chip], from_z.at[k], to)
                    for k, to in enumerate(place.lines)
                ]
            )

    def start(self):
        go(self.first)

    def halves(self, t):
        half = self.chunks[t][2] // 2
        return pl.ds(0, half), pl.ds(half, half)

    def exchange(self, t):
        own, from_core = self.bufs[t][:2]
        self.loads[t].wait()
        arrive([self.first[t]])
        add_blocks(16, lambda i: (own.at[i // 4, i % 4], from_core.at[i // 4, i % 4]))
        go(self.second[t])

    def spread(self, t):
        own, _, from_x, from_y = self.bufs[t][:4]
        low, high = self.halves(t)
        x, y = self.place.x, self.place.y
        arrive(self.second[t])
        add_blocks(8, lambda i: (own.at[i // 2, 2 * (i % 2) + x, low], from_x.at[i // 2, i % 2]))
        add_blocks(8, lambda i: (own.at[i // 2, 2 * y + i % 2, high], from_y.at[i // 2, i % 2]))
        go(self.third[t])

    def send(self, t):
        own, _, _, _, late_y, late_x, _ = self.bufs[t]
        low, high = self.halves(t)
        chip = self.place.chip
        arrive(self.third[t])
        add_blocks(4, lambda i: (own.at[i, chip, low], late_y.at[i]))
        add_blocks(4, lambda i: (own.at[i, chip, high], late_x.at[i]))
        go(self.fourth[t])

    def finish(self, t):
        own, from_z = self.bufs[t][0], self.bufs[t][6]
        index, row, rows, column, columns = self.chunks[t]
        arrive(self.fourth[t])
        total = own[self.place.z, self.place.chip].astype(f32)
        for k in range(3):
            total = total + from_z[k].astype(f32)
        self.outs[index][row : row + rows, column : column + columns] = total


def reduce_scratch(chunks):
    scratch = []
    for _, _, rows, _, columns in chunks:
        half = rows // 2
        scratch += [
            pltpu.VMEM((4, 4, rows, columns), bf16),
            pltpu.VMEM((4, 4, rows, columns), bf16),
            pltpu.VMEM((4, 2, half, columns), bf16),
            pltpu.VMEM((4, 2, half, columns), bf16),
            pltpu.VMEM((4, half, columns), bf16),
            pltpu.VMEM((4, half, columns), bf16),
            pltpu.VMEM((3, rows, columns), bf16),
        ]
    return scratch


class ReduceAlong(Reduce):
    def __init__(self, place, grad, out, buf, chunk, copies):
        self.place, self.grad, self.out, self.buf, self.chunk = place, grad, out, buf, chunk
        own, from_core, from_z, from_x, from_y, late_y, late_x = buf
        _, row, rows, column, columns = chunk
        every, wide = pl.ds(row, rows), pl.ds(column, columns)
        self.low, self.high = low, high = pl.ds(0, rows // 2), pl.ds(rows // 2, rows // 2)
        z, x, y = place.z, place.x, place.y
        self.load = copies.inside(grad.at[:, :, place.core, every, wide], own)
        self.first = copies.plan(
            grad.at[:, :, 1 - place.core, every, wide], from_core, place.to_core
        )
        self.second = [
            copies.plan(own.at[to[0]], from_z.at[k], to) for k, to in enumerate(place.lines)
        ]
        self.third = []
        for k in range(2):
            self.third.append(
                copies.plan(own.at[z, 2 * k + 1 - x, low], from_x.at[k], place.to_x)
            )
            self.third.append(
                copies.plan(own.at[z, 2 * (1 - y) + k, high], from_y.at[k], place.to_y)
            )
        self.fourth = [
            copies.plan(own.at[z, place.chip_y, low], late_y, place.to_y),
            copies.plan(own.at[z, place.chip_x, high], late_x, place.to_x),
        ]

    def exchange(self):
        own, from_core = self.buf[:2]
        self.load.wait()
        arrive([self.first])
        add_blocks(16, lambda i: (own.at[i // 4, i % 4], from_core.at[i // 4, i % 4]))
        go(self.second)

    def spread(self):
        own, _, from_z = self.buf[:3]
        z = self.place.z
        arrive(self.second)

        def body(i, _):
            total = own[z, i].astype(f32)
            for k in range(3):
                total = total + from_z[k, i].astype(f32)
            own[z, i] = total.astype(bf16)
            return 0

        lax.fori_loop(0, 4, body, 0)
        go(self.third)

    def send(self):
        own, _, _, from_x, from_y = self.buf[:5]
        z, x, y = self.place.z, self.place.x, self.place.y
        arrive(self.third)
        add_blocks(2, lambda j: (own.at[z, 2 * j + x, self.low], from_x.at[j]))
        add_blocks(2, lambda j: (own.at[z, 2 * y + j, self.high], from_y.at[j]))
        go(self.fourth)

    def finish(self):
        own, late_y, late_x = self.buf[0], self.buf[5], self.buf[6]
        z, chip = self.place.z, self.place.chip
        _, row, rows, column, columns = self.chunk
        arrive(self.fourth)
        half = rows // 2
        wide = slice(column, column + columns)
        self.out[row : row + half, wide] = own[z, chip, self.low].astype(f32) + late_y[...].astype(
            f32
        )
        self.out[row + half : row + rows, wide] = own[z, chip, self.high].astype(f32) + late_x[
            ...
        ].astype(f32)


def reduce_along_scratch(chunk):
    _, _, rows, _, columns = chunk
    half = rows // 2
    return [
        pltpu.VMEM((4, 4, rows, columns), bf16),
        pltpu.VMEM((4, 4, rows, columns), bf16),
        pltpu.VMEM((3, 4, rows, columns), bf16),
        pltpu.VMEM((2, half, columns), bf16),
        pltpu.VMEM((2, half, columns), bf16),
        pltpu.VMEM((half, columns), bf16),
        pltpu.VMEM((half, columns), bf16),
    ]


class HandBack:
    def __init__(self, place, source, target, features, send, recv, local):
        self.place, self.source, self.target = place, source, target
        self.mine = columns_of(place.s, features)
        self.send, self.recv, self.local = send, recv, local
        self.blocks = source.shape[1]

    def copy(self, b, i, d):
        rank = self.place.plane[d][1]
        n = b * self.blocks + i
        return pltpu.make_async_remote_copy(
            src_ref=self.source.at[b, i, rank],
            dst_ref=self.target.at[b, i, :, self.mine],
            send_sem=self.send.at[n, d],
            recv_sem=self.recv.at[n, d],
            device_id=self.place.plane[d],
            device_id_type=MESH,
        )

    def own(self, b, i):
        return pltpu.make_async_copy(
            self.source.at[b, i, self.place.s],
            self.target.at[b, i, :, self.mine],
            self.local.at[b * self.blocks + i],
        )

    def each(self, b, i):
        for d in range(7):
            self.copy(b, i, d).start()
        self.own(b, i).start()

    def finish(self):
        def body(n, _):
            b, i = n // self.blocks, n % self.blocks
            for d in range(7):
                self.copy(b, i, d).wait()
            self.own(b, i).wait()
            return 0

        lax.fori_loop(0, self.source.shape[0] * self.blocks, body, 0)


def hand_back_semaphores(steps):
    return [
        pltpu.SemaphoreType.DMA((steps, 7)),
        pltpu.SemaphoreType.DMA((steps, 7)),
        pltpu.SemaphoreType.DMA((steps,)),
    ]


class ReduceLines:
    copies = 4 * 7 + 3

    def __init__(self, place, grad, out, bufs, copies):
        self.place, self.grad, self.out, self.bufs = place, grad, out, bufs
        from_core, from_x, from_y, late_y, late_x, from_z = bufs
        core, x, y = place.core, place.x, place.y
        self.order = [to[0] for to in place.lines] + [place.z]
        rows = grad.shape[3]
        self.low, self.high = pl.ds(0, rows // 2), pl.ds(rows // 2, rows // 2)
        self.first, self.second, self.third, self.fourth = [], [], [], []
        for k, at in enumerate(self.order):
            self.first.append(
                copies.plan(grad.at[at, :, 1 - core], from_core.at[k], place.to_core)
            )
            step = []
            for j in range(2):
                step.append(
                    copies.plan(
                        grad.at[at, 2 * j + 1 - x, core, self.low], from_x.at[k, j], place.to_x
                    )
                )
                step.append(
                    copies.plan(
                        grad.at[at, 2 * (1 - y) + j, core, self.high], from_y.at[k, j], place.to_y
                    )
                )
            self.second.append(step)
            self.third.append(
                [
                    copies.plan(grad.at[at, place.chip_y, core, self.low], late_y.at[k], place.to_y),
                    copies.plan(
                        grad.at[at, place.chip_x, core, self.high], late_x.at[k], place.to_x
                    ),
                ]
            )
            if k < 3:
                self.fourth.append(
                    copies.plan(grad.at[at, place.chip, core], from_z.at[k], place.lines[k])
                )

    def start(self, k):
        go([self.first[k]])

    def exchange(self, k):
        arrive([self.first[k]])
        at, core = self.order[k], self.place.core
        add_blocks(4, lambda i: (self.grad.at[at, i, core], self.bufs[0].at[k, i]))
        go(self.second[k])

    def spread(self, k):
        arrive(self.second[k])
        at, core, x, y = self.order[k], self.place.core, self.place.x, self.place.y
        add_blocks(
            2, lambda j: (self.grad.at[at, 2 * j + x, core, self.low], self.bufs[1].at[k, j])
        )
        add_blocks(
            2, lambda j: (self.grad.at[at, 2 * y + j, core, self.high], self.bufs[2].at[k, j])
        )
        go(self.third[k])

    def send(self, k):
        arrive(self.third[k])
        at, core, chip = self.order[k], self.place.core, self.place.chip
        add_into(self.grad.at[at, chip, core, self.low], self.bufs[3].at[k])
        add_into(self.grad.at[at, chip, core, self.high], self.bufs[4].at[k])
        go(self.fourth[k : k + 1])

    def finish(self):
        arrive(self.fourth)
        place = self.place
        total = self.grad[place.z, place.chip, place.core].astype(f32)
        for k in range(3):
            total = total + self.bufs[5][k].astype(f32)
        self.out[...] = total


def reduce_lines_scratch(rows, columns):
    half = rows // 2
    return [
        pltpu.VMEM((4, 4, rows, columns), bf16),
        pltpu.VMEM((4, 2, half, columns), bf16),
        pltpu.VMEM((4, 2, half, columns), bf16),
        pltpu.VMEM((4, half, columns), bf16),
        pltpu.VMEM((4, half, columns), bf16),
        pltpu.VMEM((3, rows, columns), bf16),
    ]


def split_grad(item):
    return item.reshape(4, 4, 2, item.shape[0] // 32, item.shape[1])


def split_weight(item):
    return item.reshape(8, item.shape[0] // 8, item.shape[1])


def chunks_of(index, rows, columns, count):
    if rows >= 64:
        return [(index, rows // count * n, rows // count, 0, columns) for n in range(count)]
    return [(index, 0, rows, columns // count * n, columns // count) for n in range(count)]


def semaphores(remote, local):
    return [pltpu.SemaphoreType.DMA((n,)) for n in (remote, remote, local)]


def remote_call(kernel, name, collective, **options):
    return pl.pallas_call(
        kernel,
        name=name,
        compiler_params=pltpu.CompilerParams(
            collective_id=collective, has_side_effects=True, vmem_limit_bytes=vmem_bytes
        ),
        **options,
    )


def columns_of(rank, features):
    return pl.ds(pl.multiple_of(rank * features, 128), features)


def forward_fused_kernel(heads, width, count, vector_count, chunks, slopes, tokens, upstream, *refs):
    vectors, refs = refs[:vector_count], refs[vector_count:]
    weights, contract, refs = refs[:count], refs[count], refs[count + 1 :]
    tokens_out, vectors_out, joined_out, qkv_out, attended, out_t, lse, upstream_out = refs[:8]
    contract_out = refs[8]
    wholes, refs = refs[9 : 8 + count], refs[8 + count :]
    held, small, values_of, joined, normed, outgoing, qkv, result, upstream_own = refs[:9]
    attention = Forward(heads, width, slopes, qkv, result, out_t, lse, *refs[9:12])
    kept, refs = refs[12 : 11 + count], refs[11 + count :]
    head_send, head_recv = refs[:2]
    copies = Copies(*refs[5:])
    place = Place()
    z, s, lines, plane = place.z, place.s, place.lines, place.plane
    gather = Gather(place, weights, [joined, *wholes], [None, *kept], chunks, copies)
    first = [t for t, chunk in enumerate(chunks) if chunk[0] == 0]
    later = [t for t, chunk in enumerate(chunks) if chunk[0] > 0]
    features = heads * width
    back = HandBack(place, result, attended, features, *refs[2:5])
    own_seqs, parts, piece, wide = held.shape

    load = copies.inside(tokens.at[z], held.at[:, z])
    load_upstream = copies.inside(upstream.at[z], upstream_own)
    seqs = [copies.plan(tokens.at[to[0]], held.at[:, z], to) for to in lines]
    vector_copies = [copies.plan(small.at[z], small.at[z], to) for to in lines]
    upstreams = [copies.plan(upstream.at[to[0]], upstream_out.at[:, z], to) for to in lines]
    keep_upstream = copies.inside(upstream_own, upstream_out.at[:, z])
    keeping = [
        copies.inside(held, tokens_out),
        copies.inside(small, vectors_out),
        copies.inside(joined, joined_out),
    ]
    keep_qkv = copies.inside(qkv, qkv_out)
    contracts = [copies.plan(contract.at[s], contract_out.at[z], to) for to in lines]

    def to_head(d):
        return pltpu.make_async_remote_copy(
            src_ref=outgoing.at[d],
            dst_ref=qkv.at[:, :, s],
            send_sem=head_send.at[d],
            recv_sem=head_recv.at[d],
            device_id=(z, lax.rem(s + 1 + d, 8)),
            device_id_type=MESH,
        )

    go(gather.loads + [load, load_upstream])
    small[z] = jnp.zeros(small.shape[1:], bf16)
    for n, item in enumerate(vectors):
        small[z, n, : item.shape[0], :] = item[...]
    greet(lines + plane)
    for t in first:
        gather.start(t)
    go(seqs + vector_copies)
    for t in later:
        gather.start(t)
    go(contracts + upstreams)
    gather.keep()
    load.wait()
    for t in range(len(first) + 2):
        if t < len(first):
            gather.exchange(t)
        if 0 <= t - 1 < len(first):
            gather.spread(t - 1)
        if 0 <= t - 2:
            gather.share(t - 2)
    load_upstream.wait()
    keep_upstream.start()
    arrive(seqs + vector_copies)
    values_of[...] = small[...].astype(f32)

    def row_of(n):
        found = [values_of[k, n, r : r + 1, :] for k in range(4) for r in range(wide // 512)]
        return jnp.concatenate(found, axis=1)

    gain, shift = row_of(0), row_of(1)

    def norm(i, _):
        values = held[i // parts, i % parts].astype(f32)
        rows = pl.ds(pl.multiple_of(i * piece, piece), piece)
        normed[rows, :] = normalize(values, gain, shift).astype(bf16)
        return 0

    lax.fori_loop(0, own_seqs * parts, norm, 0)
    for t in first:
        gather.complete(t)
    go(keeping)

    def project(d, _):
        rank = lax.rem(s + 1 + d, 8)
        per = 8 // 4
        query_bias = values_of[rank // per, 2, pl.ds(rank % per, 1), :]
        value_bias = values_of[rank // per, 3, pl.ds(rank % per, 1), :]
        low = lax.broadcasted_iota(jnp.int32, query_bias.shape, 1) < width
        bias = jnp.concatenate(
            [
                jnp.where(low, query_bias, 0.0),
                jnp.where(low, value_bias, query_bias),
                jnp.where(low, 0.0, value_bias),
            ],
            axis=1,
        )
        weight = joined[:, :, :, columns_of(rank, 3 * features)].reshape(wide, 3 * features)
        made = (matmul(normed[...], weight) + bias).astype(bf16)
        outgoing[d] = made.reshape(outgoing.shape[1:])
        pl.when(d < 7)(lambda: to_head(d).start())
        return 0

    lax.fori_loop(0, 8, project, 0)
    own_copy = copies.inside(outgoing.at[7], qkv.at[:, :, s])
    own_copy.start()
    base = later[0]
    gather.exchange(base)
    gather.exchange(base + 1)
    own_copy.wait()
    gather.spread(base)
    gather.exchange(base + 2)
    gather.spread(base + 1)
    for d in range(7):
        to_head(d).wait_recv()
    keep_qkv.start()
    gather.share(base)
    attention.run(
        {
            1: [(gather.spread, base + 2)],
            3: [(gather.share, base + 1)],
            5: [(gather.share, base + 2)],
        },
        back.each,
    )
    for t in later:
        gather.complete(t)
    arrive(contracts + upstreams)
    back.finish()
    for d in range(7):
        to_head(d).wait_send()
    copies.finish()
    done(gather.own + [keep_upstream, keep_qkv] + keeping)


def forward_fused(tokens, upstream, vectors, weights, contract, slopes, heads, width):
    seqs, piece, features = tokens.shape
    parts = 4
    own = seqs // parts
    columns = heads * width
    length = parts * 8 * piece
    vectors = [item.reshape(-1, 128) for item in vectors]
    cut = [split_weight(item) for item in weights]
    contract = split_weight(contract)
    count, tall = len(cut), 8 * -(-max(item.shape[0] for item in vectors) // 8)
    chunks = []
    for t, pieces in enumerate((3, 1, 2)):
        chunks += chunks_of(t, *cut[t].shape[1:], pieces)
    seq_shape = (own, parts, piece, features)
    qkv_shape = (own, parts, 8, piece, 3 * columns)
    small = (parts, len(vectors), tall, 128)
    out = remote_call(
        functools.partial(forward_fused_kernel, heads, width, count, len(vectors), chunks),
        "forward_fused",
        1,
        out_shape=(
            jax.ShapeDtypeStruct(seq_shape, bf16),
            jax.ShapeDtypeStruct(small, bf16),
            jax.ShapeDtypeStruct((parts, *cut[0].shape), bf16),
            jax.ShapeDtypeStruct(qkv_shape, bf16),
            jax.ShapeDtypeStruct(seq_shape, bf16),
            *saved_shapes(own, length, heads, width),
            jax.ShapeDtypeStruct(seq_shape, bf16),
            jax.ShapeDtypeStruct((parts, *contract.shape[1:]), bf16),
            *[jax.ShapeDtypeStruct((parts, *item.shape), bf16) for item in cut[1:]],
        ),
        in_specs=[SMEM, HBM, HBM] + [VMEM] * len(vectors) + [HBM] * (count + 1),
        out_specs=(HBM,) * 5 + (VMEM, VMEM) + (HBM,) * (count + 1),
        scratch_shapes=[
            pltpu.VMEM(seq_shape, bf16),
            pltpu.VMEM(small, bf16),
            pltpu.VMEM(small, f32),
            pltpu.VMEM((parts, *cut[0].shape), bf16),
            pltpu.VMEM((own * parts * piece, features), bf16),
            pltpu.VMEM((8, own, parts, piece, 3 * columns), bf16),
            pltpu.VMEM(qkv_shape, bf16),
            pltpu.VMEM((own, parts, 8, piece, columns), bf16),
            pltpu.VMEM((own, piece, features), bf16),
            *forward_scratch(length, heads, width),
            *[pltpu.VMEM(item.shape, bf16) for item in cut[1:]],
            pltpu.SemaphoreType.DMA((7,)),
            pltpu.SemaphoreType.DMA((7,)),
            *hand_back_semaphores(own * parts),
            *semaphores(12 + len(chunks) * Gather.copies_each, 2 * count - 1 + 8),
        ],
    )(
        slopes,
        tokens.reshape(parts, own, piece, features),
        upstream.reshape(parts, own, piece, features),
        *vectors,
        *cut,
        contract,
    )
    wholes = [
        whole.reshape(4 * item.shape[0], item.shape[1])
        for whole, item in zip((out[2], *out[9:]), weights)
    ]
    found = [out[1][:, n, : item.shape[0]].reshape(-1) for n, item in enumerate(vectors)]
    return out[0], found, [*wholes, out[8]], out[3], out[4], (out[5], out[6]), out[7]


def feed_forward_kernel(
    chunks, expand, contract, contract_line, expand_bias, second, upstream, residual,
    layer_out, second_back, expand_grad, bias_grad, contract_grad,
    expand_in, contract_in, second_t, expanded, activated, grad, layer, staged, *refs,
):
    bufs, refs = refs[:6], refs[6:]
    loaded, stored, refs = refs[0], refs[1], refs[2:]
    copies = Copies(*refs)
    place = Place()
    z, lines = place.z, place.lines
    reduce = ReduceLines(place, grad, contract_grad, bufs, copies)
    gather = Gather(
        place, [contract], [contract_in], [None], chunks, copies, given=contract_line
    )
    rows, features = second.shape
    steps = 8
    wide = expand.shape[1] // steps
    own, parts, piece, _ = layer.shape

    def at(n):
        part = (z + 1 + n // 2) % 4
        return part, n % 2, pl.ds(pl.multiple_of((2 * part + n % 2) * wide, wide), wide)

    def load(n):
        _, _, where = at(n)
        return pltpu.make_async_copy(expand.at[:, where], expand_in.at[:, where], loaded.at[n])

    def contract_at(n):
        part, side, _ = at(n)
        return contract_in[part, pl.ds(4 * side, 4)].reshape(wide, features)

    def store(n):
        _, _, where = at(n)
        slot = n % 2
        return pltpu.make_async_copy(
            staged.at[slot], expand_grad.at[:, where], stored.at[slot]
        )

    returned = [copies.plan(layer.at[:, to[0]], layer_out.at[z], to) for to in lines]
    stay = copies.inside(layer.at[:, z], layer_out.at[z])
    for n in range(len(chunks)):
        gather.start(n)
    for n in range(steps):
        load(n).start()
    go(gather.loads)
    greet(place.near)
    for n in range(len(chunks)):
        gather.exchange(n)
    second_t[...] = second[...].T
    second_back[...] = residual[...]

    def forward(n, after):
        part, side, where = at(n)
        load(n).wait()
        values = matmul(second[...], expand_in[:, where]) + expand_bias[:, where]
        expanded[:, where] = values
        low = gelu_tanh(values).astype(bf16)
        activated[:, where] = low
        made = matmul(low.T, upstream[...]).astype(bf16)
        grad[part, pl.ds(2 * side, 2)] = made.reshape(2, 2, wide // 4, features)
        follow(n, after)
        return 0

    def shrink(n, after):
        _, _, where = at(n)
        second_back[...] += matmul(activated[:, where], contract_at(n))
        follow(n, after)
        return 0

    def backward(n, after):
        _, _, where = at(n)
        values = expanded[:, where]
        act_grad = matmul_rt(upstream[...], contract_at(n))
        bent = jnp.tanh(gelu_coef * (values + 0.044715 * values * values * values))
        slope = 0.5 * (1.0 + bent) + 0.5 * values * (1.0 - bent * bent) * (
            gelu_coef * (1.0 + 3.0 * 0.044715 * values * values)
        )
        diff = (act_grad * slope).astype(bf16)
        bias_grad[:, where] = jnp.sum(diff.astype(f32), axis=0, keepdims=True)
        pl.when(n >= 2)(lambda: store(n - 2).wait())
        staged[n % 2] = matmul(second_t[...], diff).astype(bf16)
        store(n).start()
        second_back[...] += matmul_rt(diff, expand_in[:, where])
        follow(n, after)
        return 0

    last = len(chunks) - 1
    forward_steps = {
        1: [(reduce.start, 0)] + [(gather.spread, n) for n in range(last)],
        2: [(gather.spread, last)],
        3: [(reduce.exchange, 0), (reduce.start, 1)],
        4: [(reduce.exchange, 1)],
        5: [(reduce.start, 2)] + [(gather.share, n) for n in range(last)],
        7: [(reduce.start, 3), (reduce.exchange, 2)],
    }
    shrink_steps = {
        1: [(reduce.spread, 0)],
        3: [(reduce.exchange, 3)],
        5: [(reduce.spread, 1), (reduce.send, 0)],
    }
    backward_steps = {
        0: [(reduce.spread, 2)],
        1: [(reduce.send, 1), (reduce.spread, 3)],
        3: [(reduce.send, 2)],
        5: [(reduce.send, 3)],
    }
    lax.fori_loop(0, steps, lambda n, _: forward(n, forward_steps), 0)
    gather.share(last)
    for n in range(len(chunks)):
        gather.complete(n)
    done(gather.loads)
    lax.fori_loop(0, steps, lambda n, _: shrink(n, shrink_steps), 0)
    layer[...] = second_back[...].astype(bf16).reshape(layer.shape)
    second_back[...] = jnp.zeros_like(second_back)
    go(returned + [stay])
    lax.fori_loop(0, steps, lambda n, _: backward(n, backward_steps), 0)
    reduce.finish()
    store(steps - 2).wait()
    store(steps - 1).wait()
    arrive(returned)
    copies.finish()
    done([stay])


def feed_forward(shape, expand, contract, line, expand_bias, second, upstream, residual):
    own, parts, piece = shape
    rows, features = second.shape
    hidden = expand.shape[1]
    wide = hidden // 8
    each = hidden // 32
    contract = split_weight(contract)
    chunks = chunks_of(0, *contract.shape[1:], 2)
    out = remote_call(
        functools.partial(feed_forward_kernel, chunks),
        "feed_forward",
        4,
        out_shape=(
            jax.ShapeDtypeStruct((parts, own, piece, features), bf16),
            jax.ShapeDtypeStruct((rows, features), f32),
            jax.ShapeDtypeStruct((features, hidden), bf16),
            jax.ShapeDtypeStruct((1, hidden), f32),
            jax.ShapeDtypeStruct((each, features), f32),
        ),
        in_specs=[HBM, HBM, HBM, VMEM, VMEM, VMEM, VMEM],
        out_specs=(HBM, VMEM, HBM, VMEM, VMEM),
        scratch_shapes=[
            pltpu.VMEM((features, hidden), bf16),
            pltpu.VMEM((4, *contract.shape), bf16),
            pltpu.VMEM((features, rows), bf16),
            pltpu.VMEM((rows, hidden), f32),
            pltpu.VMEM((rows, hidden), bf16),
            pltpu.VMEM((4, 4, 2, each, features), bf16),
            pltpu.VMEM((own, parts, piece, features), bf16),
            pltpu.VMEM((2, features, wide), bf16),
            *reduce_lines_scratch(each, features),
            pltpu.SemaphoreType.DMA((8,)),
            pltpu.SemaphoreType.DMA((2,)),
            *semaphores(
                ReduceLines.copies + 3 + len(chunks) * (Gather.copies_each - 3),
                2 + 3 * len(chunks),
            ),
        ],
    )(expand, contract, line, expand_bias, second, upstream, residual)
    return out[0].reshape(parts * own, piece, features), *out[1:]


def backward_fused_kernel(heads, width, count, chunks, *refs):
    slopes, diff_in, qkv_in, out_t_in, lse_in = refs[:5]
    grads, refs = refs[5 : 5 + count], refs[5 + count :]
    joined_out, outs, refs = refs[0], refs[1 : 1 + count], refs[1 + count :]
    diff, qkv, out_t, lse, joined = refs[:5]
    attention = Backward(heads, width, slopes, qkv, diff, out_t, lse, joined, *refs[5:12])
    bufs, refs = refs[12 : 12 + 7 * len(chunks)], refs[12 + 7 * len(chunks) :]
    copies = Copies(*refs[3:])
    place = Place()
    s, plane = place.s, place.plane
    features = heads * width
    along = ReduceAlong(place, grads[0], outs[0], bufs[:7], chunks[0], copies)
    reduce = Reduce(place, grads, outs, bufs[7:], chunks[1:], copies)
    back = HandBack(place, joined, joined_out, 3 * features, *refs[:3])

    own = [copies.inside(diff_in.at[:, :, :, columns_of(s, features)], diff.at[:, :, s])]
    own += [copies.inside(a, b) for a, b in ((qkv_in, qkv), (out_t_in, out_t), (lse_in, lse))]
    arriving = [
        copies.plan(diff_in.at[:, :, :, columns_of(to[1], features)], diff.at[:, :, s], to)
        for to in plane
    ]
    go(own + reduce.loads + [along.load])
    greet(place.lines + plane)
    go(arriving + [along.first])
    reduce.start()
    along.exchange()
    for t in range(2):
        reduce.exchange(t)
    done(own)
    arrive(arriving)
    attention.run(
        {
            1: [(reduce.spread, 0)],
            3: [(reduce.spread, 1)],
            4: [(reduce.send, 0), (along.spread,)],
            5: [(reduce.send, 1)],
            6: [(along.send,)],
        },
        back.each,
    )
    for t in range(2):
        reduce.finish(t)
    along.finish()
    back.finish()
    copies.finish()


def backward_fused(attended_diff, qkv, saved, grads, slopes, heads, width):
    own, parts, piece, columns = attended_diff.shape
    features = heads * width
    length = parts * 8 * piece
    cut = [split_grad(item) for item in grads]
    count = len(cut)
    chunks = []
    for t, pieces in enumerate((2, 1)):
        chunks += chunks_of(t, *cut[t].shape[3:], pieces)
    out = remote_call(
        functools.partial(backward_fused_kernel, heads, width, count, chunks),
        "backward_fused",
        2,
        out_shape=(
            jax.ShapeDtypeStruct((own, parts, piece, 24 * features), bf16),
            *[jax.ShapeDtypeStruct(item.shape[3:], f32) for item in cut],
        ),
        in_specs=[SMEM] + [HBM] * (4 + count),
        out_specs=(HBM,) + (VMEM,) * count,
        scratch_shapes=[
            pltpu.VMEM((own, parts, 8, piece, features), bf16),
            pltpu.VMEM(qkv.shape, bf16),
            *[pltpu.VMEM(item.shape, f32) for item in saved],
            pltpu.VMEM(qkv.shape, bf16),
            *backward_scratch(length, heads, width),
            *reduce_along_scratch(chunks[0]),
            *reduce_scratch(chunks[1:]),
            *hand_back_semaphores(own * parts),
            *semaphores(7 + len(chunks) * Reduce.copies_each, len(chunks) + 4),
        ],
    )(slopes, attended_diff, qkv, *saved, *cut)
    return out[0], out[1:]


def end_kernel(chunks, input_grad, vector, grad, input_out, vector_out, out, *refs):
    input_own, ranks, plane_sum, others = refs[:4]
    bufs, refs = refs[4 : 4 + 7 * len(chunks)], refs[4 + 7 * len(chunks) :]
    copies = Copies(*refs)
    place = Place()
    z, s, lines, plane = place.z, place.s, place.lines, place.plane
    count = len(chunks)
    reduce = Reduce(place, [grad], [out], bufs, chunks, copies)
    load = copies.inside(input_grad.at[:, z], input_own)
    load_vector = copies.inside(vector.at[:, s], ranks.at[0])
    keep = copies.inside(input_own, input_out.at[z])
    waiting = [copies.plan(input_grad.at[:, to[0]], input_out.at[z], to) for to in lines]
    vectors = [
        copies.plan(vector.at[:, to[1]], ranks.at[d + 1], to) for d, to in enumerate(plane)
    ]
    sums = [copies.plan(plane_sum.at[to[0]], others.at[k], to) for k, to in enumerate(lines)]
    go(reduce.loads + [load, load_vector])
    greet(lines + plane)
    reduce.start()
    go(waiting + vectors)
    load.wait()
    go([keep])
    for t in range(count + 2):
        if t < count:
            reduce.exchange(t)
        if t == 0:
            load_vector.wait()
            arrive(vectors)
            total = ranks[0]
            for d in range(1, 8):
                total = total + ranks[d]
            plane_sum[...] = total
            go(sums)
        if 0 <= t - 1 < count:
            reduce.spread(t - 1)
        if 0 <= t - 2:
            reduce.send(t - 2)
    arrive(sums)
    total = plane_sum[z]
    for k in range(3):
        total = total + others[k]
    vector_out[...] = total
    for t in range(count):
        reduce.finish(t)
    arrive(waiting)
    copies.finish()
    keep.wait()


def end(input_grad, vector, grad):
    own, parts, piece, features = input_grad.shape
    lanes = vector.shape[-1]
    padded = -(-lanes // 1024) * 1024
    vector = jnp.pad(vector, ((0, 0), (0, padded - lanes))).reshape(4, 8, padded // 128, 128)
    cut = split_grad(grad)
    chunks = chunks_of(0, *cut.shape[3:], 3)
    out = remote_call(
        functools.partial(end_kernel, chunks),
        "end",
        3,
        out_shape=(
            jax.ShapeDtypeStruct((parts, own, piece, features), bf16),
            jax.ShapeDtypeStruct(vector.shape[2:], f32),
            jax.ShapeDtypeStruct(cut.shape[3:], f32),
        ),
        in_specs=[HBM] * 3,
        out_specs=(HBM, VMEM, VMEM),
        scratch_shapes=[
            pltpu.VMEM((own, piece, features), bf16),
            pltpu.VMEM((8, 4, padded // 128, 128), f32),
            pltpu.VMEM((4, padded // 128, 128), f32),
            pltpu.VMEM((3, padded // 128, 128), f32),
            *reduce_scratch(chunks),
            *semaphores(3 + 7 + 3 + len(chunks) * Reduce.copies_each, 3 + len(chunks)),
        ],
    )(input_grad, vector, cut)
    return out[0].reshape(parts * own, piece, features), out[1].reshape(-1)[:lanes], out[2]


def per_device(
    layer_input,
    first_gain,
    first_shift,
    joined_weight,
    query_bias,
    value_bias,
    output_weight,
    output_bias,
    second_gain,
    second_shift,
    expand_weight,
    expand_bias,
    contract_weight,
    contract_bias,
    alibi_slopes,
    upstream,
):
    seqs, piece, features = layer_input.shape
    fs_count = lax.axis_size("fs")
    sp_count = lax.axis_size("sp")
    head_count = alibi_slopes.shape[0]
    width = features // head_count
    heads = head_count // sp_count
    rows = seqs * piece
    own = seqs // fs_count
    shape = (own, fs_count, piece)
    slopes = lax.dynamic_slice_in_dim(alibi_slopes, lax.axis_index("sp") * heads, heads)

    vectors = (
        first_gain, first_shift, query_bias, value_bias, output_bias,
        second_gain, second_shift, contract_bias, expand_bias,
    )
    fast = (fs_count, sp_count) == (4, 8) and (own, heads, width) == (2, 2, 64)
    weights = (joined_weight, output_weight, expand_weight)
    gather = lambda item: lax.all_gather(item, "fs", axis=0, tiled=True)
    if fast:
        tokens, whole, weights, qkv, attended, saved, upstream_low = forward_fused(
            layer_input, upstream, vectors, weights, contract_weight, slopes, heads, width
        )
    else:
        tokens, upstream_low = to_own_seqs(layer_input), to_own_seqs(upstream)
        whole = [gather(item) for item in vectors]
        weights = [gather(item) for item in (*weights, contract_weight)]
    joined_full, out_full, expand_full, contract_full = weights
    tokens = tokens.reshape(rows, features).astype(f32)
    gain_one, shift_one, qbias, vbias, obias, gain_two, shift_two, cbias, ebias = [
        item.astype(f32) for item in whole
    ]

    normed_f, norm_back_one = jax.vjp(normalize, tokens, gain_one, shift_one)
    normed = normed_f.astype(bf16)
    if not fast:
        joined_bias = joined_bias_of(qbias, vbias, head_count)
        joined_all = (matmul(normed, joined_full) + joined_bias).astype(bf16)
        qkv = to_heads(joined_all.reshape(*shape, 3 * features))
        attended, *saved = attention_forward(qkv, slopes, heads, width)
        attended = from_heads(attended)
    attended = attended.reshape(rows, features)
    upstream_low = upstream_low.reshape(rows, features)

    residual = tokens + (matmul(attended, out_full) + obias)
    second_f, norm_back_two = jax.vjp(normalize, residual, gain_two, shift_two)
    second = second_f.astype(bf16)
    upstream_f = upstream_low.astype(f32)
    contract_bias_grad = jnp.sum(upstream_f, axis=0)
    if fast:
        layer_output, second_back, expand_grad, expand_bias_grad, contract_grad = feed_forward(
            shape, expand_full, contract_weight, contract_full, ebias.reshape(1, -1), second,
            upstream_low, residual + cbias,
        )
        expand_bias_grad = expand_bias_grad.reshape(-1)
    else:
        expanded = matmul(second, expand_full) + ebias
        activated_f, gelu_back = jax.vjp(gelu_tanh, expanded)
        activated = activated_f.astype(bf16)
        result = residual + (matmul(activated, contract_full) + cbias)
        layer_output = result.astype(bf16).reshape(*shape, features)

        contract_grad = matmul_lt(activated, upstream_low)
        act_grad = matmul_rt(upstream_low, contract_full)
        expand_diff = gelu_back(act_grad)[0].astype(bf16)
        expand_grad = matmul_lt(second, expand_diff)
        expand_bias_grad = jnp.sum(expand_diff.astype(f32), axis=0)
        second_back = matmul_rt(expand_diff, expand_full)
    resid_part, second_gain_grad, second_shift_grad = norm_back_two(second_back)
    residual_grad = upstream_f + resid_part

    branch_diff = residual_grad.astype(bf16)
    output_weight_grad = matmul_lt(attended, branch_diff)
    output_bias_grad = jnp.sum(branch_diff.astype(f32), axis=0)
    attended_diff = matmul_rt(branch_diff, out_full).astype(bf16)
    attended_diff = attended_diff.reshape(*shape, features)
    grads = (expand_grad, output_weight_grad)
    scatter = functools.partial(
        lax.psum_scatter, axis_name=("fs", "sp"), scatter_dimension=0, tiled=True
    )
    if fast:
        joined_diff, grads = backward_fused(
            attended_diff, qkv, saved, [item.astype(bf16) for item in grads], slopes, heads, width
        )
    else:
        joined_diff = attention_backward(
            qkv, to_heads(attended_diff), *saved, slopes, heads, width
        )
        joined_diff, layer_output = from_heads(joined_diff), from_own_seqs(layer_output)
        grads = [scatter(item) for item in grads]
        contract_grad = scatter(contract_grad)
    expand_grad, output_weight_grad = grads
    joined_diff = joined_diff.reshape(rows, 3 * features)

    joined_grad = matmul_lt(normed, joined_diff)
    column_sums = jnp.sum(joined_diff.astype(f32), axis=0).reshape(head_count, 3, width)
    query_bias_grad = column_sums[:, 0].reshape(features)
    value_bias_grad = column_sums[:, 2].reshape(features)
    normed_back = matmul_rt(joined_diff, joined_full)
    input_part, first_gain_grad, first_shift_grad = norm_back_one(normed_back)
    input_grad = (residual_grad + input_part).astype(bf16).reshape(*shape, features)

    vector_grads = (
        first_gain_grad, first_shift_grad, query_bias_grad, value_bias_grad, output_bias_grad,
        second_gain_grad, second_shift_grad, contract_bias_grad, expand_bias_grad,
    )
    devices = fs_count * sp_count
    packed = jnp.concatenate([item.reshape(devices, -1) for item in vector_grads], axis=1)
    if fast:
        input_grad, packed, joined_grad = end(input_grad, packed, joined_grad.astype(bf16))
    else:
        input_grad, joined_grad = from_own_seqs(input_grad), scatter(joined_grad)
        packed = scatter(packed.reshape(-1))
    own_grads, at = [], 0
    for item in vector_grads:
        size = item.shape[0] // devices
        own_grads.append(packed[at : at + size])
        at += size
    g1, s1, qb, vb, ob, g2, s2, cb, eb = own_grads
    return (
        layer_output,
        input_grad,
        g1,
        s1,
        joined_grad,
        qb,
        vb,
        output_weight_grad,
        ob,
        g2,
        s2,
        expand_grad,
        eb,
        contract_grad,
        cb,
    )


def solution(mesh):
    tokens = P(None, ("fs", "sp"), None)
    both, both_rows = P(("fs", "sp")), P(("fs", "sp"), None)
    one, one_rows = P("fs"), P("fs", None)
    return jax.shard_map(
        per_device,
        mesh=mesh,
        in_specs=(
            tokens, one, one, one_rows, one, one, one_rows, one, one, one, one_rows, one,
            one_rows, one, P(), tokens,
        ),
        out_specs=(
            tokens, tokens, both, both, both_rows, both, both, both_rows, both, both, both,
            both_rows, both, both_rows, both,
        ),
        check_vma=False,
    )
```

```python
import functools
import math

import jax
import jax.numpy as jnp
from jax import lax
from jax.experimental import pallas as pl
from jax.experimental.pallas import tpu as pltpu
from jax.sharding import PartitionSpec as P

norm_eps = 1e-05
gelu_coef = 0.7978845608028654
masked_value = -1e30
f32 = jnp.float32
bf16 = jnp.bfloat16
MESH = pl.DeviceIdType.MESH
HBM = pl.BlockSpec(memory_space=pl.ANY)
VMEM = pl.BlockSpec(memory_space=pltpu.VMEM)
SMEM = pl.BlockSpec(memory_space=pltpu.SMEM)
vmem_bytes = 60 * 1024 * 1024


def normalize(values, norm_gain, norm_shift):
    center = values - jnp.mean(values, axis=-1, keepdims=True)
    variance = jnp.mean(center * center, axis=-1, keepdims=True)
    return center * lax.rsqrt(variance + norm_eps) * norm_gain + norm_shift


def gelu_tanh(values):
    return (
        0.5 * values * (1.0 + jnp.tanh(gelu_coef * (values + 0.044715 * values * values * values)))
    )


def matmul(left_side, right_side):
    return jnp.dot(left_side, right_side, preferred_element_type=f32)


def matmul_lt(left_side, right_side):
    return lax.dot_general(
        left_side, right_side, (((0,), (0,)), ((), ())), preferred_element_type=f32
    )


def matmul_rt(left_side, right_side):
    return lax.dot_general(
        left_side, right_side, (((1,), (1,)), ((), ())), preferred_element_type=f32
    )


def joined_bias_of(query_bias, value_bias, head_count):
    query_part = query_bias.astype(f32).reshape(head_count, -1)
    value_part = value_bias.astype(f32).reshape(head_count, -1)
    return jnp.stack([query_part, jnp.zeros_like(query_part), value_part], axis=1).reshape(-1)


def split_three(values):
    high = values.astype(bf16).astype(f32)
    rest = values - high
    middle = rest.astype(bf16).astype(f32)
    return high, middle, rest - middle


def key_columns(key_rows, slope, start):
    rows, width = key_rows.shape
    position = (start + lax.broadcasted_iota(jnp.int32, (rows, width), 0)).astype(f32)
    lane = lax.broadcasted_iota(jnp.int32, (rows, width), 1)
    high, middle, low = split_three(slope * position)
    extra = jnp.where(lane == 0, high, jnp.where(lane == 1, middle, jnp.where(lane == 2, low, 0.0)))
    return jnp.concatenate([key_rows.astype(f32), extra], axis=1).astype(bf16)


def query_columns(queries, scale):
    rows, width = queries.shape
    lane = lax.broadcasted_iota(jnp.int32, (rows, width), 1)
    ones = jnp.where(lane < 3, 1.0, 0.0)
    return jnp.concatenate([queries.astype(f32) * scale, ones], axis=1).astype(bf16)


def follow(n, after):
    for at, steps in after.items():

        def act(steps=steps):
            for step, *given in steps:
                step(*given)

        pl.when(n == at)(act)


class Forward:
    def __init__(self, heads, width, slopes, qkv, out, out_t, lse, keys, queries, values_t):
        self.heads, self.width, self.slopes, self.qkv, self.out = heads, width, slopes, qkv, out
        self.out_t, self.lse = out_t, lse
        self.keys, self.queries, self.values_t = keys, queries, values_t
        self.blocks = qkv.shape[1]
        self.block = qkv.shape[2] * qkv.shape[3]

    def rows(self, i):
        return pl.ds(pl.multiple_of(i * self.block, self.block), self.block)

    def prepare(self, b):
        width, block, qkv = self.width, self.block, self.qkv
        scale = 1.0 / math.sqrt(width)

        def body(i, _):
            rows = self.rows(i)
            for h in range(self.heads):
                base = h * 3 * width
                query, key, value = [
                    qkv[b, i, :, :, base + n * width : base + (n + 1) * width].reshape(block, width)
                    for n in range(3)
                ]
                self.keys[h, rows, :] = key_columns(key, self.slopes[h], i * block)
                self.queries[h, rows, :] = query_columns(query, scale)
                self.values_t[h, :, rows] = value.astype(f32).T.astype(bf16)
            return 0

        lax.fori_loop(0, self.blocks, body, 0)

    def one(self, b, i):
        heads, width, block = self.heads, self.width, self.block
        rows = self.rows(i)
        query = [self.queries[h, rows, :] for h in range(heads)]

        def step(j, state, diagonal):
            columns = self.rows(j)
            result = []
            for h in range(heads):
                top, total, acc = state[h]
                scores = matmul_rt(self.keys[h, columns, :], query[h])
                if diagonal:
                    key_at = lax.broadcasted_iota(jnp.int32, (block, block), 0)
                    query_at = lax.broadcasted_iota(jnp.int32, (block, block), 1)
                    scores = jnp.where(key_at <= query_at, scores, masked_value)
                newest = jnp.maximum(top, jnp.max(scores, axis=0, keepdims=True))
                shrink = jnp.exp(top - newest)
                probs = jnp.exp(scores - newest)
                total = total * shrink + jnp.sum(probs, axis=0, keepdims=True)
                acc = acc * shrink + matmul(self.values_t[h, :, columns], probs.astype(bf16))
                result.append((newest, total, acc))
            return tuple(result)

        state = tuple(
            (
                jnp.full((1, block), masked_value, f32),
                jnp.zeros((1, block), f32),
                jnp.zeros((width, block), f32),
            )
            for h in range(heads)
        )
        state = lax.fori_loop(0, i, lambda j, s: step(j, s, False), state)
        state = step(i, state, True)
        finished = []
        for h in range(heads):
            top, total, acc = state[h]
            result = acc / total
            self.out_t[b, h, :, rows] = result
            self.lse[b, h, :, rows] = top + jnp.log(total)
            finished.append(result)
        joined = finished[0] if heads == 1 else jnp.concatenate(finished, axis=0)
        self.out[b, i] = joined.T.astype(bf16).reshape(self.out.shape[2:])

    def run(self, after, each=None):
        blocks = self.blocks

        def body(n, _):
            b, i = n // blocks, n % blocks
            pl.when(i == 0)(lambda: self.prepare(b))
            self.one(b, i)
            if each is not None:
                each(b, i)
            follow(n, after)
            return 0

        lax.fori_loop(0, self.qkv.shape[0] * blocks, body, 0)


def forward_kernel(heads, width, *refs):
    Forward(heads, width, *refs).run({})


def saved_shapes(seqs, length, heads, width):
    return (
        jax.ShapeDtypeStruct((seqs, heads, width, length), f32),
        jax.ShapeDtypeStruct((seqs, heads, 1, length), f32),
    )


def forward_scratch(length, heads, width):
    return [
        pltpu.VMEM((heads, length, 2 * width), bf16),
        pltpu.VMEM((heads, length, 2 * width), bf16),
        pltpu.VMEM((heads, width, length), bf16),
    ]


def attention_forward(qkv, slopes, heads, width):
    seqs, blocks, ranks, piece, _ = qkv.shape
    length = blocks * ranks * piece
    return pl.pallas_call(
        functools.partial(forward_kernel, heads, width),
        name="attention_forward",
        out_shape=(
            jax.ShapeDtypeStruct((seqs, blocks, ranks, piece, heads * width), bf16),
            *saved_shapes(seqs, length, heads, width),
        ),
        in_specs=[SMEM, VMEM],
        out_specs=(VMEM, VMEM, VMEM),
        scratch_shapes=forward_scratch(length, heads, width),
        compiler_params=pltpu.CompilerParams(vmem_limit_bytes=vmem_bytes),
    )(slopes, qkv)


class Backward:
    def __init__(
        self, heads, width, slopes, qkv, diff, out_t, lse, joined,
        keys, queries, keys_t, values, diffs, delta, query_acc,
    ):
        self.heads, self.width, self.slopes, self.qkv, self.diff = heads, width, slopes, qkv, diff
        self.out_t, self.lse, self.joined = out_t, lse, joined
        self.keys, self.queries, self.keys_t, self.values = keys, queries, keys_t, values
        self.diffs, self.delta, self.query_acc = diffs, delta, query_acc
        self.blocks = qkv.shape[1]
        self.block = qkv.shape[2] * qkv.shape[3]

    def rows(self, i):
        return pl.ds(pl.multiple_of(i * self.block, self.block), self.block)

    def prepare(self, b):
        width, block, qkv = self.width, self.block, self.qkv
        scale = 1.0 / math.sqrt(width)

        def body(i, _):
            rows = self.rows(i)
            for h in range(self.heads):
                base = h * 3 * width
                query, key, value = [
                    qkv[b, i, :, :, base + n * width : base + (n + 1) * width].reshape(block, width)
                    for n in range(3)
                ]
                self.keys[h, rows, :] = key_columns(key, self.slopes[h], i * block)
                self.keys_t[h, :, rows] = key.astype(f32).T.astype(bf16)
                self.queries[h, rows, :] = query_columns(query, scale)
                self.values[h, rows, :] = value
                part = self.diff[b, i, :, :, h * width : (h + 1) * width].reshape(block, width)
                self.diffs[h, rows, :] = part
                self.delta[h, :, rows] = jnp.sum(
                    part.astype(f32).T * self.out_t[b, h, :, rows], axis=0, keepdims=True
                )
                self.query_acc[h, :, rows] = jnp.zeros((width, block), f32)
            return 0

        lax.fori_loop(0, self.blocks, body, 0)

    def one(self, b, j):
        heads, width, block = self.heads, self.width, self.block
        tail = self.joined.shape[2:4] + (width,)
        columns = self.rows(j)

        def step(i, state, diagonal):
            rows = self.rows(i)
            result = []
            for h in range(heads):
                key_acc, value_acc = state[h]
                query = self.queries[h, rows, :]
                part = self.diffs[h, rows, :]
                scores = matmul_rt(self.keys[h, columns, :], query)
                probs = jnp.exp(scores - self.lse[b, h, :, rows])
                if diagonal:
                    key_at = lax.broadcasted_iota(jnp.int32, (block, block), 0)
                    query_at = lax.broadcasted_iota(jnp.int32, (block, block), 1)
                    probs = jnp.where(key_at <= query_at, probs, 0.0)
                prob_diff = matmul_rt(self.values[h, columns, :], part)
                score_diff = (probs * (prob_diff - self.delta[h, :, rows])).astype(bf16)
                value_acc = value_acc + matmul(probs.astype(bf16), part)
                key_acc = key_acc + matmul(score_diff, query)
                self.query_acc[h, :, rows] += matmul(self.keys_t[h, :, columns], score_diff)
                result.append((key_acc, value_acc))
            return tuple(result)

        state = tuple(
            (jnp.zeros((block, 2 * width), f32), jnp.zeros((block, width), f32))
            for h in range(heads)
        )
        state = step(j, state, True)
        state = lax.fori_loop(j + 1, self.blocks, lambda i, s: step(i, s, False), state)
        for h in range(heads):
            base = (h * 3 + 1) * width
            key_acc, value_acc = state[h]
            self.joined[b, j, :, :, base : base + width] = (
                key_acc[:, :width].astype(bf16).reshape(tail)
            )
            self.joined[b, j, :, :, base + width : base + 2 * width] = value_acc.astype(
                bf16
            ).reshape(tail)

    def run(self, after, each=None):
        blocks = self.blocks

        def body(n, _):
            b, j = n // blocks, n % blocks
            pl.when(j == 0)(lambda: self.prepare(b))
            self.one(b, j)
            self.finish(b, j)
            if each is not None:
                each(b, j)
            follow(n, after)
            return 0

        lax.fori_loop(0, self.qkv.shape[0] * blocks, body, 0)

    def finish(self, b, j):
        width = self.width
        scale = 1.0 / math.sqrt(width)
        for h in range(self.heads):
            base = h * 3 * width
            result = (self.query_acc[h, :, self.rows(j)] * scale).T.astype(bf16)
            self.joined[b, j, :, :, base : base + width] = result.reshape(
                self.joined.shape[2:4] + (width,)
            )


def backward_kernel(heads, width, *refs):
    Backward(heads, width, *refs).run({})


def backward_scratch(length, heads, width):
    return [
        pltpu.VMEM((heads, length, 2 * width), bf16),
        pltpu.VMEM((heads, length, 2 * width), bf16),
        pltpu.VMEM((heads, width, length), bf16),
        pltpu.VMEM((heads, length, width), bf16),
        pltpu.VMEM((heads, length, width), bf16),
        pltpu.VMEM((heads, 1, length), f32),
        pltpu.VMEM((heads, width, length), f32),
    ]


def attention_backward(qkv, diff, out_t, lse, slopes, heads, width):
    length = qkv.shape[1] * qkv.shape[2] * qkv.shape[3]
    return pl.pallas_call(
        functools.partial(backward_kernel, heads, width),
        name="attention_backward",
        out_shape=jax.ShapeDtypeStruct(qkv.shape, bf16),
        in_specs=[SMEM, VMEM, VMEM, VMEM, VMEM],
        out_specs=VMEM,
        scratch_shapes=backward_scratch(length, heads, width),
        compiler_params=pltpu.CompilerParams(vmem_limit_bytes=vmem_bytes),
    )(slopes, qkv, diff, out_t, lse)


def to_own_seqs(values):
    seqs, piece, features = values.shape
    parts = lax.axis_size("fs")
    values = values.reshape(parts, seqs // parts, piece, features)
    return lax.all_to_all(values, "fs", split_axis=0, concat_axis=0).transpose(1, 0, 2, 3)


def from_own_seqs(values):
    own, parts, piece, features = values.shape
    values = lax.all_to_all(values.transpose(1, 0, 2, 3), "fs", split_axis=0, concat_axis=0)
    return values.reshape(parts * own, piece, features)


def to_heads(values):
    own, parts, piece, features = values.shape
    ranks = lax.axis_size("sp")
    values = values.reshape(own, parts, piece, ranks, features // ranks)
    return lax.all_to_all(values, "sp", split_axis=3, concat_axis=2)


def from_heads(values):
    own, parts, ranks, piece, features = values.shape
    values = lax.all_to_all(values, "sp", split_axis=2, concat_axis=3)
    return values.reshape(own, parts, piece, ranks * features)


class Copies:
    def __init__(self, send, recv, local):
        self.send, self.recv, self.local = send, recv, local
        self.used, self.used_local, self.made = 0, 0, []

    def plan(self, source, target, device):
        copy = pltpu.make_async_remote_copy(
            src_ref=source,
            dst_ref=target,
            send_sem=self.send.at[self.used],
            recv_sem=self.recv.at[self.used],
            device_id=device,
            device_id_type=MESH,
        )
        self.used += 1
        self.made.append(copy)
        return copy

    def inside(self, source, target):
        copy = pltpu.make_async_copy(source, target, self.local.at[self.used_local])
        self.used_local += 1
        return copy

    def finish(self):
        assert (self.used, self.used_local) == (self.send.shape[0], self.local.shape[0])
        for copy in self.made:
            copy.wait_send()


def go(copies):
    for copy in copies:
        copy.start()


def arrive(copies):
    for copy in copies:
        copy.wait_recv()


def done(copies):
    for copy in copies:
        copy.wait()


def greet(devices):
    barrier = pltpu.get_barrier_semaphore()
    for device in devices:
        pl.semaphore_signal(barrier, inc=1, device_id=device, device_id_type=MESH)
    pl.semaphore_wait(barrier, len(devices))


class Place:
    def __init__(self):
        z, s = lax.axis_index("fs"), lax.axis_index("sp")
        self.z, self.s = z, s
        self.core, self.chip = s % 2, s // 2
        self.x, self.y = self.chip % 2, self.chip // 2
        self.along_x = s + 2 - 4 * self.x
        self.along_y = s + 4 - 8 * self.y
        self.partner = s + 1 - 2 * self.core
        self.diagonal = self.along_x + self.along_y - s
        self.chip_x, self.chip_y = self.along_x // 2, self.along_y // 2
        self.lines = [(lax.rem(z + k, 4), s) for k in range(1, 4)]
        self.plane = [(z, lax.rem(s + d, 8)) for d in range(1, 8)]
        self.to_x, self.to_y, self.to_core = [
            (z, to) for to in (self.along_x, self.along_y, self.partner)
        ]
        self.near = self.lines + [self.to_x, self.to_y, self.to_core]


class Gather:
    copies_each = 33

    def __init__(self, place, weights, wholes, kept, chunks, copies, given=None):
        z, s, lines = place.z, place.s, place.lines
        self.ready = arrive if given is None else done
        self.loads, self.own = [], []
        for weight, whole, keep in zip(weights, wholes, kept):
            if keep is None:
                self.loads.append(copies.inside(weight, whole.at[z]))
            else:
                self.loads.append(copies.inside(weight, keep))
                self.own.append(copies.inside(keep, whole.at[z]))
        self.first, self.second, self.third, self.cores, self.last = [], [], [], [], []
        for t, row, rows, column, columns in chunks:
            whole = wholes[t]
            wide = pl.ds(column, columns)
            every = pl.ds(row, rows)
            low, high = pl.ds(row, rows // 2), pl.ds(row + rows // 2, rows // 2)

            def same(k, rank, part, to):
                where = (k, rank, part, wide)
                return copies.plan(whole.at[where], whole.at[where], to)

            if given is None:
                first = [
                    copies.plan(weights[t].at[s, every, wide], whole.at[z, s, every, wide], to)
                    for to in lines
                ]
            else:
                first = [
                    copies.inside(given.at[k, every, wide], whole.at[k, s, every, wide])
                    for k, _ in lines
                ]
            self.first.append(first)
            second, third, cores, last = [], [], [], []
            for k, _ in lines:
                second.append(same(k, s, low, place.to_x))
                second.append(same(k, s, high, place.to_y))
                cores.append(same(k, s, every, place.to_core))
                third.append(same(k, s, low, place.to_y))
                third.append(same(k, s, high, place.to_x))
                third.append(same(k, place.along_x, low, place.to_y))
                third.append(same(k, place.along_y, high, place.to_x))
                for rank in (place.along_x, place.along_y, place.diagonal):
                    last.append(same(k, rank, every, place.to_core))
            self.second.append(second)
            self.third.append(third)
            self.cores.append(cores)
            self.last.append(last)

    def keep(self):
        done(self.loads)
        go(self.own)

    def start(self, t):
        go(self.first[t])

    def exchange(self, t):
        self.ready(self.first[t])
        go(self.second[t])
        go(self.cores[t])

    def spread(self, t):
        arrive(self.second[t])
        go(self.third[t])

    def share(self, t):
        arrive(self.third[t])
        go(self.last[t])

    def complete(self, t):
        arrive(self.cores[t] + self.last[t])


def add_into(target, other):
    target[...] = (target[...].astype(f32) + other[...].astype(f32)).astype(target.dtype)


def add_blocks(steps, block_of):
    def body(i, _):
        add_into(*block_of(i))
        return 0

    lax.fori_loop(0, steps, body, 0)


class Reduce:
    copies_each = 10

    def __init__(self, place, grads, outs, bufs, chunks, copies):
        self.place, self.outs, self.chunks = place, outs, chunks
        self.bufs = [bufs[7 * t : 7 * t + 7] for t in range(len(chunks))]
        self.loads, self.first, self.second, self.third, self.fourth = [], [], [], [], []
        for (t, row, rows, column, columns), buf in zip(chunks, self.bufs):
            own, from_core, from_x, from_y, late_y, late_x, from_z = buf
            every, wide = pl.ds(row, rows), pl.ds(column, columns)
            low, high = pl.ds(0, rows // 2), pl.ds(rows // 2, rows // 2)
            self.loads.append(
                copies.inside(grads[t].at[:, :, place.core, every, wide], own)
            )
            self.first.append(
                copies.plan(
                    grads[t].at[:, :, 1 - place.core, every, wide], from_core, place.to_core
                )
            )
            step = []
            for k in range(2):
                step.append(
                    copies.plan(own.at[:, 2 * k + 1 - place.x, low], from_x.at[:, k], place.to_x)
                )
                step.append(
                    copies.plan(
                        own.at[:, 2 * (1 - place.y) + k, high], from_y.at[:, k], place.to_y
                    )
                )
            self.second.append(step)
            self.third.append(
                [
                    copies.plan(own.at[:, place.chip_y, low], late_y, place.to_y),
                    copies.plan(own.at[:, place.chip_x, high], late_x, place.to_x),
                ]
            )
            self.fourth.append(
                [
                    copies.plan(own.at[to[0], place.chip], from_z.at[k], to)
                    for k, to in enumerate(place.lines)
                ]
            )

    def start(self):
        go(self.first)

    def halves(self, t):
        half = self.chunks[t][2] // 2
        return pl.ds(0, half), pl.ds(half, half)

    def exchange(self, t):
        own, from_core = self.bufs[t][:2]
        self.loads[t].wait()
        arrive([self.first[t]])
        add_blocks(16, lambda i: (own.at[i // 4, i % 4], from_core.at[i // 4, i % 4]))
        go(self.second[t])

    def spread(self, t):
        own, _, from_x, from_y = self.bufs[t][:4]
        low, high = self.halves(t)
        x, y = self.place.x, self.place.y
        arrive(self.second[t])
        add_blocks(8, lambda i: (own.at[i // 2, 2 * (i % 2) + x, low], from_x.at[i // 2, i % 2]))
        add_blocks(8, lambda i: (own.at[i // 2, 2 * y + i % 2, high], from_y.at[i // 2, i % 2]))
        go(self.third[t])

    def send(self, t):
        own, _, _, _, late_y, late_x, _ = self.bufs[t]
        low, high = self.halves(t)
        chip = self.place.chip
        arrive(self.third[t])
        add_blocks(4, lambda i: (own.at[i, chip, low], late_y.at[i]))
        add_blocks(4, lambda i: (own.at[i, chip, high], late_x.at[i]))
        go(self.fourth[t])

    def finish(self, t):
        own, from_z = self.bufs[t][0], self.bufs[t][6]
        index, row, rows, column, columns = self.chunks[t]
        arrive(self.fourth[t])
        total = own[self.place.z, self.place.chip].astype(f32)
        for k in range(3):
            total = total + from_z[k].astype(f32)
        self.outs[index][row : row + rows, column : column + columns] = total


def reduce_scratch(chunks):
    scratch = []
    for _, _, rows, _, columns in chunks:
        half = rows // 2
        scratch += [
            pltpu.VMEM((4, 4, rows, columns), bf16),
            pltpu.VMEM((4, 4, rows, columns), bf16),
            pltpu.VMEM((4, 2, half, columns), bf16),
            pltpu.VMEM((4, 2, half, columns), bf16),
            pltpu.VMEM((4, half, columns), bf16),
            pltpu.VMEM((4, half, columns), bf16),
            pltpu.VMEM((3, rows, columns), bf16),
        ]
    return scratch


class ReduceAlong(Reduce):
    def __init__(self, place, grad, out, buf, chunk, copies):
        self.place, self.grad, self.out, self.buf, self.chunk = place, grad, out, buf, chunk
        own, from_core, from_z, from_x, from_y, late_y, late_x = buf
        _, row, rows, column, columns = chunk
        every, wide = pl.ds(row, rows), pl.ds(column, columns)
        self.low, self.high = low, high = pl.ds(0, rows // 2), pl.ds(rows // 2, rows // 2)
        z, x, y = place.z, place.x, place.y
        self.load = copies.inside(grad.at[:, :, place.core, every, wide], own)
        self.first = copies.plan(
            grad.at[:, :, 1 - place.core, every, wide], from_core, place.to_core
        )
        self.second = [
            copies.plan(own.at[to[0]], from_z.at[k], to) for k, to in enumerate(place.lines)
        ]
        self.third = []
        for k in range(2):
            self.third.append(
                copies.plan(own.at[z, 2 * k + 1 - x, low], from_x.at[k], place.to_x)
            )
            self.third.append(
                copies.plan(own.at[z, 2 * (1 - y) + k, high], from_y.at[k], place.to_y)
            )
        self.fourth = [
            copies.plan(own.at[z, place.chip_y, low], late_y, place.to_y),
            copies.plan(own.at[z, place.chip_x, high], late_x, place.to_x),
        ]

    def exchange(self):
        own, from_core = self.buf[:2]
        self.load.wait()
        arrive([self.first])
        add_blocks(16, lambda i: (own.at[i // 4, i % 4], from_core.at[i // 4, i % 4]))
        go(self.second)

    def spread(self):
        own, _, from_z = self.buf[:3]
        z = self.place.z
        arrive(self.second)

        def body(i, _):
            total = own[z, i].astype(f32)
            for k in range(3):
                total = total + from_z[k, i].astype(f32)
            own[z, i] = total.astype(bf16)
            return 0

        lax.fori_loop(0, 4, body, 0)
        go(self.third)

    def send(self):
        own, _, _, from_x, from_y = self.buf[:5]
        z, x, y = self.place.z, self.place.x, self.place.y
        arrive(self.third)
        add_blocks(2, lambda j: (own.at[z, 2 * j + x, self.low], from_x.at[j]))
        add_blocks(2, lambda j: (own.at[z, 2 * y + j, self.high], from_y.at[j]))
        go(self.fourth)

    def finish(self):
        own, late_y, late_x = self.buf[0], self.buf[5], self.buf[6]
        z, chip = self.place.z, self.place.chip
        _, row, rows, column, columns = self.chunk
        arrive(self.fourth)
        half = rows // 2
        wide = slice(column, column + columns)
        self.out[row : row + half, wide] = own[z, chip, self.low].astype(f32) + late_y[...].astype(
            f32
        )
        self.out[row + half : row + rows, wide] = own[z, chip, self.high].astype(f32) + late_x[
            ...
        ].astype(f32)


def reduce_along_scratch(chunk):
    _, _, rows, _, columns = chunk
    half = rows // 2
    return [
        pltpu.VMEM((4, 4, rows, columns), bf16),
        pltpu.VMEM((4, 4, rows, columns), bf16),
        pltpu.VMEM((3, 4, rows, columns), bf16),
        pltpu.VMEM((2, half, columns), bf16),
        pltpu.VMEM((2, half, columns), bf16),
        pltpu.VMEM((half, columns), bf16),
        pltpu.VMEM((half, columns), bf16),
    ]


class HandBack:
    def __init__(self, place, source, target, features, send, recv, local):
        self.place, self.source, self.target = place, source, target
        self.mine = columns_of(place.s, features)
        self.send, self.recv, self.local = send, recv, local
        self.blocks = source.shape[1]

    def copy(self, b, i, d):
        rank = self.place.plane[d][1]
        n = b * self.blocks + i
        return pltpu.make_async_remote_copy(
            src_ref=self.source.at[b, i, rank],
            dst_ref=self.target.at[b, i, :, self.mine],
            send_sem=self.send.at[n, d],
            recv_sem=self.recv.at[n, d],
            device_id=self.place.plane[d],
            device_id_type=MESH,
        )

    def own(self, b, i):
        return pltpu.make_async_copy(
            self.source.at[b, i, self.place.s],
            self.target.at[b, i, :, self.mine],
            self.local.at[b * self.blocks + i],
        )

    def each(self, b, i):
        for d in range(7):
            self.copy(b, i, d).start()
        self.own(b, i).start()

    def finish(self):
        def body(n, _):
            b, i = n // self.blocks, n % self.blocks
            for d in range(7):
                self.copy(b, i, d).wait()
            self.own(b, i).wait()
            return 0

        lax.fori_loop(0, self.source.shape[0] * self.blocks, body, 0)


def hand_back_semaphores(steps):
    return [
        pltpu.SemaphoreType.DMA((steps, 7)),
        pltpu.SemaphoreType.DMA((steps, 7)),
        pltpu.SemaphoreType.DMA((steps,)),
    ]


class ReduceLines:
    copies = 4 * 7 + 3

    def __init__(self, place, grad, out, bufs, copies):
        self.place, self.grad, self.out, self.bufs = place, grad, out, bufs
        from_core, from_x, from_y, late_y, late_x, from_z = bufs
        core, x, y = place.core, place.x, place.y
        self.order = [to[0] for to in place.lines] + [place.z]
        rows = grad.shape[3]
        self.low, self.high = pl.ds(0, rows // 2), pl.ds(rows // 2, rows // 2)
        self.first, self.second, self.third, self.fourth = [], [], [], []
        for k, at in enumerate(self.order):
            self.first.append(
                copies.plan(grad.at[at, :, 1 - core], from_core.at[k], place.to_core)
            )
            step = []
            for j in range(2):
                step.append(
                    copies.plan(
                        grad.at[at, 2 * j + 1 - x, core, self.low], from_x.at[k, j], place.to_x
                    )
                )
                step.append(
                    copies.plan(
                        grad.at[at, 2 * (1 - y) + j, core, self.high], from_y.at[k, j], place.to_y
                    )
                )
            self.second.append(step)
            self.third.append(
                [
                    copies.plan(grad.at[at, place.chip_y, core, self.low], late_y.at[k], place.to_y),
                    copies.plan(
                        grad.at[at, place.chip_x, core, self.high], late_x.at[k], place.to_x
                    ),
                ]
            )
            if k < 3:
                self.fourth.append(
                    copies.plan(grad.at[at, place.chip, core], from_z.at[k], place.lines[k])
                )

    def start(self, k):
        go([self.first[k]])

    def exchange(self, k):
        arrive([self.first[k]])
        at, core = self.order[k], self.place.core
        add_blocks(4, lambda i: (self.grad.at[at, i, core], self.bufs[0].at[k, i]))
        go(self.second[k])

    def spread(self, k):
        arrive(self.second[k])
        at, core, x, y = self.order[k], self.place.core, self.place.x, self.place.y
        add_blocks(
            2, lambda j: (self.grad.at[at, 2 * j + x, core, self.low], self.bufs[1].at[k, j])
        )
        add_blocks(
            2, lambda j: (self.grad.at[at, 2 * y + j, core, self.high], self.bufs[2].at[k, j])
        )
        go(self.third[k])

    def send(self, k):
        arrive(self.third[k])
        at, core, chip = self.order[k], self.place.core, self.place.chip
        add_into(self.grad.at[at, chip, core, self.low], self.bufs[3].at[k])
        add_into(self.grad.at[at, chip, core, self.high], self.bufs[4].at[k])
        go(self.fourth[k : k + 1])

    def finish(self):
        arrive(self.fourth)
        place = self.place
        total = self.grad[place.z, place.chip, place.core].astype(f32)
        for k in range(3):
            total = total + self.bufs[5][k].astype(f32)
        self.out[...] = total


def reduce_lines_scratch(rows, columns):
    half = rows // 2
    return [
        pltpu.VMEM((4, 4, rows, columns), bf16),
        pltpu.VMEM((4, 2, half, columns), bf16),
        pltpu.VMEM((4, 2, half, columns), bf16),
        pltpu.VMEM((4, half, columns), bf16),
        pltpu.VMEM((4, half, columns), bf16),
        pltpu.VMEM((3, rows, columns), bf16),
    ]


def split_grad(item):
    return item.reshape(4, 4, 2, item.shape[0] // 32, item.shape[1])


def split_weight(item):
    return item.reshape(8, item.shape[0] // 8, item.shape[1])


def chunks_of(index, rows, columns, count):
    if rows >= 64:
        return [(index, rows // count * n, rows // count, 0, columns) for n in range(count)]
    return [(index, 0, rows, columns // count * n, columns // count) for n in range(count)]


def semaphores(remote, local):
    return [pltpu.SemaphoreType.DMA((n,)) for n in (remote, remote, local)]


def remote_call(kernel, name, collective, **options):
    return pl.pallas_call(
        kernel,
        name=name,
        compiler_params=pltpu.CompilerParams(
            collective_id=collective, has_side_effects=True, vmem_limit_bytes=vmem_bytes
        ),
        **options,
    )


def columns_of(rank, features):
    return pl.ds(pl.multiple_of(rank * features, 128), features)


def forward_fused_kernel(heads, width, count, vector_count, chunks, slopes, tokens, upstream, *refs):
    vectors, refs = refs[:vector_count], refs[vector_count:]
    weights, contract, refs = refs[:count], refs[count], refs[count + 1 :]
    tokens_out, vectors_out, joined_out, qkv_out, attended, out_t, lse, upstream_out = refs[:8]
    contract_out = refs[8]
    wholes, refs = refs[9 : 8 + count], refs[8 + count :]
    held, small, values_of, joined, normed, outgoing, qkv, result, upstream_own = refs[:9]
    attention = Forward(heads, width, slopes, qkv, result, out_t, lse, *refs[9:12])
    kept, refs = refs[12 : 11 + count], refs[11 + count :]
    head_send, head_recv = refs[:2]
    copies = Copies(*refs[5:])
    place = Place()
    z, s, lines, plane = place.z, place.s, place.lines, place.plane
    gather = Gather(place, weights, [joined, *wholes], [None, *kept], chunks, copies)
    first = [t for t, chunk in enumerate(chunks) if chunk[0] == 0]
    later = [t for t, chunk in enumerate(chunks) if chunk[0] > 0]
    features = heads * width
    back = HandBack(place, result, attended, features, *refs[2:5])
    own_seqs, parts, piece, wide = held.shape

    load = copies.inside(tokens.at[z], held.at[:, z])
    load_upstream = copies.inside(upstream.at[z], upstream_own)
    seqs = [copies.plan(tokens.at[to[0]], held.at[:, z], to) for to in lines]
    vector_copies = [copies.plan(small.at[z], small.at[z], to) for to in lines]
    upstreams = [copies.plan(upstream.at[to[0]], upstream_out.at[:, z], to) for to in lines]
    keep_upstream = copies.inside(upstream_own, upstream_out.at[:, z])
    keeping = [
        copies.inside(held, tokens_out),
        copies.inside(small, vectors_out),
        copies.inside(joined, joined_out),
    ]
    keep_qkv = copies.inside(qkv, qkv_out)
    contracts = [copies.plan(contract.at[s], contract_out.at[z], to) for to in lines]

    def to_head(d):
        return pltpu.make_async_remote_copy(
            src_ref=outgoing.at[d],
            dst_ref=qkv.at[:, :, s],
            send_sem=head_send.at[d],
            recv_sem=head_recv.at[d],
            device_id=(z, lax.rem(s + 1 + d, 8)),
            device_id_type=MESH,
        )

    go(gather.loads + [load, load_upstream])
    small[z] = jnp.zeros(small.shape[1:], bf16)
    for n, item in enumerate(vectors):
        small[z, n, : item.shape[0], :] = item[...]
    greet(lines + plane)
    for t in first:
        gather.start(t)
    go(seqs + vector_copies)
    gather.keep()
    load.wait()
    for t in range(len(first) + 2):
        if t < len(first):
            gather.exchange(t)
        if 0 <= t - 1 < len(first):
            gather.spread(t - 1)
        if 0 <= t - 2:
            gather.share(t - 2)
    load_upstream.wait()
    keep_upstream.start()
    arrive(seqs + vector_copies)
    for t in later:
        gather.start(t)
    values_of[...] = small[...].astype(f32)

    def row_of(n):
        found = [values_of[k, n, r : r + 1, :] for k in range(4) for r in range(wide // 512)]
        return jnp.concatenate(found, axis=1)

    gain, shift = row_of(0), row_of(1)

    def norm(i, _):
        values = held[i // parts, i % parts].astype(f32)
        rows = pl.ds(pl.multiple_of(i * piece, piece), piece)
        normed[rows, :] = normalize(values, gain, shift).astype(bf16)
        return 0

    lax.fori_loop(0, own_seqs * parts, norm, 0)
    for t in first:
        gather.complete(t)
    go(keeping)

    def project(d, _):
        rank = lax.rem(s + 1 + d, 8)
        per = 8 // 4
        query_bias = values_of[rank // per, 2, pl.ds(rank % per, 1), :]
        value_bias = values_of[rank // per, 3, pl.ds(rank % per, 1), :]
        low = lax.broadcasted_iota(jnp.int32, query_bias.shape, 1) < width
        bias = jnp.concatenate(
            [
                jnp.where(low, query_bias, 0.0),
                jnp.where(low, value_bias, query_bias),
                jnp.where(low, 0.0, value_bias),
            ],
            axis=1,
        )
        weight = joined[:, :, :, columns_of(rank, 3 * features)].reshape(wide, 3 * features)
        made = (matmul(normed[...], weight) + bias).astype(bf16)
        outgoing[d] = made.reshape(outgoing.shape[1:])
        pl.when(d < 7)(lambda: to_head(d).start())
        return 0

    lax.fori_loop(0, 8, project, 0)
    own_copy = copies.inside(outgoing.at[7], qkv.at[:, :, s])
    own_copy.start()
    base = later[0]
    gather.exchange(base)
    gather.exchange(base + 1)
    own_copy.wait()
    gather.spread(base)
    for d in range(7):
        to_head(d).wait_recv()
    keep_qkv.start()
    attention.run(
        {
            0: [(gather.exchange, base + 2), (go, contracts), (gather.spread, base + 1)],
            2: [(gather.spread, base + 2), (gather.share, base)],
            3: [(go, upstreams)],
            5: [(gather.share, base + 1)],
            6: [(gather.share, base + 2)],
        },
        back.each,
    )
    for t in later:
        gather.complete(t)
    arrive(contracts + upstreams)
    back.finish()
    for d in range(7):
        to_head(d).wait_send()
    copies.finish()
    done(gather.own + [keep_upstream, keep_qkv] + keeping)


def forward_fused(tokens, upstream, vectors, weights, contract, slopes, heads, width):
    seqs, piece, features = tokens.shape
    parts = 4
    own = seqs // parts
    columns = heads * width
    length = parts * 8 * piece
    vectors = [item.reshape(-1, 128) for item in vectors]
    cut = [split_weight(item) for item in weights]
    contract = split_weight(contract)
    count, tall = len(cut), 8 * -(-max(item.shape[0] for item in vectors) // 8)
    chunks = []
    for t, pieces in enumerate((3, 1, 2)):
        chunks += chunks_of(t, *cut[t].shape[1:], pieces)
    seq_shape = (own, parts, piece, features)
    qkv_shape = (own, parts, 8, piece, 3 * columns)
    small = (parts, len(vectors), tall, 128)
    out = remote_call(
        functools.partial(forward_fused_kernel, heads, width, count, len(vectors), chunks),
        "forward_fused",
        1,
        out_shape=(
            jax.ShapeDtypeStruct(seq_shape, bf16),
            jax.ShapeDtypeStruct(small, bf16),
            jax.ShapeDtypeStruct((parts, *cut[0].shape), bf16),
            jax.ShapeDtypeStruct(qkv_shape, bf16),
            jax.ShapeDtypeStruct(seq_shape, bf16),
            *saved_shapes(own, length, heads, width),
            jax.ShapeDtypeStruct(seq_shape, bf16),
            jax.ShapeDtypeStruct((parts, *contract.shape[1:]), bf16),
            *[jax.ShapeDtypeStruct((parts, *item.shape), bf16) for item in cut[1:]],
        ),
        in_specs=[SMEM, HBM, HBM] + [VMEM] * len(vectors) + [HBM] * (count + 1),
        out_specs=(HBM,) * 5 + (VMEM, VMEM) + (HBM,) * (count + 1),
        scratch_shapes=[
            pltpu.VMEM(seq_shape, bf16),
            pltpu.VMEM(small, bf16),
            pltpu.VMEM(small, f32),
            pltpu.VMEM((parts, *cut[0].shape), bf16),
            pltpu.VMEM((own * parts * piece, features), bf16),
            pltpu.VMEM((8, own, parts, piece, 3 * columns), bf16),
            pltpu.VMEM(qkv_shape, bf16),
            pltpu.VMEM((own, parts, 8, piece, columns), bf16),
            pltpu.VMEM((own, piece, features), bf16),
            *forward_scratch(length, heads, width),
            *[pltpu.VMEM(item.shape, bf16) for item in cut[1:]],
            pltpu.SemaphoreType.DMA((7,)),
            pltpu.SemaphoreType.DMA((7,)),
            *hand_back_semaphores(own * parts),
            *semaphores(12 + len(chunks) * Gather.copies_each, 2 * count - 1 + 8),
        ],
    )(
        slopes,
        tokens.reshape(parts, own, piece, features),
        upstream.reshape(parts, own, piece, features),
        *vectors,
        *cut,
        contract,
    )
    wholes = [
        whole.reshape(4 * item.shape[0], item.shape[1])
        for whole, item in zip((out[2], *out[9:]), weights)
    ]
    found = [out[1][:, n, : item.shape[0]].reshape(-1) for n, item in enumerate(vectors)]
    return out[0], found, [*wholes, out[8]], out[3], out[4], (out[5], out[6]), out[7]


def feed_forward_kernel(
    chunks, expand, contract, contract_line, expand_bias, second, upstream, residual,
    layer, second_back, expand_grad, bias_grad, contract_grad,
    expand_in, contract_in, second_t, expanded, activated, grad, staged, *refs,
):
    bufs, refs = refs[:6], refs[6:]
    loaded, stored, refs = refs[0], refs[1], refs[2:]
    copies = Copies(*refs)
    place = Place()
    z = place.z
    reduce = ReduceLines(place, grad, contract_grad, bufs, copies)
    gather = Gather(
        place, [contract], [contract_in], [None], chunks, copies, given=contract_line
    )
    rows, features = second.shape
    steps = 8
    wide = expand.shape[1] // steps

    def at(n):
        part = (z + 1 + n // 2) % 4
        return part, n % 2, pl.ds(pl.multiple_of((2 * part + n % 2) * wide, wide), wide)

    def load(n):
        _, _, where = at(n)
        return pltpu.make_async_copy(expand.at[:, where], expand_in.at[:, where], loaded.at[n])

    def contract_at(n):
        part, side, _ = at(n)
        return contract_in[part, pl.ds(4 * side, 4)].reshape(wide, features)

    def store(n):
        _, _, where = at(n)
        slot = n % 2
        return pltpu.make_async_copy(
            staged.at[slot], expand_grad.at[:, where], stored.at[slot]
        )

    for n in range(len(chunks)):
        gather.start(n)
    for n in range(steps):
        load(n).start()
    go(gather.loads)
    greet(place.near)
    for n in range(len(chunks)):
        gather.exchange(n)
    second_t[...] = second[...].T
    second_back[...] = residual[...]

    def forward(n, after):
        part, side, where = at(n)
        load(n).wait()
        values = matmul(second[...], expand_in[:, where]) + expand_bias[:, where]
        expanded[:, where] = values
        low = gelu_tanh(values).astype(bf16)
        activated[:, where] = low
        made = matmul(low.T, upstream[...]).astype(bf16)
        grad[part, pl.ds(2 * side, 2)] = made.reshape(2, 2, wide // 4, features)
        follow(n, after)
        return 0

    def shrink(n, after):
        _, _, where = at(n)
        second_back[...] += matmul(activated[:, where], contract_at(n))
        follow(n, after)
        return 0

    def backward(n, after):
        _, _, where = at(n)
        values = expanded[:, where]
        act_grad = matmul_rt(upstream[...], contract_at(n))
        bent = jnp.tanh(gelu_coef * (values + 0.044715 * values * values * values))
        slope = 0.5 * (1.0 + bent) + 0.5 * values * (1.0 - bent * bent) * (
            gelu_coef * (1.0 + 3.0 * 0.044715 * values * values)
        )
        diff = (act_grad * slope).astype(bf16)
        bias_grad[:, where] = jnp.sum(diff.astype(f32), axis=0, keepdims=True)
        pl.when(n >= 2)(lambda: store(n - 2).wait())
        staged[n % 2] = matmul(second_t[...], diff).astype(bf16)
        store(n).start()
        second_back[...] += matmul_rt(diff, expand_in[:, where])
        follow(n, after)
        return 0

    last = len(chunks) - 1
    forward_steps = {
        1: [(reduce.start, 0)] + [(gather.spread, n) for n in range(last)],
        2: [(gather.spread, last)],
        3: [(reduce.exchange, 0), (reduce.start, 1)],
        5: [(reduce.start, 2), (reduce.exchange, 1)],
        7: [(reduce.start, 3), (reduce.exchange, 2)] + [(gather.share, n) for n in range(last)],
    }
    shrink_steps = {
        1: [(reduce.exchange, 3)],
        3: [(reduce.spread, 0)],
        7: [(reduce.spread, 1)],
    }
    backward_steps = {
        1: [(reduce.spread, 2)],
        2: [(reduce.spread, 3)],
        3: [(reduce.send, 0)],
        4: [(reduce.send, 1)],
        5: [(reduce.send, 2)],
        6: [(reduce.send, 3)],
    }
    lax.fori_loop(0, steps, lambda n, _: forward(n, forward_steps), 0)
    gather.share(last)
    for n in range(len(chunks)):
        gather.complete(n)
    done(gather.loads)
    lax.fori_loop(0, steps, lambda n, _: shrink(n, shrink_steps), 0)
    layer[...] = second_back[...].astype(bf16).reshape(layer.shape)
    second_back[...] = jnp.zeros_like(second_back)
    lax.fori_loop(0, steps, lambda n, _: backward(n, backward_steps), 0)
    reduce.finish()
    store(steps - 2).wait()
    store(steps - 1).wait()
    copies.finish()


def feed_forward(shape, expand, contract, line, expand_bias, second, upstream, residual):
    own, parts, piece = shape
    rows, features = second.shape
    hidden = expand.shape[1]
    wide = hidden // 8
    each = hidden // 32
    contract = split_weight(contract)
    chunks = chunks_of(0, *contract.shape[1:], 2)
    return remote_call(
        functools.partial(feed_forward_kernel, chunks),
        "feed_forward",
        4,
        out_shape=(
            jax.ShapeDtypeStruct((own, parts, piece, features), bf16),
            jax.ShapeDtypeStruct((rows, features), f32),
            jax.ShapeDtypeStruct((features, hidden), bf16),
            jax.ShapeDtypeStruct((1, hidden), f32),
            jax.ShapeDtypeStruct((each, features), f32),
        ),
        in_specs=[HBM, HBM, HBM, VMEM, VMEM, VMEM, VMEM],
        out_specs=(VMEM, VMEM, HBM, VMEM, VMEM),
        scratch_shapes=[
            pltpu.VMEM((features, hidden), bf16),
            pltpu.VMEM((4, *contract.shape), bf16),
            pltpu.VMEM((features, rows), bf16),
            pltpu.VMEM((rows, hidden), f32),
            pltpu.VMEM((rows, hidden), bf16),
            pltpu.VMEM((4, 4, 2, each, features), bf16),
            pltpu.VMEM((2, features, wide), bf16),
            *reduce_lines_scratch(each, features),
            pltpu.SemaphoreType.DMA((8,)),
            pltpu.SemaphoreType.DMA((2,)),
            *semaphores(
                ReduceLines.copies + len(chunks) * (Gather.copies_each - 3),
                1 + 3 * len(chunks),
            ),
        ],
    )(expand, contract, line, expand_bias, second, upstream, residual)


def backward_fused_kernel(heads, width, count, chunks, *refs):
    slopes, diff_in, qkv_in, out_t_in, lse_in, layer = refs[:6]
    grads, refs = refs[6 : 6 + count], refs[6 + count :]
    joined_out, layer_out, layer_own = refs[0], refs[1], refs[2 + count]
    outs, refs = refs[2 : 2 + count], refs[3 + count :]
    diff, qkv, out_t, lse, joined = refs[:5]
    attention = Backward(heads, width, slopes, qkv, diff, out_t, lse, joined, *refs[5:12])
    bufs, refs = refs[12 : 12 + 7 * len(chunks)], refs[12 + 7 * len(chunks) :]
    copies = Copies(*refs[3:])
    place = Place()
    s, plane = place.s, place.plane
    features = heads * width
    along = ReduceAlong(place, grads[0], outs[0], bufs[:7], chunks[0], copies)
    reduce = Reduce(place, grads, outs, bufs[7:], chunks[1:], copies)
    back = HandBack(place, joined, joined_out, 3 * features, *refs[:3])

    own = [copies.inside(diff_in.at[:, :, :, columns_of(s, features)], diff.at[:, :, s])]
    own += [copies.inside(a, b) for a, b in ((qkv_in, qkv), (out_t_in, out_t), (lse_in, lse))]
    arriving = [
        copies.plan(diff_in.at[:, :, :, columns_of(to[1], features)], diff.at[:, :, s], to)
        for to in plane
    ]
    returned = [copies.plan(layer.at[:, to[0]], layer_out.at[place.z], to) for to in place.lines]
    load_layer = copies.inside(layer.at[:, place.z], layer_own)
    keep_layer = copies.inside(layer_own, layer_out.at[place.z])
    go(own + reduce.loads + [along.load, load_layer])
    greet(place.lines + plane)
    go(arriving + [along.first])
    reduce.start()
    along.exchange()
    go(returned)
    for t in range(3):
        reduce.exchange(t)
    done(own + [load_layer])
    keep_layer.start()
    arrive(arriving)
    attention.run(
        {
            1: [(reduce.spread, 0)],
            2: [(along.spread,)],
            3: [(reduce.spread, 1), (reduce.spread, 2)],
            4: [(reduce.send, 0), (along.send,)],
            5: [(reduce.send, 1)],
            6: [(reduce.send, 2)],
        },
        back.each,
    )
    for t in range(3):
        reduce.finish(t)
    along.finish()
    back.finish()
    arrive(returned)
    copies.finish()
    keep_layer.wait()


def backward_fused(attended_diff, qkv, saved, layer, grads, slopes, heads, width):
    own, parts, piece, columns = attended_diff.shape
    features = heads * width
    length = parts * 8 * piece
    cut = [split_grad(item) for item in grads]
    count = len(cut)
    rows, wide = cut[0].shape[3:]
    part = 3 * wide // 8
    chunks = [
        (0, 0, rows, 0, wide // 4),
        (0, 0, rows, wide // 4, part),
        (0, 0, rows, wide // 4 + part, part),
        *chunks_of(1, *cut[1].shape[3:], 1),
    ]
    out = remote_call(
        functools.partial(backward_fused_kernel, heads, width, count, chunks),
        "backward_fused",
        2,
        out_shape=(
            jax.ShapeDtypeStruct((own, parts, piece, 24 * features), bf16),
            jax.ShapeDtypeStruct((parts, own, piece, columns), bf16),
            *[jax.ShapeDtypeStruct(item.shape[3:], f32) for item in cut],
        ),
        in_specs=[SMEM] + [HBM] * (5 + count),
        out_specs=(HBM, HBM) + (VMEM,) * count,
        scratch_shapes=[
            pltpu.VMEM((own, piece, columns), bf16),
            pltpu.VMEM((own, parts, 8, piece, features), bf16),
            pltpu.VMEM(qkv.shape, bf16),
            *[pltpu.VMEM(item.shape, f32) for item in saved],
            pltpu.VMEM(qkv.shape, bf16),
            *backward_scratch(length, heads, width),
            *reduce_along_scratch(chunks[0]),
            *reduce_scratch(chunks[1:]),
            *hand_back_semaphores(own * parts),
            *semaphores(10 + len(chunks) * Reduce.copies_each, len(chunks) + 6),
        ],
    )(slopes, attended_diff, qkv, *saved, layer, *cut)
    return out[0], out[1].reshape(parts * own, piece, columns), out[2:]


def end_kernel(chunks, input_grad, vector, grad, input_out, vector_out, out, *refs):
    input_own, ranks, plane_sum, others = refs[:4]
    bufs, refs = refs[4 : 4 + 7 * len(chunks)], refs[4 + 7 * len(chunks) :]
    copies = Copies(*refs)
    place = Place()
    z, s, lines, plane = place.z, place.s, place.lines, place.plane
    count = len(chunks)
    reduce = Reduce(place, [grad], [out], bufs, chunks, copies)
    load = copies.inside(input_grad.at[:, z], input_own)
    load_vector = copies.inside(vector.at[:, s], ranks.at[0])
    keep = copies.inside(input_own, input_out.at[z])
    waiting = [copies.plan(input_grad.at[:, to[0]], input_out.at[z], to) for to in lines]
    vectors = [
        copies.plan(vector.at[:, to[1]], ranks.at[d + 1], to) for d, to in enumerate(plane)
    ]
    sums = [copies.plan(plane_sum.at[to[0]], others.at[k], to) for k, to in enumerate(lines)]
    go(reduce.loads + [load, load_vector])
    greet(lines + plane)
    reduce.start()
    go(waiting + vectors)
    load.wait()
    go([keep])
    for t in range(count + 2):
        if t < count:
            reduce.exchange(t)
        if t == 0:
            load_vector.wait()
            arrive(vectors)
            total = ranks[0]
            for d in range(1, 8):
                total = total + ranks[d]
            plane_sum[...] = total
            go(sums)
        if 0 <= t - 1 < count:
            reduce.spread(t - 1)
        if 0 <= t - 2:
            reduce.send(t - 2)
    arrive(sums)
    total = plane_sum[z]
    for k in range(3):
        total = total + others[k]
    vector_out[...] = total
    for t in range(count):
        reduce.finish(t)
    arrive(waiting)
    copies.finish()
    keep.wait()


def end(input_grad, vector, grad):
    own, parts, piece, features = input_grad.shape
    lanes = vector.shape[-1]
    padded = -(-lanes // 1024) * 1024
    vector = jnp.pad(vector, ((0, 0), (0, padded - lanes))).reshape(4, 8, padded // 128, 128)
    cut = split_grad(grad)
    chunks = chunks_of(0, *cut.shape[3:], 3)
    out = remote_call(
        functools.partial(end_kernel, chunks),
        "end",
        3,
        out_shape=(
            jax.ShapeDtypeStruct((parts, own, piece, features), bf16),
            jax.ShapeDtypeStruct(vector.shape[2:], f32),
            jax.ShapeDtypeStruct(cut.shape[3:], f32),
        ),
        in_specs=[HBM] * 3,
        out_specs=(HBM, VMEM, VMEM),
        scratch_shapes=[
            pltpu.VMEM((own, piece, features), bf16),
            pltpu.VMEM((8, 4, padded // 128, 128), f32),
            pltpu.VMEM((4, padded // 128, 128), f32),
            pltpu.VMEM((3, padded // 128, 128), f32),
            *reduce_scratch(chunks),
            *semaphores(3 + 7 + 3 + len(chunks) * Reduce.copies_each, 3 + len(chunks)),
        ],
    )(input_grad, vector, cut)
    return out[0].reshape(parts * own, piece, features), out[1].reshape(-1)[:lanes], out[2]


def per_device(
    layer_input,
    first_gain,
    first_shift,
    joined_weight,
    query_bias,
    value_bias,
    output_weight,
    output_bias,
    second_gain,
    second_shift,
    expand_weight,
    expand_bias,
    contract_weight,
    contract_bias,
    alibi_slopes,
    upstream,
):
    seqs, piece, features = layer_input.shape
    fs_count = lax.axis_size("fs")
    sp_count = lax.axis_size("sp")
    head_count = alibi_slopes.shape[0]
    width = features // head_count
    heads = head_count // sp_count
    rows = seqs * piece
    own = seqs // fs_count
    shape = (own, fs_count, piece)
    slopes = lax.dynamic_slice_in_dim(alibi_slopes, lax.axis_index("sp") * heads, heads)

    vectors = (
        first_gain, first_shift, query_bias, value_bias, output_bias,
        second_gain, second_shift, contract_bias, expand_bias,
    )
    fast = (fs_count, sp_count) == (4, 8) and (own, heads, width) == (2, 2, 64)
    weights = (joined_weight, output_weight, expand_weight)
    gather = lambda item: lax.all_gather(item, "fs", axis=0, tiled=True)
    if fast:
        tokens, whole, weights, qkv, attended, saved, upstream_low = forward_fused(
            layer_input, upstream, vectors, weights, contract_weight, slopes, heads, width
        )
    else:
        tokens, upstream_low = to_own_seqs(layer_input), to_own_seqs(upstream)
        whole = [gather(item) for item in vectors]
        weights = [gather(item) for item in (*weights, contract_weight)]
    joined_full, out_full, expand_full, contract_full = weights
    tokens = tokens.reshape(rows, features).astype(f32)
    gain_one, shift_one, qbias, vbias, obias, gain_two, shift_two, cbias, ebias = [
        item.astype(f32) for item in whole
    ]

    normed_f, norm_back_one = jax.vjp(normalize, tokens, gain_one, shift_one)
    normed = normed_f.astype(bf16)
    if not fast:
        joined_bias = joined_bias_of(qbias, vbias, head_count)
        joined_all = (matmul(normed, joined_full) + joined_bias).astype(bf16)
        qkv = to_heads(joined_all.reshape(*shape, 3 * features))
        attended, *saved = attention_forward(qkv, slopes, heads, width)
        attended = from_heads(attended)
    attended = attended.reshape(rows, features)
    upstream_low = upstream_low.reshape(rows, features)

    residual = tokens + (matmul(attended, out_full) + obias)
    second_f, norm_back_two = jax.vjp(normalize, residual, gain_two, shift_two)
    second = second_f.astype(bf16)
    upstream_f = upstream_low.astype(f32)
    contract_bias_grad = jnp.sum(upstream_f, axis=0)
    if fast:
        layer_output, second_back, expand_grad, expand_bias_grad, contract_grad = feed_forward(
            shape, expand_full, contract_weight, contract_full, ebias.reshape(1, -1), second,
            upstream_low, residual + cbias,
        )
        expand_bias_grad = expand_bias_grad.reshape(-1)
    else:
        expanded = matmul(second, expand_full) + ebias
        activated_f, gelu_back = jax.vjp(gelu_tanh, expanded)
        activated = activated_f.astype(bf16)
        result = residual + (matmul(activated, contract_full) + cbias)
        layer_output = result.astype(bf16).reshape(*shape, features)

        contract_grad = matmul_lt(activated, upstream_low)
        act_grad = matmul_rt(upstream_low, contract_full)
        expand_diff = gelu_back(act_grad)[0].astype(bf16)
        expand_grad = matmul_lt(second, expand_diff)
        expand_bias_grad = jnp.sum(expand_diff.astype(f32), axis=0)
        second_back = matmul_rt(expand_diff, expand_full)
    resid_part, second_gain_grad, second_shift_grad = norm_back_two(second_back)
    residual_grad = upstream_f + resid_part

    branch_diff = residual_grad.astype(bf16)
    output_weight_grad = matmul_lt(attended, branch_diff)
    output_bias_grad = jnp.sum(branch_diff.astype(f32), axis=0)
    attended_diff = matmul_rt(branch_diff, out_full).astype(bf16)
    attended_diff = attended_diff.reshape(*shape, features)
    grads = (expand_grad, output_weight_grad)
    scatter = functools.partial(
        lax.psum_scatter, axis_name=("fs", "sp"), scatter_dimension=0, tiled=True
    )
    if fast:
        joined_diff, layer_output, grads = backward_fused(
            attended_diff, qkv, saved, layer_output, [item.astype(bf16) for item in grads],
            slopes, heads, width,
        )
    else:
        joined_diff = attention_backward(
            qkv, to_heads(attended_diff), *saved, slopes, heads, width
        )
        joined_diff, layer_output = from_heads(joined_diff), from_own_seqs(layer_output)
        grads = [scatter(item) for item in grads]
        contract_grad = scatter(contract_grad)
    expand_grad, output_weight_grad = grads
    joined_diff = joined_diff.reshape(rows, 3 * features)

    joined_grad = matmul_lt(normed, joined_diff)
    column_sums = jnp.sum(joined_diff.astype(f32), axis=0).reshape(head_count, 3, width)
    query_bias_grad = column_sums[:, 0].reshape(features)
    value_bias_grad = column_sums[:, 2].reshape(features)
    normed_back = matmul_rt(joined_diff, joined_full)
    input_part, first_gain_grad, first_shift_grad = norm_back_one(normed_back)
    input_grad = (residual_grad + input_part).astype(bf16).reshape(*shape, features)

    vector_grads = (
        first_gain_grad, first_shift_grad, query_bias_grad, value_bias_grad, output_bias_grad,
        second_gain_grad, second_shift_grad, contract_bias_grad, expand_bias_grad,
    )
    devices = fs_count * sp_count
    packed = jnp.concatenate([item.reshape(devices, -1) for item in vector_grads], axis=1)
    if fast:
        input_grad, packed, joined_grad = end(input_grad, packed, joined_grad.astype(bf16))
    else:
        input_grad, joined_grad = from_own_seqs(input_grad), scatter(joined_grad)
        packed = scatter(packed.reshape(-1))
    own_grads, at = [], 0
    for item in vector_grads:
        size = item.shape[0] // devices
        own_grads.append(packed[at : at + size])
        at += size
    g1, s1, qb, vb, ob, g2, s2, cb, eb = own_grads
    return (
        layer_output,
        input_grad,
        g1,
        s1,
        joined_grad,
        qb,
        vb,
        output_weight_grad,
        ob,
        g2,
        s2,
        expand_grad,
        eb,
        contract_grad,
        cb,
    )


def solution(mesh):
    tokens = P(None, ("fs", "sp"), None)
    both, both_rows = P(("fs", "sp")), P(("fs", "sp"), None)
    one, one_rows = P("fs"), P("fs", None)
    return jax.shard_map(
        per_device,
        mesh=mesh,
        in_specs=(
            tokens, one, one, one_rows, one, one, one_rows, one, one, one, one_rows, one,
            one_rows, one, P(), tokens,
        ),
        out_specs=(
            tokens, tokens, both, both, both_rows, both, both, both_rows, both, both, both,
            both_rows, both, both_rows, both,
        ),
        check_vma=False,
    )
```

```python
import functools
import math

import jax
import jax.numpy as jnp
from jax import lax
from jax.experimental import pallas as pl
from jax.experimental.pallas import tpu as pltpu
from jax.sharding import PartitionSpec as P

norm_eps = 1e-05
gelu_coef = 0.7978845608028654
masked_value = -1e30
f32 = jnp.float32
bf16 = jnp.bfloat16
MESH = pl.DeviceIdType.MESH
HBM = pl.BlockSpec(memory_space=pl.ANY)
VMEM = pl.BlockSpec(memory_space=pltpu.VMEM)
SMEM = pl.BlockSpec(memory_space=pltpu.SMEM)
vmem_bytes = 63 * 1024 * 1024


def normalize(values, norm_gain, norm_shift):
    center = values - jnp.mean(values, axis=-1, keepdims=True)
    variance = jnp.mean(center * center, axis=-1, keepdims=True)
    return center * lax.rsqrt(variance + norm_eps) * norm_gain + norm_shift


def gelu_tanh(values):
    return (
        0.5 * values * (1.0 + jnp.tanh(gelu_coef * (values + 0.044715 * values * values * values)))
    )


def matmul(left_side, right_side):
    return jnp.dot(left_side, right_side, preferred_element_type=f32)


def matmul_lt(left_side, right_side):
    return lax.dot_general(
        left_side, right_side, (((0,), (0,)), ((), ())), preferred_element_type=f32
    )


def matmul_rt(left_side, right_side):
    return lax.dot_general(
        left_side, right_side, (((1,), (1,)), ((), ())), preferred_element_type=f32
    )


def joined_bias_of(query_bias, value_bias, head_count):
    query_part = query_bias.astype(f32).reshape(head_count, -1)
    value_part = value_bias.astype(f32).reshape(head_count, -1)
    return jnp.stack([query_part, jnp.zeros_like(query_part), value_part], axis=1).reshape(-1)


def split_three(values):
    high = values.astype(bf16).astype(f32)
    rest = values - high
    middle = rest.astype(bf16).astype(f32)
    return high, middle, rest - middle


def key_columns(key_rows, slope, start):
    rows, width = key_rows.shape
    position = (start + lax.broadcasted_iota(jnp.int32, (rows, width), 0)).astype(f32)
    lane = lax.broadcasted_iota(jnp.int32, (rows, width), 1)
    high, middle, low = split_three(slope * position)
    extra = jnp.where(lane == 0, high, jnp.where(lane == 1, middle, jnp.where(lane == 2, low, 0.0)))
    return jnp.concatenate([key_rows.astype(f32), extra], axis=1).astype(bf16)


def query_columns(queries, scale):
    rows, width = queries.shape
    lane = lax.broadcasted_iota(jnp.int32, (rows, width), 1)
    ones = jnp.where(lane < 3, 1.0, 0.0)
    return jnp.concatenate([queries.astype(f32) * scale, ones], axis=1).astype(bf16)


def follow(n, after):
    for at, steps in after.items():

        def act(steps=steps):
            for step, *given in steps:
                step(*given)

        pl.when(n == at)(act)


class Forward:
    def __init__(self, heads, width, slopes, qkv, out, out_t, lse, keys, queries, values_t):
        self.heads, self.width, self.slopes, self.qkv, self.out = heads, width, slopes, qkv, out
        self.out_t, self.lse = out_t, lse
        self.keys, self.queries, self.values_t = keys, queries, values_t
        self.blocks = qkv.shape[1]
        self.block = qkv.shape[2] * qkv.shape[3]

    def rows(self, i):
        return pl.ds(pl.multiple_of(i * self.block, self.block), self.block)

    def prepare(self, b):
        width, block, qkv = self.width, self.block, self.qkv
        scale = 1.0 / math.sqrt(width)

        def body(i, _):
            rows = self.rows(i)
            for h in range(self.heads):
                base = h * 3 * width
                query, key, value = [
                    qkv[b, i, :, :, base + n * width : base + (n + 1) * width].reshape(block, width)
                    for n in range(3)
                ]
                self.keys[h, rows, :] = key_columns(key, self.slopes[h], i * block)
                self.queries[h, rows, :] = query_columns(query, scale)
                self.values_t[h, :, rows] = value.astype(f32).T.astype(bf16)
            return 0

        lax.fori_loop(0, self.blocks, body, 0)

    def one(self, b, i):
        heads, width, block = self.heads, self.width, self.block
        rows = self.rows(i)
        query = [self.queries[h, rows, :] for h in range(heads)]

        def step(j, state, diagonal):
            columns = self.rows(j)
            result = []
            for h in range(heads):
                top, total, acc = state[h]
                scores = matmul_rt(self.keys[h, columns, :], query[h])
                if diagonal:
                    key_at = lax.broadcasted_iota(jnp.int32, (block, block), 0)
                    query_at = lax.broadcasted_iota(jnp.int32, (block, block), 1)
                    scores = jnp.where(key_at <= query_at, scores, masked_value)
                newest = jnp.maximum(top, jnp.max(scores, axis=0, keepdims=True))
                shrink = jnp.exp(top - newest)
                probs = jnp.exp(scores - newest)
                total = total * shrink + jnp.sum(probs, axis=0, keepdims=True)
                acc = acc * shrink + matmul(self.values_t[h, :, columns], probs.astype(bf16))
                result.append((newest, total, acc))
            return tuple(result)

        state = tuple(
            (
                jnp.full((1, block), masked_value, f32),
                jnp.zeros((1, block), f32),
                jnp.zeros((width, block), f32),
            )
            for h in range(heads)
        )
        state = lax.fori_loop(0, i, lambda j, s: step(j, s, False), state)
        state = step(i, state, True)
        finished = []
        for h in range(heads):
            top, total, acc = state[h]
            result = acc / total
            self.out_t[b, h, :, rows] = result
            self.lse[b, h, :, rows] = top + jnp.log(total)
            finished.append(result)
        joined = finished[0] if heads == 1 else jnp.concatenate(finished, axis=0)
        self.out[b, i] = joined.T.astype(bf16).reshape(self.out.shape[2:])

    def run(self, after, each=None):
        blocks = self.blocks

        def body(n, _):
            b, i = n // blocks, n % blocks
            pl.when(i == 0)(lambda: self.prepare(b))
            self.one(b, i)
            if each is not None:
                each(b, i)
            follow(n, after)
            return 0

        lax.fori_loop(0, self.qkv.shape[0] * blocks, body, 0)


def forward_kernel(heads, width, *refs):
    Forward(heads, width, *refs).run({})


def saved_shapes(seqs, length, heads, width):
    return (
        jax.ShapeDtypeStruct((seqs, heads, width, length), f32),
        jax.ShapeDtypeStruct((seqs, heads, 1, length), f32),
    )


def forward_scratch(length, heads, width):
    return [
        pltpu.VMEM((heads, length, 2 * width), bf16),
        pltpu.VMEM((heads, length, 2 * width), bf16),
        pltpu.VMEM((heads, width, length), bf16),
    ]


def attention_forward(qkv, slopes, heads, width):
    seqs, blocks, ranks, piece, _ = qkv.shape
    length = blocks * ranks * piece
    return pl.pallas_call(
        functools.partial(forward_kernel, heads, width),
        name="attention_forward",
        out_shape=(
            jax.ShapeDtypeStruct((seqs, blocks, ranks, piece, heads * width), bf16),
            *saved_shapes(seqs, length, heads, width),
        ),
        in_specs=[SMEM, VMEM],
        out_specs=(VMEM, VMEM, VMEM),
        scratch_shapes=forward_scratch(length, heads, width),
        compiler_params=pltpu.CompilerParams(vmem_limit_bytes=vmem_bytes),
    )(slopes, qkv)


class Backward:
    def __init__(
        self, heads, width, slopes, qkv, diff, out_t, lse, joined,
        keys, queries, keys_t, values, diffs, delta, query_acc,
    ):
        self.heads, self.width, self.slopes, self.qkv, self.diff = heads, width, slopes, qkv, diff
        self.out_t, self.lse, self.joined = out_t, lse, joined
        self.keys, self.queries, self.keys_t, self.values = keys, queries, keys_t, values
        self.diffs, self.delta, self.query_acc = diffs, delta, query_acc
        self.blocks = qkv.shape[1]
        self.block = qkv.shape[2] * qkv.shape[3]

    def rows(self, i):
        return pl.ds(pl.multiple_of(i * self.block, self.block), self.block)

    def prepare(self, b):
        width, block, qkv = self.width, self.block, self.qkv
        scale = 1.0 / math.sqrt(width)

        def body(i, _):
            rows = self.rows(i)
            for h in range(self.heads):
                base = h * 3 * width
                query, key, value = [
                    qkv[b, i, :, :, base + n * width : base + (n + 1) * width].reshape(block, width)
                    for n in range(3)
                ]
                self.keys[h, rows, :] = key_columns(key, self.slopes[h], i * block)
                self.keys_t[h, :, rows] = key.astype(f32).T.astype(bf16)
                self.queries[h, rows, :] = query_columns(query, scale)
                self.values[h, rows, :] = value
                part = self.diff[b, i, :, :, h * width : (h + 1) * width].reshape(block, width)
                self.diffs[h, rows, :] = part
                self.delta[h, :, rows] = jnp.sum(
                    part.astype(f32).T * self.out_t[b, h, :, rows], axis=0, keepdims=True
                )
                self.query_acc[h, :, rows] = jnp.zeros((width, block), f32)
            return 0

        lax.fori_loop(0, self.blocks, body, 0)

    def one(self, b, j):
        heads, width, block = self.heads, self.width, self.block
        tail = self.joined.shape[2:4] + (width,)
        columns = self.rows(j)

        def step(i, state, diagonal):
            rows = self.rows(i)
            result = []
            for h in range(heads):
                key_acc, value_acc = state[h]
                query = self.queries[h, rows, :]
                part = self.diffs[h, rows, :]
                scores = matmul_rt(self.keys[h, columns, :], query)
                probs = jnp.exp(scores - self.lse[b, h, :, rows])
                if diagonal:
                    key_at = lax.broadcasted_iota(jnp.int32, (block, block), 0)
                    query_at = lax.broadcasted_iota(jnp.int32, (block, block), 1)
                    probs = jnp.where(key_at <= query_at, probs, 0.0)
                prob_diff = matmul_rt(self.values[h, columns, :], part)
                score_diff = (probs * (prob_diff - self.delta[h, :, rows])).astype(bf16)
                value_acc = value_acc + matmul(probs.astype(bf16), part)
                key_acc = key_acc + matmul(score_diff, query)
                self.query_acc[h, :, rows] += matmul(self.keys_t[h, :, columns], score_diff)
                result.append((key_acc, value_acc))
            return tuple(result)

        state = tuple(
            (jnp.zeros((block, 2 * width), f32), jnp.zeros((block, width), f32))
            for h in range(heads)
        )
        state = step(j, state, True)
        state = lax.fori_loop(j + 1, self.blocks, lambda i, s: step(i, s, False), state)
        for h in range(heads):
            base = (h * 3 + 1) * width
            key_acc, value_acc = state[h]
            self.joined[b, j, :, :, base : base + width] = (
                key_acc[:, :width].astype(bf16).reshape(tail)
            )
            self.joined[b, j, :, :, base + width : base + 2 * width] = value_acc.astype(
                bf16
            ).reshape(tail)

    def run(self, after, each=None):
        blocks = self.blocks

        def body(n, _):
            b, j = n // blocks, n % blocks
            pl.when(j == 0)(lambda: self.prepare(b))
            self.one(b, j)
            self.finish(b, j)
            if each is not None:
                each(b, j)
            follow(n, after)
            return 0

        lax.fori_loop(0, self.qkv.shape[0] * blocks, body, 0)

    def finish(self, b, j):
        width = self.width
        scale = 1.0 / math.sqrt(width)
        for h in range(self.heads):
            base = h * 3 * width
            result = (self.query_acc[h, :, self.rows(j)] * scale).T.astype(bf16)
            self.joined[b, j, :, :, base : base + width] = result.reshape(
                self.joined.shape[2:4] + (width,)
            )


def backward_kernel(heads, width, *refs):
    Backward(heads, width, *refs).run({})


def backward_scratch(length, heads, width):
    return [
        pltpu.VMEM((heads, length, 2 * width), bf16),
        pltpu.VMEM((heads, length, 2 * width), bf16),
        pltpu.VMEM((heads, width, length), bf16),
        pltpu.VMEM((heads, length, width), bf16),
        pltpu.VMEM((heads, length, width), bf16),
        pltpu.VMEM((heads, 1, length), f32),
        pltpu.VMEM((heads, width, length), f32),
    ]


def attention_backward(qkv, diff, out_t, lse, slopes, heads, width):
    length = qkv.shape[1] * qkv.shape[2] * qkv.shape[3]
    return pl.pallas_call(
        functools.partial(backward_kernel, heads, width),
        name="attention_backward",
        out_shape=jax.ShapeDtypeStruct(qkv.shape, bf16),
        in_specs=[SMEM, VMEM, VMEM, VMEM, VMEM],
        out_specs=VMEM,
        scratch_shapes=backward_scratch(length, heads, width),
        compiler_params=pltpu.CompilerParams(vmem_limit_bytes=vmem_bytes),
    )(slopes, qkv, diff, out_t, lse)


def to_own_seqs(values):
    seqs, piece, features = values.shape
    parts = lax.axis_size("fs")
    values = values.reshape(parts, seqs // parts, piece, features)
    return lax.all_to_all(values, "fs", split_axis=0, concat_axis=0).transpose(1, 0, 2, 3)


def from_own_seqs(values):
    own, parts, piece, features = values.shape
    values = lax.all_to_all(values.transpose(1, 0, 2, 3), "fs", split_axis=0, concat_axis=0)
    return values.reshape(parts * own, piece, features)


def to_heads(values):
    own, parts, piece, features = values.shape
    ranks = lax.axis_size("sp")
    values = values.reshape(own, parts, piece, ranks, features // ranks)
    return lax.all_to_all(values, "sp", split_axis=3, concat_axis=2)


def from_heads(values):
    own, parts, ranks, piece, features = values.shape
    values = lax.all_to_all(values, "sp", split_axis=2, concat_axis=3)
    return values.reshape(own, parts, piece, ranks * features)


class Copies:
    def __init__(self, send, recv, local):
        self.send, self.recv, self.local = send, recv, local
        self.used, self.used_local, self.made = 0, 0, []

    def plan(self, source, target, device):
        copy = pltpu.make_async_remote_copy(
            src_ref=source,
            dst_ref=target,
            send_sem=self.send.at[self.used],
            recv_sem=self.recv.at[self.used],
            device_id=device,
            device_id_type=MESH,
        )
        self.used += 1
        self.made.append(copy)
        return copy

    def inside(self, source, target):
        copy = pltpu.make_async_copy(source, target, self.local.at[self.used_local])
        self.used_local += 1
        return copy

    def finish(self):
        assert (self.used, self.used_local) == (self.send.shape[0], self.local.shape[0])
        for copy in self.made:
            copy.wait_send()


def go(copies):
    for copy in copies:
        copy.start()


def arrive(copies):
    for copy in copies:
        copy.wait_recv()


def done(copies):
    for copy in copies:
        copy.wait()


def greet(devices):
    barrier = pltpu.get_barrier_semaphore()
    for device in devices:
        pl.semaphore_signal(barrier, inc=1, device_id=device, device_id_type=MESH)
    pl.semaphore_wait(barrier, len(devices))


class Place:
    def __init__(self):
        z, s = lax.axis_index("fs"), lax.axis_index("sp")
        self.z, self.s = z, s
        self.core, self.chip = s % 2, s // 2
        self.x, self.y = self.chip % 2, self.chip // 2
        self.along_x = s + 2 - 4 * self.x
        self.along_y = s + 4 - 8 * self.y
        self.partner = s + 1 - 2 * self.core
        self.diagonal = self.along_x + self.along_y - s
        self.chip_x, self.chip_y = self.along_x // 2, self.along_y // 2
        self.lines = [(lax.rem(z + k, 4), s) for k in range(1, 4)]
        self.plane = [(z, lax.rem(s + d, 8)) for d in range(1, 8)]
        self.to_x, self.to_y, self.to_core = [
            (z, to) for to in (self.along_x, self.along_y, self.partner)
        ]
        self.near = self.lines + [self.to_x, self.to_y, self.to_core]


class Gather:
    copies_each = 33

    def __init__(self, place, weights, wholes, kept, chunks, copies, given=None):
        z, s, lines = place.z, place.s, place.lines
        self.ready = arrive if given is None else done
        self.loads, self.own = [], []
        for weight, whole, keep in zip(weights, wholes, kept):
            if keep is None:
                self.loads.append(copies.inside(weight, whole.at[z]))
            else:
                self.loads.append(copies.inside(weight, keep))
                self.own.append(copies.inside(keep, whole.at[z]))
        self.first, self.second, self.third, self.cores, self.last = [], [], [], [], []
        for t, row, rows, column, columns in chunks:
            whole = wholes[t]
            wide = pl.ds(column, columns)
            every = pl.ds(row, rows)
            low, high = pl.ds(row, rows // 2), pl.ds(row + rows // 2, rows // 2)

            def same(k, rank, part, to):
                where = (k, rank, part, wide)
                return copies.plan(whole.at[where], whole.at[where], to)

            if given is None:
                first = [
                    copies.plan(weights[t].at[s, every, wide], whole.at[z, s, every, wide], to)
                    for to in lines
                ]
            else:
                first = [
                    copies.inside(given.at[k, every, wide], whole.at[k, s, every, wide])
                    for k, _ in lines
                ]
            self.first.append(first)
            second, third, cores, last = [], [], [], []
            for k, _ in lines:
                second.append(same(k, s, low, place.to_x))
                second.append(same(k, s, high, place.to_y))
                cores.append(same(k, s, every, place.to_core))
                third.append(same(k, s, low, place.to_y))
                third.append(same(k, s, high, place.to_x))
                third.append(same(k, place.along_x, low, place.to_y))
                third.append(same(k, place.along_y, high, place.to_x))
                for rank in (place.along_x, place.along_y, place.diagonal):
                    last.append(same(k, rank, every, place.to_core))
            self.second.append(second)
            self.third.append(third)
            self.cores.append(cores)
            self.last.append(last)

    def keep(self):
        done(self.loads)
        go(self.own)

    def start(self, t):
        go(self.first[t])

    def exchange(self, t):
        self.ready(self.first[t])
        go(self.second[t])
        go(self.cores[t])

    def spread(self, t):
        arrive(self.second[t])
        go(self.third[t])

    def share(self, t):
        arrive(self.third[t])
        go(self.last[t])

    def complete(self, t):
        arrive(self.cores[t] + self.last[t])


def add_into(target, other):
    target[...] = (target[...].astype(f32) + other[...].astype(f32)).astype(target.dtype)


def add_blocks(steps, block_of):
    def body(i, _):
        add_into(*block_of(i))
        return 0

    lax.fori_loop(0, steps, body, 0)


class Reduce:
    copies_each = 10

    def __init__(self, place, grads, outs, bufs, chunks, copies):
        self.place, self.outs, self.chunks = place, outs, chunks
        self.bufs = [bufs[7 * t : 7 * t + 7] for t in range(len(chunks))]
        self.loads, self.first, self.second, self.third, self.fourth = [], [], [], [], []
        for (t, row, rows, column, columns), buf in zip(chunks, self.bufs):
            own, from_core, from_x, from_y, late_y, late_x, from_z = buf
            every, wide = pl.ds(row, rows), pl.ds(column, columns)
            low, high = pl.ds(0, rows // 2), pl.ds(rows // 2, rows // 2)
            self.loads.append(
                copies.inside(grads[t].at[:, :, place.core, every, wide], own)
            )
            self.first.append(
                copies.plan(
                    grads[t].at[:, :, 1 - place.core, every, wide], from_core, place.to_core
                )
            )
            step = []
            for k in range(2):
                step.append(
                    copies.plan(own.at[:, 2 * k + 1 - place.x, low], from_x.at[:, k], place.to_x)
                )
                step.append(
                    copies.plan(
                        own.at[:, 2 * (1 - place.y) + k, high], from_y.at[:, k], place.to_y
                    )
                )
            self.second.append(step)
            self.third.append(
                [
                    copies.plan(own.at[:, place.chip_y, low], late_y, place.to_y),
                    copies.plan(own.at[:, place.chip_x, high], late_x, place.to_x),
                ]
            )
            self.fourth.append(
                [
                    copies.plan(own.at[to[0], place.chip], from_z.at[k], to)
                    for k, to in enumerate(place.lines)
                ]
            )

    def start(self):
        go(self.first)

    def halves(self, t):
        half = self.chunks[t][2] // 2
        return pl.ds(0, half), pl.ds(half, half)

    def exchange(self, t):
        own, from_core = self.bufs[t][:2]
        self.loads[t].wait()
        arrive([self.first[t]])
        add_blocks(16, lambda i: (own.at[i // 4, i % 4], from_core.at[i // 4, i % 4]))
        go(self.second[t])

    def spread(self, t):
        own, _, from_x, from_y = self.bufs[t][:4]
        low, high = self.halves(t)
        x, y = self.place.x, self.place.y
        arrive(self.second[t])
        add_blocks(8, lambda i: (own.at[i // 2, 2 * (i % 2) + x, low], from_x.at[i // 2, i % 2]))
        add_blocks(8, lambda i: (own.at[i // 2, 2 * y + i % 2, high], from_y.at[i // 2, i % 2]))
        go(self.third[t])

    def send(self, t):
        own, _, _, _, late_y, late_x, _ = self.bufs[t]
        low, high = self.halves(t)
        chip = self.place.chip
        arrive(self.third[t])
        add_blocks(4, lambda i: (own.at[i, chip, low], late_y.at[i]))
        add_blocks(4, lambda i: (own.at[i, chip, high], late_x.at[i]))
        go(self.fourth[t])

    def finish(self, t):
        own, from_z = self.bufs[t][0], self.bufs[t][6]
        index, row, rows, column, columns = self.chunks[t]
        arrive(self.fourth[t])
        total = own[self.place.z, self.place.chip].astype(f32)
        for k in range(3):
            total = total + from_z[k].astype(f32)
        self.outs[index][row : row + rows, column : column + columns] = total


def reduce_scratch(chunks):
    scratch = []
    for _, _, rows, _, columns in chunks:
        half = rows // 2
        scratch += [
            pltpu.VMEM((4, 4, rows, columns), bf16),
            pltpu.VMEM((4, 4, rows, columns), bf16),
            pltpu.VMEM((4, 2, half, columns), bf16),
            pltpu.VMEM((4, 2, half, columns), bf16),
            pltpu.VMEM((4, half, columns), bf16),
            pltpu.VMEM((4, half, columns), bf16),
            pltpu.VMEM((3, rows, columns), bf16),
        ]
    return scratch


class ReduceAlong(Reduce):
    def __init__(self, place, grad, out, buf, chunk, copies):
        self.place, self.grad, self.out, self.buf, self.chunk = place, grad, out, buf, chunk
        own, from_core, from_z, from_x, from_y, late_y, late_x = buf
        _, row, rows, column, columns = chunk
        every, wide = pl.ds(row, rows), pl.ds(column, columns)
        self.low, self.high = low, high = pl.ds(0, rows // 2), pl.ds(rows // 2, rows // 2)
        z, x, y = place.z, place.x, place.y
        self.load = copies.inside(grad.at[:, :, place.core, every, wide], own)
        self.first = copies.plan(
            grad.at[:, :, 1 - place.core, every, wide], from_core, place.to_core
        )
        self.second = [
            copies.plan(own.at[to[0]], from_z.at[k], to) for k, to in enumerate(place.lines)
        ]
        self.third = []
        for k in range(2):
            self.third.append(
                copies.plan(own.at[z, 2 * k + 1 - x, low], from_x.at[k], place.to_x)
            )
            self.third.append(
                copies.plan(own.at[z, 2 * (1 - y) + k, high], from_y.at[k], place.to_y)
            )
        self.fourth = [
            copies.plan(own.at[z, place.chip_y, low], late_y, place.to_y),
            copies.plan(own.at[z, place.chip_x, high], late_x, place.to_x),
        ]

    def exchange(self):
        own, from_core = self.buf[:2]
        self.load.wait()
        arrive([self.first])
        add_blocks(16, lambda i: (own.at[i // 4, i % 4], from_core.at[i // 4, i % 4]))
        go(self.second)

    def spread(self):
        own, _, from_z = self.buf[:3]
        z = self.place.z
        arrive(self.second)

        def body(i, _):
            total = own[z, i].astype(f32)
            for k in range(3):
                total = total + from_z[k, i].astype(f32)
            own[z, i] = total.astype(bf16)
            return 0

        lax.fori_loop(0, 4, body, 0)
        go(self.third)

    def send(self):
        own, _, _, from_x, from_y = self.buf[:5]
        z, x, y = self.place.z, self.place.x, self.place.y
        arrive(self.third)
        add_blocks(2, lambda j: (own.at[z, 2 * j + x, self.low], from_x.at[j]))
        add_blocks(2, lambda j: (own.at[z, 2 * y + j, self.high], from_y.at[j]))
        go(self.fourth)

    def finish(self):
        own, late_y, late_x = self.buf[0], self.buf[5], self.buf[6]
        z, chip = self.place.z, self.place.chip
        _, row, rows, column, columns = self.chunk
        arrive(self.fourth)
        half = rows // 2
        wide = slice(column, column + columns)
        self.out[row : row + half, wide] = own[z, chip, self.low].astype(f32) + late_y[...].astype(
            f32
        )
        self.out[row + half : row + rows, wide] = own[z, chip, self.high].astype(f32) + late_x[
            ...
        ].astype(f32)


def reduce_along_scratch(chunk):
    _, _, rows, _, columns = chunk
    half = rows // 2
    return [
        pltpu.VMEM((4, 4, rows, columns), bf16),
        pltpu.VMEM((4, 4, rows, columns), bf16),
        pltpu.VMEM((3, 4, rows, columns), bf16),
        pltpu.VMEM((2, half, columns), bf16),
        pltpu.VMEM((2, half, columns), bf16),
        pltpu.VMEM((half, columns), bf16),
        pltpu.VMEM((half, columns), bf16),
    ]


class HandBack:
    def __init__(self, place, source, target, features, send, recv, local):
        self.place, self.source, self.target = place, source, target
        self.mine = columns_of(place.s, features)
        self.send, self.recv, self.local = send, recv, local
        self.blocks = source.shape[1]

    def copy(self, b, i, d):
        rank = self.place.plane[d][1]
        n = b * self.blocks + i
        return pltpu.make_async_remote_copy(
            src_ref=self.source.at[b, i, rank],
            dst_ref=self.target.at[b, i, :, self.mine],
            send_sem=self.send.at[n, d],
            recv_sem=self.recv.at[n, d],
            device_id=self.place.plane[d],
            device_id_type=MESH,
        )

    def own(self, b, i):
        return pltpu.make_async_copy(
            self.source.at[b, i, self.place.s],
            self.target.at[b, i, :, self.mine],
            self.local.at[b * self.blocks + i],
        )

    def each(self, b, i):
        for d in range(7):
            self.copy(b, i, d).start()
        self.own(b, i).start()

    def finish(self):
        def body(n, _):
            b, i = n // self.blocks, n % self.blocks
            for d in range(7):
                self.copy(b, i, d).wait()
            self.own(b, i).wait()
            return 0

        lax.fori_loop(0, self.source.shape[0] * self.blocks, body, 0)


def hand_back_semaphores(steps):
    return [
        pltpu.SemaphoreType.DMA((steps, 7)),
        pltpu.SemaphoreType.DMA((steps, 7)),
        pltpu.SemaphoreType.DMA((steps,)),
    ]


class ReduceLines:
    copies = 4 * 7 + 3

    def __init__(self, place, grad, out, bufs, copies):
        self.place, self.grad, self.out, self.bufs = place, grad, out, bufs
        from_core, from_x, from_y, late_y, late_x, from_z = bufs
        core, x, y = place.core, place.x, place.y
        self.order = [to[0] for to in place.lines] + [place.z]
        rows = grad.shape[3]
        self.low, self.high = pl.ds(0, rows // 2), pl.ds(rows // 2, rows // 2)
        self.first, self.second, self.third, self.fourth = [], [], [], []
        for k, at in enumerate(self.order):
            self.first.append(
                copies.plan(grad.at[at, :, 1 - core], from_core.at[k], place.to_core)
            )
            step = []
            for j in range(2):
                step.append(
                    copies.plan(
                        grad.at[at, 2 * j + 1 - x, core, self.low], from_x.at[k, j], place.to_x
                    )
                )
                step.append(
                    copies.plan(
                        grad.at[at, 2 * (1 - y) + j, core, self.high], from_y.at[k, j], place.to_y
                    )
                )
            self.second.append(step)
            self.third.append(
                [
                    copies.plan(grad.at[at, place.chip_y, core, self.low], late_y.at[k], place.to_y),
                    copies.plan(
                        grad.at[at, place.chip_x, core, self.high], late_x.at[k], place.to_x
                    ),
                ]
            )
            if k < 3:
                self.fourth.append(
                    copies.plan(grad.at[at, place.chip, core], from_z.at[k], place.lines[k])
                )

    def start(self, k):
        go([self.first[k]])

    def exchange(self, k):
        arrive([self.first[k]])
        at, core = self.order[k], self.place.core
        add_blocks(4, lambda i: (self.grad.at[at, i, core], self.bufs[0].at[k, i]))
        go(self.second[k])

    def spread(self, k):
        arrive(self.second[k])
        at, core, x, y = self.order[k], self.place.core, self.place.x, self.place.y
        add_blocks(
            2, lambda j: (self.grad.at[at, 2 * j + x, core, self.low], self.bufs[1].at[k, j])
        )
        add_blocks(
            2, lambda j: (self.grad.at[at, 2 * y + j, core, self.high], self.bufs[2].at[k, j])
        )
        go(self.third[k])

    def send(self, k):
        arrive(self.third[k])
        at, core, chip = self.order[k], self.place.core, self.place.chip
        add_into(self.grad.at[at, chip, core, self.low], self.bufs[3].at[k])
        add_into(self.grad.at[at, chip, core, self.high], self.bufs[4].at[k])
        go(self.fourth[k : k + 1])

    def finish(self):
        arrive(self.fourth)
        place = self.place
        total = self.grad[place.z, place.chip, place.core].astype(f32)
        for k in range(3):
            total = total + self.bufs[5][k].astype(f32)
        self.out[...] = total


def reduce_lines_scratch(rows, columns):
    half = rows // 2
    return [
        pltpu.VMEM((4, 4, rows, columns), bf16),
        pltpu.VMEM((4, 2, half, columns), bf16),
        pltpu.VMEM((4, 2, half, columns), bf16),
        pltpu.VMEM((4, half, columns), bf16),
        pltpu.VMEM((4, half, columns), bf16),
        pltpu.VMEM((3, rows, columns), bf16),
    ]


def split_grad(item):
    return item.reshape(4, 4, 2, item.shape[0] // 32, item.shape[1])


def split_weight(item):
    return item.reshape(8, item.shape[0] // 8, item.shape[1])


def chunks_of(index, rows, columns, count):
    if rows >= 64:
        return [(index, rows // count * n, rows // count, 0, columns) for n in range(count)]
    return [(index, 0, rows, columns // count * n, columns // count) for n in range(count)]


def semaphores(remote, local):
    return [pltpu.SemaphoreType.DMA((n,)) for n in (remote, remote, local)]


def remote_call(kernel, name, collective, **options):
    return pl.pallas_call(
        kernel,
        name=name,
        compiler_params=pltpu.CompilerParams(
            collective_id=collective, has_side_effects=True, vmem_limit_bytes=vmem_bytes
        ),
        **options,
    )


def columns_of(rank, features):
    return pl.ds(pl.multiple_of(rank * features, 128), features)


def forward_fused_kernel(heads, width, count, vector_count, chunks, slopes, tokens, upstream, *refs):
    vectors, refs = refs[:vector_count], refs[vector_count:]
    weights, contract, refs = refs[:count], refs[count], refs[count + 1 :]
    tokens_out, vectors_out, joined_out, qkv_out, attended, out_t, lse, upstream_out = refs[:8]
    contract_out = refs[8]
    wholes, refs = refs[9 : 8 + count], refs[8 + count :]
    held, small, values_of, joined, normed, outgoing, qkv, result, upstream_own = refs[:9]
    attention = Forward(heads, width, slopes, qkv, result, out_t, lse, *refs[9:12])
    kept, refs = refs[12 : 11 + count], refs[11 + count :]
    head_send, head_recv = refs[:2]
    copies = Copies(*refs[5:])
    place = Place()
    z, s, lines, plane = place.z, place.s, place.lines, place.plane
    gather = Gather(place, weights, [joined, *wholes], [None, *kept], chunks, copies)
    first = [t for t, chunk in enumerate(chunks) if chunk[0] == 0]
    later = [t for t, chunk in enumerate(chunks) if chunk[0] > 0]
    features = heads * width
    back = HandBack(place, result, attended, features, *refs[2:5])
    own_seqs, parts, piece, wide = held.shape

    load = copies.inside(tokens.at[z], held.at[:, z])
    load_upstream = copies.inside(upstream.at[z], upstream_own)
    seqs = [copies.plan(tokens.at[to[0]], held.at[:, z], to) for to in lines]
    vector_copies = [copies.plan(small.at[z], small.at[z], to) for to in lines]
    upstreams = [copies.plan(upstream.at[to[0]], upstream_out.at[:, z], to) for to in lines]
    keep_upstream = copies.inside(upstream_own, upstream_out.at[:, z])
    keeping = [
        copies.inside(held, tokens_out),
        copies.inside(small, vectors_out),
        copies.inside(joined, joined_out),
    ]
    keep_qkv = copies.inside(qkv, qkv_out)
    contracts = [copies.plan(contract.at[s], contract_out.at[z], to) for to in lines]

    def to_head(d):
        return pltpu.make_async_remote_copy(
            src_ref=outgoing.at[d],
            dst_ref=qkv.at[:, :, s],
            send_sem=head_send.at[d],
            recv_sem=head_recv.at[d],
            device_id=(z, lax.rem(s + 1 + d, 8)),
            device_id_type=MESH,
        )

    go(gather.loads + [load, load_upstream])
    small[z] = jnp.zeros(small.shape[1:], bf16)
    for n, item in enumerate(vectors):
        small[z, n, : item.shape[0], :] = item[...]
    greet(lines + plane)
    for t in first:
        gather.start(t)
    go(seqs + vector_copies)
    gather.keep()
    load.wait()
    for t in range(len(first) + 2):
        if t < len(first):
            gather.exchange(t)
        if 0 <= t - 1 < len(first):
            gather.spread(t - 1)
        if 0 <= t - 2:
            gather.share(t - 2)
    load_upstream.wait()
    keep_upstream.start()
    arrive(seqs + vector_copies)
    for t in later:
        gather.start(t)
    values_of[...] = small[...].astype(f32)

    def row_of(n):
        found = [values_of[k, n, r : r + 1, :] for k in range(4) for r in range(wide // 512)]
        return jnp.concatenate(found, axis=1)

    gain, shift = row_of(0), row_of(1)

    def norm(i, _):
        values = held[i // parts, i % parts].astype(f32)
        rows = pl.ds(pl.multiple_of(i * piece, piece), piece)
        normed[rows, :] = normalize(values, gain, shift).astype(bf16)
        return 0

    lax.fori_loop(0, own_seqs * parts, norm, 0)
    for t in first:
        gather.complete(t)
    go(keeping)

    def project(d, _):
        rank = lax.rem(s + 1 + d, 8)
        per = 8 // 4
        query_bias = values_of[rank // per, 2, pl.ds(rank % per, 1), :]
        value_bias = values_of[rank // per, 3, pl.ds(rank % per, 1), :]
        low = lax.broadcasted_iota(jnp.int32, query_bias.shape, 1) < width
        bias = jnp.concatenate(
            [
                jnp.where(low, query_bias, 0.0),
                jnp.where(low, value_bias, query_bias),
                jnp.where(low, 0.0, value_bias),
            ],
            axis=1,
        )
        weight = joined[:, :, :, columns_of(rank, 3 * features)].reshape(wide, 3 * features)
        made = (matmul(normed[...], weight) + bias).astype(bf16)
        outgoing[d] = made.reshape(outgoing.shape[1:])
        pl.when(d < 7)(lambda: to_head(d).start())
        return 0

    lax.fori_loop(0, 8, project, 0)
    own_copy = copies.inside(outgoing.at[7], qkv.at[:, :, s])
    own_copy.start()
    base = later[0]
    gather.exchange(base)
    gather.exchange(base + 1)
    own_copy.wait()
    gather.spread(base)
    for d in range(7):
        to_head(d).wait_recv()
    keep_qkv.start()
    attention.run(
        {
            0: [(gather.exchange, base + 2), (go, contracts), (gather.spread, base + 1)],
            2: [(gather.spread, base + 2), (gather.share, base)],
            3: [(go, upstreams)],
            5: [(gather.share, base + 1)],
            6: [(gather.share, base + 2)],
        },
        back.each,
    )
    for t in later:
        gather.complete(t)
    arrive(contracts + upstreams)
    back.finish()
    for d in range(7):
        to_head(d).wait_send()
    copies.finish()
    done(gather.own + [keep_upstream, keep_qkv] + keeping)


def forward_fused(tokens, upstream, vectors, weights, contract, slopes, heads, width):
    seqs, piece, features = tokens.shape
    parts = 4
    own = seqs // parts
    columns = heads * width
    length = parts * 8 * piece
    vectors = [item.reshape(-1, 128) for item in vectors]
    cut = [split_weight(item) for item in weights]
    contract = split_weight(contract)
    count, tall = len(cut), 8 * -(-max(item.shape[0] for item in vectors) // 8)
    chunks = []
    for t, pieces in enumerate((3, 1, 2)):
        chunks += chunks_of(t, *cut[t].shape[1:], pieces)
    seq_shape = (own, parts, piece, features)
    qkv_shape = (own, parts, 8, piece, 3 * columns)
    small = (parts, len(vectors), tall, 128)
    out = remote_call(
        functools.partial(forward_fused_kernel, heads, width, count, len(vectors), chunks),
        "forward_fused",
        1,
        out_shape=(
            jax.ShapeDtypeStruct(seq_shape, bf16),
            jax.ShapeDtypeStruct(small, bf16),
            jax.ShapeDtypeStruct((parts, *cut[0].shape), bf16),
            jax.ShapeDtypeStruct(qkv_shape, bf16),
            jax.ShapeDtypeStruct(seq_shape, bf16),
            *saved_shapes(own, length, heads, width),
            jax.ShapeDtypeStruct(seq_shape, bf16),
            jax.ShapeDtypeStruct((parts, *contract.shape[1:]), bf16),
            *[jax.ShapeDtypeStruct((parts, *item.shape), bf16) for item in cut[1:]],
        ),
        in_specs=[SMEM, HBM, HBM] + [VMEM] * len(vectors) + [HBM] * (count + 1),
        out_specs=(HBM,) * 5 + (VMEM, VMEM) + (HBM,) * (count + 1),
        scratch_shapes=[
            pltpu.VMEM(seq_shape, bf16),
            pltpu.VMEM(small, bf16),
            pltpu.VMEM(small, f32),
            pltpu.VMEM((parts, *cut[0].shape), bf16),
            pltpu.VMEM((own * parts * piece, features), bf16),
            pltpu.VMEM((8, own, parts, piece, 3 * columns), bf16),
            pltpu.VMEM(qkv_shape, bf16),
            pltpu.VMEM((own, parts, 8, piece, columns), bf16),
            pltpu.VMEM((own, piece, features), bf16),
            *forward_scratch(length, heads, width),
            *[pltpu.VMEM(item.shape, bf16) for item in cut[1:]],
            pltpu.SemaphoreType.DMA((7,)),
            pltpu.SemaphoreType.DMA((7,)),
            *hand_back_semaphores(own * parts),
            *semaphores(12 + len(chunks) * Gather.copies_each, 2 * count - 1 + 8),
        ],
    )(
        slopes,
        tokens.reshape(parts, own, piece, features),
        upstream.reshape(parts, own, piece, features),
        *vectors,
        *cut,
        contract,
    )
    wholes = [
        whole.reshape(4 * item.shape[0], item.shape[1])
        for whole, item in zip((out[2], *out[9:]), weights)
    ]
    found = [out[1][:, n, : item.shape[0]].reshape(-1) for n, item in enumerate(vectors)]
    return out[0], found, [*wholes, out[8]], out[3], out[4], (out[5], out[6]), out[7]


def feed_forward_kernel(
    chunks, expand, contract, contract_line, out_weight,
    expand_bias, upstream, tokens, attended, out_bias, gain, shift, contract_bias,
    layer, residual_grad, attended_diff, expand_grad, out_grad, contract_grad,
    bias_grad, gain_grad, shift_grad, out_bias_grad,
    expand_in, contract_in, residual, second, second_t, expanded, activated, grad, staged, *refs,
):
    second_back = residual_grad
    bufs, refs = refs[:6], refs[6:]
    loaded, stored, refs = refs[0], refs[1], refs[2:]
    copies = Copies(*refs)
    place = Place()
    z = place.z
    reduce = ReduceLines(place, grad, contract_grad, bufs, copies)
    gather = Gather(
        place, [contract], [contract_in], [None], chunks, copies, given=contract_line
    )
    rows, features = second.shape
    steps = 8
    wide = expand.shape[1] // steps

    def at(n):
        part = (z + 1 + n // 2) % 4
        return part, n % 2, pl.ds(pl.multiple_of((2 * part + n % 2) * wide, wide), wide)

    def load(n):
        _, _, where = at(n)
        return pltpu.make_async_copy(expand.at[:, where], expand_in.at[:, where], loaded.at[n])

    def contract_at(n):
        part, side, _ = at(n)
        return contract_in[part, pl.ds(4 * side, 4)].reshape(wide, features)

    def store(n):
        _, _, where = at(n)
        slot = n % 2
        return pltpu.make_async_copy(
            staged.at[slot], expand_grad.at[:, where], stored.at[slot]
        )

    halves = [pl.ds(0, wide), pl.ds(wide, wide)]
    out_loads = [
        pltpu.make_async_copy(out_weight.at[:, half], staged.at[n], stored.at[n])
        for n, half in enumerate(halves)
    ]
    out_stores = [
        pltpu.make_async_copy(staged.at[n], out_grad.at[:, half], stored.at[n])
        for n, half in enumerate(halves)
    ]
    part_rows = rows // 8

    def rows_at(i):
        return pl.ds(pl.multiple_of(i * part_rows, part_rows), part_rows)

    for n in range(len(chunks)):
        gather.start(n)
    go(out_loads)
    for n in range(steps):
        load(n).start()
    go(gather.loads)
    greet(place.near)
    for n in range(len(chunks)):
        gather.exchange(n)
    for n, half in enumerate(halves):
        out_loads[n].wait()
        residual[:, half] = (
            tokens[:, half].astype(f32) + (matmul(attended[...], staged[n]) + out_bias[:, half])
        )

    def norm(i, _):
        values = residual[rows_at(i), :]
        second[rows_at(i), :] = normalize(values, gain[...], shift[...]).astype(bf16)
        second_back[rows_at(i), :] = values + contract_bias[...]
        return 0

    lax.fori_loop(0, 8, norm, 0)
    for n in range(len(chunks) - 1):
        gather.spread(n)
    second_t[...] = second[...].T

    def forward(n, after):
        part, side, where = at(n)
        load(n).wait()
        values = matmul(second[...], expand_in[:, where]) + expand_bias[:, where]
        expanded[:, where] = values
        low = gelu_tanh(values).astype(bf16)
        activated[:, where] = low
        made = matmul(low.T, upstream[...]).astype(bf16)
        grad[part, pl.ds(2 * side, 2)] = made.reshape(2, 2, wide // 4, features)
        follow(n, after)
        return 0

    def shrink(n, after):
        _, _, where = at(n)
        second_back[...] += matmul(activated[:, where], contract_at(n))
        follow(n, after)
        return 0

    def backward(n, after):
        _, _, where = at(n)
        values = expanded[:, where]
        act_grad = matmul_rt(upstream[...], contract_at(n))
        bent = jnp.tanh(gelu_coef * (values + 0.044715 * values * values * values))
        slope = 0.5 * (1.0 + bent) + 0.5 * values * (1.0 - bent * bent) * (
            gelu_coef * (1.0 + 3.0 * 0.044715 * values * values)
        )
        diff = (act_grad * slope).astype(bf16)
        bias_grad[:, where] = jnp.sum(diff.astype(f32), axis=0, keepdims=True)
        pl.when(n >= 2)(lambda: store(n - 2).wait())
        staged[n % 2] = matmul(second_t[...], diff).astype(bf16)
        store(n).start()
        second_back[...] += matmul_rt(diff, expand_in[:, where])
        follow(n, after)
        return 0

    last = len(chunks) - 1
    forward_steps = {
        0: [(gather.spread, last)],
        1: [(reduce.start, 0)],
        3: [(reduce.exchange, 0), (reduce.start, 1)],
        5: [(reduce.start, 2), (reduce.exchange, 1)],
        7: [(reduce.start, 3), (reduce.exchange, 2)] + [(gather.share, n) for n in range(last)],
    }
    shrink_steps = {
        1: [(reduce.exchange, 3)],
        3: [(reduce.spread, 0)],
        7: [(reduce.spread, 1)],
    }
    backward_steps = {
        1: [(reduce.spread, 2)],
        2: [(reduce.spread, 3)],
        3: [(reduce.send, 0)],
        4: [(reduce.send, 1)],
        5: [(reduce.send, 2)],
        6: [(reduce.send, 3)],
    }
    lax.fori_loop(0, steps, lambda n, _: forward(n, forward_steps), 0)
    gather.share(last)
    for n in range(len(chunks)):
        gather.complete(n)
    done(gather.loads)
    lax.fori_loop(0, steps, lambda n, _: shrink(n, shrink_steps), 0)
    layer[...] = second_back[...].astype(bf16).reshape(layer.shape)
    second_back[...] = jnp.zeros_like(second_back)
    lax.fori_loop(0, steps, lambda n, _: backward(n, backward_steps), 0)
    store(steps - 2).wait()
    store(steps - 1).wait()
    go(out_loads)
    second_t[...] = attended[...].T

    def norm_back(i, sums):
        values, back = residual[rows_at(i), :], second_back[rows_at(i), :]
        center = values - jnp.mean(values, axis=-1, keepdims=True)
        inverse = lax.rsqrt(jnp.mean(center * center, axis=-1, keepdims=True) + norm_eps)
        normal = center * inverse
        scaled = back * gain[...]
        even = jnp.mean(scaled, axis=-1, keepdims=True)
        along = jnp.mean(scaled * normal, axis=-1, keepdims=True)
        total = upstream[rows_at(i), :].astype(f32) + inverse * (scaled - even - normal * along)
        low = total.astype(bf16)
        residual_grad[rows_at(i), :] = total
        second[rows_at(i), :] = low
        found = (back * normal, back, low.astype(f32))
        return tuple(
            kept + jnp.sum(item, axis=0, keepdims=True) for kept, item in zip(sums, found)
        )

    nothing = jnp.zeros((1, features), f32)
    sums = lax.fori_loop(0, 8, norm_back, (nothing, nothing, nothing))
    gain_grad[...], shift_grad[...], out_bias_grad[...] = sums
    done(out_loads)
    branch_diff = second
    made = matmul_rt(branch_diff[:, halves[0]], staged[0])
    made = (made + matmul_rt(branch_diff[:, halves[1]], staged[1])).astype(bf16)
    attended_diff[...] = made.reshape(attended_diff.shape)
    for n, half in enumerate(halves):
        staged[n] = matmul(second_t[...], branch_diff[:, half]).astype(bf16)
        out_stores[n].start()
    reduce.finish()
    done(out_stores)
    copies.finish()


def feed_forward(shape, expand, contract, line, out_weight, tokens, upstream, attended, vectors):
    own, parts, piece = shape
    rows, features = tokens.shape
    hidden = expand.shape[1]
    wide = hidden // 8
    each = hidden // 32
    contract = split_weight(contract)
    chunks = chunks_of(0, *contract.shape[1:], 2)
    out_bias, gain, shift, expand_bias, contract_bias = [item.reshape(1, -1) for item in vectors]
    seq_shape = (own, parts, piece, features)
    return remote_call(
        functools.partial(feed_forward_kernel, chunks),
        "feed_forward",
        4,
        out_shape=(
            jax.ShapeDtypeStruct(seq_shape, bf16),
            jax.ShapeDtypeStruct((rows, features), f32),
            jax.ShapeDtypeStruct(seq_shape, bf16),
            jax.ShapeDtypeStruct((features, hidden), bf16),
            jax.ShapeDtypeStruct((features, features), bf16),
            jax.ShapeDtypeStruct((each, features), f32),
            jax.ShapeDtypeStruct((1, hidden), f32),
            *[jax.ShapeDtypeStruct((1, features), f32)] * 3,
        ),
        in_specs=[HBM] * 4 + [VMEM] * 8,
        out_specs=(VMEM, VMEM, VMEM, HBM, HBM) + (VMEM,) * 5,
        scratch_shapes=[
            pltpu.VMEM((features, hidden), bf16),
            pltpu.VMEM((4, *contract.shape), bf16),
            pltpu.VMEM((rows, features), f32),
            pltpu.VMEM((rows, features), bf16),
            pltpu.VMEM((features, rows), bf16),
            pltpu.VMEM((rows, hidden), f32),
            pltpu.VMEM((rows, hidden), bf16),
            pltpu.VMEM((4, 4, 2, each, features), bf16),
            pltpu.VMEM((2, features, wide), bf16),
            *reduce_lines_scratch(each, features),
            pltpu.SemaphoreType.DMA((8,)),
            pltpu.SemaphoreType.DMA((2,)),
            *semaphores(
                ReduceLines.copies + len(chunks) * (Gather.copies_each - 3),
                1 + 3 * len(chunks),
            ),
        ],
    )(
        expand, contract, line, out_weight,
        expand_bias, upstream, tokens, attended, out_bias, gain, shift, contract_bias,
    )


def backward_fused_kernel(heads, width, count, chunks, *refs):
    slopes, diff_in, qkv_in, out_t_in, lse_in, layer = refs[:6]
    grads, refs = refs[6 : 6 + count], refs[6 + count :]
    joined_out, layer_out, layer_own = refs[0], refs[1], refs[2 + count]
    outs, refs = refs[2 : 2 + count], refs[3 + count :]
    diff, qkv, out_t, lse, joined = refs[:5]
    attention = Backward(heads, width, slopes, qkv, diff, out_t, lse, joined, *refs[5:12])
    bufs, refs = refs[12 : 12 + 7 * len(chunks)], refs[12 + 7 * len(chunks) :]
    copies = Copies(*refs[3:])
    place = Place()
    s, plane = place.s, place.plane
    features = heads * width
    along = ReduceAlong(place, grads[0], outs[0], bufs[:7], chunks[0], copies)
    reduce = Reduce(place, grads, outs, bufs[7:], chunks[1:], copies)
    back = HandBack(place, joined, joined_out, 3 * features, *refs[:3])

    own = [copies.inside(diff_in.at[:, :, :, columns_of(s, features)], diff.at[:, :, s])]
    own += [copies.inside(a, b) for a, b in ((qkv_in, qkv), (out_t_in, out_t), (lse_in, lse))]
    arriving = [
        copies.plan(diff_in.at[:, :, :, columns_of(to[1], features)], diff.at[:, :, s], to)
        for to in plane
    ]
    returned = [copies.plan(layer.at[:, to[0]], layer_out.at[place.z], to) for to in place.lines]
    load_layer = copies.inside(layer.at[:, place.z], layer_own)
    keep_layer = copies.inside(layer_own, layer_out.at[place.z])
    go(own + reduce.loads + [along.load, load_layer])
    greet(place.lines + plane)
    go(arriving + [along.first])
    reduce.start()
    along.exchange()
    go(returned)
    for t in range(3):
        reduce.exchange(t)
    done(own + [load_layer])
    keep_layer.start()
    arrive(arriving)
    attention.run(
        {
            1: [(reduce.spread, 0)],
            2: [(along.spread,)],
            3: [(reduce.spread, 1), (reduce.spread, 2)],
            4: [(reduce.send, 0), (along.send,)],
            5: [(reduce.send, 1)],
            6: [(reduce.send, 2)],
        },
        back.each,
    )
    for t in range(3):
        reduce.finish(t)
    along.finish()
    back.finish()
    arrive(returned)
    copies.finish()
    keep_layer.wait()


def backward_fused(attended_diff, qkv, saved, layer, grads, slopes, heads, width):
    own, parts, piece, columns = attended_diff.shape
    features = heads * width
    length = parts * 8 * piece
    cut = [split_grad(item) for item in grads]
    count = len(cut)
    rows, wide = cut[0].shape[3:]
    part = 3 * wide // 8
    chunks = [
        (0, 0, rows, 0, wide // 4),
        (0, 0, rows, wide // 4, part),
        (0, 0, rows, wide // 4 + part, part),
        *chunks_of(1, *cut[1].shape[3:], 1),
    ]
    out = remote_call(
        functools.partial(backward_fused_kernel, heads, width, count, chunks),
        "backward_fused",
        2,
        out_shape=(
            jax.ShapeDtypeStruct((own, parts, piece, 24 * features), bf16),
            jax.ShapeDtypeStruct((parts, own, piece, columns), bf16),
            *[jax.ShapeDtypeStruct(item.shape[3:], f32) for item in cut],
        ),
        in_specs=[SMEM] + [HBM] * (5 + count),
        out_specs=(HBM, HBM) + (VMEM,) * count,
        scratch_shapes=[
            pltpu.VMEM((own, piece, columns), bf16),
            pltpu.VMEM((own, parts, 8, piece, features), bf16),
            pltpu.VMEM(qkv.shape, bf16),
            *[pltpu.VMEM(item.shape, f32) for item in saved],
            pltpu.VMEM(qkv.shape, bf16),
            *backward_scratch(length, heads, width),
            *reduce_along_scratch(chunks[0]),
            *reduce_scratch(chunks[1:]),
            *hand_back_semaphores(own * parts),
            *semaphores(10 + len(chunks) * Reduce.copies_each, len(chunks) + 6),
        ],
    )(slopes, attended_diff, qkv, *saved, layer, *cut)
    return out[0], out[1].reshape(parts * own, piece, columns), out[2:]


def end_kernel(chunks, input_grad, vector, grad, input_out, vector_out, out, *refs):
    input_own, ranks, plane_sum, others = refs[:4]
    bufs, refs = refs[4 : 4 + 7 * len(chunks)], refs[4 + 7 * len(chunks) :]
    copies = Copies(*refs)
    place = Place()
    z, s, lines, plane = place.z, place.s, place.lines, place.plane
    count = len(chunks)
    reduce = Reduce(place, [grad], [out], bufs, chunks, copies)
    load = copies.inside(input_grad.at[:, z], input_own)
    load_vector = copies.inside(vector.at[:, s], ranks.at[0])
    keep = copies.inside(input_own, input_out.at[z])
    waiting = [copies.plan(input_grad.at[:, to[0]], input_out.at[z], to) for to in lines]
    vectors = [
        copies.plan(vector.at[:, to[1]], ranks.at[d + 1], to) for d, to in enumerate(plane)
    ]
    sums = [copies.plan(plane_sum.at[to[0]], others.at[k], to) for k, to in enumerate(lines)]
    go(reduce.loads + [load, load_vector])
    greet(lines + plane)
    reduce.start()
    go(waiting + vectors)
    load.wait()
    go([keep])
    for t in range(count + 2):
        if t < count:
            reduce.exchange(t)
        if t == 0:
            load_vector.wait()
            arrive(vectors)
            total = ranks[0]
            for d in range(1, 8):
                total = total + ranks[d]
            plane_sum[...] = total
            go(sums)
        if 0 <= t - 1 < count:
            reduce.spread(t - 1)
        if 0 <= t - 2:
            reduce.send(t - 2)
    arrive(sums)
    total = plane_sum[z]
    for k in range(3):
        total = total + others[k]
    vector_out[...] = total
    for t in range(count):
        reduce.finish(t)
    arrive(waiting)
    copies.finish()
    keep.wait()


def end(input_grad, vector, grad):
    own, parts, piece, features = input_grad.shape
    lanes = vector.shape[-1]
    padded = -(-lanes // 1024) * 1024
    vector = jnp.pad(vector, ((0, 0), (0, padded - lanes))).reshape(4, 8, padded // 128, 128)
    cut = split_grad(grad)
    chunks = chunks_of(0, *cut.shape[3:], 3)
    out = remote_call(
        functools.partial(end_kernel, chunks),
        "end",
        3,
        out_shape=(
            jax.ShapeDtypeStruct((parts, own, piece, features), bf16),
            jax.ShapeDtypeStruct(vector.shape[2:], f32),
            jax.ShapeDtypeStruct(cut.shape[3:], f32),
        ),
        in_specs=[HBM] * 3,
        out_specs=(HBM, VMEM, VMEM),
        scratch_shapes=[
            pltpu.VMEM((own, piece, features), bf16),
            pltpu.VMEM((8, 4, padded // 128, 128), f32),
            pltpu.VMEM((4, padded // 128, 128), f32),
            pltpu.VMEM((3, padded // 128, 128), f32),
            *reduce_scratch(chunks),
            *semaphores(3 + 7 + 3 + len(chunks) * Reduce.copies_each, 3 + len(chunks)),
        ],
    )(input_grad, vector, cut)
    return out[0].reshape(parts * own, piece, features), out[1].reshape(-1)[:lanes], out[2]


def per_device(
    layer_input,
    first_gain,
    first_shift,
    joined_weight,
    query_bias,
    value_bias,
    output_weight,
    output_bias,
    second_gain,
    second_shift,
    expand_weight,
    expand_bias,
    contract_weight,
    contract_bias,
    alibi_slopes,
    upstream,
):
    seqs, piece, features = layer_input.shape
    fs_count = lax.axis_size("fs")
    sp_count = lax.axis_size("sp")
    head_count = alibi_slopes.shape[0]
    width = features // head_count
    heads = head_count // sp_count
    rows = seqs * piece
    own = seqs // fs_count
    shape = (own, fs_count, piece)
    slopes = lax.dynamic_slice_in_dim(alibi_slopes, lax.axis_index("sp") * heads, heads)

    vectors = (
        first_gain, first_shift, query_bias, value_bias, output_bias,
        second_gain, second_shift, contract_bias, expand_bias,
    )
    fast = (fs_count, sp_count) == (4, 8) and (own, heads, width) == (2, 2, 64)
    fast = fast and expand_weight.shape[1] == 4 * features
    weights = (joined_weight, output_weight, expand_weight)
    gather = lambda item: lax.all_gather(item, "fs", axis=0, tiled=True)
    if fast:
        tokens, whole, weights, qkv, attended, saved, upstream_low = forward_fused(
            layer_input, upstream, vectors, weights, contract_weight, slopes, heads, width
        )
    else:
        tokens, upstream_low = to_own_seqs(layer_input), to_own_seqs(upstream)
        whole = [gather(item) for item in vectors]
        weights = [gather(item) for item in (*weights, contract_weight)]
    joined_full, out_full, expand_full, contract_full = weights
    tokens_low = tokens.reshape(rows, features)
    tokens = tokens_low.astype(f32)
    gain_one, shift_one, qbias, vbias, obias, gain_two, shift_two, cbias, ebias = [
        item.astype(f32) for item in whole
    ]

    normed_f, norm_back_one = jax.vjp(normalize, tokens, gain_one, shift_one)
    normed = normed_f.astype(bf16)
    if not fast:
        joined_bias = joined_bias_of(qbias, vbias, head_count)
        joined_all = (matmul(normed, joined_full) + joined_bias).astype(bf16)
        qkv = to_heads(joined_all.reshape(*shape, 3 * features))
        attended, *saved = attention_forward(qkv, slopes, heads, width)
        attended = from_heads(attended)
    attended = attended.reshape(rows, features)
    upstream_low = upstream_low.reshape(rows, features)

    upstream_f = upstream_low.astype(f32)
    contract_bias_grad = jnp.sum(upstream_f, axis=0)
    if fast:
        (
            layer_output, residual_grad, attended_diff, expand_grad, output_weight_grad,
            contract_grad, *small,
        ) = feed_forward(
            shape, expand_full, contract_weight, contract_full, out_full, tokens_low, upstream_low,
            attended, (obias, gain_two, shift_two, ebias, cbias),
        )
        expand_bias_grad, second_gain_grad, second_shift_grad, output_bias_grad = [
            item.reshape(-1) for item in small
        ]
    else:
        residual = tokens + (matmul(attended, out_full) + obias)
        second_f, norm_back_two = jax.vjp(normalize, residual, gain_two, shift_two)
        second = second_f.astype(bf16)
        expanded = matmul(second, expand_full) + ebias
        activated_f, gelu_back = jax.vjp(gelu_tanh, expanded)
        activated = activated_f.astype(bf16)
        result = residual + (matmul(activated, contract_full) + cbias)
        layer_output = result.astype(bf16).reshape(*shape, features)

        contract_grad = matmul_lt(activated, upstream_low)
        act_grad = matmul_rt(upstream_low, contract_full)
        expand_diff = gelu_back(act_grad)[0].astype(bf16)
        expand_grad = matmul_lt(second, expand_diff)
        expand_bias_grad = jnp.sum(expand_diff.astype(f32), axis=0)
        second_back = matmul_rt(expand_diff, expand_full)
        resid_part, second_gain_grad, second_shift_grad = norm_back_two(second_back)
        residual_grad = upstream_f + resid_part

        branch_diff = residual_grad.astype(bf16)
        output_weight_grad = matmul_lt(attended, branch_diff)
        output_bias_grad = jnp.sum(branch_diff.astype(f32), axis=0)
        attended_diff = matmul_rt(branch_diff, out_full).astype(bf16)
        attended_diff = attended_diff.reshape(*shape, features)
    grads = (expand_grad, output_weight_grad)
    scatter = functools.partial(
        lax.psum_scatter, axis_name=("fs", "sp"), scatter_dimension=0, tiled=True
    )
    if fast:
        joined_diff, layer_output, grads = backward_fused(
            attended_diff, qkv, saved, layer_output, [item.astype(bf16) for item in grads],
            slopes, heads, width,
        )
    else:
        joined_diff = attention_backward(
            qkv, to_heads(attended_diff), *saved, slopes, heads, width
        )
        joined_diff, layer_output = from_heads(joined_diff), from_own_seqs(layer_output)
        grads = [scatter(item) for item in grads]
        contract_grad = scatter(contract_grad)
    expand_grad, output_weight_grad = grads
    joined_diff = joined_diff.reshape(rows, 3 * features)

    joined_grad = matmul_lt(normed, joined_diff)
    column_sums = jnp.sum(joined_diff.astype(f32), axis=0).reshape(head_count, 3, width)
    query_bias_grad = column_sums[:, 0].reshape(features)
    value_bias_grad = column_sums[:, 2].reshape(features)
    normed_back = matmul_rt(joined_diff, joined_full)
    input_part, first_gain_grad, first_shift_grad = norm_back_one(normed_back)
    input_grad = (residual_grad + input_part).astype(bf16).reshape(*shape, features)

    vector_grads = (
        first_gain_grad, first_shift_grad, query_bias_grad, value_bias_grad, output_bias_grad,
        second_gain_grad, second_shift_grad, contract_bias_grad, expand_bias_grad,
    )
    devices = fs_count * sp_count
    packed = jnp.concatenate([item.reshape(devices, -1) for item in vector_grads], axis=1)
    if fast:
        input_grad, packed, joined_grad = end(input_grad, packed, joined_grad.astype(bf16))
    else:
        input_grad, joined_grad = from_own_seqs(input_grad), scatter(joined_grad)
        packed = scatter(packed.reshape(-1))
    own_grads, at = [], 0
    for item in vector_grads:
        size = item.shape[0] // devices
        own_grads.append(packed[at : at + size])
        at += size
    g1, s1, qb, vb, ob, g2, s2, cb, eb = own_grads
    return (
        layer_output,
        input_grad,
        g1,
        s1,
        joined_grad,
        qb,
        vb,
        output_weight_grad,
        ob,
        g2,
        s2,
        expand_grad,
        eb,
        contract_grad,
        cb,
    )


def solution(mesh):
    tokens = P(None, ("fs", "sp"), None)
    both, both_rows = P(("fs", "sp")), P(("fs", "sp"), None)
    one, one_rows = P("fs"), P("fs", None)
    return jax.shard_map(
        per_device,
        mesh=mesh,
        in_specs=(
            tokens, one, one, one_rows, one, one, one_rows, one, one, one, one_rows, one,
            one_rows, one, P(), tokens,
        ),
        out_specs=(
            tokens, tokens, both, both, both_rows, both, both, both_rows, both, both, both,
            both_rows, both, both_rows, both,
        ),
        check_vma=False,
    )
```

```python
import functools
import math

import jax
import jax.numpy as jnp
from jax import lax
from jax.experimental import pallas as pl
from jax.experimental.pallas import tpu as pltpu
from jax.sharding import PartitionSpec as P

norm_eps = 1e-05
gelu_coef = 0.7978845608028654
masked_value = -1e30
f32 = jnp.float32
bf16 = jnp.bfloat16
MESH = pl.DeviceIdType.MESH
HBM = pl.BlockSpec(memory_space=pl.ANY)
VMEM = pl.BlockSpec(memory_space=pltpu.VMEM)
SMEM = pl.BlockSpec(memory_space=pltpu.SMEM)
vmem_bytes = 63 * 1024 * 1024


def normalize(values, norm_gain, norm_shift):
    center = values - jnp.mean(values, axis=-1, keepdims=True)
    variance = jnp.mean(center * center, axis=-1, keepdims=True)
    return center * lax.rsqrt(variance + norm_eps) * norm_gain + norm_shift


def normalize_back(values, back, norm_gain):
    center = values - jnp.mean(values, axis=-1, keepdims=True)
    inverse = lax.rsqrt(jnp.mean(center * center, axis=-1, keepdims=True) + norm_eps)
    normal = center * inverse
    scaled = back * norm_gain
    even = jnp.mean(scaled, axis=-1, keepdims=True)
    along = jnp.mean(scaled * normal, axis=-1, keepdims=True)
    return inverse * (scaled - even - normal * along), normal


def gelu_tanh(values):
    return (
        0.5 * values * (1.0 + jnp.tanh(gelu_coef * (values + 0.044715 * values * values * values)))
    )


def matmul(left_side, right_side):
    return jnp.dot(left_side, right_side, preferred_element_type=f32)


def matmul_lt(left_side, right_side):
    return lax.dot_general(
        left_side, right_side, (((0,), (0,)), ((), ())), preferred_element_type=f32
    )


def matmul_rt(left_side, right_side):
    return lax.dot_general(
        left_side, right_side, (((1,), (1,)), ((), ())), preferred_element_type=f32
    )


def joined_bias_of(query_bias, value_bias, head_count):
    query_part = query_bias.astype(f32).reshape(head_count, -1)
    value_part = value_bias.astype(f32).reshape(head_count, -1)
    return jnp.stack([query_part, jnp.zeros_like(query_part), value_part], axis=1).reshape(-1)


def split_three(values):
    high = values.astype(bf16).astype(f32)
    rest = values - high
    middle = rest.astype(bf16).astype(f32)
    return high, middle, rest - middle


def key_columns(key_rows, slope, start):
    rows, width = key_rows.shape
    position = (start + lax.broadcasted_iota(jnp.int32, (rows, width), 0)).astype(f32)
    lane = lax.broadcasted_iota(jnp.int32, (rows, width), 1)
    high, middle, low = split_three(slope * position)
    extra = jnp.where(lane == 0, high, jnp.where(lane == 1, middle, jnp.where(lane == 2, low, 0.0)))
    return jnp.concatenate([key_rows.astype(f32), extra], axis=1).astype(bf16)


def query_columns(queries, scale):
    rows, width = queries.shape
    lane = lax.broadcasted_iota(jnp.int32, (rows, width), 1)
    ones = jnp.where(lane < 3, 1.0, 0.0)
    return jnp.concatenate([queries.astype(f32) * scale, ones], axis=1).astype(bf16)


def follow(n, after):
    for at, steps in after.items():

        def act(steps=steps):
            for step, *given in steps:
                step(*given)

        pl.when(n == at)(act)


class Forward:
    def __init__(self, heads, width, slopes, qkv, out, out_t, lse, keys, queries, values_t):
        self.heads, self.width, self.slopes, self.qkv, self.out = heads, width, slopes, qkv, out
        self.out_t, self.lse = out_t, lse
        self.keys, self.queries, self.values_t = keys, queries, values_t
        self.blocks = qkv.shape[1]
        self.block = qkv.shape[2] * qkv.shape[3]

    def rows(self, i):
        return pl.ds(pl.multiple_of(i * self.block, self.block), self.block)

    def prepare(self, b):
        width, block, qkv = self.width, self.block, self.qkv
        scale = 1.0 / math.sqrt(width)

        def body(i, _):
            rows = self.rows(i)
            for h in range(self.heads):
                base = h * 3 * width
                query, key, value = [
                    qkv[b, i, :, :, base + n * width : base + (n + 1) * width].reshape(block, width)
                    for n in range(3)
                ]
                self.keys[h, rows, :] = key_columns(key, self.slopes[h], i * block)
                self.queries[h, rows, :] = query_columns(query, scale)
                self.values_t[h, :, rows] = value.astype(f32).T.astype(bf16)
            return 0

        lax.fori_loop(0, self.blocks, body, 0)

    def one(self, b, i):
        heads, width, block = self.heads, self.width, self.block
        rows = self.rows(i)
        query = [self.queries[h, rows, :] for h in range(heads)]

        def step(j, state, diagonal):
            columns = self.rows(j)
            result = []
            for h in range(heads):
                top, total, acc = state[h]
                scores = matmul_rt(self.keys[h, columns, :], query[h])
                if diagonal:
                    key_at = lax.broadcasted_iota(jnp.int32, (block, block), 0)
                    query_at = lax.broadcasted_iota(jnp.int32, (block, block), 1)
                    scores = jnp.where(key_at <= query_at, scores, masked_value)
                newest = jnp.maximum(top, jnp.max(scores, axis=0, keepdims=True))
                shrink = jnp.exp(top - newest)
                probs = jnp.exp(scores - newest)
                total = total * shrink + jnp.sum(probs, axis=0, keepdims=True)
                acc = acc * shrink + matmul(self.values_t[h, :, columns], probs.astype(bf16))
                result.append((newest, total, acc))
            return tuple(result)

        state = tuple(
            (
                jnp.full((1, block), masked_value, f32),
                jnp.zeros((1, block), f32),
                jnp.zeros((width, block), f32),
            )
            for h in range(heads)
        )
        state = lax.fori_loop(0, i, lambda j, s: step(j, s, False), state)
        state = step(i, state, True)
        finished = []
        for h in range(heads):
            top, total, acc = state[h]
            result = acc / total
            self.out_t[b, h, :, rows] = result
            self.lse[b, h, :, rows] = top + jnp.log(total)
            finished.append(result)
        joined = finished[0] if heads == 1 else jnp.concatenate(finished, axis=0)
        self.out[b, i] = joined.T.astype(bf16).reshape(self.out.shape[2:])

    def run(self, after, each=None):
        blocks = self.blocks

        def body(n, _):
            b, i = n // blocks, n % blocks
            pl.when(i == 0)(lambda: self.prepare(b))
            self.one(b, i)
            if each is not None:
                each(b, i)
            follow(n, after)
            return 0

        lax.fori_loop(0, self.qkv.shape[0] * blocks, body, 0)


def forward_kernel(heads, width, *refs):
    Forward(heads, width, *refs).run({})


def saved_shapes(seqs, length, heads, width):
    return (
        jax.ShapeDtypeStruct((seqs, heads, width, length), f32),
        jax.ShapeDtypeStruct((seqs, heads, 1, length), f32),
    )


def forward_scratch(length, heads, width):
    return [
        pltpu.VMEM((heads, length, 2 * width), bf16),
        pltpu.VMEM((heads, length, 2 * width), bf16),
        pltpu.VMEM((heads, width, length), bf16),
    ]


def attention_forward(qkv, slopes, heads, width):
    seqs, blocks, ranks, piece, _ = qkv.shape
    length = blocks * ranks * piece
    return pl.pallas_call(
        functools.partial(forward_kernel, heads, width),
        name="attention_forward",
        out_shape=(
            jax.ShapeDtypeStruct((seqs, blocks, ranks, piece, heads * width), bf16),
            *saved_shapes(seqs, length, heads, width),
        ),
        in_specs=[SMEM, VMEM],
        out_specs=(VMEM, VMEM, VMEM),
        scratch_shapes=forward_scratch(length, heads, width),
        compiler_params=pltpu.CompilerParams(vmem_limit_bytes=vmem_bytes),
    )(slopes, qkv)


class Backward:
    def __init__(
        self, heads, width, slopes, qkv, diff, out_t, lse, joined,
        keys, queries, keys_t, values, diffs, delta, query_acc,
    ):
        self.heads, self.width, self.slopes, self.qkv, self.diff = heads, width, slopes, qkv, diff
        self.out_t, self.lse, self.joined = out_t, lse, joined
        self.keys, self.queries, self.keys_t, self.values = keys, queries, keys_t, values
        self.diffs, self.delta, self.query_acc = diffs, delta, query_acc
        self.blocks = qkv.shape[1]
        self.block = qkv.shape[2] * qkv.shape[3]

    def rows(self, i):
        return pl.ds(pl.multiple_of(i * self.block, self.block), self.block)

    def prepare(self, b):
        width, block, qkv = self.width, self.block, self.qkv
        scale = 1.0 / math.sqrt(width)

        def body(i, _):
            rows = self.rows(i)
            for h in range(self.heads):
                base = h * 3 * width
                query, key, value = [
                    qkv[b, i, :, :, base + n * width : base + (n + 1) * width].reshape(block, width)
                    for n in range(3)
                ]
                self.keys[h, rows, :] = key_columns(key, self.slopes[h], i * block)
                self.keys_t[h, :, rows] = key.astype(f32).T.astype(bf16)
                self.queries[h, rows, :] = query_columns(query, scale)
                self.values[h, rows, :] = value
                part = self.diff[b, i, :, :, h * width : (h + 1) * width].reshape(block, width)
                self.diffs[h, rows, :] = part
                self.delta[h, :, rows] = jnp.sum(
                    part.astype(f32).T * self.out_t[b, h, :, rows], axis=0, keepdims=True
                )
                self.query_acc[h, :, rows] = jnp.zeros((width, block), f32)
            return 0

        lax.fori_loop(0, self.blocks, body, 0)

    def one(self, b, j):
        heads, width, block = self.heads, self.width, self.block
        tail = self.joined.shape[2:4] + (width,)
        columns = self.rows(j)

        def step(i, state, diagonal):
            rows = self.rows(i)
            result = []
            for h in range(heads):
                key_acc, value_acc = state[h]
                query = self.queries[h, rows, :]
                part = self.diffs[h, rows, :]
                scores = matmul_rt(self.keys[h, columns, :], query)
                probs = jnp.exp(scores - self.lse[b, h, :, rows])
                if diagonal:
                    key_at = lax.broadcasted_iota(jnp.int32, (block, block), 0)
                    query_at = lax.broadcasted_iota(jnp.int32, (block, block), 1)
                    probs = jnp.where(key_at <= query_at, probs, 0.0)
                prob_diff = matmul_rt(self.values[h, columns, :], part)
                score_diff = (probs * (prob_diff - self.delta[h, :, rows])).astype(bf16)
                value_acc = value_acc + matmul(probs.astype(bf16), part)
                key_acc = key_acc + matmul(score_diff, query)
                self.query_acc[h, :, rows] += matmul(self.keys_t[h, :, columns], score_diff)
                result.append((key_acc, value_acc))
            return tuple(result)

        state = tuple(
            (jnp.zeros((block, 2 * width), f32), jnp.zeros((block, width), f32))
            for h in range(heads)
        )
        state = step(j, state, True)
        state = lax.fori_loop(j + 1, self.blocks, lambda i, s: step(i, s, False), state)
        for h in range(heads):
            base = (h * 3 + 1) * width
            key_acc, value_acc = state[h]
            self.joined[b, j, :, :, base : base + width] = (
                key_acc[:, :width].astype(bf16).reshape(tail)
            )
            self.joined[b, j, :, :, base + width : base + 2 * width] = value_acc.astype(
                bf16
            ).reshape(tail)

    def run(self, after, each=None):
        blocks = self.blocks

        def body(n, _):
            b, j = n // blocks, n % blocks
            pl.when(j == 0)(lambda: self.prepare(b))
            self.one(b, j)
            self.finish(b, j)
            if each is not None:
                each(b, j)
            follow(n, after)
            return 0

        lax.fori_loop(0, self.qkv.shape[0] * blocks, body, 0)

    def finish(self, b, j):
        width = self.width
        scale = 1.0 / math.sqrt(width)
        for h in range(self.heads):
            base = h * 3 * width
            result = (self.query_acc[h, :, self.rows(j)] * scale).T.astype(bf16)
            self.joined[b, j, :, :, base : base + width] = result.reshape(
                self.joined.shape[2:4] + (width,)
            )


def backward_kernel(heads, width, *refs):
    Backward(heads, width, *refs).run({})


def backward_scratch(length, heads, width):
    return [
        pltpu.VMEM((heads, length, 2 * width), bf16),
        pltpu.VMEM((heads, length, 2 * width), bf16),
        pltpu.VMEM((heads, width, length), bf16),
        pltpu.VMEM((heads, length, width), bf16),
        pltpu.VMEM((heads, length, width), bf16),
        pltpu.VMEM((heads, 1, length), f32),
        pltpu.VMEM((heads, width, length), f32),
    ]


def attention_backward(qkv, diff, out_t, lse, slopes, heads, width):
    length = qkv.shape[1] * qkv.shape[2] * qkv.shape[3]
    return pl.pallas_call(
        functools.partial(backward_kernel, heads, width),
        name="attention_backward",
        out_shape=jax.ShapeDtypeStruct(qkv.shape, bf16),
        in_specs=[SMEM, VMEM, VMEM, VMEM, VMEM],
        out_specs=VMEM,
        scratch_shapes=backward_scratch(length, heads, width),
        compiler_params=pltpu.CompilerParams(vmem_limit_bytes=vmem_bytes),
    )(slopes, qkv, diff, out_t, lse)


def to_own_seqs(values):
    seqs, piece, features = values.shape
    parts = lax.axis_size("fs")
    values = values.reshape(parts, seqs // parts, piece, features)
    return lax.all_to_all(values, "fs", split_axis=0, concat_axis=0).transpose(1, 0, 2, 3)


def from_own_seqs(values):
    own, parts, piece, features = values.shape
    values = lax.all_to_all(values.transpose(1, 0, 2, 3), "fs", split_axis=0, concat_axis=0)
    return values.reshape(parts * own, piece, features)


def to_heads(values):
    own, parts, piece, features = values.shape
    ranks = lax.axis_size("sp")
    values = values.reshape(own, parts, piece, ranks, features // ranks)
    return lax.all_to_all(values, "sp", split_axis=3, concat_axis=2)


def from_heads(values):
    own, parts, ranks, piece, features = values.shape
    values = lax.all_to_all(values, "sp", split_axis=2, concat_axis=3)
    return values.reshape(own, parts, piece, ranks * features)


class Copies:
    def __init__(self, send, recv, local):
        self.send, self.recv, self.local = send, recv, local
        self.used, self.used_local, self.made = 0, 0, []

    def plan(self, source, target, device):
        copy = pltpu.make_async_remote_copy(
            src_ref=source,
            dst_ref=target,
            send_sem=self.send.at[self.used],
            recv_sem=self.recv.at[self.used],
            device_id=device,
            device_id_type=MESH,
        )
        self.used += 1
        self.made.append(copy)
        return copy

    def inside(self, source, target):
        copy = pltpu.make_async_copy(source, target, self.local.at[self.used_local])
        self.used_local += 1
        return copy

    def finish(self):
        assert (self.used, self.used_local) == (self.send.shape[0], self.local.shape[0])
        for copy in self.made:
            copy.wait_send()


def go(copies):
    for copy in copies:
        copy.start()


def arrive(copies):
    for copy in copies:
        copy.wait_recv()


def done(copies):
    for copy in copies:
        copy.wait()


def greet(devices):
    barrier = pltpu.get_barrier_semaphore()
    for device in devices:
        pl.semaphore_signal(barrier, inc=1, device_id=device, device_id_type=MESH)
    pl.semaphore_wait(barrier, len(devices))


class Place:
    def __init__(self):
        z, s = lax.axis_index("fs"), lax.axis_index("sp")
        self.z, self.s = z, s
        self.core, self.chip = s % 2, s // 2
        self.x, self.y = self.chip % 2, self.chip // 2
        self.along_x = s + 2 - 4 * self.x
        self.along_y = s + 4 - 8 * self.y
        self.partner = s + 1 - 2 * self.core
        self.diagonal = self.along_x + self.along_y - s
        self.chip_x, self.chip_y = self.along_x // 2, self.along_y // 2
        self.lines = [(lax.rem(z + k, 4), s) for k in range(1, 4)]
        self.plane = [(z, lax.rem(s + d, 8)) for d in range(1, 8)]
        self.to_x, self.to_y, self.to_core = [
            (z, to) for to in (self.along_x, self.along_y, self.partner)
        ]
        self.near = self.lines + [self.to_x, self.to_y, self.to_core]


class Gather:
    copies_each = 33

    def __init__(self, place, weights, wholes, kept, chunks, copies, given=None):
        z, s, lines = place.z, place.s, place.lines
        self.ready = arrive if given is None else done
        self.loads, self.own = [], []
        for weight, whole, keep in zip(weights, wholes, kept):
            if keep is None:
                self.loads.append(copies.inside(weight, whole.at[z]))
            else:
                self.loads.append(copies.inside(weight, keep))
                self.own.append(copies.inside(keep, whole.at[z]))
        self.first, self.second, self.third, self.cores, self.last = [], [], [], [], []
        for t, row, rows, column, columns in chunks:
            whole = wholes[t]
            wide = pl.ds(column, columns)
            every = pl.ds(row, rows)
            low, high = pl.ds(row, rows // 2), pl.ds(row + rows // 2, rows // 2)

            def same(k, rank, part, to):
                where = (k, rank, part, wide)
                return copies.plan(whole.at[where], whole.at[where], to)

            if given is None:
                first = [
                    copies.plan(weights[t].at[s, every, wide], whole.at[z, s, every, wide], to)
                    for to in lines
                ]
            else:
                first = [
                    copies.inside(given.at[k, every, wide], whole.at[k, s, every, wide])
                    for k, _ in lines
                ]
            self.first.append(first)
            second, third, cores, last = [], [], [], []
            for k, _ in lines:
                second.append(same(k, s, low, place.to_x))
                second.append(same(k, s, high, place.to_y))
                cores.append(same(k, s, every, place.to_core))
                third.append(same(k, s, low, place.to_y))
                third.append(same(k, s, high, place.to_x))
                third.append(same(k, place.along_x, low, place.to_y))
                third.append(same(k, place.along_y, high, place.to_x))
                for rank in (place.along_x, place.along_y, place.diagonal):
                    last.append(same(k, rank, every, place.to_core))
            self.second.append(second)
            self.third.append(third)
            self.cores.append(cores)
            self.last.append(last)

    def keep(self):
        done(self.loads)
        go(self.own)

    def start(self, t):
        go(self.first[t])

    def exchange(self, t):
        self.ready(self.first[t])
        go(self.second[t])
        go(self.cores[t])

    def spread(self, t):
        arrive(self.second[t])
        go(self.third[t])

    def share(self, t):
        arrive(self.third[t])
        go(self.last[t])

    def complete(self, t):
        arrive(self.cores[t] + self.last[t])


def add_into(target, other):
    target[...] = (target[...].astype(f32) + other[...].astype(f32)).astype(target.dtype)


def add_blocks(steps, block_of):
    def body(i, _):
        add_into(*block_of(i))
        return 0

    lax.fori_loop(0, steps, body, 0)


class Reduce:
    copies_each = 10

    def __init__(self, place, grads, outs, bufs, chunks, copies):
        self.place, self.outs, self.chunks = place, outs, chunks
        self.bufs = [bufs[7 * t : 7 * t + 7] for t in range(len(chunks))]
        self.loads, self.first, self.second, self.third, self.fourth = [], [], [], [], []
        for (t, row, rows, column, columns), buf in zip(chunks, self.bufs):
            own, from_core, from_x, from_y, late_y, late_x, from_z = buf
            every, wide = pl.ds(row, rows), pl.ds(column, columns)
            low, high = pl.ds(0, rows // 2), pl.ds(rows // 2, rows // 2)
            self.loads.append(
                copies.inside(grads[t].at[:, :, place.core, every, wide], own)
            )
            self.first.append(
                copies.plan(
                    grads[t].at[:, :, 1 - place.core, every, wide], from_core, place.to_core
                )
            )
            step = []
            for k in range(2):
                step.append(
                    copies.plan(own.at[:, 2 * k + 1 - place.x, low], from_x.at[:, k], place.to_x)
                )
                step.append(
                    copies.plan(
                        own.at[:, 2 * (1 - place.y) + k, high], from_y.at[:, k], place.to_y
                    )
                )
            self.second.append(step)
            self.third.append(
                [
                    copies.plan(own.at[:, place.chip_y, low], late_y, place.to_y),
                    copies.plan(own.at[:, place.chip_x, high], late_x, place.to_x),
                ]
            )
            self.fourth.append(
                [
                    copies.plan(own.at[to[0], place.chip], from_z.at[k], to)
                    for k, to in enumerate(place.lines)
                ]
            )

    def start(self):
        go(self.first)

    def begin(self, t):
        go([self.loads[t], self.first[t]])

    def halves(self, t):
        half = self.chunks[t][2] // 2
        return pl.ds(0, half), pl.ds(half, half)

    def exchange(self, t):
        own, from_core = self.bufs[t][:2]
        self.loads[t].wait()
        arrive([self.first[t]])
        add_blocks(16, lambda i: (own.at[i // 4, i % 4], from_core.at[i // 4, i % 4]))
        go(self.second[t])

    def spread(self, t):
        own, _, from_x, from_y = self.bufs[t][:4]
        low, high = self.halves(t)
        x, y = self.place.x, self.place.y
        arrive(self.second[t])
        add_blocks(8, lambda i: (own.at[i // 2, 2 * (i % 2) + x, low], from_x.at[i // 2, i % 2]))
        add_blocks(8, lambda i: (own.at[i // 2, 2 * y + i % 2, high], from_y.at[i // 2, i % 2]))
        go(self.third[t])

    def send(self, t):
        own, _, _, _, late_y, late_x, _ = self.bufs[t]
        low, high = self.halves(t)
        chip = self.place.chip
        arrive(self.third[t])
        add_blocks(4, lambda i: (own.at[i, chip, low], late_y.at[i]))
        add_blocks(4, lambda i: (own.at[i, chip, high], late_x.at[i]))
        go(self.fourth[t])

    def finish(self, t):
        own, from_z = self.bufs[t][0], self.bufs[t][6]
        index, row, rows, column, columns = self.chunks[t]
        arrive(self.fourth[t])
        total = own[self.place.z, self.place.chip].astype(f32)
        for k in range(3):
            total = total + from_z[k].astype(f32)
        self.outs[index][row : row + rows, column : column + columns] = total


def reduce_scratch(chunks):
    scratch = []
    for _, _, rows, _, columns in chunks:
        half = rows // 2
        scratch += [
            pltpu.VMEM((4, 4, rows, columns), bf16),
            pltpu.VMEM((4, 4, rows, columns), bf16),
            pltpu.VMEM((4, 2, half, columns), bf16),
            pltpu.VMEM((4, 2, half, columns), bf16),
            pltpu.VMEM((4, half, columns), bf16),
            pltpu.VMEM((4, half, columns), bf16),
            pltpu.VMEM((3, rows, columns), bf16),
        ]
    return scratch


class ReduceAlong(Reduce):
    def __init__(self, place, grad, out, buf, chunk, copies):
        self.place, self.grad, self.out, self.buf, self.chunk = place, grad, out, buf, chunk
        own, from_core, from_z, from_x, from_y, late_y, late_x = buf
        _, row, rows, column, columns = chunk
        every, wide = pl.ds(row, rows), pl.ds(column, columns)
        self.low, self.high = low, high = pl.ds(0, rows // 2), pl.ds(rows // 2, rows // 2)
        z, x, y = place.z, place.x, place.y
        self.load = copies.inside(grad.at[:, :, place.core, every, wide], own)
        self.first = copies.plan(
            grad.at[:, :, 1 - place.core, every, wide], from_core, place.to_core
        )
        self.second = [
            copies.plan(own.at[to[0]], from_z.at[k], to) for k, to in enumerate(place.lines)
        ]
        self.third = []
        for k in range(2):
            self.third.append(
                copies.plan(own.at[z, 2 * k + 1 - x, low], from_x.at[k], place.to_x)
            )
            self.third.append(
                copies.plan(own.at[z, 2 * (1 - y) + k, high], from_y.at[k], place.to_y)
            )
        self.fourth = [
            copies.plan(own.at[z, place.chip_y, low], late_y, place.to_y),
            copies.plan(own.at[z, place.chip_x, high], late_x, place.to_x),
        ]

    def exchange(self):
        own, from_core = self.buf[:2]
        self.load.wait()
        arrive([self.first])
        add_blocks(16, lambda i: (own.at[i // 4, i % 4], from_core.at[i // 4, i % 4]))
        go(self.second)

    def spread(self):
        own, _, from_z = self.buf[:3]
        z = self.place.z
        arrive(self.second)

        def body(i, _):
            total = own[z, i].astype(f32)
            for k in range(3):
                total = total + from_z[k, i].astype(f32)
            own[z, i] = total.astype(bf16)
            return 0

        lax.fori_loop(0, 4, body, 0)
        go(self.third)

    def send(self):
        own, _, _, from_x, from_y = self.buf[:5]
        z, x, y = self.place.z, self.place.x, self.place.y
        arrive(self.third)
        add_blocks(2, lambda j: (own.at[z, 2 * j + x, self.low], from_x.at[j]))
        add_blocks(2, lambda j: (own.at[z, 2 * y + j, self.high], from_y.at[j]))
        go(self.fourth)

    def finish(self):
        own, late_y, late_x = self.buf[0], self.buf[5], self.buf[6]
        z, chip = self.place.z, self.place.chip
        _, row, rows, column, columns = self.chunk
        arrive(self.fourth)
        half = rows // 2
        wide = slice(column, column + columns)
        self.out[row : row + half, wide] = own[z, chip, self.low].astype(f32) + late_y[...].astype(
            f32
        )
        self.out[row + half : row + rows, wide] = own[z, chip, self.high].astype(f32) + late_x[
            ...
        ].astype(f32)


def reduce_along_scratch(chunk):
    _, _, rows, _, columns = chunk
    half = rows // 2
    return [
        pltpu.VMEM((4, 4, rows, columns), bf16),
        pltpu.VMEM((4, 4, rows, columns), bf16),
        pltpu.VMEM((3, 4, rows, columns), bf16),
        pltpu.VMEM((2, half, columns), bf16),
        pltpu.VMEM((2, half, columns), bf16),
        pltpu.VMEM((half, columns), bf16),
        pltpu.VMEM((half, columns), bf16),
    ]


class HandBack:
    def __init__(self, place, source, target, features, send, recv, local):
        self.place, self.source, self.target = place, source, target
        self.mine = columns_of(place.s, features)
        self.send, self.recv, self.local = send, recv, local
        self.blocks = source.shape[1]

    def copy(self, b, i, d):
        rank = self.place.plane[d][1]
        n = b * self.blocks + i
        return pltpu.make_async_remote_copy(
            src_ref=self.source.at[b, i, rank],
            dst_ref=self.target.at[b, i, :, self.mine],
            send_sem=self.send.at[n, d],
            recv_sem=self.recv.at[n, d],
            device_id=self.place.plane[d],
            device_id_type=MESH,
        )

    def own(self, b, i):
        return pltpu.make_async_copy(
            self.source.at[b, i, self.place.s],
            self.target.at[b, i, :, self.mine],
            self.local.at[b * self.blocks + i],
        )

    def each(self, b, i):
        for d in range(7):
            self.copy(b, i, d).start()
        self.own(b, i).start()

    def finish(self):
        def body(n, _):
            b, i = n // self.blocks, n % self.blocks
            for d in range(7):
                self.copy(b, i, d).wait()
            self.own(b, i).wait()
            return 0

        lax.fori_loop(0, self.source.shape[0] * self.blocks, body, 0)


def hand_back_semaphores(steps):
    return [
        pltpu.SemaphoreType.DMA((steps, 7)),
        pltpu.SemaphoreType.DMA((steps, 7)),
        pltpu.SemaphoreType.DMA((steps,)),
    ]


class ReduceLines:
    copies = 4 * 7 + 3

    def __init__(self, place, grad, out, bufs, copies):
        self.place, self.grad, self.out, self.bufs = place, grad, out, bufs
        from_core, from_x, from_y, late_y, late_x, from_z = bufs
        core, x, y = place.core, place.x, place.y
        self.order = [to[0] for to in place.lines] + [place.z]
        rows = grad.shape[3]
        self.low, self.high = pl.ds(0, rows // 2), pl.ds(rows // 2, rows // 2)
        self.first, self.second, self.third, self.fourth = [], [], [], []
        for k, at in enumerate(self.order):
            self.first.append(
                copies.plan(grad.at[at, :, 1 - core], from_core.at[k], place.to_core)
            )
            step = []
            for j in range(2):
                step.append(
                    copies.plan(
                        grad.at[at, 2 * j + 1 - x, core, self.low], from_x.at[k, j], place.to_x
                    )
                )
                step.append(
                    copies.plan(
                        grad.at[at, 2 * (1 - y) + j, core, self.high], from_y.at[k, j], place.to_y
                    )
                )
            self.second.append(step)
            self.third.append(
                [
                    copies.plan(grad.at[at, place.chip_y, core, self.low], late_y.at[k], place.to_y),
                    copies.plan(
                        grad.at[at, place.chip_x, core, self.high], late_x.at[k], place.to_x
                    ),
                ]
            )
            if k < 3:
                self.fourth.append(
                    copies.plan(grad.at[at, place.chip, core], from_z.at[k], place.lines[k])
                )

    def start(self, k):
        go([self.first[k]])

    def exchange(self, k):
        arrive([self.first[k]])
        at, core = self.order[k], self.place.core
        add_blocks(4, lambda i: (self.grad.at[at, i, core], self.bufs[0].at[k, i]))
        go(self.second[k])

    def spread(self, k):
        arrive(self.second[k])
        at, core, x, y = self.order[k], self.place.core, self.place.x, self.place.y
        add_blocks(
            2, lambda j: (self.grad.at[at, 2 * j + x, core, self.low], self.bufs[1].at[k, j])
        )
        add_blocks(
            2, lambda j: (self.grad.at[at, 2 * y + j, core, self.high], self.bufs[2].at[k, j])
        )
        go(self.third[k])

    def send(self, k):
        arrive(self.third[k])
        at, core, chip = self.order[k], self.place.core, self.place.chip
        add_into(self.grad.at[at, chip, core, self.low], self.bufs[3].at[k])
        add_into(self.grad.at[at, chip, core, self.high], self.bufs[4].at[k])
        go(self.fourth[k : k + 1])

    def finish(self):
        arrive(self.fourth)
        place = self.place
        total = self.grad[place.z, place.chip, place.core].astype(f32)
        for k in range(3):
            total = total + self.bufs[5][k].astype(f32)
        self.out[...] = total


def reduce_lines_scratch(rows, columns):
    half = rows // 2
    return [
        pltpu.VMEM((4, 4, rows, columns), bf16),
        pltpu.VMEM((4, 2, half, columns), bf16),
        pltpu.VMEM((4, 2, half, columns), bf16),
        pltpu.VMEM((4, half, columns), bf16),
        pltpu.VMEM((4, half, columns), bf16),
        pltpu.VMEM((3, rows, columns), bf16),
    ]


def split_grad(item):
    return item.reshape(4, 4, 2, item.shape[0] // 32, item.shape[1])


def split_weight(item):
    return item.reshape(8, item.shape[0] // 8, item.shape[1])


def chunks_of(index, rows, columns, count):
    if rows >= 64:
        return [(index, rows // count * n, rows // count, 0, columns) for n in range(count)]
    return [(index, 0, rows, columns // count * n, columns // count) for n in range(count)]


def semaphores(remote, local):
    return [pltpu.SemaphoreType.DMA((n,)) for n in (remote, remote, local)]


def remote_call(kernel, name, collective, **options):
    return pl.pallas_call(
        kernel,
        name=name,
        compiler_params=pltpu.CompilerParams(
            collective_id=collective, has_side_effects=True, vmem_limit_bytes=vmem_bytes
        ),
        **options,
    )


def columns_of(rank, features):
    return pl.ds(pl.multiple_of(rank * features, 128), features)


def forward_fused_kernel(heads, width, count, vector_count, chunks, slopes, tokens, upstream, *refs):
    vectors, refs = refs[:vector_count], refs[vector_count:]
    weights, contract, refs = refs[:count], refs[count], refs[count + 1 :]
    tokens_out, vectors_out, joined_out, qkv_out, attended, out_t, lse, upstream_out = refs[:8]
    contract_out = refs[8]
    wholes, refs = refs[9 : 8 + count], refs[8 + count :]
    held, small, values_of, joined, normed, outgoing, qkv, result, upstream_own = refs[:9]
    attention = Forward(heads, width, slopes, qkv, result, out_t, lse, *refs[9:12])
    kept, refs = refs[12 : 11 + count], refs[11 + count :]
    head_send, head_recv = refs[:2]
    copies = Copies(*refs[5:])
    place = Place()
    z, s, lines, plane = place.z, place.s, place.lines, place.plane
    gather = Gather(place, weights, [joined, *wholes], [None, *kept], chunks, copies)
    first = [t for t, chunk in enumerate(chunks) if chunk[0] == 0]
    later = [t for t, chunk in enumerate(chunks) if chunk[0] > 0]
    features = heads * width
    back = HandBack(place, result, attended, features, *refs[2:5])
    own_seqs, parts, piece, wide = held.shape

    load = copies.inside(tokens.at[z], held.at[:, z])
    load_upstream = copies.inside(upstream.at[z], upstream_own)
    seqs = [copies.plan(tokens.at[to[0]], held.at[:, z], to) for to in lines]
    vector_copies = [copies.plan(small.at[z], small.at[z], to) for to in lines]
    upstreams = [copies.plan(upstream.at[to[0]], upstream_out.at[:, z], to) for to in lines]
    keep_upstream = copies.inside(upstream_own, upstream_out.at[:, z])
    keeping = [
        copies.inside(held, tokens_out),
        copies.inside(small, vectors_out),
        copies.inside(joined, joined_out),
    ]
    keep_qkv = copies.inside(qkv, qkv_out)
    contracts = [copies.plan(contract.at[s], contract_out.at[z], to) for to in lines]

    def to_head(d):
        return pltpu.make_async_remote_copy(
            src_ref=outgoing.at[d],
            dst_ref=qkv.at[:, :, s],
            send_sem=head_send.at[d],
            recv_sem=head_recv.at[d],
            device_id=(z, lax.rem(s + 1 + d, 8)),
            device_id_type=MESH,
        )

    go(gather.loads + [load, load_upstream])
    small[z] = jnp.zeros(small.shape[1:], bf16)
    for n, item in enumerate(vectors):
        small[z, n, : item.shape[0], :] = item[...]
    greet(lines + plane)
    for t in first:
        gather.start(t)
    go(seqs + vector_copies)
    gather.keep()
    load.wait()
    for t in range(len(first) + 2):
        if t < len(first):
            gather.exchange(t)
        if 0 <= t - 1 < len(first):
            gather.spread(t - 1)
        if 0 <= t - 2:
            gather.share(t - 2)
    load_upstream.wait()
    keep_upstream.start()
    arrive(seqs + vector_copies)
    for t in later:
        gather.start(t)
    values_of[...] = small[...].astype(f32)

    def row_of(n):
        found = [values_of[k, n, r : r + 1, :] for k in range(4) for r in range(wide // 512)]
        return jnp.concatenate(found, axis=1)

    gain, shift = row_of(0), row_of(1)

    def norm(i, _):
        values = held[i // parts, i % parts].astype(f32)
        rows = pl.ds(pl.multiple_of(i * piece, piece), piece)
        normed[rows, :] = normalize(values, gain, shift).astype(bf16)
        return 0

    lax.fori_loop(0, own_seqs * parts, norm, 0)
    for t in first:
        gather.complete(t)
    go(keeping)

    def project(d, _):
        rank = lax.rem(s + 1 + d, 8)
        per = 8 // 4
        query_bias = values_of[rank // per, 2, pl.ds(rank % per, 1), :]
        value_bias = values_of[rank // per, 3, pl.ds(rank % per, 1), :]
        low = lax.broadcasted_iota(jnp.int32, query_bias.shape, 1) < width
        bias = jnp.concatenate(
            [
                jnp.where(low, query_bias, 0.0),
                jnp.where(low, value_bias, query_bias),
                jnp.where(low, 0.0, value_bias),
            ],
            axis=1,
        )
        weight = joined[:, :, :, columns_of(rank, 3 * features)].reshape(wide, 3 * features)
        made = (matmul(normed[...], weight) + bias).astype(bf16)
        outgoing[d] = made.reshape(outgoing.shape[1:])
        pl.when(d < 7)(lambda: to_head(d).start())
        return 0

    lax.fori_loop(0, 8, project, 0)
    own_copy = copies.inside(outgoing.at[7], qkv.at[:, :, s])
    own_copy.start()
    base = later[0]
    gather.exchange(base)
    gather.exchange(base + 1)
    own_copy.wait()
    gather.spread(base)
    for d in range(7):
        to_head(d).wait_recv()
    keep_qkv.start()
    attention.run(
        {
            0: [(gather.exchange, base + 2), (go, contracts), (gather.spread, base + 1)],
            2: [(gather.spread, base + 2), (gather.share, base)],
            3: [(go, upstreams)],
            5: [(gather.share, base + 1)],
            6: [(gather.share, base + 2)],
        },
        back.each,
    )
    for t in later:
        gather.complete(t)
    arrive(contracts + upstreams)
    back.finish()
    for d in range(7):
        to_head(d).wait_send()
    copies.finish()
    done(gather.own + [keep_upstream, keep_qkv] + keeping)


def forward_fused(tokens, upstream, vectors, weights, contract, slopes, heads, width):
    seqs, piece, features = tokens.shape
    parts = 4
    own = seqs // parts
    columns = heads * width
    length = parts * 8 * piece
    vectors = [item.reshape(-1, 128) for item in vectors]
    cut = [split_weight(item) for item in weights]
    contract = split_weight(contract)
    count, tall = len(cut), 8 * -(-max(item.shape[0] for item in vectors) // 8)
    chunks = []
    for t, pieces in enumerate((3, 1, 2)):
        chunks += chunks_of(t, *cut[t].shape[1:], pieces)
    seq_shape = (own, parts, piece, features)
    qkv_shape = (own, parts, 8, piece, 3 * columns)
    small = (parts, len(vectors), tall, 128)
    out = remote_call(
        functools.partial(forward_fused_kernel, heads, width, count, len(vectors), chunks),
        "forward_fused",
        1,
        out_shape=(
            jax.ShapeDtypeStruct(seq_shape, bf16),
            jax.ShapeDtypeStruct(small, bf16),
            jax.ShapeDtypeStruct((parts, *cut[0].shape), bf16),
            jax.ShapeDtypeStruct(qkv_shape, bf16),
            jax.ShapeDtypeStruct(seq_shape, bf16),
            *saved_shapes(own, length, heads, width),
            jax.ShapeDtypeStruct(seq_shape, bf16),
            jax.ShapeDtypeStruct((parts, *contract.shape[1:]), bf16),
            *[jax.ShapeDtypeStruct((parts, *item.shape), bf16) for item in cut[1:]],
        ),
        in_specs=[SMEM, HBM, HBM] + [VMEM] * len(vectors) + [HBM] * (count + 1),
        out_specs=(HBM,) * 5 + (VMEM, VMEM) + (HBM,) * (count + 1),
        scratch_shapes=[
            pltpu.VMEM(seq_shape, bf16),
            pltpu.VMEM(small, bf16),
            pltpu.VMEM(small, f32),
            pltpu.VMEM((parts, *cut[0].shape), bf16),
            pltpu.VMEM((own * parts * piece, features), bf16),
            pltpu.VMEM((8, own, parts, piece, 3 * columns), bf16),
            pltpu.VMEM(qkv_shape, bf16),
            pltpu.VMEM((own, parts, 8, piece, columns), bf16),
            pltpu.VMEM((own, piece, features), bf16),
            *forward_scratch(length, heads, width),
            *[pltpu.VMEM(item.shape, bf16) for item in cut[1:]],
            pltpu.SemaphoreType.DMA((7,)),
            pltpu.SemaphoreType.DMA((7,)),
            *hand_back_semaphores(own * parts),
            *semaphores(12 + len(chunks) * Gather.copies_each, 2 * count - 1 + 8),
        ],
    )(
        slopes,
        tokens.reshape(parts, own, piece, features),
        upstream.reshape(parts, own, piece, features),
        *vectors,
        *cut,
        contract,
    )
    wholes = [
        whole.reshape(4 * item.shape[0], item.shape[1])
        for whole, item in zip((out[2], *out[9:]), weights)
    ]
    found = [out[1][:, n, : item.shape[0]].reshape(-1) for n, item in enumerate(vectors)]
    return out[0], found, [*wholes, out[8]], out[3], out[4], (out[5], out[6]), out[7]


def feed_forward_kernel(
    chunks, expand, contract, contract_line, out_weight,
    expand_bias, upstream, tokens, attended, out_bias, gain, shift, contract_bias,
    layer, residual_grad, attended_diff, expand_grad, out_grad, contract_grad,
    bias_grad, gain_grad, shift_grad, out_bias_grad,
    expand_in, contract_in, residual, second, second_t, expanded, activated, grad, staged, *refs,
):
    second_back = residual_grad
    bufs, refs = refs[:6], refs[6:]
    loaded, stored, refs = refs[0], refs[1], refs[2:]
    copies = Copies(*refs)
    place = Place()
    z = place.z
    reduce = ReduceLines(place, grad, contract_grad, bufs, copies)
    gather = Gather(
        place, [contract], [contract_in], [None], chunks, copies, given=contract_line
    )
    rows, features = second.shape
    steps = 8
    wide = expand.shape[1] // steps

    def at(n):
        part = (z + 1 + n // 2) % 4
        return part, n % 2, pl.ds(pl.multiple_of((2 * part + n % 2) * wide, wide), wide)

    def load(n):
        _, _, where = at(n)
        return pltpu.make_async_copy(expand.at[:, where], expand_in.at[:, where], loaded.at[n])

    def contract_at(n):
        part, side, _ = at(n)
        return contract_in[part, pl.ds(4 * side, 4)].reshape(wide, features)

    def store(n):
        _, _, where = at(n)
        slot = n % 2
        return pltpu.make_async_copy(
            staged.at[slot], expand_grad.at[:, where], stored.at[slot]
        )

    halves = [pl.ds(0, wide), pl.ds(wide, wide)]
    out_loads = [
        pltpu.make_async_copy(out_weight.at[:, half], staged.at[n], stored.at[n])
        for n, half in enumerate(halves)
    ]
    out_stores = [
        pltpu.make_async_copy(staged.at[n], out_grad.at[:, half], stored.at[n])
        for n, half in enumerate(halves)
    ]
    part_rows = rows // 8

    def rows_at(i):
        return pl.ds(pl.multiple_of(i * part_rows, part_rows), part_rows)

    for n in range(len(chunks)):
        gather.start(n)
    go(out_loads)
    for n in range(steps):
        load(n).start()
    go(gather.loads)
    greet(place.near)
    for n in range(len(chunks)):
        gather.exchange(n)
    for n, half in enumerate(halves):
        out_loads[n].wait()
        residual[:, half] = (
            tokens[:, half].astype(f32) + (matmul(attended[...], staged[n]) + out_bias[:, half])
        )

    def norm(i, _):
        values = residual[rows_at(i), :]
        second[rows_at(i), :] = normalize(values, gain[...], shift[...]).astype(bf16)
        second_back[rows_at(i), :] = values + contract_bias[...]
        return 0

    lax.fori_loop(0, 8, norm, 0)
    for n in range(len(chunks) - 1):
        gather.spread(n)
    second_t[...] = second[...].T

    def forward(n, after):
        part, side, where = at(n)
        load(n).wait()
        values = matmul(second[...], expand_in[:, where]) + expand_bias[:, where]
        expanded[:, where] = values
        low = gelu_tanh(values).astype(bf16)
        activated[:, where] = low
        made = matmul(low.T, upstream[...]).astype(bf16)
        grad[part, pl.ds(2 * side, 2)] = made.reshape(2, 2, wide // 4, features)
        follow(n, after)
        return 0

    def shrink(n, after):
        _, _, where = at(n)
        second_back[...] += matmul(activated[:, where], contract_at(n))
        follow(n, after)
        return 0

    def backward(n, after):
        _, _, where = at(n)
        values = expanded[:, where]
        act_grad = matmul_rt(upstream[...], contract_at(n))
        bent = jnp.tanh(gelu_coef * (values + 0.044715 * values * values * values))
        slope = 0.5 * (1.0 + bent) + 0.5 * values * (1.0 - bent * bent) * (
            gelu_coef * (1.0 + 3.0 * 0.044715 * values * values)
        )
        diff = (act_grad * slope).astype(bf16)
        bias_grad[:, where] = jnp.sum(diff.astype(f32), axis=0, keepdims=True)
        pl.when(n >= 2)(lambda: store(n - 2).wait())
        staged[n % 2] = matmul(second_t[...], diff).astype(bf16)
        store(n).start()
        second_back[...] += matmul_rt(diff, expand_in[:, where])
        follow(n, after)
        return 0

    last = len(chunks) - 1
    forward_steps = {
        0: [(gather.spread, last)],
        1: [(reduce.start, 0)],
        3: [(reduce.exchange, 0), (reduce.start, 1)],
        5: [(reduce.start, 2), (reduce.exchange, 1)],
        7: [(reduce.start, 3), (reduce.exchange, 2)] + [(gather.share, n) for n in range(last)],
    }
    shrink_steps = {
        1: [(reduce.exchange, 3)],
        3: [(reduce.spread, 0)],
        7: [(reduce.spread, 1)],
    }
    backward_steps = {
        1: [(reduce.spread, 2)],
        2: [(reduce.spread, 3)],
        3: [(reduce.send, 0)],
        4: [(reduce.send, 1)],
        5: [(reduce.send, 2)],
        6: [(reduce.send, 3)],
    }
    lax.fori_loop(0, steps, lambda n, _: forward(n, forward_steps), 0)
    gather.share(last)
    for n in range(len(chunks)):
        gather.complete(n)
    done(gather.loads)
    lax.fori_loop(0, steps, lambda n, _: shrink(n, shrink_steps), 0)
    layer[...] = second_back[...].astype(bf16).reshape(layer.shape)
    second_back[...] = jnp.zeros_like(second_back)
    lax.fori_loop(0, steps, lambda n, _: backward(n, backward_steps), 0)
    store(steps - 2).wait()
    store(steps - 1).wait()
    go(out_loads)
    second_t[...] = attended[...].T

    def norm_back(i, sums):
        back = second_back[rows_at(i), :]
        part, normal = normalize_back(residual[rows_at(i), :], back, gain[...])
        total = upstream[rows_at(i), :].astype(f32) + part
        low = total.astype(bf16)
        residual_grad[rows_at(i), :] = total
        second[rows_at(i), :] = low
        found = (back * normal, back, low.astype(f32))
        return tuple(
            kept + jnp.sum(item, axis=0, keepdims=True) for kept, item in zip(sums, found)
        )

    nothing = jnp.zeros((1, features), f32)
    sums = lax.fori_loop(0, 8, norm_back, (nothing, nothing, nothing))
    gain_grad[...], shift_grad[...], out_bias_grad[...] = sums
    done(out_loads)
    branch_diff = second
    made = matmul_rt(branch_diff[:, halves[0]], staged[0])
    made = (made + matmul_rt(branch_diff[:, halves[1]], staged[1])).astype(bf16)
    attended_diff[...] = made.reshape(attended_diff.shape)
    for n, half in enumerate(halves):
        staged[n] = matmul(second_t[...], branch_diff[:, half]).astype(bf16)
        out_stores[n].start()
    reduce.finish()
    done(out_stores)
    copies.finish()


def feed_forward(shape, expand, contract, line, out_weight, tokens, upstream, attended, vectors):
    own, parts, piece = shape
    rows, features = tokens.shape
    hidden = expand.shape[1]
    wide = hidden // 8
    each = hidden // 32
    contract = split_weight(contract)
    chunks = chunks_of(0, *contract.shape[1:], 2)
    out_bias, gain, shift, expand_bias, contract_bias = [item.reshape(1, -1) for item in vectors]
    seq_shape = (own, parts, piece, features)
    return remote_call(
        functools.partial(feed_forward_kernel, chunks),
        "feed_forward",
        4,
        out_shape=(
            jax.ShapeDtypeStruct(seq_shape, bf16),
            jax.ShapeDtypeStruct((rows, features), f32),
            jax.ShapeDtypeStruct(seq_shape, bf16),
            jax.ShapeDtypeStruct((features, hidden), bf16),
            jax.ShapeDtypeStruct((features, features), bf16),
            jax.ShapeDtypeStruct((each, features), f32),
            jax.ShapeDtypeStruct((1, hidden), f32),
            *[jax.ShapeDtypeStruct((1, features), f32)] * 3,
        ),
        in_specs=[HBM] * 4 + [VMEM] * 8,
        out_specs=(VMEM, VMEM, VMEM, HBM, HBM) + (VMEM,) * 5,
        scratch_shapes=[
            pltpu.VMEM((features, hidden), bf16),
            pltpu.VMEM((4, *contract.shape), bf16),
            pltpu.VMEM((rows, features), f32),
            pltpu.VMEM((rows, features), bf16),
            pltpu.VMEM((features, rows), bf16),
            pltpu.VMEM((rows, hidden), f32),
            pltpu.VMEM((rows, hidden), bf16),
            pltpu.VMEM((4, 4, 2, each, features), bf16),
            pltpu.VMEM((2, features, wide), bf16),
            *reduce_lines_scratch(each, features),
            pltpu.SemaphoreType.DMA((8,)),
            pltpu.SemaphoreType.DMA((2,)),
            *semaphores(
                ReduceLines.copies + len(chunks) * (Gather.copies_each - 3),
                1 + 3 * len(chunks),
            ),
        ],
    )(
        expand, contract, line, out_weight,
        expand_bias, upstream, tokens, attended, out_bias, gain, shift, contract_bias,
    )


def backward_fused_kernel(heads, width, count, chunks, *refs):
    slopes, diff_in, qkv_in, out_t_in, lse_in, layer = refs[:6]
    grads, refs = refs[6 : 6 + count], refs[6 + count :]
    joined_out, layer_out, layer_own = refs[0], refs[1], refs[2 + count]
    outs, refs = refs[2 : 2 + count], refs[3 + count :]
    diff, qkv, out_t, lse, joined = refs[:5]
    attention = Backward(heads, width, slopes, qkv, diff, out_t, lse, joined, *refs[5:12])
    bufs, refs = refs[12 : 12 + 7 * len(chunks)], refs[12 + 7 * len(chunks) :]
    copies = Copies(*refs[3:])
    place = Place()
    s, plane = place.s, place.plane
    features = heads * width
    along = ReduceAlong(place, grads[0], outs[0], bufs[:7], chunks[0], copies)
    reduce = Reduce(place, grads, outs, bufs[7:], chunks[1:], copies)
    back = HandBack(place, joined, joined_out, 3 * features, *refs[:3])

    own = [copies.inside(diff_in.at[:, :, :, columns_of(s, features)], diff.at[:, :, s])]
    own += [copies.inside(a, b) for a, b in ((qkv_in, qkv), (out_t_in, out_t), (lse_in, lse))]
    arriving = [
        copies.plan(diff_in.at[:, :, :, columns_of(to[1], features)], diff.at[:, :, s], to)
        for to in plane
    ]
    returned = [copies.plan(layer.at[:, to[0]], layer_out.at[place.z], to) for to in place.lines]
    load_layer = copies.inside(layer.at[:, place.z], layer_own)
    keep_layer = copies.inside(layer_own, layer_out.at[place.z])
    go(own + reduce.loads + [along.load, load_layer])
    greet(place.lines + plane)
    go(arriving + [along.first])
    reduce.start()
    along.exchange()
    go(returned)
    for t in range(3):
        reduce.exchange(t)
    done(own + [load_layer])
    keep_layer.start()
    arrive(arriving)
    attention.run(
        {
            1: [(reduce.spread, 0)],
            2: [(along.spread,)],
            3: [(reduce.spread, 1), (reduce.spread, 2)],
            4: [(reduce.send, 0), (along.send,)],
            5: [(reduce.send, 1)],
            6: [(reduce.send, 2)],
        },
        back.each,
    )
    for t in range(3):
        reduce.finish(t)
    along.finish()
    back.finish()
    arrive(returned)
    copies.finish()
    keep_layer.wait()


def backward_fused(attended_diff, qkv, saved, layer, grads, slopes, heads, width):
    own, parts, piece, columns = attended_diff.shape
    features = heads * width
    length = parts * 8 * piece
    cut = [split_grad(item) for item in grads]
    count = len(cut)
    rows, wide = cut[0].shape[3:]
    part = 3 * wide // 8
    chunks = [
        (0, 0, rows, 0, wide // 4),
        (0, 0, rows, wide // 4, part),
        (0, 0, rows, wide // 4 + part, part),
        *chunks_of(1, *cut[1].shape[3:], 1),
    ]
    out = remote_call(
        functools.partial(backward_fused_kernel, heads, width, count, chunks),
        "backward_fused",
        2,
        out_shape=(
            jax.ShapeDtypeStruct((own, parts, piece, 24 * features), bf16),
            jax.ShapeDtypeStruct((parts, own, piece, columns), bf16),
            *[jax.ShapeDtypeStruct(item.shape[3:], f32) for item in cut],
        ),
        in_specs=[SMEM] + [HBM] * (5 + count),
        out_specs=(HBM, HBM) + (VMEM,) * count,
        scratch_shapes=[
            pltpu.VMEM((own, piece, columns), bf16),
            pltpu.VMEM((own, parts, 8, piece, features), bf16),
            pltpu.VMEM(qkv.shape, bf16),
            *[pltpu.VMEM(item.shape, f32) for item in saved],
            pltpu.VMEM(qkv.shape, bf16),
            *backward_scratch(length, heads, width),
            *reduce_along_scratch(chunks[0]),
            *reduce_scratch(chunks[1:]),
            *hand_back_semaphores(own * parts),
            *semaphores(10 + len(chunks) * Reduce.copies_each, len(chunks) + 6),
        ],
    )(slopes, attended_diff, qkv, *saved, layer, *cut)
    return out[0], out[1].reshape(parts * own, piece, columns), out[2:]


def end_kernel(
    width, joined_diff, joined_weight, tokens, residual_grad, gain, shift, out_bias_grad,
    second_gain_grad, second_shift_grad, contract_bias_grad, expand_bias_grad,
    input_out, vector_out, out,
    diff_in, weight_in, normed, normed_t, back, grads, held, vectors, others, ranks, *refs,
):
    count = grads.shape[0]
    bufs, refs = refs[: 7 * count], refs[7 * count :]
    loaded, copies = refs[0], Copies(*refs[1:])
    place = Place()
    z, lines, plane = place.z, place.lines, place.plane
    rows, features = tokens.shape
    own_seqs, parts, piece, _ = held.shape
    columns = [pl.ds(features * n, features) for n in range(count)]
    chunks = [(n, 0, grads.shape[4], 0, features) for n in range(count)]
    outs = [out.at[:, where] for where in columns]
    reduce = Reduce(place, [grads.at[n] for n in range(count)], outs, bufs, chunks, copies)
    loads = [
        (
            pltpu.make_async_copy(joined_diff.at[:, c], diff_in.at[:, c], loaded.at[0, n]),
            pltpu.make_async_copy(joined_weight.at[:, c], weight_in.at[:, c], loaded.at[1, n]),
        )
        for n, c in enumerate(columns)
    ]
    returned = [copies.plan(held.at[:, to[0]], input_out.at[z], to) for to in lines]
    stay = copies.inside(held.at[:, z], input_out.at[z])
    along = [copies.plan(vectors.at[to[0]], others.at[k], to) for k, to in enumerate(lines)]
    across = [copies.plan(ranks.at[0], ranks.at[d + 1], to) for d, to in enumerate(plane)]

    for load in loads:
        go(load)
    greet(lines + plane)
    for n, where in enumerate(columns):
        done(loads[n])
        part = matmul_rt(diff_in[:, where], weight_in[:, where])
        back[...] = part if n == 0 else back[...] + part

    def norm_back(i, sums):
        at = pl.ds(pl.multiple_of(i * piece, piece), piece)
        values, given = tokens[at, :].astype(f32), back[at, :]
        part, normal = normalize_back(values, given, gain[...])
        normed[at, :] = (normal * gain[...] + shift[...]).astype(bf16)
        total = (residual_grad[at, :] + part).astype(bf16)
        held[i // parts, i % parts] = total
        found = (given * normal, given)
        return tuple(
            kept + jnp.sum(item, axis=0, keepdims=True) for kept, item in zip(sums, found)
        )

    nothing = jnp.zeros((1, features), f32)
    gain_grad, shift_grad = lax.fori_loop(0, own_seqs * parts, norm_back, (nothing, nothing))
    go(returned + [stay])
    normed_t[...] = normed[...].T
    sums = []
    for n, where in enumerate(columns):
        made = matmul(normed_t[...], diff_in[:, where]).astype(bf16)
        grads[n] = made.reshape(grads.shape[1:])
        reduce.begin(n)
        sums.append(jnp.sum(diff_in[:, where].astype(f32), axis=0, keepdims=True))
        if n > 0:
            reduce.exchange(n - 1)

    sums = jnp.concatenate(sums, axis=1)
    low = lax.broadcasted_iota(jnp.int32, (1, 128), 1) < width
    query_grad, value_grad = [], []
    for r in range(features // 128):
        first, middle, last = [sums[:, (3 * r + n) * 128 : (3 * r + n + 1) * 128] for n in range(3)]
        query_grad.append(jnp.where(low, first, middle))
        value_grad.append(jnp.where(low, middle, last))
    given = [
        gain_grad, shift_grad, jnp.concatenate(query_grad, axis=1),
        jnp.concatenate(value_grad, axis=1), out_bias_grad[...], second_gain_grad[...],
        second_shift_grad[...], contract_bias_grad[...], expand_bias_grad[...],
    ]
    row = 0
    for item in given:
        each = item.shape[1] // 512
        for k in range(4):
            for r in range(each):
                start = (k * each + r) * 128
                vectors[k, row + r : row + r + 1, :] = item[:, start : start + 128]
        row += each
    go(along)
    reduce.spread(0)
    reduce.exchange(count - 1)
    arrive(along)
    total = vectors[z]
    for k in range(3):
        total = total + others[k]
    ranks[0] = total
    go(across)
    for n in range(1, count):
        reduce.send(n - 1)
        reduce.spread(n)
    reduce.send(count - 1)
    arrive(across)
    total = ranks[0]
    for d in range(1, 8):
        total = total + ranks[d]
    vector_out[...] = total
    for n in range(count):
        reduce.finish(n)
    arrive(returned)
    copies.finish()
    stay.wait()


def end(shape, joined_diff, joined_weight, tokens, residual_grad, gain, shift, vectors, width):
    own, parts, piece = shape
    rows, features = tokens.shape
    count = joined_diff.shape[1] // features
    each = features // 32
    vectors = [item.reshape(1, -1) for item in (gain, shift, *vectors)]
    tall = (4 * features + sum(item.shape[1] for item in vectors[2:])) // 512
    chunks = [(n, 0, each, 0, features) for n in range(count)]
    out = remote_call(
        functools.partial(end_kernel, width),
        "end",
        3,
        out_shape=(
            jax.ShapeDtypeStruct((parts, own, piece, features), bf16),
            jax.ShapeDtypeStruct((tall, 128), f32),
            jax.ShapeDtypeStruct((each, count * features), f32),
        ),
        in_specs=[HBM, HBM] + [VMEM] * (2 + len(vectors)),
        out_specs=(HBM, VMEM, VMEM),
        scratch_shapes=[
            pltpu.VMEM((rows, count * features), bf16),
            pltpu.VMEM((features, count * features), bf16),
            pltpu.VMEM((rows, features), bf16),
            pltpu.VMEM((features, rows), bf16),
            pltpu.VMEM((rows, features), f32),
            pltpu.VMEM((count, 4, 4, 2, each, features), bf16),
            pltpu.VMEM((own, parts, piece, features), bf16),
            pltpu.VMEM((4, tall, 128), f32),
            pltpu.VMEM((3, tall, 128), f32),
            pltpu.VMEM((8, tall, 128), f32),
            *reduce_scratch(chunks),
            pltpu.SemaphoreType.DMA((2, count)),
            *semaphores(3 + 3 + 7 + count * Reduce.copies_each, 1 + count),
        ],
    )(joined_diff, joined_weight, tokens, residual_grad, *vectors)
    each = features // 32
    split = 8 * features // 512
    place = lax.axis_index("sp")
    short = out[1][:split].reshape(8, features // 4)
    short = lax.dynamic_slice_in_dim(short, place * each, each, 1)
    long = out[1][split:].reshape(-1)
    size = long.shape[0] // 8
    long = lax.dynamic_slice_in_dim(long, place * size, size)
    own_grads = [short[n] for n in range(8)] + [long]
    return out[0].reshape(parts * own, piece, features), own_grads, out[2]


def per_device(
    layer_input,
    first_gain,
    first_shift,
    joined_weight,
    query_bias,
    value_bias,
    output_weight,
    output_bias,
    second_gain,
    second_shift,
    expand_weight,
    expand_bias,
    contract_weight,
    contract_bias,
    alibi_slopes,
    upstream,
):
    seqs, piece, features = layer_input.shape
    fs_count = lax.axis_size("fs")
    sp_count = lax.axis_size("sp")
    head_count = alibi_slopes.shape[0]
    width = features // head_count
    heads = head_count // sp_count
    rows = seqs * piece
    own = seqs // fs_count
    shape = (own, fs_count, piece)
    slopes = lax.dynamic_slice_in_dim(alibi_slopes, lax.axis_index("sp") * heads, heads)

    vectors = (
        first_gain, first_shift, query_bias, value_bias, output_bias,
        second_gain, second_shift, contract_bias, expand_bias,
    )
    fast = (fs_count, sp_count) == (4, 8) and (own, heads, width) == (2, 2, 64)
    fast = fast and expand_weight.shape[1] == 4 * features
    weights = (joined_weight, output_weight, expand_weight)
    gather = lambda item: lax.all_gather(item, "fs", axis=0, tiled=True)
    if fast:
        tokens, whole, weights, qkv, attended, saved, upstream_low = forward_fused(
            layer_input, upstream, vectors, weights, contract_weight, slopes, heads, width
        )
    else:
        tokens, upstream_low = to_own_seqs(layer_input), to_own_seqs(upstream)
        whole = [gather(item) for item in vectors]
        weights = [gather(item) for item in (*weights, contract_weight)]
    joined_full, out_full, expand_full, contract_full = weights
    tokens_low = tokens.reshape(rows, features)
    tokens = tokens_low.astype(f32)
    gain_one, shift_one, qbias, vbias, obias, gain_two, shift_two, cbias, ebias = [
        item.astype(f32) for item in whole
    ]

    normed_f, norm_back_one = jax.vjp(normalize, tokens, gain_one, shift_one)
    normed = normed_f.astype(bf16)
    if not fast:
        joined_bias = joined_bias_of(qbias, vbias, head_count)
        joined_all = (matmul(normed, joined_full) + joined_bias).astype(bf16)
        qkv = to_heads(joined_all.reshape(*shape, 3 * features))
        attended, *saved = attention_forward(qkv, slopes, heads, width)
        attended = from_heads(attended)
    attended = attended.reshape(rows, features)
    upstream_low = upstream_low.reshape(rows, features)

    upstream_f = upstream_low.astype(f32)
    contract_bias_grad = jnp.sum(upstream_f, axis=0)
    if fast:
        (
            layer_output, residual_grad, attended_diff, expand_grad, output_weight_grad,
            contract_grad, *small,
        ) = feed_forward(
            shape, expand_full, contract_weight, contract_full, out_full, tokens_low, upstream_low,
            attended, (obias, gain_two, shift_two, ebias, cbias),
        )
        expand_bias_grad, second_gain_grad, second_shift_grad, output_bias_grad = [
            item.reshape(-1) for item in small
        ]
    else:
        residual = tokens + (matmul(attended, out_full) + obias)
        second_f, norm_back_two = jax.vjp(normalize, residual, gain_two, shift_two)
        second = second_f.astype(bf16)
        expanded = matmul(second, expand_full) + ebias
        activated_f, gelu_back = jax.vjp(gelu_tanh, expanded)
        activated = activated_f.astype(bf16)
        result = residual + (matmul(activated, contract_full) + cbias)
        layer_output = result.astype(bf16).reshape(*shape, features)

        contract_grad = matmul_lt(activated, upstream_low)
        act_grad = matmul_rt(upstream_low, contract_full)
        expand_diff = gelu_back(act_grad)[0].astype(bf16)
        expand_grad = matmul_lt(second, expand_diff)
        expand_bias_grad = jnp.sum(expand_diff.astype(f32), axis=0)
        second_back = matmul_rt(expand_diff, expand_full)
        resid_part, second_gain_grad, second_shift_grad = norm_back_two(second_back)
        residual_grad = upstream_f + resid_part

        branch_diff = residual_grad.astype(bf16)
        output_weight_grad = matmul_lt(attended, branch_diff)
        output_bias_grad = jnp.sum(branch_diff.astype(f32), axis=0)
        attended_diff = matmul_rt(branch_diff, out_full).astype(bf16)
        attended_diff = attended_diff.reshape(*shape, features)
    grads = (expand_grad, output_weight_grad)
    scatter = functools.partial(
        lax.psum_scatter, axis_name=("fs", "sp"), scatter_dimension=0, tiled=True
    )
    if fast:
        joined_diff, layer_output, grads = backward_fused(
            attended_diff, qkv, saved, layer_output, [item.astype(bf16) for item in grads],
            slopes, heads, width,
        )
    else:
        joined_diff = attention_backward(
            qkv, to_heads(attended_diff), *saved, slopes, heads, width
        )
        joined_diff, layer_output = from_heads(joined_diff), from_own_seqs(layer_output)
        grads = [scatter(item) for item in grads]
        contract_grad = scatter(contract_grad)
    expand_grad, output_weight_grad = grads
    joined_diff = joined_diff.reshape(rows, 3 * features)

    if fast:
        input_grad, own_grads, joined_grad = end(
            shape, joined_diff, joined_full, tokens_low, residual_grad, gain_one, shift_one,
            (
                output_bias_grad, second_gain_grad, second_shift_grad, contract_bias_grad,
                expand_bias_grad,
            ),
            width,
        )
    else:
        joined_grad = matmul_lt(normed, joined_diff)
        column_sums = jnp.sum(joined_diff.astype(f32), axis=0).reshape(head_count, 3, width)
        query_bias_grad = column_sums[:, 0].reshape(features)
        value_bias_grad = column_sums[:, 2].reshape(features)
        normed_back = matmul_rt(joined_diff, joined_full)
        input_part, first_gain_grad, first_shift_grad = norm_back_one(normed_back)
        input_grad = (residual_grad + input_part).astype(bf16).reshape(*shape, features)

        vector_grads = (
            first_gain_grad, first_shift_grad, query_bias_grad, value_bias_grad,
            output_bias_grad, second_gain_grad, second_shift_grad, contract_bias_grad,
            expand_bias_grad,
        )
        devices = fs_count * sp_count
        packed = jnp.concatenate([item.reshape(devices, -1) for item in vector_grads], axis=1)
        input_grad, joined_grad = from_own_seqs(input_grad), scatter(joined_grad)
        packed = scatter(packed.reshape(-1))
        own_grads, at = [], 0
        for item in vector_grads:
            size = item.shape[0] // devices
            own_grads.append(packed[at : at + size])
            at += size
    g1, s1, qb, vb, ob, g2, s2, cb, eb = own_grads
    return (
        layer_output,
        input_grad,
        g1,
        s1,
        joined_grad,
        qb,
        vb,
        output_weight_grad,
        ob,
        g2,
        s2,
        expand_grad,
        eb,
        contract_grad,
        cb,
    )


def solution(mesh):
    tokens = P(None, ("fs", "sp"), None)
    both, both_rows = P(("fs", "sp")), P(("fs", "sp"), None)
    one, one_rows = P("fs"), P("fs", None)
    return jax.shard_map(
        per_device,
        mesh=mesh,
        in_specs=(
            tokens, one, one, one_rows, one, one, one_rows, one, one, one, one_rows, one,
            one_rows, one, P(), tokens,
        ),
        out_specs=(
            tokens, tokens, both, both, both_rows, both, both, both_rows, both, both, both,
            both_rows, both, both_rows, both,
        ),
        check_vma=False,
    )
```

```python
import functools
import math

import jax
import jax.numpy as jnp
from jax import lax
from jax.experimental import pallas as pl
from jax.experimental.pallas import tpu as pltpu
from jax.sharding import PartitionSpec as P

norm_eps = 1e-05
gelu_coef = 0.7978845608028654
masked_value = -1e30
f32 = jnp.float32
bf16 = jnp.bfloat16
MESH = pl.DeviceIdType.MESH
HBM = pl.BlockSpec(memory_space=pl.ANY)
VMEM = pl.BlockSpec(memory_space=pltpu.VMEM)
SMEM = pl.BlockSpec(memory_space=pltpu.SMEM)
vmem_bytes = 63 * 1024 * 1024


def normalize(values, norm_gain, norm_shift):
    center = values - jnp.mean(values, axis=-1, keepdims=True)
    variance = jnp.mean(center * center, axis=-1, keepdims=True)
    return center * lax.rsqrt(variance + norm_eps) * norm_gain + norm_shift


def normalize_back(values, back, norm_gain):
    center = values - jnp.mean(values, axis=-1, keepdims=True)
    inverse = lax.rsqrt(jnp.mean(center * center, axis=-1, keepdims=True) + norm_eps)
    normal = center * inverse
    scaled = back * norm_gain
    even = jnp.mean(scaled, axis=-1, keepdims=True)
    along = jnp.mean(scaled * normal, axis=-1, keepdims=True)
    return inverse * (scaled - even - normal * along), normal


def gelu_tanh(values):
    return (
        0.5 * values * (1.0 + jnp.tanh(gelu_coef * (values + 0.044715 * values * values * values)))
    )


def matmul(left_side, right_side):
    return jnp.dot(left_side, right_side, preferred_element_type=f32)


def matmul_lt(left_side, right_side):
    return lax.dot_general(
        left_side, right_side, (((0,), (0,)), ((), ())), preferred_element_type=f32
    )


def matmul_rt(left_side, right_side):
    return lax.dot_general(
        left_side, right_side, (((1,), (1,)), ((), ())), preferred_element_type=f32
    )


def joined_bias_of(query_bias, value_bias, head_count):
    query_part = query_bias.astype(f32).reshape(head_count, -1)
    value_part = value_bias.astype(f32).reshape(head_count, -1)
    return jnp.stack([query_part, jnp.zeros_like(query_part), value_part], axis=1).reshape(-1)


def split_three(values):
    high = values.astype(bf16).astype(f32)
    rest = values - high
    middle = rest.astype(bf16).astype(f32)
    return high, middle, rest - middle


def key_columns(key_rows, slope, start):
    rows, width = key_rows.shape
    position = (start + lax.broadcasted_iota(jnp.int32, (rows, width), 0)).astype(f32)
    lane = lax.broadcasted_iota(jnp.int32, (rows, width), 1)
    high, middle, low = split_three(slope * position)
    extra = jnp.where(lane == 0, high, jnp.where(lane == 1, middle, jnp.where(lane == 2, low, 0.0)))
    return jnp.concatenate([key_rows.astype(f32), extra], axis=1).astype(bf16)


def query_columns(queries, scale):
    rows, width = queries.shape
    lane = lax.broadcasted_iota(jnp.int32, (rows, width), 1)
    ones = jnp.where(lane < 3, 1.0, 0.0)
    return jnp.concatenate([queries.astype(f32) * scale, ones], axis=1).astype(bf16)


def follow(n, after):
    for at, steps in after.items():

        def act(steps=steps):
            for step, *given in steps:
                step(*given)

        pl.when(n == at)(act)


class Forward:
    def __init__(self, heads, width, slopes, qkv, out, out_t, lse, keys, queries, values_t):
        self.heads, self.width, self.slopes, self.qkv, self.out = heads, width, slopes, qkv, out
        self.out_t, self.lse = out_t, lse
        self.keys, self.queries, self.values_t = keys, queries, values_t
        self.head = 0
        self.blocks = qkv.shape[1]
        self.block = qkv.shape[2] * qkv.shape[3]

    def rows(self, i):
        return pl.ds(pl.multiple_of(i * self.block, self.block), self.block)

    def prepare(self, b):
        width, block, qkv = self.width, self.block, self.qkv
        scale = 1.0 / math.sqrt(width)

        def body(i, _):
            rows = self.rows(i)
            for h in range(self.heads):
                base = h * 3 * width
                query, key, value = [
                    qkv[b, i, :, :, base + n * width : base + (n + 1) * width].reshape(block, width)
                    for n in range(3)
                ]
                self.keys[h, rows, :] = key_columns(key, self.slopes[self.head + h], i * block)
                self.queries[h, rows, :] = query_columns(query, scale)
                self.values_t[h, :, rows] = value.astype(f32).T.astype(bf16)
            return 0

        lax.fori_loop(0, self.blocks, body, 0)

    def one(self, b, i):
        heads, width, block = self.heads, self.width, self.block
        rows = self.rows(i)
        query = [self.queries[h, rows, :] for h in range(heads)]

        def step(j, state, diagonal):
            columns = self.rows(j)
            result = []
            for h in range(heads):
                top, total, acc = state[h]
                scores = matmul_rt(self.keys[h, columns, :], query[h])
                if diagonal:
                    key_at = lax.broadcasted_iota(jnp.int32, (block, block), 0)
                    query_at = lax.broadcasted_iota(jnp.int32, (block, block), 1)
                    scores = jnp.where(key_at <= query_at, scores, masked_value)
                newest = jnp.maximum(top, jnp.max(scores, axis=0, keepdims=True))
                shrink = jnp.exp(top - newest)
                probs = jnp.exp(scores - newest)
                total = total * shrink + jnp.sum(probs, axis=0, keepdims=True)
                acc = acc * shrink + matmul(self.values_t[h, :, columns], probs.astype(bf16))
                result.append((newest, total, acc))
            return tuple(result)

        state = tuple(
            (
                jnp.full((1, block), masked_value, f32),
                jnp.zeros((1, block), f32),
                jnp.zeros((width, block), f32),
            )
            for h in range(heads)
        )
        state = lax.fori_loop(0, i, lambda j, s: step(j, s, False), state)
        state = step(i, state, True)
        finished = []
        for h in range(heads):
            top, total, acc = state[h]
            result = acc / total
            self.out_t[b, h, :, rows] = result
            self.lse[b, h, :, rows] = top + jnp.log(total)
            finished.append(result)
        joined = finished[0] if heads == 1 else jnp.concatenate(finished, axis=0)
        self.out[b, i] = joined.T.astype(bf16).reshape(self.out.shape[2:])

    def run(self, after, each=None):
        blocks = self.blocks

        def body(n, _):
            b, i = n // blocks, n % blocks
            pl.when(i == 0)(lambda: self.prepare(b))
            self.one(b, i)
            if each is not None:
                each(b, i)
            follow(n, after)
            return 0

        lax.fori_loop(0, self.qkv.shape[0] * blocks, body, 0)


def forward_kernel(heads, width, *refs):
    Forward(heads, width, *refs).run({})


def saved_shapes(seqs, length, heads, width):
    return (
        jax.ShapeDtypeStruct((seqs, heads, width, length), f32),
        jax.ShapeDtypeStruct((seqs, heads, 1, length), f32),
    )


def forward_scratch(length, heads, width):
    return [
        pltpu.VMEM((heads, length, 2 * width), bf16),
        pltpu.VMEM((heads, length, 2 * width), bf16),
        pltpu.VMEM((heads, width, length), bf16),
    ]


def attention_forward(qkv, slopes, heads, width):
    seqs, blocks, ranks, piece, _ = qkv.shape
    length = blocks * ranks * piece
    return pl.pallas_call(
        functools.partial(forward_kernel, heads, width),
        name="attention_forward",
        out_shape=(
            jax.ShapeDtypeStruct((seqs, blocks, ranks, piece, heads * width), bf16),
            *saved_shapes(seqs, length, heads, width),
        ),
        in_specs=[SMEM, VMEM],
        out_specs=(VMEM, VMEM, VMEM),
        scratch_shapes=forward_scratch(length, heads, width),
        compiler_params=pltpu.CompilerParams(vmem_limit_bytes=vmem_bytes),
    )(slopes, qkv)


class Backward:
    def __init__(
        self, heads, width, slopes, qkv, diff, out_t, lse, joined,
        keys, queries, keys_t, values, diffs, delta, query_acc,
    ):
        self.heads, self.width, self.slopes, self.qkv, self.diff = heads, width, slopes, qkv, diff
        self.out_t, self.lse, self.joined = out_t, lse, joined
        self.keys, self.queries, self.keys_t, self.values = keys, queries, keys_t, values
        self.diffs, self.delta, self.query_acc = diffs, delta, query_acc
        self.head = 0
        self.blocks = qkv.shape[1]
        self.block = qkv.shape[2] * qkv.shape[3]

    def rows(self, i):
        return pl.ds(pl.multiple_of(i * self.block, self.block), self.block)

    def prepare(self, b):
        width, block, qkv = self.width, self.block, self.qkv
        scale = 1.0 / math.sqrt(width)

        def body(i, _):
            rows = self.rows(i)
            for h in range(self.heads):
                base = h * 3 * width
                query, key, value = [
                    qkv[b, i, :, :, base + n * width : base + (n + 1) * width].reshape(block, width)
                    for n in range(3)
                ]
                self.keys[h, rows, :] = key_columns(key, self.slopes[self.head + h], i * block)
                self.keys_t[h, :, rows] = key.astype(f32).T.astype(bf16)
                self.queries[h, rows, :] = query_columns(query, scale)
                self.values[h, rows, :] = value
                part = self.diff[b, i, :, :, h * width : (h + 1) * width].reshape(block, width)
                self.diffs[h, rows, :] = part
                self.delta[h, :, rows] = jnp.sum(
                    part.astype(f32).T * self.out_t[b, h, :, rows], axis=0, keepdims=True
                )
                self.query_acc[h, :, rows] = jnp.zeros((width, block), f32)
            return 0

        lax.fori_loop(0, self.blocks, body, 0)

    def one(self, b, j):
        heads, width, block = self.heads, self.width, self.block
        tail = self.joined.shape[2:4] + (width,)
        columns = self.rows(j)

        def step(i, state, diagonal):
            rows = self.rows(i)
            result = []
            for h in range(heads):
                key_acc, value_acc = state[h]
                query = self.queries[h, rows, :]
                part = self.diffs[h, rows, :]
                scores = matmul_rt(self.keys[h, columns, :], query)
                probs = jnp.exp(scores - self.lse[b, h, :, rows])
                if diagonal:
                    key_at = lax.broadcasted_iota(jnp.int32, (block, block), 0)
                    query_at = lax.broadcasted_iota(jnp.int32, (block, block), 1)
                    probs = jnp.where(key_at <= query_at, probs, 0.0)
                prob_diff = matmul_rt(self.values[h, columns, :], part)
                score_diff = (probs * (prob_diff - self.delta[h, :, rows])).astype(bf16)
                value_acc = value_acc + matmul(probs.astype(bf16), part)
                key_acc = key_acc + matmul(score_diff, query)
                self.query_acc[h, :, rows] += matmul(self.keys_t[h, :, columns], score_diff)
                result.append((key_acc, value_acc))
            return tuple(result)

        state = tuple(
            (jnp.zeros((block, 2 * width), f32), jnp.zeros((block, width), f32))
            for h in range(heads)
        )
        state = step(j, state, True)
        state = lax.fori_loop(j + 1, self.blocks, lambda i, s: step(i, s, False), state)
        for h in range(heads):
            base = (h * 3 + 1) * width
            key_acc, value_acc = state[h]
            self.joined[b, j, :, :, base : base + width] = (
                key_acc[:, :width].astype(bf16).reshape(tail)
            )
            self.joined[b, j, :, :, base + width : base + 2 * width] = value_acc.astype(
                bf16
            ).reshape(tail)

    def run(self, after, each=None):
        blocks = self.blocks

        def body(n, _):
            b, j = n // blocks, n % blocks
            pl.when(j == 0)(lambda: self.prepare(b))
            self.one(b, j)
            self.finish(b, j)
            if each is not None:
                each(b, j)
            follow(n, after)
            return 0

        lax.fori_loop(0, self.qkv.shape[0] * blocks, body, 0)

    def finish(self, b, j):
        width = self.width
        scale = 1.0 / math.sqrt(width)
        for h in range(self.heads):
            base = h * 3 * width
            result = (self.query_acc[h, :, self.rows(j)] * scale).T.astype(bf16)
            self.joined[b, j, :, :, base : base + width] = result.reshape(
                self.joined.shape[2:4] + (width,)
            )


def backward_kernel(heads, width, *refs):
    Backward(heads, width, *refs).run({})


def backward_scratch(length, heads, width):
    return [
        pltpu.VMEM((heads, length, 2 * width), bf16),
        pltpu.VMEM((heads, length, 2 * width), bf16),
        pltpu.VMEM((heads, width, length), bf16),
        pltpu.VMEM((heads, length, width), bf16),
        pltpu.VMEM((heads, length, width), bf16),
        pltpu.VMEM((heads, 1, length), f32),
        pltpu.VMEM((heads, width, length), f32),
    ]


def attention_backward(qkv, diff, out_t, lse, slopes, heads, width):
    length = qkv.shape[1] * qkv.shape[2] * qkv.shape[3]
    return pl.pallas_call(
        functools.partial(backward_kernel, heads, width),
        name="attention_backward",
        out_shape=jax.ShapeDtypeStruct(qkv.shape, bf16),
        in_specs=[SMEM, VMEM, VMEM, VMEM, VMEM],
        out_specs=VMEM,
        scratch_shapes=backward_scratch(length, heads, width),
        compiler_params=pltpu.CompilerParams(vmem_limit_bytes=vmem_bytes),
    )(slopes, qkv, diff, out_t, lse)


def to_own_seqs(values):
    seqs, piece, features = values.shape
    parts = lax.axis_size("fs")
    values = values.reshape(parts, seqs // parts, piece, features)
    return lax.all_to_all(values, "fs", split_axis=0, concat_axis=0).transpose(1, 0, 2, 3)


def from_own_seqs(values):
    own, parts, piece, features = values.shape
    values = lax.all_to_all(values.transpose(1, 0, 2, 3), "fs", split_axis=0, concat_axis=0)
    return values.reshape(parts * own, piece, features)


def to_heads(values):
    own, parts, piece, features = values.shape
    ranks = lax.axis_size("sp")
    values = values.reshape(own, parts, piece, ranks, features // ranks)
    return lax.all_to_all(values, "sp", split_axis=3, concat_axis=2)


def from_heads(values):
    own, parts, ranks, piece, features = values.shape
    values = lax.all_to_all(values, "sp", split_axis=2, concat_axis=3)
    return values.reshape(own, parts, piece, ranks * features)


class Copies:
    def __init__(self, send, recv, local):
        self.send, self.recv, self.local = send, recv, local
        self.used, self.used_local, self.made = 0, 0, []

    def plan(self, source, target, device):
        copy = pltpu.make_async_remote_copy(
            src_ref=source,
            dst_ref=target,
            send_sem=self.send.at[self.used],
            recv_sem=self.recv.at[self.used],
            device_id=device,
            device_id_type=MESH,
        )
        self.used += 1
        self.made.append(copy)
        return copy

    def inside(self, source, target):
        copy = pltpu.make_async_copy(source, target, self.local.at[self.used_local])
        self.used_local += 1
        return copy

    def finish(self):
        assert (self.used, self.used_local) == (self.send.shape[0], self.local.shape[0])
        for copy in self.made:
            copy.wait_send()


def go(copies):
    for copy in copies:
        copy.start()


def arrive(copies):
    for copy in copies:
        copy.wait_recv()


def done(copies):
    for copy in copies:
        copy.wait()


def greet(devices):
    barrier = pltpu.get_barrier_semaphore()
    for device in devices:
        pl.semaphore_signal(barrier, inc=1, device_id=device, device_id_type=MESH)
    pl.semaphore_wait(barrier, len(devices))


class Place:
    def __init__(self):
        z, s = lax.axis_index("fs"), lax.axis_index("sp")
        self.z, self.s = z, s
        self.core, self.chip = s % 2, s // 2
        self.x, self.y = self.chip % 2, self.chip // 2
        self.along_x = s + 2 - 4 * self.x
        self.along_y = s + 4 - 8 * self.y
        self.partner = s + 1 - 2 * self.core
        self.diagonal = self.along_x + self.along_y - s
        self.chip_x, self.chip_y = self.along_x // 2, self.along_y // 2
        self.lines = [(lax.rem(z + k, 4), s) for k in range(1, 4)]
        self.plane = [(z, lax.rem(s + d, 8)) for d in range(1, 8)]
        self.to_x, self.to_y, self.to_core = [
            (z, to) for to in (self.along_x, self.along_y, self.partner)
        ]
        self.near = self.lines + [self.to_x, self.to_y, self.to_core]


class Gather:
    copies_each = 33

    def __init__(self, place, weights, wholes, kept, chunks, copies, given=None):
        z, s, lines = place.z, place.s, place.lines
        self.ready = arrive if given is None else done
        self.loads, self.own = [], []
        for weight, whole, keep in zip(weights, wholes, kept):
            if keep is None:
                self.loads.append(copies.inside(weight, whole.at[z]))
            else:
                self.loads.append(copies.inside(weight, keep))
                self.own.append(copies.inside(keep, whole.at[z]))
        self.first, self.second, self.third, self.cores, self.last = [], [], [], [], []
        for t, row, rows, column, columns in chunks:
            whole = wholes[t]
            wide = pl.ds(column, columns)
            every = pl.ds(row, rows)
            low, high = pl.ds(row, rows // 2), pl.ds(row + rows // 2, rows // 2)

            def same(k, rank, part, to):
                where = (k, rank, part, wide)
                return copies.plan(whole.at[where], whole.at[where], to)

            if given is None:
                first = [
                    copies.plan(weights[t].at[s, every, wide], whole.at[z, s, every, wide], to)
                    for to in lines
                ]
            else:
                first = [
                    copies.inside(given.at[k, every, wide], whole.at[k, s, every, wide])
                    for k, _ in lines
                ]
            self.first.append(first)
            second, third, cores, last = [], [], [], []
            for k, _ in lines:
                second.append(same(k, s, low, place.to_x))
                second.append(same(k, s, high, place.to_y))
                cores.append(same(k, s, every, place.to_core))
                third.append(same(k, s, low, place.to_y))
                third.append(same(k, s, high, place.to_x))
                third.append(same(k, place.along_x, low, place.to_y))
                third.append(same(k, place.along_y, high, place.to_x))
                for rank in (place.along_x, place.along_y, place.diagonal):
                    last.append(same(k, rank, every, place.to_core))
            self.second.append(second)
            self.third.append(third)
            self.cores.append(cores)
            self.last.append(last)

    def keep(self):
        done(self.loads)
        go(self.own)

    def start(self, t):
        go(self.first[t])

    def exchange(self, t):
        self.ready(self.first[t])
        go(self.second[t])
        go(self.cores[t])

    def spread(self, t):
        arrive(self.second[t])
        go(self.third[t])

    def share(self, t):
        arrive(self.third[t])
        go(self.last[t])

    def complete(self, t):
        arrive(self.cores[t] + self.last[t])


def add_into(target, other):
    target[...] = (target[...].astype(f32) + other[...].astype(f32)).astype(target.dtype)


def add_blocks(steps, block_of):
    def body(i, _):
        add_into(*block_of(i))
        return 0

    lax.fori_loop(0, steps, body, 0)


class Reduce:
    copies_each = 10

    def __init__(self, place, grads, outs, bufs, chunks, copies):
        self.place, self.outs, self.chunks = place, outs, chunks
        self.bufs = [bufs[7 * t : 7 * t + 7] for t in range(len(chunks))]
        self.loads, self.first, self.second, self.third, self.fourth = [], [], [], [], []
        for (t, row, rows, column, columns), buf in zip(chunks, self.bufs):
            own, from_core, from_x, from_y, late_y, late_x, from_z = buf
            every, wide = pl.ds(row, rows), pl.ds(column, columns)
            low, high = pl.ds(0, rows // 2), pl.ds(rows // 2, rows // 2)
            self.loads.append(
                copies.inside(grads[t].at[:, :, place.core, every, wide], own)
            )
            self.first.append(
                copies.plan(
                    grads[t].at[:, :, 1 - place.core, every, wide], from_core, place.to_core
                )
            )
            step = []
            for k in range(2):
                step.append(
                    copies.plan(own.at[:, 2 * k + 1 - place.x, low], from_x.at[:, k], place.to_x)
                )
                step.append(
                    copies.plan(
                        own.at[:, 2 * (1 - place.y) + k, high], from_y.at[:, k], place.to_y
                    )
                )
            self.second.append(step)
            self.third.append(
                [
                    copies.plan(own.at[:, place.chip_y, low], late_y, place.to_y),
                    copies.plan(own.at[:, place.chip_x, high], late_x, place.to_x),
                ]
            )
            self.fourth.append(
                [
                    copies.plan(own.at[to[0], place.chip], from_z.at[k], to)
                    for k, to in enumerate(place.lines)
                ]
            )

    def start(self):
        go(self.first)

    def begin(self, t):
        go([self.loads[t], self.first[t]])

    def halves(self, t):
        half = self.chunks[t][2] // 2
        return pl.ds(0, half), pl.ds(half, half)

    def exchange(self, t):
        own, from_core = self.bufs[t][:2]
        self.loads[t].wait()
        arrive([self.first[t]])
        add_blocks(16, lambda i: (own.at[i // 4, i % 4], from_core.at[i // 4, i % 4]))
        go(self.second[t])

    def spread(self, t):
        own, _, from_x, from_y = self.bufs[t][:4]
        low, high = self.halves(t)
        x, y = self.place.x, self.place.y
        arrive(self.second[t])
        add_blocks(8, lambda i: (own.at[i // 2, 2 * (i % 2) + x, low], from_x.at[i // 2, i % 2]))
        add_blocks(8, lambda i: (own.at[i // 2, 2 * y + i % 2, high], from_y.at[i // 2, i % 2]))
        go(self.third[t])

    def send(self, t):
        own, _, _, _, late_y, late_x, _ = self.bufs[t]
        low, high = self.halves(t)
        chip = self.place.chip
        arrive(self.third[t])
        add_blocks(4, lambda i: (own.at[i, chip, low], late_y.at[i]))
        add_blocks(4, lambda i: (own.at[i, chip, high], late_x.at[i]))
        go(self.fourth[t])

    def finish(self, t):
        own, from_z = self.bufs[t][0], self.bufs[t][6]
        index, row, rows, column, columns = self.chunks[t]
        arrive(self.fourth[t])
        total = own[self.place.z, self.place.chip].astype(f32)
        for k in range(3):
            total = total + from_z[k].astype(f32)
        self.outs[index][row : row + rows, column : column + columns] = total


def reduce_scratch(chunks):
    scratch = []
    for _, _, rows, _, columns in chunks:
        half = rows // 2
        scratch += [
            pltpu.VMEM((4, 4, rows, columns), bf16),
            pltpu.VMEM((4, 4, rows, columns), bf16),
            pltpu.VMEM((4, 2, half, columns), bf16),
            pltpu.VMEM((4, 2, half, columns), bf16),
            pltpu.VMEM((4, half, columns), bf16),
            pltpu.VMEM((4, half, columns), bf16),
            pltpu.VMEM((3, rows, columns), bf16),
        ]
    return scratch


class ReduceAlong(Reduce):
    def __init__(self, place, grad, out, buf, chunk, copies):
        self.place, self.grad, self.out, self.buf, self.chunk = place, grad, out, buf, chunk
        own, from_core, from_z, from_x, from_y, late_y, late_x = buf
        _, row, rows, column, columns = chunk
        every, wide = pl.ds(row, rows), pl.ds(column, columns)
        self.low, self.high = low, high = pl.ds(0, rows // 2), pl.ds(rows // 2, rows // 2)
        z, x, y = place.z, place.x, place.y
        self.load = copies.inside(grad.at[:, :, place.core, every, wide], own)
        self.first = copies.plan(
            grad.at[:, :, 1 - place.core, every, wide], from_core, place.to_core
        )
        self.second = [
            copies.plan(own.at[to[0]], from_z.at[k], to) for k, to in enumerate(place.lines)
        ]
        self.third = []
        for k in range(2):
            self.third.append(
                copies.plan(own.at[z, 2 * k + 1 - x, low], from_x.at[k], place.to_x)
            )
            self.third.append(
                copies.plan(own.at[z, 2 * (1 - y) + k, high], from_y.at[k], place.to_y)
            )
        self.fourth = [
            copies.plan(own.at[z, place.chip_y, low], late_y, place.to_y),
            copies.plan(own.at[z, place.chip_x, high], late_x, place.to_x),
        ]

    def exchange(self):
        own, from_core = self.buf[:2]
        self.load.wait()
        arrive([self.first])
        add_blocks(16, lambda i: (own.at[i // 4, i % 4], from_core.at[i // 4, i % 4]))
        go(self.second)

    def spread(self):
        own, _, from_z = self.buf[:3]
        z = self.place.z
        arrive(self.second)

        def body(i, _):
            total = own[z, i].astype(f32)
            for k in range(3):
                total = total + from_z[k, i].astype(f32)
            own[z, i] = total.astype(bf16)
            return 0

        lax.fori_loop(0, 4, body, 0)
        go(self.third)

    def send(self):
        own, _, _, from_x, from_y = self.buf[:5]
        z, x, y = self.place.z, self.place.x, self.place.y
        arrive(self.third)
        add_blocks(2, lambda j: (own.at[z, 2 * j + x, self.low], from_x.at[j]))
        add_blocks(2, lambda j: (own.at[z, 2 * y + j, self.high], from_y.at[j]))
        go(self.fourth)

    def finish(self):
        own, late_y, late_x = self.buf[0], self.buf[5], self.buf[6]
        z, chip = self.place.z, self.place.chip
        _, row, rows, column, columns = self.chunk
        arrive(self.fourth)
        half = rows // 2
        wide = slice(column, column + columns)
        self.out[row : row + half, wide] = own[z, chip, self.low].astype(f32) + late_y[...].astype(
            f32
        )
        self.out[row + half : row + rows, wide] = own[z, chip, self.high].astype(f32) + late_x[
            ...
        ].astype(f32)


def reduce_along_scratch(chunk):
    _, _, rows, _, columns = chunk
    half = rows // 2
    return [
        pltpu.VMEM((4, 4, rows, columns), bf16),
        pltpu.VMEM((4, 4, rows, columns), bf16),
        pltpu.VMEM((3, 4, rows, columns), bf16),
        pltpu.VMEM((2, half, columns), bf16),
        pltpu.VMEM((2, half, columns), bf16),
        pltpu.VMEM((half, columns), bf16),
        pltpu.VMEM((half, columns), bf16),
    ]


class HandBack:
    def __init__(self, place, source, target, features, send, recv, local):
        self.place, self.source, self.target = place, source, target
        self.mine = columns_of(place.s, features)
        self.send, self.recv, self.local = send, recv, local
        self.blocks = source.shape[1]

    def copy(self, b, i, d):
        rank = self.place.plane[d][1]
        n = b * self.blocks + i
        return pltpu.make_async_remote_copy(
            src_ref=self.source.at[b, i, rank],
            dst_ref=self.target.at[b, i, :, self.mine],
            send_sem=self.send.at[n, d],
            recv_sem=self.recv.at[n, d],
            device_id=self.place.plane[d],
            device_id_type=MESH,
        )

    def own(self, b, i):
        return pltpu.make_async_copy(
            self.source.at[b, i, self.place.s],
            self.target.at[b, i, :, self.mine],
            self.local.at[b * self.blocks + i],
        )

    def each(self, b, i):
        for d in range(7):
            self.copy(b, i, d).start()
        self.own(b, i).start()

    def finish(self):
        def body(n, _):
            b, i = n // self.blocks, n % self.blocks
            for d in range(7):
                self.copy(b, i, d).wait()
            self.own(b, i).wait()
            return 0

        lax.fori_loop(0, self.source.shape[0] * self.blocks, body, 0)


def hand_back_semaphores(steps):
    return [
        pltpu.SemaphoreType.DMA((steps, 7)),
        pltpu.SemaphoreType.DMA((steps, 7)),
        pltpu.SemaphoreType.DMA((steps,)),
    ]


class ReduceLines:
    copies = 4 * 7 + 3 + 3 + 6

    def __init__(self, place, grad, out, bufs, copies):
        self.place, self.grad, self.out, self.bufs = place, grad, out, bufs
        from_core, from_x, from_y, late_y, late_x, from_z = bufs[:6]
        early_z, own_x, own_y, own_late_y, own_late_x = bufs[6:]
        core, x, y = place.core, place.x, place.y
        self.order = [to[0] for to in place.lines] + [place.z]
        rows = grad.shape[3]
        low, high = pl.ds(0, rows // 2), pl.ds(rows // 2, rows // 2)
        cut = from_z.shape[2]
        most, rest = pl.ds(0, cut), pl.ds(cut, grad.shape[4] - cut)
        self.low, self.high, self.all = (low, most), (high, most), (pl.ds(0, rows), most)
        self.low_rest, self.high_rest = (low, rest), (high, rest)
        self.all_rest = (pl.ds(0, rows), rest)
        z = place.z
        self.early = [
            copies.plan(grad.at[(to[0], pl.ds(0, 4), core, *self.all_rest)], early_z.at[k], to)
            for k, to in enumerate(place.lines)
        ]
        self.own_second, self.own_third = [], []
        for j in range(2):
            self.own_second.append(
                copies.plan(
                    grad.at[(z, 2 * j + 1 - x, core, *self.low_rest)], own_x.at[j], place.to_x
                )
            )
            self.own_second.append(
                copies.plan(
                    grad.at[(z, 2 * (1 - y) + j, core, *self.high_rest)], own_y.at[j], place.to_y
                )
            )
        self.own_third = [
            copies.plan(
                grad.at[(z, place.chip_y, core, *self.low_rest)], own_late_y, place.to_y
            ),
            copies.plan(
                grad.at[(z, place.chip_x, core, *self.high_rest)], own_late_x, place.to_x
            ),
        ]
        self.first, self.second, self.third, self.fourth = [], [], [], []
        for k, at in enumerate(self.order):
            self.first.append(
                copies.plan(grad.at[at, :, 1 - core], from_core.at[k], place.to_core)
            )
            step = []
            for j in range(2):
                step.append(
                    copies.plan(
                        grad.at[(at, 2 * j + 1 - x, core, *self.low)], from_x.at[k, j], place.to_x
                    )
                )
                step.append(
                    copies.plan(
                        grad.at[(at, 2 * (1 - y) + j, core, *self.high)], from_y.at[k, j], place.to_y
                    )
                )
            self.second.append(step)
            self.third.append(
                [
                    copies.plan(
                        grad.at[(at, place.chip_y, core, *self.low)], late_y.at[k], place.to_y
                    ),
                    copies.plan(
                        grad.at[(at, place.chip_x, core, *self.high)], late_x.at[k], place.to_x
                    ),
                ]
            )
            if k < 3:
                self.fourth.append(
                    copies.plan(
                        grad.at[(at, place.chip, core, *self.all)], from_z.at[k], place.lines[k]
                    )
                )

    def start(self, k):
        go([self.first[k]])

    def exchange(self, k):
        arrive([self.first[k]])
        at, core = self.order[k], self.place.core
        add_blocks(4, lambda i: (self.grad.at[at, i, core], self.bufs[0].at[k, i]))
        go(self.second[k] + self.early[k : k + 1])

    def spread(self, k):
        arrive(self.second[k])
        at, core, x, y = self.order[k], self.place.core, self.place.x, self.place.y
        add_blocks(
            2, lambda j: (self.grad.at[(at, 2 * j + x, core, *self.low)], self.bufs[1].at[k, j])
        )
        add_blocks(
            2, lambda j: (self.grad.at[(at, 2 * y + j, core, *self.high)], self.bufs[2].at[k, j])
        )
        go(self.third[k])

    def send(self, k):
        arrive(self.third[k])
        at, core, chip = self.order[k], self.place.core, self.place.chip
        add_into(self.grad.at[(at, chip, core, *self.low)], self.bufs[3].at[k])
        add_into(self.grad.at[(at, chip, core, *self.high)], self.bufs[4].at[k])
        go(self.fourth[k : k + 1])

    def own_spread(self):
        arrive(self.early)
        z, core = self.place.z, self.place.core

        def body(i, _):
            target = self.grad.at[(z, i, core, *self.all_rest)]
            total = target[...].astype(f32)
            for k in range(3):
                total = total + self.bufs[6][k, i].astype(f32)
            target[...] = total.astype(bf16)
            return 0

        lax.fori_loop(0, 4, body, 0)
        go(self.own_second)

    def own_send(self):
        arrive(self.own_second)
        z, core, x, y = self.place.z, self.place.core, self.place.x, self.place.y
        for j in range(2):
            add_into(self.grad.at[(z, 2 * j + x, core, *self.low_rest)], self.bufs[7].at[j])
            add_into(self.grad.at[(z, 2 * y + j, core, *self.high_rest)], self.bufs[8].at[j])
        go(self.own_third)

    def finish(self):
        arrive(self.fourth + self.own_third)
        place = self.place
        at = (place.z, place.chip, place.core)
        total = self.grad[(*at, *self.all)].astype(f32)
        for k in range(3):
            total = total + self.bufs[5][k].astype(f32)
        cut = total.shape[1]
        half = total.shape[0] // 2
        self.out[:, :cut] = total
        self.out[:half, cut:] = self.grad[(*at, *self.low_rest)].astype(f32) + self.bufs[9][
            ...
        ].astype(f32)
        self.out[half:, cut:] = self.grad[(*at, *self.high_rest)].astype(f32) + self.bufs[10][
            ...
        ].astype(f32)


def reduce_lines_scratch(rows, columns, rest):
    half = rows // 2
    most = columns - rest
    return [
        pltpu.VMEM((4, 4, rows, columns), bf16),
        pltpu.VMEM((4, 2, half, most), bf16),
        pltpu.VMEM((4, 2, half, most), bf16),
        pltpu.VMEM((4, half, most), bf16),
        pltpu.VMEM((4, half, most), bf16),
        pltpu.VMEM((3, rows, most), bf16),
        pltpu.VMEM((3, 4, rows, rest), bf16),
        pltpu.VMEM((2, half, rest), bf16),
        pltpu.VMEM((2, half, rest), bf16),
        pltpu.VMEM((half, rest), bf16),
        pltpu.VMEM((half, rest), bf16),
    ]


def split_grad(item):
    return item.reshape(4, 4, 2, item.shape[0] // 32, item.shape[1])


def split_weight(item):
    return item.reshape(8, item.shape[0] // 8, item.shape[1])


def chunks_of(index, rows, columns, count):
    if rows >= 64:
        return [(index, rows // count * n, rows // count, 0, columns) for n in range(count)]
    return [(index, 0, rows, columns // count * n, columns // count) for n in range(count)]


def semaphores(remote, local):
    return [pltpu.SemaphoreType.DMA((n,)) for n in (remote, remote, local)]


def remote_call(kernel, name, collective, **options):
    return pl.pallas_call(
        kernel,
        name=name,
        compiler_params=pltpu.CompilerParams(
            collective_id=collective, has_side_effects=True, vmem_limit_bytes=vmem_bytes
        ),
        **options,
    )


def row_of(packed, n, size):
    found = [packed[k, n, r : r + 1, :] for k in range(4) for r in range(size // 512)]
    return jnp.concatenate(found, axis=1)


def columns_of(rank, features):
    return pl.ds(pl.multiple_of(rank * features, 128), features)


def forward_fused_kernel(heads, width, count, vector_count, chunks, slopes, tokens, upstream, *refs):
    vectors, refs = refs[:vector_count], refs[vector_count:]
    weights, contract, refs = refs[:count], refs[count], refs[count + 1 :]
    tokens_out, vectors_out, joined_out, qkv_out, attended, out_t, lse, upstream_out = refs[:8]
    contract_out = refs[8]
    wholes, refs = refs[9 : 8 + count], refs[8 + count :]
    held, small, values_of, joined, normed, outgoing, qkv, result, upstream_own = refs[:9]
    attention = Forward(heads, width, slopes, qkv, result, out_t, lse, *refs[9:12])
    kept, refs = refs[12 : 11 + count], refs[11 + count :]
    head_send, head_recv = refs[:2]
    copies = Copies(*refs[5:])
    place = Place()
    z, s, lines, plane = place.z, place.s, place.lines, place.plane
    attention.head = s * heads
    gather = Gather(place, weights, [joined, *wholes], [None, *kept], chunks, copies)
    first = [t for t, chunk in enumerate(chunks) if chunk[0] == 0]
    later = [t for t, chunk in enumerate(chunks) if chunk[0] > 0]
    features = heads * width
    back = HandBack(place, result, attended, features, *refs[2:5])
    own_seqs, parts, piece, wide = held.shape

    load = copies.inside(tokens.at[z], held.at[:, z])
    load_upstream = copies.inside(upstream.at[z], upstream_own)
    seqs = [copies.plan(tokens.at[to[0]], held.at[:, z], to) for to in lines]
    vector_copies = [copies.plan(small.at[z], small.at[z], to) for to in lines]
    upstreams = [copies.plan(upstream.at[to[0]], upstream_out.at[:, z], to) for to in lines]
    keep_upstream = copies.inside(upstream_own, upstream_out.at[:, z])
    keeping = [
        copies.inside(held, tokens_out),
        copies.inside(small, vectors_out),
        copies.inside(joined, joined_out),
    ]
    keep_qkv = copies.inside(qkv, qkv_out)
    contracts = [copies.plan(contract.at[s], contract_out.at[z], to) for to in lines]

    def to_head(d):
        return pltpu.make_async_remote_copy(
            src_ref=outgoing.at[d],
            dst_ref=qkv.at[:, :, s],
            send_sem=head_send.at[d],
            recv_sem=head_recv.at[d],
            device_id=(z, lax.rem(s + 1 + d, 8)),
            device_id_type=MESH,
        )

    go(gather.loads + [load, load_upstream])
    small[z] = jnp.zeros(small.shape[1:], bf16)
    for n, item in enumerate(vectors):
        small[z, n, : item.shape[0], :] = item[...]
    greet(lines + plane)
    for t in first:
        gather.start(t)
    go(seqs + vector_copies)
    gather.keep()
    load.wait()
    for t in range(len(first) + 2):
        if t < len(first):
            gather.exchange(t)
        if 0 <= t - 1 < len(first):
            gather.spread(t - 1)
        if 0 <= t - 2:
            gather.share(t - 2)
    load_upstream.wait()
    keep_upstream.start()
    arrive(seqs + vector_copies)
    for t in later:
        gather.start(t)
    values_of[...] = small[...].astype(f32)

    gain, shift = row_of(values_of, 0, wide), row_of(values_of, 1, wide)

    def norm(i, _):
        values = held[i // parts, i % parts].astype(f32)
        rows = pl.ds(pl.multiple_of(i * piece, piece), piece)
        normed[rows, :] = normalize(values, gain, shift).astype(bf16)
        return 0

    lax.fori_loop(0, own_seqs * parts, norm, 0)
    for t in first:
        gather.complete(t)
    go(keeping)

    def project(d, _):
        rank = lax.rem(s + 1 + d, 8)
        per = 8 // 4
        query_bias = values_of[rank // per, 2, pl.ds(rank % per, 1), :]
        value_bias = values_of[rank // per, 3, pl.ds(rank % per, 1), :]
        low = lax.broadcasted_iota(jnp.int32, query_bias.shape, 1) < width
        bias = jnp.concatenate(
            [
                jnp.where(low, query_bias, 0.0),
                jnp.where(low, value_bias, query_bias),
                jnp.where(low, 0.0, value_bias),
            ],
            axis=1,
        )
        weight = joined[:, :, :, columns_of(rank, 3 * features)].reshape(wide, 3 * features)
        made = (matmul(normed[...], weight) + bias).astype(bf16)
        outgoing[d] = made.reshape(outgoing.shape[1:])
        pl.when(d < 7)(lambda: to_head(d).start())
        return 0

    lax.fori_loop(0, 8, project, 0)
    own_copy = copies.inside(outgoing.at[7], qkv.at[:, :, s])
    own_copy.start()
    base = later[0]
    gather.exchange(base)
    gather.exchange(base + 1)
    own_copy.wait()
    gather.spread(base)
    for d in range(7):
        to_head(d).wait_recv()
    keep_qkv.start()
    attention.run(
        {
            0: [(gather.exchange, base + 2), (go, contracts), (gather.spread, base + 1)],
            2: [(gather.spread, base + 2), (gather.share, base)],
            3: [(go, upstreams)],
            5: [(gather.share, base + 1)],
            6: [(gather.share, base + 2)],
        },
        back.each,
    )
    for t in later:
        gather.complete(t)
    arrive(contracts + upstreams)
    back.finish()
    for d in range(7):
        to_head(d).wait_send()
    copies.finish()
    done(gather.own + [keep_upstream, keep_qkv] + keeping)


def forward_fused(tokens, upstream, vectors, weights, contract, slopes, heads, width):
    seqs, piece, features = tokens.shape
    parts = 4
    own = seqs // parts
    columns = heads * width
    length = parts * 8 * piece
    vectors = [item.reshape(-1, 128) for item in vectors]
    cut = [split_weight(item) for item in weights]
    contract = split_weight(contract)
    count, tall = len(cut), 8 * -(-max(item.shape[0] for item in vectors) // 8)
    chunks = []
    for t, pieces in enumerate((3, 1, 2)):
        chunks += chunks_of(t, *cut[t].shape[1:], pieces)
    seq_shape = (own, parts, piece, features)
    qkv_shape = (own, parts, 8, piece, 3 * columns)
    small = (parts, len(vectors), tall, 128)
    out = remote_call(
        functools.partial(forward_fused_kernel, heads, width, count, len(vectors), chunks),
        "forward_fused",
        1,
        out_shape=(
            jax.ShapeDtypeStruct(seq_shape, bf16),
            jax.ShapeDtypeStruct(small, bf16),
            jax.ShapeDtypeStruct((parts, *cut[0].shape), bf16),
            jax.ShapeDtypeStruct(qkv_shape, bf16),
            jax.ShapeDtypeStruct(seq_shape, bf16),
            *saved_shapes(own, length, heads, width),
            jax.ShapeDtypeStruct(seq_shape, bf16),
            jax.ShapeDtypeStruct((parts, *contract.shape[1:]), bf16),
            *[jax.ShapeDtypeStruct((parts, *item.shape), bf16) for item in cut[1:]],
        ),
        in_specs=[SMEM, HBM, HBM] + [VMEM] * len(vectors) + [HBM] * (count + 1),
        out_specs=(HBM,) * 5 + (VMEM, VMEM) + (HBM,) * (count + 1),
        scratch_shapes=[
            pltpu.VMEM(seq_shape, bf16),
            pltpu.VMEM(small, bf16),
            pltpu.VMEM(small, f32),
            pltpu.VMEM((parts, *cut[0].shape), bf16),
            pltpu.VMEM((own * parts * piece, features), bf16),
            pltpu.VMEM((8, own, parts, piece, 3 * columns), bf16),
            pltpu.VMEM(qkv_shape, bf16),
            pltpu.VMEM((own, parts, 8, piece, columns), bf16),
            pltpu.VMEM((own, piece, features), bf16),
            *forward_scratch(length, heads, width),
            *[pltpu.VMEM(item.shape, bf16) for item in cut[1:]],
            pltpu.SemaphoreType.DMA((7,)),
            pltpu.SemaphoreType.DMA((7,)),
            *hand_back_semaphores(own * parts),
            *semaphores(12 + len(chunks) * Gather.copies_each, 2 * count - 1 + 8),
        ],
    )(
        slopes,
        tokens.reshape(parts, own, piece, features),
        upstream.reshape(parts, own, piece, features),
        *vectors,
        *cut,
        contract,
    )
    wholes = [
        whole.reshape(4 * item.shape[0], item.shape[1])
        for whole, item in zip((out[2], *out[9:]), weights)
    ]
    return out[0], out[1], [*wholes, out[8]], out[3], out[4], (out[5], out[6]), out[7]


def feed_forward_kernel(
    chunks, expand, contract, contract_line, out_weight,
    small, upstream, tokens, attended,
    layer, residual_grad, attended_diff, expand_grad, out_grad, contract_grad,
    bias_grad, gain_grad, shift_grad, out_bias_grad, contract_bias_grad,
    values_of, expand_bias, expand_in, contract_in, residual, second, second_t, expanded, activated, grad, staged, *refs,
):
    second_back = residual_grad
    bufs, refs = refs[:11], refs[11:]
    loaded, stored, refs = refs[0], refs[1], refs[2:]
    copies = Copies(*refs)
    place = Place()
    z = place.z
    reduce = ReduceLines(place, grad, contract_grad, bufs, copies)
    gather = Gather(
        place, [contract], [contract_in], [None], chunks, copies, given=contract_line
    )
    rows, features = second.shape
    steps = 8
    wide = expand.shape[1] // steps

    def at(n):
        part = (z + 1 + n // 2) % 4
        return part, n % 2, pl.ds(pl.multiple_of((2 * part + n % 2) * wide, wide), wide)

    def load(n):
        _, _, where = at(n)
        return pltpu.make_async_copy(expand.at[:, where], expand_in.at[:, where], loaded.at[n])

    def contract_at(n):
        part, side, _ = at(n)
        return contract_in[part, pl.ds(4 * side, 4)].reshape(wide, features)

    def store(n):
        _, _, where = at(n)
        slot = n % 2
        return pltpu.make_async_copy(
            staged.at[slot], expand_grad.at[:, where], stored.at[slot]
        )

    halves = [pl.ds(0, wide), pl.ds(wide, wide)]
    out_loads = [
        pltpu.make_async_copy(out_weight.at[:, half], staged.at[n], stored.at[n])
        for n, half in enumerate(halves)
    ]
    out_stores = [
        pltpu.make_async_copy(staged.at[n], out_grad.at[:, half], stored.at[n])
        for n, half in enumerate(halves)
    ]
    part_rows = rows // 8

    def rows_at(i):
        return pl.ds(pl.multiple_of(i * part_rows, part_rows), part_rows)

    for n in range(len(chunks)):
        gather.start(n)
    go(out_loads)
    for n in range(steps):
        load(n).start()
    go(gather.loads)
    greet(place.near)
    for n in range(len(chunks)):
        gather.exchange(n)
    values_of[...] = small[...].astype(f32)
    out_bias, gain, shift, contract_bias = [
        row_of(values_of, n, features) for n in (4, 5, 6, 7)
    ]
    expand_bias[...] = row_of(values_of, 8, steps * wide)
    for n, half in enumerate(halves):
        out_loads[n].wait()
        bias = out_bias[:, n * wide : (n + 1) * wide]
        residual[:, half] = (
            tokens[:, half].astype(f32) + (matmul(attended[...], staged[n]) + bias)
        )

    def norm(i, _):
        values = residual[rows_at(i), :]
        second[rows_at(i), :] = normalize(values, gain, shift).astype(bf16)
        second_back[rows_at(i), :] = values + contract_bias
        return 0

    lax.fori_loop(0, 8, norm, 0)
    for n in range(len(chunks) - 1):
        gather.spread(n)
    second_t[...] = second[...].T

    def forward(n, after):
        part, side, where = at(n)
        load(n).wait()
        values = matmul(second[...], expand_in[:, where]) + expand_bias[:, where]
        expanded[:, where] = values
        low = gelu_tanh(values).astype(bf16)
        activated[:, where] = low
        made = matmul(low.T, upstream[...]).astype(bf16)
        grad[part, pl.ds(2 * side, 2)] = made.reshape(2, 2, wide // 4, features)
        follow(n, after)
        return 0

    def shrink(n, after):
        _, _, where = at(n)
        second_back[...] += matmul(activated[:, where], contract_at(n))
        follow(n, after)
        return 0

    def backward(n, after):
        _, _, where = at(n)
        values = expanded[:, where]
        act_grad = matmul_rt(upstream[...], contract_at(n))
        bent = jnp.tanh(gelu_coef * (values + 0.044715 * values * values * values))
        slope = 0.5 * (1.0 + bent) + 0.5 * values * (1.0 - bent * bent) * (
            gelu_coef * (1.0 + 3.0 * 0.044715 * values * values)
        )
        diff = (act_grad * slope).astype(bf16)
        bias_grad[:, where] = jnp.sum(diff.astype(f32), axis=0, keepdims=True)
        pl.when(n >= 2)(lambda: store(n - 2).wait())
        staged[n % 2] = matmul(second_t[...], diff).astype(bf16)
        store(n).start()
        second_back[...] += matmul_rt(diff, expand_in[:, where])
        follow(n, after)
        return 0

    last = len(chunks) - 1
    forward_steps = {
        0: [(gather.spread, last)],
        1: [(reduce.start, 0)],
        3: [(reduce.exchange, 0), (reduce.start, 1)],
        5: [(reduce.start, 2), (reduce.exchange, 1)],
        7: [(reduce.start, 3), (reduce.exchange, 2)] + [(gather.share, n) for n in range(last)],
    }
    shrink_steps = {
        1: [(reduce.exchange, 3)],
        3: [(reduce.spread, 0)],
        7: [(reduce.spread, 1)],
    }
    backward_steps = {
        1: [(reduce.spread, 2)],
        2: [(reduce.spread, 3)],
        3: [(reduce.send, 0), (reduce.own_spread,)],
        4: [(reduce.send, 1)],
        5: [(reduce.send, 2)],
        6: [(reduce.send, 3), (reduce.own_send,)],
    }
    lax.fori_loop(0, steps, lambda n, _: forward(n, forward_steps), 0)
    gather.share(last)
    for n in range(len(chunks)):
        gather.complete(n)
    done(gather.loads)
    lax.fori_loop(0, steps, lambda n, _: shrink(n, shrink_steps), 0)
    layer[...] = second_back[...].astype(bf16).reshape(layer.shape)
    second_back[...] = jnp.zeros_like(second_back)
    lax.fori_loop(0, steps, lambda n, _: backward(n, backward_steps), 0)
    store(steps - 2).wait()
    store(steps - 1).wait()
    go(out_loads)
    second_t[...] = attended[...].T

    def norm_back(i, sums):
        back = second_back[rows_at(i), :]
        part, normal = normalize_back(residual[rows_at(i), :], back, gain)
        given = upstream[rows_at(i), :].astype(f32)
        total = given + part
        low = total.astype(bf16)
        residual_grad[rows_at(i), :] = total
        second[rows_at(i), :] = low
        found = (back * normal, back, low.astype(f32), given)
        return tuple(
            kept + jnp.sum(item, axis=0, keepdims=True) for kept, item in zip(sums, found)
        )

    nothing = jnp.zeros((1, features), f32)
    sums = lax.fori_loop(0, 8, norm_back, (nothing,) * 4)
    gain_grad[...], shift_grad[...], out_bias_grad[...], contract_bias_grad[...] = sums
    done(out_loads)
    branch_diff = second
    made = matmul_rt(branch_diff[:, halves[0]], staged[0])
    made = (made + matmul_rt(branch_diff[:, halves[1]], staged[1])).astype(bf16)
    attended_diff[...] = made.reshape(attended_diff.shape)
    for n, half in enumerate(halves):
        staged[n] = matmul(second_t[...], branch_diff[:, half]).astype(bf16)
        out_stores[n].start()
    reduce.finish()
    done(out_stores)
    copies.finish()


def feed_forward(shape, expand, contract, line, out_weight, tokens, upstream, attended, small):
    own, parts, piece = shape
    rows, features = tokens.shape
    hidden = expand.shape[1]
    wide = hidden // 8
    each = hidden // 32
    contract = split_weight(contract)
    chunks = chunks_of(0, *contract.shape[1:], 2)
    seq_shape = (own, parts, piece, features)
    return remote_call(
        functools.partial(feed_forward_kernel, chunks),
        "feed_forward",
        4,
        out_shape=(
            jax.ShapeDtypeStruct(seq_shape, bf16),
            jax.ShapeDtypeStruct((rows, features), f32),
            jax.ShapeDtypeStruct(seq_shape, bf16),
            jax.ShapeDtypeStruct((features, hidden), bf16),
            jax.ShapeDtypeStruct((features, features), bf16),
            jax.ShapeDtypeStruct((each, features), f32),
            jax.ShapeDtypeStruct((1, hidden), f32),
            *[jax.ShapeDtypeStruct((1, features), f32)] * 4,
        ),
        in_specs=[HBM] * 4 + [VMEM] * 4,
        out_specs=(VMEM, VMEM, VMEM, HBM, HBM) + (VMEM,) * 6,
        scratch_shapes=[
            pltpu.VMEM(small.shape, f32),
            pltpu.VMEM((1, hidden), f32),
            pltpu.VMEM((features, hidden), bf16),
            pltpu.VMEM((4, *contract.shape), bf16),
            pltpu.VMEM((rows, features), f32),
            pltpu.VMEM((rows, features), bf16),
            pltpu.VMEM((features, rows), bf16),
            pltpu.VMEM((rows, hidden), f32),
            pltpu.VMEM((rows, hidden), bf16),
            pltpu.VMEM((4, 4, 2, each, features), bf16),
            pltpu.VMEM((2, features, wide), bf16),
            *reduce_lines_scratch(each, features, features // 4),
            pltpu.SemaphoreType.DMA((8,)),
            pltpu.SemaphoreType.DMA((2,)),
            *semaphores(
                ReduceLines.copies + len(chunks) * (Gather.copies_each - 3),
                1 + 3 * len(chunks),
            ),
        ],
    )(expand, contract, line, out_weight, small, upstream, tokens, attended)


def backward_fused_kernel(heads, width, count, chunks, *refs):
    slopes, diff_in, qkv_in, out_t_in, lse_in, layer = refs[:6]
    grads, refs = refs[6 : 6 + count], refs[6 + count :]
    joined_out, layer_out, layer_own = refs[0], refs[1], refs[2 + count]
    outs, refs = refs[2 : 2 + count], refs[3 + count :]
    diff, qkv, out_t, lse, joined = refs[:5]
    attention = Backward(heads, width, slopes, qkv, diff, out_t, lse, joined, *refs[5:12])
    bufs, refs = refs[12 : 12 + 7 * len(chunks)], refs[12 + 7 * len(chunks) :]
    copies = Copies(*refs[3:])
    place = Place()
    s, plane = place.s, place.plane
    attention.head = s * heads
    features = heads * width
    along = ReduceAlong(place, grads[0], outs[0], bufs[:7], chunks[0], copies)
    reduce = Reduce(place, grads, outs, bufs[7:], chunks[1:], copies)
    back = HandBack(place, joined, joined_out, 3 * features, *refs[:3])

    own = [copies.inside(diff_in.at[:, :, :, columns_of(s, features)], diff.at[:, :, s])]
    own += [copies.inside(a, b) for a, b in ((qkv_in, qkv), (out_t_in, out_t), (lse_in, lse))]
    arriving = [
        copies.plan(diff_in.at[:, :, :, columns_of(to[1], features)], diff.at[:, :, s], to)
        for to in plane
    ]
    returned = [copies.plan(layer.at[:, to[0]], layer_out.at[place.z], to) for to in place.lines]
    load_layer = copies.inside(layer.at[:, place.z], layer_own)
    keep_layer = copies.inside(layer_own, layer_out.at[place.z])
    go(own + reduce.loads + [along.load, load_layer])
    greet(place.lines + plane)
    go(arriving + [along.first])
    reduce.start()
    along.exchange()
    go(returned)
    for t in range(3):
        reduce.exchange(t)
    done(own + [load_layer])
    keep_layer.start()
    arrive(arriving)
    attention.run(
        {
            1: [(reduce.spread, 0)],
            2: [(along.spread,)],
            3: [(reduce.spread, 1), (reduce.spread, 2)],
            4: [(reduce.send, 0), (along.send,)],
            5: [(reduce.send, 1)],
            6: [(reduce.send, 2)],
        },
        back.each,
    )
    for t in range(3):
        reduce.finish(t)
    along.finish()
    back.finish()
    arrive(returned)
    copies.finish()
    keep_layer.wait()


def backward_fused(attended_diff, qkv, saved, layer, grads, slopes, heads, width):
    own, parts, piece, columns = attended_diff.shape
    features = heads * width
    length = parts * 8 * piece
    cut = [split_grad(item) for item in grads]
    count = len(cut)
    rows, wide = cut[0].shape[3:]
    part = 3 * wide // 8
    chunks = [
        (0, 0, rows, 0, wide // 4),
        (0, 0, rows, wide // 4, part),
        (0, 0, rows, wide // 4 + part, part),
        *chunks_of(1, *cut[1].shape[3:], 1),
    ]
    out = remote_call(
        functools.partial(backward_fused_kernel, heads, width, count, chunks),
        "backward_fused",
        2,
        out_shape=(
            jax.ShapeDtypeStruct((own, parts, piece, 24 * features), bf16),
            jax.ShapeDtypeStruct((parts, own, piece, columns), bf16),
            *[jax.ShapeDtypeStruct(item.shape[3:], f32) for item in cut],
        ),
        in_specs=[SMEM] + [HBM] * (5 + count),
        out_specs=(HBM, HBM) + (VMEM,) * count,
        scratch_shapes=[
            pltpu.VMEM((own, piece, columns), bf16),
            pltpu.VMEM((own, parts, 8, piece, features), bf16),
            pltpu.VMEM(qkv.shape, bf16),
            *[pltpu.VMEM(item.shape, f32) for item in saved],
            pltpu.VMEM(qkv.shape, bf16),
            *backward_scratch(length, heads, width),
            *reduce_along_scratch(chunks[0]),
            *reduce_scratch(chunks[1:]),
            *hand_back_semaphores(own * parts),
            *semaphores(10 + len(chunks) * Reduce.copies_each, len(chunks) + 6),
        ],
    )(slopes, attended_diff, qkv, *saved, layer, *cut)
    return out[0], out[1].reshape(parts * own, piece, columns), out[2:]


def end_kernel(
    width, joined_diff, joined_weight, tokens, residual_grad, small, out_bias_grad,
    second_gain_grad, second_shift_grad, contract_bias_grad, expand_bias_grad,
    input_out, vector_out, out,
    values_of, diff_in, weight_in, normed, normed_t, back, grads, held, vectors, others, ranks,
    *refs,
):
    count = grads.shape[0]
    bufs, refs = refs[: 7 * count], refs[7 * count :]
    loaded, copies = refs[0], Copies(*refs[1:])
    place = Place()
    z, lines, plane = place.z, place.lines, place.plane
    rows, features = tokens.shape
    own_seqs, parts, piece, _ = held.shape
    columns = [pl.ds(features * n, features) for n in range(count)]
    chunks = [(n, 0, grads.shape[4], 0, features) for n in range(count)]
    outs = [out.at[:, where] for where in columns]
    reduce = Reduce(place, [grads.at[n] for n in range(count)], outs, bufs, chunks, copies)
    loads = [
        (
            pltpu.make_async_copy(joined_diff.at[:, c], diff_in.at[:, c], loaded.at[0, n]),
            pltpu.make_async_copy(joined_weight.at[:, c], weight_in.at[:, c], loaded.at[1, n]),
        )
        for n, c in enumerate(columns)
    ]
    returned = [copies.plan(held.at[:, to[0]], input_out.at[z], to) for to in lines]
    stay = copies.inside(held.at[:, z], input_out.at[z])
    along = [copies.plan(vectors.at[to[0]], others.at[k], to) for k, to in enumerate(lines)]
    across = [copies.plan(ranks.at[0], ranks.at[d + 1], to) for d, to in enumerate(plane)]

    for load in loads:
        go(load)
    values_of[...] = small[...].astype(f32)
    gain, shift = row_of(values_of, 0, features), row_of(values_of, 1, features)
    greet(lines + plane)
    for n, where in enumerate(columns):
        done(loads[n])
        part = matmul_rt(diff_in[:, where], weight_in[:, where])
        back[...] = part if n == 0 else back[...] + part

    def norm_back(i, sums):
        at = pl.ds(pl.multiple_of(i * piece, piece), piece)
        values, given = tokens[at, :].astype(f32), back[at, :]
        part, normal = normalize_back(values, given, gain)
        normed[at, :] = (normal * gain + shift).astype(bf16)
        total = (residual_grad[at, :] + part).astype(bf16)
        held[i // parts, i % parts] = total
        found = (given * normal, given)
        return tuple(
            kept + jnp.sum(item, axis=0, keepdims=True) for kept, item in zip(sums, found)
        )

    nothing = jnp.zeros((1, features), f32)
    gain_grad, shift_grad = lax.fori_loop(0, own_seqs * parts, norm_back, (nothing, nothing))
    go(returned + [stay])
    normed_t[...] = normed[...].T
    sums = []
    for n, where in enumerate(columns):
        made = matmul(normed_t[...], diff_in[:, where]).astype(bf16)
        grads[n] = made.reshape(grads.shape[1:])
        reduce.begin(n)
        sums.append(jnp.sum(diff_in[:, where].astype(f32), axis=0, keepdims=True))
        if n > 0:
            reduce.exchange(n - 1)

    sums = jnp.concatenate(sums, axis=1)
    low = lax.broadcasted_iota(jnp.int32, (1, 128), 1) < width
    query_grad, value_grad = [], []
    for r in range(features // 128):
        first, middle, last = [sums[:, (3 * r + n) * 128 : (3 * r + n + 1) * 128] for n in range(3)]
        query_grad.append(jnp.where(low, first, middle))
        value_grad.append(jnp.where(low, middle, last))
    given = [
        gain_grad, shift_grad, jnp.concatenate(query_grad, axis=1),
        jnp.concatenate(value_grad, axis=1), out_bias_grad[...], second_gain_grad[...],
        second_shift_grad[...], contract_bias_grad[...], expand_bias_grad[...],
    ]
    row = 0
    for item in given:
        each = item.shape[1] // 512
        for k in range(4):
            for r in range(each):
                start = (k * each + r) * 128
                vectors[k, row + r : row + r + 1, :] = item[:, start : start + 128]
        row += each
    go(along)
    reduce.spread(0)
    reduce.exchange(count - 1)
    arrive(along)
    total = vectors[z]
    for k in range(3):
        total = total + others[k]
    ranks[0] = total
    go(across)
    for n in range(1, count):
        reduce.send(n - 1)
        reduce.spread(n)
    reduce.send(count - 1)
    arrive(across)
    total = ranks[0]
    for d in range(1, 8):
        total = total + ranks[d]
    vector_out[...] = total
    for n in range(count):
        reduce.finish(n)
    arrive(returned)
    copies.finish()
    stay.wait()


def end(shape, joined_diff, joined_weight, tokens, residual_grad, small, vectors, width):
    own, parts, piece = shape
    rows, features = tokens.shape
    count = joined_diff.shape[1] // features
    each = features // 32
    tall = (4 * features + sum(item.shape[1] for item in vectors)) // 512
    chunks = [(n, 0, each, 0, features) for n in range(count)]
    out = remote_call(
        functools.partial(end_kernel, width),
        "end",
        3,
        out_shape=(
            jax.ShapeDtypeStruct((parts, own, piece, features), bf16),
            jax.ShapeDtypeStruct((tall, 128), f32),
            jax.ShapeDtypeStruct((each, count * features), f32),
        ),
        in_specs=[HBM, HBM] + [VMEM] * (3 + len(vectors)),
        out_specs=(HBM, VMEM, VMEM),
        scratch_shapes=[
            pltpu.VMEM(small.shape, f32),
            pltpu.VMEM((rows, count * features), bf16),
            pltpu.VMEM((features, count * features), bf16),
            pltpu.VMEM((rows, features), bf16),
            pltpu.VMEM((features, rows), bf16),
            pltpu.VMEM((rows, features), f32),
            pltpu.VMEM((count, 4, 4, 2, each, features), bf16),
            pltpu.VMEM((own, parts, piece, features), bf16),
            pltpu.VMEM((4, tall, 128), f32),
            pltpu.VMEM((3, tall, 128), f32),
            pltpu.VMEM((8, tall, 128), f32),
            *reduce_scratch(chunks),
            pltpu.SemaphoreType.DMA((2, count)),
            *semaphores(3 + 3 + 7 + count * Reduce.copies_each, 1 + count),
        ],
    )(joined_diff, joined_weight, tokens, residual_grad, small, *vectors)
    return out[0].reshape(parts * own, piece, features), out[1], out[2]


def hand_out_kernel(sizes, vector, *refs):
    count = (len(refs) - len(sizes) - 1) // 3
    arrays, outs, smalls = refs[:count], refs[count : 2 * count], refs[2 * count :]
    smalls, kept, sems = smalls[: len(sizes)], smalls[len(sizes) : -1], refs[-1]
    s = lax.axis_index("sp")
    loads = [pltpu.make_async_copy(a, k, sems.at[n]) for n, (a, k) in enumerate(zip(arrays, kept))]
    stores = [
        pltpu.make_async_copy(k, o, sems.at[count + n]) for n, (k, o) in enumerate(zip(kept, outs))
    ]
    go(loads)
    row = 0
    for out, size in zip(smalls, sizes):
        per = 128 // size
        found = vector[pl.ds(row + s // per, 1), :]
        if per > 1:
            found = pltpu.roll(found, lax.rem(128 - s % per * size, 128), 1)
        out[...] = found[:, :size]
        row += 8 // per
    for load, store in zip(loads, stores):
        load.wait()
        store.start()
    done(stores)


def hand_out(vector, sizes, arrays):
    out = pl.pallas_call(
        functools.partial(hand_out_kernel, sizes),
        name="hand_out",
        out_shape=(
            *[jax.ShapeDtypeStruct(item.shape, item.dtype) for item in arrays],
            *[jax.ShapeDtypeStruct((1, size), f32) for size in sizes],
        ),
        in_specs=[VMEM] + [HBM] * len(arrays),
        out_specs=(HBM,) * len(arrays) + (VMEM,) * len(sizes),
        scratch_shapes=[
            *[pltpu.VMEM(item.shape, item.dtype) for item in arrays],
            pltpu.SemaphoreType.DMA((2 * len(arrays),)),
        ],
        compiler_params=pltpu.CompilerParams(vmem_limit_bytes=vmem_bytes),
    )(vector, *arrays)
    return out[: len(arrays)], [item.reshape(-1) for item in out[len(arrays) :]]


def per_device(
    layer_input,
    first_gain,
    first_shift,
    joined_weight,
    query_bias,
    value_bias,
    output_weight,
    output_bias,
    second_gain,
    second_shift,
    expand_weight,
    expand_bias,
    contract_weight,
    contract_bias,
    alibi_slopes,
    upstream,
):
    seqs, piece, features = layer_input.shape
    fs_count = lax.axis_size("fs")
    sp_count = lax.axis_size("sp")
    head_count = alibi_slopes.shape[0]
    width = features // head_count
    heads = head_count // sp_count
    rows = seqs * piece
    own = seqs // fs_count
    shape = (own, fs_count, piece)

    vectors = (
        first_gain, first_shift, query_bias, value_bias, output_bias,
        second_gain, second_shift, contract_bias, expand_bias,
    )
    fast = (fs_count, sp_count) == (4, 8) and (own, heads, width) == (2, 2, 64)
    fast = fast and expand_weight.shape[1] == 4 * features
    if fast:
        weights = (joined_weight, output_weight, expand_weight)
        tokens, small, weights, qkv, attended, saved, upstream_low = forward_fused(
            layer_input, upstream, vectors, weights, contract_weight, alibi_slopes, heads, width
        )
        joined_full, out_full, expand_full, contract_line = weights
        tokens = tokens.reshape(rows, features)
        (
            layer_output, residual_grad, attended_diff, expand_grad, output_weight_grad,
            contract_grad, eb, g2, s2, ob, cb,
        ) = feed_forward(
            shape, expand_full, contract_weight, contract_line, out_full, tokens,
            upstream_low.reshape(rows, features), attended.reshape(rows, features), small,
        )
        joined_diff, layer_output, grads = backward_fused(
            attended_diff, qkv, saved, layer_output, (expand_grad, output_weight_grad),
            alibi_slopes, heads, width,
        )
        input_grad, vector, joined_grad = end(
            shape, joined_diff.reshape(rows, 3 * features), joined_full, tokens, residual_grad,
            small, (ob, g2, s2, cb, eb), width,
        )
        devices = fs_count * sp_count
        sizes = [4 * item.shape[0] // devices for item in vectors]
        arrays, (g1, s1, qb, vb, ob, g2, s2, cb, eb) = hand_out(
            vector, sizes, (layer_output, input_grad, joined_grad, grads[1], grads[0], contract_grad)
        )
        layer_output, input_grad, joined_grad, output_grad, expand_grad, contract_grad = arrays
        return (
            layer_output, input_grad, g1, s1, joined_grad, qb, vb, output_grad, ob, g2, s2,
            expand_grad, eb, contract_grad, cb,
        )

    slopes = lax.dynamic_slice_in_dim(alibi_slopes, lax.axis_index("sp") * heads, heads)
    gather = lambda item: lax.all_gather(item, "fs", axis=0, tiled=True)
    scatter = functools.partial(
        lax.psum_scatter, axis_name=("fs", "sp"), scatter_dimension=0, tiled=True
    )
    gain_one, shift_one, qbias, vbias, obias, gain_two, shift_two, cbias, ebias = [
        gather(item).astype(f32) for item in vectors
    ]
    joined_full, out_full, expand_full, contract_full = [
        gather(item) for item in (joined_weight, output_weight, expand_weight, contract_weight)
    ]
    tokens = to_own_seqs(layer_input).reshape(rows, features).astype(f32)
    upstream_low = to_own_seqs(upstream).reshape(rows, features)

    normed_f, norm_back_one = jax.vjp(normalize, tokens, gain_one, shift_one)
    normed = normed_f.astype(bf16)
    joined_bias = joined_bias_of(qbias, vbias, head_count)
    joined_all = (matmul(normed, joined_full) + joined_bias).astype(bf16)
    qkv = to_heads(joined_all.reshape(*shape, 3 * features))
    attended, *saved = attention_forward(qkv, slopes, heads, width)
    attended = from_heads(attended).reshape(rows, features)
    upstream_f = upstream_low.astype(f32)
    contract_bias_grad = jnp.sum(upstream_f, axis=0)
    residual = tokens + (matmul(attended, out_full) + obias)
    second_f, norm_back_two = jax.vjp(normalize, residual, gain_two, shift_two)
    second = second_f.astype(bf16)
    expanded = matmul(second, expand_full) + ebias
    activated_f, gelu_back = jax.vjp(gelu_tanh, expanded)
    activated = activated_f.astype(bf16)
    result = residual + (matmul(activated, contract_full) + cbias)
    layer_output = result.astype(bf16).reshape(*shape, features)

    contract_grad = matmul_lt(activated, upstream_low)
    act_grad = matmul_rt(upstream_low, contract_full)
    expand_diff = gelu_back(act_grad)[0].astype(bf16)
    expand_grad = matmul_lt(second, expand_diff)
    expand_bias_grad = jnp.sum(expand_diff.astype(f32), axis=0)
    second_back = matmul_rt(expand_diff, expand_full)
    resid_part, second_gain_grad, second_shift_grad = norm_back_two(second_back)
    residual_grad = upstream_f + resid_part

    branch_diff = residual_grad.astype(bf16)
    output_weight_grad = matmul_lt(attended, branch_diff)
    output_bias_grad = jnp.sum(branch_diff.astype(f32), axis=0)
    attended_diff = matmul_rt(branch_diff, out_full).astype(bf16)
    attended_diff = attended_diff.reshape(*shape, features)
    joined_diff = attention_backward(qkv, to_heads(attended_diff), *saved, slopes, heads, width)
    joined_diff = from_heads(joined_diff).reshape(rows, 3 * features)
    joined_grad = matmul_lt(normed, joined_diff)
    column_sums = jnp.sum(joined_diff.astype(f32), axis=0).reshape(head_count, 3, width)
    query_bias_grad = column_sums[:, 0].reshape(features)
    value_bias_grad = column_sums[:, 2].reshape(features)
    normed_back = matmul_rt(joined_diff, joined_full)
    input_part, first_gain_grad, first_shift_grad = norm_back_one(normed_back)
    input_grad = (residual_grad + input_part).astype(bf16).reshape(*shape, features)

    vector_grads = (
        first_gain_grad, first_shift_grad, query_bias_grad, value_bias_grad,
        output_bias_grad, second_gain_grad, second_shift_grad, contract_bias_grad,
        expand_bias_grad,
    )
    devices = fs_count * sp_count
    packed = jnp.concatenate([item.reshape(devices, -1) for item in vector_grads], axis=1)
    packed = scatter(packed.reshape(-1))
    own_grads, at = [], 0
    for item in vector_grads:
        size = item.shape[0] // devices
        own_grads.append(packed[at : at + size])
        at += size
    g1, s1, qb, vb, ob, g2, s2, cb, eb = own_grads
    return (
        from_own_seqs(layer_output), from_own_seqs(input_grad), g1, s1, scatter(joined_grad), qb,
        vb, scatter(output_weight_grad), ob, g2, s2, scatter(expand_grad), eb,
        scatter(contract_grad), cb,
    )


def solution(mesh):
    tokens = P(None, ("fs", "sp"), None)
    both, both_rows = P(("fs", "sp")), P(("fs", "sp"), None)
    one, one_rows = P("fs"), P("fs", None)
    return jax.shard_map(
        per_device,
        mesh=mesh,
        in_specs=(
            tokens, one, one, one_rows, one, one, one_rows, one, one, one, one_rows, one,
            one_rows, one, P(), tokens,
        ),
        out_specs=(
            tokens, tokens, both, both, both_rows, both, both, both_rows, both, both, both,
            both_rows, both, both_rows, both,
        ),
        check_vma=False,
    )
```

```python
import functools
import math

import jax
import jax.numpy as jnp
from jax import lax
from jax.experimental import pallas as pl
from jax.experimental.pallas import tpu as pltpu
from jax.sharding import PartitionSpec as P

norm_eps = 1e-05
gelu_coef = 0.7978845608028654
masked_value = -1e30
f32 = jnp.float32
bf16 = jnp.bfloat16
MESH = pl.DeviceIdType.MESH
HBM = pl.BlockSpec(memory_space=pl.ANY)
VMEM = pl.BlockSpec(memory_space=pltpu.VMEM)
SMEM = pl.BlockSpec(memory_space=pltpu.SMEM)
vmem_bytes = 63 * 1024 * 1024


def normalize(values, norm_gain, norm_shift):
    center = values - jnp.mean(values, axis=-1, keepdims=True)
    variance = jnp.mean(center * center, axis=-1, keepdims=True)
    return center * lax.rsqrt(variance + norm_eps) * norm_gain + norm_shift


def normalize_back(values, back, norm_gain):
    center = values - jnp.mean(values, axis=-1, keepdims=True)
    inverse = lax.rsqrt(jnp.mean(center * center, axis=-1, keepdims=True) + norm_eps)
    normal = center * inverse
    scaled = back * norm_gain
    even = jnp.mean(scaled, axis=-1, keepdims=True)
    along = jnp.mean(scaled * normal, axis=-1, keepdims=True)
    return inverse * (scaled - even - normal * along), normal


def gelu_tanh(values):
    return (
        0.5 * values * (1.0 + jnp.tanh(gelu_coef * (values + 0.044715 * values * values * values)))
    )


def matmul(left_side, right_side):
    return jnp.dot(left_side, right_side, preferred_element_type=f32)


def matmul_lt(left_side, right_side):
    return lax.dot_general(
        left_side, right_side, (((0,), (0,)), ((), ())), preferred_element_type=f32
    )


def matmul_rt(left_side, right_side):
    return lax.dot_general(
        left_side, right_side, (((1,), (1,)), ((), ())), preferred_element_type=f32
    )


def joined_bias_of(query_bias, value_bias, head_count):
    query_part = query_bias.astype(f32).reshape(head_count, -1)
    value_part = value_bias.astype(f32).reshape(head_count, -1)
    return jnp.stack([query_part, jnp.zeros_like(query_part), value_part], axis=1).reshape(-1)


def split_three(values):
    high = values.astype(bf16).astype(f32)
    rest = values - high
    middle = rest.astype(bf16).astype(f32)
    return high, middle, rest - middle


def key_columns(key_rows, slope, start):
    rows, width = key_rows.shape
    position = (start + lax.broadcasted_iota(jnp.int32, (rows, width), 0)).astype(f32)
    lane = lax.broadcasted_iota(jnp.int32, (rows, width), 1)
    high, middle, low = split_three(slope * position)
    extra = jnp.where(lane == 0, high, jnp.where(lane == 1, middle, jnp.where(lane == 2, low, 0.0)))
    return jnp.concatenate([key_rows.astype(f32), extra], axis=1).astype(bf16)


def query_columns(queries, scale):
    rows, width = queries.shape
    lane = lax.broadcasted_iota(jnp.int32, (rows, width), 1)
    ones = jnp.where(lane < 3, 1.0, 0.0)
    return jnp.concatenate([queries.astype(f32) * scale, ones], axis=1).astype(bf16)


def follow(n, after):
    for at, steps in after.items():

        def act(steps=steps):
            for step, *given in steps:
                step(*given)

        pl.when(n == at)(act)


class Forward:
    def __init__(self, heads, width, slopes, qkv, out, out_t, lse, keys, queries, values_t):
        self.heads, self.width, self.slopes, self.qkv, self.out = heads, width, slopes, qkv, out
        self.out_t, self.lse = out_t, lse
        self.keys, self.queries, self.values_t = keys, queries, values_t
        self.head = 0
        self.blocks = qkv.shape[1]
        self.block = qkv.shape[2] * qkv.shape[3]

    def rows(self, i):
        return pl.ds(pl.multiple_of(i * self.block, self.block), self.block)

    def prepare(self, b):
        width, block, qkv = self.width, self.block, self.qkv
        scale = 1.0 / math.sqrt(width)

        def body(i, _):
            rows = self.rows(i)
            for h in range(self.heads):
                base = h * 3 * width
                query, key, value = [
                    qkv[b, i, :, :, base + n * width : base + (n + 1) * width].reshape(block, width)
                    for n in range(3)
                ]
                self.keys[h, rows, :] = key_columns(key, self.slopes[self.head + h], i * block)
                self.queries[h, rows, :] = query_columns(query, scale)
                self.values_t[h, :, rows] = value.astype(f32).T.astype(bf16)
            return 0

        lax.fori_loop(0, self.blocks, body, 0)

    def one(self, b, i):
        heads, width, block = self.heads, self.width, self.block
        rows = self.rows(i)
        query = [self.queries[h, rows, :] for h in range(heads)]

        def step(j, state, diagonal):
            columns = self.rows(j)
            result = []
            for h in range(heads):
                top, total, acc = state[h]
                scores = matmul_rt(self.keys[h, columns, :], query[h])
                if diagonal:
                    key_at = lax.broadcasted_iota(jnp.int32, (block, block), 0)
                    query_at = lax.broadcasted_iota(jnp.int32, (block, block), 1)
                    scores = jnp.where(key_at <= query_at, scores, masked_value)
                newest = jnp.maximum(top, jnp.max(scores, axis=0, keepdims=True))
                shrink = jnp.exp(top - newest)
                probs = jnp.exp(scores - newest)
                total = total * shrink + jnp.sum(probs, axis=0, keepdims=True)
                acc = acc * shrink + matmul(self.values_t[h, :, columns], probs.astype(bf16))
                result.append((newest, total, acc))
            return tuple(result)

        state = tuple(
            (
                jnp.full((1, block), masked_value, f32),
                jnp.zeros((1, block), f32),
                jnp.zeros((width, block), f32),
            )
            for h in range(heads)
        )
        state = lax.fori_loop(0, i, lambda j, s: step(j, s, False), state)
        state = step(i, state, True)
        finished = []
        for h in range(heads):
            top, total, acc = state[h]
            result = acc / total
            self.out_t[b, h, :, rows] = result
            self.lse[b, h, :, rows] = top + jnp.log(total)
            finished.append(result)
        joined = finished[0] if heads == 1 else jnp.concatenate(finished, axis=0)
        self.out[b, i] = joined.T.astype(bf16).reshape(self.out.shape[2:])

    def run(self, after, each=None):
        blocks = self.blocks

        def body(n, _):
            b, i = n // blocks, n % blocks
            pl.when(i == 0)(lambda: self.prepare(b))
            self.one(b, i)
            if each is not None:
                each(b, i)
            follow(n, after)
            return 0

        lax.fori_loop(0, self.qkv.shape[0] * blocks, body, 0)


def forward_kernel(heads, width, *refs):
    Forward(heads, width, *refs).run({})


def saved_shapes(seqs, length, heads, width):
    return (
        jax.ShapeDtypeStruct((seqs, heads, width, length), f32),
        jax.ShapeDtypeStruct((seqs, heads, 1, length), f32),
    )


def forward_scratch(length, heads, width):
    return [
        pltpu.VMEM((heads, length, 2 * width), bf16),
        pltpu.VMEM((heads, length, 2 * width), bf16),
        pltpu.VMEM((heads, width, length), bf16),
    ]


def attention_forward(qkv, slopes, heads, width):
    seqs, blocks, ranks, piece, _ = qkv.shape
    length = blocks * ranks * piece
    return pl.pallas_call(
        functools.partial(forward_kernel, heads, width),
        name="attention_forward",
        out_shape=(
            jax.ShapeDtypeStruct((seqs, blocks, ranks, piece, heads * width), bf16),
            *saved_shapes(seqs, length, heads, width),
        ),
        in_specs=[SMEM, VMEM],
        out_specs=(VMEM, VMEM, VMEM),
        scratch_shapes=forward_scratch(length, heads, width),
        compiler_params=pltpu.CompilerParams(vmem_limit_bytes=vmem_bytes),
    )(slopes, qkv)


class Backward:
    def __init__(
        self, heads, width, slopes, qkv, diff, out_t, lse, joined,
        keys, queries, keys_t, values, diffs, delta, query_acc,
    ):
        self.heads, self.width, self.slopes, self.qkv, self.diff = heads, width, slopes, qkv, diff
        self.out_t, self.lse, self.joined = out_t, lse, joined
        self.keys, self.queries, self.keys_t, self.values = keys, queries, keys_t, values
        self.diffs, self.delta, self.query_acc = diffs, delta, query_acc
        self.head = 0
        self.blocks = qkv.shape[1]
        self.block = qkv.shape[2] * qkv.shape[3]

    def rows(self, i):
        return pl.ds(pl.multiple_of(i * self.block, self.block), self.block)

    def prepare(self, b):
        width, block, qkv = self.width, self.block, self.qkv
        scale = 1.0 / math.sqrt(width)

        def body(i, _):
            rows = self.rows(i)
            for h in range(self.heads):
                base = h * 3 * width
                query, key, value = [
                    qkv[b, i, :, :, base + n * width : base + (n + 1) * width].reshape(block, width)
                    for n in range(3)
                ]
                self.keys[h, rows, :] = key_columns(key, self.slopes[self.head + h], i * block)
                self.keys_t[h, :, rows] = key.astype(f32).T.astype(bf16)
                self.queries[h, rows, :] = query_columns(query, scale)
                self.values[h, rows, :] = value
                part = self.diff[b, i, :, :, h * width : (h + 1) * width].reshape(block, width)
                self.diffs[h, rows, :] = part
                self.delta[h, :, rows] = jnp.sum(
                    part.astype(f32).T * self.out_t[b, h, :, rows], axis=0, keepdims=True
                )
                self.query_acc[h, :, rows] = jnp.zeros((width, block), f32)
            return 0

        lax.fori_loop(0, self.blocks, body, 0)

    def one(self, b, j):
        heads, width, block = self.heads, self.width, self.block
        tail = self.joined.shape[2:4] + (width,)
        columns = self.rows(j)

        def step(i, state, diagonal):
            rows = self.rows(i)
            result = []
            for h in range(heads):
                key_acc, value_acc = state[h]
                query = self.queries[h, rows, :]
                part = self.diffs[h, rows, :]
                scores = matmul_rt(self.keys[h, columns, :], query)
                probs = jnp.exp(scores - self.lse[b, h, :, rows])
                if diagonal:
                    key_at = lax.broadcasted_iota(jnp.int32, (block, block), 0)
                    query_at = lax.broadcasted_iota(jnp.int32, (block, block), 1)
                    probs = jnp.where(key_at <= query_at, probs, 0.0)
                prob_diff = matmul_rt(self.values[h, columns, :], part)
                score_diff = (probs * (prob_diff - self.delta[h, :, rows])).astype(bf16)
                value_acc = value_acc + matmul(probs.astype(bf16), part)
                key_acc = key_acc + matmul(score_diff, query)
                self.query_acc[h, :, rows] += matmul(self.keys_t[h, :, columns], score_diff)
                result.append((key_acc, value_acc))
            return tuple(result)

        state = tuple(
            (jnp.zeros((block, 2 * width), f32), jnp.zeros((block, width), f32))
            for h in range(heads)
        )
        state = step(j, state, True)
        state = lax.fori_loop(j + 1, self.blocks, lambda i, s: step(i, s, False), state)
        for h in range(heads):
            base = (h * 3 + 1) * width
            key_acc, value_acc = state[h]
            self.joined[b, j, :, :, base : base + width] = (
                key_acc[:, :width].astype(bf16).reshape(tail)
            )
            self.joined[b, j, :, :, base + width : base + 2 * width] = value_acc.astype(
                bf16
            ).reshape(tail)

    def run(self, after, each=None):
        blocks = self.blocks

        def body(n, _):
            b, j = n // blocks, n % blocks
            pl.when(j == 0)(lambda: self.prepare(b))
            self.one(b, j)
            self.finish(b, j)
            if each is not None:
                each(b, j)
            follow(n, after)
            return 0

        lax.fori_loop(0, self.qkv.shape[0] * blocks, body, 0)

    def finish(self, b, j):
        width = self.width
        scale = 1.0 / math.sqrt(width)
        for h in range(self.heads):
            base = h * 3 * width
            result = (self.query_acc[h, :, self.rows(j)] * scale).T.astype(bf16)
            self.joined[b, j, :, :, base : base + width] = result.reshape(
                self.joined.shape[2:4] + (width,)
            )


def backward_kernel(heads, width, *refs):
    Backward(heads, width, *refs).run({})


def backward_scratch(length, heads, width):
    return [
        pltpu.VMEM((heads, length, 2 * width), bf16),
        pltpu.VMEM((heads, length, 2 * width), bf16),
        pltpu.VMEM((heads, width, length), bf16),
        pltpu.VMEM((heads, length, width), bf16),
        pltpu.VMEM((heads, length, width), bf16),
        pltpu.VMEM((heads, 1, length), f32),
        pltpu.VMEM((heads, width, length), f32),
    ]


def attention_backward(qkv, diff, out_t, lse, slopes, heads, width):
    length = qkv.shape[1] * qkv.shape[2] * qkv.shape[3]
    return pl.pallas_call(
        functools.partial(backward_kernel, heads, width),
        name="attention_backward",
        out_shape=jax.ShapeDtypeStruct(qkv.shape, bf16),
        in_specs=[SMEM, VMEM, VMEM, VMEM, VMEM],
        out_specs=VMEM,
        scratch_shapes=backward_scratch(length, heads, width),
        compiler_params=pltpu.CompilerParams(vmem_limit_bytes=vmem_bytes),
    )(slopes, qkv, diff, out_t, lse)


def to_own_seqs(values):
    seqs, piece, features = values.shape
    parts = lax.axis_size("fs")
    values = values.reshape(parts, seqs // parts, piece, features)
    return lax.all_to_all(values, "fs", split_axis=0, concat_axis=0).transpose(1, 0, 2, 3)


def from_own_seqs(values):
    own, parts, piece, features = values.shape
    values = lax.all_to_all(values.transpose(1, 0, 2, 3), "fs", split_axis=0, concat_axis=0)
    return values.reshape(parts * own, piece, features)


def to_heads(values):
    own, parts, piece, features = values.shape
    ranks = lax.axis_size("sp")
    values = values.reshape(own, parts, piece, ranks, features // ranks)
    return lax.all_to_all(values, "sp", split_axis=3, concat_axis=2)


def from_heads(values):
    own, parts, ranks, piece, features = values.shape
    values = lax.all_to_all(values, "sp", split_axis=2, concat_axis=3)
    return values.reshape(own, parts, piece, ranks * features)


class Copies:
    def __init__(self, send, recv, local):
        self.send, self.recv, self.local = send, recv, local
        self.used, self.used_local, self.made, self.partial = 0, 0, [], []

    def plan(self, source, target, device, at=None, only=None):
        send, recv = (self.used, self.used) if at is None else at
        copy = pltpu.make_async_remote_copy(
            src_ref=source,
            dst_ref=target,
            send_sem=self.send.at[send],
            recv_sem=self.recv.at[recv],
            device_id=device,
            device_id_type=MESH,
        )
        if at is None:
            self.used += 1
        if only is None:
            self.made.append(copy)
        else:
            self.partial.append((only, copy))
        return copy

    def take(self, count):
        self.used += count
        return range(self.used - count, self.used)

    def inside(self, source, target):
        copy = pltpu.make_async_copy(source, target, self.local.at[self.used_local])
        self.used_local += 1
        return copy

    def finish(self):
        assert (self.used, self.used_local) == (self.send.shape[0], self.local.shape[0])
        for copy in self.made:
            copy.wait_send()
        for only, copy in self.partial:
            pl.when(only)(copy.wait_send)


def go(copies):
    for copy in copies:
        copy.start()


def arrive(copies):
    for copy in copies:
        copy.wait_recv()


def done(copies):
    for copy in copies:
        copy.wait()


def greet(devices):
    barrier = pltpu.get_barrier_semaphore()
    for device in devices:
        pl.semaphore_signal(barrier, inc=1, device_id=device, device_id_type=MESH)
    pl.semaphore_wait(barrier, len(devices))


def paired(z, mask):
    return 2 * ((z // 2 + mask // 2) % 2) + (z + mask) % 2


class Place:
    def __init__(self):
        z, s = lax.axis_index("fs"), lax.axis_index("sp")
        self.z, self.s = z, s
        self.core, self.chip = s % 2, s // 2
        self.x, self.y = self.chip % 2, self.chip // 2
        self.along_x = s + 2 - 4 * self.x
        self.along_y = s + 4 - 8 * self.y
        self.partner = s + 1 - 2 * self.core
        self.diagonal = self.along_x + self.along_y - s
        self.chip_x, self.chip_y = self.along_x // 2, self.along_y // 2
        self.lines = [(paired(z, 3 - k), s) for k in range(3)]
        self.plane = [(z, lax.rem(s + d, 8)) for d in range(1, 8)]
        self.to_x, self.to_y, self.to_core = [
            (z, to) for to in (self.along_x, self.along_y, self.partner)
        ]
        self.beside = z + 1 - 2 * (z % 2)
        self.inner = ((z + 1) // 2) % 2
        self.other_inner, self.other_outer = 2 - z // 2, 3 * (1 - z // 2)
        self.near = self.lines + [self.to_x, self.to_y, self.to_core]


class Gather:
    copies_each = 33

    def __init__(self, place, weights, wholes, kept, chunks, copies, given=None, relayed=()):
        z, s, lines = place.z, place.s, place.lines
        self.is_given = given is not None
        self.inner, self.passed = place.inner == 1, {}
        self.loads, self.own = [], []
        for weight, whole, keep in zip(weights, wholes, kept):
            if keep is None:
                self.loads.append(copies.inside(weight, whole.at[z]))
            else:
                self.loads.append(copies.inside(weight, keep))
                self.own.append(copies.inside(keep, whole.at[z]))
        self.first, self.second, self.third, self.cores, self.last = [], [], [], [], []
        for t, row, rows, column, columns in chunks:
            whole = wholes[t]
            wide = pl.ds(column, columns)
            every = pl.ds(row, rows)
            low, high = pl.ds(row, rows // 2), pl.ds(row + rows // 2, rows // 2)

            def same(k, rank, part, to):
                where = (k, rank, part, wide)
                return copies.plan(whole.at[where], whole.at[where], to)

            number = len(self.first)
            if number in relayed:
                near, middle, far, second = copies.take(4)
                part = (s, every, wide)
                beside = (place.beside, s)
                first = [
                    copies.plan(
                        weights[t].at[part], whole.at[(z, *part)], beside, at=(near, near)
                    ),
                    copies.plan(
                        weights[t].at[part],
                        whole.at[(z, *part)],
                        (place.other_inner, s),
                        at=(second, middle + 1 - place.inner),
                    ),
                ]
                self.passed[number] = [
                    copies.plan(
                        whole.at[(k, *part)], whole.at[(k, *part)], beside, at=(n, n),
                        only=self.inner,
                    )
                    for k, n in ((place.other_inner, middle), (place.other_outer, far))
                ]
            elif given is None:
                first = [
                    copies.plan(weights[t].at[s, every, wide], whole.at[z, s, every, wide], to)
                    for to in lines
                ]
            else:
                first = [
                    copies.inside(given.at[k, every, wide], whole.at[k, s, every, wide])
                    for k, _ in lines
                ]
            self.first.append(first)
            second, third, cores, last = [], [], [], []
            for k, _ in lines:
                second.append(same(k, s, low, place.to_x))
                second.append(same(k, s, high, place.to_y))
                cores.append(same(k, s, every, place.to_core))
                third.append(same(k, s, low, place.to_y))
                third.append(same(k, s, high, place.to_x))
                third.append(same(k, place.along_x, low, place.to_y))
                third.append(same(k, place.along_y, high, place.to_x))
                for rank in (place.along_x, place.along_y, place.diagonal):
                    last.append(same(k, rank, every, place.to_core))
            self.second.append(second)
            self.third.append(third)
            self.cores.append(cores)
            self.last.append(last)

    def keep(self):
        done(self.loads)
        go(self.own)

    def start(self, t):
        go(self.first[t])

    def exchange(self, t):
        if t in self.passed:
            arrive(self.first[t][:1])
            for copy in self.passed[t]:
                copy.wait_recv()
                pl.when(self.inner)(copy.start)
        elif self.is_given:
            done(self.first[t])
        else:
            arrive(self.first[t])
        go(self.second[t])
        go(self.cores[t])

    def spread(self, t):
        arrive(self.second[t])
        go(self.third[t])

    def share(self, t):
        arrive(self.third[t])
        go(self.last[t])

    def complete(self, t):
        arrive(self.cores[t] + self.last[t])


def add_into(target, other):
    target[...] = (target[...].astype(f32) + other[...].astype(f32)).astype(target.dtype)


def add_blocks(steps, block_of):
    def body(i, _):
        add_into(*block_of(i))
        return 0

    lax.fori_loop(0, steps, body, 0)


class Reduce:
    copies_each = 10

    def __init__(self, place, grads, outs, bufs, chunks, copies):
        self.place, self.outs, self.chunks = place, outs, chunks
        self.bufs = [bufs[7 * t : 7 * t + 7] for t in range(len(chunks))]
        self.loads, self.first, self.second, self.third, self.fourth = [], [], [], [], []
        for (t, row, rows, column, columns), buf in zip(chunks, self.bufs):
            own, from_core, from_x, from_y, late_y, late_x, from_z = buf
            every, wide = pl.ds(row, rows), pl.ds(column, columns)
            low, high = pl.ds(0, rows // 2), pl.ds(rows // 2, rows // 2)
            self.loads.append(
                copies.inside(grads[t].at[:, :, place.core, every, wide], own)
            )
            self.first.append(
                copies.plan(
                    grads[t].at[:, :, 1 - place.core, every, wide], from_core, place.to_core
                )
            )
            step = []
            for k in range(2):
                step.append(
                    copies.plan(own.at[:, 2 * k + 1 - place.x, low], from_x.at[:, k], place.to_x)
                )
                step.append(
                    copies.plan(
                        own.at[:, 2 * (1 - place.y) + k, high], from_y.at[:, k], place.to_y
                    )
                )
            self.second.append(step)
            self.third.append(
                [
                    copies.plan(own.at[:, place.chip_y, low], late_y, place.to_y),
                    copies.plan(own.at[:, place.chip_x, high], late_x, place.to_x),
                ]
            )
            self.fourth.append(
                [
                    copies.plan(own.at[to[0], place.chip], from_z.at[k], to)
                    for k, to in enumerate(place.lines)
                ]
            )

    def start(self):
        go(self.first)

    def begin(self, t):
        go([self.loads[t], self.first[t]])

    def halves(self, t):
        half = self.chunks[t][2] // 2
        return pl.ds(0, half), pl.ds(half, half)

    def exchange(self, t):
        own, from_core = self.bufs[t][:2]
        self.loads[t].wait()
        arrive([self.first[t]])
        add_blocks(16, lambda i: (own.at[i // 4, i % 4], from_core.at[i // 4, i % 4]))
        go(self.second[t])

    def spread(self, t):
        own, _, from_x, from_y = self.bufs[t][:4]
        low, high = self.halves(t)
        x, y = self.place.x, self.place.y
        arrive(self.second[t])
        add_blocks(8, lambda i: (own.at[i // 2, 2 * (i % 2) + x, low], from_x.at[i // 2, i % 2]))
        add_blocks(8, lambda i: (own.at[i // 2, 2 * y + i % 2, high], from_y.at[i // 2, i % 2]))
        go(self.third[t])

    def send(self, t):
        own, _, _, _, late_y, late_x, _ = self.bufs[t]
        low, high = self.halves(t)
        chip = self.place.chip
        arrive(self.third[t])
        add_blocks(4, lambda i: (own.at[i, chip, low], late_y.at[i]))
        add_blocks(4, lambda i: (own.at[i, chip, high], late_x.at[i]))
        go(self.fourth[t])

    def finish(self, t):
        own, from_z = self.bufs[t][0], self.bufs[t][6]
        index, row, rows, column, columns = self.chunks[t]
        arrive(self.fourth[t])
        total = own[self.place.z, self.place.chip].astype(f32)
        for k in range(3):
            total = total + from_z[k].astype(f32)
        self.outs[index][row : row + rows, column : column + columns] = total


def reduce_scratch(chunks):
    scratch = []
    for _, _, rows, _, columns in chunks:
        half = rows // 2
        scratch += [
            pltpu.VMEM((4, 4, rows, columns), bf16),
            pltpu.VMEM((4, 4, rows, columns), bf16),
            pltpu.VMEM((4, 2, half, columns), bf16),
            pltpu.VMEM((4, 2, half, columns), bf16),
            pltpu.VMEM((4, half, columns), bf16),
            pltpu.VMEM((4, half, columns), bf16),
            pltpu.VMEM((3, rows, columns), bf16),
        ]
    return scratch


class ReduceAlong(Reduce):
    def __init__(self, place, grad, out, buf, chunk, copies):
        self.place, self.grad, self.out, self.buf, self.chunk = place, grad, out, buf, chunk
        own, from_core, from_z, from_x, from_y, late_y, late_x = buf
        _, row, rows, column, columns = chunk
        every, wide = pl.ds(row, rows), pl.ds(column, columns)
        self.low, self.high = low, high = pl.ds(0, rows // 2), pl.ds(rows // 2, rows // 2)
        z, x, y = place.z, place.x, place.y
        self.load = copies.inside(grad.at[:, :, place.core, every, wide], own)
        self.first = copies.plan(
            grad.at[:, :, 1 - place.core, every, wide], from_core, place.to_core
        )
        self.second = [
            copies.plan(own.at[to[0]], from_z.at[k], to) for k, to in enumerate(place.lines)
        ]
        self.third = []
        for k in range(2):
            self.third.append(
                copies.plan(own.at[z, 2 * k + 1 - x, low], from_x.at[k], place.to_x)
            )
            self.third.append(
                copies.plan(own.at[z, 2 * (1 - y) + k, high], from_y.at[k], place.to_y)
            )
        self.fourth = [
            copies.plan(own.at[z, place.chip_y, low], late_y, place.to_y),
            copies.plan(own.at[z, place.chip_x, high], late_x, place.to_x),
        ]

    def exchange(self):
        own, from_core = self.buf[:2]
        self.load.wait()
        arrive([self.first])
        add_blocks(16, lambda i: (own.at[i // 4, i % 4], from_core.at[i // 4, i % 4]))
        go(self.second)

    def spread(self):
        own, _, from_z = self.buf[:3]
        z = self.place.z
        arrive(self.second)

        def body(i, _):
            total = own[z, i].astype(f32)
            for k in range(3):
                total = total + from_z[k, i].astype(f32)
            own[z, i] = total.astype(bf16)
            return 0

        lax.fori_loop(0, 4, body, 0)
        go(self.third)

    def send(self):
        own, _, _, from_x, from_y = self.buf[:5]
        z, x, y = self.place.z, self.place.x, self.place.y
        arrive(self.third)
        add_blocks(2, lambda j: (own.at[z, 2 * j + x, self.low], from_x.at[j]))
        add_blocks(2, lambda j: (own.at[z, 2 * y + j, self.high], from_y.at[j]))
        go(self.fourth)

    def finish(self):
        own, late_y, late_x = self.buf[0], self.buf[5], self.buf[6]
        z, chip = self.place.z, self.place.chip
        _, row, rows, column, columns = self.chunk
        arrive(self.fourth)
        half = rows // 2
        wide = slice(column, column + columns)
        self.out[row : row + half, wide] = own[z, chip, self.low].astype(f32) + late_y[...].astype(
            f32
        )
        self.out[row + half : row + rows, wide] = own[z, chip, self.high].astype(f32) + late_x[
            ...
        ].astype(f32)


def reduce_along_scratch(chunk):
    _, _, rows, _, columns = chunk
    half = rows // 2
    return [
        pltpu.VMEM((4, 4, rows, columns), bf16),
        pltpu.VMEM((4, 4, rows, columns), bf16),
        pltpu.VMEM((3, 4, rows, columns), bf16),
        pltpu.VMEM((2, half, columns), bf16),
        pltpu.VMEM((2, half, columns), bf16),
        pltpu.VMEM((half, columns), bf16),
        pltpu.VMEM((half, columns), bf16),
    ]


class HandBack:
    def __init__(self, place, source, target, features, send, recv, local):
        self.place, self.source, self.target = place, source, target
        self.mine = columns_of(place.s, features)
        self.send, self.recv, self.local = send, recv, local
        self.blocks = source.shape[1]

    def copy(self, b, i, d):
        rank = self.place.plane[d][1]
        n = b * self.blocks + i
        return pltpu.make_async_remote_copy(
            src_ref=self.source.at[b, i, rank],
            dst_ref=self.target.at[b, i, :, self.mine],
            send_sem=self.send.at[n, d],
            recv_sem=self.recv.at[n, d],
            device_id=self.place.plane[d],
            device_id_type=MESH,
        )

    def own(self, b, i):
        return pltpu.make_async_copy(
            self.source.at[b, i, self.place.s],
            self.target.at[b, i, :, self.mine],
            self.local.at[b * self.blocks + i],
        )

    def each(self, b, i):
        for d in range(7):
            self.copy(b, i, d).start()
        self.own(b, i).start()

    def finish(self):
        def body(n, _):
            b, i = n // self.blocks, n % self.blocks
            for d in range(7):
                self.copy(b, i, d).wait()
            self.own(b, i).wait()
            return 0

        lax.fori_loop(0, self.source.shape[0] * self.blocks, body, 0)


def hand_back_semaphores(steps):
    return [
        pltpu.SemaphoreType.DMA((steps, 7)),
        pltpu.SemaphoreType.DMA((steps, 7)),
        pltpu.SemaphoreType.DMA((steps,)),
    ]


class ReduceLines:
    copies = 4 * 7 + 3 + 3 + 6

    def __init__(self, place, grad, out, bufs, copies):
        self.place, self.grad, self.out, self.bufs = place, grad, out, bufs
        from_core, from_x, from_y, late_y, late_x, from_z = bufs[:6]
        early_z, own_x, own_y, own_late_y, own_late_x = bufs[6:]
        core, x, y = place.core, place.x, place.y
        self.order = [to[0] for to in place.lines] + [place.z]
        rows = grad.shape[3]
        low, high = pl.ds(0, rows // 2), pl.ds(rows // 2, rows // 2)
        cut = from_z.shape[2]
        most, rest = pl.ds(0, cut), pl.ds(cut, grad.shape[4] - cut)
        self.low, self.high, self.all = (low, most), (high, most), (pl.ds(0, rows), most)
        self.low_rest, self.high_rest = (low, rest), (high, rest)
        self.all_rest = (pl.ds(0, rows), rest)
        z = place.z
        self.early = [
            copies.plan(grad.at[(to[0], pl.ds(0, 4), core, *self.all_rest)], early_z.at[k], to)
            for k, to in enumerate(place.lines)
        ]
        self.own_second, self.own_third = [], []
        for j in range(2):
            self.own_second.append(
                copies.plan(
                    grad.at[(z, 2 * j + 1 - x, core, *self.low_rest)], own_x.at[j], place.to_x
                )
            )
            self.own_second.append(
                copies.plan(
                    grad.at[(z, 2 * (1 - y) + j, core, *self.high_rest)], own_y.at[j], place.to_y
                )
            )
        self.own_third = [
            copies.plan(
                grad.at[(z, place.chip_y, core, *self.low_rest)], own_late_y, place.to_y
            ),
            copies.plan(
                grad.at[(z, place.chip_x, core, *self.high_rest)], own_late_x, place.to_x
            ),
        ]
        self.first, self.second, self.third, self.fourth = [], [], [], []
        for k, at in enumerate(self.order):
            self.first.append(
                copies.plan(grad.at[at, :, 1 - core], from_core.at[k], place.to_core)
            )
            step = []
            for j in range(2):
                step.append(
                    copies.plan(
                        grad.at[(at, 2 * j + 1 - x, core, *self.low)], from_x.at[k, j], place.to_x
                    )
                )
                step.append(
                    copies.plan(
                        grad.at[(at, 2 * (1 - y) + j, core, *self.high)], from_y.at[k, j], place.to_y
                    )
                )
            self.second.append(step)
            self.third.append(
                [
                    copies.plan(
                        grad.at[(at, place.chip_y, core, *self.low)], late_y.at[k], place.to_y
                    ),
                    copies.plan(
                        grad.at[(at, place.chip_x, core, *self.high)], late_x.at[k], place.to_x
                    ),
                ]
            )
            if k < 3:
                self.fourth.append(
                    copies.plan(
                        grad.at[(at, place.chip, core, *self.all)], from_z.at[k], place.lines[k]
                    )
                )

    def start(self, k):
        go([self.first[k]])

    def exchange(self, k):
        arrive([self.first[k]])
        at, core = self.order[k], self.place.core
        add_blocks(4, lambda i: (self.grad.at[at, i, core], self.bufs[0].at[k, i]))
        go(self.second[k] + self.early[k : k + 1])

    def spread(self, k):
        arrive(self.second[k])
        at, core, x, y = self.order[k], self.place.core, self.place.x, self.place.y
        add_blocks(
            2, lambda j: (self.grad.at[(at, 2 * j + x, core, *self.low)], self.bufs[1].at[k, j])
        )
        add_blocks(
            2, lambda j: (self.grad.at[(at, 2 * y + j, core, *self.high)], self.bufs[2].at[k, j])
        )
        go(self.third[k])

    def send(self, k):
        arrive(self.third[k])
        at, core, chip = self.order[k], self.place.core, self.place.chip
        add_into(self.grad.at[(at, chip, core, *self.low)], self.bufs[3].at[k])
        add_into(self.grad.at[(at, chip, core, *self.high)], self.bufs[4].at[k])
        go(self.fourth[k : k + 1])

    def own_spread(self):
        arrive(self.early)
        z, core = self.place.z, self.place.core

        def body(i, _):
            target = self.grad.at[(z, i, core, *self.all_rest)]
            total = target[...].astype(f32)
            for k in range(3):
                total = total + self.bufs[6][k, i].astype(f32)
            target[...] = total.astype(bf16)
            return 0

        lax.fori_loop(0, 4, body, 0)
        go(self.own_second)

    def own_send(self):
        arrive(self.own_second)
        z, core, x, y = self.place.z, self.place.core, self.place.x, self.place.y
        for j in range(2):
            add_into(self.grad.at[(z, 2 * j + x, core, *self.low_rest)], self.bufs[7].at[j])
            add_into(self.grad.at[(z, 2 * y + j, core, *self.high_rest)], self.bufs[8].at[j])
        go(self.own_third)

    def finish(self):
        arrive(self.fourth + self.own_third)
        place = self.place
        at = (place.z, place.chip, place.core)
        total = self.grad[(*at, *self.all)].astype(f32)
        for k in range(3):
            total = total + self.bufs[5][k].astype(f32)
        cut = total.shape[1]
        half = total.shape[0] // 2
        self.out[:, :cut] = total
        self.out[:half, cut:] = self.grad[(*at, *self.low_rest)].astype(f32) + self.bufs[9][
            ...
        ].astype(f32)
        self.out[half:, cut:] = self.grad[(*at, *self.high_rest)].astype(f32) + self.bufs[10][
            ...
        ].astype(f32)


def reduce_lines_scratch(rows, columns, rest):
    half = rows // 2
    most = columns - rest
    return [
        pltpu.VMEM((4, 4, rows, columns), bf16),
        pltpu.VMEM((4, 2, half, most), bf16),
        pltpu.VMEM((4, 2, half, most), bf16),
        pltpu.VMEM((4, half, most), bf16),
        pltpu.VMEM((4, half, most), bf16),
        pltpu.VMEM((3, rows, most), bf16),
        pltpu.VMEM((3, 4, rows, rest), bf16),
        pltpu.VMEM((2, half, rest), bf16),
        pltpu.VMEM((2, half, rest), bf16),
        pltpu.VMEM((half, rest), bf16),
        pltpu.VMEM((half, rest), bf16),
    ]


def split_grad(item):
    return item.reshape(4, 4, 2, item.shape[0] // 32, item.shape[1])


def split_weight(item):
    return item.reshape(8, item.shape[0] // 8, item.shape[1])


def chunks_of(index, rows, columns, count):
    if rows >= 64:
        return [(index, rows // count * n, rows // count, 0, columns) for n in range(count)]
    return [(index, 0, rows, columns // count * n, columns // count) for n in range(count)]


def semaphores(remote, local):
    return [pltpu.SemaphoreType.DMA((n,)) for n in (remote, remote, local)]


def remote_call(kernel, name, collective, **options):
    return pl.pallas_call(
        kernel,
        name=name,
        compiler_params=pltpu.CompilerParams(
            collective_id=collective, has_side_effects=True, vmem_limit_bytes=vmem_bytes
        ),
        **options,
    )


def row_of(packed, n, size):
    found = [packed[k, n, r : r + 1, :] for k in range(4) for r in range(size // 512)]
    return jnp.concatenate(found, axis=1)


def columns_of(rank, features):
    return pl.ds(pl.multiple_of(rank * features, 128), features)


def forward_fused_kernel(heads, width, count, vector_count, chunks, slopes, tokens, upstream, *refs):
    vectors, refs = refs[:vector_count], refs[vector_count:]
    weights, contract, refs = refs[:count], refs[count], refs[count + 1 :]
    tokens_out, vectors_out, joined_out, qkv_out, attended, out_t, lse, upstream_out = refs[:8]
    contract_out = refs[8]
    wholes, refs = refs[9 : 8 + count], refs[8 + count :]
    held, small, values_of, joined, normed, outgoing, qkv, result, upstream_own = refs[:9]
    attention = Forward(heads, width, slopes, qkv, result, out_t, lse, *refs[9:12])
    kept, refs = refs[12 : 11 + count], refs[11 + count :]
    head_send, head_recv = refs[:2]
    copies = Copies(*refs[5:])
    place = Place()
    z, s, lines, plane = place.z, place.s, place.lines, place.plane
    attention.head = s * heads
    first = [t for t, chunk in enumerate(chunks) if chunk[0] == 0]
    gather = Gather(
        place, weights, [joined, *wholes], [None, *kept], chunks, copies, relayed=first
    )
    later = [t for t, chunk in enumerate(chunks) if chunk[0] > 0]
    features = heads * width
    back = HandBack(place, result, attended, features, *refs[2:5])
    own_seqs, parts, piece, wide = held.shape

    load = copies.inside(tokens.at[z], held.at[:, z])
    load_upstream = copies.inside(upstream.at[z], upstream_own)
    seqs = [copies.plan(tokens.at[to[0]], held.at[:, z], to) for to in lines]
    vector_copies = [copies.plan(small.at[z], small.at[z], to) for to in lines]
    upstreams = [copies.plan(upstream.at[to[0]], upstream_out.at[:, z], to) for to in lines]
    keep_upstream = copies.inside(upstream_own, upstream_out.at[:, z])
    keeping = [
        copies.inside(held, tokens_out),
        copies.inside(small, vectors_out),
        copies.inside(joined, joined_out),
    ]
    keep_qkv = copies.inside(qkv, qkv_out)
    contracts = [copies.plan(contract.at[s], contract_out.at[z], to) for to in lines]

    def to_head(d):
        return pltpu.make_async_remote_copy(
            src_ref=outgoing.at[d],
            dst_ref=qkv.at[:, :, s],
            send_sem=head_send.at[d],
            recv_sem=head_recv.at[d],
            device_id=(z, lax.rem(s + 1 + d, 8)),
            device_id_type=MESH,
        )

    go(gather.loads + [load, load_upstream])
    small[z] = jnp.zeros(small.shape[1:], bf16)
    for n, item in enumerate(vectors):
        small[z, n, : item.shape[0], :] = item[...]
    greet(lines + plane)
    for t in first:
        gather.start(t)
    go(seqs + vector_copies)
    gather.keep()
    load.wait()
    for t in range(len(first) + 2):
        if t < len(first):
            gather.exchange(t)
        if 0 <= t - 1 < len(first):
            gather.spread(t - 1)
        if 0 <= t - 2:
            gather.share(t - 2)
    load_upstream.wait()
    keep_upstream.start()
    arrive(seqs + vector_copies)
    for t in later:
        gather.start(t)
    values_of[...] = small[...].astype(f32)

    gain, shift = row_of(values_of, 0, wide), row_of(values_of, 1, wide)

    def norm(i, _):
        values = held[i // parts, i % parts].astype(f32)
        rows = pl.ds(pl.multiple_of(i * piece, piece), piece)
        normed[rows, :] = normalize(values, gain, shift).astype(bf16)
        return 0

    lax.fori_loop(0, own_seqs * parts, norm, 0)
    for t in first:
        gather.complete(t)
    go(keeping)

    def project(d, _):
        rank = lax.rem(s + 1 + d, 8)
        per = 8 // 4
        query_bias = values_of[rank // per, 2, pl.ds(rank % per, 1), :]
        value_bias = values_of[rank // per, 3, pl.ds(rank % per, 1), :]
        low = lax.broadcasted_iota(jnp.int32, query_bias.shape, 1) < width
        bias = jnp.concatenate(
            [
                jnp.where(low, query_bias, 0.0),
                jnp.where(low, value_bias, query_bias),
                jnp.where(low, 0.0, value_bias),
            ],
            axis=1,
        )
        weight = joined[:, :, :, columns_of(rank, 3 * features)].reshape(wide, 3 * features)
        made = (matmul(normed[...], weight) + bias).astype(bf16)
        outgoing[d] = made.reshape(outgoing.shape[1:])
        pl.when(d < 7)(lambda: to_head(d).start())
        return 0

    lax.fori_loop(0, 8, project, 0)
    own_copy = copies.inside(outgoing.at[7], qkv.at[:, :, s])
    own_copy.start()
    base = later[0]
    gather.exchange(base)
    gather.exchange(base + 1)
    own_copy.wait()
    gather.spread(base)
    go(contracts)
    for d in range(7):
        to_head(d).wait_recv()
    keep_qkv.start()
    attention.run(
        {
            0: [(gather.exchange, base + 2), (go, upstreams), (gather.spread, base + 1)],
            2: [(gather.spread, base + 2), (gather.share, base)],
            5: [(gather.share, base + 1)],
            6: [(gather.share, base + 2)],
        },
        back.each,
    )
    for t in later:
        gather.complete(t)
    arrive(contracts + upstreams)
    back.finish()
    for d in range(7):
        to_head(d).wait_send()
    copies.finish()
    done(gather.own + [keep_upstream, keep_qkv] + keeping)


def forward_fused(tokens, upstream, vectors, weights, contract, slopes, heads, width):
    seqs, piece, features = tokens.shape
    parts = 4
    own = seqs // parts
    columns = heads * width
    length = parts * 8 * piece
    vectors = [item.reshape(-1, 128) for item in vectors]
    cut = [split_weight(item) for item in weights]
    contract = split_weight(contract)
    count, tall = len(cut), 8 * -(-max(item.shape[0] for item in vectors) // 8)
    chunks = []
    for t, pieces in enumerate((3, 1, 2)):
        chunks += chunks_of(t, *cut[t].shape[1:], pieces)
    seq_shape = (own, parts, piece, features)
    qkv_shape = (own, parts, 8, piece, 3 * columns)
    small = (parts, len(vectors), tall, 128)
    out = remote_call(
        functools.partial(forward_fused_kernel, heads, width, count, len(vectors), chunks),
        "forward_fused",
        1,
        out_shape=(
            jax.ShapeDtypeStruct(seq_shape, bf16),
            jax.ShapeDtypeStruct(small, bf16),
            jax.ShapeDtypeStruct((parts, *cut[0].shape), bf16),
            jax.ShapeDtypeStruct(qkv_shape, bf16),
            jax.ShapeDtypeStruct(seq_shape, bf16),
            *saved_shapes(own, length, heads, width),
            jax.ShapeDtypeStruct(seq_shape, bf16),
            jax.ShapeDtypeStruct((parts, *contract.shape[1:]), bf16),
            *[jax.ShapeDtypeStruct((parts, *item.shape), bf16) for item in cut[1:]],
        ),
        in_specs=[SMEM, HBM, HBM] + [VMEM] * len(vectors) + [HBM] * (count + 1),
        out_specs=(HBM,) * 5 + (VMEM, VMEM) + (HBM,) * (count + 1),
        scratch_shapes=[
            pltpu.VMEM(seq_shape, bf16),
            pltpu.VMEM(small, bf16),
            pltpu.VMEM(small, f32),
            pltpu.VMEM((parts, *cut[0].shape), bf16),
            pltpu.VMEM((own * parts * piece, features), bf16),
            pltpu.VMEM((8, own, parts, piece, 3 * columns), bf16),
            pltpu.VMEM(qkv_shape, bf16),
            pltpu.VMEM((own, parts, 8, piece, columns), bf16),
            pltpu.VMEM((own, piece, features), bf16),
            *forward_scratch(length, heads, width),
            *[pltpu.VMEM(item.shape, bf16) for item in cut[1:]],
            pltpu.SemaphoreType.DMA((7,)),
            pltpu.SemaphoreType.DMA((7,)),
            *hand_back_semaphores(own * parts),
            *semaphores(12 + 3 + len(chunks) * Gather.copies_each, 2 * count - 1 + 8),
        ],
    )(
        slopes,
        tokens.reshape(parts, own, piece, features),
        upstream.reshape(parts, own, piece, features),
        *vectors,
        *cut,
        contract,
    )
    wholes = [
        whole.reshape(4 * item.shape[0], item.shape[1])
        for whole, item in zip((out[2], *out[9:]), weights)
    ]
    return out[0], out[1], [*wholes, out[8]], out[3], out[4], (out[5], out[6]), out[7]


def feed_forward_kernel(
    chunks, expand, contract, contract_line, out_weight,
    small, upstream, tokens, attended,
    layer, residual_grad, attended_diff, expand_grad, out_grad, contract_grad,
    bias_grad, gain_grad, shift_grad, out_bias_grad, contract_bias_grad,
    values_of, expand_bias, expand_in, contract_in, residual, second, second_t, expanded, activated, grad, staged, *refs,
):
    second_back = residual_grad
    bufs, refs = refs[:11], refs[11:]
    loaded, stored, refs = refs[0], refs[1], refs[2:]
    copies = Copies(*refs)
    place = Place()
    z = place.z
    reduce = ReduceLines(place, grad, contract_grad, bufs, copies)
    gather = Gather(
        place, [contract], [contract_in], [None], chunks, copies, given=contract_line
    )
    rows, features = second.shape
    steps = 8
    wide = expand.shape[1] // steps

    def at(n):
        part = paired(z, 3 - n // 2)
        return part, n % 2, pl.ds(pl.multiple_of((2 * part + n % 2) * wide, wide), wide)

    def load(n):
        _, _, where = at(n)
        return pltpu.make_async_copy(expand.at[:, where], expand_in.at[:, where], loaded.at[n])

    def contract_at(n):
        part, side, _ = at(n)
        return contract_in[part, pl.ds(4 * side, 4)].reshape(wide, features)

    def store(n):
        _, _, where = at(n)
        slot = n % 2
        return pltpu.make_async_copy(
            staged.at[slot], expand_grad.at[:, where], stored.at[slot]
        )

    halves = [pl.ds(0, wide), pl.ds(wide, wide)]
    out_loads = [
        pltpu.make_async_copy(out_weight.at[:, half], staged.at[n], stored.at[n])
        for n, half in enumerate(halves)
    ]
    out_stores = [
        pltpu.make_async_copy(staged.at[n], out_grad.at[:, half], stored.at[n])
        for n, half in enumerate(halves)
    ]
    part_rows = rows // 8

    def rows_at(i):
        return pl.ds(pl.multiple_of(i * part_rows, part_rows), part_rows)

    for n in range(len(chunks)):
        gather.start(n)
    go(out_loads)
    for n in range(steps):
        load(n).start()
    go(gather.loads)
    greet(place.near)
    for n in range(len(chunks)):
        gather.exchange(n)
    values_of[...] = small[...].astype(f32)
    out_bias, gain, shift, contract_bias = [
        row_of(values_of, n, features) for n in (4, 5, 6, 7)
    ]
    expand_bias[...] = row_of(values_of, 8, steps * wide)
    for n, half in enumerate(halves):
        out_loads[n].wait()
        bias = out_bias[:, n * wide : (n + 1) * wide]
        residual[:, half] = (
            tokens[:, half].astype(f32) + (matmul(attended[...], staged[n]) + bias)
        )

    def norm(i, _):
        values = residual[rows_at(i), :]
        second[rows_at(i), :] = normalize(values, gain, shift).astype(bf16)
        second_back[rows_at(i), :] = values + contract_bias
        return 0

    lax.fori_loop(0, 8, norm, 0)
    for n in range(len(chunks) - 1):
        gather.spread(n)
    second_t[...] = second[...].T

    def forward(n, after):
        part, side, where = at(n)
        load(n).wait()
        values = matmul(second[...], expand_in[:, where]) + expand_bias[:, where]
        expanded[:, where] = values
        low = gelu_tanh(values).astype(bf16)
        activated[:, where] = low
        made = matmul(low.T, upstream[...]).astype(bf16)
        grad[part, pl.ds(2 * side, 2)] = made.reshape(2, 2, wide // 4, features)
        follow(n, after)
        return 0

    def shrink(n, after):
        _, _, where = at(n)
        second_back[...] += matmul(activated[:, where], contract_at(n))
        follow(n, after)
        return 0

    def backward(n, after):
        _, _, where = at(n)
        values = expanded[:, where]
        act_grad = matmul_rt(upstream[...], contract_at(n))
        bent = jnp.tanh(gelu_coef * (values + 0.044715 * values * values * values))
        slope = 0.5 * (1.0 + bent) + 0.5 * values * (1.0 - bent * bent) * (
            gelu_coef * (1.0 + 3.0 * 0.044715 * values * values)
        )
        diff = (act_grad * slope).astype(bf16)
        bias_grad[:, where] = jnp.sum(diff.astype(f32), axis=0, keepdims=True)
        pl.when(n >= 2)(lambda: store(n - 2).wait())
        staged[n % 2] = matmul(second_t[...], diff).astype(bf16)
        store(n).start()
        second_back[...] += matmul_rt(diff, expand_in[:, where])
        follow(n, after)
        return 0

    last = len(chunks) - 1
    forward_steps = {
        0: [(gather.spread, last)],
        1: [(reduce.start, 0)],
        3: [(reduce.exchange, 0), (reduce.start, 1)],
        5: [(reduce.start, 2), (reduce.exchange, 1)],
        7: [(reduce.start, 3), (reduce.exchange, 2)] + [(gather.share, n) for n in range(last)],
    }
    shrink_steps = {
        1: [(reduce.exchange, 3)],
        3: [(reduce.spread, 0)],
        7: [(reduce.spread, 1)],
    }
    backward_steps = {
        1: [(reduce.spread, 2)],
        2: [(reduce.spread, 3)],
        3: [(reduce.send, 0), (reduce.own_spread,)],
        4: [(reduce.send, 1)],
        5: [(reduce.send, 2)],
        6: [(reduce.send, 3), (reduce.own_send,)],
    }
    lax.fori_loop(0, steps, lambda n, _: forward(n, forward_steps), 0)
    gather.share(last)
    for n in range(len(chunks)):
        gather.complete(n)
    done(gather.loads)
    lax.fori_loop(0, steps, lambda n, _: shrink(n, shrink_steps), 0)
    layer[...] = second_back[...].astype(bf16).reshape(layer.shape)
    second_back[...] = jnp.zeros_like(second_back)
    lax.fori_loop(0, steps, lambda n, _: backward(n, backward_steps), 0)
    store(steps - 2).wait()
    store(steps - 1).wait()
    go(out_loads)
    second_t[...] = attended[...].T

    def norm_back(i, sums):
        back = second_back[rows_at(i), :]
        part, normal = normalize_back(residual[rows_at(i), :], back, gain)
        given = upstream[rows_at(i), :].astype(f32)
        total = given + part
        low = total.astype(bf16)
        residual_grad[rows_at(i), :] = total
        second[rows_at(i), :] = low
        found = (back * normal, back, low.astype(f32), given)
        return tuple(
            kept + jnp.sum(item, axis=0, keepdims=True) for kept, item in zip(sums, found)
        )

    nothing = jnp.zeros((1, features), f32)
    sums = lax.fori_loop(0, 8, norm_back, (nothing,) * 4)
    gain_grad[...], shift_grad[...], out_bias_grad[...], contract_bias_grad[...] = sums
    done(out_loads)
    branch_diff = second
    made = matmul_rt(branch_diff[:, halves[0]], staged[0])
    made = (made + matmul_rt(branch_diff[:, halves[1]], staged[1])).astype(bf16)
    attended_diff[...] = made.reshape(attended_diff.shape)
    for n, half in enumerate(halves):
        staged[n] = matmul(second_t[...], branch_diff[:, half]).astype(bf16)
        out_stores[n].start()
    reduce.finish()
    done(out_stores)
    copies.finish()


def feed_forward(shape, expand, contract, line, out_weight, tokens, upstream, attended, small):
    own, parts, piece = shape
    rows, features = tokens.shape
    hidden = expand.shape[1]
    wide = hidden // 8
    each = hidden // 32
    contract = split_weight(contract)
    chunks = chunks_of(0, *contract.shape[1:], 2)
    seq_shape = (own, parts, piece, features)
    return remote_call(
        functools.partial(feed_forward_kernel, chunks),
        "feed_forward",
        4,
        out_shape=(
            jax.ShapeDtypeStruct(seq_shape, bf16),
            jax.ShapeDtypeStruct((rows, features), f32),
            jax.ShapeDtypeStruct(seq_shape, bf16),
            jax.ShapeDtypeStruct((features, hidden), bf16),
            jax.ShapeDtypeStruct((features, features), bf16),
            jax.ShapeDtypeStruct((each, features), f32),
            jax.ShapeDtypeStruct((1, hidden), f32),
            *[jax.ShapeDtypeStruct((1, features), f32)] * 4,
        ),
        in_specs=[HBM] * 4 + [VMEM] * 4,
        out_specs=(VMEM, VMEM, VMEM, HBM, HBM) + (VMEM,) * 6,
        scratch_shapes=[
            pltpu.VMEM(small.shape, f32),
            pltpu.VMEM((1, hidden), f32),
            pltpu.VMEM((features, hidden), bf16),
            pltpu.VMEM((4, *contract.shape), bf16),
            pltpu.VMEM((rows, features), f32),
            pltpu.VMEM((rows, features), bf16),
            pltpu.VMEM((features, rows), bf16),
            pltpu.VMEM((rows, hidden), f32),
            pltpu.VMEM((rows, hidden), bf16),
            pltpu.VMEM((4, 4, 2, each, features), bf16),
            pltpu.VMEM((2, features, wide), bf16),
            *reduce_lines_scratch(each, features, features // 4),
            pltpu.SemaphoreType.DMA((8,)),
            pltpu.SemaphoreType.DMA((2,)),
            *semaphores(
                ReduceLines.copies + len(chunks) * (Gather.copies_each - 3),
                1 + 3 * len(chunks),
            ),
        ],
    )(expand, contract, line, out_weight, small, upstream, tokens, attended)


def backward_fused_kernel(heads, width, count, chunks, *refs):
    slopes, diff_in, qkv_in, out_t_in, lse_in, layer = refs[:6]
    grads, refs = refs[6 : 6 + count], refs[6 + count :]
    joined_out, layer_out, layer_own = refs[0], refs[1], refs[2 + count]
    outs, refs = refs[2 : 2 + count], refs[3 + count :]
    diff, qkv, out_t, lse, joined = refs[:5]
    attention = Backward(heads, width, slopes, qkv, diff, out_t, lse, joined, *refs[5:12])
    bufs, refs = refs[12 : 12 + 7 * len(chunks)], refs[12 + 7 * len(chunks) :]
    copies = Copies(*refs[3:])
    place = Place()
    s, plane = place.s, place.plane
    attention.head = s * heads
    features = heads * width
    along = ReduceAlong(place, grads[0], outs[0], bufs[:7], chunks[0], copies)
    reduce = Reduce(place, grads, outs, bufs[7:], chunks[1:], copies)
    back = HandBack(place, joined, joined_out, 3 * features, *refs[:3])

    own = [copies.inside(diff_in.at[:, :, :, columns_of(s, features)], diff.at[:, :, s])]
    own += [copies.inside(a, b) for a, b in ((qkv_in, qkv), (out_t_in, out_t), (lse_in, lse))]
    arriving = [
        copies.plan(diff_in.at[:, :, :, columns_of(to[1], features)], diff.at[:, :, s], to)
        for to in plane
    ]
    returned = [copies.plan(layer.at[:, to[0]], layer_out.at[place.z], to) for to in place.lines]
    load_layer = copies.inside(layer.at[:, place.z], layer_own)
    keep_layer = copies.inside(layer_own, layer_out.at[place.z])
    go(own + reduce.loads + [along.load, load_layer])
    greet(place.lines + plane)
    go(arriving + [along.first])
    reduce.start()
    along.exchange()
    go(returned)
    for t in range(3):
        reduce.exchange(t)
    done(own + [load_layer])
    keep_layer.start()
    arrive(arriving)
    attention.run(
        {
            1: [(reduce.spread, 0)],
            2: [(along.spread,)],
            3: [(reduce.spread, 1), (reduce.spread, 2)],
            4: [(reduce.send, 0), (along.send,)],
            5: [(reduce.send, 1)],
            6: [(reduce.send, 2)],
        },
        back.each,
    )
    for t in range(3):
        reduce.finish(t)
    along.finish()
    back.finish()
    arrive(returned)
    copies.finish()
    keep_layer.wait()


def backward_fused(attended_diff, qkv, saved, layer, grads, slopes, heads, width):
    own, parts, piece, columns = attended_diff.shape
    features = heads * width
    length = parts * 8 * piece
    cut = [split_grad(item) for item in grads]
    count = len(cut)
    rows, wide = cut[0].shape[3:]
    part = 3 * wide // 8
    chunks = [
        (0, 0, rows, 0, wide // 4),
        (0, 0, rows, wide // 4, part),
        (0, 0, rows, wide // 4 + part, part),
        *chunks_of(1, *cut[1].shape[3:], 1),
    ]
    out = remote_call(
        functools.partial(backward_fused_kernel, heads, width, count, chunks),
        "backward_fused",
        2,
        out_shape=(
            jax.ShapeDtypeStruct((own, parts, piece, 24 * features), bf16),
            jax.ShapeDtypeStruct((parts, own, piece, columns), bf16),
            *[jax.ShapeDtypeStruct(item.shape[3:], f32) for item in cut],
        ),
        in_specs=[SMEM] + [HBM] * (5 + count),
        out_specs=(HBM, HBM) + (VMEM,) * count,
        scratch_shapes=[
            pltpu.VMEM((own, piece, columns), bf16),
            pltpu.VMEM((own, parts, 8, piece, features), bf16),
            pltpu.VMEM(qkv.shape, bf16),
            *[pltpu.VMEM(item.shape, f32) for item in saved],
            pltpu.VMEM(qkv.shape, bf16),
            *backward_scratch(length, heads, width),
            *reduce_along_scratch(chunks[0]),
            *reduce_scratch(chunks[1:]),
            *hand_back_semaphores(own * parts),
            *semaphores(10 + len(chunks) * Reduce.copies_each, len(chunks) + 6),
        ],
    )(slopes, attended_diff, qkv, *saved, layer, *cut)
    return out[0], out[1].reshape(parts * own, piece, columns), out[2:]


def end_kernel(
    width, joined_diff, joined_weight, tokens, residual_grad, small, out_bias_grad,
    second_gain_grad, second_shift_grad, contract_bias_grad, expand_bias_grad,
    input_out, vector_out, out,
    values_of, diff_in, weight_in, normed, normed_t, back, grads, held, vectors, others, ranks,
    *refs,
):
    count = grads.shape[0]
    bufs, refs = refs[: 7 * count], refs[7 * count :]
    loaded, copies = refs[0], Copies(*refs[1:])
    place = Place()
    z, lines, plane = place.z, place.lines, place.plane
    rows, features = tokens.shape
    own_seqs, parts, piece, _ = held.shape
    columns = [pl.ds(features * n, features) for n in range(count)]
    chunks = [(n, 0, grads.shape[4], 0, features) for n in range(count)]
    outs = [out.at[:, where] for where in columns]
    reduce = Reduce(place, [grads.at[n] for n in range(count)], outs, bufs, chunks, copies)
    loads = [
        (
            pltpu.make_async_copy(joined_diff.at[:, c], diff_in.at[:, c], loaded.at[0, n]),
            pltpu.make_async_copy(joined_weight.at[:, c], weight_in.at[:, c], loaded.at[1, n]),
        )
        for n, c in enumerate(columns)
    ]
    returned = [copies.plan(held.at[:, to[0]], input_out.at[z], to) for to in lines]
    stay = copies.inside(held.at[:, z], input_out.at[z])
    along = [copies.plan(vectors.at[to[0]], others.at[k], to) for k, to in enumerate(lines)]
    across = [copies.plan(ranks.at[0], ranks.at[d + 1], to) for d, to in enumerate(plane)]

    for load in loads:
        go(load)
    values_of[...] = small[...].astype(f32)
    gain, shift = row_of(values_of, 0, features), row_of(values_of, 1, features)
    greet(lines + plane)
    for n, where in enumerate(columns):
        done(loads[n])
        part = matmul_rt(diff_in[:, where], weight_in[:, where])
        back[...] = part if n == 0 else back[...] + part

    def norm_back(i, sums):
        at = pl.ds(pl.multiple_of(i * piece, piece), piece)
        values, given = tokens[at, :].astype(f32), back[at, :]
        part, normal = normalize_back(values, given, gain)
        normed[at, :] = (normal * gain + shift).astype(bf16)
        total = (residual_grad[at, :] + part).astype(bf16)
        held[i // parts, i % parts] = total
        found = (given * normal, given)
        return tuple(
            kept + jnp.sum(item, axis=0, keepdims=True) for kept, item in zip(sums, found)
        )

    nothing = jnp.zeros((1, features), f32)
    gain_grad, shift_grad = lax.fori_loop(0, own_seqs * parts, norm_back, (nothing, nothing))
    go(returned + [stay])
    normed_t[...] = normed[...].T
    sums = []
    for n, where in enumerate(columns):
        made = matmul(normed_t[...], diff_in[:, where]).astype(bf16)
        grads[n] = made.reshape(grads.shape[1:])
        reduce.begin(n)
        sums.append(jnp.sum(diff_in[:, where].astype(f32), axis=0, keepdims=True))
        if n > 0:
            reduce.exchange(n - 1)

    sums = jnp.concatenate(sums, axis=1)
    low = lax.broadcasted_iota(jnp.int32, (1, 128), 1) < width
    query_grad, value_grad = [], []
    for r in range(features // 128):
        first, middle, last = [sums[:, (3 * r + n) * 128 : (3 * r + n + 1) * 128] for n in range(3)]
        query_grad.append(jnp.where(low, first, middle))
        value_grad.append(jnp.where(low, middle, last))
    given = [
        gain_grad, shift_grad, jnp.concatenate(query_grad, axis=1),
        jnp.concatenate(value_grad, axis=1), out_bias_grad[...], second_gain_grad[...],
        second_shift_grad[...], contract_bias_grad[...], expand_bias_grad[...],
    ]
    row = 0
    for item in given:
        each = item.shape[1] // 512
        for k in range(4):
            for r in range(each):
                start = (k * each + r) * 128
                vectors[k, row + r : row + r + 1, :] = item[:, start : start + 128]
        row += each
    go(along)
    reduce.spread(0)
    reduce.exchange(count - 1)
    arrive(along)
    total = vectors[z]
    for k in range(3):
        total = total + others[k]
    ranks[0] = total
    go(across)
    for n in range(1, count):
        reduce.send(n - 1)
        reduce.spread(n)
    reduce.send(count - 1)
    arrive(across)
    total = ranks[0]
    for d in range(1, 8):
        total = total + ranks[d]
    vector_out[...] = total
    for n in range(count):
        reduce.finish(n)
    arrive(returned)
    copies.finish()
    stay.wait()


def end(shape, joined_diff, joined_weight, tokens, residual_grad, small, vectors, width):
    own, parts, piece = shape
    rows, features = tokens.shape
    count = joined_diff.shape[1] // features
    each = features // 32
    tall = (4 * features + sum(item.shape[1] for item in vectors)) // 512
    chunks = [(n, 0, each, 0, features) for n in range(count)]
    out = remote_call(
        functools.partial(end_kernel, width),
        "end",
        3,
        out_shape=(
            jax.ShapeDtypeStruct((parts, own, piece, features), bf16),
            jax.ShapeDtypeStruct((tall, 128), f32),
            jax.ShapeDtypeStruct((each, count * features), f32),
        ),
        in_specs=[HBM, HBM] + [VMEM] * (3 + len(vectors)),
        out_specs=(HBM, VMEM, VMEM),
        scratch_shapes=[
            pltpu.VMEM(small.shape, f32),
            pltpu.VMEM((rows, count * features), bf16),
            pltpu.VMEM((features, count * features), bf16),
            pltpu.VMEM((rows, features), bf16),
            pltpu.VMEM((features, rows), bf16),
            pltpu.VMEM((rows, features), f32),
            pltpu.VMEM((count, 4, 4, 2, each, features), bf16),
            pltpu.VMEM((own, parts, piece, features), bf16),
            pltpu.VMEM((4, tall, 128), f32),
            pltpu.VMEM((3, tall, 128), f32),
            pltpu.VMEM((8, tall, 128), f32),
            *reduce_scratch(chunks),
            pltpu.SemaphoreType.DMA((2, count)),
            *semaphores(3 + 3 + 7 + count * Reduce.copies_each, 1 + count),
        ],
    )(joined_diff, joined_weight, tokens, residual_grad, small, *vectors)
    return out[0].reshape(parts * own, piece, features), out[1], out[2]


def hand_out_kernel(sizes, vector, *refs):
    count = (len(refs) - len(sizes) - 1) // 3
    arrays, outs, smalls = refs[:count], refs[count : 2 * count], refs[2 * count :]
    smalls, kept, sems = smalls[: len(sizes)], smalls[len(sizes) : -1], refs[-1]
    s = lax.axis_index("sp")
    loads = [pltpu.make_async_copy(a, k, sems.at[n]) for n, (a, k) in enumerate(zip(arrays, kept))]
    stores = [
        pltpu.make_async_copy(k, o, sems.at[count + n]) for n, (k, o) in enumerate(zip(kept, outs))
    ]
    go(loads)
    row = 0
    for out, size in zip(smalls, sizes):
        per = 128 // size
        found = vector[pl.ds(row + s // per, 1), :]
        if per > 1:
            found = pltpu.roll(found, lax.rem(128 - s % per * size, 128), 1)
        out[...] = found[:, :size]
        row += 8 // per
    for load, store in zip(loads, stores):
        load.wait()
        store.start()
    done(stores)


def hand_out(vector, sizes, arrays):
    out = pl.pallas_call(
        functools.partial(hand_out_kernel, sizes),
        name="hand_out",
        out_shape=(
            *[jax.ShapeDtypeStruct(item.shape, item.dtype) for item in arrays],
            *[jax.ShapeDtypeStruct((1, size), f32) for size in sizes],
        ),
        in_specs=[VMEM] + [HBM] * len(arrays),
        out_specs=(HBM,) * len(arrays) + (VMEM,) * len(sizes),
        scratch_shapes=[
            *[pltpu.VMEM(item.shape, item.dtype) for item in arrays],
            pltpu.SemaphoreType.DMA((2 * len(arrays),)),
        ],
        compiler_params=pltpu.CompilerParams(vmem_limit_bytes=vmem_bytes),
    )(vector, *arrays)
    return out[: len(arrays)], [item.reshape(-1) for item in out[len(arrays) :]]


def per_device(
    layer_input,
    first_gain,
    first_shift,
    joined_weight,
    query_bias,
    value_bias,
    output_weight,
    output_bias,
    second_gain,
    second_shift,
    expand_weight,
    expand_bias,
    contract_weight,
    contract_bias,
    alibi_slopes,
    upstream,
):
    seqs, piece, features = layer_input.shape
    fs_count = lax.axis_size("fs")
    sp_count = lax.axis_size("sp")
    head_count = alibi_slopes.shape[0]
    width = features // head_count
    heads = head_count // sp_count
    rows = seqs * piece
    own = seqs // fs_count
    shape = (own, fs_count, piece)

    vectors = (
        first_gain, first_shift, query_bias, value_bias, output_bias,
        second_gain, second_shift, contract_bias, expand_bias,
    )
    fast = (fs_count, sp_count) == (4, 8) and (own, heads, width) == (2, 2, 64)
    fast = fast and expand_weight.shape[1] == 4 * features
    if fast:
        weights = (joined_weight, output_weight, expand_weight)
        tokens, small, weights, qkv, attended, saved, upstream_low = forward_fused(
            layer_input, upstream, vectors, weights, contract_weight, alibi_slopes, heads, width
        )
        joined_full, out_full, expand_full, contract_line = weights
        tokens = tokens.reshape(rows, features)
        (
            layer_output, residual_grad, attended_diff, expand_grad, output_weight_grad,
            contract_grad, eb, g2, s2, ob, cb,
        ) = feed_forward(
            shape, expand_full, contract_weight, contract_line, out_full, tokens,
            upstream_low.reshape(rows, features), attended.reshape(rows, features), small,
        )
        joined_diff, layer_output, grads = backward_fused(
            attended_diff, qkv, saved, layer_output, (expand_grad, output_weight_grad),
            alibi_slopes, heads, width,
        )
        input_grad, vector, joined_grad = end(
            shape, joined_diff.reshape(rows, 3 * features), joined_full, tokens, residual_grad,
            small, (ob, g2, s2, cb, eb), width,
        )
        devices = fs_count * sp_count
        sizes = [4 * item.shape[0] // devices for item in vectors]
        arrays, (g1, s1, qb, vb, ob, g2, s2, cb, eb) = hand_out(
            vector, sizes, (layer_output, input_grad, joined_grad, grads[1], grads[0], contract_grad)
        )
        layer_output, input_grad, joined_grad, output_grad, expand_grad, contract_grad = arrays
        return (
            layer_output, input_grad, g1, s1, joined_grad, qb, vb, output_grad, ob, g2, s2,
            expand_grad, eb, contract_grad, cb,
        )

    slopes = lax.dynamic_slice_in_dim(alibi_slopes, lax.axis_index("sp") * heads, heads)
    gather = lambda item: lax.all_gather(item, "fs", axis=0, tiled=True)
    scatter = functools.partial(
        lax.psum_scatter, axis_name=("fs", "sp"), scatter_dimension=0, tiled=True
    )
    gain_one, shift_one, qbias, vbias, obias, gain_two, shift_two, cbias, ebias = [
        gather(item).astype(f32) for item in vectors
    ]
    joined_full, out_full, expand_full, contract_full = [
        gather(item) for item in (joined_weight, output_weight, expand_weight, contract_weight)
    ]
    tokens = to_own_seqs(layer_input).reshape(rows, features).astype(f32)
    upstream_low = to_own_seqs(upstream).reshape(rows, features)

    normed_f, norm_back_one = jax.vjp(normalize, tokens, gain_one, shift_one)
    normed = normed_f.astype(bf16)
    joined_bias = joined_bias_of(qbias, vbias, head_count)
    joined_all = (matmul(normed, joined_full) + joined_bias).astype(bf16)
    qkv = to_heads(joined_all.reshape(*shape, 3 * features))
    attended, *saved = attention_forward(qkv, slopes, heads, width)
    attended = from_heads(attended).reshape(rows, features)
    upstream_f = upstream_low.astype(f32)
    contract_bias_grad = jnp.sum(upstream_f, axis=0)
    residual = tokens + (matmul(attended, out_full) + obias)
    second_f, norm_back_two = jax.vjp(normalize, residual, gain_two, shift_two)
    second = second_f.astype(bf16)
    expanded = matmul(second, expand_full) + ebias
    activated_f, gelu_back = jax.vjp(gelu_tanh, expanded)
    activated = activated_f.astype(bf16)
    result = residual + (matmul(activated, contract_full) + cbias)
    layer_output = result.astype(bf16).reshape(*shape, features)

    contract_grad = matmul_lt(activated, upstream_low)
    act_grad = matmul_rt(upstream_low, contract_full)
    expand_diff = gelu_back(act_grad)[0].astype(bf16)
    expand_grad = matmul_lt(second, expand_diff)
    expand_bias_grad = jnp.sum(expand_diff.astype(f32), axis=0)
    second_back = matmul_rt(expand_diff, expand_full)
    resid_part, second_gain_grad, second_shift_grad = norm_back_two(second_back)
    residual_grad = upstream_f + resid_part

    branch_diff = residual_grad.astype(bf16)
    output_weight_grad = matmul_lt(attended, branch_diff)
    output_bias_grad = jnp.sum(branch_diff.astype(f32), axis=0)
    attended_diff = matmul_rt(branch_diff, out_full).astype(bf16)
    attended_diff = attended_diff.reshape(*shape, features)
    joined_diff = attention_backward(qkv, to_heads(attended_diff), *saved, slopes, heads, width)
    joined_diff = from_heads(joined_diff).reshape(rows, 3 * features)
    joined_grad = matmul_lt(normed, joined_diff)
    column_sums = jnp.sum(joined_diff.astype(f32), axis=0).reshape(head_count, 3, width)
    query_bias_grad = column_sums[:, 0].reshape(features)
    value_bias_grad = column_sums[:, 2].reshape(features)
    normed_back = matmul_rt(joined_diff, joined_full)
    input_part, first_gain_grad, first_shift_grad = norm_back_one(normed_back)
    input_grad = (residual_grad + input_part).astype(bf16).reshape(*shape, features)

    vector_grads = (
        first_gain_grad, first_shift_grad, query_bias_grad, value_bias_grad,
        output_bias_grad, second_gain_grad, second_shift_grad, contract_bias_grad,
        expand_bias_grad,
    )
    devices = fs_count * sp_count
    packed = jnp.concatenate([item.reshape(devices, -1) for item in vector_grads], axis=1)
    packed = scatter(packed.reshape(-1))
    own_grads, at = [], 0
    for item in vector_grads:
        size = item.shape[0] // devices
        own_grads.append(packed[at : at + size])
        at += size
    g1, s1, qb, vb, ob, g2, s2, cb, eb = own_grads
    return (
        from_own_seqs(layer_output), from_own_seqs(input_grad), g1, s1, scatter(joined_grad), qb,
        vb, scatter(output_weight_grad), ob, g2, s2, scatter(expand_grad), eb,
        scatter(contract_grad), cb,
    )


def solution(mesh):
    tokens = P(None, ("fs", "sp"), None)
    both, both_rows = P(("fs", "sp")), P(("fs", "sp"), None)
    one, one_rows = P("fs"), P("fs", None)
    return jax.shard_map(
        per_device,
        mesh=mesh,
        in_specs=(
            tokens, one, one, one_rows, one, one, one_rows, one, one, one, one_rows, one,
            one_rows, one, P(), tokens,
        ),
        out_specs=(
            tokens, tokens, both, both, both_rows, both, both, both_rows, both, both, both,
            both_rows, both, both_rows, both,
        ),
        check_vma=False,
    )
```

```python
import functools
import math

import jax
import jax.numpy as jnp
from jax import lax
from jax.experimental import pallas as pl
from jax.experimental.pallas import tpu as pltpu
from jax.sharding import PartitionSpec as P

norm_eps = 1e-05
gelu_coef = 0.7978845608028654
masked_value = -1e30
f32 = jnp.float32
bf16 = jnp.bfloat16
MESH = pl.DeviceIdType.MESH
HBM = pl.BlockSpec(memory_space=pl.ANY)
VMEM = pl.BlockSpec(memory_space=pltpu.VMEM)
SMEM = pl.BlockSpec(memory_space=pltpu.SMEM)
vmem_bytes = 63 * 1024 * 1024


def normalize(values, norm_gain, norm_shift):
    center = values - jnp.mean(values, axis=-1, keepdims=True)
    variance = jnp.mean(center * center, axis=-1, keepdims=True)
    return center * lax.rsqrt(variance + norm_eps) * norm_gain + norm_shift


def normalize_back(values, back, norm_gain):
    center = values - jnp.mean(values, axis=-1, keepdims=True)
    inverse = lax.rsqrt(jnp.mean(center * center, axis=-1, keepdims=True) + norm_eps)
    normal = center * inverse
    scaled = back * norm_gain
    even = jnp.mean(scaled, axis=-1, keepdims=True)
    along = jnp.mean(scaled * normal, axis=-1, keepdims=True)
    return inverse * (scaled - even - normal * along), normal


def gelu_tanh(values):
    return (
        0.5 * values * (1.0 + jnp.tanh(gelu_coef * (values + 0.044715 * values * values * values)))
    )


def matmul(left_side, right_side):
    return jnp.dot(left_side, right_side, preferred_element_type=f32)


def matmul_lt(left_side, right_side):
    return lax.dot_general(
        left_side, right_side, (((0,), (0,)), ((), ())), preferred_element_type=f32
    )


def matmul_rt(left_side, right_side):
    return lax.dot_general(
        left_side, right_side, (((1,), (1,)), ((), ())), preferred_element_type=f32
    )


def joined_bias_of(query_bias, value_bias, head_count):
    query_part = query_bias.astype(f32).reshape(head_count, -1)
    value_part = value_bias.astype(f32).reshape(head_count, -1)
    return jnp.stack([query_part, jnp.zeros_like(query_part), value_part], axis=1).reshape(-1)


def split_three(values):
    high = values.astype(bf16).astype(f32)
    rest = values - high
    middle = rest.astype(bf16).astype(f32)
    return high, middle, rest - middle


def key_columns(key_rows, slope, start):
    rows, width = key_rows.shape
    position = (start + lax.broadcasted_iota(jnp.int32, (rows, width), 0)).astype(f32)
    lane = lax.broadcasted_iota(jnp.int32, (rows, width), 1)
    high, middle, low = split_three(slope * position)
    extra = jnp.where(lane == 0, high, jnp.where(lane == 1, middle, jnp.where(lane == 2, low, 0.0)))
    return jnp.concatenate([key_rows.astype(f32), extra], axis=1).astype(bf16)


def query_columns(queries, scale):
    rows, width = queries.shape
    lane = lax.broadcasted_iota(jnp.int32, (rows, width), 1)
    ones = jnp.where(lane < 3, 1.0, 0.0)
    return jnp.concatenate([queries.astype(f32) * scale, ones], axis=1).astype(bf16)


def follow(n, after):
    for at, steps in after.items():

        def act(steps=steps):
            for step, *given in steps:
                step(*given)

        pl.when(n == at)(act)


class Forward:
    def __init__(self, heads, width, slopes, qkv, out, out_t, lse, keys, queries, values_t):
        self.heads, self.width, self.slopes, self.qkv, self.out = heads, width, slopes, qkv, out
        self.out_t, self.lse = out_t, lse
        self.keys, self.queries, self.values_t = keys, queries, values_t
        self.head = 0
        self.blocks = qkv.shape[1]
        self.block = qkv.shape[2] * qkv.shape[3]

    def rows(self, i):
        return pl.ds(pl.multiple_of(i * self.block, self.block), self.block)

    def prepare(self, b):
        width, block, qkv = self.width, self.block, self.qkv
        scale = 1.0 / math.sqrt(width)

        def body(i, _):
            rows = self.rows(i)
            for h in range(self.heads):
                base = h * 3 * width
                query, key, value = [
                    qkv[b, i, :, :, base + n * width : base + (n + 1) * width].reshape(block, width)
                    for n in range(3)
                ]
                self.keys[h, rows, :] = key_columns(key, self.slopes[self.head + h], i * block)
                self.queries[h, rows, :] = query_columns(query, scale)
                self.values_t[h, :, rows] = value.astype(f32).T.astype(bf16)
            return 0

        lax.fori_loop(0, self.blocks, body, 0)

    def one(self, b, i):
        heads, width, block = self.heads, self.width, self.block
        rows = self.rows(i)
        query = [self.queries[h, rows, :] for h in range(heads)]

        def step(j, state, diagonal):
            columns = self.rows(j)
            result = []
            for h in range(heads):
                top, total, acc = state[h]
                scores = matmul_rt(self.keys[h, columns, :], query[h])
                if diagonal:
                    key_at = lax.broadcasted_iota(jnp.int32, (block, block), 0)
                    query_at = lax.broadcasted_iota(jnp.int32, (block, block), 1)
                    scores = jnp.where(key_at <= query_at, scores, masked_value)
                newest = jnp.maximum(top, jnp.max(scores, axis=0, keepdims=True))
                shrink = jnp.exp(top - newest)
                probs = jnp.exp(scores - newest)
                total = total * shrink + jnp.sum(probs, axis=0, keepdims=True)
                acc = acc * shrink + matmul(self.values_t[h, :, columns], probs.astype(bf16))
                result.append((newest, total, acc))
            return tuple(result)

        state = tuple(
            (
                jnp.full((1, block), masked_value, f32),
                jnp.zeros((1, block), f32),
                jnp.zeros((width, block), f32),
            )
            for h in range(heads)
        )
        state = lax.fori_loop(0, i, lambda j, s: step(j, s, False), state)
        state = step(i, state, True)
        finished = []
        for h in range(heads):
            top, total, acc = state[h]
            result = acc / total
            self.out_t[b, h, :, rows] = result
            self.lse[b, h, :, rows] = top + jnp.log(total)
            finished.append(result)
        joined = finished[0] if heads == 1 else jnp.concatenate(finished, axis=0)
        self.out[b, i] = joined.T.astype(bf16).reshape(self.out.shape[2:])

    def run(self, after, each=None):
        blocks = self.blocks

        def body(n, _):
            b, i = n // blocks, n % blocks
            pl.when(i == 0)(lambda: self.prepare(b))
            self.one(b, i)
            if each is not None:
                each(b, i)
            follow(n, after)
            return 0

        lax.fori_loop(0, self.qkv.shape[0] * blocks, body, 0)


def forward_kernel(heads, width, *refs):
    Forward(heads, width, *refs).run({})


def saved_shapes(seqs, length, heads, width):
    return (
        jax.ShapeDtypeStruct((seqs, heads, width, length), f32),
        jax.ShapeDtypeStruct((seqs, heads, 1, length), f32),
    )


def forward_scratch(length, heads, width):
    return [
        pltpu.VMEM((heads, length, 2 * width), bf16),
        pltpu.VMEM((heads, length, 2 * width), bf16),
        pltpu.VMEM((heads, width, length), bf16),
    ]


def attention_forward(qkv, slopes, heads, width):
    seqs, blocks, ranks, piece, _ = qkv.shape
    length = blocks * ranks * piece
    return pl.pallas_call(
        functools.partial(forward_kernel, heads, width),
        name="attention_forward",
        out_shape=(
            jax.ShapeDtypeStruct((seqs, blocks, ranks, piece, heads * width), bf16),
            *saved_shapes(seqs, length, heads, width),
        ),
        in_specs=[SMEM, VMEM],
        out_specs=(VMEM, VMEM, VMEM),
        scratch_shapes=forward_scratch(length, heads, width),
        compiler_params=pltpu.CompilerParams(vmem_limit_bytes=vmem_bytes),
    )(slopes, qkv)


class Backward:
    def __init__(
        self, heads, width, slopes, qkv, diff, out_t, lse, joined,
        keys, queries, keys_t, values, diffs, delta, query_acc,
    ):
        self.heads, self.width, self.slopes, self.qkv, self.diff = heads, width, slopes, qkv, diff
        self.out_t, self.lse, self.joined = out_t, lse, joined
        self.keys, self.queries, self.keys_t, self.values = keys, queries, keys_t, values
        self.diffs, self.delta, self.query_acc = diffs, delta, query_acc
        self.head = 0
        self.blocks = qkv.shape[1]
        self.block = qkv.shape[2] * qkv.shape[3]

    def rows(self, i):
        return pl.ds(pl.multiple_of(i * self.block, self.block), self.block)

    def prepare(self, b):
        width, block, qkv = self.width, self.block, self.qkv
        scale = 1.0 / math.sqrt(width)

        def body(i, _):
            rows = self.rows(i)
            for h in range(self.heads):
                base = h * 3 * width
                query, key, value = [
                    qkv[b, i, :, :, base + n * width : base + (n + 1) * width].reshape(block, width)
                    for n in range(3)
                ]
                self.keys[h, rows, :] = key_columns(key, self.slopes[self.head + h], i * block)
                self.keys_t[h, :, rows] = key.astype(f32).T.astype(bf16)
                self.queries[h, rows, :] = query_columns(query, scale)
                self.values[h, rows, :] = value
                part = self.diff[b, i, :, :, h * width : (h + 1) * width].reshape(block, width)
                self.diffs[h, rows, :] = part
                self.delta[h, :, rows] = jnp.sum(
                    part.astype(f32).T * self.out_t[b, h, :, rows], axis=0, keepdims=True
                )
                self.query_acc[h, :, rows] = jnp.zeros((width, block), f32)
            return 0

        lax.fori_loop(0, self.blocks, body, 0)

    def one(self, b, j):
        heads, width, block = self.heads, self.width, self.block
        tail = self.joined.shape[2:4] + (width,)
        columns = self.rows(j)

        def step(i, state, diagonal):
            rows = self.rows(i)
            result = []
            for h in range(heads):
                key_acc, value_acc = state[h]
                query = self.queries[h, rows, :]
                part = self.diffs[h, rows, :]
                scores = matmul_rt(self.keys[h, columns, :], query)
                probs = jnp.exp(scores - self.lse[b, h, :, rows])
                if diagonal:
                    key_at = lax.broadcasted_iota(jnp.int32, (block, block), 0)
                    query_at = lax.broadcasted_iota(jnp.int32, (block, block), 1)
                    probs = jnp.where(key_at <= query_at, probs, 0.0)
                prob_diff = matmul_rt(self.values[h, columns, :], part)
                score_diff = (probs * (prob_diff - self.delta[h, :, rows])).astype(bf16)
                value_acc = value_acc + matmul(probs.astype(bf16), part)
                key_acc = key_acc + matmul(score_diff, query)
                self.query_acc[h, :, rows] += matmul(self.keys_t[h, :, columns], score_diff)
                result.append((key_acc, value_acc))
            return tuple(result)

        state = tuple(
            (jnp.zeros((block, 2 * width), f32), jnp.zeros((block, width), f32))
            for h in range(heads)
        )
        state = step(j, state, True)
        state = lax.fori_loop(j + 1, self.blocks, lambda i, s: step(i, s, False), state)
        for h in range(heads):
            base = (h * 3 + 1) * width
            key_acc, value_acc = state[h]
            self.joined[b, j, :, :, base : base + width] = (
                key_acc[:, :width].astype(bf16).reshape(tail)
            )
            self.joined[b, j, :, :, base + width : base + 2 * width] = value_acc.astype(
                bf16
            ).reshape(tail)

    def run(self, after, each=None):
        blocks = self.blocks

        def body(n, _):
            b, j = n // blocks, n % blocks
            pl.when(j == 0)(lambda: self.prepare(b))
            self.one(b, j)
            self.finish(b, j)
            if each is not None:
                each(b, j)
            follow(n, after)
            return 0

        lax.fori_loop(0, self.qkv.shape[0] * blocks, body, 0)

    def finish(self, b, j):
        width = self.width
        scale = 1.0 / math.sqrt(width)
        for h in range(self.heads):
            base = h * 3 * width
            result = (self.query_acc[h, :, self.rows(j)] * scale).T.astype(bf16)
            self.joined[b, j, :, :, base : base + width] = result.reshape(
                self.joined.shape[2:4] + (width,)
            )


def backward_kernel(heads, width, *refs):
    Backward(heads, width, *refs).run({})


def backward_scratch(length, heads, width):
    return [
        pltpu.VMEM((heads, length, 2 * width), bf16),
        pltpu.VMEM((heads, length, 2 * width), bf16),
        pltpu.VMEM((heads, width, length), bf16),
        pltpu.VMEM((heads, length, width), bf16),
        pltpu.VMEM((heads, length, width), bf16),
        pltpu.VMEM((heads, 1, length), f32),
        pltpu.VMEM((heads, width, length), f32),
    ]


def attention_backward(qkv, diff, out_t, lse, slopes, heads, width):
    length = qkv.shape[1] * qkv.shape[2] * qkv.shape[3]
    return pl.pallas_call(
        functools.partial(backward_kernel, heads, width),
        name="attention_backward",
        out_shape=jax.ShapeDtypeStruct(qkv.shape, bf16),
        in_specs=[SMEM, VMEM, VMEM, VMEM, VMEM],
        out_specs=VMEM,
        scratch_shapes=backward_scratch(length, heads, width),
        compiler_params=pltpu.CompilerParams(vmem_limit_bytes=vmem_bytes),
    )(slopes, qkv, diff, out_t, lse)


def to_own_seqs(values):
    seqs, piece, features = values.shape
    parts = lax.axis_size("fs")
    values = values.reshape(parts, seqs // parts, piece, features)
    return lax.all_to_all(values, "fs", split_axis=0, concat_axis=0).transpose(1, 0, 2, 3)


def from_own_seqs(values):
    own, parts, piece, features = values.shape
    values = lax.all_to_all(values.transpose(1, 0, 2, 3), "fs", split_axis=0, concat_axis=0)
    return values.reshape(parts * own, piece, features)


def to_heads(values):
    own, parts, piece, features = values.shape
    ranks = lax.axis_size("sp")
    values = values.reshape(own, parts, piece, ranks, features // ranks)
    return lax.all_to_all(values, "sp", split_axis=3, concat_axis=2)


def from_heads(values):
    own, parts, ranks, piece, features = values.shape
    values = lax.all_to_all(values, "sp", split_axis=2, concat_axis=3)
    return values.reshape(own, parts, piece, ranks * features)


class Copies:
    def __init__(self, send, recv, local):
        self.send, self.recv, self.local = send, recv, local
        self.used, self.used_local, self.made, self.partial = 0, 0, [], []

    def plan(self, source, target, device, at=None, only=None):
        send, recv = (self.used, self.used) if at is None else at
        copy = pltpu.make_async_remote_copy(
            src_ref=source,
            dst_ref=target,
            send_sem=self.send.at[send],
            recv_sem=self.recv.at[recv],
            device_id=device,
            device_id_type=MESH,
        )
        if at is None:
            self.used += 1
        if only is None:
            self.made.append(copy)
        else:
            self.partial.append((only, copy))
        return copy

    def take(self, count):
        self.used += count
        return range(self.used - count, self.used)

    def inside(self, source, target):
        copy = pltpu.make_async_copy(source, target, self.local.at[self.used_local])
        self.used_local += 1
        return copy

    def finish(self):
        assert (self.used, self.used_local) == (self.send.shape[0], self.local.shape[0])
        for copy in self.made:
            copy.wait_send()
        for only, copy in self.partial:
            pl.when(only)(copy.wait_send)


def go(copies):
    for copy in copies:
        copy.start()


def arrive(copies):
    for copy in copies:
        copy.wait_recv()


def done(copies):
    for copy in copies:
        copy.wait()


def greet(devices):
    barrier = pltpu.get_barrier_semaphore()
    for device in devices:
        pl.semaphore_signal(barrier, inc=1, device_id=device, device_id_type=MESH)
    pl.semaphore_wait(barrier, len(devices))


def paired(z, mask):
    return 2 * ((z // 2 + mask // 2) % 2) + (z + mask) % 2


class Place:
    def __init__(self):
        z, s = lax.axis_index("fs"), lax.axis_index("sp")
        self.z, self.s = z, s
        self.core, self.chip = s % 2, s // 2
        self.x, self.y = self.chip % 2, self.chip // 2
        self.along_x = s + 2 - 4 * self.x
        self.along_y = s + 4 - 8 * self.y
        self.partner = s + 1 - 2 * self.core
        self.diagonal = self.along_x + self.along_y - s
        self.chip_x, self.chip_y = self.along_x // 2, self.along_y // 2
        self.lines = [(paired(z, 3 - k), s) for k in range(3)]
        self.plane = [(z, lax.rem(s + d, 8)) for d in range(1, 8)]
        self.to_x, self.to_y, self.to_core = [
            (z, to) for to in (self.along_x, self.along_y, self.partner)
        ]
        self.beside = z + 1 - 2 * (z % 2)
        self.inner = ((z + 1) // 2) % 2
        self.other_inner, self.other_outer = 2 - z // 2, 3 * (1 - z // 2)
        self.near = self.lines + [self.to_x, self.to_y, self.to_core]


class Gather:
    copies_each = 33

    def __init__(self, place, weights, wholes, kept, chunks, copies, given=None, relayed=()):
        z, s, lines = place.z, place.s, place.lines
        self.is_given = given is not None
        self.inner, self.passed = place.inner == 1, {}
        self.loads, self.own = [], []
        for weight, whole, keep in zip(weights, wholes, kept):
            if keep is None:
                self.loads.append(copies.inside(weight, whole.at[z]))
            else:
                self.loads.append(copies.inside(weight, keep))
                self.own.append(copies.inside(keep, whole.at[z]))
        self.first, self.second, self.third, self.cores, self.last = [], [], [], [], []
        for t, row, rows, column, columns in chunks:
            whole = wholes[t]
            wide = pl.ds(column, columns)
            every = pl.ds(row, rows)
            low, high = pl.ds(row, rows // 2), pl.ds(row + rows // 2, rows // 2)

            def same(k, rank, part, to):
                where = (k, rank, part, wide)
                return copies.plan(whole.at[where], whole.at[where], to)

            number = len(self.first)
            if number in relayed:
                near, middle, far, second = copies.take(4)
                part = (s, every, wide)
                beside = (place.beside, s)
                first = [
                    copies.plan(
                        weights[t].at[part], whole.at[(z, *part)], beside, at=(near, near)
                    ),
                    copies.plan(
                        weights[t].at[part],
                        whole.at[(z, *part)],
                        (place.other_inner, s),
                        at=(second, middle + 1 - place.inner),
                    ),
                ]
                self.passed[number] = [
                    copies.plan(
                        whole.at[(k, *part)], whole.at[(k, *part)], beside, at=(n, n),
                        only=self.inner,
                    )
                    for k, n in ((place.other_inner, middle), (place.other_outer, far))
                ]
            elif given is None:
                first = [
                    copies.plan(weights[t].at[s, every, wide], whole.at[z, s, every, wide], to)
                    for to in lines
                ]
            else:
                first = [
                    copies.inside(given.at[k, every, wide], whole.at[k, s, every, wide])
                    for k, _ in lines
                ]
            self.first.append(first)
            second, third, cores, last = [], [], [], []
            for k, _ in lines:
                second.append(same(k, s, low, place.to_x))
                second.append(same(k, s, high, place.to_y))
                cores.append(same(k, s, every, place.to_core))
                third.append(same(k, s, low, place.to_y))
                third.append(same(k, s, high, place.to_x))
                third.append(same(k, place.along_x, low, place.to_y))
                third.append(same(k, place.along_y, high, place.to_x))
                for rank in (place.along_x, place.along_y, place.diagonal):
                    last.append(same(k, rank, every, place.to_core))
            self.second.append(second)
            self.third.append(third)
            self.cores.append(cores)
            self.last.append(last)

    def keep(self):
        done(self.loads)
        go(self.own)

    def start(self, t):
        go(self.first[t])

    def pass_on(self, t):
        def act():
            for copy in self.passed[t]:
                copy.wait_recv()
                copy.start()

        pl.when(self.inner)(act)

    def exchange(self, t):
        if t in self.passed:
            arrive(self.first[t][:1])
            pl.when(jnp.logical_not(self.inner))(lambda: arrive(self.passed[t]))
        elif self.is_given:
            done(self.first[t])
        else:
            arrive(self.first[t])
        go(self.second[t])
        go(self.cores[t])

    def spread(self, t):
        arrive(self.second[t])
        go(self.third[t])

    def share(self, t):
        arrive(self.third[t])
        go(self.last[t])

    def complete(self, t):
        arrive(self.cores[t] + self.last[t])


def add_into(target, other):
    target[...] = (target[...].astype(f32) + other[...].astype(f32)).astype(target.dtype)


def add_blocks(steps, block_of):
    def body(i, _):
        add_into(*block_of(i))
        return 0

    lax.fori_loop(0, steps, body, 0)


class Reduce:
    copies_each = 10

    def __init__(self, place, grads, outs, bufs, chunks, copies):
        self.place, self.outs, self.chunks = place, outs, chunks
        self.bufs = [bufs[7 * t : 7 * t + 7] for t in range(len(chunks))]
        self.loads, self.first, self.second, self.third, self.fourth = [], [], [], [], []
        for (t, row, rows, column, columns), buf in zip(chunks, self.bufs):
            own, from_core, from_x, from_y, late_y, late_x, from_z = buf
            every, wide = pl.ds(row, rows), pl.ds(column, columns)
            low, high = pl.ds(0, rows // 2), pl.ds(rows // 2, rows // 2)
            self.loads.append(
                copies.inside(grads[t].at[:, :, place.core, every, wide], own)
            )
            self.first.append(
                copies.plan(
                    grads[t].at[:, :, 1 - place.core, every, wide], from_core, place.to_core
                )
            )
            step = []
            for k in range(2):
                step.append(
                    copies.plan(own.at[:, 2 * k + 1 - place.x, low], from_x.at[:, k], place.to_x)
                )
                step.append(
                    copies.plan(
                        own.at[:, 2 * (1 - place.y) + k, high], from_y.at[:, k], place.to_y
                    )
                )
            self.second.append(step)
            self.third.append(
                [
                    copies.plan(own.at[:, place.chip_y, low], late_y, place.to_y),
                    copies.plan(own.at[:, place.chip_x, high], late_x, place.to_x),
                ]
            )
            self.fourth.append(
                [
                    copies.plan(own.at[to[0], place.chip], from_z.at[k], to)
                    for k, to in enumerate(place.lines)
                ]
            )

    def start(self):
        go(self.first)

    def begin(self, t):
        go([self.loads[t], self.first[t]])

    def halves(self, t):
        half = self.chunks[t][2] // 2
        return pl.ds(0, half), pl.ds(half, half)

    def exchange(self, t):
        own, from_core = self.bufs[t][:2]
        self.loads[t].wait()
        arrive([self.first[t]])
        add_blocks(16, lambda i: (own.at[i // 4, i % 4], from_core.at[i // 4, i % 4]))
        go(self.second[t])

    def spread(self, t):
        own, _, from_x, from_y = self.bufs[t][:4]
        low, high = self.halves(t)
        x, y = self.place.x, self.place.y
        arrive(self.second[t])
        add_blocks(8, lambda i: (own.at[i // 2, 2 * (i % 2) + x, low], from_x.at[i // 2, i % 2]))
        add_blocks(8, lambda i: (own.at[i // 2, 2 * y + i % 2, high], from_y.at[i // 2, i % 2]))
        go(self.third[t])

    def send(self, t):
        own, _, _, _, late_y, late_x, _ = self.bufs[t]
        low, high = self.halves(t)
        chip = self.place.chip
        arrive(self.third[t])
        add_blocks(4, lambda i: (own.at[i, chip, low], late_y.at[i]))
        add_blocks(4, lambda i: (own.at[i, chip, high], late_x.at[i]))
        go(self.fourth[t])

    def finish(self, t):
        own, from_z = self.bufs[t][0], self.bufs[t][6]
        index, row, rows, column, columns = self.chunks[t]
        arrive(self.fourth[t])
        total = own[self.place.z, self.place.chip].astype(f32)
        for k in range(3):
            total = total + from_z[k].astype(f32)
        self.outs[index][row : row + rows, column : column + columns] = total


def reduce_scratch(chunks):
    scratch = []
    for _, _, rows, _, columns in chunks:
        half = rows // 2
        scratch += [
            pltpu.VMEM((4, 4, rows, columns), bf16),
            pltpu.VMEM((4, 4, rows, columns), bf16),
            pltpu.VMEM((4, 2, half, columns), bf16),
            pltpu.VMEM((4, 2, half, columns), bf16),
            pltpu.VMEM((4, half, columns), bf16),
            pltpu.VMEM((4, half, columns), bf16),
            pltpu.VMEM((3, rows, columns), bf16),
        ]
    return scratch


class ReduceAlong(Reduce):
    def __init__(self, place, grad, out, buf, chunk, copies):
        self.place, self.grad, self.out, self.buf, self.chunk = place, grad, out, buf, chunk
        own, from_core, from_z, from_x, from_y, late_y, late_x = buf
        _, row, rows, column, columns = chunk
        every, wide = pl.ds(row, rows), pl.ds(column, columns)
        self.low, self.high = low, high = pl.ds(0, rows // 2), pl.ds(rows // 2, rows // 2)
        z, x, y = place.z, place.x, place.y
        self.load = copies.inside(grad.at[:, :, place.core, every, wide], own)
        self.first = copies.plan(
            grad.at[:, :, 1 - place.core, every, wide], from_core, place.to_core
        )
        self.second = [
            copies.plan(own.at[to[0]], from_z.at[k], to) for k, to in enumerate(place.lines)
        ]
        self.third = []
        for k in range(2):
            self.third.append(
                copies.plan(own.at[z, 2 * k + 1 - x, low], from_x.at[k], place.to_x)
            )
            self.third.append(
                copies.plan(own.at[z, 2 * (1 - y) + k, high], from_y.at[k], place.to_y)
            )
        self.fourth = [
            copies.plan(own.at[z, place.chip_y, low], late_y, place.to_y),
            copies.plan(own.at[z, place.chip_x, high], late_x, place.to_x),
        ]

    def exchange(self):
        own, from_core = self.buf[:2]
        self.load.wait()
        arrive([self.first])
        add_blocks(16, lambda i: (own.at[i // 4, i % 4], from_core.at[i // 4, i % 4]))
        go(self.second)

    def spread(self):
        own, _, from_z = self.buf[:3]
        z = self.place.z
        arrive(self.second)

        def body(i, _):
            total = own[z, i].astype(f32)
            for k in range(3):
                total = total + from_z[k, i].astype(f32)
            own[z, i] = total.astype(bf16)
            return 0

        lax.fori_loop(0, 4, body, 0)
        go(self.third)

    def send(self):
        own, _, _, from_x, from_y = self.buf[:5]
        z, x, y = self.place.z, self.place.x, self.place.y
        arrive(self.third)
        add_blocks(2, lambda j: (own.at[z, 2 * j + x, self.low], from_x.at[j]))
        add_blocks(2, lambda j: (own.at[z, 2 * y + j, self.high], from_y.at[j]))
        go(self.fourth)

    def finish(self):
        own, late_y, late_x = self.buf[0], self.buf[5], self.buf[6]
        z, chip = self.place.z, self.place.chip
        _, row, rows, column, columns = self.chunk
        arrive(self.fourth)
        half = rows // 2
        wide = slice(column, column + columns)
        self.out[row : row + half, wide] = own[z, chip, self.low].astype(f32) + late_y[...].astype(
            f32
        )
        self.out[row + half : row + rows, wide] = own[z, chip, self.high].astype(f32) + late_x[
            ...
        ].astype(f32)


def reduce_along_scratch(chunk):
    _, _, rows, _, columns = chunk
    half = rows // 2
    return [
        pltpu.VMEM((4, 4, rows, columns), bf16),
        pltpu.VMEM((4, 4, rows, columns), bf16),
        pltpu.VMEM((3, 4, rows, columns), bf16),
        pltpu.VMEM((2, half, columns), bf16),
        pltpu.VMEM((2, half, columns), bf16),
        pltpu.VMEM((half, columns), bf16),
        pltpu.VMEM((half, columns), bf16),
    ]


class HandBack:
    def __init__(self, place, source, target, features, send, recv, local):
        self.place, self.source, self.target = place, source, target
        self.mine = columns_of(place.s, features)
        self.send, self.recv, self.local = send, recv, local
        self.blocks = source.shape[1]

    def copy(self, b, i, d):
        rank = self.place.plane[d][1]
        n = b * self.blocks + i
        return pltpu.make_async_remote_copy(
            src_ref=self.source.at[b, i, rank],
            dst_ref=self.target.at[b, i, :, self.mine],
            send_sem=self.send.at[n, d],
            recv_sem=self.recv.at[n, d],
            device_id=self.place.plane[d],
            device_id_type=MESH,
        )

    def own(self, b, i):
        return pltpu.make_async_copy(
            self.source.at[b, i, self.place.s],
            self.target.at[b, i, :, self.mine],
            self.local.at[b * self.blocks + i],
        )

    def each(self, b, i):
        for d in range(7):
            self.copy(b, i, d).start()
        self.own(b, i).start()

    def finish(self):
        def body(n, _):
            b, i = n // self.blocks, n % self.blocks
            for d in range(7):
                self.copy(b, i, d).wait()
            self.own(b, i).wait()
            return 0

        lax.fori_loop(0, self.source.shape[0] * self.blocks, body, 0)


def hand_back_semaphores(steps):
    return [
        pltpu.SemaphoreType.DMA((steps, 7)),
        pltpu.SemaphoreType.DMA((steps, 7)),
        pltpu.SemaphoreType.DMA((steps,)),
    ]


class ReduceLines:
    copies = 4 * 7 + 3 + 3 + 6

    def __init__(self, place, grad, out, bufs, copies):
        self.place, self.grad, self.out, self.bufs = place, grad, out, bufs
        from_core, from_x, from_y, late_y, late_x, from_z = bufs[:6]
        early_z, own_x, own_y, own_late_y, own_late_x = bufs[6:]
        core, x, y = place.core, place.x, place.y
        self.order = [to[0] for to in place.lines] + [place.z]
        rows = grad.shape[3]
        low, high = pl.ds(0, rows // 2), pl.ds(rows // 2, rows // 2)
        cut = from_z.shape[2]
        most, rest = pl.ds(0, cut), pl.ds(cut, grad.shape[4] - cut)
        self.low, self.high, self.all = (low, most), (high, most), (pl.ds(0, rows), most)
        self.low_rest, self.high_rest = (low, rest), (high, rest)
        self.all_rest = (pl.ds(0, rows), rest)
        z = place.z
        self.early = [
            copies.plan(grad.at[(to[0], pl.ds(0, 4), core, *self.all_rest)], early_z.at[k], to)
            for k, to in enumerate(place.lines)
        ]
        self.own_second, self.own_third = [], []
        for j in range(2):
            self.own_second.append(
                copies.plan(
                    grad.at[(z, 2 * j + 1 - x, core, *self.low_rest)], own_x.at[j], place.to_x
                )
            )
            self.own_second.append(
                copies.plan(
                    grad.at[(z, 2 * (1 - y) + j, core, *self.high_rest)], own_y.at[j], place.to_y
                )
            )
        self.own_third = [
            copies.plan(
                grad.at[(z, place.chip_y, core, *self.low_rest)], own_late_y, place.to_y
            ),
            copies.plan(
                grad.at[(z, place.chip_x, core, *self.high_rest)], own_late_x, place.to_x
            ),
        ]
        self.first, self.second, self.third, self.fourth = [], [], [], []
        for k, at in enumerate(self.order):
            self.first.append(
                copies.plan(grad.at[at, :, 1 - core], from_core.at[k], place.to_core)
            )
            step = []
            for j in range(2):
                step.append(
                    copies.plan(
                        grad.at[(at, 2 * j + 1 - x, core, *self.low)], from_x.at[k, j], place.to_x
                    )
                )
                step.append(
                    copies.plan(
                        grad.at[(at, 2 * (1 - y) + j, core, *self.high)], from_y.at[k, j], place.to_y
                    )
                )
            self.second.append(step)
            self.third.append(
                [
                    copies.plan(
                        grad.at[(at, place.chip_y, core, *self.low)], late_y.at[k], place.to_y
                    ),
                    copies.plan(
                        grad.at[(at, place.chip_x, core, *self.high)], late_x.at[k], place.to_x
                    ),
                ]
            )
            if k < 3:
                self.fourth.append(
                    copies.plan(
                        grad.at[(at, place.chip, core, *self.all)], from_z.at[k], place.lines[k]
                    )
                )

    def start(self, k):
        go([self.first[k]])

    def exchange(self, k):
        arrive([self.first[k]])
        at, core = self.order[k], self.place.core
        add_blocks(4, lambda i: (self.grad.at[at, i, core], self.bufs[0].at[k, i]))
        go(self.second[k] + self.early[k : k + 1])

    def spread(self, k):
        arrive(self.second[k])
        at, core, x, y = self.order[k], self.place.core, self.place.x, self.place.y
        add_blocks(
            2, lambda j: (self.grad.at[(at, 2 * j + x, core, *self.low)], self.bufs[1].at[k, j])
        )
        add_blocks(
            2, lambda j: (self.grad.at[(at, 2 * y + j, core, *self.high)], self.bufs[2].at[k, j])
        )
        go(self.third[k])

    def send(self, k):
        arrive(self.third[k])
        at, core, chip = self.order[k], self.place.core, self.place.chip
        add_into(self.grad.at[(at, chip, core, *self.low)], self.bufs[3].at[k])
        add_into(self.grad.at[(at, chip, core, *self.high)], self.bufs[4].at[k])
        go(self.fourth[k : k + 1])

    def own_spread(self):
        arrive(self.early)
        z, core = self.place.z, self.place.core

        def body(i, _):
            target = self.grad.at[(z, i, core, *self.all_rest)]
            total = target[...].astype(f32)
            for k in range(3):
                total = total + self.bufs[6][k, i].astype(f32)
            target[...] = total.astype(bf16)
            return 0

        lax.fori_loop(0, 4, body, 0)
        go(self.own_second)

    def own_send(self):
        arrive(self.own_second)
        z, core, x, y = self.place.z, self.place.core, self.place.x, self.place.y
        for j in range(2):
            add_into(self.grad.at[(z, 2 * j + x, core, *self.low_rest)], self.bufs[7].at[j])
            add_into(self.grad.at[(z, 2 * y + j, core, *self.high_rest)], self.bufs[8].at[j])
        go(self.own_third)

    def finish(self):
        arrive(self.fourth + self.own_third)
        place = self.place
        at = (place.z, place.chip, place.core)
        total = self.grad[(*at, *self.all)].astype(f32)
        for k in range(3):
            total = total + self.bufs[5][k].astype(f32)
        cut = total.shape[1]
        half = total.shape[0] // 2
        self.out[:, :cut] = total
        self.out[:half, cut:] = self.grad[(*at, *self.low_rest)].astype(f32) + self.bufs[9][
            ...
        ].astype(f32)
        self.out[half:, cut:] = self.grad[(*at, *self.high_rest)].astype(f32) + self.bufs[10][
            ...
        ].astype(f32)


def reduce_lines_scratch(rows, columns, rest):
    half = rows // 2
    most = columns - rest
    return [
        pltpu.VMEM((4, 4, rows, columns), bf16),
        pltpu.VMEM((4, 2, half, most), bf16),
        pltpu.VMEM((4, 2, half, most), bf16),
        pltpu.VMEM((4, half, most), bf16),
        pltpu.VMEM((4, half, most), bf16),
        pltpu.VMEM((3, rows, most), bf16),
        pltpu.VMEM((3, 4, rows, rest), bf16),
        pltpu.VMEM((2, half, rest), bf16),
        pltpu.VMEM((2, half, rest), bf16),
        pltpu.VMEM((half, rest), bf16),
        pltpu.VMEM((half, rest), bf16),
    ]


def split_grad(item):
    return item.reshape(4, 4, 2, item.shape[0] // 32, item.shape[1])


def split_weight(item):
    return item.reshape(8, item.shape[0] // 8, item.shape[1])


def chunks_of(index, rows, columns, count):
    if rows >= 64:
        return [(index, rows // count * n, rows // count, 0, columns) for n in range(count)]
    return [(index, 0, rows, columns // count * n, columns // count) for n in range(count)]


def semaphores(remote, local):
    return [pltpu.SemaphoreType.DMA((n,)) for n in (remote, remote, local)]


def remote_call(kernel, name, collective, **options):
    return pl.pallas_call(
        kernel,
        name=name,
        compiler_params=pltpu.CompilerParams(
            collective_id=collective, has_side_effects=True, vmem_limit_bytes=vmem_bytes
        ),
        **options,
    )


def row_of(packed, n, size):
    found = [packed[k, n, r : r + 1, :] for k in range(4) for r in range(size // 512)]
    return jnp.concatenate(found, axis=1)


def columns_of(rank, features):
    return pl.ds(pl.multiple_of(rank * features, 128), features)


def forward_fused_kernel(heads, width, count, vector_count, chunks, slopes, tokens, upstream, *refs):
    vectors, refs = refs[:vector_count], refs[vector_count:]
    weights, contract, refs = refs[:count], refs[count], refs[count + 1 :]
    tokens_out, vectors_out, joined_out, qkv_out, attended, *saved, upstream_out = refs[:8]
    contract_out = refs[8]
    wholes, refs = refs[9 : 8 + count], refs[8 + count :]
    held, small, values_of, joined, normed, outgoing, qkv, result, upstream_own = refs[:9]
    attention = Forward(heads, width, slopes, qkv, result, *refs[9:14])
    kept, refs = refs[14 : 13 + count], refs[13 + count :]
    head_send, head_recv = refs[:2]
    copies = Copies(*refs[5:])
    place = Place()
    z, s, lines, plane = place.z, place.s, place.lines, place.plane
    attention.head = s * heads
    first = [t for t, chunk in enumerate(chunks) if chunk[0] == 0]
    gather = Gather(
        place, weights, [joined, *wholes], [None, *kept], chunks, copies, relayed=first
    )
    later = [t for t, chunk in enumerate(chunks) if chunk[0] > 0]
    features = heads * width
    back = HandBack(place, result, attended, features, *refs[2:5])
    own_seqs, parts, piece, wide = held.shape

    load = copies.inside(tokens.at[z], held.at[:, z])
    load_upstream = copies.inside(upstream.at[z], upstream_own)
    seqs = [copies.plan(tokens.at[to[0]], held.at[:, z], to) for to in lines]
    vector_copies = [copies.plan(small.at[z], small.at[z], to) for to in lines]
    upstreams = [copies.plan(upstream.at[to[0]], upstream_out.at[:, z], to) for to in lines]
    keep_upstream = copies.inside(upstream_own, upstream_out.at[:, z])
    keeping = [
        copies.inside(held, tokens_out),
        copies.inside(small, vectors_out),
        copies.inside(joined, joined_out),
    ]
    keep_qkv = copies.inside(qkv, qkv_out)
    keep_saved = [copies.inside(attention.out_t, saved[0]), copies.inside(attention.lse, saved[1])]
    contracts = [copies.plan(contract.at[s], contract_out.at[z], to) for to in lines]

    def to_head(d):
        return pltpu.make_async_remote_copy(
            src_ref=outgoing.at[d],
            dst_ref=qkv.at[:, :, s],
            send_sem=head_send.at[d],
            recv_sem=head_recv.at[d],
            device_id=(z, lax.rem(s + 1 + d, 8)),
            device_id_type=MESH,
        )

    go(gather.loads + [load, load_upstream])
    small[z] = jnp.zeros(small.shape[1:], bf16)
    for n, item in enumerate(vectors):
        small[z, n, : item.shape[0], :] = item[...]
    greet(lines + plane)
    for t in first:
        gather.start(t)
    for t in first:
        gather.pass_on(t)
    go(seqs + vector_copies)
    gather.keep()
    load.wait()
    for t in range(len(first) + 2):
        if t < len(first):
            gather.exchange(t)
        if 0 <= t - 1 < len(first):
            gather.spread(t - 1)
        if 0 <= t - 2:
            gather.share(t - 2)
    load_upstream.wait()
    keep_upstream.start()
    arrive(seqs + vector_copies)
    for t in later:
        gather.start(t)
    values_of[...] = small[...].astype(f32)

    gain, shift = row_of(values_of, 0, wide), row_of(values_of, 1, wide)

    def norm(i, _):
        values = held[i // parts, i % parts].astype(f32)
        rows = pl.ds(pl.multiple_of(i * piece, piece), piece)
        normed[rows, :] = normalize(values, gain, shift).astype(bf16)
        return 0

    lax.fori_loop(0, own_seqs * parts, norm, 0)
    for t in first:
        gather.complete(t)
    go(keeping)

    def project(d, _):
        rank = lax.rem(s + 1 + d, 8)
        per = 8 // 4
        query_bias = values_of[rank // per, 2, pl.ds(rank % per, 1), :]
        value_bias = values_of[rank // per, 3, pl.ds(rank % per, 1), :]
        low = lax.broadcasted_iota(jnp.int32, query_bias.shape, 1) < width
        bias = jnp.concatenate(
            [
                jnp.where(low, query_bias, 0.0),
                jnp.where(low, value_bias, query_bias),
                jnp.where(low, 0.0, value_bias),
            ],
            axis=1,
        )
        weight = joined[:, :, :, columns_of(rank, 3 * features)].reshape(wide, 3 * features)
        made = (matmul(normed[...], weight) + bias).astype(bf16)
        outgoing[d] = made.reshape(outgoing.shape[1:])
        pl.when(d < 7)(lambda: to_head(d).start())
        return 0

    lax.fori_loop(0, 8, project, 0)
    own_copy = copies.inside(outgoing.at[7], qkv.at[:, :, s])
    own_copy.start()
    base = later[0]
    gather.exchange(base)
    gather.exchange(base + 1)
    own_copy.wait()
    gather.spread(base)
    go(contracts)
    for d in range(7):
        to_head(d).wait_recv()
    keep_qkv.start()
    attention.run(
        {
            0: [(gather.exchange, base + 2), (go, upstreams), (gather.spread, base + 1)],
            2: [(gather.spread, base + 2), (gather.share, base)],
            5: [(gather.share, base + 1)],
            6: [(gather.share, base + 2)],
        },
        back.each,
    )
    go(keep_saved)
    for t in later:
        gather.complete(t)
    arrive(contracts + upstreams)
    back.finish()
    for d in range(7):
        to_head(d).wait_send()
    copies.finish()
    done(gather.own + [keep_upstream, keep_qkv] + keep_saved + keeping)


def forward_fused(tokens, upstream, vectors, weights, contract, slopes, heads, width):
    seqs, piece, features = tokens.shape
    parts = 4
    own = seqs // parts
    columns = heads * width
    length = parts * 8 * piece
    vectors = [item.reshape(-1, 128) for item in vectors]
    cut = [split_weight(item) for item in weights]
    contract = split_weight(contract)
    count, tall = len(cut), 8 * -(-max(item.shape[0] for item in vectors) // 8)
    chunks = []
    for t, pieces in enumerate((3, 1, 2)):
        chunks += chunks_of(t, *cut[t].shape[1:], pieces)
    seq_shape = (own, parts, piece, features)
    qkv_shape = (own, parts, 8, piece, 3 * columns)
    small = (parts, len(vectors), tall, 128)
    out = remote_call(
        functools.partial(forward_fused_kernel, heads, width, count, len(vectors), chunks),
        "forward_fused",
        1,
        out_shape=(
            jax.ShapeDtypeStruct(seq_shape, bf16),
            jax.ShapeDtypeStruct(small, bf16),
            jax.ShapeDtypeStruct((parts, *cut[0].shape), bf16),
            jax.ShapeDtypeStruct(qkv_shape, bf16),
            jax.ShapeDtypeStruct(seq_shape, bf16),
            *saved_shapes(own, length, heads, width),
            jax.ShapeDtypeStruct(seq_shape, bf16),
            jax.ShapeDtypeStruct((parts, *contract.shape[1:]), bf16),
            *[jax.ShapeDtypeStruct((parts, *item.shape), bf16) for item in cut[1:]],
        ),
        in_specs=[SMEM, HBM, HBM] + [VMEM] * len(vectors) + [HBM] * (count + 1),
        out_specs=(HBM,) * (8 + count),
        scratch_shapes=[
            pltpu.VMEM(seq_shape, bf16),
            pltpu.VMEM(small, bf16),
            pltpu.VMEM(small, f32),
            pltpu.VMEM((parts, *cut[0].shape), bf16),
            pltpu.VMEM((own * parts * piece, features), bf16),
            pltpu.VMEM((8, own, parts, piece, 3 * columns), bf16),
            pltpu.VMEM(qkv_shape, bf16),
            pltpu.VMEM((own, parts, 8, piece, columns), bf16),
            pltpu.VMEM((own, piece, features), bf16),
            *[pltpu.VMEM(item.shape, f32) for item in saved_shapes(own, length, heads, width)],
            *forward_scratch(length, heads, width),
            *[pltpu.VMEM(item.shape, bf16) for item in cut[1:]],
            pltpu.SemaphoreType.DMA((7,)),
            pltpu.SemaphoreType.DMA((7,)),
            *hand_back_semaphores(own * parts),
            *semaphores(12 + 3 + len(chunks) * Gather.copies_each, 2 * count - 1 + 10),
        ],
    )(
        slopes,
        tokens.reshape(parts, own, piece, features),
        upstream.reshape(parts, own, piece, features),
        *vectors,
        *cut,
        contract,
    )
    wholes = [
        whole.reshape(4 * item.shape[0], item.shape[1])
        for whole, item in zip((out[2], *out[9:]), weights)
    ]
    return out[0], out[1], [*wholes, out[8]], out[3], out[4], (out[5], out[6]), out[7]


def feed_forward_kernel(
    chunks, expand, contract, contract_line, out_weight,
    small, upstream_in, tokens_in, attended_in,
    layer_out, residual_out, diff_out, expand_grad, out_grad, contract_grad,
    bias_grad, gain_grad, shift_grad, out_bias_grad, contract_bias_grad,
    upstream, tokens, attended, layer, residual_grad, attended_diff, values_of, expand_bias, expand_in, contract_in, residual, second, second_t, expanded, activated, grad, staged, *refs,
):
    second_back = residual_grad
    bufs, refs = refs[:11], refs[11:]
    loaded, stored, refs = refs[0], refs[1], refs[2:]
    copies = Copies(*refs)
    place = Place()
    z = place.z
    given = [
        copies.inside(a, b)
        for a, b in ((attended_in, attended), (tokens_in, tokens), (upstream_in, upstream))
    ]
    keep_layer = copies.inside(layer, layer_out)
    keep_residual = copies.inside(residual_grad, residual_out)
    keep_diff = copies.inside(attended_diff, diff_out)
    reduce = ReduceLines(place, grad, contract_grad, bufs, copies)
    gather = Gather(
        place, [contract], [contract_in], [None], chunks, copies, given=contract_line
    )
    rows, features = second.shape
    steps = 8
    wide = expand.shape[1] // steps

    def at(n):
        part = paired(z, 3 - n // 2)
        return part, n % 2, pl.ds(pl.multiple_of((2 * part + n % 2) * wide, wide), wide)

    def load(n):
        _, _, where = at(n)
        return pltpu.make_async_copy(expand.at[:, where], expand_in.at[:, where], loaded.at[n])

    def contract_at(n):
        part, side, _ = at(n)
        return contract_in[part, pl.ds(4 * side, 4)].reshape(wide, features)

    def store(n):
        _, _, where = at(n)
        slot = n % 2
        return pltpu.make_async_copy(
            staged.at[slot], expand_grad.at[:, where], stored.at[slot]
        )

    halves = [pl.ds(0, wide), pl.ds(wide, wide)]
    out_loads = [
        pltpu.make_async_copy(out_weight.at[:, half], staged.at[n], stored.at[n])
        for n, half in enumerate(halves)
    ]
    out_stores = [
        pltpu.make_async_copy(staged.at[n], out_grad.at[:, half], stored.at[n])
        for n, half in enumerate(halves)
    ]
    part_rows = rows // 8

    def rows_at(i):
        return pl.ds(pl.multiple_of(i * part_rows, part_rows), part_rows)

    for n in range(len(chunks)):
        gather.start(n)
    go(given[:2] + out_loads + given[2:])
    for n in range(steps):
        load(n).start()
    go(gather.loads)
    greet(place.near)
    for n in range(len(chunks)):
        gather.exchange(n)
    values_of[...] = small[...].astype(f32)
    out_bias, gain, shift, contract_bias = [
        row_of(values_of, n, features) for n in (4, 5, 6, 7)
    ]
    expand_bias[...] = row_of(values_of, 8, steps * wide)
    done(given)
    for n, half in enumerate(halves):
        out_loads[n].wait()
        bias = out_bias[:, n * wide : (n + 1) * wide]
        residual[:, half] = (
            tokens[:, half].astype(f32) + (matmul(attended[...], staged[n]) + bias)
        )

    def norm(i, _):
        values = residual[rows_at(i), :]
        second[rows_at(i), :] = normalize(values, gain, shift).astype(bf16)
        second_back[rows_at(i), :] = values + contract_bias
        return 0

    lax.fori_loop(0, 8, norm, 0)
    for n in range(len(chunks) - 1):
        gather.spread(n)
    second_t[...] = second[...].T

    def forward(n, after):
        part, side, where = at(n)
        load(n).wait()
        values = matmul(second[...], expand_in[:, where]) + expand_bias[:, where]
        expanded[:, where] = values
        low = gelu_tanh(values).astype(bf16)
        activated[:, where] = low
        made = matmul(low.T, upstream[...]).astype(bf16)
        grad[part, pl.ds(2 * side, 2)] = made.reshape(2, 2, wide // 4, features)
        follow(n, after)
        return 0

    def shrink(n, after):
        _, _, where = at(n)
        second_back[...] += matmul(activated[:, where], contract_at(n))
        follow(n, after)
        return 0

    def backward(n, after):
        _, _, where = at(n)
        values = expanded[:, where]
        act_grad = matmul_rt(upstream[...], contract_at(n))
        bent = jnp.tanh(gelu_coef * (values + 0.044715 * values * values * values))
        slope = 0.5 * (1.0 + bent) + 0.5 * values * (1.0 - bent * bent) * (
            gelu_coef * (1.0 + 3.0 * 0.044715 * values * values)
        )
        diff = (act_grad * slope).astype(bf16)
        bias_grad[:, where] = jnp.sum(diff.astype(f32), axis=0, keepdims=True)
        pl.when(n >= 2)(lambda: store(n - 2).wait())
        staged[n % 2] = matmul(second_t[...], diff).astype(bf16)
        store(n).start()
        second_back[...] += matmul_rt(diff, expand_in[:, where])
        follow(n, after)
        return 0

    last = len(chunks) - 1
    forward_steps = {
        0: [(gather.spread, last)],
        1: [(reduce.start, 0)],
        3: [(reduce.exchange, 0), (reduce.start, 1)],
        5: [(reduce.start, 2), (reduce.exchange, 1)],
        7: [(reduce.start, 3), (reduce.exchange, 2)] + [(gather.share, n) for n in range(last)],
    }
    shrink_steps = {
        1: [(reduce.exchange, 3)],
        3: [(reduce.spread, 0)],
        7: [(reduce.spread, 1)],
    }
    backward_steps = {
        1: [(reduce.spread, 2)],
        2: [(reduce.spread, 3)],
        3: [(reduce.send, 0), (reduce.own_spread,)],
        4: [(reduce.send, 1)],
        5: [(reduce.send, 2)],
        6: [(reduce.send, 3), (reduce.own_send,)],
    }
    lax.fori_loop(0, steps, lambda n, _: forward(n, forward_steps), 0)
    gather.share(last)
    for n in range(len(chunks)):
        gather.complete(n)
    done(gather.loads)
    lax.fori_loop(0, steps, lambda n, _: shrink(n, shrink_steps), 0)
    layer[...] = second_back[...].astype(bf16).reshape(layer.shape)
    keep_layer.start()
    second_back[...] = jnp.zeros_like(second_back)
    lax.fori_loop(0, steps, lambda n, _: backward(n, backward_steps), 0)
    store(steps - 2).wait()
    store(steps - 1).wait()
    go(out_loads)
    second_t[...] = attended[...].T

    def norm_back(i, sums):
        back = second_back[rows_at(i), :]
        part, normal = normalize_back(residual[rows_at(i), :], back, gain)
        given = upstream[rows_at(i), :].astype(f32)
        total = given + part
        low = total.astype(bf16)
        residual_grad[rows_at(i), :] = total
        second[rows_at(i), :] = low
        found = (back * normal, back, low.astype(f32), given)
        return tuple(
            kept + jnp.sum(item, axis=0, keepdims=True) for kept, item in zip(sums, found)
        )

    nothing = jnp.zeros((1, features), f32)
    sums = lax.fori_loop(0, 8, norm_back, (nothing,) * 4)
    gain_grad[...], shift_grad[...], out_bias_grad[...], contract_bias_grad[...] = sums
    keep_residual.start()
    done(out_loads)
    branch_diff = second
    made = matmul_rt(branch_diff[:, halves[0]], staged[0])
    made = (made + matmul_rt(branch_diff[:, halves[1]], staged[1])).astype(bf16)
    attended_diff[...] = made.reshape(attended_diff.shape)
    keep_diff.start()
    for n, half in enumerate(halves):
        staged[n] = matmul(second_t[...], branch_diff[:, half]).astype(bf16)
        out_stores[n].start()
    reduce.finish()
    done(out_stores + [keep_layer, keep_residual, keep_diff])
    copies.finish()


def feed_forward(shape, expand, contract, line, out_weight, tokens, upstream, attended, small):
    own, parts, piece = shape
    rows, features = tokens.shape
    hidden = expand.shape[1]
    wide = hidden // 8
    each = hidden // 32
    contract = split_weight(contract)
    chunks = chunks_of(0, *contract.shape[1:], 2)
    seq_shape = (own, parts, piece, features)
    return remote_call(
        functools.partial(feed_forward_kernel, chunks),
        "feed_forward",
        4,
        out_shape=(
            jax.ShapeDtypeStruct(seq_shape, bf16),
            jax.ShapeDtypeStruct((rows, features), f32),
            jax.ShapeDtypeStruct(seq_shape, bf16),
            jax.ShapeDtypeStruct((features, hidden), bf16),
            jax.ShapeDtypeStruct((features, features), bf16),
            jax.ShapeDtypeStruct((each, features), f32),
            jax.ShapeDtypeStruct((1, hidden), f32),
            *[jax.ShapeDtypeStruct((1, features), f32)] * 4,
        ),
        in_specs=[HBM] * 4 + [VMEM] + [HBM] * 3,
        out_specs=(HBM,) * 5 + (VMEM,) * 6,
        scratch_shapes=[
            *[pltpu.VMEM((rows, features), bf16)] * 3,
            pltpu.VMEM(seq_shape, bf16),
            pltpu.VMEM((rows, features), f32),
            pltpu.VMEM(seq_shape, bf16),
            pltpu.VMEM(small.shape, f32),
            pltpu.VMEM((1, hidden), f32),
            pltpu.VMEM((features, hidden), bf16),
            pltpu.VMEM((4, *contract.shape), bf16),
            pltpu.VMEM((rows, features), f32),
            pltpu.VMEM((rows, features), bf16),
            pltpu.VMEM((features, rows), bf16),
            pltpu.VMEM((rows, hidden), f32),
            pltpu.VMEM((rows, hidden), bf16),
            pltpu.VMEM((4, 4, 2, each, features), bf16),
            pltpu.VMEM((2, features, wide), bf16),
            *reduce_lines_scratch(each, features, features // 4),
            pltpu.SemaphoreType.DMA((8,)),
            pltpu.SemaphoreType.DMA((2,)),
            *semaphores(
                ReduceLines.copies + len(chunks) * (Gather.copies_each - 3),
                7 + 3 * len(chunks),
            ),
        ],
    )(expand, contract, line, out_weight, small, upstream, tokens, attended)


def backward_fused_kernel(heads, width, count, chunks, *refs):
    slopes, diff_in, qkv_in, out_t_in, lse_in, layer = refs[:6]
    grads, refs = refs[6 : 6 + count], refs[6 + count :]
    joined_out, layer_out, layer_own = refs[0], refs[1], refs[2 + count]
    outs, refs = refs[2 : 2 + count], refs[3 + count :]
    diff, qkv, out_t, lse, joined = refs[:5]
    attention = Backward(heads, width, slopes, qkv, diff, out_t, lse, joined, *refs[5:12])
    bufs, refs = refs[12 : 12 + 7 * len(chunks)], refs[12 + 7 * len(chunks) :]
    copies = Copies(*refs[3:])
    place = Place()
    s, plane = place.s, place.plane
    attention.head = s * heads
    features = heads * width
    along = ReduceAlong(place, grads[0], outs[0], bufs[:7], chunks[0], copies)
    reduce = Reduce(place, grads, outs, bufs[7:], chunks[1:], copies)
    back = HandBack(place, joined, joined_out, 3 * features, *refs[:3])

    own = [copies.inside(diff_in.at[:, :, :, columns_of(s, features)], diff.at[:, :, s])]
    own += [copies.inside(a, b) for a, b in ((qkv_in, qkv), (out_t_in, out_t), (lse_in, lse))]
    arriving = [
        copies.plan(diff_in.at[:, :, :, columns_of(to[1], features)], diff.at[:, :, s], to)
        for to in plane
    ]
    returned = [copies.plan(layer.at[:, to[0]], layer_out.at[place.z], to) for to in place.lines]
    load_layer = copies.inside(layer.at[:, place.z], layer_own)
    keep_layer = copies.inside(layer_own, layer_out.at[place.z])
    go(own + reduce.loads + [along.load, load_layer])
    greet(place.lines + plane)
    go(arriving + [along.first])
    reduce.start()
    along.exchange()
    go(returned)
    for t in range(3):
        reduce.exchange(t)
    done(own + [load_layer])
    keep_layer.start()
    arrive(arriving)
    attention.run(
        {
            1: [(reduce.spread, 0)],
            2: [(along.spread,)],
            3: [(reduce.spread, 1), (reduce.spread, 2)],
            4: [(reduce.send, 0), (along.send,)],
            5: [(reduce.send, 1)],
            6: [(reduce.send, 2)],
        },
        back.each,
    )
    for t in range(3):
        reduce.finish(t)
    along.finish()
    back.finish()
    arrive(returned)
    copies.finish()
    keep_layer.wait()


def backward_fused(attended_diff, qkv, saved, layer, grads, slopes, heads, width):
    own, parts, piece, columns = attended_diff.shape
    features = heads * width
    length = parts * 8 * piece
    cut = [split_grad(item) for item in grads]
    count = len(cut)
    rows, wide = cut[0].shape[3:]
    early, part = 3 * wide // 8, 5 * wide // 16
    chunks = [
        (0, 0, rows, 0, early),
        (0, 0, rows, early, part),
        (0, 0, rows, early + part, part),
        *chunks_of(1, *cut[1].shape[3:], 1),
    ]
    out = remote_call(
        functools.partial(backward_fused_kernel, heads, width, count, chunks),
        "backward_fused",
        2,
        out_shape=(
            jax.ShapeDtypeStruct((own, parts, piece, 24 * features), bf16),
            jax.ShapeDtypeStruct((parts, own, piece, columns), bf16),
            *[jax.ShapeDtypeStruct(item.shape[3:], f32) for item in cut],
        ),
        in_specs=[SMEM] + [HBM] * (5 + count),
        out_specs=(HBM, HBM) + (VMEM,) * count,
        scratch_shapes=[
            pltpu.VMEM((own, piece, columns), bf16),
            pltpu.VMEM((own, parts, 8, piece, features), bf16),
            pltpu.VMEM(qkv.shape, bf16),
            *[pltpu.VMEM(item.shape, f32) for item in saved],
            pltpu.VMEM(qkv.shape, bf16),
            *backward_scratch(length, heads, width),
            *reduce_along_scratch(chunks[0]),
            *reduce_scratch(chunks[1:]),
            *hand_back_semaphores(own * parts),
            *semaphores(10 + len(chunks) * Reduce.copies_each, len(chunks) + 6),
        ],
    )(slopes, attended_diff, qkv, *saved, layer, *cut)
    return out[0], out[1].reshape(parts * own, piece, columns), out[2:]


def end_kernel(
    width, joined_diff, joined_weight, tokens_in, residual_in, small, out_bias_grad,
    second_gain_grad, second_shift_grad, contract_bias_grad, expand_bias_grad,
    input_out, vector_out, out,
    tokens, residual_grad, values_of, diff_in, weight_in, normed, normed_t, back, grads, held,
    vectors, others, ranks, *refs,
):
    count = grads.shape[0]
    bufs, refs = refs[: 7 * count], refs[7 * count :]
    loaded, copies = refs[0], Copies(*refs[1:])
    place = Place()
    z, lines, plane = place.z, place.lines, place.plane
    rows, features = tokens.shape
    own_seqs, parts, piece, _ = held.shape
    columns = [pl.ds(features * n, features) for n in range(count)]
    chunks = [(n, 0, grads.shape[4], 0, features) for n in range(count)]
    outs = [out.at[:, where] for where in columns]
    reduce = Reduce(place, [grads.at[n] for n in range(count)], outs, bufs, chunks, copies)
    loads = [
        (
            pltpu.make_async_copy(joined_diff.at[:, c], diff_in.at[:, c], loaded.at[0, n]),
            pltpu.make_async_copy(joined_weight.at[:, c], weight_in.at[:, c], loaded.at[1, n]),
        )
        for n, c in enumerate(columns)
    ]
    returned = [copies.plan(held.at[:, to[0]], input_out.at[z], to) for to in lines]
    stay = copies.inside(held.at[:, z], input_out.at[z])
    along = [copies.plan(vectors.at[to[0]], others.at[k], to) for k, to in enumerate(lines)]
    across = [copies.plan(ranks.at[0], ranks.at[d + 1], to) for d, to in enumerate(plane)]

    given_loads = [copies.inside(tokens_in, tokens), copies.inside(residual_in, residual_grad)]
    for load in loads:
        go(load)
    go(given_loads)
    values_of[...] = small[...].astype(f32)
    gain, shift = row_of(values_of, 0, features), row_of(values_of, 1, features)
    greet(lines + plane)
    for n, where in enumerate(columns):
        done(loads[n])
        part = matmul_rt(diff_in[:, where], weight_in[:, where])
        back[...] = part if n == 0 else back[...] + part

    def norm_back(i, sums):
        at = pl.ds(pl.multiple_of(i * piece, piece), piece)
        values, given = tokens[at, :].astype(f32), back[at, :]
        part, normal = normalize_back(values, given, gain)
        normed[at, :] = (normal * gain + shift).astype(bf16)
        total = (residual_grad[at, :] + part).astype(bf16)
        held[i // parts, i % parts] = total
        found = (given * normal, given)
        return tuple(
            kept + jnp.sum(item, axis=0, keepdims=True) for kept, item in zip(sums, found)
        )

    done(given_loads)
    nothing = jnp.zeros((1, features), f32)
    gain_grad, shift_grad = lax.fori_loop(0, own_seqs * parts, norm_back, (nothing, nothing))
    go(returned + [stay])
    normed_t[...] = normed[...].T
    sums = []
    for n, where in enumerate(columns):
        made = matmul(normed_t[...], diff_in[:, where]).astype(bf16)
        grads[n] = made.reshape(grads.shape[1:])
        reduce.begin(n)
        sums.append(jnp.sum(diff_in[:, where].astype(f32), axis=0, keepdims=True))
        if n > 0:
            reduce.exchange(n - 1)

    sums = jnp.concatenate(sums, axis=1)
    low = lax.broadcasted_iota(jnp.int32, (1, 128), 1) < width
    query_grad, value_grad = [], []
    for r in range(features // 128):
        first, middle, last = [sums[:, (3 * r + n) * 128 : (3 * r + n + 1) * 128] for n in range(3)]
        query_grad.append(jnp.where(low, first, middle))
        value_grad.append(jnp.where(low, middle, last))
    given = [
        gain_grad, shift_grad, jnp.concatenate(query_grad, axis=1),
        jnp.concatenate(value_grad, axis=1), out_bias_grad[...], second_gain_grad[...],
        second_shift_grad[...], contract_bias_grad[...], expand_bias_grad[...],
    ]
    row = 0
    for item in given:
        each = item.shape[1] // 512
        for k in range(4):
            for r in range(each):
                start = (k * each + r) * 128
                vectors[k, row + r : row + r + 1, :] = item[:, start : start + 128]
        row += each
    go(along)
    reduce.spread(0)
    reduce.exchange(count - 1)
    arrive(along)
    total = vectors[z]
    for k in range(3):
        total = total + others[k]
    ranks[0] = total
    go(across)
    for n in range(1, count):
        reduce.send(n - 1)
        reduce.spread(n)
    reduce.send(count - 1)
    arrive(across)
    total = ranks[0]
    for d in range(1, 8):
        total = total + ranks[d]
    vector_out[...] = total
    for n in range(count):
        reduce.finish(n)
    arrive(returned)
    copies.finish()
    stay.wait()


def end(shape, joined_diff, joined_weight, tokens, residual_grad, small, vectors, width):
    own, parts, piece = shape
    rows, features = tokens.shape
    count = joined_diff.shape[1] // features
    each = features // 32
    tall = (4 * features + sum(item.shape[1] for item in vectors)) // 512
    chunks = [(n, 0, each, 0, features) for n in range(count)]
    out = remote_call(
        functools.partial(end_kernel, width),
        "end",
        3,
        out_shape=(
            jax.ShapeDtypeStruct((parts, own, piece, features), bf16),
            jax.ShapeDtypeStruct((tall, 128), f32),
            jax.ShapeDtypeStruct((each, count * features), f32),
        ),
        in_specs=[HBM] * 4 + [VMEM] * (1 + len(vectors)),
        out_specs=(HBM, VMEM, VMEM),
        scratch_shapes=[
            pltpu.VMEM((rows, features), bf16),
            pltpu.VMEM((rows, features), f32),
            pltpu.VMEM(small.shape, f32),
            pltpu.VMEM((rows, count * features), bf16),
            pltpu.VMEM((features, count * features), bf16),
            pltpu.VMEM((rows, features), bf16),
            pltpu.VMEM((features, rows), bf16),
            pltpu.VMEM((rows, features), f32),
            pltpu.VMEM((count, 4, 4, 2, each, features), bf16),
            pltpu.VMEM((own, parts, piece, features), bf16),
            pltpu.VMEM((4, tall, 128), f32),
            pltpu.VMEM((3, tall, 128), f32),
            pltpu.VMEM((8, tall, 128), f32),
            *reduce_scratch(chunks),
            pltpu.SemaphoreType.DMA((2, count)),
            *semaphores(3 + 3 + 7 + count * Reduce.copies_each, 3 + count),
        ],
    )(joined_diff, joined_weight, tokens, residual_grad, small, *vectors)
    return out[0].reshape(parts * own, piece, features), out[1], out[2]


def hand_out_kernel(sizes, vector, *refs):
    count = (len(refs) - len(sizes) - 1) // 3
    arrays, outs, smalls = refs[:count], refs[count : 2 * count], refs[2 * count :]
    smalls, kept, sems = smalls[: len(sizes)], smalls[len(sizes) : -1], refs[-1]
    s = lax.axis_index("sp")
    loads = [pltpu.make_async_copy(a, k, sems.at[n]) for n, (a, k) in enumerate(zip(arrays, kept))]
    stores = [
        pltpu.make_async_copy(k, o, sems.at[count + n]) for n, (k, o) in enumerate(zip(kept, outs))
    ]
    go(loads)
    row = 0
    for out, size in zip(smalls, sizes):
        per = 128 // size
        found = vector[pl.ds(row + s // per, 1), :]
        if per > 1:
            found = pltpu.roll(found, lax.rem(128 - s % per * size, 128), 1)
        out[...] = found[:, :size]
        row += 8 // per
    for load, store in zip(loads, stores):
        load.wait()
        store.start()
    done(stores)


def hand_out(vector, sizes, arrays):
    out = pl.pallas_call(
        functools.partial(hand_out_kernel, sizes),
        name="hand_out",
        out_shape=(
            *[jax.ShapeDtypeStruct(item.shape, item.dtype) for item in arrays],
            *[jax.ShapeDtypeStruct((1, size), f32) for size in sizes],
        ),
        in_specs=[VMEM] + [HBM] * len(arrays),
        out_specs=(HBM,) * len(arrays) + (VMEM,) * len(sizes),
        scratch_shapes=[
            *[pltpu.VMEM(item.shape, item.dtype) for item in arrays],
            pltpu.SemaphoreType.DMA((2 * len(arrays),)),
        ],
        compiler_params=pltpu.CompilerParams(vmem_limit_bytes=vmem_bytes),
    )(vector, *arrays)
    return out[: len(arrays)], [item.reshape(-1) for item in out[len(arrays) :]]


def per_device(
    layer_input,
    first_gain,
    first_shift,
    joined_weight,
    query_bias,
    value_bias,
    output_weight,
    output_bias,
    second_gain,
    second_shift,
    expand_weight,
    expand_bias,
    contract_weight,
    contract_bias,
    alibi_slopes,
    upstream,
):
    seqs, piece, features = layer_input.shape
    fs_count = lax.axis_size("fs")
    sp_count = lax.axis_size("sp")
    head_count = alibi_slopes.shape[0]
    width = features // head_count
    heads = head_count // sp_count
    rows = seqs * piece
    own = seqs // fs_count
    shape = (own, fs_count, piece)

    vectors = (
        first_gain, first_shift, query_bias, value_bias, output_bias,
        second_gain, second_shift, contract_bias, expand_bias,
    )
    fast = (fs_count, sp_count) == (4, 8) and (own, heads, width) == (2, 2, 64)
    fast = fast and expand_weight.shape[1] == 4 * features
    if fast:
        weights = (joined_weight, output_weight, expand_weight)
        tokens, small, weights, qkv, attended, saved, upstream_low = forward_fused(
            layer_input, upstream, vectors, weights, contract_weight, alibi_slopes, heads, width
        )
        joined_full, out_full, expand_full, contract_line = weights
        tokens = tokens.reshape(rows, features)
        (
            layer_output, residual_grad, attended_diff, expand_grad, output_weight_grad,
            contract_grad, eb, g2, s2, ob, cb,
        ) = feed_forward(
            shape, expand_full, contract_weight, contract_line, out_full, tokens,
            upstream_low.reshape(rows, features), attended.reshape(rows, features), small,
        )
        joined_diff, layer_output, grads = backward_fused(
            attended_diff, qkv, saved, layer_output, (expand_grad, output_weight_grad),
            alibi_slopes, heads, width,
        )
        input_grad, vector, joined_grad = end(
            shape, joined_diff.reshape(rows, 3 * features), joined_full, tokens, residual_grad,
            small, (ob, g2, s2, cb, eb), width,
        )
        devices = fs_count * sp_count
        sizes = [4 * item.shape[0] // devices for item in vectors]
        arrays, (g1, s1, qb, vb, ob, g2, s2, cb, eb) = hand_out(
            vector, sizes, (layer_output, input_grad, joined_grad, grads[1], grads[0], contract_grad)
        )
        layer_output, input_grad, joined_grad, output_grad, expand_grad, contract_grad = arrays
        return (
            layer_output, input_grad, g1, s1, joined_grad, qb, vb, output_grad, ob, g2, s2,
            expand_grad, eb, contract_grad, cb,
        )

    slopes = lax.dynamic_slice_in_dim(alibi_slopes, lax.axis_index("sp") * heads, heads)
    gather = lambda item: lax.all_gather(item, "fs", axis=0, tiled=True)
    scatter = functools.partial(
        lax.psum_scatter, axis_name=("fs", "sp"), scatter_dimension=0, tiled=True
    )
    gain_one, shift_one, qbias, vbias, obias, gain_two, shift_two, cbias, ebias = [
        gather(item).astype(f32) for item in vectors
    ]
    joined_full, out_full, expand_full, contract_full = [
        gather(item) for item in (joined_weight, output_weight, expand_weight, contract_weight)
    ]
    tokens = to_own_seqs(layer_input).reshape(rows, features).astype(f32)
    upstream_low = to_own_seqs(upstream).reshape(rows, features)

    normed_f, norm_back_one = jax.vjp(normalize, tokens, gain_one, shift_one)
    normed = normed_f.astype(bf16)
    joined_bias = joined_bias_of(qbias, vbias, head_count)
    joined_all = (matmul(normed, joined_full) + joined_bias).astype(bf16)
    qkv = to_heads(joined_all.reshape(*shape, 3 * features))
    attended, *saved = attention_forward(qkv, slopes, heads, width)
    attended = from_heads(attended).reshape(rows, features)
    upstream_f = upstream_low.astype(f32)
    contract_bias_grad = jnp.sum(upstream_f, axis=0)
    residual = tokens + (matmul(attended, out_full) + obias)
    second_f, norm_back_two = jax.vjp(normalize, residual, gain_two, shift_two)
    second = second_f.astype(bf16)
    expanded = matmul(second, expand_full) + ebias
    activated_f, gelu_back = jax.vjp(gelu_tanh, expanded)
    activated = activated_f.astype(bf16)
    result = residual + (matmul(activated, contract_full) + cbias)
    layer_output = result.astype(bf16).reshape(*shape, features)

    contract_grad = matmul_lt(activated, upstream_low)
    act_grad = matmul_rt(upstream_low, contract_full)
    expand_diff = gelu_back(act_grad)[0].astype(bf16)
    expand_grad = matmul_lt(second, expand_diff)
    expand_bias_grad = jnp.sum(expand_diff.astype(f32), axis=0)
    second_back = matmul_rt(expand_diff, expand_full)
    resid_part, second_gain_grad, second_shift_grad = norm_back_two(second_back)
    residual_grad = upstream_f + resid_part

    branch_diff = residual_grad.astype(bf16)
    output_weight_grad = matmul_lt(attended, branch_diff)
    output_bias_grad = jnp.sum(branch_diff.astype(f32), axis=0)
    attended_diff = matmul_rt(branch_diff, out_full).astype(bf16)
    attended_diff = attended_diff.reshape(*shape, features)
    joined_diff = attention_backward(qkv, to_heads(attended_diff), *saved, slopes, heads, width)
    joined_diff = from_heads(joined_diff).reshape(rows, 3 * features)
    joined_grad = matmul_lt(normed, joined_diff)
    column_sums = jnp.sum(joined_diff.astype(f32), axis=0).reshape(head_count, 3, width)
    query_bias_grad = column_sums[:, 0].reshape(features)
    value_bias_grad = column_sums[:, 2].reshape(features)
    normed_back = matmul_rt(joined_diff, joined_full)
    input_part, first_gain_grad, first_shift_grad = norm_back_one(normed_back)
    input_grad = (residual_grad + input_part).astype(bf16).reshape(*shape, features)

    vector_grads = (
        first_gain_grad, first_shift_grad, query_bias_grad, value_bias_grad,
        output_bias_grad, second_gain_grad, second_shift_grad, contract_bias_grad,
        expand_bias_grad,
    )
    devices = fs_count * sp_count
    packed = jnp.concatenate([item.reshape(devices, -1) for item in vector_grads], axis=1)
    packed = scatter(packed.reshape(-1))
    own_grads, at = [], 0
    for item in vector_grads:
        size = item.shape[0] // devices
        own_grads.append(packed[at : at + size])
        at += size
    g1, s1, qb, vb, ob, g2, s2, cb, eb = own_grads
    return (
        from_own_seqs(layer_output), from_own_seqs(input_grad), g1, s1, scatter(joined_grad), qb,
        vb, scatter(output_weight_grad), ob, g2, s2, scatter(expand_grad), eb,
        scatter(contract_grad), cb,
    )


def solution(mesh):
    tokens = P(None, ("fs", "sp"), None)
    both, both_rows = P(("fs", "sp")), P(("fs", "sp"), None)
    one, one_rows = P("fs"), P("fs", None)
    return jax.shard_map(
        per_device,
        mesh=mesh,
        in_specs=(
            tokens, one, one, one_rows, one, one, one_rows, one, one, one, one_rows, one,
            one_rows, one, P(), tokens,
        ),
        out_specs=(
            tokens, tokens, both, both, both_rows, both, both, both_rows, both, both, both,
            both_rows, both, both_rows, both,
        ),
        check_vma=False,
    )
```

```python
import functools
import math

import jax
import jax.numpy as jnp
from jax import lax
from jax.experimental import pallas as pl
from jax.experimental.pallas import tpu as pltpu
from jax.sharding import PartitionSpec as P

norm_eps = 1e-05
gelu_coef = 0.7978845608028654
masked_value = -1e30
f32 = jnp.float32
bf16 = jnp.bfloat16
MESH = pl.DeviceIdType.MESH
HBM = pl.BlockSpec(memory_space=pl.ANY)
VMEM = pl.BlockSpec(memory_space=pltpu.VMEM)
SMEM = pl.BlockSpec(memory_space=pltpu.SMEM)
vmem_bytes = 63 * 1024 * 1024


def normalize(values, norm_gain, norm_shift):
    center = values - jnp.mean(values, axis=-1, keepdims=True)
    variance = jnp.mean(center * center, axis=-1, keepdims=True)
    return center * lax.rsqrt(variance + norm_eps) * norm_gain + norm_shift


def normalize_back(values, back, norm_gain):
    center = values - jnp.mean(values, axis=-1, keepdims=True)
    inverse = lax.rsqrt(jnp.mean(center * center, axis=-1, keepdims=True) + norm_eps)
    normal = center * inverse
    scaled = back * norm_gain
    even = jnp.mean(scaled, axis=-1, keepdims=True)
    along = jnp.mean(scaled * normal, axis=-1, keepdims=True)
    return inverse * (scaled - even - normal * along), normal


def gelu_tanh(values):
    return (
        0.5 * values * (1.0 + jnp.tanh(gelu_coef * (values + 0.044715 * values * values * values)))
    )


def matmul(left_side, right_side):
    return jnp.dot(left_side, right_side, preferred_element_type=f32)


def matmul_lt(left_side, right_side):
    return lax.dot_general(
        left_side, right_side, (((0,), (0,)), ((), ())), preferred_element_type=f32
    )


def matmul_rt(left_side, right_side):
    return lax.dot_general(
        left_side, right_side, (((1,), (1,)), ((), ())), preferred_element_type=f32
    )


def joined_bias_of(query_bias, value_bias, head_count):
    query_part = query_bias.astype(f32).reshape(head_count, -1)
    value_part = value_bias.astype(f32).reshape(head_count, -1)
    return jnp.stack([query_part, jnp.zeros_like(query_part), value_part], axis=1).reshape(-1)


def split_three(values):
    high = values.astype(bf16).astype(f32)
    rest = values - high
    middle = rest.astype(bf16).astype(f32)
    return high, middle, rest - middle


def key_columns(key_rows, slope, start):
    rows, width = key_rows.shape
    position = (start + lax.broadcasted_iota(jnp.int32, (rows, width), 0)).astype(f32)
    lane = lax.broadcasted_iota(jnp.int32, (rows, width), 1)
    high, middle, low = split_three(slope * position)
    extra = jnp.where(lane == 0, high, jnp.where(lane == 1, middle, jnp.where(lane == 2, low, 0.0)))
    return jnp.concatenate([key_rows.astype(f32), extra], axis=1).astype(bf16)


def query_columns(queries, scale):
    rows, width = queries.shape
    lane = lax.broadcasted_iota(jnp.int32, (rows, width), 1)
    ones = jnp.where(lane < 3, 1.0, 0.0)
    return jnp.concatenate([queries.astype(f32) * scale, ones], axis=1).astype(bf16)


def follow(n, after):
    for at, steps in after.items():

        def act(steps=steps):
            for step, *given in steps:
                step(*given)

        pl.when(n == at)(act)


class Forward:
    def __init__(self, heads, width, slopes, qkv, out, out_t, lse, keys, queries, values_t):
        self.heads, self.width, self.slopes, self.qkv, self.out = heads, width, slopes, qkv, out
        self.out_t, self.lse = out_t, lse
        self.keys, self.queries, self.values_t = keys, queries, values_t
        self.head = 0
        self.blocks = qkv.shape[1]
        self.block = qkv.shape[2] * qkv.shape[3]

    def rows(self, i):
        return pl.ds(pl.multiple_of(i * self.block, self.block), self.block)

    def prepare(self, b):
        width, block, qkv = self.width, self.block, self.qkv
        scale = 1.0 / math.sqrt(width)

        def body(i, _):
            rows = self.rows(i)
            for h in range(self.heads):
                base = h * 3 * width
                query, key, value = [
                    qkv[b, i, :, :, base + n * width : base + (n + 1) * width].reshape(block, width)
                    for n in range(3)
                ]
                self.keys[h, rows, :] = key_columns(key, self.slopes[self.head + h], i * block)
                self.queries[h, rows, :] = query_columns(query, scale)
                self.values_t[h, :, rows] = value.astype(f32).T.astype(bf16)
            return 0

        lax.fori_loop(0, self.blocks, body, 0)

    def one(self, b, i):
        heads, width, block = self.heads, self.width, self.block
        rows = self.rows(i)
        query = [self.queries[h, rows, :] for h in range(heads)]

        def step(j, state, diagonal):
            columns = self.rows(j)
            result = []
            for h in range(heads):
                top, total, acc = state[h]
                scores = matmul_rt(self.keys[h, columns, :], query[h])
                if diagonal:
                    key_at = lax.broadcasted_iota(jnp.int32, (block, block), 0)
                    query_at = lax.broadcasted_iota(jnp.int32, (block, block), 1)
                    scores = jnp.where(key_at <= query_at, scores, masked_value)
                newest = jnp.maximum(top, jnp.max(scores, axis=0, keepdims=True))
                shrink = jnp.exp(top - newest)
                probs = jnp.exp(scores - newest)
                total = total * shrink + jnp.sum(probs, axis=0, keepdims=True)
                acc = acc * shrink + matmul(self.values_t[h, :, columns], probs.astype(bf16))
                result.append((newest, total, acc))
            return tuple(result)

        state = tuple(
            (
                jnp.full((1, block), masked_value, f32),
                jnp.zeros((1, block), f32),
                jnp.zeros((width, block), f32),
            )
            for h in range(heads)
        )
        state = lax.fori_loop(0, i, lambda j, s: step(j, s, False), state)
        state = step(i, state, True)
        finished = []
        for h in range(heads):
            top, total, acc = state[h]
            result = acc / total
            self.out_t[b, h, :, rows] = result
            self.lse[b, h, :, rows] = top + jnp.log(total)
            finished.append(result)
        joined = finished[0] if heads == 1 else jnp.concatenate(finished, axis=0)
        self.out[b, i] = joined.T.astype(bf16).reshape(self.out.shape[2:])

    def run(self, after, each=None):
        blocks = self.blocks

        def body(n, _):
            b, i = n // blocks, n % blocks
            pl.when(i == 0)(lambda: self.prepare(b))
            self.one(b, i)
            if each is not None:
                each(b, i)
            follow(n, after)
            return 0

        lax.fori_loop(0, self.qkv.shape[0] * blocks, body, 0)


def forward_kernel(heads, width, *refs):
    Forward(heads, width, *refs).run({})


def saved_shapes(seqs, length, heads, width):
    return (
        jax.ShapeDtypeStruct((seqs, heads, width, length), f32),
        jax.ShapeDtypeStruct((seqs, heads, 1, length), f32),
    )


def forward_scratch(length, heads, width):
    return [
        pltpu.VMEM((heads, length, 2 * width), bf16),
        pltpu.VMEM((heads, length, 2 * width), bf16),
        pltpu.VMEM((heads, width, length), bf16),
    ]


def attention_forward(qkv, slopes, heads, width):
    seqs, blocks, ranks, piece, _ = qkv.shape
    length = blocks * ranks * piece
    return pl.pallas_call(
        functools.partial(forward_kernel, heads, width),
        name="attention_forward",
        out_shape=(
            jax.ShapeDtypeStruct((seqs, blocks, ranks, piece, heads * width), bf16),
            *saved_shapes(seqs, length, heads, width),
        ),
        in_specs=[SMEM, VMEM],
        out_specs=(VMEM, VMEM, VMEM),
        scratch_shapes=forward_scratch(length, heads, width),
        compiler_params=pltpu.CompilerParams(vmem_limit_bytes=vmem_bytes),
    )(slopes, qkv)


class Backward:
    def __init__(
        self, heads, width, slopes, qkv, diff, out_t, lse, joined,
        keys, queries, keys_t, values, diffs, delta, query_acc,
    ):
        self.heads, self.width, self.slopes, self.qkv, self.diff = heads, width, slopes, qkv, diff
        self.out_t, self.lse, self.joined = out_t, lse, joined
        self.keys, self.queries, self.keys_t, self.values = keys, queries, keys_t, values
        self.diffs, self.delta, self.query_acc = diffs, delta, query_acc
        self.head = 0
        self.blocks = qkv.shape[1]
        self.block = qkv.shape[2] * qkv.shape[3]

    def rows(self, i):
        return pl.ds(pl.multiple_of(i * self.block, self.block), self.block)

    def prepare(self, b):
        width, block, qkv = self.width, self.block, self.qkv
        scale = 1.0 / math.sqrt(width)

        def body(i, _):
            rows = self.rows(i)
            for h in range(self.heads):
                base = h * 3 * width
                query, key, value = [
                    qkv[b, i, :, :, base + n * width : base + (n + 1) * width].reshape(block, width)
                    for n in range(3)
                ]
                self.keys[h, rows, :] = key_columns(key, self.slopes[self.head + h], i * block)
                self.keys_t[h, :, rows] = key.astype(f32).T.astype(bf16)
                self.queries[h, rows, :] = query_columns(query, scale)
                self.values[h, rows, :] = value
                part = self.diff[b, i, :, :, h * width : (h + 1) * width].reshape(block, width)
                self.diffs[h, rows, :] = part
                self.delta[h, :, rows] = jnp.sum(
                    part.astype(f32).T * self.out_t[b, h, :, rows], axis=0, keepdims=True
                )
                self.query_acc[h, :, rows] = jnp.zeros((width, block), f32)
            return 0

        lax.fori_loop(0, self.blocks, body, 0)

    def one(self, b, j):
        heads, width, block = self.heads, self.width, self.block
        tail = self.joined.shape[2:4] + (width,)
        columns = self.rows(j)

        def step(i, state, diagonal):
            rows = self.rows(i)
            result = []
            for h in range(heads):
                key_acc, value_acc = state[h]
                query = self.queries[h, rows, :]
                part = self.diffs[h, rows, :]
                scores = matmul_rt(self.keys[h, columns, :], query)
                probs = jnp.exp(scores - self.lse[b, h, :, rows])
                if diagonal:
                    key_at = lax.broadcasted_iota(jnp.int32, (block, block), 0)
                    query_at = lax.broadcasted_iota(jnp.int32, (block, block), 1)
                    probs = jnp.where(key_at <= query_at, probs, 0.0)
                prob_diff = matmul_rt(self.values[h, columns, :], part)
                score_diff = (probs * (prob_diff - self.delta[h, :, rows])).astype(bf16)
                value_acc = value_acc + matmul(probs.astype(bf16), part)
                key_acc = key_acc + matmul(score_diff, query)
                self.query_acc[h, :, rows] += matmul(self.keys_t[h, :, columns], score_diff)
                result.append((key_acc, value_acc))
            return tuple(result)

        state = tuple(
            (jnp.zeros((block, 2 * width), f32), jnp.zeros((block, width), f32))
            for h in range(heads)
        )
        state = step(j, state, True)
        state = lax.fori_loop(j + 1, self.blocks, lambda i, s: step(i, s, False), state)
        for h in range(heads):
            base = (h * 3 + 1) * width
            key_acc, value_acc = state[h]
            self.joined[b, j, :, :, base : base + width] = (
                key_acc[:, :width].astype(bf16).reshape(tail)
            )
            self.joined[b, j, :, :, base + width : base + 2 * width] = value_acc.astype(
                bf16
            ).reshape(tail)

    def run(self, after, each=None):
        blocks = self.blocks

        def body(n, _):
            b, j = n // blocks, n % blocks
            pl.when(j == 0)(lambda: self.prepare(b))
            self.one(b, j)
            self.finish(b, j)
            if each is not None:
                each(b, j)
            follow(n, after)
            return 0

        lax.fori_loop(0, self.qkv.shape[0] * blocks, body, 0)

    def finish(self, b, j):
        width = self.width
        scale = 1.0 / math.sqrt(width)
        for h in range(self.heads):
            base = h * 3 * width
            result = (self.query_acc[h, :, self.rows(j)] * scale).T.astype(bf16)
            self.joined[b, j, :, :, base : base + width] = result.reshape(
                self.joined.shape[2:4] + (width,)
            )


def backward_kernel(heads, width, *refs):
    Backward(heads, width, *refs).run({})


def backward_scratch(length, heads, width):
    return [
        pltpu.VMEM((heads, length, 2 * width), bf16),
        pltpu.VMEM((heads, length, 2 * width), bf16),
        pltpu.VMEM((heads, width, length), bf16),
        pltpu.VMEM((heads, length, width), bf16),
        pltpu.VMEM((heads, length, width), bf16),
        pltpu.VMEM((heads, 1, length), f32),
        pltpu.VMEM((heads, width, length), f32),
    ]


def attention_backward(qkv, diff, out_t, lse, slopes, heads, width):
    length = qkv.shape[1] * qkv.shape[2] * qkv.shape[3]
    return pl.pallas_call(
        functools.partial(backward_kernel, heads, width),
        name="attention_backward",
        out_shape=jax.ShapeDtypeStruct(qkv.shape, bf16),
        in_specs=[SMEM, VMEM, VMEM, VMEM, VMEM],
        out_specs=VMEM,
        scratch_shapes=backward_scratch(length, heads, width),
        compiler_params=pltpu.CompilerParams(vmem_limit_bytes=vmem_bytes),
    )(slopes, qkv, diff, out_t, lse)


def to_own_seqs(values):
    seqs, piece, features = values.shape
    parts = lax.axis_size("fs")
    values = values.reshape(parts, seqs // parts, piece, features)
    return lax.all_to_all(values, "fs", split_axis=0, concat_axis=0).transpose(1, 0, 2, 3)


def from_own_seqs(values):
    own, parts, piece, features = values.shape
    values = lax.all_to_all(values.transpose(1, 0, 2, 3), "fs", split_axis=0, concat_axis=0)
    return values.reshape(parts * own, piece, features)


def to_heads(values):
    own, parts, piece, features = values.shape
    ranks = lax.axis_size("sp")
    values = values.reshape(own, parts, piece, ranks, features // ranks)
    return lax.all_to_all(values, "sp", split_axis=3, concat_axis=2)


def from_heads(values):
    own, parts, ranks, piece, features = values.shape
    values = lax.all_to_all(values, "sp", split_axis=2, concat_axis=3)
    return values.reshape(own, parts, piece, ranks * features)


class Copies:
    def __init__(self, send, recv, local):
        self.send, self.recv, self.local = send, recv, local
        self.used, self.used_local, self.made, self.partial = 0, 0, [], []

    def plan(self, source, target, device, at=None, only=None):
        send, recv = (self.used, self.used) if at is None else at
        copy = pltpu.make_async_remote_copy(
            src_ref=source,
            dst_ref=target,
            send_sem=self.send.at[send],
            recv_sem=self.recv.at[recv],
            device_id=device,
            device_id_type=MESH,
        )
        if at is None:
            self.used += 1
        if only is None:
            self.made.append(copy)
        else:
            self.partial.append((only, copy))
        return copy

    def take(self, count):
        self.used += count
        return range(self.used - count, self.used)

    def inside(self, source, target):
        copy = pltpu.make_async_copy(source, target, self.local.at[self.used_local])
        self.used_local += 1
        return copy

    def finish(self):
        assert (self.used, self.used_local) == (self.send.shape[0], self.local.shape[0])
        for copy in self.made:
            copy.wait_send()
        for only, copy in self.partial:
            pl.when(only)(copy.wait_send)


def go(copies):
    for copy in copies:
        copy.start()


def arrive(copies):
    for copy in copies:
        copy.wait_recv()


def done(copies):
    for copy in copies:
        copy.wait()


def greet(devices):
    barrier = pltpu.get_barrier_semaphore()
    for device in devices:
        pl.semaphore_signal(barrier, inc=1, device_id=device, device_id_type=MESH)
    pl.semaphore_wait(barrier, len(devices))


def paired(z, mask):
    return 2 * ((z // 2 + mask // 2) % 2) + (z + mask) % 2


class Place:
    def __init__(self):
        z, s = lax.axis_index("fs"), lax.axis_index("sp")
        self.z, self.s = z, s
        self.core, self.chip = s % 2, s // 2
        self.x, self.y = self.chip % 2, self.chip // 2
        self.along_x = s + 2 - 4 * self.x
        self.along_y = s + 4 - 8 * self.y
        self.partner = s + 1 - 2 * self.core
        self.diagonal = self.along_x + self.along_y - s
        self.chip_x, self.chip_y = self.along_x // 2, self.along_y // 2
        self.lines = [(paired(z, 3 - k), s) for k in range(3)]
        self.plane = [(z, lax.rem(s + d, 8)) for d in range(1, 8)]
        self.to_x, self.to_y, self.to_core = [
            (z, to) for to in (self.along_x, self.along_y, self.partner)
        ]
        self.beside = z + 1 - 2 * (z % 2)
        self.inner = ((z + 1) // 2) % 2
        self.other_inner, self.other_outer = 2 - z // 2, 3 * (1 - z // 2)
        self.near = self.lines + [self.to_x, self.to_y, self.to_core]


class Gather:
    copies_each = 33

    def __init__(self, place, weights, wholes, kept, chunks, copies, given=None, relayed=()):
        z, s, lines = place.z, place.s, place.lines
        self.is_given = given is not None
        self.inner, self.passed = place.inner == 1, {}
        self.loads, self.own = [], []
        for weight, whole, keep in zip(weights, wholes, kept):
            if keep is None:
                self.loads.append(copies.inside(weight, whole.at[z]))
            else:
                self.loads.append(copies.inside(weight, keep))
                self.own.append(copies.inside(keep, whole.at[z]))
        self.first, self.second, self.third, self.cores, self.last = [], [], [], [], []
        for t, row, rows, column, columns in chunks:
            whole = wholes[t]
            wide = pl.ds(column, columns)
            every = pl.ds(row, rows)
            low, high = pl.ds(row, rows // 2), pl.ds(row + rows // 2, rows // 2)

            def same(k, rank, part, to):
                where = (k, rank, part, wide)
                return copies.plan(whole.at[where], whole.at[where], to)

            number = len(self.first)
            if number in relayed:
                near, middle, far, second = copies.take(4)
                part = (s, every, wide)
                beside = (place.beside, s)
                first = [
                    copies.plan(
                        weights[t].at[part], whole.at[(z, *part)], beside, at=(near, near)
                    ),
                    copies.plan(
                        weights[t].at[part],
                        whole.at[(z, *part)],
                        (place.other_inner, s),
                        at=(second, middle + 1 - place.inner),
                    ),
                ]
                self.passed[number] = [
                    copies.plan(
                        whole.at[(k, *part)], whole.at[(k, *part)], beside, at=(n, n),
                        only=self.inner,
                    )
                    for k, n in ((place.other_inner, middle), (place.other_outer, far))
                ]
            elif given is None:
                first = [
                    copies.plan(weights[t].at[s, every, wide], whole.at[z, s, every, wide], to)
                    for to in lines
                ]
            else:
                first = [
                    copies.inside(given.at[k, every, wide], whole.at[k, s, every, wide])
                    for k, _ in lines
                ]
            self.first.append(first)
            second, third, cores, last = [], [], [], []
            for k, _ in lines:
                second.append(same(k, s, low, place.to_x))
                second.append(same(k, s, high, place.to_y))
                cores.append(same(k, s, every, place.to_core))
                third.append(same(k, s, low, place.to_y))
                third.append(same(k, s, high, place.to_x))
                third.append(same(k, place.along_x, low, place.to_y))
                third.append(same(k, place.along_y, high, place.to_x))
                for rank in (place.along_x, place.along_y, place.diagonal):
                    last.append(same(k, rank, every, place.to_core))
            self.second.append(second)
            self.third.append(third)
            self.cores.append(cores)
            self.last.append(last)

    def keep(self):
        done(self.loads)
        go(self.own)

    def start(self, t):
        go(self.first[t])

    def pass_on(self, t):
        def act():
            for copy in self.passed[t]:
                copy.wait_recv()
                copy.start()

        pl.when(self.inner)(act)

    def exchange(self, t):
        if t in self.passed:
            arrive(self.first[t][:1])
            pl.when(jnp.logical_not(self.inner))(lambda: arrive(self.passed[t]))
        elif self.is_given:
            done(self.first[t])
        else:
            arrive(self.first[t])
        go(self.second[t])
        go(self.cores[t])

    def spread(self, t):
        arrive(self.second[t])
        go(self.third[t])

    def share(self, t):
        arrive(self.third[t])
        go(self.last[t])

    def complete(self, t):
        arrive(self.cores[t] + self.last[t])


def add_into(target, other):
    target[...] = (target[...].astype(f32) + other[...].astype(f32)).astype(target.dtype)


def add_blocks(steps, block_of):
    def body(i, _):
        add_into(*block_of(i))
        return 0

    lax.fori_loop(0, steps, body, 0)


class Reduce:
    copies_each = 10

    def __init__(self, place, grads, outs, bufs, chunks, copies):
        self.place, self.outs, self.chunks = place, outs, chunks
        self.bufs = [bufs[7 * t : 7 * t + 7] for t in range(len(chunks))]
        self.loads, self.first, self.second, self.third, self.fourth = [], [], [], [], []
        for (t, row, rows, column, columns), buf in zip(chunks, self.bufs):
            own, from_core, from_x, from_y, late_y, late_x, from_z = buf
            every, wide = pl.ds(row, rows), pl.ds(column, columns)
            low, high = pl.ds(0, rows // 2), pl.ds(rows // 2, rows // 2)
            self.loads.append(
                copies.inside(grads[t].at[:, :, place.core, every, wide], own)
            )
            self.first.append(
                copies.plan(
                    grads[t].at[:, :, 1 - place.core, every, wide], from_core, place.to_core
                )
            )
            step = []
            for k in range(2):
                step.append(
                    copies.plan(own.at[:, 2 * k + 1 - place.x, low], from_x.at[:, k], place.to_x)
                )
                step.append(
                    copies.plan(
                        own.at[:, 2 * (1 - place.y) + k, high], from_y.at[:, k], place.to_y
                    )
                )
            self.second.append(step)
            self.third.append(
                [
                    copies.plan(own.at[:, place.chip_y, low], late_y, place.to_y),
                    copies.plan(own.at[:, place.chip_x, high], late_x, place.to_x),
                ]
            )
            self.fourth.append(
                [
                    copies.plan(own.at[to[0], place.chip], from_z.at[k], to)
                    for k, to in enumerate(place.lines)
                ]
            )

    def start(self):
        go(self.first)

    def begin(self, t):
        go([self.loads[t], self.first[t]])

    def halves(self, t):
        half = self.chunks[t][2] // 2
        return pl.ds(0, half), pl.ds(half, half)

    def exchange(self, t):
        own, from_core = self.bufs[t][:2]
        self.loads[t].wait()
        arrive([self.first[t]])
        add_blocks(16, lambda i: (own.at[i // 4, i % 4], from_core.at[i // 4, i % 4]))
        go(self.second[t])

    def spread(self, t):
        own, _, from_x, from_y = self.bufs[t][:4]
        low, high = self.halves(t)
        x, y = self.place.x, self.place.y
        arrive(self.second[t])
        add_blocks(8, lambda i: (own.at[i // 2, 2 * (i % 2) + x, low], from_x.at[i // 2, i % 2]))
        add_blocks(8, lambda i: (own.at[i // 2, 2 * y + i % 2, high], from_y.at[i // 2, i % 2]))
        go(self.third[t])

    def send(self, t):
        own, _, _, _, late_y, late_x, _ = self.bufs[t]
        low, high = self.halves(t)
        chip = self.place.chip
        arrive(self.third[t])
        add_blocks(4, lambda i: (own.at[i, chip, low], late_y.at[i]))
        add_blocks(4, lambda i: (own.at[i, chip, high], late_x.at[i]))
        go(self.fourth[t])

    def finish(self, t):
        own, from_z = self.bufs[t][0], self.bufs[t][6]
        index, row, rows, column, columns = self.chunks[t]
        arrive(self.fourth[t])
        total = own[self.place.z, self.place.chip].astype(f32)
        for k in range(3):
            total = total + from_z[k].astype(f32)
        self.outs[index][row : row + rows, column : column + columns] = total


def reduce_scratch(chunks):
    scratch = []
    for _, _, rows, _, columns in chunks:
        half = rows // 2
        scratch += [
            pltpu.VMEM((4, 4, rows, columns), bf16),
            pltpu.VMEM((4, 4, rows, columns), bf16),
            pltpu.VMEM((4, 2, half, columns), bf16),
            pltpu.VMEM((4, 2, half, columns), bf16),
            pltpu.VMEM((4, half, columns), bf16),
            pltpu.VMEM((4, half, columns), bf16),
            pltpu.VMEM((3, rows, columns), bf16),
        ]
    return scratch


class ReduceAlong(Reduce):
    def __init__(self, place, grad, out, buf, chunk, copies):
        self.place, self.grad, self.out, self.buf, self.chunk = place, grad, out, buf, chunk
        own, from_core, from_z, from_x, from_y, late_y, late_x = buf
        _, row, rows, column, columns = chunk
        every, wide = pl.ds(row, rows), pl.ds(column, columns)
        self.low, self.high = low, high = pl.ds(0, rows // 2), pl.ds(rows // 2, rows // 2)
        z, x, y = place.z, place.x, place.y
        self.load = copies.inside(grad.at[:, :, place.core, every, wide], own)
        self.first = copies.plan(
            grad.at[:, :, 1 - place.core, every, wide], from_core, place.to_core
        )
        self.second = [
            copies.plan(own.at[to[0]], from_z.at[k], to) for k, to in enumerate(place.lines)
        ]
        self.third = []
        for k in range(2):
            self.third.append(
                copies.plan(own.at[z, 2 * k + 1 - x, low], from_x.at[k], place.to_x)
            )
            self.third.append(
                copies.plan(own.at[z, 2 * (1 - y) + k, high], from_y.at[k], place.to_y)
            )
        self.fourth = [
            copies.plan(own.at[z, place.chip_y, low], late_y, place.to_y),
            copies.plan(own.at[z, place.chip_x, high], late_x, place.to_x),
        ]

    def exchange(self):
        own, from_core = self.buf[:2]
        self.load.wait()
        arrive([self.first])
        add_blocks(16, lambda i: (own.at[i // 4, i % 4], from_core.at[i // 4, i % 4]))
        go(self.second)

    def spread(self):
        own, _, from_z = self.buf[:3]
        z = self.place.z
        arrive(self.second)

        def body(i, _):
            total = own[z, i].astype(f32)
            for k in range(3):
                total = total + from_z[k, i].astype(f32)
            own[z, i] = total.astype(bf16)
            return 0

        lax.fori_loop(0, 4, body, 0)
        go(self.third)

    def send(self):
        own, _, _, from_x, from_y = self.buf[:5]
        z, x, y = self.place.z, self.place.x, self.place.y
        arrive(self.third)
        add_blocks(2, lambda j: (own.at[z, 2 * j + x, self.low], from_x.at[j]))
        add_blocks(2, lambda j: (own.at[z, 2 * y + j, self.high], from_y.at[j]))
        go(self.fourth)

    def finish(self):
        own, late_y, late_x = self.buf[0], self.buf[5], self.buf[6]
        z, chip = self.place.z, self.place.chip
        _, row, rows, column, columns = self.chunk
        arrive(self.fourth)
        half = rows // 2
        wide = slice(column, column + columns)
        self.out[row : row + half, wide] = own[z, chip, self.low].astype(f32) + late_y[...].astype(
            f32
        )
        self.out[row + half : row + rows, wide] = own[z, chip, self.high].astype(f32) + late_x[
            ...
        ].astype(f32)


def reduce_along_scratch(chunk):
    _, _, rows, _, columns = chunk
    half = rows // 2
    return [
        pltpu.VMEM((4, 4, rows, columns), bf16),
        pltpu.VMEM((4, 4, rows, columns), bf16),
        pltpu.VMEM((3, 4, rows, columns), bf16),
        pltpu.VMEM((2, half, columns), bf16),
        pltpu.VMEM((2, half, columns), bf16),
        pltpu.VMEM((half, columns), bf16),
        pltpu.VMEM((half, columns), bf16),
    ]


class HandBack:
    def __init__(self, place, source, target, features, send, recv, local):
        self.place, self.source, self.target = place, source, target
        self.mine = columns_of(place.s, features)
        self.send, self.recv, self.local = send, recv, local
        self.blocks = source.shape[1]

    def copy(self, b, i, d):
        rank = self.place.plane[d][1]
        n = b * self.blocks + i
        return pltpu.make_async_remote_copy(
            src_ref=self.source.at[b, i, rank],
            dst_ref=self.target.at[b, i, :, self.mine],
            send_sem=self.send.at[n, d],
            recv_sem=self.recv.at[n, d],
            device_id=self.place.plane[d],
            device_id_type=MESH,
        )

    def own(self, b, i):
        return pltpu.make_async_copy(
            self.source.at[b, i, self.place.s],
            self.target.at[b, i, :, self.mine],
            self.local.at[b * self.blocks + i],
        )

    def each(self, b, i):
        for d in range(7):
            self.copy(b, i, d).start()
        self.own(b, i).start()

    def finish(self):
        def body(n, _):
            b, i = n // self.blocks, n % self.blocks
            for d in range(7):
                self.copy(b, i, d).wait()
            self.own(b, i).wait()
            return 0

        lax.fori_loop(0, self.source.shape[0] * self.blocks, body, 0)


def hand_back_semaphores(steps):
    return [
        pltpu.SemaphoreType.DMA((steps, 7)),
        pltpu.SemaphoreType.DMA((steps, 7)),
        pltpu.SemaphoreType.DMA((steps,)),
    ]


class ReduceLines:
    copies = 4 * 7 + 3 + 3 + 6

    def __init__(self, place, grad, out, bufs, copies):
        self.place, self.grad, self.out, self.bufs = place, grad, out, bufs
        from_core, from_x, from_y, late_y, late_x, from_z = bufs[:6]
        early_z, own_x, own_y, own_late_y, own_late_x = bufs[6:]
        core, x, y = place.core, place.x, place.y
        self.order = [to[0] for to in place.lines] + [place.z]
        rows = grad.shape[3]
        low, high = pl.ds(0, rows // 2), pl.ds(rows // 2, rows // 2)
        cut = from_z.shape[2]
        most, rest = pl.ds(0, cut), pl.ds(cut, grad.shape[4] - cut)
        self.low, self.high, self.all = (low, most), (high, most), (pl.ds(0, rows), most)
        self.low_rest, self.high_rest = (low, rest), (high, rest)
        self.all_rest = (pl.ds(0, rows), rest)
        z = place.z
        self.early = [
            copies.plan(grad.at[(to[0], pl.ds(0, 4), core, *self.all_rest)], early_z.at[k], to)
            for k, to in enumerate(place.lines)
        ]
        self.own_second, self.own_third = [], []
        for j in range(2):
            self.own_second.append(
                copies.plan(
                    grad.at[(z, 2 * j + 1 - x, core, *self.low_rest)], own_x.at[j], place.to_x
                )
            )
            self.own_second.append(
                copies.plan(
                    grad.at[(z, 2 * (1 - y) + j, core, *self.high_rest)], own_y.at[j], place.to_y
                )
            )
        self.own_third = [
            copies.plan(
                grad.at[(z, place.chip_y, core, *self.low_rest)], own_late_y, place.to_y
            ),
            copies.plan(
                grad.at[(z, place.chip_x, core, *self.high_rest)], own_late_x, place.to_x
            ),
        ]
        self.first, self.second, self.third, self.fourth = [], [], [], []
        for k, at in enumerate(self.order):
            self.first.append(
                copies.plan(grad.at[at, :, 1 - core], from_core.at[k], place.to_core)
            )
            step = []
            for j in range(2):
                step.append(
                    copies.plan(
                        grad.at[(at, 2 * j + 1 - x, core, *self.low)], from_x.at[k, j], place.to_x
                    )
                )
                step.append(
                    copies.plan(
                        grad.at[(at, 2 * (1 - y) + j, core, *self.high)], from_y.at[k, j], place.to_y
                    )
                )
            self.second.append(step)
            self.third.append(
                [
                    copies.plan(
                        grad.at[(at, place.chip_y, core, *self.low)], late_y.at[k], place.to_y
                    ),
                    copies.plan(
                        grad.at[(at, place.chip_x, core, *self.high)], late_x.at[k], place.to_x
                    ),
                ]
            )
            if k < 3:
                self.fourth.append(
                    copies.plan(
                        grad.at[(at, place.chip, core, *self.all)], from_z.at[k], place.lines[k]
                    )
                )

    def start(self, k):
        go([self.first[k]])

    def exchange(self, k):
        arrive([self.first[k]])
        at, core = self.order[k], self.place.core
        add_blocks(4, lambda i: (self.grad.at[at, i, core], self.bufs[0].at[k, i]))
        go(self.second[k] + self.early[k : k + 1])

    def spread(self, k):
        arrive(self.second[k])
        at, core, x, y = self.order[k], self.place.core, self.place.x, self.place.y
        add_blocks(
            2, lambda j: (self.grad.at[(at, 2 * j + x, core, *self.low)], self.bufs[1].at[k, j])
        )
        add_blocks(
            2, lambda j: (self.grad.at[(at, 2 * y + j, core, *self.high)], self.bufs[2].at[k, j])
        )
        go(self.third[k])

    def send(self, k):
        arrive(self.third[k])
        at, core, chip = self.order[k], self.place.core, self.place.chip
        add_into(self.grad.at[(at, chip, core, *self.low)], self.bufs[3].at[k])
        add_into(self.grad.at[(at, chip, core, *self.high)], self.bufs[4].at[k])
        go(self.fourth[k : k + 1])

    def own_spread(self):
        arrive(self.early)
        z, core = self.place.z, self.place.core

        def body(i, _):
            target = self.grad.at[(z, i, core, *self.all_rest)]
            total = target[...].astype(f32)
            for k in range(3):
                total = total + self.bufs[6][k, i].astype(f32)
            target[...] = total.astype(bf16)
            return 0

        lax.fori_loop(0, 4, body, 0)
        go(self.own_second)

    def own_send(self):
        arrive(self.own_second)
        z, core, x, y = self.place.z, self.place.core, self.place.x, self.place.y
        for j in range(2):
            add_into(self.grad.at[(z, 2 * j + x, core, *self.low_rest)], self.bufs[7].at[j])
            add_into(self.grad.at[(z, 2 * y + j, core, *self.high_rest)], self.bufs[8].at[j])
        go(self.own_third)

    def finish(self):
        arrive(self.fourth + self.own_third)
        place = self.place
        at = (place.z, place.chip, place.core)
        total = self.grad[(*at, *self.all)].astype(f32)
        for k in range(3):
            total = total + self.bufs[5][k].astype(f32)
        cut = total.shape[1]
        half = total.shape[0] // 2
        self.out[:, :cut] = total
        self.out[:half, cut:] = self.grad[(*at, *self.low_rest)].astype(f32) + self.bufs[9][
            ...
        ].astype(f32)
        self.out[half:, cut:] = self.grad[(*at, *self.high_rest)].astype(f32) + self.bufs[10][
            ...
        ].astype(f32)


def reduce_lines_scratch(rows, columns, rest):
    half = rows // 2
    most = columns - rest
    return [
        pltpu.VMEM((4, 4, rows, columns), bf16),
        pltpu.VMEM((4, 2, half, most), bf16),
        pltpu.VMEM((4, 2, half, most), bf16),
        pltpu.VMEM((4, half, most), bf16),
        pltpu.VMEM((4, half, most), bf16),
        pltpu.VMEM((3, rows, most), bf16),
        pltpu.VMEM((3, 4, rows, rest), bf16),
        pltpu.VMEM((2, half, rest), bf16),
        pltpu.VMEM((2, half, rest), bf16),
        pltpu.VMEM((half, rest), bf16),
        pltpu.VMEM((half, rest), bf16),
    ]


def split_grad(item):
    return item.reshape(4, 4, 2, item.shape[0] // 32, item.shape[1])


def split_weight(item):
    return item.reshape(8, item.shape[0] // 8, item.shape[1])


def chunks_of(index, rows, columns, count):
    if rows >= 64:
        return [(index, rows // count * n, rows // count, 0, columns) for n in range(count)]
    return [(index, 0, rows, columns // count * n, columns // count) for n in range(count)]


def semaphores(remote, local):
    return [pltpu.SemaphoreType.DMA((n,)) for n in (remote, remote, local)]


def remote_call(kernel, name, collective, **options):
    return pl.pallas_call(
        kernel,
        name=name,
        compiler_params=pltpu.CompilerParams(
            collective_id=collective, has_side_effects=True, vmem_limit_bytes=vmem_bytes
        ),
        **options,
    )


def row_of(packed, n, size):
    found = [packed[k, n, r : r + 1, :] for k in range(4) for r in range(size // 512)]
    return jnp.concatenate(found, axis=1)


def columns_of(rank, features):
    return pl.ds(pl.multiple_of(rank * features, 128), features)


def forward_fused_kernel(heads, width, count, vector_count, chunks, slopes, tokens, upstream, *refs):
    vectors, refs = refs[:vector_count], refs[vector_count:]
    weights, contract, refs = refs[:count], refs[count], refs[count + 1 :]
    tokens_out, vectors_out, joined_out, qkv_out, attended, *saved, upstream_out = refs[:8]
    contract_out = refs[8]
    wholes, refs = refs[9 : 8 + count], refs[8 + count :]
    held, small, values_of, joined, normed, outgoing, qkv, result, upstream_own = refs[:9]
    attention = Forward(heads, width, slopes, qkv, result, *refs[9:14])
    kept, refs = refs[14 : 13 + count], refs[13 + count :]
    head_send, head_recv = refs[:2]
    copies = Copies(*refs[5:])
    place = Place()
    z, s, lines, plane = place.z, place.s, place.lines, place.plane
    attention.head = s * heads
    first = [t for t, chunk in enumerate(chunks) if chunk[0] == 0]
    gather = Gather(
        place, weights, [joined, *wholes], [None, *kept], chunks, copies, relayed=first
    )
    later = [t for t, chunk in enumerate(chunks) if chunk[0] > 0]
    features = heads * width
    back = HandBack(place, result, attended, features, *refs[2:5])
    own_seqs, parts, piece, wide = held.shape

    load = copies.inside(tokens.at[z], held.at[:, z])
    load_upstream = copies.inside(upstream.at[z], upstream_own)
    seqs = [copies.plan(tokens.at[to[0]], held.at[:, z], to) for to in lines]
    vector_copies = [copies.plan(small.at[z], small.at[z], to) for to in lines]
    upstreams = [copies.plan(upstream.at[to[0]], upstream_out.at[:, z], to) for to in lines]
    keep_upstream = copies.inside(upstream_own, upstream_out.at[:, z])
    keeping = [
        copies.inside(held, tokens_out),
        copies.inside(small, vectors_out),
        copies.inside(joined, joined_out),
    ]
    keep_qkv = copies.inside(qkv, qkv_out)
    keep_saved = [copies.inside(attention.out_t, saved[0]), copies.inside(attention.lse, saved[1])]
    contracts = [copies.plan(contract.at[s], contract_out.at[z], to) for to in lines]

    def to_head(d):
        return pltpu.make_async_remote_copy(
            src_ref=outgoing.at[d],
            dst_ref=qkv.at[:, :, s],
            send_sem=head_send.at[d],
            recv_sem=head_recv.at[d],
            device_id=(z, lax.rem(s + 1 + d, 8)),
            device_id_type=MESH,
        )

    go(gather.loads + [load, load_upstream])
    small[z] = jnp.zeros(small.shape[1:], bf16)
    for n, item in enumerate(vectors):
        small[z, n, : item.shape[0], :] = item[...]
    greet(lines + plane)
    for t in first:
        gather.start(t)
    for t in first:
        gather.pass_on(t)
    go(seqs + vector_copies)
    gather.keep()
    load.wait()
    for t in range(len(first) + 2):
        if t < len(first):
            gather.exchange(t)
        if 0 <= t - 1 < len(first):
            gather.spread(t - 1)
        if 0 <= t - 2:
            gather.share(t - 2)
    load_upstream.wait()
    keep_upstream.start()
    arrive(seqs + vector_copies)
    for t in later:
        gather.start(t)
    values_of[...] = small[...].astype(f32)

    gain, shift = row_of(values_of, 0, wide), row_of(values_of, 1, wide)

    def norm(i, _):
        values = held[i // parts, i % parts].astype(f32)
        rows = pl.ds(pl.multiple_of(i * piece, piece), piece)
        normed[rows, :] = normalize(values, gain, shift).astype(bf16)
        return 0

    lax.fori_loop(0, own_seqs * parts, norm, 0)
    for t in first:
        gather.complete(t)
    go(keeping)

    def project(d, _):
        rank = lax.rem(s + 1 + d, 8)
        per = 8 // 4
        query_bias = values_of[rank // per, 2, pl.ds(rank % per, 1), :]
        value_bias = values_of[rank // per, 3, pl.ds(rank % per, 1), :]
        low = lax.broadcasted_iota(jnp.int32, query_bias.shape, 1) < width
        bias = jnp.concatenate(
            [
                jnp.where(low, query_bias, 0.0),
                jnp.where(low, value_bias, query_bias),
                jnp.where(low, 0.0, value_bias),
            ],
            axis=1,
        )
        weight = joined[:, :, :, columns_of(rank, 3 * features)].reshape(wide, 3 * features)
        made = (matmul(normed[...], weight) + bias).astype(bf16)
        outgoing[d] = made.reshape(outgoing.shape[1:])
        pl.when(d < 7)(lambda: to_head(d).start())
        return 0

    lax.fori_loop(0, 8, project, 0)
    own_copy = copies.inside(outgoing.at[7], qkv.at[:, :, s])
    own_copy.start()
    base = later[0]
    gather.exchange(base)
    gather.exchange(base + 1)
    own_copy.wait()
    gather.spread(base)
    go(contracts)
    for d in range(7):
        to_head(d).wait_recv()
    keep_qkv.start()
    attention.run(
        {
            0: [(gather.exchange, base + 2), (go, upstreams), (gather.spread, base + 1)],
            2: [(gather.spread, base + 2), (gather.share, base)],
            5: [(gather.share, base + 1)],
            6: [(gather.share, base + 2)],
        },
        back.each,
    )
    go(keep_saved)
    for t in later:
        gather.complete(t)
    arrive(contracts + upstreams)
    back.finish()
    for d in range(7):
        to_head(d).wait_send()
    copies.finish()
    done(gather.own + [keep_upstream, keep_qkv] + keep_saved + keeping)


def forward_fused(tokens, upstream, vectors, weights, contract, slopes, heads, width):
    seqs, piece, features = tokens.shape
    parts = 4
    own = seqs // parts
    columns = heads * width
    length = parts * 8 * piece
    vectors = [item.reshape(-1, 128) for item in vectors]
    cut = [split_weight(item) for item in weights]
    contract = split_weight(contract)
    count, tall = len(cut), 8 * -(-max(item.shape[0] for item in vectors) // 8)
    chunks = []
    for t, pieces in enumerate((3, 1, 2)):
        chunks += chunks_of(t, *cut[t].shape[1:], pieces)
    seq_shape = (own, parts, piece, features)
    qkv_shape = (own, parts, 8, piece, 3 * columns)
    small = (parts, len(vectors), tall, 128)
    out = remote_call(
        functools.partial(forward_fused_kernel, heads, width, count, len(vectors), chunks),
        "forward_fused",
        1,
        out_shape=(
            jax.ShapeDtypeStruct(seq_shape, bf16),
            jax.ShapeDtypeStruct(small, bf16),
            jax.ShapeDtypeStruct((parts, *cut[0].shape), bf16),
            jax.ShapeDtypeStruct(qkv_shape, bf16),
            jax.ShapeDtypeStruct(seq_shape, bf16),
            *saved_shapes(own, length, heads, width),
            jax.ShapeDtypeStruct(seq_shape, bf16),
            jax.ShapeDtypeStruct((parts, *contract.shape[1:]), bf16),
            *[jax.ShapeDtypeStruct((parts, *item.shape), bf16) for item in cut[1:]],
        ),
        in_specs=[SMEM, HBM, HBM] + [VMEM] * len(vectors) + [HBM] * (count + 1),
        out_specs=(HBM,) * (8 + count),
        scratch_shapes=[
            pltpu.VMEM(seq_shape, bf16),
            pltpu.VMEM(small, bf16),
            pltpu.VMEM(small, f32),
            pltpu.VMEM((parts, *cut[0].shape), bf16),
            pltpu.VMEM((own * parts * piece, features), bf16),
            pltpu.VMEM((8, own, parts, piece, 3 * columns), bf16),
            pltpu.VMEM(qkv_shape, bf16),
            pltpu.VMEM((own, parts, 8, piece, columns), bf16),
            pltpu.VMEM((own, piece, features), bf16),
            *[pltpu.VMEM(item.shape, f32) for item in saved_shapes(own, length, heads, width)],
            *forward_scratch(length, heads, width),
            *[pltpu.VMEM(item.shape, bf16) for item in cut[1:]],
            pltpu.SemaphoreType.DMA((7,)),
            pltpu.SemaphoreType.DMA((7,)),
            *hand_back_semaphores(own * parts),
            *semaphores(12 + 3 + len(chunks) * Gather.copies_each, 2 * count - 1 + 10),
        ],
    )(
        slopes,
        tokens.reshape(parts, own, piece, features),
        upstream.reshape(parts, own, piece, features),
        *vectors,
        *cut,
        contract,
    )
    wholes = [
        whole.reshape(4 * item.shape[0], item.shape[1])
        for whole, item in zip((out[2], *out[9:]), weights)
    ]
    return out[0], out[1], [*wholes, out[8]], out[3], out[4], (out[5], out[6]), out[7]


def feed_forward_kernel(
    chunks, expand, contract, contract_line, out_weight,
    small, upstream_in, tokens_in, attended_in,
    layer_out, residual_out, diff_out, expand_grad, out_grad, contract_grad,
    bias_grad, gain_grad, shift_grad, out_bias_grad, contract_bias_grad,
    upstream, tokens, attended, layer, residual_grad, attended_diff, values_of, expand_bias, expand_in, contract_in, residual, second, second_t, expanded, activated, grad, staged, *refs,
):
    second_back = residual_grad
    bufs, refs = refs[:11], refs[11:]
    loaded, stored, refs = refs[0], refs[1], refs[2:]
    copies = Copies(*refs)
    place = Place()
    z = place.z
    given = [
        copies.inside(a, b)
        for a, b in ((attended_in, attended), (tokens_in, tokens), (upstream_in, upstream))
    ]
    keep_layer = copies.inside(layer, layer_out)
    keep_residual = copies.inside(residual_grad, residual_out)
    keep_diff = copies.inside(attended_diff, diff_out)
    reduce = ReduceLines(place, grad, contract_grad, bufs, copies)
    gather = Gather(
        place, [contract], [contract_in], [None], chunks, copies, given=contract_line
    )
    rows, features = second.shape
    steps = 8
    wide = expand.shape[1] // steps

    def at(n):
        part = paired(z, 3 - n // 2)
        return part, n % 2, pl.ds(pl.multiple_of((2 * part + n % 2) * wide, wide), wide)

    def load(n):
        _, _, where = at(n)
        return pltpu.make_async_copy(expand.at[:, where], expand_in.at[:, where], loaded.at[n])

    def contract_at(n):
        part, side, _ = at(n)
        return contract_in[part, pl.ds(4 * side, 4)].reshape(wide, features)

    def store(n):
        _, _, where = at(n)
        slot = n % 2
        return pltpu.make_async_copy(
            staged.at[slot], expand_grad.at[:, where], stored.at[slot]
        )

    halves = [pl.ds(0, wide), pl.ds(wide, wide)]
    out_loads = [
        pltpu.make_async_copy(out_weight.at[:, half], staged.at[n], stored.at[n])
        for n, half in enumerate(halves)
    ]
    out_stores = [
        pltpu.make_async_copy(staged.at[n], out_grad.at[:, half], stored.at[n])
        for n, half in enumerate(halves)
    ]
    part_rows = rows // 8

    def rows_at(i):
        return pl.ds(pl.multiple_of(i * part_rows, part_rows), part_rows)

    for n in range(len(chunks)):
        gather.start(n)
    go(given[:2] + out_loads + given[2:])
    for n in range(steps):
        load(n).start()
    go(gather.loads)
    greet(place.near)
    for n in range(len(chunks)):
        gather.exchange(n)
    values_of[...] = small[...].astype(f32)
    out_bias, gain, shift, contract_bias = [
        row_of(values_of, n, features) for n in (4, 5, 6, 7)
    ]
    expand_bias[...] = row_of(values_of, 8, steps * wide)
    done(given)
    for n, half in enumerate(halves):
        out_loads[n].wait()
        bias = out_bias[:, n * wide : (n + 1) * wide]
        residual[:, half] = (
            tokens[:, half].astype(f32) + (matmul(attended[...], staged[n]) + bias)
        )

    def norm(i, _):
        values = residual[rows_at(i), :]
        second[rows_at(i), :] = normalize(values, gain, shift).astype(bf16)
        second_back[rows_at(i), :] = values + contract_bias
        return 0

    lax.fori_loop(0, 8, norm, 0)
    for n in range(len(chunks) - 1):
        gather.spread(n)
    second_t[...] = second[...].T

    def forward(n, after):
        part, side, where = at(n)
        load(n).wait()
        values = matmul(second[...], expand_in[:, where]) + expand_bias[:, where]
        expanded[:, where] = values
        low = gelu_tanh(values).astype(bf16)
        activated[:, where] = low
        made = matmul(low.T, upstream[...]).astype(bf16)
        grad[part, pl.ds(2 * side, 2)] = made.reshape(2, 2, wide // 4, features)
        follow(n, after)
        return 0

    def shrink(n, after):
        where = pl.ds(pl.multiple_of(n * (features // 4), 128), features // 4)
        weight = contract_in[:, :, :, where].reshape(steps * wide, features // 4)
        second_back[:, where] += matmul(activated[...], weight)
        follow(n, after)
        return 0

    def backward(n, after):
        _, _, where = at(n)
        values = expanded[:, where]
        act_grad = matmul_rt(upstream[...], contract_at(n))
        bent = jnp.tanh(gelu_coef * (values + 0.044715 * values * values * values))
        slope = 0.5 * (1.0 + bent) + 0.5 * values * (1.0 - bent * bent) * (
            gelu_coef * (1.0 + 3.0 * 0.044715 * values * values)
        )
        diff = (act_grad * slope).astype(bf16)
        bias_grad[:, where] = jnp.sum(diff.astype(f32), axis=0, keepdims=True)
        pl.when(n >= 2)(lambda: store(n - 2).wait())
        staged[n % 2] = matmul(second_t[...], diff).astype(bf16)
        store(n).start()
        second_back[...] += matmul_rt(diff, expand_in[:, where])
        follow(n, after)
        return 0

    last = len(chunks) - 1
    forward_steps = {
        0: [(gather.spread, last)],
        1: [(reduce.start, 0)],
        3: [(reduce.exchange, 0), (reduce.start, 1)],
        5: [(reduce.start, 2), (reduce.exchange, 1)],
        7: [(reduce.start, 3), (reduce.exchange, 2)] + [(gather.share, n) for n in range(last)],
    }
    shrink_steps = {
        0: [(reduce.exchange, 3)],
        1: [(reduce.spread, 0)],
        3: [(reduce.spread, 1)],
    }
    backward_steps = {
        1: [(reduce.spread, 2)],
        2: [(reduce.spread, 3)],
        3: [(reduce.send, 0), (reduce.own_spread,)],
        4: [(reduce.send, 1)],
        5: [(reduce.send, 2)],
        6: [(reduce.send, 3), (reduce.own_send,)],
    }
    lax.fori_loop(0, steps, lambda n, _: forward(n, forward_steps), 0)
    gather.share(last)
    for n in range(len(chunks)):
        gather.complete(n)
    done(gather.loads)
    lax.fori_loop(0, 4, lambda n, _: shrink(n, shrink_steps), 0)
    layer[...] = second_back[...].astype(bf16).reshape(layer.shape)
    keep_layer.start()
    second_back[...] = jnp.zeros_like(second_back)
    lax.fori_loop(0, steps, lambda n, _: backward(n, backward_steps), 0)
    store(steps - 2).wait()
    store(steps - 1).wait()
    go(out_loads)
    second_t[...] = attended[...].T

    def norm_back(i, sums):
        back = second_back[rows_at(i), :]
        part, normal = normalize_back(residual[rows_at(i), :], back, gain)
        given = upstream[rows_at(i), :].astype(f32)
        total = given + part
        low = total.astype(bf16)
        residual_grad[rows_at(i), :] = total
        second[rows_at(i), :] = low
        found = (back * normal, back, low.astype(f32), given)
        return tuple(
            kept + jnp.sum(item, axis=0, keepdims=True) for kept, item in zip(sums, found)
        )

    nothing = jnp.zeros((1, features), f32)
    sums = lax.fori_loop(0, 8, norm_back, (nothing,) * 4)
    gain_grad[...], shift_grad[...], out_bias_grad[...], contract_bias_grad[...] = sums
    keep_residual.start()
    done(out_loads)
    branch_diff = second
    made = matmul_rt(branch_diff[:, halves[0]], staged[0])
    made = (made + matmul_rt(branch_diff[:, halves[1]], staged[1])).astype(bf16)
    attended_diff[...] = made.reshape(attended_diff.shape)
    keep_diff.start()
    for n, half in enumerate(halves):
        staged[n] = matmul(second_t[...], branch_diff[:, half]).astype(bf16)
        out_stores[n].start()
    reduce.finish()
    done(out_stores + [keep_layer, keep_residual, keep_diff])
    copies.finish()


def feed_forward(shape, expand, contract, line, out_weight, tokens, upstream, attended, small):
    own, parts, piece = shape
    rows, features = tokens.shape
    hidden = expand.shape[1]
    wide = hidden // 8
    each = hidden // 32
    contract = split_weight(contract)
    chunks = chunks_of(0, *contract.shape[1:], 2)
    seq_shape = (own, parts, piece, features)
    return remote_call(
        functools.partial(feed_forward_kernel, chunks),
        "feed_forward",
        4,
        out_shape=(
            jax.ShapeDtypeStruct(seq_shape, bf16),
            jax.ShapeDtypeStruct((rows, features), f32),
            jax.ShapeDtypeStruct(seq_shape, bf16),
            jax.ShapeDtypeStruct((features, hidden), bf16),
            jax.ShapeDtypeStruct((features, features), bf16),
            jax.ShapeDtypeStruct((each, features), f32),
            jax.ShapeDtypeStruct((1, hidden), f32),
            *[jax.ShapeDtypeStruct((1, features), f32)] * 4,
        ),
        in_specs=[HBM] * 4 + [VMEM] + [HBM] * 3,
        out_specs=(HBM,) * 5 + (VMEM,) * 6,
        scratch_shapes=[
            *[pltpu.VMEM((rows, features), bf16)] * 3,
            pltpu.VMEM(seq_shape, bf16),
            pltpu.VMEM((rows, features), f32),
            pltpu.VMEM(seq_shape, bf16),
            pltpu.VMEM(small.shape, f32),
            pltpu.VMEM((1, hidden), f32),
            pltpu.VMEM((features, hidden), bf16),
            pltpu.VMEM((4, *contract.shape), bf16),
            pltpu.VMEM((rows, features), f32),
            pltpu.VMEM((rows, features), bf16),
            pltpu.VMEM((features, rows), bf16),
            pltpu.VMEM((rows, hidden), f32),
            pltpu.VMEM((rows, hidden), bf16),
            pltpu.VMEM((4, 4, 2, each, features), bf16),
            pltpu.VMEM((2, features, wide), bf16),
            *reduce_lines_scratch(each, features, features // 4),
            pltpu.SemaphoreType.DMA((8,)),
            pltpu.SemaphoreType.DMA((2,)),
            *semaphores(
                ReduceLines.copies + len(chunks) * (Gather.copies_each - 3),
                7 + 3 * len(chunks),
            ),
        ],
    )(expand, contract, line, out_weight, small, upstream, tokens, attended)


def backward_fused_kernel(heads, width, count, chunks, *refs):
    slopes, diff_in, qkv_in, out_t_in, lse_in, layer = refs[:6]
    grads, refs = refs[6 : 6 + count], refs[6 + count :]
    joined_out, layer_out, layer_own = refs[0], refs[1], refs[2 + count]
    outs, refs = refs[2 : 2 + count], refs[3 + count :]
    diff, qkv, out_t, lse, joined = refs[:5]
    attention = Backward(heads, width, slopes, qkv, diff, out_t, lse, joined, *refs[5:12])
    bufs, refs = refs[12 : 12 + 7 * len(chunks)], refs[12 + 7 * len(chunks) :]
    copies = Copies(*refs[3:])
    place = Place()
    s, plane = place.s, place.plane
    attention.head = s * heads
    features = heads * width
    along = ReduceAlong(place, grads[0], outs[0], bufs[:7], chunks[0], copies)
    reduce = Reduce(place, grads, outs, bufs[7:], chunks[1:], copies)
    back = HandBack(place, joined, joined_out, 3 * features, *refs[:3])

    own = [copies.inside(diff_in.at[:, :, :, columns_of(s, features)], diff.at[:, :, s])]
    own += [copies.inside(a, b) for a, b in ((qkv_in, qkv), (out_t_in, out_t), (lse_in, lse))]
    arriving = [
        copies.plan(diff_in.at[:, :, :, columns_of(to[1], features)], diff.at[:, :, s], to)
        for to in plane
    ]
    returned = [copies.plan(layer.at[:, to[0]], layer_out.at[place.z], to) for to in place.lines]
    load_layer = copies.inside(layer.at[:, place.z], layer_own)
    keep_layer = copies.inside(layer_own, layer_out.at[place.z])
    go(own + reduce.loads + [along.load, load_layer])
    greet(place.lines + plane)
    go(arriving + [along.first])
    reduce.start()
    along.exchange()
    go(returned)
    for t in range(3):
        reduce.exchange(t)
    done(own + [load_layer])
    keep_layer.start()
    arrive(arriving)
    attention.run(
        {
            1: [(reduce.spread, 0)],
            2: [(along.spread,)],
            3: [(reduce.spread, 1), (reduce.spread, 2)],
            4: [(reduce.send, 0), (along.send,)],
            5: [(reduce.send, 1)],
            6: [(reduce.send, 2)],
        },
        back.each,
    )
    for t in range(3):
        reduce.finish(t)
    along.finish()
    back.finish()
    arrive(returned)
    copies.finish()
    keep_layer.wait()


def backward_fused(attended_diff, qkv, saved, layer, grads, slopes, heads, width):
    own, parts, piece, columns = attended_diff.shape
    features = heads * width
    length = parts * 8 * piece
    cut = [split_grad(item) for item in grads]
    count = len(cut)
    rows, wide = cut[0].shape[3:]
    early, part = 5 * wide // 16, 11 * wide // 32
    chunks = [
        (0, 0, rows, 0, early),
        (0, 0, rows, early, part),
        (0, 0, rows, early + part, part),
        *chunks_of(1, *cut[1].shape[3:], 1),
    ]
    out = remote_call(
        functools.partial(backward_fused_kernel, heads, width, count, chunks),
        "backward_fused",
        2,
        out_shape=(
            jax.ShapeDtypeStruct((own, parts, piece, 24 * features), bf16),
            jax.ShapeDtypeStruct((parts, own, piece, columns), bf16),
            *[jax.ShapeDtypeStruct(item.shape[3:], f32) for item in cut],
        ),
        in_specs=[SMEM] + [HBM] * (5 + count),
        out_specs=(HBM, HBM) + (VMEM,) * count,
        scratch_shapes=[
            pltpu.VMEM((own, piece, columns), bf16),
            pltpu.VMEM((own, parts, 8, piece, features), bf16),
            pltpu.VMEM(qkv.shape, bf16),
            *[pltpu.VMEM(item.shape, f32) for item in saved],
            pltpu.VMEM(qkv.shape, bf16),
            *backward_scratch(length, heads, width),
            *reduce_along_scratch(chunks[0]),
            *reduce_scratch(chunks[1:]),
            *hand_back_semaphores(own * parts),
            *semaphores(10 + len(chunks) * Reduce.copies_each, len(chunks) + 6),
        ],
    )(slopes, attended_diff, qkv, *saved, layer, *cut)
    return out[0], out[1].reshape(parts * own, piece, columns), out[2:]


def end_kernel(
    width, joined_diff, joined_weight, tokens_in, residual_in, small, out_bias_grad,
    second_gain_grad, second_shift_grad, contract_bias_grad, expand_bias_grad,
    input_out, vector_out, out,
    tokens, residual_grad, values_of, diff_in, weight_in, normed, normed_t, back, grads, held,
    vectors, others, ranks, *refs,
):
    count = grads.shape[0]
    bufs, refs = refs[: 7 * count], refs[7 * count :]
    loaded, copies = refs[0], Copies(*refs[1:])
    place = Place()
    z, lines, plane = place.z, place.lines, place.plane
    rows, features = tokens.shape
    own_seqs, parts, piece, _ = held.shape
    columns = [pl.ds(features * n, features) for n in range(count)]
    chunks = [(n, 0, grads.shape[4], 0, features) for n in range(count)]
    outs = [out.at[:, where] for where in columns]
    reduce = Reduce(place, [grads.at[n] for n in range(count)], outs, bufs, chunks, copies)
    loads = [
        (
            pltpu.make_async_copy(joined_diff.at[:, c], diff_in.at[:, c], loaded.at[0, n]),
            pltpu.make_async_copy(joined_weight.at[:, c], weight_in.at[:, c], loaded.at[1, n]),
        )
        for n, c in enumerate(columns)
    ]
    returned = [copies.plan(held.at[:, to[0]], input_out.at[z], to) for to in lines]
    stay = copies.inside(held.at[:, z], input_out.at[z])
    along = [copies.plan(vectors.at[to[0]], others.at[k], to) for k, to in enumerate(lines)]
    across = [copies.plan(ranks.at[0], ranks.at[d + 1], to) for d, to in enumerate(plane)]

    given_loads = [copies.inside(tokens_in, tokens), copies.inside(residual_in, residual_grad)]
    for load in loads:
        go(load)
    go(given_loads)
    values_of[...] = small[...].astype(f32)
    gain, shift = row_of(values_of, 0, features), row_of(values_of, 1, features)
    greet(lines + plane)
    for n, where in enumerate(columns):
        done(loads[n])
        part = matmul_rt(diff_in[:, where], weight_in[:, where])
        back[...] = part if n == 0 else back[...] + part

    def norm_back(i, sums):
        at = pl.ds(pl.multiple_of(i * piece, piece), piece)
        values, given = tokens[at, :].astype(f32), back[at, :]
        part, normal = normalize_back(values, given, gain)
        normed[at, :] = (normal * gain + shift).astype(bf16)
        total = (residual_grad[at, :] + part).astype(bf16)
        held[i // parts, i % parts] = total
        found = (given * normal, given)
        return tuple(
            kept + jnp.sum(item, axis=0, keepdims=True) for kept, item in zip(sums, found)
        )

    done(given_loads)
    nothing = jnp.zeros((1, features), f32)
    gain_grad, shift_grad = lax.fori_loop(0, own_seqs * parts, norm_back, (nothing, nothing))
    go(returned + [stay])
    normed_t[...] = normed[...].T
    sums = []
    for n, where in enumerate(columns):
        made = matmul(normed_t[...], diff_in[:, where]).astype(bf16)
        grads[n] = made.reshape(grads.shape[1:])
        reduce.begin(n)
        sums.append(jnp.sum(diff_in[:, where].astype(f32), axis=0, keepdims=True))
        if n > 0:
            reduce.exchange(n - 1)

    sums = jnp.concatenate(sums, axis=1)
    low = lax.broadcasted_iota(jnp.int32, (1, 128), 1) < width
    query_grad, value_grad = [], []
    for r in range(features // 128):
        first, middle, last = [sums[:, (3 * r + n) * 128 : (3 * r + n + 1) * 128] for n in range(3)]
        query_grad.append(jnp.where(low, first, middle))
        value_grad.append(jnp.where(low, middle, last))
    given = [
        gain_grad, shift_grad, jnp.concatenate(query_grad, axis=1),
        jnp.concatenate(value_grad, axis=1), out_bias_grad[...], second_gain_grad[...],
        second_shift_grad[...], contract_bias_grad[...], expand_bias_grad[...],
    ]
    row = 0
    for item in given:
        each = item.shape[1] // 512
        for k in range(4):
            for r in range(each):
                start = (k * each + r) * 128
                vectors[k, row + r : row + r + 1, :] = item[:, start : start + 128]
        row += each
    go(along)
    reduce.spread(0)
    reduce.exchange(count - 1)
    arrive(along)
    total = vectors[z]
    for k in range(3):
        total = total + others[k]
    ranks[0] = total
    go(across)
    for n in range(1, count):
        reduce.send(n - 1)
        reduce.spread(n)
    reduce.send(count - 1)
    arrive(across)
    total = ranks[0]
    for d in range(1, 8):
        total = total + ranks[d]
    vector_out[...] = total
    for n in range(count):
        reduce.finish(n)
    arrive(returned)
    copies.finish()
    stay.wait()


def end(shape, joined_diff, joined_weight, tokens, residual_grad, small, vectors, width):
    own, parts, piece = shape
    rows, features = tokens.shape
    count = joined_diff.shape[1] // features
    each = features // 32
    tall = (4 * features + sum(item.shape[1] for item in vectors)) // 512
    chunks = [(n, 0, each, 0, features) for n in range(count)]
    out = remote_call(
        functools.partial(end_kernel, width),
        "end",
        3,
        out_shape=(
            jax.ShapeDtypeStruct((parts, own, piece, features), bf16),
            jax.ShapeDtypeStruct((tall, 128), f32),
            jax.ShapeDtypeStruct((each, count * features), f32),
        ),
        in_specs=[HBM] * 4 + [VMEM] * (1 + len(vectors)),
        out_specs=(HBM, VMEM, VMEM),
        scratch_shapes=[
            pltpu.VMEM((rows, features), bf16),
            pltpu.VMEM((rows, features), f32),
            pltpu.VMEM(small.shape, f32),
            pltpu.VMEM((rows, count * features), bf16),
            pltpu.VMEM((features, count * features), bf16),
            pltpu.VMEM((rows, features), bf16),
            pltpu.VMEM((features, rows), bf16),
            pltpu.VMEM((rows, features), f32),
            pltpu.VMEM((count, 4, 4, 2, each, features), bf16),
            pltpu.VMEM((own, parts, piece, features), bf16),
            pltpu.VMEM((4, tall, 128), f32),
            pltpu.VMEM((3, tall, 128), f32),
            pltpu.VMEM((8, tall, 128), f32),
            *reduce_scratch(chunks),
            pltpu.SemaphoreType.DMA((2, count)),
            *semaphores(3 + 3 + 7 + count * Reduce.copies_each, 3 + count),
        ],
    )(joined_diff, joined_weight, tokens, residual_grad, small, *vectors)
    return out[0].reshape(parts * own, piece, features), out[1], out[2]


def hand_out_kernel(sizes, vector, *refs):
    count = (len(refs) - len(sizes) - 1) // 3
    arrays, outs, smalls = refs[:count], refs[count : 2 * count], refs[2 * count :]
    smalls, kept, sems = smalls[: len(sizes)], smalls[len(sizes) : -1], refs[-1]
    s = lax.axis_index("sp")
    loads = [pltpu.make_async_copy(a, k, sems.at[n]) for n, (a, k) in enumerate(zip(arrays, kept))]
    stores = [
        pltpu.make_async_copy(k, o, sems.at[count + n]) for n, (k, o) in enumerate(zip(kept, outs))
    ]
    go(loads)
    row = 0
    for out, size in zip(smalls, sizes):
        per = 128 // size
        found = vector[pl.ds(row + s // per, 1), :]
        if per > 1:
            found = pltpu.roll(found, lax.rem(128 - s % per * size, 128), 1)
        out[...] = found[:, :size]
        row += 8 // per
    for load, store in zip(loads, stores):
        load.wait()
        store.start()
    done(stores)


def hand_out(vector, sizes, arrays):
    out = pl.pallas_call(
        functools.partial(hand_out_kernel, sizes),
        name="hand_out",
        out_shape=(
            *[jax.ShapeDtypeStruct(item.shape, item.dtype) for item in arrays],
            *[jax.ShapeDtypeStruct((1, size), f32) for size in sizes],
        ),
        in_specs=[VMEM] + [HBM] * len(arrays),
        out_specs=(HBM,) * len(arrays) + (VMEM,) * len(sizes),
        scratch_shapes=[
            *[pltpu.VMEM(item.shape, item.dtype) for item in arrays],
            pltpu.SemaphoreType.DMA((2 * len(arrays),)),
        ],
        compiler_params=pltpu.CompilerParams(vmem_limit_bytes=vmem_bytes),
    )(vector, *arrays)
    return out[: len(arrays)], [item.reshape(-1) for item in out[len(arrays) :]]


def per_device(
    layer_input,
    first_gain,
    first_shift,
    joined_weight,
    query_bias,
    value_bias,
    output_weight,
    output_bias,
    second_gain,
    second_shift,
    expand_weight,
    expand_bias,
    contract_weight,
    contract_bias,
    alibi_slopes,
    upstream,
):
    seqs, piece, features = layer_input.shape
    fs_count = lax.axis_size("fs")
    sp_count = lax.axis_size("sp")
    head_count = alibi_slopes.shape[0]
    width = features // head_count
    heads = head_count // sp_count
    rows = seqs * piece
    own = seqs // fs_count
    shape = (own, fs_count, piece)

    vectors = (
        first_gain, first_shift, query_bias, value_bias, output_bias,
        second_gain, second_shift, contract_bias, expand_bias,
    )
    fast = (fs_count, sp_count) == (4, 8) and (own, heads, width) == (2, 2, 64)
    fast = fast and expand_weight.shape[1] == 4 * features
    if fast:
        weights = (joined_weight, output_weight, expand_weight)
        tokens, small, weights, qkv, attended, saved, upstream_low = forward_fused(
            layer_input, upstream, vectors, weights, contract_weight, alibi_slopes, heads, width
        )
        joined_full, out_full, expand_full, contract_line = weights
        tokens = tokens.reshape(rows, features)
        (
            layer_output, residual_grad, attended_diff, expand_grad, output_weight_grad,
            contract_grad, eb, g2, s2, ob, cb,
        ) = feed_forward(
            shape, expand_full, contract_weight, contract_line, out_full, tokens,
            upstream_low.reshape(rows, features), attended.reshape(rows, features), small,
        )
        joined_diff, layer_output, grads = backward_fused(
            attended_diff, qkv, saved, layer_output, (expand_grad, output_weight_grad),
            alibi_slopes, heads, width,
        )
        input_grad, vector, joined_grad = end(
            shape, joined_diff.reshape(rows, 3 * features), joined_full, tokens, residual_grad,
            small, (ob, g2, s2, cb, eb), width,
        )
        devices = fs_count * sp_count
        sizes = [4 * item.shape[0] // devices for item in vectors]
        arrays, (g1, s1, qb, vb, ob, g2, s2, cb, eb) = hand_out(
            vector, sizes, (layer_output, input_grad, joined_grad, grads[1], grads[0], contract_grad)
        )
        layer_output, input_grad, joined_grad, output_grad, expand_grad, contract_grad = arrays
        return (
            layer_output, input_grad, g1, s1, joined_grad, qb, vb, output_grad, ob, g2, s2,
            expand_grad, eb, contract_grad, cb,
        )

    slopes = lax.dynamic_slice_in_dim(alibi_slopes, lax.axis_index("sp") * heads, heads)
    gather = lambda item: lax.all_gather(item, "fs", axis=0, tiled=True)
    scatter = functools.partial(
        lax.psum_scatter, axis_name=("fs", "sp"), scatter_dimension=0, tiled=True
    )
    gain_one, shift_one, qbias, vbias, obias, gain_two, shift_two, cbias, ebias = [
        gather(item).astype(f32) for item in vectors
    ]
    joined_full, out_full, expand_full, contract_full = [
        gather(item) for item in (joined_weight, output_weight, expand_weight, contract_weight)
    ]
    tokens = to_own_seqs(layer_input).reshape(rows, features).astype(f32)
    upstream_low = to_own_seqs(upstream).reshape(rows, features)

    normed_f, norm_back_one = jax.vjp(normalize, tokens, gain_one, shift_one)
    normed = normed_f.astype(bf16)
    joined_bias = joined_bias_of(qbias, vbias, head_count)
    joined_all = (matmul(normed, joined_full) + joined_bias).astype(bf16)
    qkv = to_heads(joined_all.reshape(*shape, 3 * features))
    attended, *saved = attention_forward(qkv, slopes, heads, width)
    attended = from_heads(attended).reshape(rows, features)
    upstream_f = upstream_low.astype(f32)
    contract_bias_grad = jnp.sum(upstream_f, axis=0)
    residual = tokens + (matmul(attended, out_full) + obias)
    second_f, norm_back_two = jax.vjp(normalize, residual, gain_two, shift_two)
    second = second_f.astype(bf16)
    expanded = matmul(second, expand_full) + ebias
    activated_f, gelu_back = jax.vjp(gelu_tanh, expanded)
    activated = activated_f.astype(bf16)
    result = residual + (matmul(activated, contract_full) + cbias)
    layer_output = result.astype(bf16).reshape(*shape, features)

    contract_grad = matmul_lt(activated, upstream_low)
    act_grad = matmul_rt(upstream_low, contract_full)
    expand_diff = gelu_back(act_grad)[0].astype(bf16)
    expand_grad = matmul_lt(second, expand_diff)
    expand_bias_grad = jnp.sum(expand_diff.astype(f32), axis=0)
    second_back = matmul_rt(expand_diff, expand_full)
    resid_part, second_gain_grad, second_shift_grad = norm_back_two(second_back)
    residual_grad = upstream_f + resid_part

    branch_diff = residual_grad.astype(bf16)
    output_weight_grad = matmul_lt(attended, branch_diff)
    output_bias_grad = jnp.sum(branch_diff.astype(f32), axis=0)
    attended_diff = matmul_rt(branch_diff, out_full).astype(bf16)
    attended_diff = attended_diff.reshape(*shape, features)
    joined_diff = attention_backward(qkv, to_heads(attended_diff), *saved, slopes, heads, width)
    joined_diff = from_heads(joined_diff).reshape(rows, 3 * features)
    joined_grad = matmul_lt(normed, joined_diff)
    column_sums = jnp.sum(joined_diff.astype(f32), axis=0).reshape(head_count, 3, width)
    query_bias_grad = column_sums[:, 0].reshape(features)
    value_bias_grad = column_sums[:, 2].reshape(features)
    normed_back = matmul_rt(joined_diff, joined_full)
    input_part, first_gain_grad, first_shift_grad = norm_back_one(normed_back)
    input_grad = (residual_grad + input_part).astype(bf16).reshape(*shape, features)

    vector_grads = (
        first_gain_grad, first_shift_grad, query_bias_grad, value_bias_grad,
        output_bias_grad, second_gain_grad, second_shift_grad, contract_bias_grad,
        expand_bias_grad,
    )
    devices = fs_count * sp_count
    packed = jnp.concatenate([item.reshape(devices, -1) for item in vector_grads], axis=1)
    packed = scatter(packed.reshape(-1))
    own_grads, at = [], 0
    for item in vector_grads:
        size = item.shape[0] // devices
        own_grads.append(packed[at : at + size])
        at += size
    g1, s1, qb, vb, ob, g2, s2, cb, eb = own_grads
    return (
        from_own_seqs(layer_output), from_own_seqs(input_grad), g1, s1, scatter(joined_grad), qb,
        vb, scatter(output_weight_grad), ob, g2, s2, scatter(expand_grad), eb,
        scatter(contract_grad), cb,
    )


def solution(mesh):
    tokens = P(None, ("fs", "sp"), None)
    both, both_rows = P(("fs", "sp")), P(("fs", "sp"), None)
    one, one_rows = P("fs"), P("fs", None)
    return jax.shard_map(
        per_device,
        mesh=mesh,
        in_specs=(
            tokens, one, one, one_rows, one, one, one_rows, one, one, one, one_rows, one,
            one_rows, one, P(), tokens,
        ),
        out_specs=(
            tokens, tokens, both, both, both_rows, both, both, both_rows, both, both, both,
            both_rows, both, both_rows, both,
        ),
        check_vma=False,
    )
```

```python
import functools
import math

import jax
import jax.numpy as jnp
from jax import lax
from jax.experimental import pallas as pl
from jax.experimental.pallas import tpu as pltpu
from jax.sharding import PartitionSpec as P

norm_eps = 1e-05
gelu_coef = 0.7978845608028654
masked_value = -1e30
f32 = jnp.float32
bf16 = jnp.bfloat16
MESH = pl.DeviceIdType.MESH
HBM = pl.BlockSpec(memory_space=pl.ANY)
VMEM = pl.BlockSpec(memory_space=pltpu.VMEM)
SMEM = pl.BlockSpec(memory_space=pltpu.SMEM)
vmem_bytes = 63 * 1024 * 1024


def normalize(values, norm_gain, norm_shift):
    center = values - jnp.mean(values, axis=-1, keepdims=True)
    variance = jnp.mean(center * center, axis=-1, keepdims=True)
    return center * lax.rsqrt(variance + norm_eps) * norm_gain + norm_shift


def normalize_back(values, back, norm_gain):
    center = values - jnp.mean(values, axis=-1, keepdims=True)
    inverse = lax.rsqrt(jnp.mean(center * center, axis=-1, keepdims=True) + norm_eps)
    normal = center * inverse
    scaled = back * norm_gain
    even = jnp.mean(scaled, axis=-1, keepdims=True)
    along = jnp.mean(scaled * normal, axis=-1, keepdims=True)
    return inverse * (scaled - even - normal * along), normal


def gelu_tanh(values):
    return (
        0.5 * values * (1.0 + jnp.tanh(gelu_coef * (values + 0.044715 * values * values * values)))
    )


def matmul(left_side, right_side):
    return jnp.dot(left_side, right_side, preferred_element_type=f32)


def matmul_lt(left_side, right_side):
    return lax.dot_general(
        left_side, right_side, (((0,), (0,)), ((), ())), preferred_element_type=f32
    )


def matmul_rt(left_side, right_side):
    return lax.dot_general(
        left_side, right_side, (((1,), (1,)), ((), ())), preferred_element_type=f32
    )


def joined_bias_of(query_bias, value_bias, head_count):
    query_part = query_bias.astype(f32).reshape(head_count, -1)
    value_part = value_bias.astype(f32).reshape(head_count, -1)
    return jnp.stack([query_part, jnp.zeros_like(query_part), value_part], axis=1).reshape(-1)


def split_three(values):
    high = values.astype(bf16).astype(f32)
    rest = values - high
    middle = rest.astype(bf16).astype(f32)
    return high, middle, rest - middle


def key_columns(key_rows, slope, start):
    rows, width = key_rows.shape
    position = (start + lax.broadcasted_iota(jnp.int32, (rows, width), 0)).astype(f32)
    lane = lax.broadcasted_iota(jnp.int32, (rows, width), 1)
    high, middle, low = split_three(slope * position)
    extra = jnp.where(lane == 0, high, jnp.where(lane == 1, middle, jnp.where(lane == 2, low, 0.0)))
    return jnp.concatenate([key_rows.astype(f32), extra], axis=1).astype(bf16)


def query_columns(queries, scale):
    rows, width = queries.shape
    lane = lax.broadcasted_iota(jnp.int32, (rows, width), 1)
    ones = jnp.where(lane < 3, 1.0, 0.0)
    return jnp.concatenate([queries.astype(f32) * scale, ones], axis=1).astype(bf16)


def follow(n, after):
    for at, steps in after.items():

        def act(steps=steps):
            for step, *given in steps:
                step(*given)

        pl.when(n == at)(act)


class Forward:
    def __init__(self, heads, width, slopes, qkv, out, out_t, lse, keys, queries, values_t):
        self.heads, self.width, self.slopes, self.qkv, self.out = heads, width, slopes, qkv, out
        self.out_t, self.lse = out_t, lse
        self.keys, self.queries, self.values_t = keys, queries, values_t
        self.head = 0
        self.blocks = qkv.shape[1]
        self.block = qkv.shape[2] * qkv.shape[3]

    def rows(self, i):
        return pl.ds(pl.multiple_of(i * self.block, self.block), self.block)

    def prepare(self, b):
        width, block, qkv = self.width, self.block, self.qkv
        scale = 1.0 / math.sqrt(width)

        def body(i, _):
            rows = self.rows(i)
            for h in range(self.heads):
                base = h * 3 * width
                query, key, value = [
                    qkv[b, i, :, :, base + n * width : base + (n + 1) * width].reshape(block, width)
                    for n in range(3)
                ]
                self.keys[h, rows, :] = key_columns(key, self.slopes[self.head + h], i * block)
                self.queries[h, rows, :] = query_columns(query, scale)
                self.values_t[h, :, rows] = value.astype(f32).T.astype(bf16)
            return 0

        lax.fori_loop(0, self.blocks, body, 0)

    def one(self, b, i):
        heads, width, block = self.heads, self.width, self.block
        rows = self.rows(i)
        query = [self.queries[h, rows, :] for h in range(heads)]

        def step(j, state, diagonal):
            columns = self.rows(j)
            result = []
            for h in range(heads):
                top, total, acc = state[h]
                scores = matmul_rt(self.keys[h, columns, :], query[h])
                if diagonal:
                    key_at = lax.broadcasted_iota(jnp.int32, (block, block), 0)
                    query_at = lax.broadcasted_iota(jnp.int32, (block, block), 1)
                    scores = jnp.where(key_at <= query_at, scores, masked_value)
                newest = jnp.maximum(top, jnp.max(scores, axis=0, keepdims=True))
                shrink = jnp.exp(top - newest)
                probs = jnp.exp(scores - newest)
                total = total * shrink + jnp.sum(probs, axis=0, keepdims=True)
                acc = acc * shrink + matmul(self.values_t[h, :, columns], probs.astype(bf16))
                result.append((newest, total, acc))
            return tuple(result)

        state = tuple(
            (
                jnp.full((1, block), masked_value, f32),
                jnp.zeros((1, block), f32),
                jnp.zeros((width, block), f32),
            )
            for h in range(heads)
        )
        state = lax.fori_loop(0, i, lambda j, s: step(j, s, False), state)
        state = step(i, state, True)
        finished = []
        for h in range(heads):
            top, total, acc = state[h]
            result = acc / total
            self.out_t[b, h, :, rows] = result
            self.lse[b, h, :, rows] = top + jnp.log(total)
            finished.append(result)
        joined = finished[0] if heads == 1 else jnp.concatenate(finished, axis=0)
        self.out[b, i] = joined.T.astype(bf16).reshape(self.out.shape[2:])

    def run(self, after, each=None):
        blocks = self.blocks

        def body(n, _):
            b, i = n // blocks, n % blocks
            pl.when(i == 0)(lambda: self.prepare(b))
            self.one(b, i)
            if each is not None:
                each(b, i)
            follow(n, after)
            return 0

        lax.fori_loop(0, self.qkv.shape[0] * blocks, body, 0)


def forward_kernel(heads, width, *refs):
    Forward(heads, width, *refs).run({})


def saved_shapes(seqs, length, heads, width):
    return (
        jax.ShapeDtypeStruct((seqs, heads, width, length), f32),
        jax.ShapeDtypeStruct((seqs, heads, 1, length), f32),
    )


def forward_scratch(length, heads, width):
    return [
        pltpu.VMEM((heads, length, 2 * width), bf16),
        pltpu.VMEM((heads, length, 2 * width), bf16),
        pltpu.VMEM((heads, width, length), bf16),
    ]


def attention_forward(qkv, slopes, heads, width):
    seqs, blocks, ranks, piece, _ = qkv.shape
    length = blocks * ranks * piece
    return pl.pallas_call(
        functools.partial(forward_kernel, heads, width),
        name="attention_forward",
        out_shape=(
            jax.ShapeDtypeStruct((seqs, blocks, ranks, piece, heads * width), bf16),
            *saved_shapes(seqs, length, heads, width),
        ),
        in_specs=[SMEM, VMEM],
        out_specs=(VMEM, VMEM, VMEM),
        scratch_shapes=forward_scratch(length, heads, width),
        compiler_params=pltpu.CompilerParams(vmem_limit_bytes=vmem_bytes),
    )(slopes, qkv)


class Backward:
    def __init__(
        self, heads, width, slopes, qkv, diff, out_t, lse, joined,
        keys, queries, keys_t, values, diffs, delta, query_acc,
    ):
        self.heads, self.width, self.slopes, self.qkv, self.diff = heads, width, slopes, qkv, diff
        self.out_t, self.lse, self.joined = out_t, lse, joined
        self.keys, self.queries, self.keys_t, self.values = keys, queries, keys_t, values
        self.diffs, self.delta, self.query_acc = diffs, delta, query_acc
        self.head = 0
        self.blocks = qkv.shape[1]
        self.block = qkv.shape[2] * qkv.shape[3]

    def rows(self, i):
        return pl.ds(pl.multiple_of(i * self.block, self.block), self.block)

    def prepare(self, b):
        width, block, qkv = self.width, self.block, self.qkv
        scale = 1.0 / math.sqrt(width)

        def body(i, _):
            rows = self.rows(i)
            for h in range(self.heads):
                base = h * 3 * width
                query, key, value = [
                    qkv[b, i, :, :, base + n * width : base + (n + 1) * width].reshape(block, width)
                    for n in range(3)
                ]
                self.keys[h, rows, :] = key_columns(key, self.slopes[self.head + h], i * block)
                self.keys_t[h, :, rows] = key.astype(f32).T.astype(bf16)
                self.queries[h, rows, :] = query_columns(query, scale)
                self.values[h, rows, :] = value
                part = self.diff[b, i, :, :, h * width : (h + 1) * width].reshape(block, width)
                self.diffs[h, rows, :] = part
                self.delta[h, :, rows] = jnp.sum(
                    part.astype(f32).T * self.out_t[b, h, :, rows], axis=0, keepdims=True
                )
                self.query_acc[h, :, rows] = jnp.zeros((width, block), f32)
            return 0

        lax.fori_loop(0, self.blocks, body, 0)

    def one(self, b, j):
        heads, width, block = self.heads, self.width, self.block
        tail = self.joined.shape[2:4] + (width,)
        columns = self.rows(j)

        def step(i, state, diagonal):
            rows = self.rows(i)
            result = []
            for h in range(heads):
                key_acc, value_acc = state[h]
                query = self.queries[h, rows, :]
                part = self.diffs[h, rows, :]
                scores = matmul_rt(self.keys[h, columns, :], query)
                probs = jnp.exp(scores - self.lse[b, h, :, rows])
                if diagonal:
                    key_at = lax.broadcasted_iota(jnp.int32, (block, block), 0)
                    query_at = lax.broadcasted_iota(jnp.int32, (block, block), 1)
                    probs = jnp.where(key_at <= query_at, probs, 0.0)
                prob_diff = matmul_rt(self.values[h, columns, :], part)
                score_diff = (probs * (prob_diff - self.delta[h, :, rows])).astype(bf16)
                value_acc = value_acc + matmul(probs.astype(bf16), part)
                key_acc = key_acc + matmul(score_diff, query)
                self.query_acc[h, :, rows] += matmul(self.keys_t[h, :, columns], score_diff)
                result.append((key_acc, value_acc))
            return tuple(result)

        state = tuple(
            (jnp.zeros((block, 2 * width), f32), jnp.zeros((block, width), f32))
            for h in range(heads)
        )
        state = step(j, state, True)
        state = lax.fori_loop(j + 1, self.blocks, lambda i, s: step(i, s, False), state)
        for h in range(heads):
            base = (h * 3 + 1) * width
            key_acc, value_acc = state[h]
            self.joined[b, j, :, :, base : base + width] = (
                key_acc[:, :width].astype(bf16).reshape(tail)
            )
            self.joined[b, j, :, :, base + width : base + 2 * width] = value_acc.astype(
                bf16
            ).reshape(tail)

    def run(self, after, each=None):
        blocks = self.blocks

        def body(n, _):
            b, j = n // blocks, n % blocks
            pl.when(j == 0)(lambda: self.prepare(b))
            self.one(b, j)
            self.finish(b, j)
            if each is not None:
                each(b, j)
            follow(n, after)
            return 0

        lax.fori_loop(0, self.qkv.shape[0] * blocks, body, 0)

    def finish(self, b, j):
        width = self.width
        scale = 1.0 / math.sqrt(width)
        for h in range(self.heads):
            base = h * 3 * width
            result = (self.query_acc[h, :, self.rows(j)] * scale).T.astype(bf16)
            self.joined[b, j, :, :, base : base + width] = result.reshape(
                self.joined.shape[2:4] + (width,)
            )


def backward_kernel(heads, width, *refs):
    Backward(heads, width, *refs).run({})


def backward_scratch(length, heads, width):
    return [
        pltpu.VMEM((heads, length, 2 * width), bf16),
        pltpu.VMEM((heads, length, 2 * width), bf16),
        pltpu.VMEM((heads, width, length), bf16),
        pltpu.VMEM((heads, length, width), bf16),
        pltpu.VMEM((heads, length, width), bf16),
        pltpu.VMEM((heads, 1, length), f32),
        pltpu.VMEM((heads, width, length), f32),
    ]


def attention_backward(qkv, diff, out_t, lse, slopes, heads, width):
    length = qkv.shape[1] * qkv.shape[2] * qkv.shape[3]
    return pl.pallas_call(
        functools.partial(backward_kernel, heads, width),
        name="attention_backward",
        out_shape=jax.ShapeDtypeStruct(qkv.shape, bf16),
        in_specs=[SMEM, VMEM, VMEM, VMEM, VMEM],
        out_specs=VMEM,
        scratch_shapes=backward_scratch(length, heads, width),
        compiler_params=pltpu.CompilerParams(vmem_limit_bytes=vmem_bytes),
    )(slopes, qkv, diff, out_t, lse)


def to_own_seqs(values):
    seqs, piece, features = values.shape
    parts = lax.axis_size("fs")
    values = values.reshape(parts, seqs // parts, piece, features)
    return lax.all_to_all(values, "fs", split_axis=0, concat_axis=0).transpose(1, 0, 2, 3)


def from_own_seqs(values):
    own, parts, piece, features = values.shape
    values = lax.all_to_all(values.transpose(1, 0, 2, 3), "fs", split_axis=0, concat_axis=0)
    return values.reshape(parts * own, piece, features)


def to_heads(values):
    own, parts, piece, features = values.shape
    ranks = lax.axis_size("sp")
    values = values.reshape(own, parts, piece, ranks, features // ranks)
    return lax.all_to_all(values, "sp", split_axis=3, concat_axis=2)


def from_heads(values):
    own, parts, ranks, piece, features = values.shape
    values = lax.all_to_all(values, "sp", split_axis=2, concat_axis=3)
    return values.reshape(own, parts, piece, ranks * features)


class Copies:
    def __init__(self, send, recv, local):
        self.send, self.recv, self.local = send, recv, local
        self.used, self.used_local, self.made, self.partial = 0, 0, [], []

    def plan(self, source, target, device, at=None, only=None):
        send, recv = (self.used, self.used) if at is None else at
        copy = pltpu.make_async_remote_copy(
            src_ref=source,
            dst_ref=target,
            send_sem=self.send.at[send],
            recv_sem=self.recv.at[recv],
            device_id=device,
            device_id_type=MESH,
        )
        if at is None:
            self.used += 1
        if only is None:
            self.made.append(copy)
        else:
            self.partial.append((only, copy))
        return copy

    def take(self, count):
        self.used += count
        return range(self.used - count, self.used)

    def inside(self, source, target):
        copy = pltpu.make_async_copy(source, target, self.local.at[self.used_local])
        self.used_local += 1
        return copy

    def finish(self):
        assert (self.used, self.used_local) == (self.send.shape[0], self.local.shape[0])
        for copy in self.made:
            copy.wait_send()
        for only, copy in self.partial:
            pl.when(only)(copy.wait_send)


def go(copies):
    for copy in copies:
        copy.start()


def arrive(copies):
    for copy in copies:
        copy.wait_recv()


def done(copies):
    for copy in copies:
        copy.wait()


def greet(devices):
    barrier = pltpu.get_barrier_semaphore()
    for device in devices:
        pl.semaphore_signal(barrier, inc=1, device_id=device, device_id_type=MESH)
    pl.semaphore_wait(barrier, len(devices))


def paired(z, mask):
    return 2 * ((z // 2 + mask // 2) % 2) + (z + mask) % 2


class Place:
    def __init__(self):
        z, s = lax.axis_index("fs"), lax.axis_index("sp")
        self.z, self.s = z, s
        self.core, self.chip = s % 2, s // 2
        self.x, self.y = self.chip % 2, self.chip // 2
        self.along_x = s + 2 - 4 * self.x
        self.along_y = s + 4 - 8 * self.y
        self.partner = s + 1 - 2 * self.core
        self.diagonal = self.along_x + self.along_y - s
        self.chip_x, self.chip_y = self.along_x // 2, self.along_y // 2
        self.lines = [(paired(z, 3 - k), s) for k in range(3)]
        self.plane = [(z, lax.rem(s + d, 8)) for d in range(1, 8)]
        self.to_x, self.to_y, self.to_core = [
            (z, to) for to in (self.along_x, self.along_y, self.partner)
        ]
        self.beside = z + 1 - 2 * (z % 2)
        self.inner = ((z + 1) // 2) % 2
        self.other_inner, self.other_outer = 2 - z // 2, 3 * (1 - z // 2)
        self.near = self.lines + [self.to_x, self.to_y, self.to_core]


class Gather:
    copies_each = 33

    def __init__(self, place, weights, wholes, kept, chunks, copies, given=None, relayed=()):
        z, s, lines = place.z, place.s, place.lines
        self.is_given = given is not None
        self.inner, self.passed = place.inner == 1, {}
        self.loads, self.own = [], []
        for weight, whole, keep in zip(weights, wholes, kept):
            if keep is None:
                self.loads.append(copies.inside(weight, whole.at[z]))
            else:
                self.loads.append(copies.inside(weight, keep))
                self.own.append(copies.inside(keep, whole.at[z]))
        self.first, self.second, self.third, self.cores, self.last = [], [], [], [], []
        for t, row, rows, column, columns in chunks:
            whole = wholes[t]
            wide = pl.ds(column, columns)
            every = pl.ds(row, rows)
            low, high = pl.ds(row, rows // 2), pl.ds(row + rows // 2, rows // 2)

            def same(k, rank, part, to):
                where = (k, rank, part, wide)
                return copies.plan(whole.at[where], whole.at[where], to)

            number = len(self.first)
            if number in relayed:
                near, middle, far, second = copies.take(4)
                part = (s, every, wide)
                beside = (place.beside, s)
                first = [
                    copies.plan(
                        weights[t].at[part], whole.at[(z, *part)], beside, at=(near, near)
                    ),
                    copies.plan(
                        weights[t].at[part],
                        whole.at[(z, *part)],
                        (place.other_inner, s),
                        at=(second, middle + 1 - place.inner),
                    ),
                ]
                self.passed[number] = [
                    copies.plan(
                        whole.at[(k, *part)], whole.at[(k, *part)], beside, at=(n, n),
                        only=self.inner,
                    )
                    for k, n in ((place.other_inner, middle), (place.other_outer, far))
                ]
            elif given is None:
                first = [
                    copies.plan(weights[t].at[s, every, wide], whole.at[z, s, every, wide], to)
                    for to in lines
                ]
            else:
                first = [
                    copies.inside(given.at[k, every, wide], whole.at[k, s, every, wide])
                    for k, _ in lines
                ]
            self.first.append(first)
            second, third, cores, last = [], [], [], []
            for k, _ in lines:
                second.append(same(k, s, low, place.to_x))
                second.append(same(k, s, high, place.to_y))
                cores.append(same(k, s, every, place.to_core))
                third.append(same(k, s, low, place.to_y))
                third.append(same(k, s, high, place.to_x))
                third.append(same(k, place.along_x, low, place.to_y))
                third.append(same(k, place.along_y, high, place.to_x))
                for rank in (place.along_x, place.along_y, place.diagonal):
                    last.append(same(k, rank, every, place.to_core))
            self.second.append(second)
            self.third.append(third)
            self.cores.append(cores)
            self.last.append(last)

    def keep(self):
        done(self.loads)
        go(self.own)

    def start(self, t):
        go(self.first[t])

    def pass_on(self, t):
        def act():
            for copy in self.passed[t]:
                copy.wait_recv()
                copy.start()

        pl.when(self.inner)(act)

    def exchange(self, t):
        if t in self.passed:
            arrive(self.first[t][:1])
            pl.when(jnp.logical_not(self.inner))(lambda: arrive(self.passed[t]))
        elif self.is_given:
            done(self.first[t])
        else:
            arrive(self.first[t])
        go(self.second[t])
        go(self.cores[t])

    def spread(self, t):
        arrive(self.second[t])
        go(self.third[t])

    def share(self, t):
        arrive(self.third[t])
        go(self.last[t])

    def complete(self, t):
        arrive(self.cores[t] + self.last[t])


def add_into(target, other):
    target[...] = (target[...].astype(f32) + other[...].astype(f32)).astype(target.dtype)


def add_blocks(steps, block_of):
    def body(i, _):
        add_into(*block_of(i))
        return 0

    lax.fori_loop(0, steps, body, 0)


class Reduce:
    copies_each = 10

    def __init__(self, place, grads, outs, bufs, chunks, copies):
        self.place, self.outs, self.chunks = place, outs, chunks
        self.bufs = [bufs[7 * t : 7 * t + 7] for t in range(len(chunks))]
        self.loads, self.first, self.second, self.third, self.fourth = [], [], [], [], []
        for (t, row, rows, column, columns), buf in zip(chunks, self.bufs):
            own, from_core, from_x, from_y, late_y, late_x, from_z = buf
            every, wide = pl.ds(row, rows), pl.ds(column, columns)
            low, high = pl.ds(0, rows // 2), pl.ds(rows // 2, rows // 2)
            self.loads.append(
                copies.inside(grads[t].at[:, :, place.core, every, wide], own)
            )
            self.first.append(
                copies.plan(
                    grads[t].at[:, :, 1 - place.core, every, wide], from_core, place.to_core
                )
            )
            step = []
            for k in range(2):
                step.append(
                    copies.plan(own.at[:, 2 * k + 1 - place.x, low], from_x.at[:, k], place.to_x)
                )
                step.append(
                    copies.plan(
                        own.at[:, 2 * (1 - place.y) + k, high], from_y.at[:, k], place.to_y
                    )
                )
            self.second.append(step)
            self.third.append(
                [
                    copies.plan(own.at[:, place.chip_y, low], late_y, place.to_y),
                    copies.plan(own.at[:, place.chip_x, high], late_x, place.to_x),
                ]
            )
            self.fourth.append(
                [
                    copies.plan(own.at[to[0], place.chip], from_z.at[k], to)
                    for k, to in enumerate(place.lines)
                ]
            )

    def start(self):
        go(self.first)

    def begin(self, t):
        go([self.loads[t], self.first[t]])

    def halves(self, t):
        half = self.chunks[t][2] // 2
        return pl.ds(0, half), pl.ds(half, half)

    def exchange(self, t):
        own, from_core = self.bufs[t][:2]
        self.loads[t].wait()
        arrive([self.first[t]])
        add_blocks(16, lambda i: (own.at[i // 4, i % 4], from_core.at[i // 4, i % 4]))
        go(self.second[t])

    def spread(self, t):
        own, _, from_x, from_y = self.bufs[t][:4]
        low, high = self.halves(t)
        x, y = self.place.x, self.place.y
        arrive(self.second[t])
        add_blocks(8, lambda i: (own.at[i // 2, 2 * (i % 2) + x, low], from_x.at[i // 2, i % 2]))
        add_blocks(8, lambda i: (own.at[i // 2, 2 * y + i % 2, high], from_y.at[i // 2, i % 2]))
        go(self.third[t])

    def send(self, t):
        own, _, _, _, late_y, late_x, _ = self.bufs[t]
        low, high = self.halves(t)
        chip = self.place.chip
        arrive(self.third[t])
        add_blocks(4, lambda i: (own.at[i, chip, low], late_y.at[i]))
        add_blocks(4, lambda i: (own.at[i, chip, high], late_x.at[i]))
        go(self.fourth[t])

    def finish(self, t):
        own, from_z = self.bufs[t][0], self.bufs[t][6]
        index, row, rows, column, columns = self.chunks[t]
        arrive(self.fourth[t])
        total = own[self.place.z, self.place.chip].astype(f32)
        for k in range(3):
            total = total + from_z[k].astype(f32)
        self.outs[index][row : row + rows, column : column + columns] = total


def reduce_scratch(chunks):
    scratch = []
    for _, _, rows, _, columns in chunks:
        half = rows // 2
        scratch += [
            pltpu.VMEM((4, 4, rows, columns), bf16),
            pltpu.VMEM((4, 4, rows, columns), bf16),
            pltpu.VMEM((4, 2, half, columns), bf16),
            pltpu.VMEM((4, 2, half, columns), bf16),
            pltpu.VMEM((4, half, columns), bf16),
            pltpu.VMEM((4, half, columns), bf16),
            pltpu.VMEM((3, rows, columns), bf16),
        ]
    return scratch


class ReduceAlong(Reduce):
    def __init__(self, place, grad, out, buf, chunk, copies):
        self.place, self.grad, self.out, self.buf, self.chunk = place, grad, out, buf, chunk
        own, from_core, from_z, from_x, from_y, late_y, late_x = buf
        _, row, rows, column, columns = chunk
        every, wide = pl.ds(row, rows), pl.ds(column, columns)
        self.low, self.high = low, high = pl.ds(0, rows // 2), pl.ds(rows // 2, rows // 2)
        z, x, y = place.z, place.x, place.y
        self.load = copies.inside(grad.at[:, :, place.core, every, wide], own)
        self.first = copies.plan(
            grad.at[:, :, 1 - place.core, every, wide], from_core, place.to_core
        )
        self.second = [
            copies.plan(own.at[to[0]], from_z.at[k], to) for k, to in enumerate(place.lines)
        ]
        self.third = []
        for k in range(2):
            self.third.append(
                copies.plan(own.at[z, 2 * k + 1 - x, low], from_x.at[k], place.to_x)
            )
            self.third.append(
                copies.plan(own.at[z, 2 * (1 - y) + k, high], from_y.at[k], place.to_y)
            )
        self.fourth = [
            copies.plan(own.at[z, place.chip_y, low], late_y, place.to_y),
            copies.plan(own.at[z, place.chip_x, high], late_x, place.to_x),
        ]

    def exchange(self):
        own, from_core = self.buf[:2]
        self.load.wait()
        arrive([self.first])
        add_blocks(16, lambda i: (own.at[i // 4, i % 4], from_core.at[i // 4, i % 4]))
        go(self.second)

    def spread(self):
        own, _, from_z = self.buf[:3]
        z = self.place.z
        arrive(self.second)

        def body(i, _):
            total = own[z, i].astype(f32)
            for k in range(3):
                total = total + from_z[k, i].astype(f32)
            own[z, i] = total.astype(bf16)
            return 0

        lax.fori_loop(0, 4, body, 0)
        go(self.third)

    def send(self):
        own, _, _, from_x, from_y = self.buf[:5]
        z, x, y = self.place.z, self.place.x, self.place.y
        arrive(self.third)
        add_blocks(2, lambda j: (own.at[z, 2 * j + x, self.low], from_x.at[j]))
        add_blocks(2, lambda j: (own.at[z, 2 * y + j, self.high], from_y.at[j]))
        go(self.fourth)

    def finish(self):
        own, late_y, late_x = self.buf[0], self.buf[5], self.buf[6]
        z, chip = self.place.z, self.place.chip
        _, row, rows, column, columns = self.chunk
        arrive(self.fourth)
        half = rows // 2
        wide = slice(column, column + columns)
        self.out[row : row + half, wide] = own[z, chip, self.low].astype(f32) + late_y[...].astype(
            f32
        )
        self.out[row + half : row + rows, wide] = own[z, chip, self.high].astype(f32) + late_x[
            ...
        ].astype(f32)


def reduce_along_scratch(chunk):
    _, _, rows, _, columns = chunk
    half = rows // 2
    return [
        pltpu.VMEM((4, 4, rows, columns), bf16),
        pltpu.VMEM((4, 4, rows, columns), bf16),
        pltpu.VMEM((3, 4, rows, columns), bf16),
        pltpu.VMEM((2, half, columns), bf16),
        pltpu.VMEM((2, half, columns), bf16),
        pltpu.VMEM((half, columns), bf16),
        pltpu.VMEM((half, columns), bf16),
    ]


class HandBack:
    def __init__(self, place, source, target, features, send, recv, local):
        self.place, self.source, self.target = place, source, target
        self.mine = columns_of(place.s, features)
        self.send, self.recv, self.local = send, recv, local
        self.blocks = source.shape[1]

    def copy(self, b, i, d):
        rank = self.place.plane[d][1]
        n = b * self.blocks + i
        return pltpu.make_async_remote_copy(
            src_ref=self.source.at[b, i, rank],
            dst_ref=self.target.at[b, i, :, self.mine],
            send_sem=self.send.at[n, d],
            recv_sem=self.recv.at[n, d],
            device_id=self.place.plane[d],
            device_id_type=MESH,
        )

    def own(self, b, i):
        return pltpu.make_async_copy(
            self.source.at[b, i, self.place.s],
            self.target.at[b, i, :, self.mine],
            self.local.at[b * self.blocks + i],
        )

    def each(self, b, i):
        for d in range(7):
            self.copy(b, i, d).start()
        self.own(b, i).start()

    def finish(self):
        def body(n, _):
            b, i = n // self.blocks, n % self.blocks
            for d in range(7):
                self.copy(b, i, d).wait()
            self.own(b, i).wait()
            return 0

        lax.fori_loop(0, self.source.shape[0] * self.blocks, body, 0)


def hand_back_semaphores(steps):
    return [
        pltpu.SemaphoreType.DMA((steps, 7)),
        pltpu.SemaphoreType.DMA((steps, 7)),
        pltpu.SemaphoreType.DMA((steps,)),
    ]


class ReduceLines:
    copies = 4 * 7 + 3 + 3 + 6

    def __init__(self, place, grad, out, bufs, copies):
        self.place, self.grad, self.out, self.bufs = place, grad, out, bufs
        from_core, from_x, from_y, late_y, late_x, from_z = bufs[:6]
        early_z, own_x, own_y, own_late_y, own_late_x = bufs[6:]
        core, x, y = place.core, place.x, place.y
        self.order = [to[0] for to in place.lines] + [place.z]
        rows = grad.shape[3]
        low, high = pl.ds(0, rows // 2), pl.ds(rows // 2, rows // 2)
        cut = from_z.shape[2]
        most, rest = pl.ds(0, cut), pl.ds(cut, grad.shape[4] - cut)
        self.low, self.high, self.all = (low, most), (high, most), (pl.ds(0, rows), most)
        self.low_rest, self.high_rest = (low, rest), (high, rest)
        self.all_rest = (pl.ds(0, rows), rest)
        z = place.z
        self.early = [
            copies.plan(grad.at[(to[0], pl.ds(0, 4), core, *self.all_rest)], early_z.at[k], to)
            for k, to in enumerate(place.lines)
        ]
        self.own_second, self.own_third = [], []
        for j in range(2):
            self.own_second.append(
                copies.plan(
                    grad.at[(z, 2 * j + 1 - x, core, *self.low_rest)], own_x.at[j], place.to_x
                )
            )
            self.own_second.append(
                copies.plan(
                    grad.at[(z, 2 * (1 - y) + j, core, *self.high_rest)], own_y.at[j], place.to_y
                )
            )
        self.own_third = [
            copies.plan(
                grad.at[(z, place.chip_y, core, *self.low_rest)], own_late_y, place.to_y
            ),
            copies.plan(
                grad.at[(z, place.chip_x, core, *self.high_rest)], own_late_x, place.to_x
            ),
        ]
        self.first, self.second, self.third, self.fourth = [], [], [], []
        for k, at in enumerate(self.order):
            self.first.append(
                copies.plan(grad.at[at, :, 1 - core], from_core.at[k], place.to_core)
            )
            step = []
            for j in range(2):
                step.append(
                    copies.plan(
                        grad.at[(at, 2 * j + 1 - x, core, *self.low)], from_x.at[k, j], place.to_x
                    )
                )
                step.append(
                    copies.plan(
                        grad.at[(at, 2 * (1 - y) + j, core, *self.high)], from_y.at[k, j], place.to_y
                    )
                )
            self.second.append(step)
            self.third.append(
                [
                    copies.plan(
                        grad.at[(at, place.chip_y, core, *self.low)], late_y.at[k], place.to_y
                    ),
                    copies.plan(
                        grad.at[(at, place.chip_x, core, *self.high)], late_x.at[k], place.to_x
                    ),
                ]
            )
            if k < 3:
                self.fourth.append(
                    copies.plan(
                        grad.at[(at, place.chip, core, *self.all)], from_z.at[k], place.lines[k]
                    )
                )

    def start(self, k):
        go([self.first[k]])

    def exchange(self, k):
        arrive([self.first[k]])
        at, core = self.order[k], self.place.core
        add_blocks(4, lambda i: (self.grad.at[at, i, core], self.bufs[0].at[k, i]))
        go(self.second[k] + self.early[k : k + 1])

    def spread(self, k):
        arrive(self.second[k])
        at, core, x, y = self.order[k], self.place.core, self.place.x, self.place.y
        add_blocks(
            2, lambda j: (self.grad.at[(at, 2 * j + x, core, *self.low)], self.bufs[1].at[k, j])
        )
        add_blocks(
            2, lambda j: (self.grad.at[(at, 2 * y + j, core, *self.high)], self.bufs[2].at[k, j])
        )
        go(self.third[k])

    def send(self, k):
        arrive(self.third[k])
        at, core, chip = self.order[k], self.place.core, self.place.chip
        add_into(self.grad.at[(at, chip, core, *self.low)], self.bufs[3].at[k])
        add_into(self.grad.at[(at, chip, core, *self.high)], self.bufs[4].at[k])
        go(self.fourth[k : k + 1])

    def own_spread(self):
        arrive(self.early)
        z, core = self.place.z, self.place.core

        def body(i, _):
            target = self.grad.at[(z, i, core, *self.all_rest)]
            total = target[...].astype(f32)
            for k in range(3):
                total = total + self.bufs[6][k, i].astype(f32)
            target[...] = total.astype(bf16)
            return 0

        lax.fori_loop(0, 4, body, 0)
        go(self.own_second)

    def own_send(self):
        arrive(self.own_second)
        z, core, x, y = self.place.z, self.place.core, self.place.x, self.place.y
        for j in range(2):
            add_into(self.grad.at[(z, 2 * j + x, core, *self.low_rest)], self.bufs[7].at[j])
            add_into(self.grad.at[(z, 2 * y + j, core, *self.high_rest)], self.bufs[8].at[j])
        go(self.own_third)

    def finish(self):
        arrive(self.fourth + self.own_third)
        place = self.place
        at = (place.z, place.chip, place.core)
        total = self.grad[(*at, *self.all)].astype(f32)
        for k in range(3):
            total = total + self.bufs[5][k].astype(f32)
        cut = total.shape[1]
        half = total.shape[0] // 2
        self.out[:, :cut] = total
        self.out[:half, cut:] = self.grad[(*at, *self.low_rest)].astype(f32) + self.bufs[9][
            ...
        ].astype(f32)
        self.out[half:, cut:] = self.grad[(*at, *self.high_rest)].astype(f32) + self.bufs[10][
            ...
        ].astype(f32)


def reduce_lines_scratch(rows, columns, rest):
    half = rows // 2
    most = columns - rest
    return [
        pltpu.VMEM((4, 4, rows, columns), bf16),
        pltpu.VMEM((4, 2, half, most), bf16),
        pltpu.VMEM((4, 2, half, most), bf16),
        pltpu.VMEM((4, half, most), bf16),
        pltpu.VMEM((4, half, most), bf16),
        pltpu.VMEM((3, rows, most), bf16),
        pltpu.VMEM((3, 4, rows, rest), bf16),
        pltpu.VMEM((2, half, rest), bf16),
        pltpu.VMEM((2, half, rest), bf16),
        pltpu.VMEM((half, rest), bf16),
        pltpu.VMEM((half, rest), bf16),
    ]


def split_grad(item):
    return item.reshape(4, 4, 2, item.shape[0] // 32, item.shape[1])


def split_weight(item):
    return item.reshape(8, item.shape[0] // 8, item.shape[1])


def chunks_of(index, rows, columns, count):
    if rows >= 64:
        return [(index, rows // count * n, rows // count, 0, columns) for n in range(count)]
    return [(index, 0, rows, columns // count * n, columns // count) for n in range(count)]


def semaphores(remote, local):
    return [pltpu.SemaphoreType.DMA((n,)) for n in (remote, remote, local)]


def remote_call(kernel, name, collective, **options):
    return pl.pallas_call(
        kernel,
        name=name,
        compiler_params=pltpu.CompilerParams(
            collective_id=collective, has_side_effects=True, vmem_limit_bytes=vmem_bytes
        ),
        **options,
    )


def row_of(packed, n, size):
    found = [packed[k, n, r : r + 1, :] for k in range(4) for r in range(size // 512)]
    return jnp.concatenate(found, axis=1)


def columns_of(rank, features):
    return pl.ds(pl.multiple_of(rank * features, 128), features)


def forward_fused_kernel(heads, width, count, vector_count, chunks, slopes, tokens, upstream, *refs):
    vectors, refs = refs[:vector_count], refs[vector_count:]
    weights, contract, refs = refs[:count], refs[count], refs[count + 1 :]
    tokens_out, vectors_out, joined_out, qkv_out, attended, *saved, upstream_out = refs[:8]
    contract_out = refs[8]
    wholes, refs = refs[9 : 8 + count], refs[8 + count :]
    held, small, values_of, joined, normed, outgoing, qkv, result, upstream_own = refs[:9]
    attention = Forward(heads, width, slopes, qkv, result, *refs[9:14])
    kept, refs = refs[14 : 13 + count], refs[13 + count :]
    head_send, head_recv = refs[:2]
    copies = Copies(*refs[5:])
    place = Place()
    z, s, lines, plane = place.z, place.s, place.lines, place.plane
    attention.head = s * heads
    first = [t for t, chunk in enumerate(chunks) if chunk[0] == 0]
    gather = Gather(
        place, weights, [joined, *wholes], [None, *kept], chunks, copies, relayed=first
    )
    later = [t for t, chunk in enumerate(chunks) if chunk[0] > 0]
    features = heads * width
    back = HandBack(place, result, attended, features, *refs[2:5])
    own_seqs, parts, piece, wide = held.shape

    load = copies.inside(tokens.at[z], held.at[:, z])
    load_upstream = copies.inside(upstream.at[z], upstream_own)
    seqs = [copies.plan(tokens.at[to[0]], held.at[:, z], to) for to in lines]
    vector_copies = [copies.plan(small.at[z], small.at[z], to) for to in lines]
    upstreams = [copies.plan(upstream.at[to[0]], upstream_out.at[:, z], to) for to in lines]
    keep_upstream = copies.inside(upstream_own, upstream_out.at[:, z])
    keeping = [
        copies.inside(held, tokens_out),
        copies.inside(small, vectors_out),
        copies.inside(joined, joined_out),
    ]
    keep_qkv = copies.inside(qkv, qkv_out)
    keep_saved = [copies.inside(attention.out_t, saved[0]), copies.inside(attention.lse, saved[1])]
    contracts = [copies.plan(contract.at[s], contract_out.at[z], to) for to in lines]

    def to_head(d):
        return pltpu.make_async_remote_copy(
            src_ref=outgoing.at[d],
            dst_ref=qkv.at[:, :, s],
            send_sem=head_send.at[d],
            recv_sem=head_recv.at[d],
            device_id=(z, lax.rem(s + 1 + d, 8)),
            device_id_type=MESH,
        )

    go(gather.loads + [load, load_upstream])
    small[z] = jnp.zeros(small.shape[1:], bf16)
    for n, item in enumerate(vectors):
        small[z, n, : item.shape[0], :] = item[...]
    greet(lines + plane)
    for t in first:
        gather.start(t)
    for t in first:
        gather.pass_on(t)
    go(seqs + vector_copies)
    gather.keep()
    load.wait()
    for t in range(len(first) + 2):
        if t < len(first):
            gather.exchange(t)
        if 0 <= t - 1 < len(first):
            gather.spread(t - 1)
        if 0 <= t - 2:
            gather.share(t - 2)
    load_upstream.wait()
    keep_upstream.start()
    arrive(seqs + vector_copies)
    for t in later:
        gather.start(t)
    values_of[...] = small[...].astype(f32)

    gain, shift = row_of(values_of, 0, wide), row_of(values_of, 1, wide)

    def norm(i, _):
        values = held[i // parts, i % parts].astype(f32)
        rows = pl.ds(pl.multiple_of(i * piece, piece), piece)
        normed[rows, :] = normalize(values, gain, shift).astype(bf16)
        return 0

    lax.fori_loop(0, own_seqs * parts, norm, 0)
    for t in first:
        gather.complete(t)
    go(keeping)

    def project(d, _):
        rank = lax.rem(s + 1 + d, 8)
        per = 8 // 4
        query_bias = values_of[rank // per, 2, pl.ds(rank % per, 1), :]
        value_bias = values_of[rank // per, 3, pl.ds(rank % per, 1), :]
        low = lax.broadcasted_iota(jnp.int32, query_bias.shape, 1) < width
        bias = jnp.concatenate(
            [
                jnp.where(low, query_bias, 0.0),
                jnp.where(low, value_bias, query_bias),
                jnp.where(low, 0.0, value_bias),
            ],
            axis=1,
        )
        weight = joined[:, :, :, columns_of(rank, 3 * features)].reshape(wide, 3 * features)
        made = (matmul(normed[...], weight) + bias).astype(bf16)
        outgoing[d] = made.reshape(outgoing.shape[1:])
        pl.when(d < 7)(lambda: to_head(d).start())
        return 0

    lax.fori_loop(0, 8, project, 0)
    own_copy = copies.inside(outgoing.at[7], qkv.at[:, :, s])
    own_copy.start()
    base = later[0]
    gather.exchange(base)
    gather.exchange(base + 1)
    own_copy.wait()
    gather.spread(base)
    go(contracts)
    for d in range(7):
        to_head(d).wait_recv()
    keep_qkv.start()
    attention.run(
        {
            0: [(gather.exchange, base + 2), (gather.spread, base + 1)],
            1: [(go, upstreams)],
            2: [(gather.spread, base + 2), (gather.share, base)],
            5: [(gather.share, base + 1)],
            6: [(gather.share, base + 2)],
        },
        back.each,
    )
    go(keep_saved)
    for t in later:
        gather.complete(t)
    arrive(contracts + upstreams)
    back.finish()
    for d in range(7):
        to_head(d).wait_send()
    copies.finish()
    done(gather.own + [keep_upstream, keep_qkv] + keep_saved + keeping)


def forward_fused(tokens, upstream, vectors, weights, contract, slopes, heads, width):
    seqs, piece, features = tokens.shape
    parts = 4
    own = seqs // parts
    columns = heads * width
    length = parts * 8 * piece
    vectors = [item.reshape(-1, 128) for item in vectors]
    cut = [split_weight(item) for item in weights]
    contract = split_weight(contract)
    count, tall = len(cut), 8 * -(-max(item.shape[0] for item in vectors) // 8)
    chunks = []
    for t, pieces in enumerate((3, 1, 2)):
        chunks += chunks_of(t, *cut[t].shape[1:], pieces)
    seq_shape = (own, parts, piece, features)
    qkv_shape = (own, parts, 8, piece, 3 * columns)
    small = (parts, len(vectors), tall, 128)
    out = remote_call(
        functools.partial(forward_fused_kernel, heads, width, count, len(vectors), chunks),
        "forward_fused",
        1,
        out_shape=(
            jax.ShapeDtypeStruct(seq_shape, bf16),
            jax.ShapeDtypeStruct(small, bf16),
            jax.ShapeDtypeStruct((parts, *cut[0].shape), bf16),
            jax.ShapeDtypeStruct(qkv_shape, bf16),
            jax.ShapeDtypeStruct(seq_shape, bf16),
            *saved_shapes(own, length, heads, width),
            jax.ShapeDtypeStruct(seq_shape, bf16),
            jax.ShapeDtypeStruct((parts, *contract.shape[1:]), bf16),
            *[jax.ShapeDtypeStruct((parts, *item.shape), bf16) for item in cut[1:]],
        ),
        in_specs=[SMEM, HBM, HBM] + [VMEM] * len(vectors) + [HBM] * (count + 1),
        out_specs=(HBM,) * (8 + count),
        scratch_shapes=[
            pltpu.VMEM(seq_shape, bf16),
            pltpu.VMEM(small, bf16),
            pltpu.VMEM(small, f32),
            pltpu.VMEM((parts, *cut[0].shape), bf16),
            pltpu.VMEM((own * parts * piece, features), bf16),
            pltpu.VMEM((8, own, parts, piece, 3 * columns), bf16),
            pltpu.VMEM(qkv_shape, bf16),
            pltpu.VMEM((own, parts, 8, piece, columns), bf16),
            pltpu.VMEM((own, piece, features), bf16),
            *[pltpu.VMEM(item.shape, f32) for item in saved_shapes(own, length, heads, width)],
            *forward_scratch(length, heads, width),
            *[pltpu.VMEM(item.shape, bf16) for item in cut[1:]],
            pltpu.SemaphoreType.DMA((7,)),
            pltpu.SemaphoreType.DMA((7,)),
            *hand_back_semaphores(own * parts),
            *semaphores(12 + 3 + len(chunks) * Gather.copies_each, 2 * count - 1 + 10),
        ],
    )(
        slopes,
        tokens.reshape(parts, own, piece, features),
        upstream.reshape(parts, own, piece, features),
        *vectors,
        *cut,
        contract,
    )
    wholes = [
        whole.reshape(4 * item.shape[0], item.shape[1])
        for whole, item in zip((out[2], *out[9:]), weights)
    ]
    return out[0], out[1], [*wholes, out[8]], out[3], out[4], (out[5], out[6]), out[7]


def feed_forward_kernel(
    chunks, expand, contract, contract_line, out_weight,
    small, upstream_in, tokens_in, attended_in,
    layer_out, residual_out, diff_out, expand_grad, out_grad, contract_grad,
    bias_grad, gain_grad, shift_grad, out_bias_grad, contract_bias_grad,
    upstream, tokens, attended, layer, residual_grad, attended_diff, values_of, expand_bias, expand_in, contract_in, residual, second, second_t, expanded, activated, grad, staged, *refs,
):
    second_back = residual_grad
    bufs, refs = refs[:11], refs[11:]
    loaded, stored, refs = refs[0], refs[1], refs[2:]
    copies = Copies(*refs)
    place = Place()
    z = place.z
    given = [
        copies.inside(a, b)
        for a, b in ((attended_in, attended), (tokens_in, tokens), (upstream_in, upstream))
    ]
    keep_layer = copies.inside(layer, layer_out)
    keep_residual = copies.inside(residual_grad, residual_out)
    keep_diff = copies.inside(attended_diff, diff_out)
    reduce = ReduceLines(place, grad, contract_grad, bufs, copies)
    gather = Gather(
        place, [contract], [contract_in], [None], chunks, copies, given=contract_line
    )
    rows, features = second.shape
    steps = 8
    wide = expand.shape[1] // steps

    def at(n):
        part = paired(z, 3 - n // 2)
        return part, n % 2, pl.ds(pl.multiple_of((2 * part + n % 2) * wide, wide), wide)

    def load(n):
        _, _, where = at(n)
        return pltpu.make_async_copy(expand.at[:, where], expand_in.at[:, where], loaded.at[n])

    def contract_at(n):
        part, side, _ = at(n)
        return contract_in[part, pl.ds(4 * side, 4)].reshape(wide, features)

    def store(n):
        _, _, where = at(n)
        slot = n % 2
        return pltpu.make_async_copy(
            staged.at[slot], expand_grad.at[:, where], stored.at[slot]
        )

    halves = [pl.ds(0, wide), pl.ds(wide, wide)]
    out_loads = [
        pltpu.make_async_copy(out_weight.at[:, half], staged.at[n], stored.at[n])
        for n, half in enumerate(halves)
    ]
    out_stores = [
        pltpu.make_async_copy(staged.at[n], out_grad.at[:, half], stored.at[n])
        for n, half in enumerate(halves)
    ]
    part_rows = rows // 8

    def rows_at(i):
        return pl.ds(pl.multiple_of(i * part_rows, part_rows), part_rows)

    for n in range(len(chunks)):
        gather.start(n)
    go(given[:2] + out_loads + given[2:])
    for n in range(steps):
        load(n).start()
    go(gather.loads)
    greet(place.near)
    for n in range(len(chunks)):
        gather.exchange(n)
    values_of[...] = small[...].astype(f32)
    out_bias, gain, shift, contract_bias = [
        row_of(values_of, n, features) for n in (4, 5, 6, 7)
    ]
    expand_bias[...] = row_of(values_of, 8, steps * wide)
    done(given)
    for n, half in enumerate(halves):
        out_loads[n].wait()
        bias = out_bias[:, n * wide : (n + 1) * wide]
        residual[:, half] = (
            tokens[:, half].astype(f32) + (matmul(attended[...], staged[n]) + bias)
        )

    def norm(i, _):
        values = residual[rows_at(i), :]
        second[rows_at(i), :] = normalize(values, gain, shift).astype(bf16)
        second_back[rows_at(i), :] = values + contract_bias
        return 0

    lax.fori_loop(0, 8, norm, 0)
    for n in range(len(chunks) - 1):
        gather.spread(n)
    second_t[...] = second[...].T

    def forward(n, after):
        part, side, where = at(n)
        load(n).wait()
        values = matmul(second[...], expand_in[:, where]) + expand_bias[:, where]
        expanded[:, where] = values
        low = gelu_tanh(values).astype(bf16)
        activated[:, where] = low
        made = matmul(low.T, upstream[...]).astype(bf16)
        grad[part, pl.ds(2 * side, 2)] = made.reshape(2, 2, wide // 4, features)
        follow(n, after)
        return 0

    def shrink(n, after):
        where = pl.ds(pl.multiple_of(n * (features // 4), 128), features // 4)
        weight = contract_in[:, :, :, where].reshape(steps * wide, features // 4)
        second_back[:, where] += matmul(activated[...], weight)
        follow(n, after)
        return 0

    def backward(n, after):
        _, _, where = at(n)
        values = expanded[:, where]
        act_grad = matmul_rt(upstream[...], contract_at(n))
        bent = jnp.tanh(gelu_coef * (values + 0.044715 * values * values * values))
        slope = 0.5 * (1.0 + bent) + 0.5 * values * (1.0 - bent * bent) * (
            gelu_coef * (1.0 + 3.0 * 0.044715 * values * values)
        )
        diff = (act_grad * slope).astype(bf16)
        bias_grad[:, where] = jnp.sum(diff.astype(f32), axis=0, keepdims=True)
        pl.when(n >= 2)(lambda: store(n - 2).wait())
        staged[n % 2] = matmul(second_t[...], diff).astype(bf16)
        store(n).start()
        second_back[...] += matmul_rt(diff, expand_in[:, where])
        follow(n, after)
        return 0

    last = len(chunks) - 1
    forward_steps = {
        0: [(gather.spread, last)],
        1: [(reduce.start, 0)],
        3: [(reduce.exchange, 0), (reduce.start, 1)],
        5: [(reduce.start, 2), (reduce.exchange, 1)],
        7: [(reduce.start, 3), (reduce.exchange, 2)] + [(gather.share, n) for n in range(last)],
    }
    shrink_steps = {
        0: [(reduce.exchange, 3)],
        1: [(reduce.spread, 0)],
        3: [(reduce.spread, 1)],
    }
    backward_steps = {
        1: [(reduce.spread, 2)],
        2: [(reduce.spread, 3)],
        3: [(reduce.send, 0), (reduce.own_spread,)],
        4: [(reduce.send, 1)],
        5: [(reduce.send, 2)],
        6: [(reduce.send, 3), (reduce.own_send,)],
    }
    lax.fori_loop(0, steps, lambda n, _: forward(n, forward_steps), 0)
    gather.share(last)
    for n in range(len(chunks)):
        gather.complete(n)
    done(gather.loads)
    lax.fori_loop(0, 4, lambda n, _: shrink(n, shrink_steps), 0)
    layer[...] = second_back[...].astype(bf16).reshape(layer.shape)
    keep_layer.start()
    second_back[...] = jnp.zeros_like(second_back)
    lax.fori_loop(0, steps, lambda n, _: backward(n, backward_steps), 0)
    store(steps - 2).wait()
    store(steps - 1).wait()
    go(out_loads)
    second_t[...] = attended[...].T

    def norm_back(i, sums):
        back = second_back[rows_at(i), :]
        part, normal = normalize_back(residual[rows_at(i), :], back, gain)
        given = upstream[rows_at(i), :].astype(f32)
        total = given + part
        low = total.astype(bf16)
        residual_grad[rows_at(i), :] = total
        second[rows_at(i), :] = low
        found = (back * normal, back, low.astype(f32), given)
        return tuple(
            kept + jnp.sum(item, axis=0, keepdims=True) for kept, item in zip(sums, found)
        )

    nothing = jnp.zeros((1, features), f32)
    sums = lax.fori_loop(0, 8, norm_back, (nothing,) * 4)
    gain_grad[...], shift_grad[...], out_bias_grad[...], contract_bias_grad[...] = sums
    keep_residual.start()
    done(out_loads)
    branch_diff = second
    made = matmul_rt(branch_diff[:, halves[0]], staged[0])
    made = (made + matmul_rt(branch_diff[:, halves[1]], staged[1])).astype(bf16)
    attended_diff[...] = made.reshape(attended_diff.shape)
    keep_diff.start()
    for n, half in enumerate(halves):
        staged[n] = matmul(second_t[...], branch_diff[:, half]).astype(bf16)
        out_stores[n].start()
    reduce.finish()
    done(out_stores + [keep_layer, keep_residual, keep_diff])
    copies.finish()


def feed_forward(shape, expand, contract, line, out_weight, tokens, upstream, attended, small):
    own, parts, piece = shape
    rows, features = tokens.shape
    hidden = expand.shape[1]
    wide = hidden // 8
    each = hidden // 32
    contract = split_weight(contract)
    chunks = chunks_of(0, *contract.shape[1:], 2)
    seq_shape = (own, parts, piece, features)
    return remote_call(
        functools.partial(feed_forward_kernel, chunks),
        "feed_forward",
        4,
        out_shape=(
            jax.ShapeDtypeStruct(seq_shape, bf16),
            jax.ShapeDtypeStruct((rows, features), f32),
            jax.ShapeDtypeStruct(seq_shape, bf16),
            jax.ShapeDtypeStruct((features, hidden), bf16),
            jax.ShapeDtypeStruct((features, features), bf16),
            jax.ShapeDtypeStruct((each, features), f32),
            jax.ShapeDtypeStruct((1, hidden), f32),
            *[jax.ShapeDtypeStruct((1, features), f32)] * 4,
        ),
        in_specs=[HBM] * 4 + [VMEM] + [HBM] * 3,
        out_specs=(HBM,) * 5 + (VMEM,) * 6,
        scratch_shapes=[
            *[pltpu.VMEM((rows, features), bf16)] * 3,
            pltpu.VMEM(seq_shape, bf16),
            pltpu.VMEM((rows, features), f32),
            pltpu.VMEM(seq_shape, bf16),
            pltpu.VMEM(small.shape, f32),
            pltpu.VMEM((1, hidden), f32),
            pltpu.VMEM((features, hidden), bf16),
            pltpu.VMEM((4, *contract.shape), bf16),
            pltpu.VMEM((rows, features), f32),
            pltpu.VMEM((rows, features), bf16),
            pltpu.VMEM((features, rows), bf16),
            pltpu.VMEM((rows, hidden), f32),
            pltpu.VMEM((rows, hidden), bf16),
            pltpu.VMEM((4, 4, 2, each, features), bf16),
            pltpu.VMEM((2, features, wide), bf16),
            *reduce_lines_scratch(each, features, features // 4),
            pltpu.SemaphoreType.DMA((8,)),
            pltpu.SemaphoreType.DMA((2,)),
            *semaphores(
                ReduceLines.copies + len(chunks) * (Gather.copies_each - 3),
                7 + 3 * len(chunks),
            ),
        ],
    )(expand, contract, line, out_weight, small, upstream, tokens, attended)


def backward_fused_kernel(heads, width, count, chunks, *refs):
    slopes, diff_in, qkv_in, out_t_in, lse_in, layer = refs[:6]
    grads, refs = refs[6 : 6 + count], refs[6 + count :]
    joined_out, layer_out, layer_own = refs[0], refs[1], refs[2 + count]
    outs, refs = refs[2 : 2 + count], refs[3 + count :]
    diff, qkv, out_t, lse, joined = refs[:5]
    attention = Backward(heads, width, slopes, qkv, diff, out_t, lse, joined, *refs[5:12])
    bufs, refs = refs[12 : 12 + 7 * len(chunks)], refs[12 + 7 * len(chunks) :]
    copies = Copies(*refs[3:])
    place = Place()
    s, plane = place.s, place.plane
    attention.head = s * heads
    features = heads * width
    along = ReduceAlong(place, grads[0], outs[0], bufs[:7], chunks[0], copies)
    reduce = Reduce(place, grads, outs, bufs[7:], chunks[1:], copies)
    back = HandBack(place, joined, joined_out, 3 * features, *refs[:3])

    own = [copies.inside(diff_in.at[:, :, :, columns_of(s, features)], diff.at[:, :, s])]
    own += [copies.inside(a, b) for a, b in ((qkv_in, qkv), (out_t_in, out_t), (lse_in, lse))]
    arriving = [
        copies.plan(diff_in.at[:, :, :, columns_of(to[1], features)], diff.at[:, :, s], to)
        for to in plane
    ]
    returned = [copies.plan(layer.at[:, to[0]], layer_out.at[place.z], to) for to in place.lines]
    load_layer = copies.inside(layer.at[:, place.z], layer_own)
    keep_layer = copies.inside(layer_own, layer_out.at[place.z])
    go(own + reduce.loads + [along.load, load_layer])
    greet(place.lines + plane)
    go(arriving + [along.first])
    reduce.start()
    along.exchange()
    go(returned)
    for t in range(3):
        reduce.exchange(t)
    done(own + [load_layer])
    keep_layer.start()
    arrive(arriving)
    attention.run(
        {
            1: [(reduce.spread, 0)],
            2: [(along.spread,)],
            3: [(reduce.spread, 1), (reduce.spread, 2)],
            4: [(reduce.send, 0), (along.send,)],
            5: [(reduce.send, 1)],
            6: [(reduce.send, 2)],
        },
        back.each,
    )
    for t in range(3):
        reduce.finish(t)
    along.finish()
    back.finish()
    arrive(returned)
    copies.finish()
    keep_layer.wait()


def backward_fused(attended_diff, qkv, saved, layer, grads, slopes, heads, width):
    own, parts, piece, columns = attended_diff.shape
    features = heads * width
    length = parts * 8 * piece
    cut = [split_grad(item) for item in grads]
    count = len(cut)
    rows, wide = cut[0].shape[3:]
    early, part = 5 * wide // 16, 11 * wide // 32
    chunks = [
        (0, 0, rows, 0, early),
        (0, 0, rows, early, part),
        (0, 0, rows, early + part, part),
        *chunks_of(1, *cut[1].shape[3:], 1),
    ]
    out = remote_call(
        functools.partial(backward_fused_kernel, heads, width, count, chunks),
        "backward_fused",
        2,
        out_shape=(
            jax.ShapeDtypeStruct((own, parts, piece, 24 * features), bf16),
            jax.ShapeDtypeStruct((parts, own, piece, columns), bf16),
            *[jax.ShapeDtypeStruct(item.shape[3:], f32) for item in cut],
        ),
        in_specs=[SMEM] + [HBM] * (5 + count),
        out_specs=(HBM, HBM) + (VMEM,) * count,
        scratch_shapes=[
            pltpu.VMEM((own, piece, columns), bf16),
            pltpu.VMEM((own, parts, 8, piece, features), bf16),
            pltpu.VMEM(qkv.shape, bf16),
            *[pltpu.VMEM(item.shape, f32) for item in saved],
            pltpu.VMEM(qkv.shape, bf16),
            *backward_scratch(length, heads, width),
            *reduce_along_scratch(chunks[0]),
            *reduce_scratch(chunks[1:]),
            *hand_back_semaphores(own * parts),
            *semaphores(10 + len(chunks) * Reduce.copies_each, len(chunks) + 6),
        ],
    )(slopes, attended_diff, qkv, *saved, layer, *cut)
    return out[0], out[1].reshape(parts * own, piece, columns), out[2:]


def end_kernel(
    width, joined_diff, joined_weight, tokens_in, residual_in, small, out_bias_grad,
    second_gain_grad, second_shift_grad, contract_bias_grad, expand_bias_grad,
    input_out, vector_out, out,
    tokens, residual_grad, values_of, diff_in, weight_in, normed, normed_t, back, grads, held,
    vectors, others, ranks, *refs,
):
    count = grads.shape[0]
    bufs, refs = refs[: 7 * count], refs[7 * count :]
    loaded, copies = refs[0], Copies(*refs[1:])
    place = Place()
    z, lines, plane = place.z, place.lines, place.plane
    rows, features = tokens.shape
    own_seqs, parts, piece, _ = held.shape
    columns = [pl.ds(features * n, features) for n in range(count)]
    chunks = [(n, 0, grads.shape[4], 0, features) for n in range(count)]
    outs = [out.at[:, where] for where in columns]
    reduce = Reduce(place, [grads.at[n] for n in range(count)], outs, bufs, chunks, copies)
    loads = [
        (
            pltpu.make_async_copy(joined_diff.at[:, c], diff_in.at[:, c], loaded.at[0, n]),
            pltpu.make_async_copy(joined_weight.at[:, c], weight_in.at[:, c], loaded.at[1, n]),
        )
        for n, c in enumerate(columns)
    ]
    returned = [copies.plan(held.at[:, to[0]], input_out.at[z], to) for to in lines]
    stay = copies.inside(held.at[:, z], input_out.at[z])
    along = [copies.plan(vectors.at[to[0]], others.at[k], to) for k, to in enumerate(lines)]
    across = [copies.plan(ranks.at[0], ranks.at[d + 1], to) for d, to in enumerate(plane)]

    given_loads = [copies.inside(tokens_in, tokens), copies.inside(residual_in, residual_grad)]
    for load in loads:
        go(load)
    go(given_loads)
    values_of[...] = small[...].astype(f32)
    gain, shift = row_of(values_of, 0, features), row_of(values_of, 1, features)
    greet(lines + plane)
    for n, where in enumerate(columns):
        done(loads[n])
        part = matmul_rt(diff_in[:, where], weight_in[:, where])
        back[...] = part if n == 0 else back[...] + part

    def norm_back(i, sums):
        at = pl.ds(pl.multiple_of(i * piece, piece), piece)
        values, given = tokens[at, :].astype(f32), back[at, :]
        part, normal = normalize_back(values, given, gain)
        normed[at, :] = (normal * gain + shift).astype(bf16)
        total = (residual_grad[at, :] + part).astype(bf16)
        held[i // parts, i % parts] = total
        found = (given * normal, given)
        return tuple(
            kept + jnp.sum(item, axis=0, keepdims=True) for kept, item in zip(sums, found)
        )

    done(given_loads)
    nothing = jnp.zeros((1, features), f32)
    gain_grad, shift_grad = lax.fori_loop(0, own_seqs * parts, norm_back, (nothing, nothing))
    go(returned + [stay])
    normed_t[...] = normed[...].T
    sums = []
    for n, where in enumerate(columns):
        made = matmul(normed_t[...], diff_in[:, where]).astype(bf16)
        grads[n] = made.reshape(grads.shape[1:])
        reduce.begin(n)
        sums.append(jnp.sum(diff_in[:, where].astype(f32), axis=0, keepdims=True))
        if n > 0:
            reduce.exchange(n - 1)

    sums = jnp.concatenate(sums, axis=1)
    low = lax.broadcasted_iota(jnp.int32, (1, 128), 1) < width
    query_grad, value_grad = [], []
    for r in range(features // 128):
        first, middle, last = [sums[:, (3 * r + n) * 128 : (3 * r + n + 1) * 128] for n in range(3)]
        query_grad.append(jnp.where(low, first, middle))
        value_grad.append(jnp.where(low, middle, last))
    given = [
        gain_grad, shift_grad, jnp.concatenate(query_grad, axis=1),
        jnp.concatenate(value_grad, axis=1), out_bias_grad[...], second_gain_grad[...],
        second_shift_grad[...], contract_bias_grad[...], expand_bias_grad[...],
    ]
    row = 0
    for item in given:
        each = item.shape[1] // 512
        for k in range(4):
            for r in range(each):
                start = (k * each + r) * 128
                vectors[k, row + r : row + r + 1, :] = item[:, start : start + 128]
        row += each
    go(along)
    reduce.spread(0)
    reduce.exchange(count - 1)
    arrive(along)
    total = vectors[z]
    for k in range(3):
        total = total + others[k]
    ranks[0] = total
    go(across)
    for n in range(1, count):
        reduce.send(n - 1)
        reduce.spread(n)
    reduce.send(count - 1)
    arrive(across)
    total = ranks[0]
    for d in range(1, 8):
        total = total + ranks[d]
    vector_out[...] = total
    for n in range(count):
        reduce.finish(n)
    arrive(returned)
    copies.finish()
    stay.wait()


def end(shape, joined_diff, joined_weight, tokens, residual_grad, small, vectors, width):
    own, parts, piece = shape
    rows, features = tokens.shape
    count = joined_diff.shape[1] // features
    each = features // 32
    tall = (4 * features + sum(item.shape[1] for item in vectors)) // 512
    chunks = [(n, 0, each, 0, features) for n in range(count)]
    out = remote_call(
        functools.partial(end_kernel, width),
        "end",
        3,
        out_shape=(
            jax.ShapeDtypeStruct((parts, own, piece, features), bf16),
            jax.ShapeDtypeStruct((tall, 128), f32),
            jax.ShapeDtypeStruct((each, count * features), f32),
        ),
        in_specs=[HBM] * 4 + [VMEM] * (1 + len(vectors)),
        out_specs=(HBM, VMEM, VMEM),
        scratch_shapes=[
            pltpu.VMEM((rows, features), bf16),
            pltpu.VMEM((rows, features), f32),
            pltpu.VMEM(small.shape, f32),
            pltpu.VMEM((rows, count * features), bf16),
            pltpu.VMEM((features, count * features), bf16),
            pltpu.VMEM((rows, features), bf16),
            pltpu.VMEM((features, rows), bf16),
            pltpu.VMEM((rows, features), f32),
            pltpu.VMEM((count, 4, 4, 2, each, features), bf16),
            pltpu.VMEM((own, parts, piece, features), bf16),
            pltpu.VMEM((4, tall, 128), f32),
            pltpu.VMEM((3, tall, 128), f32),
            pltpu.VMEM((8, tall, 128), f32),
            *reduce_scratch(chunks),
            pltpu.SemaphoreType.DMA((2, count)),
            *semaphores(3 + 3 + 7 + count * Reduce.copies_each, 3 + count),
        ],
    )(joined_diff, joined_weight, tokens, residual_grad, small, *vectors)
    return out[0].reshape(parts * own, piece, features), out[1], out[2]


def hand_out_kernel(sizes, vector, *refs):
    count = (len(refs) - len(sizes) - 1) // 3
    arrays, outs, smalls = refs[:count], refs[count : 2 * count], refs[2 * count :]
    smalls, kept, sems = smalls[: len(sizes)], smalls[len(sizes) : -1], refs[-1]
    s = lax.axis_index("sp")
    loads = [pltpu.make_async_copy(a, k, sems.at[n]) for n, (a, k) in enumerate(zip(arrays, kept))]
    stores = [
        pltpu.make_async_copy(k, o, sems.at[count + n]) for n, (k, o) in enumerate(zip(kept, outs))
    ]
    go(loads)
    row = 0
    for out, size in zip(smalls, sizes):
        per = 128 // size
        found = vector[pl.ds(row + s // per, 1), :]
        if per > 1:
            found = pltpu.roll(found, lax.rem(128 - s % per * size, 128), 1)
        out[...] = found[:, :size]
        row += 8 // per
    for load, store in zip(loads, stores):
        load.wait()
        store.start()
    done(stores)


def hand_out(vector, sizes, arrays):
    out = pl.pallas_call(
        functools.partial(hand_out_kernel, sizes),
        name="hand_out",
        out_shape=(
            *[jax.ShapeDtypeStruct(item.shape, item.dtype) for item in arrays],
            *[jax.ShapeDtypeStruct((1, size), f32) for size in sizes],
        ),
        in_specs=[VMEM] + [HBM] * len(arrays),
        out_specs=(HBM,) * len(arrays) + (VMEM,) * len(sizes),
        scratch_shapes=[
            *[pltpu.VMEM(item.shape, item.dtype) for item in arrays],
            pltpu.SemaphoreType.DMA((2 * len(arrays),)),
        ],
        compiler_params=pltpu.CompilerParams(vmem_limit_bytes=vmem_bytes),
    )(vector, *arrays)
    return out[: len(arrays)], [item.reshape(-1) for item in out[len(arrays) :]]


def per_device(
    layer_input,
    first_gain,
    first_shift,
    joined_weight,
    query_bias,
    value_bias,
    output_weight,
    output_bias,
    second_gain,
    second_shift,
    expand_weight,
    expand_bias,
    contract_weight,
    contract_bias,
    alibi_slopes,
    upstream,
):
    seqs, piece, features = layer_input.shape
    fs_count = lax.axis_size("fs")
    sp_count = lax.axis_size("sp")
    head_count = alibi_slopes.shape[0]
    width = features // head_count
    heads = head_count // sp_count
    rows = seqs * piece
    own = seqs // fs_count
    shape = (own, fs_count, piece)

    vectors = (
        first_gain, first_shift, query_bias, value_bias, output_bias,
        second_gain, second_shift, contract_bias, expand_bias,
    )
    fast = (fs_count, sp_count) == (4, 8) and (own, heads, width) == (2, 2, 64)
    fast = fast and expand_weight.shape[1] == 4 * features
    if fast:
        weights = (joined_weight, output_weight, expand_weight)
        tokens, small, weights, qkv, attended, saved, upstream_low = forward_fused(
            layer_input, upstream, vectors, weights, contract_weight, alibi_slopes, heads, width
        )
        joined_full, out_full, expand_full, contract_line = weights
        tokens = tokens.reshape(rows, features)
        (
            layer_output, residual_grad, attended_diff, expand_grad, output_weight_grad,
            contract_grad, eb, g2, s2, ob, cb,
        ) = feed_forward(
            shape, expand_full, contract_weight, contract_line, out_full, tokens,
            upstream_low.reshape(rows, features), attended.reshape(rows, features), small,
        )
        joined_diff, layer_output, grads = backward_fused(
            attended_diff, qkv, saved, layer_output, (expand_grad, output_weight_grad),
            alibi_slopes, heads, width,
        )
        input_grad, vector, joined_grad = end(
            shape, joined_diff.reshape(rows, 3 * features), joined_full, tokens, residual_grad,
            small, (ob, g2, s2, cb, eb), width,
        )
        devices = fs_count * sp_count
        sizes = [4 * item.shape[0] // devices for item in vectors]
        arrays, (g1, s1, qb, vb, ob, g2, s2, cb, eb) = hand_out(
            vector, sizes, (layer_output, input_grad, joined_grad, grads[1], grads[0], contract_grad)
        )
        layer_output, input_grad, joined_grad, output_grad, expand_grad, contract_grad = arrays
        return (
            layer_output, input_grad, g1, s1, joined_grad, qb, vb, output_grad, ob, g2, s2,
            expand_grad, eb, contract_grad, cb,
        )

    slopes = lax.dynamic_slice_in_dim(alibi_slopes, lax.axis_index("sp") * heads, heads)
    gather = lambda item: lax.all_gather(item, "fs", axis=0, tiled=True)
    scatter = functools.partial(
        lax.psum_scatter, axis_name=("fs", "sp"), scatter_dimension=0, tiled=True
    )
    gain_one, shift_one, qbias, vbias, obias, gain_two, shift_two, cbias, ebias = [
        gather(item).astype(f32) for item in vectors
    ]
    joined_full, out_full, expand_full, contract_full = [
        gather(item) for item in (joined_weight, output_weight, expand_weight, contract_weight)
    ]
    tokens = to_own_seqs(layer_input).reshape(rows, features).astype(f32)
    upstream_low = to_own_seqs(upstream).reshape(rows, features)

    normed_f, norm_back_one = jax.vjp(normalize, tokens, gain_one, shift_one)
    normed = normed_f.astype(bf16)
    joined_bias = joined_bias_of(qbias, vbias, head_count)
    joined_all = (matmul(normed, joined_full) + joined_bias).astype(bf16)
    qkv = to_heads(joined_all.reshape(*shape, 3 * features))
    attended, *saved = attention_forward(qkv, slopes, heads, width)
    attended = from_heads(attended).reshape(rows, features)
    upstream_f = upstream_low.astype(f32)
    contract_bias_grad = jnp.sum(upstream_f, axis=0)
    residual = tokens + (matmul(attended, out_full) + obias)
    second_f, norm_back_two = jax.vjp(normalize, residual, gain_two, shift_two)
    second = second_f.astype(bf16)
    expanded = matmul(second, expand_full) + ebias
    activated_f, gelu_back = jax.vjp(gelu_tanh, expanded)
    activated = activated_f.astype(bf16)
    result = residual + (matmul(activated, contract_full) + cbias)
    layer_output = result.astype(bf16).reshape(*shape, features)

    contract_grad = matmul_lt(activated, upstream_low)
    act_grad = matmul_rt(upstream_low, contract_full)
    expand_diff = gelu_back(act_grad)[0].astype(bf16)
    expand_grad = matmul_lt(second, expand_diff)
    expand_bias_grad = jnp.sum(expand_diff.astype(f32), axis=0)
    second_back = matmul_rt(expand_diff, expand_full)
    resid_part, second_gain_grad, second_shift_grad = norm_back_two(second_back)
    residual_grad = upstream_f + resid_part

    branch_diff = residual_grad.astype(bf16)
    output_weight_grad = matmul_lt(attended, branch_diff)
    output_bias_grad = jnp.sum(branch_diff.astype(f32), axis=0)
    attended_diff = matmul_rt(branch_diff, out_full).astype(bf16)
    attended_diff = attended_diff.reshape(*shape, features)
    joined_diff = attention_backward(qkv, to_heads(attended_diff), *saved, slopes, heads, width)
    joined_diff = from_heads(joined_diff).reshape(rows, 3 * features)
    joined_grad = matmul_lt(normed, joined_diff)
    column_sums = jnp.sum(joined_diff.astype(f32), axis=0).reshape(head_count, 3, width)
    query_bias_grad = column_sums[:, 0].reshape(features)
    value_bias_grad = column_sums[:, 2].reshape(features)
    normed_back = matmul_rt(joined_diff, joined_full)
    input_part, first_gain_grad, first_shift_grad = norm_back_one(normed_back)
    input_grad = (residual_grad + input_part).astype(bf16).reshape(*shape, features)

    vector_grads = (
        first_gain_grad, first_shift_grad, query_bias_grad, value_bias_grad,
        output_bias_grad, second_gain_grad, second_shift_grad, contract_bias_grad,
        expand_bias_grad,
    )
    devices = fs_count * sp_count
    packed = jnp.concatenate([item.reshape(devices, -1) for item in vector_grads], axis=1)
    packed = scatter(packed.reshape(-1))
    own_grads, at = [], 0
    for item in vector_grads:
        size = item.shape[0] // devices
        own_grads.append(packed[at : at + size])
        at += size
    g1, s1, qb, vb, ob, g2, s2, cb, eb = own_grads
    return (
        from_own_seqs(layer_output), from_own_seqs(input_grad), g1, s1, scatter(joined_grad), qb,
        vb, scatter(output_weight_grad), ob, g2, s2, scatter(expand_grad), eb,
        scatter(contract_grad), cb,
    )


def solution(mesh):
    tokens = P(None, ("fs", "sp"), None)
    both, both_rows = P(("fs", "sp")), P(("fs", "sp"), None)
    one, one_rows = P("fs"), P("fs", None)
    return jax.shard_map(
        per_device,
        mesh=mesh,
        in_specs=(
            tokens, one, one, one_rows, one, one, one_rows, one, one, one, one_rows, one,
            one_rows, one, P(), tokens,
        ),
        out_specs=(
            tokens, tokens, both, both, both_rows, both, both, both_rows, both, both, both,
            both_rows, both, both_rows, both,
        ),
        check_vma=False,
    )
```
